128 devices in a mesh: dp: 16 (over z, y), fsdp: 8 (over x, core).
Axes of the slice: x: 4, y: 4, z: 4, core: 2. Of those that a mesh axis runs over, the one named last changes fastest.
Arguments:
- x_in: bfloat16 [128, 256, 768], P(('dp', 'fsdp'))
- grad_y: bfloat16 [128, 256, 768], P(('dp', 'fsdp'))
- norm_scale: bfloat16 [2, 768], P(None, 'fsdp')
- w_in: bfloat16 [2, 768, 7040], P(None, 'fsdp')
- w_out: bfloat16 [2, 3840, 768], P(None, 'fsdp')
Outputs:
- output 1: bfloat16 [128, 256, 768], P(('dp', 'fsdp'))
- output 2: bfloat16 [128, 256, 768], P(('dp', 'fsdp'))
- output 3: float32 [2, 768], P(None, 'fsdp')
- output 4: float32 [2, 768, 7040], P(None, 'fsdp')
- output 5: float32 [2, 3840, 768], P(None, 'fsdp')
All inputs are finite; a program needn't handle non-finite values.
Results may differ from the reference program's by a relative error of at most 0.0145081.
Values are sent between devices in bfloat16 or wider.
A program may use at most 1 GiB of HBM per device.

```python
import jax
import jax.numpy as jnp
from jax import lax

MODEL_DIM = 768
N_HEADS = 12
HEAD_DIM = 64
FF_DIM = 3072
SEQ_LEN = 256
BATCH = 128
N_LAYERS = 2

PROJ_DIM = MODEL_DIM + 2 * HEAD_DIM + 2 * FF_DIM
CAT_DIM = MODEL_DIM + FF_DIM


def setup_inputs(seed: int = 0) -> dict:
    rng_keys = jax.random.split(jax.random.key(seed), 5)
    x_in = jax.random.normal(rng_keys[0], (BATCH, SEQ_LEN, MODEL_DIM), jnp.float32)
    grad_y = jax.random.normal(rng_keys[1], (BATCH, SEQ_LEN, MODEL_DIM), jnp.float32)
    norm_scale = 1.0 + 0.3 * jax.random.normal(rng_keys[2], (N_LAYERS, MODEL_DIM), jnp.float32)
    w_in = jax.random.normal(rng_keys[3], (N_LAYERS, MODEL_DIM, PROJ_DIM), jnp.float32) * MODEL_DIM ** -0.5
    w_out = jax.random.normal(rng_keys[4], (N_LAYERS, CAT_DIM, MODEL_DIM), jnp.float32) * CAT_DIM ** -0.5
    return {
        "x_in": x_in.astype(jnp.bfloat16),
        "grad_y": grad_y.astype(jnp.bfloat16),
        "norm_scale": norm_scale.astype(jnp.bfloat16),
        "w_in": w_in.astype(jnp.bfloat16),
        "w_out": w_out.astype(jnp.bfloat16),
    }


def layer_norm(hidden, gain_vec):
    hid_f32 = hidden.astype(jnp.float32)
    centered = hid_f32 - jnp.mean(hid_f32, axis=-1, keepdims=True)
    variance = jnp.mean(centered * centered, axis=-1, keepdims=True)
    return (centered * lax.rsqrt(variance + 1e-6) * gain_vec).astype(jnp.bfloat16)


def rotary_tables():
    half_dim = HEAD_DIM // 2
    inv_freq = 10000.0 ** (-(jnp.arange(half_dim, dtype=jnp.float32) * 2.0 / HEAD_DIM))
    angles = jnp.arange(SEQ_LEN, dtype=jnp.float32)[:, None] * inv_freq[None, :]
    return jnp.cos(angles), jnp.sin(angles)


def rotate(vectors, cos_tab, sin_tab):
    half_dim = vectors.shape[-1] // 2
    lo_half = vectors[..., :half_dim]
    hi_half = vectors[..., half_dim:]
    return jnp.concatenate([lo_half * cos_tab - hi_half * sin_tab, hi_half * cos_tab + lo_half * sin_tab], axis=-1)


def mix_seq(projected):
    kv_end = MODEL_DIM + 2 * HEAD_DIM
    queries = projected[:, :MODEL_DIM].reshape(SEQ_LEN, N_HEADS, HEAD_DIM).astype(jnp.float32) * HEAD_DIM ** -0.5
    key_vec = projected[:, MODEL_DIM:MODEL_DIM + HEAD_DIM].astype(jnp.float32)
    val_vec = projected[:, MODEL_DIM + HEAD_DIM:kv_end].astype(jnp.float32)
    gate_act = projected[:, kv_end:kv_end + FF_DIM].astype(jnp.float32)
    up_act = projected[:, kv_end + FF_DIM:].astype(jnp.float32)
    cos_tab, sin_tab = rotary_tables()
    q_rot = rotate(queries, cos_tab[:, None, :], sin_tab[:, None, :]).astype(jnp.bfloat16).astype(jnp.float32)
    k_rot = rotate(key_vec, cos_tab, sin_tab).astype(jnp.bfloat16).astype(jnp.float32)
    scores = jnp.einsum("qhd,kd->hqk", q_rot, k_rot)
    positions = jnp.arange(SEQ_LEN)
    scores = jnp.where(positions[:, None] >= positions[None, :], scores, -1e30)
    attn_probs = jax.nn.softmax(scores, axis=-1).astype(jnp.bfloat16).astype(jnp.float32)
    attn_out = jnp.einsum("hqk,kd->qhd", attn_probs, val_vec).astype(jnp.bfloat16).reshape(SEQ_LEN, MODEL_DIM)
    mlp_out = (jax.nn.silu(gate_act) * up_act).astype(jnp.bfloat16)
    return jnp.concatenate([attn_out, mlp_out], axis=-1)


def mix_backward(seq_pair):
    projected, grad_mixed = seq_pair
    return jax.vjp(mix_seq, projected)[1](grad_mixed)[0]


def layer_forward(hidden, gain_vec, w_in_l, w_out_l):
    normed = layer_norm(hidden, gain_vec.astype(jnp.float32))
    projected = jnp.dot(normed.reshape(-1, MODEL_DIM), w_in_l, preferred_element_type=jnp.float32).astype(jnp.bfloat16)
    projected = projected.reshape(BATCH, SEQ_LEN, PROJ_DIM)
    mixed_out = lax.map(mix_seq, projected)
    block_out = jnp.dot(mixed_out.reshape(-1, CAT_DIM), w_out_l, preferred_element_type=jnp.float32)
    layer_out = (hidden.astype(jnp.float32) + block_out.reshape(BATCH, SEQ_LEN, MODEL_DIM)).astype(jnp.bfloat16)
    return layer_out, normed, projected, mixed_out


def layer_backward(hidden, gain_vec, w_in_l, w_out_l, grad_out):
    normed, projected, mixed_out = layer_forward(hidden, gain_vec, w_in_l, w_out_l)[1:]
    grad_rows = grad_out.reshape(-1, MODEL_DIM)
    grad_w_out = jnp.dot(mixed_out.reshape(-1, CAT_DIM).T, grad_rows, preferred_element_type=jnp.float32)
    grad_mixed = jnp.dot(grad_rows, w_out_l.T, preferred_element_type=jnp.float32).astype(jnp.bfloat16)
    grad_proj = lax.map(mix_backward, (projected, grad_mixed.reshape(BATCH, SEQ_LEN, CAT_DIM)))
    grad_proj_rows = grad_proj.reshape(-1, PROJ_DIM)
    grad_w_in = jnp.dot(normed.reshape(-1, MODEL_DIM).T, grad_proj_rows, preferred_element_type=jnp.float32)
    grad_normed = jnp.dot(grad_proj_rows, w_in_l.T, preferred_element_type=jnp.float32).astype(jnp.bfloat16)
    norm_vjp = jax.vjp(layer_norm, hidden, gain_vec.astype(jnp.float32))[1]
    grad_hidden, grad_gain = norm_vjp(grad_normed.reshape(BATCH, SEQ_LEN, MODEL_DIM))
    grad_in = (grad_out.astype(jnp.float32) + grad_hidden.astype(jnp.float32)).astype(jnp.bfloat16)
    return grad_in, grad_gain, grad_w_in, grad_w_out


def reference(x_in, grad_y, norm_scale, w_in, w_out):
    layer_inputs = []
    hidden = x_in
    for layer_idx in range(N_LAYERS):
        layer_inputs.append(hidden)
        hidden = layer_forward(hidden, norm_scale[layer_idx], w_in[layer_idx], w_out[layer_idx])[0]
    grad_hidden = grad_y
    scale_grads = []
    in_grads = []
    out_grads = []
    for layer_idx in reversed(range(N_LAYERS)):
        grad_hidden, grad_gain, grad_w_in, grad_w_out = layer_backward(
            layer_inputs[layer_idx], norm_scale[layer_idx], w_in[layer_idx], w_out[layer_idx], grad_hidden)
        scale_grads.append(grad_gain)
        in_grads.append(grad_w_in)
        out_grads.append(grad_w_out)
    return (hidden, grad_hidden, jnp.stack(scale_grads[::-1]), jnp.stack(in_grads[::-1]), jnp.stack(out_grads[::-1]))
```

```python
import functools
import jax
import jax.numpy as jnp
from jax import lax
from jax.experimental import pallas as pl
from jax.experimental.pallas import tpu as pltpu
from jax.sharding import PartitionSpec as P

MESH_ID = pl.DeviceIdType.MESH
BOTH = (1, -1)
AROUND = (1, -1, 2)
PARTS = (True, False)


class Links:
    def __init__(self, send_sems, recv_sems):
        self.send_sems, self.recv_sems = send_sems, recv_sems
        self.slots, self.sent = {}, []

    def _slot(self, key):
        return self.slots.setdefault(key, len(self.slots))

    def send(self, key, src, dst, device):
        slot = self._slot(key)
        copy = pltpu.make_async_remote_copy(
            src_ref=src, dst_ref=dst, send_sem=self.send_sems.at[slot], recv_sem=self.recv_sems.at[slot],
            device_id=device, device_id_type=MESH_ID)
        copy.start()
        self.sent.append(copy)

    def arrive(self, key, landed, device):
        slot = self._slot(key)
        pltpu.make_async_remote_copy(
            src_ref=landed, dst_ref=landed, send_sem=self.send_sems.at[slot], recv_sem=self.recv_sems.at[slot],
            device_id=device, device_id_type=MESH_ID).wait_recv()

    def drain(self):
        for copy in self.sent:
            copy.wait_send()


def rem(a, n):
    return a % n if isinstance(a, int) else lax.rem(a, n)


def chip_position():
    f, d = lax.axis_index("fsdp"), lax.axis_index("dp")
    return f // 2, rem(d, 4), d // 4, rem(f, 2)


def device_at(x, y, z, core):
    return (z * 4 + y, x * 2 + core)


def step(coord, by):
    return rem(coord + 4 + by, 4)


def announce(devices):
    barrier = pltpu.get_barrier_semaphore()
    for device in devices:
        pl.semaphore_signal(barrier, inc=1, device_id=device, device_id_type=MESH_ID)
    pl.semaphore_wait(barrier, len(devices))


def plan(tasks, latency=2.5):
    free, landed, order, now = {}, {}, [], 0.0
    left = list(tasks)
    while left:
        best = None
        for place, (name, rank, start, needs, after, sends) in enumerate(left):
            if all(n[0] in landed for n in needs) and all(n in landed for n in after):
                ready = max([start, now] + [landed[task][i] for task, i in needs])
                best = min(best or (ready, rank, place), (ready, rank, place))
        now, _, place = best
        name, _, _, _, _, sends = left.pop(place)
        order.append(name)
        now += 0.2
        landed[name] = []
        for link, cost in sends:
            free[link] = max(now, free.get(link, 0.0)) + cost
            landed[name].append(free[link] + latency)
    return order


def gather_order(rows_i, cols_i, rows_o, cols_o, starts):
    rate = 23300.0
    tasks = []
    for m in range(4):
        is_in = m % 2 == 0
        edge = cols_i // 128 * 4 // 9 // 2 * 256
        size = {"y": rows_i // 4 * edge, "x": rows_i * (cols_i - 2 * edge)} if is_in else {"y": rows_o // 4 * cols_o // 2}
        size["z"] = size["y"]
        for color in "yzx" if is_in else "yz":
            cost = size[color] / rate
            both = [(("x", by), cost) for by in BOTH]
            spread = [((color, by), cost) for by in BOTH] if color != "x" else []
            tasks.append((("reach", m, color), m, starts[m], [], [], both))
            for i, by in enumerate(BOTH):
                tasks.append((("relay", m, color, by), m, 0.0, [(("reach", m, color), i)], [], [(("x", by), cost / 2)] + spread))
            halves = [(("relay", m, color, by), 0) for by in BOTH]
            tasks.append((("far", m, color), m, 0.0, halves, [], spread))
            if color == "x":
                continue
            for off, source, first in ((-1, ("relay", m, color, 1), 1), (1, ("relay", m, color, -1), 1), (2, ("far", m, color), 0)):
                for i, by in enumerate(BOTH):
                    tasks.append((("pass", m, color, off, by), m, 0.0, [(source, first + i)], [], [((color, by), cost / 2)]))
                halves = [(("pass", m, color, off, by), 0) for by in BOTH]
                tasks.append((("close", m, color, off), m, 0.0, halves, [], []))
        for off in (-1, 1, 2):
            last = [("close", m, color, off) for color in "yz"]
            if is_in:
                last.append(("far", m, "x") if off == 2 else ("relay", m, "x", -off))
            tasks.append((("hand", m, off), m, 0.0, [], last, []))
    return plan(tasks)


def gather_kernel(order, sc_in, wi_in, wo_in, sc_out, wi_a, wo_a, wi_b, wo_b, own_i, own_o, ssem, rsem, lsem):
    x, y, z, core = chip_position()
    here = device_at(x, y, z, core)
    twin = device_at(x, y, z, 1 - core)
    rows_i, cols_i = wi_in.shape[1:]
    rows_o, cols_o = wo_in.shape[1:]
    quarter_i, quarter_o = rows_i // 4, rows_o // 4
    third_i = cols_i // 128 * 4 // 9 // 2 * 256
    half_o = cols_o // 2
    cut_o = quarter_o // 16 * 8 + 8 if quarter_o % 16 else quarter_o // 2
    place = {"x": x, "y": y, "z": z}

    def peer(axis, by):
        moved = dict(place)
        moved[axis] = step(place[axis], by)
        return device_at(moved["x"], moved["y"], moved["z"], core)

    peers = [peer(axis, by) for axis in "xyz" for by in BOTH]
    others = [(lax.axis_index("dp"), lax.rem(lax.axis_index("fsdp") + k, 8)) for k in range(1, 8)]
    announce(others + peers[2:])
    links = Links(ssem, rsem)

    mats = []
    for layer, (wi, wo) in enumerate(((wi_a, wo_a), (wi_b, wo_b))):
        mats.append((wi_in.at[layer], wi, own_i.at[layer], True))
        mats.append((wo_in.at[layer], wo, own_o.at[layer], False))

    def region(is_in, color, q):
        if is_in:
            if color == "x":
                lo, hi = 2 * third_i, cols_i
                rows = (0, rows_i)
            else:
                lo, hi = (0, third_i) if color == "y" else (third_i, 2 * third_i)
                rows = (q * quarter_i, quarter_i)
            mid = lo + ((hi - lo) // 128 + 1) // 2 * 128
            return (rows, (lo, hi - lo)), (rows, (lo, mid - lo)), (rows, (mid, hi - mid))
        cols = (0, half_o) if color == "y" else (half_o, half_o)
        start = q * quarter_o
        return ((start, quarter_o), cols), ((start, cut_o), cols), ((start + cut_o, quarter_o - cut_o), cols)

    def at(ref, lead, area):
        (r, nr), (c, nc) = area
        if not isinstance(r, int):
            r = pl.multiple_of(r, 8)
        return ref.at[(*lead, pl.ds(r, nr), pl.ds(c, nc))]

    def colors(m):
        return "yzx" if mats[m][3] else "yz"

    def reach(m, color):
        src, out, _, is_in = mats[m]
        area = region(is_in, color, place[color])[0]
        for by in BOTH:
            links.send((m, "x1", color, by), at(src, (), area), at(out, (x, core), area), peer("x", by))

    def launch(m, color, off):
        _, out, _, is_in = mats[m]
        block = at(out, (step(x, off), core), region(is_in, color, place[color])[0])
        for by in BOTH:
            links.send((m, "p1", color, off, by), block, block, peer(color, by))

    def relay(m, color, by):
        _, out, _, is_in = mats[m]
        xb = step(x, -by)
        areas = region(is_in, color, place[color])
        links.arrive((m, "x1", color, by), at(out, (xb, core), areas[0]), peer("x", -by))
        part = at(out, (xb, core), areas[1] if by == 1 else areas[2])
        links.send((m, "x2", color, by), part, part, peer("x", by))
        if color != "x":
            launch(m, color, -by)

    def far(m, color):
        _, out, _, is_in = mats[m]
        areas = region(is_in, color, place[color])
        for by in BOTH:
            links.arrive((m, "x2", color, by), at(out, (step(x, 2), core), areas[1] if by == 1 else areas[2]), peer("x", -by))
        if color != "x":
            launch(m, color, 2)

    def pass_on(m, color, off, by):
        _, out, _, is_in = mats[m]
        xb = step(x, off)
        areas = region(is_in, color, step(place[color], -by))
        links.arrive((m, "p1", color, off, by), at(out, (xb, core), areas[0]), peer(color, -by))
        part = at(out, (xb, core), areas[1] if by == 1 else areas[2])
        links.send((m, "p2", color, off, by), part, part, peer(color, by))

    def close(m, color, off):
        _, out, _, is_in = mats[m]
        areas = region(is_in, color, step(place[color], 2))
        for by in BOTH:
            links.arrive((m, "p2", color, off, by), at(out, (step(x, off), core), areas[1] if by == 1 else areas[2]), peer(color, -by))

    def hand(m, off):
        _, out, _, _ = mats[m]
        links.send((m, "d2d", off), out.at[step(x, off), core], out.at[step(x, off), core], twin)

    stages = {"reach": reach, "relay": relay, "far": far, "pass": pass_on, "close": close, "hand": hand}

    loads = []
    for m, (src, out, own, _) in enumerate(mats):
        load = pltpu.make_async_copy(src, own, lsem.at[0, m])
        load.start()
        loads.append(load)
    for k, device in enumerate(others):
        links.send(("sc", k), sc_in, sc_out.at[lax.axis_index("fsdp")], device)
    for m, (src, out, own, _) in enumerate(mats):
        links.send((m, "d2d", 0), src, out.at[x, core], twin)
    stores = []
    for m, (src, out, own, _) in enumerate(mats):
        loads[m].wait()
        store = pltpu.make_async_copy(own, out.at[x, core], lsem.at[1, m])
        store.start()
        stores.append(store)
    own_scale = pltpu.make_async_copy(sc_in, sc_out.at[lax.axis_index("fsdp")], lsem.at[2, 0])
    own_scale.start()
    for kind, *task in order:
        stages[kind](*task)
    for m, (src, out, own, _) in enumerate(mats):
        for off in (0, -1, 1, 2):
            xb = step(x, off)
            links.arrive((m, "d2d", off), out.at[xb, 1 - core], twin)
        stores[m].wait()
    own_scale.wait()
    for k in range(7):
        source = lax.rem(lax.axis_index("fsdp") + 7 - k, 8)
        links.arrive(("sc", k), sc_out.at[source], others[k])
    links.drain()


def gather_weights(scale_tile, w_in, w_out, starts=None, n_copies=320):
    any_space = pl.BlockSpec(memory_space=pl.ANY)
    wi = jax.ShapeDtypeStruct((4, 2, *w_in.shape[1:]), w_in.dtype)
    wo = jax.ShapeDtypeStruct((4, 2, *w_out.shape[1:]), w_out.dtype)
    return pl.pallas_call(
        functools.partial(gather_kernel, gather_order(*w_in.shape[1:], *w_out.shape[1:], starts or (0, 0, 0, 0))),
        out_shape=(jax.ShapeDtypeStruct((8, *scale_tile.shape), scale_tile.dtype), wi, wo, wi, wo),
        in_specs=[any_space] * 3,
        out_specs=[any_space] * 5,
        scratch_shapes=[
            pltpu.VMEM(w_in.shape, w_in.dtype),
            pltpu.VMEM(w_out.shape, w_out.dtype),
            pltpu.SemaphoreType.DMA((n_copies,)),
            pltpu.SemaphoreType.DMA((n_copies,)),
            pltpu.SemaphoreType.DMA((3, 4)),
        ],
        compiler_params=pltpu.CompilerParams(collective_id=0, has_side_effects=True, vmem_limit_bytes=12 * 2 ** 20),
        name="gather_weights",
    )(scale_tile, w_in, w_out)


FLOW_AXES = {"x": "yz", "y": "zx", "z": "xy"}
FLOWS = (("x", 1), ("x", -1), ("z", 1), ("z", -1), ("y", 1), ("y", -1))
GROUPS = (("yz", (0, 1, 2)), ("zy", (3, 4, 5)))


def block_of(ref, is_in, color, b, width, base):
    cols = pl.ds(base, width if color == "z" and is_in else width * (4 if is_in else 1))
    if is_in:
        if color == "x":
            return ref.at[b, :, :, cols]
        if color == "y":
            return ref.at[:, b, :, cols]
        return ref.at[:, :, :, pl.ds(pl.multiple_of(base + b * width, 128) if not isinstance(b, int) else base + b * width, width)]
    if color == "x":
        return ref.at[b, :, :, :, cols]
    if color == "y":
        return ref.at[:, b, :, :, cols]
    return ref.at[:, :, b, :, cols]


def second(ref, is_in, color, b, width):
    if is_in:
        if color == "y":
            return ref.at[:, :, pl.ds(pl.multiple_of(b * width, 128) if not isinstance(b, int) else b * width, width)]
        return ref.at[b]
    return ref.at[:, b] if color == "y" else ref.at[b]


def third(ref, is_in, color, b, width):
    if is_in and color == "x":
        return ref.at[:, pl.ds(pl.multiple_of(b * width, 128) if not isinstance(b, int) else b * width, width)]
    return ref.at[b]


def reduce_kernel(widths, order, *refs):
    n = 2
    ga, gb = refs[0:n], refs[n:2 * n]
    oa, ob = refs[2 * n:3 * n], refs[3 * n:4 * n]
    (wx, wy, wz, wb, rx, ry, rz, rb, sx, sy, sz, sb, tx, ty, tz, tb, fa, fb, ssem, rsem, lsem, osem) = refs[4 * n:]
    x, y, z, core = chip_position()
    place = {"x": x, "y": y, "z": z}
    work = {"x": wx, "y": wy, "z": wz}
    ring1 = {"x": rx, "y": ry, "z": rz}
    ring2 = {"x": sx, "y": sy, "z": sz}
    last = {"x": tx, "y": ty, "z": tz}
    bases = [sum(widths[:k]) * 4 for k in range(6)]

    def peer(axis, by):
        moved = dict(place)
        moved[axis] = step(place[axis], by)
        return device_at(moved["x"], moved["y"], moved["z"], core)

    announce([peer(axis, by) for axis in "xyz" for by in AROUND])
    links = Links(ssem, rsem)
    local = {}

    def buf(table, flat, l, k, slot, is_in):
        color, by = FLOWS[k]
        return table[color].at[l, (1 - by) // 2, slot] if is_in else flat.at[l, k, slot]

    def load(l, k, is_in, b, dst, tag):
        color, _ = FLOWS[k]
        src = block_of((ga if is_in else gb)[l], is_in, color, b, widths[k] if is_in else 128, bases[k] if is_in else 128 * k)
        copy = pltpu.make_async_copy(src, dst, lsem.at[l, k, 0 if is_in else 1, tag])
        copy.start()
        local[l, k, is_in, tag] = copy

    def p1(l, k, s, is_in):
        color, by = FLOWS[k]
        a = place[color]
        width = widths[k] if is_in else 128
        base = bases[k] if is_in else 128 * k
        r = [buf(ring1, rb, l, k, i, is_in) for i in range(3)]
        w = [buf(work, wb, l, k, i, is_in) for i in range(2)]
        if s == 0:
            src = block_of((ga if is_in else gb)[l], is_in, color, step(a, -by), width, base)
            links.send((l, k, is_in, "p1", 0), src, r[0], peer(color, by))
            load(l, k, is_in, step(a, -2 * by), w[1], 0)
            load(l, k, is_in, step(a, -3 * by), w[0], 1)
            return
        mine = (None, w[1], w[0], r[0])[s]
        links.arrive((l, k, is_in, "p1", s - 1), r[s - 1], peer(color, -by))
        local[l, k, is_in, s - 1].wait()
        add_into(mine, r[s - 1])
        if s < 3:
            links.send((l, k, is_in, "p1", s), mine, r[s], peer(color, by))
            if s == 1:
                load(l, k, is_in, a, r[0], 2)
        else:
            p2(l, k, 0, is_in)

    def p2(l, k, s, is_in):
        color, by = FLOWS[k]
        axis = FLOW_AXES[color][0]
        a = place[axis]
        width = widths[k] if is_in else 128
        total = buf(ring1, rb, l, k, 0, is_in)
        r = [buf(ring2, sb, l, k, i, is_in) for i in range(3)]
        mine = second(total, is_in, color, step(a, -by * (1 + s)), width)
        if s:
            links.arrive((l, k, is_in, "p2", s - 1), r[s - 1], peer(axis, -by))
            add_into(mine, r[s - 1])
        if s < 3:
            links.send((l, k, is_in, "p2", s), mine, r[s], peer(axis, by))
        else:
            axis = FLOW_AXES[color][1]
            for slot, o in enumerate(AROUND):
                part = third(mine, is_in, color, step(place[axis], o), width)
                links.send((l, k, is_in, "p3", o), part, buf(last, tb, l, k, slot, is_in), peer(axis, o))

    def final(l, k, is_in):
        return (fa.at[l, :, pl.ds(sum(widths[:k]), widths[k])] if is_in else fb.at[l, :, pl.ds(128 * k, 128)])

    def p3(l, k, is_in):
        color, by = FLOWS[k]
        axis2, axis3 = FLOW_AXES[color]
        width = widths[k] if is_in else 128
        t = [buf(last, tb, l, k, i, is_in) for i in range(3)]
        for slot, o in enumerate(AROUND):
            links.arrive((l, k, is_in, "p3", o), t[slot], peer(axis3, -o))
        mine = third(second(buf(ring1, rb, l, k, 0, is_in), is_in, color, place[axis2], width), is_in, color, place[axis3], width)
        final(l, k, is_in)[...] = (mine[...] + t[0][...]) + (t[1][...] + t[2][...])

    def pieces(l, g, p, q):
        _, flows = GROUPS[g]
        out = []
        for k in flows:
            lo = bases[k] + q * widths[k]
            lo = lo if isinstance(lo, int) else pl.multiple_of(lo, 128)
            out.append(oa[l].at[p, :, pl.ds(lo, widths[k])])
        out.append(ob[l].at[p, q, :, pl.ds(128 * flows[0], 128 * len(flows))])
        return out

    def fronts(l, g):
        _, flows = GROUPS[g]
        out = [fa.at[l, :, pl.ds(sum(widths[:k]), widths[k])] for k in flows]
        out.append(fb.at[l, :, pl.ds(128 * flows[0], 128 * len(flows))])
        return out

    def line(l, g, at2, part):
        order2, flows = GROUPS[g]
        along = slice(None) if part is None else pl.ds(2 * part, 2)
        out = []
        for k in flows:
            if order2 == "yz":
                lo = bases[k] + at2 * widths[k]
                lo = lo if isinstance(lo, int) else pl.multiple_of(lo, 128)
                out.append(oa[l].at[along, :, pl.ds(lo, widths[k])])
            else:
                span = 4 * widths[k] if part is None else 2 * widths[k]
                out.append(oa[l].at[at2, :, pl.ds(bases[k] + (part or 0) * 2 * widths[k], span)])
        cols = pl.ds(128 * flows[0], 128 * len(flows))
        out.append(ob[l].at[along, at2, :, cols] if order2 == "yz" else ob[l].at[at2, along, :, cols])
        return out

    def ag(l, g, s, is_in):
        first, then = GROUPS[g][0]
        own = [place[first], place[then]]
        mine = range(3) if is_in else (3,)

        def spot(i, j):
            return pieces(l, g, i, j) if first == "y" else pieces(l, g, j, i)

        forward = (1, 1, -1, -1) if g == 0 else (1, 1, 1, -1)
        if s == 0:
            src, dst = fronts(l, g), spot(own[0], own[1])
            for i in mine:
                for by in BOTH:
                    links.send((l, g, "a1", i, by), src[i], dst[i], peer(first, by))
                copy = pltpu.make_async_copy(src[i], dst[i], osem.at[l, g, i])
                copy.start()
                local[l, g, i] = copy
        elif s == 1:
            for by in BOTH:
                landed = spot(step(own[0], -by), own[1])
                for i in mine:
                    links.arrive((l, g, "a1", i, by), landed[i], peer(first, -by))
                    if forward[i] == by:
                        links.send((l, g, "b1", i), landed[i], landed[i], peer(first, by))
        elif s == 2:
            landed = spot(step(own[0], 2), own[1])
            part = line(l, g, own[1], None)
            for i in mine:
                local[l, g, i].wait()
                links.arrive((l, g, "b1", i), landed[i], peer(first, -forward[i]))
                for by in BOTH:
                    links.send((l, g, "a2", i, by), part[i], part[i], peer(then, by))
        elif s == 3:
            for by in BOTH:
                at2 = step(own[1], -by)
                whole, half = line(l, g, at2, None), line(l, g, at2, (1 - by) // 2)
                for i in mine:
                    links.arrive((l, g, "a2", i, by), whole[i], peer(then, -by))
                    links.send((l, g, "a3", i, by), half[i], half[i], peer(then, by))
        else:
            at2 = step(own[1], 2)
            for by in BOTH:
                half = line(l, g, at2, (1 - by) // 2)
                for i in mine:
                    links.arrive((l, g, "a3", i, by), half[i], peer(then, -by))

    stages = {"p1": p1, "p2": p2, "p3": lambda l, k, s, is_in: p3(l, k, is_in), "ag": ag}

    for kind, *task in order:
        stages[kind](*task)
    links.drain()


def add_into(dst, src):
    lead = dst.shape[:-2]
    if len(lead) == 2:
        @pl.loop(0, lead[0])
        def _(i):
            for j in range(lead[1]):
                dst[i, j] += src[i, j]
    elif len(lead) == 1:
        @pl.loop(0, lead[0])
        def _(i):
            dst[i] += src[i]
    else:
        dst[...] += src[...]


def reduce_order(widths, rows, rows_b, starts):
    rate = 11650.0
    tasks = []
    for l in range(2):
        for is_in in PARTS:
            for k, (color, by) in enumerate(FLOWS):
                axes = color + FLOW_AXES[color]
                full = 16 * (rows * widths[k] if is_in else rows_b * 128) / rate
                chain = [("p1", l, k, s, is_in) for s in range(4)] + [("p2", l, k, s, is_in) for s in (1, 2, 3)] + [("p3", l, k, 0, is_in)]
                sends = [[((axes[0], by), full)]] * 3 + [[((axes[1], by), full / 4)]] * 3
                sends += [[((axes[2], o), full / 16) for o in (1, -1, 1)], []]
                for i, task in enumerate(chain):
                    needs = [(chain[i - 1], j) for j in range(len(sends[i - 1]))] if i else []
                    tasks.append((task, (l, i - 8), starts[is_in][l] if i == 0 else 0.0, needs, [], sends[i]))
            for g, ((first, then), flows) in enumerate(GROUPS):
                piece = sum(rows * widths[k] if is_in else rows_b * 128 for k in flows) / rate
                for s, (axis, n) in enumerate(((first, 1), (first, 0.5), (then, 4), (then, 2), (None, 0))):
                    needs = [(("ag", l, g, s - 1, is_in), j) for j in (0, 1)] if s else []
                    after = [] if s else [("p3", l, k, 0, is_in) for k in flows]
                    sends = [((axis, by), piece * n) for by in BOTH] if axis else []
                    tasks.append((("ag", l, g, s, is_in), (l, s - 5), 0.0, needs, after, sends))
    return plan(tasks)


def reduce_gradients(ga, gb, widths=(384, 384, 256, 256, 256, 256), starts=None):
    any_space = pl.BlockSpec(memory_space=pl.ANY)
    rows = ga[0].shape[2]
    rows_b = gb[0].shape[3]
    cols = 4 * sum(widths)
    f32 = jnp.float32
    wx, wz, wy = widths[0], widths[2], widths[4]

    def buffers(slots, whole):
        a = {"x": (4, rows, 4 * wx), "y": (4, rows, 4 * wy), "z": (4, 4, rows, wz)}
        b = {"x": (rows, 4 * wx), "y": (4, rows, wy), "z": (4, rows, wz)}
        c = {"x": (rows, wx), "y": (rows, wy), "z": (rows, wz)}
        flat = ((4, 4), (4,), ())[whole]
        per = (a, b, c)[whole]
        return [pltpu.VMEM((2, 2, slots, *per[color]), f32) for color in "xyz"] + [
            pltpu.VMEM((2, 6, slots, *flat, rows_b, 128), f32)]

    oa = jax.ShapeDtypeStruct((4, rows, cols), f32)
    ob = jax.ShapeDtypeStruct((4, 4, rows_b, 768), f32)
    outs = pl.pallas_call(
        functools.partial(reduce_kernel, widths, reduce_order(widths, rows, rows_b, starts or {True: (0, 40), False: (0, 60)})),
        out_shape=(oa, oa, ob, ob),
        in_specs=[any_space] * 4,
        out_specs=[any_space] * 4,
        scratch_shapes=[
            *buffers(2, 0), *buffers(3, 0), *buffers(3, 1), *buffers(3, 2),
            pltpu.VMEM((2, rows, sum(widths)), f32), pltpu.VMEM((2, rows_b, 768), f32),
            pltpu.SemaphoreType.DMA((400,)), pltpu.SemaphoreType.DMA((400,)),
            pltpu.SemaphoreType.DMA((2, 6, 2, 3)), pltpu.SemaphoreType.DMA((2, 2, 4)),
        ],
        compiler_params=pltpu.CompilerParams(collective_id=1, has_side_effects=True, vmem_limit_bytes=60 * 2 ** 20),
        name="reduce_gradients",
    )(*ga, *gb)
    return outs[:2], outs[2:]


def rotary_tables(seq_len, head_dim):
    half_dim = head_dim // 2
    inv_freq = 10000.0 ** (-(jnp.arange(half_dim, dtype=jnp.float32) * 2.0 / head_dim))
    angles = jnp.arange(seq_len, dtype=jnp.float32)[:, None] * inv_freq[None, :]
    return jnp.cos(angles), jnp.sin(angles)


def rotate(vectors, cos_tab, sin_tab):
    half_dim = vectors.shape[-1] // 2
    lo_half = vectors[..., :half_dim]
    hi_half = vectors[..., half_dim:]
    return jnp.concatenate([lo_half * cos_tab - hi_half * sin_tab, hi_half * cos_tab + lo_half * sin_tab], axis=-1)


def layer_norm(hidden, gain_vec):
    hid_f32 = hidden.astype(jnp.float32)
    centered = hid_f32 - jnp.mean(hid_f32, axis=-1, keepdims=True)
    variance = jnp.mean(centered * centered, axis=-1, keepdims=True)
    return (centered * lax.rsqrt(variance + 1e-6) * gain_vec).astype(jnp.bfloat16)


def mix_block(projected, model_dim, ff_dim, head_dim):
    n_batch, seq_len, _ = projected.shape
    n_heads = model_dim // head_dim
    kv_end = model_dim + 2 * head_dim
    queries = projected[..., :model_dim].reshape(n_batch, seq_len, n_heads, head_dim).astype(jnp.float32) * head_dim ** -0.5
    key_vec = projected[..., model_dim:model_dim + head_dim].astype(jnp.float32)
    val_vec = projected[..., model_dim + head_dim:kv_end]
    gate_act = projected[..., kv_end:kv_end + ff_dim].astype(jnp.float32)
    up_act = projected[..., kv_end + ff_dim:].astype(jnp.float32)
    cos_tab, sin_tab = rotary_tables(seq_len, head_dim)
    q_rot = rotate(queries, cos_tab[:, None, :], sin_tab[:, None, :]).astype(jnp.bfloat16)
    k_rot = rotate(key_vec, cos_tab, sin_tab).astype(jnp.bfloat16)
    scores = jnp.einsum("crie,cle->cirl", q_rot, k_rot, preferred_element_type=jnp.float32)
    positions = jnp.arange(seq_len)
    scores = jnp.where(positions[:, None] >= positions[None, :], scores, -1e30)
    attn_probs = jax.nn.softmax(scores, axis=-1).astype(jnp.bfloat16)
    attn_out = jnp.einsum("cirl,cle->crie", attn_probs, val_vec, preferred_element_type=jnp.float32)
    attn_out = attn_out.astype(jnp.bfloat16).reshape(n_batch, seq_len, model_dim)
    mlp_out = (jax.nn.silu(gate_act) * up_act).astype(jnp.bfloat16)
    return jnp.concatenate([attn_out, mlp_out], axis=-1)


def solution(mesh):
    fsdp_size = mesh.shape["fsdp"]
    batch_spec = P(("dp", "fsdp"), None, None)
    scale_spec = P(None, "fsdp")
    weight_spec = P(None, "fsdp", None)
    twins = [(f, f ^ 1) for f in range(fsdp_size)]

    def swap(value):
        return lax.ppermute(value, "fsdp", twins)

    def device_step(x_in, grad_y, norm_scale, w_in, w_out):
        n_layers = w_in.shape[0]
        seq_len, model_dim = x_in.shape[1:]
        proj_dim = w_in.shape[2]
        ff_dim = w_out.shape[1] * fsdp_size - model_dim
        head_dim = (proj_dim - model_dim - 2 * ff_dim) // 2
        core = lax.rem(lax.axis_index("fsdp"), 2)
        rows, rows_out = norm_scale.shape[1], w_out.shape[1]
        scale_tile = jnp.pad(norm_scale.astype(jnp.float32), ((0, 8 - n_layers), (0, 128 - rows)))
        scales, *gathered = gather_weights(scale_tile, w_in, w_out)
        scale_full = scales[:, :n_layers, :rows].transpose(1, 0, 2).reshape(n_layers, model_dim)
        w_in_full = [gathered[0].reshape(model_dim, -1), gathered[2].reshape(model_dim, -1)]
        w_out_full = [gathered[1].reshape(-1, model_dim), gathered[3].reshape(-1, model_dim)]
        mix_fn = functools.partial(mix_block, model_dim=model_dim, ff_dim=ff_dim, head_dim=head_dim)

        def split(value, which):
            parts = value.reshape(seq_len, 4, 2, -1)
            return lax.dynamic_index_in_dim(parts, which, 2, keepdims=False)

        saved_acts = []
        hidden = x_in
        for layer_idx in range(n_layers):
            normed = layer_norm(hidden, scale_full[layer_idx])
            projected = jnp.einsum("bsd,de->bse", normed, w_in_full[layer_idx], preferred_element_type=jnp.float32).astype(jnp.bfloat16)
            mixed_out = mix_fn(projected)
            block_out = jnp.einsum("bsf,fd->bsd", mixed_out, w_out_full[layer_idx], preferred_element_type=jnp.float32)
            saved_acts.append((hidden, normed, projected, mixed_out))
            hidden = (hidden.astype(jnp.float32) + block_out).astype(jnp.bfloat16)
        grad_hidden = grad_y
        in_parts = [None] * n_layers
        out_parts = [None] * n_layers
        for layer_idx in reversed(range(n_layers)):
            layer_in, normed, projected, mixed_out = saved_acts[layer_idx]
            grad_mixed = jnp.einsum("bsd,fd->bsf", grad_hidden, w_out_full[layer_idx], preferred_element_type=jnp.float32).astype(jnp.bfloat16)
            grad_proj = jax.vjp(mix_fn, projected)[1](grad_mixed)[0]
            grad_normed = jnp.einsum("bse,de->bsd", grad_proj, w_in_full[layer_idx], preferred_element_type=jnp.float32).astype(jnp.bfloat16)
            grad_in, part_scale = jax.vjp(layer_norm, layer_in, scale_full[layer_idx])[1](grad_normed)

            def pair(value):
                return jnp.concatenate([split(value, core), swap(split(value, 1 - core))], axis=0)

            def both(value):
                return jnp.concatenate([value, swap(value)], axis=0)

            rows_pair = pair(normed[0]).reshape(2 * seq_len, -1)
            cols_pair = jnp.pad(both(grad_proj[0]), ((0, 0), (0, 128)))
            part_in = lax.dot_general(rows_pair, cols_pair, (((0,), (0,)), ((), ())), preferred_element_type=jnp.float32)
            in_parts[layer_idx] = part_in.reshape(4, 4, rows // 4, proj_dim + 128)
            mixed_pair = jnp.pad(pair(mixed_out[0]), ((0, 0), (0, 0), (0, 32))).reshape(2 * seq_len, -1)
            part_out = lax.dot_general(mixed_pair, both(grad_hidden[0]), (((0,), (0,)), ((), ())), preferred_element_type=jnp.float32)
            part_out = part_out.reshape(4, rows_out + 32, model_dim)
            scale_blocks = part_scale.reshape(4, 2, rows)
            scale_pair = lax.dynamic_index_in_dim(scale_blocks, core, 1) + swap(lax.dynamic_index_in_dim(scale_blocks, 1 - core, 1))
            part_out = lax.dynamic_update_slice(part_out, scale_pair, (0, rows_out, 0))
            out_parts[layer_idx] = part_out.reshape(4, 4, 4, (rows_out + 32) // 16, model_dim)
            grad_hidden = (grad_hidden.astype(jnp.float32) + grad_in.astype(jnp.float32)).astype(jnp.bfloat16)
        in_sums, out_sums = reduce_gradients(in_parts[::-1], out_parts[::-1])
        in_grads = jnp.stack([g.reshape(rows, -1)[:, :proj_dim] for g in in_sums[::-1]])
        out_rows = [g.reshape(-1, model_dim) for g in out_sums[::-1]]
        out_grads = jnp.stack([g[:rows_out] for g in out_rows])
        scale_grads = jnp.stack([g[rows_out, :rows] for g in out_rows])
        return hidden, grad_hidden, scale_grads, in_grads, out_grads

    return jax.shard_map(
        device_step,
        mesh=mesh,
        in_specs=(batch_spec, batch_spec, scale_spec, weight_spec, weight_spec),
        out_specs=(batch_spec, batch_spec, scale_spec, weight_spec, weight_spec),
        check_vma=False,
    )
```

```python
import functools
import jax
import jax.numpy as jnp
from jax import lax
from jax.experimental import pallas as pl
from jax.experimental.pallas import tpu as pltpu
from jax.sharding import PartitionSpec as P

MESH_ID = pl.DeviceIdType.MESH
BOTH = (1, -1)
AROUND = (1, -1, 2)
PARTS = (True, False)
ALL = ...
LANE, WIDE, STRIP, HEAD = 128, 256, 512, 64
ROW, BAND, SIDE, PAIR = 8, 32, 4, 2


class Links:
    def __init__(self, send_sems, recv_sems):
        self.send_sems, self.recv_sems = send_sems, recv_sems
        self.slots, self.sent = {}, []

    def _slot(self, key):
        return self.slots.setdefault(key, len(self.slots))

    def send(self, key, src, dst, device):
        slot = self._slot(key)
        copy = pltpu.make_async_remote_copy(
            src_ref=src, dst_ref=dst, send_sem=self.send_sems.at[slot], recv_sem=self.recv_sems.at[slot],
            device_id=device, device_id_type=MESH_ID)
        copy.start()
        self.sent.append(copy)

    def arrive(self, key, landed, device):
        slot = self._slot(key)
        pltpu.make_async_remote_copy(
            src_ref=landed, dst_ref=landed, send_sem=self.send_sems.at[slot], recv_sem=self.recv_sems.at[slot],
            device_id=device, device_id_type=MESH_ID).wait_recv()

    def drain(self):
        for copy in self.sent:
            copy.wait_send()
        self.sent.clear()


def rem(a, n):
    return a % n if isinstance(a, int) else lax.rem(a, n)


def chip_position():
    f, d = lax.axis_index("fsdp"), lax.axis_index("dp")
    return f // PAIR, rem(d, SIDE), d // SIDE, rem(f, PAIR)


def device_at(x, y, z, core):
    return (z * SIDE + y, x * PAIR + core)


def step(coord, by):
    return rem(coord + SIDE + by, SIDE)


def announce(devices):
    barrier = pltpu.get_barrier_semaphore()
    for device in devices:
        pl.semaphore_signal(barrier, inc=1, device_id=device, device_id_type=MESH_ID)
    pl.semaphore_wait(barrier, len(devices))


def plan(tasks, latency=2.5):
    free, landed, order, now = {}, {}, [], 0.0
    left = list(tasks)
    while left:
        best = None
        for place, (name, rank, start, needs, after, sends) in enumerate(left):
            if all(n[0] in landed for n in needs) and all(n in landed for n in after):
                ready = max([start, now] + [landed[task][i] for task, i in needs])
                best = min(best or (ready, rank, place), (ready, rank, place))
        now, _, place = best
        name, _, _, _, _, sends = left.pop(place)
        order.append(name)
        now += 0.2
        landed[name] = []
        for link, cost in sends:
            free[link] = max(now, free.get(link, 0.0)) + cost
            landed[name].append(free[link] + latency)
    return order


def gather_order(rows_i, cols_i, rows_o, cols_o, starts):
    rate = 23300.0
    tasks = []
    for m in range(SIDE):
        is_in = m % PAIR == 0
        edge = cols_i // LANE * SIDE // 9 // PAIR * WIDE
        size = {"y": rows_i // SIDE * edge, "x": rows_i * (cols_i - PAIR * edge)} if is_in else {"y": rows_o // SIDE * cols_o // PAIR}
        size["z"] = size["y"]
        for color in "yzx" if is_in else "yz":
            cost = size[color] / rate
            both = [(("x", by), cost) for by in BOTH]
            spread = [((color, by), cost) for by in BOTH] if color != "x" else []
            tasks.append((("reach", m, color), m, starts[m], [], [], both))
            for i, by in enumerate(BOTH):
                tasks.append((("relay", m, color, by), m, 0.0, [(("reach", m, color), i)], [], [(("x", by), cost / PAIR)] + spread))
            halves = [(("relay", m, color, by), 0) for by in BOTH]
            tasks.append((("far", m, color), m, 0.0, halves, [], spread))
            if color == "x":
                continue
            for off, source, first in ((-1, ("relay", m, color, 1), 1), (1, ("relay", m, color, -1), 1), (PAIR, ("far", m, color), 0)):
                for i, by in enumerate(BOTH):
                    tasks.append((("pass", m, color, off, by), m, 0.0, [(source, first + i)], [], [((color, by), cost / PAIR)]))
                halves = [(("pass", m, color, off, by), 0) for by in BOTH]
                tasks.append((("close", m, color, off), m, 0.0, halves, [], []))
        for off in (-1, 1, PAIR):
            last = [("close", m, color, off) for color in "yz"]
            if is_in:
                last.append(("far", m, "x") if off == PAIR else ("relay", m, "x", -off))
            tasks.append((("hand", m, off), m, 0.0, [], last, []))
    return plan(tasks)


def gather_kernel(order, sc_in, wi_in, wo_in, sc_out, wi_a, wo_a, wi_b, wo_b, own_i, own_o, ssem, rsem, lsem):
    x, y, z, core = chip_position()
    here = device_at(x, y, z, core)
    twin = device_at(x, y, z, 1 - core)
    rows_i, cols_i = wi_in.shape[1:]
    rows_o, cols_o = wo_in.shape[1:]
    quarter_i, quarter_o = rows_i // SIDE, rows_o // SIDE
    third_i = cols_i // LANE * SIDE // 9 // PAIR * WIDE
    half_o = cols_o // PAIR
    cut_o = quarter_o // 16 * ROW + ROW if quarter_o % 16 else quarter_o // PAIR
    place = {"x": x, "y": y, "z": z}

    def peer(axis, by):
        moved = dict(place)
        moved[axis] = step(place[axis], by)
        return device_at(moved["x"], moved["y"], moved["z"], core)

    peers = [peer(axis, by) for axis in "xyz" for by in BOTH]
    others = [(lax.axis_index("dp"), lax.rem(lax.axis_index("fsdp") + k, ROW)) for k in range(1, ROW)]
    announce(others + peers[PAIR:])
    links = Links(ssem, rsem)

    mats = []
    for layer, (wi, wo) in enumerate(((wi_a, wo_a), (wi_b, wo_b))):
        mats.append((wi_in.at[layer], wi, own_i.at[layer], True))
        mats.append((wo_in.at[layer], wo, own_o.at[layer], False))

    def region(is_in, color, q):
        if is_in:
            if color == "x":
                lo, hi = PAIR * third_i, cols_i
                rows = (0, rows_i)
            else:
                lo, hi = (0, third_i) if color == "y" else (third_i, PAIR * third_i)
                rows = (q * quarter_i, quarter_i)
            mid = lo + ((hi - lo) // LANE + 1) // PAIR * LANE
            return (rows, (lo, hi - lo)), (rows, (lo, mid - lo)), (rows, (mid, hi - mid))
        cols = (0, half_o) if color == "y" else (half_o, half_o)
        start = q * quarter_o
        return ((start, quarter_o), cols), ((start, cut_o), cols), ((start + cut_o, quarter_o - cut_o), cols)

    def at(ref, lead, area):
        (r, nr), (c, nc) = area
        if not isinstance(r, int):
            r = pl.multiple_of(r, ROW)
        return ref.at[(*lead, pl.ds(r, nr), pl.ds(c, nc))]

    def colors(m):
        return "yzx" if mats[m][3] else "yz"

    def reach(m, color):
        src, out, _, is_in = mats[m]
        area = region(is_in, color, place[color])[0]
        for by in BOTH:
            links.send((m, "x1", color, by), at(src, (), area), at(out, (x, core), area), peer("x", by))

    def launch(m, color, off):
        _, out, _, is_in = mats[m]
        block = at(out, (step(x, off), core), region(is_in, color, place[color])[0])
        for by in BOTH:
            links.send((m, "p1", color, off, by), block, block, peer(color, by))

    def relay(m, color, by):
        _, out, _, is_in = mats[m]
        xb = step(x, -by)
        areas = region(is_in, color, place[color])
        links.arrive((m, "x1", color, by), at(out, (xb, core), areas[0]), peer("x", -by))
        part = at(out, (xb, core), areas[1] if by == 1 else areas[PAIR])
        links.send((m, "x2", color, by), part, part, peer("x", by))
        if color != "x":
            launch(m, color, -by)

    def far(m, color):
        _, out, _, is_in = mats[m]
        areas = region(is_in, color, place[color])
        for by in BOTH:
            links.arrive((m, "x2", color, by), at(out, (step(x, PAIR), core), areas[1] if by == 1 else areas[PAIR]), peer("x", -by))
        if color != "x":
            launch(m, color, PAIR)

    def pass_on(m, color, off, by):
        _, out, _, is_in = mats[m]
        xb = step(x, off)
        areas = region(is_in, color, step(place[color], -by))
        links.arrive((m, "p1", color, off, by), at(out, (xb, core), areas[0]), peer(color, -by))
        part = at(out, (xb, core), areas[1] if by == 1 else areas[PAIR])
        links.send((m, "p2", color, off, by), part, part, peer(color, by))

    def close(m, color, off):
        _, out, _, is_in = mats[m]
        areas = region(is_in, color, step(place[color], PAIR))
        for by in BOTH:
            links.arrive((m, "p2", color, off, by), at(out, (step(x, off), core), areas[1] if by == 1 else areas[PAIR]), peer(color, -by))

    def hand(m, off):
        _, out, _, _ = mats[m]
        links.send((m, "d2d", off), out.at[step(x, off), core], out.at[step(x, off), core], twin)

    stages = {"reach": reach, "relay": relay, "far": far, "pass": pass_on, "close": close, "hand": hand}

    loads = []
    for m, (src, out, own, _) in enumerate(mats):
        load = pltpu.make_async_copy(src, own, lsem.at[0, m])
        load.start()
        loads.append(load)
    for k, device in enumerate(others):
        links.send(("sc", k), sc_in, sc_out.at[lax.axis_index("fsdp")], device)
    for m, (src, out, own, _) in enumerate(mats):
        links.send((m, "d2d", 0), src, out.at[x, core], twin)
    stores = []
    for m, (src, out, own, _) in enumerate(mats):
        loads[m].wait()
        store = pltpu.make_async_copy(own, out.at[x, core], lsem.at[1, m])
        store.start()
        stores.append(store)
    own_scale = pltpu.make_async_copy(sc_in, sc_out.at[lax.axis_index("fsdp")], lsem.at[PAIR, 0])
    own_scale.start()
    for kind, *task in order:
        stages[kind](*task)
    for m, (src, out, own, _) in enumerate(mats):
        for off in (0, -1, 1, PAIR):
            xb = step(x, off)
            links.arrive((m, "d2d", off), out.at[xb, 1 - core], twin)
        stores[m].wait()
    own_scale.wait()
    for k in range(7):
        source = lax.rem(lax.axis_index("fsdp") + 7 - k, ROW)
        links.arrive(("sc", k), sc_out.at[source], others[k])
    links.drain()


def gather_weights(scale_tile, w_in, w_out, starts=None, n_copies=320):
    any_space = pl.BlockSpec(memory_space=pl.ANY)
    wi = jax.ShapeDtypeStruct((SIDE, PAIR, *w_in.shape[1:]), w_in.dtype)
    wo = jax.ShapeDtypeStruct((SIDE, PAIR, *w_out.shape[1:]), w_out.dtype)
    return pl.pallas_call(
        functools.partial(gather_kernel, gather_order(*w_in.shape[1:], *w_out.shape[1:], starts or (0, 0, 0, 0))),
        out_shape=(jax.ShapeDtypeStruct((ROW, *scale_tile.shape), scale_tile.dtype), wi, wo, wi, wo),
        in_specs=[any_space] * 3,
        out_specs=[any_space] * 5,
        scratch_shapes=[
            pltpu.VMEM(w_in.shape, w_in.dtype),
            pltpu.VMEM(w_out.shape, w_out.dtype),
            pltpu.SemaphoreType.DMA((n_copies,)),
            pltpu.SemaphoreType.DMA((n_copies,)),
            pltpu.SemaphoreType.DMA((3, SIDE)),
        ],
        compiler_params=pltpu.CompilerParams(collective_id=0, has_side_effects=True, vmem_limit_bytes=12 << 20),
        name="gather_weights",
    )(scale_tile, w_in, w_out)


FLOW_AXES = {"x": "yz", "y": "zx", "z": "xy"}
FLOWS = (("x", 1), ("x", -1), ("z", 1), ("z", -1), ("y", 1), ("y", -1))
GROUPS = (("yz", (0, 1, PAIR)), ("zy", (3, SIDE, 5)))


def block_of(ref, is_in, color, b, width, base):
    cols = pl.ds(base, width if color == "z" and is_in else width * (SIDE if is_in else 1))
    if is_in:
        if color == "x":
            return ref.at[b, :, :, cols]
        if color == "y":
            return ref.at[:, b, :, cols]
        return ref.at[:, :, :, pl.ds(pl.multiple_of(base + b * width, LANE) if not isinstance(b, int) else base + b * width, width)]
    if color == "x":
        return ref.at[b, :, :, :, cols]
    if color == "y":
        return ref.at[:, b, :, :, cols]
    return ref.at[:, :, b, :, cols]


def second(ref, is_in, color, b, width):
    if is_in:
        if color == "y":
            return ref.at[:, :, pl.ds(pl.multiple_of(b * width, LANE) if not isinstance(b, int) else b * width, width)]
        return ref.at[b]
    return ref.at[:, b] if color == "y" else ref.at[b]


def third(ref, is_in, color, b, width):
    if is_in and color == "x":
        return ref.at[:, pl.ds(pl.multiple_of(b * width, LANE) if not isinstance(b, int) else b * width, width)]
    return ref.at[b]


def reduce_kernel(widths, order, *refs):
    n = PAIR
    ga, gb = refs[0:n], refs[n:PAIR * n]
    oa, ob = refs[PAIR * n:3 * n], refs[3 * n:SIDE * n]
    (wx, wy, wz, wb, rx, ry, rz, rb, sx, sy, sz, sb, tx, ty, tz, tb, fa, fb, ssem, rsem, lsem, osem) = refs[SIDE * n:]
    x, y, z, core = chip_position()
    place = {"x": x, "y": y, "z": z}
    work = {"x": wx, "y": wy, "z": wz}
    ring1 = {"x": rx, "y": ry, "z": rz}
    ring2 = {"x": sx, "y": sy, "z": sz}
    last = {"x": tx, "y": ty, "z": tz}
    bases = [sum(widths[:k]) * SIDE for k in range(6)]

    def peer(axis, by):
        moved = dict(place)
        moved[axis] = step(place[axis], by)
        return device_at(moved["x"], moved["y"], moved["z"], core)

    announce([peer(axis, by) for axis in "xyz" for by in AROUND])
    links = Links(ssem, rsem)
    local = {}

    def buf(table, flat, l, k, slot, is_in):
        color, by = FLOWS[k]
        return table[color].at[l, (1 - by) // PAIR, slot] if is_in else flat.at[l, k, slot]

    def load(l, k, is_in, b, dst, tag):
        color, _ = FLOWS[k]
        src = block_of((ga if is_in else gb)[l], is_in, color, b, widths[k] if is_in else LANE, bases[k] if is_in else LANE * k)
        copy = pltpu.make_async_copy(src, dst, lsem.at[l, k, 0 if is_in else 1, tag])
        copy.start()
        local[l, k, is_in, tag] = copy

    def p1(l, k, s, is_in):
        color, by = FLOWS[k]
        a = place[color]
        width = widths[k] if is_in else LANE
        base = bases[k] if is_in else LANE * k
        r = [buf(ring1, rb, l, k, i, is_in) for i in range(3)]
        w = [buf(work, wb, l, k, i, is_in) for i in range(PAIR)]
        if s == 0:
            src = block_of((ga if is_in else gb)[l], is_in, color, step(a, -by), width, base)
            links.send((l, k, is_in, "p1", 0), src, r[0], peer(color, by))
            load(l, k, is_in, step(a, -PAIR * by), w[1], 0)
            load(l, k, is_in, step(a, -3 * by), w[0], 1)
            return
        mine = (None, w[1], w[0], r[0])[s]
        links.arrive((l, k, is_in, "p1", s - 1), r[s - 1], peer(color, -by))
        local[l, k, is_in, s - 1].wait()
        add_into(mine, r[s - 1])
        if s < 3:
            links.send((l, k, is_in, "p1", s), mine, r[s], peer(color, by))
            if s == 1:
                load(l, k, is_in, a, r[0], PAIR)
        else:
            p2(l, k, 0, is_in)

    def p2(l, k, s, is_in):
        color, by = FLOWS[k]
        axis = FLOW_AXES[color][0]
        a = place[axis]
        width = widths[k] if is_in else LANE
        total = buf(ring1, rb, l, k, 0, is_in)
        r = [buf(ring2, sb, l, k, i, is_in) for i in range(3)]
        mine = second(total, is_in, color, step(a, -by * (1 + s)), width)
        if s:
            links.arrive((l, k, is_in, "p2", s - 1), r[s - 1], peer(axis, -by))
            add_into(mine, r[s - 1])
        if s < 3:
            links.send((l, k, is_in, "p2", s), mine, r[s], peer(axis, by))
        else:
            axis = FLOW_AXES[color][1]
            for slot, o in enumerate(AROUND):
                part = third(mine, is_in, color, step(place[axis], o), width)
                links.send((l, k, is_in, "p3", o), part, buf(last, tb, l, k, slot, is_in), peer(axis, o))

    def final(l, k, is_in):
        return (fa.at[l, :, pl.ds(sum(widths[:k]), widths[k])] if is_in else fb.at[l, :, pl.ds(LANE * k, LANE)])

    def p3(l, k, is_in):
        color, by = FLOWS[k]
        axis2, axis3 = FLOW_AXES[color]
        width = widths[k] if is_in else LANE
        t = [buf(last, tb, l, k, i, is_in) for i in range(3)]
        for slot, o in enumerate(AROUND):
            links.arrive((l, k, is_in, "p3", o), t[slot], peer(axis3, -o))
        mine = third(second(buf(ring1, rb, l, k, 0, is_in), is_in, color, place[axis2], width), is_in, color, place[axis3], width)
        final(l, k, is_in)[ALL] = (mine[ALL] + t[0][ALL]) + (t[1][ALL] + t[PAIR][ALL])

    def pieces(l, g, p, q):
        _, flows = GROUPS[g]
        out = []
        for k in flows:
            lo = bases[k] + q * widths[k]
            lo = lo if isinstance(lo, int) else pl.multiple_of(lo, LANE)
            out.append(oa[l].at[p, :, pl.ds(lo, widths[k])])
        out.append(ob[l].at[p, q, :, pl.ds(LANE * flows[0], LANE * len(flows))])
        return out

    def fronts(l, g):
        _, flows = GROUPS[g]
        out = [fa.at[l, :, pl.ds(sum(widths[:k]), widths[k])] for k in flows]
        out.append(fb.at[l, :, pl.ds(LANE * flows[0], LANE * len(flows))])
        return out

    def line(l, g, at2, part):
        order2, flows = GROUPS[g]
        along = slice(None) if part is None else pl.ds(PAIR * part, PAIR)
        out = []
        for k in flows:
            if order2 == "yz":
                lo = bases[k] + at2 * widths[k]
                lo = lo if isinstance(lo, int) else pl.multiple_of(lo, LANE)
                out.append(oa[l].at[along, :, pl.ds(lo, widths[k])])
            else:
                span = SIDE * widths[k] if part is None else PAIR * widths[k]
                out.append(oa[l].at[at2, :, pl.ds(bases[k] + (part or 0) * PAIR * widths[k], span)])
        cols = pl.ds(LANE * flows[0], LANE * len(flows))
        out.append(ob[l].at[along, at2, :, cols] if order2 == "yz" else ob[l].at[at2, along, :, cols])
        return out

    def ag(l, g, s, is_in):
        first, then = GROUPS[g][0]
        own = [place[first], place[then]]
        mine = range(3) if is_in else (3,)

        def spot(i, j):
            return pieces(l, g, i, j) if first == "y" else pieces(l, g, j, i)

        forward = (1, 1, -1, -1) if g == 0 else (1, 1, 1, -1)
        if s == 0:
            src, dst = fronts(l, g), spot(own[0], own[1])
            for i in mine:
                for by in BOTH:
                    links.send((l, g, "a1", i, by), src[i], dst[i], peer(first, by))
                copy = pltpu.make_async_copy(src[i], dst[i], osem.at[l, g, i])
                copy.start()
                local[l, g, i] = copy
        elif s == 1:
            for by in BOTH:
                landed = spot(step(own[0], -by), own[1])
                for i in mine:
                    links.arrive((l, g, "a1", i, by), landed[i], peer(first, -by))
                    if forward[i] == by:
                        links.send((l, g, "b1", i), landed[i], landed[i], peer(first, by))
        elif s == PAIR:
            landed = spot(step(own[0], PAIR), own[1])
            part = line(l, g, own[1], None)
            for i in mine:
                local[l, g, i].wait()
                links.arrive((l, g, "b1", i), landed[i], peer(first, -forward[i]))
                for by in BOTH:
                    links.send((l, g, "a2", i, by), part[i], part[i], peer(then, by))
        elif s == 3:
            for by in BOTH:
                at2 = step(own[1], -by)
                whole, half = line(l, g, at2, None), line(l, g, at2, (1 - by) // PAIR)
                for i in mine:
                    links.arrive((l, g, "a2", i, by), whole[i], peer(then, -by))
                    links.send((l, g, "a3", i, by), half[i], half[i], peer(then, by))
        else:
            at2 = step(own[1], PAIR)
            for by in BOTH:
                half = line(l, g, at2, (1 - by) // PAIR)
                for i in mine:
                    links.arrive((l, g, "a3", i, by), half[i], peer(then, -by))

    stages = {"p1": p1, "p2": p2, "p3": lambda l, k, s, is_in: p3(l, k, is_in), "ag": ag}

    for kind, *task in order:
        stages[kind](*task)
    links.drain()


def add_into(dst, src):
    lead = dst.shape[:-PAIR]
    if len(lead) == PAIR:
        @pl.loop(0, lead[0])
        def _(i):
            for j in range(lead[1]):
                dst[i, j] += src[i, j]
    elif len(lead) == 1:
        @pl.loop(0, lead[0])
        def _(i):
            dst[i] += src[i]
    else:
        dst[ALL] += src[ALL]


def reduce_order(widths, rows, rows_b, starts):
    rate = 11650.0
    tasks = []
    for l in range(PAIR):
        for is_in in PARTS:
            for k, (color, by) in enumerate(FLOWS):
                axes = color + FLOW_AXES[color]
                full = 16 * (rows * widths[k] if is_in else rows_b * LANE) / rate
                chain = [("p1", l, k, s, is_in) for s in range(SIDE)] + [("p2", l, k, s, is_in) for s in (1, PAIR, 3)] + [("p3", l, k, 0, is_in)]
                sends = [[((axes[0], by), full)]] * 3 + [[((axes[1], by), full / SIDE)]] * 3
                sends += [[((axes[PAIR], o), full / 16) for o in (1, -1, 1)], []]
                for i, task in enumerate(chain):
                    needs = [(chain[i - 1], j) for j in range(len(sends[i - 1]))] if i else []
                    tasks.append((task, (l, i - ROW), starts[is_in][l] if i == 0 else 0.0, needs, [], sends[i]))
            for g, ((first, then), flows) in enumerate(GROUPS):
                piece = sum(rows * widths[k] if is_in else rows_b * LANE for k in flows) / rate
                for s, (axis, n) in enumerate(((first, 1), (first, 0.5), (then, SIDE), (then, PAIR), (None, 0))):
                    needs = [(("ag", l, g, s - 1, is_in), j) for j in (0, 1)] if s else []
                    after = [] if s else [("p3", l, k, 0, is_in) for k in flows]
                    sends = [((axis, by), piece * n) for by in BOTH] if axis else []
                    tasks.append((("ag", l, g, s, is_in), (l, s - 5), 0.0, needs, after, sends))
    return plan(tasks)


def reduce_gradients(ga, gb, widths=(384, 384, WIDE, WIDE, WIDE, WIDE), starts=None):
    any_space = pl.BlockSpec(memory_space=pl.ANY)
    rows = ga[0].shape[PAIR]
    rows_b = gb[0].shape[3]
    cols = SIDE * sum(widths)
    f32 = jnp.float32
    wx, wz, wy = widths[0], widths[PAIR], widths[SIDE]

    def buffers(slots, whole):
        a = {"x": (SIDE, rows, SIDE * wx), "y": (SIDE, rows, SIDE * wy), "z": (SIDE, SIDE, rows, wz)}
        b = {"x": (rows, SIDE * wx), "y": (SIDE, rows, wy), "z": (SIDE, rows, wz)}
        c = {"x": (rows, wx), "y": (rows, wy), "z": (rows, wz)}
        flat = ((SIDE, SIDE), (SIDE,), ())[whole]
        per = (a, b, c)[whole]
        return [pltpu.VMEM((PAIR, PAIR, slots, *per[color]), f32) for color in "xyz"] + [
            pltpu.VMEM((PAIR, 6, slots, *flat, rows_b, LANE), f32)]

    oa = jax.ShapeDtypeStruct((SIDE, rows, cols), f32)
    ob = jax.ShapeDtypeStruct((SIDE, SIDE, rows_b, 768), f32)
    outs = pl.pallas_call(
        functools.partial(reduce_kernel, widths, reduce_order(widths, rows, rows_b, starts or {True: (0, 40), False: (0, 60)})),
        out_shape=(oa, oa, ob, ob),
        in_specs=[any_space] * SIDE,
        out_specs=[any_space] * SIDE,
        scratch_shapes=[
            *buffers(PAIR, 0), *buffers(3, 0), *buffers(3, 1), *buffers(3, PAIR),
            pltpu.VMEM((PAIR, rows, sum(widths)), f32), pltpu.VMEM((PAIR, rows_b, 768), f32),
            pltpu.SemaphoreType.DMA((400,)), pltpu.SemaphoreType.DMA((400,)),
            pltpu.SemaphoreType.DMA((PAIR, 6, PAIR, 3)), pltpu.SemaphoreType.DMA((PAIR, PAIR, SIDE)),
        ],
        compiler_params=pltpu.CompilerParams(collective_id=1, has_side_effects=True, vmem_limit_bytes=60 << 20),
        name="reduce_gradients",
    )(*ga, *gb)
    return outs[:PAIR], outs[PAIR:]


BF, F32 = jnp.bfloat16, jnp.float32


def product(a, b, contract=((1,), (0,))):
    return lax.dot_general(a, b, (contract, ((), ())), preferred_element_type=F32)


def lanes(start, size):
    return pl.ds(start if isinstance(start, int) else pl.multiple_of(start, LANE), size)


def layers_kernel(x_ref, dy_ref, gain_ref, cos_ref, sin_ref, turn_ref, wi_a, wo_a, wi_b, wo_b,
                  y_ref, gx_ref, ht_a, ht_b, z_a, z_b, mt_a, mt_b, yp_a, yp_b, sc_out,
                  wi, wo, z, om, h, hid, qr, kts, vts, ksl, scores, dscores, pcat, dscat,
                  dot_heads, qt, dht, dkv, omt, ht, dyt, sc, load_sems, own_sems, send_sems, recv_sems):
    seq, dim = x_ref.shape
    ff = (wi_a.shape[1] - dim - LANE) // PAIR
    x, y, zc, core = chip_position()
    twin = device_at(x, y, zc, 1 - core)
    announce([twin])
    links = Links(send_sems, recv_sems)
    stored, used = [], []
    loads = []
    for i, (src, dst) in enumerate(((wi_a, wi.at[0]), (wo_a, wo.at[0]), (wi_b, wi.at[1]), (wo_b, wo.at[1]))):
        copy = pltpu.make_async_copy(src, dst, load_sems.at[i])
        copy.start()
        loads.append(copy)

    def keep(src, dst):
        copy = pltpu.make_async_copy(src, dst, own_sems.at[len(used)])
        copy.start()
        used.append(copy)
        stored.append(copy)

    def settle():
        for copy in stored:
            copy.wait()
        stored.clear()
        links.drain()

    def share(key, src, out, place):
        keep(src, place(out, 0))
        links.send(key, src, place(out, 1), twin)

    z[:, :, wi.shape[PAIR]:] = jnp.zeros((PAIR, seq, z.shape[PAIR] - wi.shape[PAIR]), BF)
    entry = (x_ref, hid.at[0])
    kts[ALL] = jnp.zeros(kts.shape, BF)
    vts[ALL] = jnp.zeros(vts.shape, BF)

    def normalise(l, src):
        @pl.loop(0, seq // BAND)
        def _(r):
            rows = pl.ds(pl.multiple_of(r * BAND, BAND), BAND)
            v = src[rows].astype(F32)
            v = v - jnp.mean(v, axis=-1, keepdims=True)
            var = jnp.mean(v * v, axis=-1, keepdims=True)
            h[l, rows] = (v * lax.rsqrt(var + 1e-6) * gain_ref[l:l + 1]).astype(BF)

    def project(l):
        def part(at, size):
            z[l, :, lanes(at, size)] = product(h[l], wi[l, :, lanes(at, size)]).astype(BF)

        n = wi.shape[PAIR] // STRIP

        @pl.loop(0, n)
        def _(i):
            part(i * STRIP, STRIP)
        part(n * STRIP, wi.shape[PAIR] - n * STRIP)

    def heads(l):
        cos, sin = cos_ref[ALL], sin_ref[ALL]
        for g in range(dim // WIDE):
            q = z[l, :, g * WIDE:(g + 1) * WIDE]
            qr[l, :, g * WIDE:(g + 1) * WIDE] = ((q.astype(F32) * cos + product(q, turn_ref[ALL]) * sin) * 0.125).astype(BF)
        kv = z[l, :, dim:dim + LANE]
        turned = kv.astype(F32) * cos[:, :LANE] + product(kv, turn_ref[:LANE, :LANE]) * sin[:, :LANE]
        first = lax.broadcasted_iota(jnp.int32, turned.shape, 1) < HEAD
        key_lo = jnp.where(first, turned, 0.0)
        val_hi = jnp.where(first, 0.0, kv.astype(F32))
        return key_lo, pltpu.roll(key_lo, HEAD, 1), pltpu.roll(val_hi, HEAD, 1), val_hi

    def slot_rows(ref, lo, hi):
        zero = jnp.zeros((seq, LANE), BF)
        lo, hi = lo.astype(BF), hi.astype(BF)
        for i, (left, right) in enumerate(((lo, zero), (hi, zero), (zero, lo), (zero, hi))):
            ref[i * seq:(i + 1) * seq, :LANE] = left
            ref[i * seq:(i + 1) * seq, LANE:] = right

    def slot_cols(ref, lo):
        flat = lo.T[:HEAD].astype(BF)
        for i in range(SIDE):
            ref[HEAD * i:HEAD * (i + 1), i * seq:(i + 1) * seq] = flat

    def chances(rows, r, i):
        s = scores[rows, i * seq:(i + 1) * seq]
        at = lax.broadcasted_iota(jnp.int32, s.shape, 0) + r * BAND
        s = jnp.where(at >= lax.broadcasted_iota(jnp.int32, s.shape, 1), s, -1e30)
        e = jnp.exp(s - jnp.max(s, axis=-1, keepdims=True))
        return e * (1.0 / jnp.sum(e, axis=-1, keepdims=True))

    def attend(l):
        key_lo, _, val_lo, val_hi = heads(l)
        slot_cols(kts, key_lo)
        slot_rows(ksl, val_lo, val_hi)

        @pl.loop(0, dim // WIDE)
        def _(g):
            cols = lanes(g * WIDE, WIDE)
            scores[ALL] = product(qr[l, :, cols], kts[ALL])

            @pl.loop(0, seq // BAND)
            def _(r):
                rows = pl.ds(pl.multiple_of(r * BAND, BAND), BAND)
                for i in range(SIDE):
                    pcat[rows, i * seq:(i + 1) * seq] = chances(rows, r, i).astype(BF)
            om[:, cols] = product(pcat[ALL], ksl[ALL]).astype(BF)

    def mlp(l):
        @pl.loop(0, seq // BAND)
        def _(r):
            rows = pl.ds(pl.multiple_of(r * BAND, BAND), BAND)

            @pl.loop(0, ff // STRIP)
            def _(i):
                gate = z[l, rows, lanes(dim + LANE + i * STRIP, STRIP)].astype(F32)
                up = z[l, rows, lanes(dim + LANE + ff + i * STRIP, STRIP)].astype(F32)
                om[rows, lanes(dim + i * STRIP, STRIP)] = (gate * jax.nn.sigmoid(gate) * up).astype(BF)

    def put_out(l, dst):
        for n in range(dim // WIDE):
            cols = slice(n * WIDE, (n + 1) * WIDE)
            total = product(om[ALL], wo[l, :, cols])
            dst[:, cols] = (entry[l][:, cols].astype(F32) + total).astype(BF)

    def flip(src, dst, width):
        @pl.loop(0, width // WIDE)
        def _(i):
            dst[pl.ds(pl.multiple_of(i * WIDE, WIDE), WIDE)] = src(i * WIDE).T

    def backward(l, dy):
        flip(lambda at: dy[:, lanes(at, WIDE)], dyt, dim)

        @pl.loop(0, wo.shape[1] // dim)
        def _(n):
            rows = pl.ds(pl.multiple_of(n * dim, dim), dim)
            part = product(wo[l, rows], dyt[ALL]).astype(BF)
            om[:, lanes(n * dim, dim)] = part.T

            @pl.when(n == 0)
            def _():
                dot_heads[ALL] = part

        @pl.loop(0, seq // BAND)
        def _(r):
            rows = pl.ds(pl.multiple_of(r * BAND, BAND), BAND)

            @pl.loop(0, ff // STRIP)
            def _(i):
                gate_at, up_at = lanes(dim + LANE + i * STRIP, STRIP), lanes(dim + LANE + ff + i * STRIP, STRIP)
                gate, up = z[l, rows, gate_at].astype(F32), z[l, rows, up_at].astype(F32)
                d = om[rows, lanes(dim + i * STRIP, STRIP)].astype(F32)
                sig = jax.nn.sigmoid(gate)
                du = d * up
                z[l, rows, gate_at] = (du * sig + du * gate * (sig * (1.0 - sig))).astype(BF)
                z[l, rows, up_at] = (d * (gate * sig)).astype(BF)

        key_lo, key_hi, val_lo, val_hi = heads(l)
        slot_cols(kts, key_lo)
        slot_cols(vts, val_lo)
        slot_rows(ksl, key_lo, key_hi)
        dkv[ALL] = jnp.zeros(dkv.shape, F32)
        flip(lambda at: qr[l, :, lanes(at, WIDE)], qt, dim)

        @pl.loop(0, dim // WIDE)
        def _(g):
            cols = lanes(g * WIDE, WIDE)
            scores[ALL] = product(qr[l, :, cols], kts[ALL])
            dscores[ALL] = product(om[:, cols], vts[ALL])

            @pl.loop(0, seq // BAND)
            def _(r):
                rows = pl.ds(pl.multiple_of(r * BAND, BAND), BAND)
                for i in range(SIDE):
                    at = slice(i * seq, (i + 1) * seq)
                    p = chances(rows, r, i)
                    pcat[rows, at] = p.astype(BF)
                    pd = p * dscores[rows, at].astype(BF).astype(F32)
                    dscat[rows, at] = (pd - p * jnp.sum(pd, axis=-1, keepdims=True)).astype(BF)
            dq = product(dscat[ALL], ksl[ALL]).astype(BF)
            back = dq.astype(F32) * cos_ref[ALL] - product(dq, turn_ref[ALL]) * sin_ref[ALL]
            z[l, :, cols] = (back * 0.125).astype(BF)
            for i in range(SIDE):
                head = pl.ds(pl.multiple_of(g * WIDE + i * HEAD, HEAD), HEAD)
                at = slice(i * seq, (i + 1) * seq)
                dkv[:HEAD] += product(qt[head], dscat[:, at])
                dkv[HEAD:] += product(dot_heads[head], pcat[:, at])

        dkv_t = dkv[ALL].T
        dk = dkv_t.astype(BF)
        turned = dk.astype(F32) * cos_ref[:, :LANE] - product(dk, turn_ref[:LANE, :LANE]) * sin_ref[:, :LANE]
        first = lax.broadcasted_iota(jnp.int32, turned.shape, 1) < HEAD
        z[l, :, dim:dim + LANE] = jnp.where(first, turned, dkv_t).astype(BF)

    def backward_rows(l, dy, dst):
        n, width = wi.shape[PAIR] // 1408, 1408
        for i in range(n):
            at = slice(i * width, (i + 1) * width)
            part = product(wi[l, :, at], z[l, :, at], ((1,), (1,)))
            dht[ALL] = part if i == 0 else dht[ALL] + part
        for i in range(dim // WIDE):
            cols = slice(i * WIDE, (i + 1) * WIDE)
            h[l, :, cols] = dht[cols].T.astype(BF)
        sc[l] = jnp.zeros(sc.shape[1:], F32)

        @pl.loop(0, seq // BAND)
        def _(r):
            rows = pl.ds(pl.multiple_of(r * BAND, BAND), BAND)
            v = entry[l][rows].astype(F32)
            v = v - jnp.mean(v, axis=-1, keepdims=True)
            scale = lax.rsqrt(jnp.mean(v * v, axis=-1, keepdims=True) + 1e-6)
            hat = v * scale
            d = h[l, rows].astype(F32)
            each = (d * hat).reshape(SIDE, ROW, dim)
            sc[l] += (each[0] + each[1]) + (each[PAIR] + each[3])
            d = d * gain_ref[l:l + 1]
            d = scale * (d - jnp.mean(d, axis=-1, keepdims=True) - hat * jnp.mean(d * hat, axis=-1, keepdims=True))
            dst[rows] = (dy[rows].astype(F32) + d.astype(BF).astype(F32)).astype(BF)

    def give_rows(l, name, src, out):
        size = src.shape[0] // ROW
        for b in range(SIDE):
            mine = src.at[pl.ds(pl.multiple_of((PAIR * b + core) * size, BAND), size)]
            other = src.at[pl.ds(pl.multiple_of((PAIR * b + 1 - core) * size, BAND), size)]
            keep(mine, out.at[b, :, pl.ds(0, seq)])
            links.send((name, l, b), other, out.at[b, :, pl.ds(seq, seq)], twin)

    for l in range(PAIR):
        loads[PAIR * l].wait()
        normalise(l, entry[l])
        settle()
        flip(lambda at: h[l, :, lanes(at, WIDE)], ht, dim)
        project(l)
        attend(l)
        mlp(l)
        flip(lambda at: om[:, lanes(at, WIDE)], omt, om.shape[1])
        loads[PAIR * l + 1].wait()
        put_out(l, hid.at[0] if l == 0 else y_ref)
        give_rows(l, "ht", ht, (ht_a, ht_b)[l])
        give_rows(l, "mt", omt, (mt_a, mt_b)[l])
    share(("y", 1), dy_ref, yp_b, lambda out, far: out.at[pl.ds(far * seq, seq)])
    for l, dy, dst in ((1, dy_ref, hid.at[1]), (0, hid.at[1], gx_ref)):
        if l == 0:
            share(("y", 0), dy, yp_a, lambda out, far: out.at[pl.ds(far * seq, seq)])
        backward(l, dy)
        share(("z", l), z.at[l], (z_a, z_b)[l], lambda out, far: out.at[pl.ds(far * seq, seq)])
        backward_rows(l, dy, dst)
        share(("sc", l), sc.at[l], sc_out.at[l], lambda out, far: out.at[far])
    settle()
    for l in range(PAIR):
        for b in range(SIDE):
            links.arrive(("ht", l, b), (ht_a, ht_b)[l].at[b, :, pl.ds(seq, seq)], twin)
            links.arrive(("mt", l, b), (mt_a, mt_b)[l].at[b, :, pl.ds(seq, seq)], twin)
        links.arrive(("y", l), (yp_a, yp_b)[l].at[pl.ds(seq, seq)], twin)
        links.arrive(("z", l), (z_a, z_b)[l].at[pl.ds(seq, seq)], twin)
        links.arrive(("sc", l), sc_out.at[l, 1], twin)


def run_layers(x, dy, gain, cos, sin, turn, weights):
    seq, dim = x.shape
    proj, cat = weights[0].shape[1], weights[1].shape[0]
    wide = proj + LANE
    any_space, vmem = pl.BlockSpec(memory_space=pltpu.HBM), pl.BlockSpec(memory_space=pltpu.VMEM)
    out = lambda *shape, dtype=BF: jax.ShapeDtypeStruct(shape, dtype)
    buffer = lambda *shape, dtype=BF: pltpu.VMEM(shape, dtype)
    pair = PAIR * seq
    return pl.pallas_call(
        layers_kernel,
        out_shape=(out(seq, dim), out(seq, dim), *[out(SIDE, dim // ROW, pair)] * PAIR, *[out(pair, wide)] * PAIR, *[out(SIDE, cat // ROW, pair)] * PAIR,
                   *[out(pair, dim)] * PAIR, out(PAIR, PAIR, ROW, dim, dtype=F32)),
        in_specs=[vmem] * 6 + [any_space] * SIDE,
        out_specs=[vmem] * PAIR + [any_space] * 9,
        scratch_shapes=[
            buffer(PAIR, dim, proj), buffer(PAIR, cat, dim), buffer(PAIR, seq, wide), buffer(seq, cat), buffer(PAIR, seq, dim),
            buffer(PAIR, seq, dim), buffer(PAIR, seq, dim),
            buffer(WIDE, SIDE * seq), buffer(WIDE, SIDE * seq), buffer(SIDE * seq, WIDE),
            buffer(seq, SIDE * seq, dtype=F32), buffer(seq, SIDE * seq, dtype=F32), buffer(seq, SIDE * seq), buffer(seq, SIDE * seq),
            buffer(dim, seq), buffer(dim, seq), buffer(dim, seq, dtype=F32), buffer(LANE, seq, dtype=F32),
            buffer(cat, seq), buffer(dim, seq), buffer(dim, seq), buffer(PAIR, ROW, dim, dtype=F32),
            pltpu.SemaphoreType.DMA((SIDE,)), pltpu.SemaphoreType.DMA((BAND,)), pltpu.SemaphoreType.DMA((BAND,)), pltpu.SemaphoreType.DMA((BAND,)),
        ],
        compiler_params=pltpu.CompilerParams(collective_id=PAIR, has_side_effects=True, vmem_limit_bytes=67043328),
        name="run_layers",
    )(x, dy, gain, cos, sin, turn, *weights)


def rotary_tables(seq_len, head_dim):
    half_dim = head_dim // PAIR
    inv_freq = 10000.0 ** (-(jnp.arange(half_dim, dtype=jnp.float32) * 2.0 / head_dim))
    angles = jnp.arange(seq_len, dtype=jnp.float32)[:, None] * inv_freq[None, :]
    return jnp.cos(angles), jnp.sin(angles)


def solution(mesh):
    fsdp_size = mesh.shape["fsdp"]
    batch_spec = P(("dp", "fsdp"), None, None)
    scale_spec = P(None, "fsdp")
    weight_spec = P(None, "fsdp", None)

    def device_step(x_in, grad_y, norm_scale, w_in, w_out):
        n_layers = w_in.shape[0]
        seq_len, model_dim = x_in.shape[1:]
        proj_dim = w_in.shape[PAIR]
        ff_dim = w_out.shape[1] * fsdp_size - model_dim
        head_dim = (proj_dim - model_dim - PAIR * ff_dim) // PAIR
        rows, rows_out = norm_scale.shape[1], w_out.shape[1]
        scale_tile = jnp.pad(norm_scale.astype(jnp.float32), ((0, ROW - n_layers), (0, LANE - rows)))
        scales, *gathered = gather_weights(scale_tile, w_in, w_out)
        scale_full = scales[:, :n_layers, :rows].transpose(1, 0, PAIR).reshape(n_layers, model_dim)
        cos_tab, sin_tab = rotary_tables(seq_len, head_dim)
        cos_tab, sin_tab = jnp.tile(cos_tab, (1, ROW)), jnp.tile(sin_tab, (1, ROW))
        lane = jnp.arange(WIDE)
        down = lane[:, None] - lane[None, :]
        low = lane[None, :] % head_dim < head_dim // PAIR
        turn = jnp.where(low & (down == BAND), -1.0, jnp.where(~low & (down == -BAND), 1.0, 0.0)).astype(jnp.bfloat16)
        weights = [w.reshape(-1, w.shape[-1]) for w in gathered]
        hidden, grad_hidden, *rest = run_layers(x_in[0], grad_y[0], jnp.pad(scale_full, ((0, ROW - n_layers), (0, 0))), cos_tab, sin_tab, turn, weights)
        h_rows, z_cols, m_rows, y_cols, scale_parts = rest[0:PAIR], rest[PAIR:SIDE], rest[SIDE:6], rest[6:ROW], rest[ROW]
        in_parts, out_parts = [], []
        for l in range(n_layers):
            part_in = jnp.dot(h_rows[l].reshape(SIDE * rows, -1), z_cols[l], preferred_element_type=jnp.float32)
            in_parts.append(part_in.reshape(SIDE, SIDE, rows // SIDE, proj_dim + LANE))
            part_out = jnp.dot(m_rows[l].reshape(SIDE * rows_out, -1), y_cols[l], preferred_element_type=jnp.float32).reshape(SIDE, rows_out, model_dim)
            part_out = jnp.pad(part_out, ((0, 0), (0, BAND), (0, 0)))
            part_scale = jnp.broadcast_to(scale_parts[l].sum((0, 1)), (SIDE, 1, model_dim))
            part_out = lax.dynamic_update_slice(part_out, part_scale, (0, rows_out, 0))
            out_parts.append(part_out.reshape(SIDE, SIDE, SIDE, (rows_out + BAND) // 16, model_dim))
        in_sums, out_sums = reduce_gradients(in_parts[::-1], out_parts[::-1])
        in_grads = jnp.stack([g.reshape(rows, -1)[:, :proj_dim] for g in in_sums[::-1]])
        out_rows = [g.reshape(-1, model_dim) for g in out_sums[::-1]]
        out_grads = jnp.stack([g[:rows_out] for g in out_rows])
        scale_grads = jnp.stack([lax.dynamic_slice(g[rows_out], (lax.axis_index("fsdp") * rows,), (rows,)) for g in out_rows])
        return hidden[None], grad_hidden[None], scale_grads, in_grads, out_grads

    return jax.shard_map(
        device_step,
        mesh=mesh,
        in_specs=(batch_spec, batch_spec, scale_spec, weight_spec, weight_spec),
        out_specs=(batch_spec, batch_spec, scale_spec, weight_spec, weight_spec),
        check_vma=False,
    )
```

```python
import functools
import jax
import jax.numpy as jnp
from jax import lax
from jax.experimental import pallas as pl
from jax.experimental.pallas import tpu as pltpu
from jax.sharding import PartitionSpec as P

MESH_ID = pl.DeviceIdType.MESH
BOTH = (1, -1)
AROUND = (1, -1, 2)
PARTS = (True, False)
ALL = ...
LANE, WIDE, STRIP, HEAD = 128, 256, 512, 64
ROW, BAND, SIDE, PAIR = 8, 32, 4, 2


class Links:
    def __init__(self, send_sems, recv_sems):
        self.send_sems, self.recv_sems = send_sems, recv_sems
        self.slots, self.batches, self.sent = {}, {}, {}

    def send(self, key, src, dst, device, landing=None, whole=None, batch=None):
        slot = self.slots.setdefault(landing or key, len(self.slots))
        leaving = self.batches.setdefault(batch or key, len(self.batches))
        copy = pltpu.make_async_remote_copy(
            src_ref=src, dst_ref=dst, send_sem=self.send_sems.at[leaving], recv_sem=self.recv_sems.at[slot],
            device_id=device, device_id_type=MESH_ID)
        copy.start()
        self.sent[batch or key] = (whole or src, leaving)

    def arrive(self, key, landed):
        slot = self.slots.setdefault(key, len(self.slots))
        pltpu.make_async_copy(landed, landed, self.recv_sems.at[slot]).wait()

    def drain(self):
        for left, leaving in self.sent.values():
            pltpu.make_async_copy(left, left, self.send_sems.at[leaving]).wait()
        self.sent.clear()


def rem(a, n):
    return a % n if isinstance(a, int) else lax.rem(a, n)


def chip_position():
    f, d = lax.axis_index("fsdp"), lax.axis_index("dp")
    return f // PAIR, rem(d, SIDE), d // SIDE, rem(f, PAIR)


def device_at(x, y, z, core):
    return (z * SIDE + y, x * PAIR + core)


def step(coord, by):
    return rem(coord + SIDE + by, SIDE)


def announce(devices):
    barrier = pltpu.get_barrier_semaphore()
    for device in devices:
        pl.semaphore_signal(barrier, inc=1, device_id=device, device_id_type=MESH_ID)
    pl.semaphore_wait(barrier, len(devices))


def plan(tasks, latency=2.5):
    free, landed, order, now = {}, {}, [], 0.0
    left = list(tasks)
    while left:
        best = None
        for place, (name, rank, start, needs, after, _, _) in enumerate(left):
            if all(n[0] in landed for n in needs) and all(n in landed for n in after):
                ready = max([start, now] + [landed[task][i] for task, i in needs])
                best = min(best or (ready, rank, place), (ready, rank, place))
        now, _, place = best
        name, _, _, _, _, sends, cost = left.pop(place)
        order.append(name)
        now += cost
        landed[name] = []
        for link, time in sends:
            free[link] = max(now, free.get(link, 0.0)) + time
            landed[name].append(free[link] + latency)
    return order


def gather_order(rows_i, cols_i, rows_o, cols_o, starts):
    rate = 23300.0
    tasks = []
    for m in range(SIDE):
        is_in = m % PAIR == 0
        edge = cols_i // LANE * SIDE // 9 // PAIR * WIDE
        size = {"y": rows_i // SIDE * edge, "x": rows_i * (cols_i - PAIR * edge)} if is_in else {"y": rows_o // SIDE * cols_o // PAIR}
        size["z"] = size["y"]
        for color in "yzx" if is_in else "yz":
            cost = size[color] / rate
            both = [(("x", by), cost) for by in BOTH]
            spread = [((color, by), cost) for by in BOTH] if color != "x" else []
            tasks.append((("reach", m, color), m, starts[m], [], [], both, 0.2))
            for i, by in enumerate(BOTH):
                tasks.append((("relay", m, color, by), m, 0.0, [(("reach", m, color), i)], [], [(("x", by), cost / PAIR)] + spread, 0.2))
            halves = [(("relay", m, color, by), 0) for by in BOTH]
            tasks.append((("far", m, color), m, 0.0, halves, [], spread, 0.2))
            if color == "x":
                continue
            for off, source, first in ((-1, ("relay", m, color, 1), 1), (1, ("relay", m, color, -1), 1), (PAIR, ("far", m, color), 0)):
                for i, by in enumerate(BOTH):
                    tasks.append((("pass", m, color, off, by), m, 0.0, [(source, first + i)], [], [((color, by), cost / PAIR)], 0.2))
                halves = [(("pass", m, color, off, by), 0) for by in BOTH]
                tasks.append((("close", m, color, off), m, 0.0, halves, [], [], 0.2))
        for off in (-1, 1, PAIR):
            last = [("close", m, color, off) for color in "yz"]
            if is_in:
                last.append(("far", m, "x") if off == PAIR else ("relay", m, "x", -off))
            tasks.append((("hand", m, off), m, 0.0, [], last, [], 0.2))
    return plan(tasks)


def gather_kernel(order, sc_in, wi_in, wo_in, sc_out, wi_a, wo_a, wi_b, wo_b, own_i, own_o, ssem, rsem, lsem):
    x, y, z, core = chip_position()
    here = device_at(x, y, z, core)
    twin = device_at(x, y, z, 1 - core)
    rows_i, cols_i = wi_in.shape[1:]
    rows_o, cols_o = wo_in.shape[1:]
    quarter_i, quarter_o = rows_i // SIDE, rows_o // SIDE
    third_i = cols_i // LANE * SIDE // 9 // PAIR * WIDE
    half_o = cols_o // PAIR
    cut_o = quarter_o // 16 * ROW + ROW if quarter_o % 16 else quarter_o // PAIR
    place = {"x": x, "y": y, "z": z}

    spots = {(axis, o): step(place[axis], o) for axis in "xyz" for o in range(SIDE)}

    def spot(axis, o):
        return spots[axis, o % SIDE]

    table = {}
    for axis in "xyz":
        for o in range(1, SIDE):
            moved = {**place, axis: spot(axis, o)}
            table[axis, o] = device_at(moved["x"], moved["y"], moved["z"], core)

    def peer(axis, o):
        return table[axis, o % SIDE]

    peers = [peer(axis, by) for axis in "xyz" for by in BOTH]
    others = [(lax.axis_index("dp"), lax.rem(lax.axis_index("fsdp") + k, ROW)) for k in range(1, ROW)]
    announce(others + peers[PAIR:])
    links = Links(ssem, rsem)

    mats = []
    for layer, (wi, wo) in enumerate(((wi_a, wo_a), (wi_b, wo_b))):
        mats.append((wi_in.at[layer], wi, own_i.at[layer], True))
        mats.append((wo_in.at[layer], wo, own_o.at[layer], False))

    def region(is_in, color, q):
        if is_in:
            if color == "x":
                lo, hi = PAIR * third_i, cols_i
                rows = (0, rows_i)
            else:
                lo, hi = (0, third_i) if color == "y" else (third_i, PAIR * third_i)
                rows = (q * quarter_i, quarter_i)
            mid = lo + ((hi - lo) // LANE + 1) // PAIR * LANE
            return (rows, (lo, hi - lo)), (rows, (lo, mid - lo)), (rows, (mid, hi - mid))
        cols = (0, half_o) if color == "y" else (half_o, half_o)
        start = q * quarter_o
        return ((start, quarter_o), cols), ((start, cut_o), cols), ((start + cut_o, quarter_o - cut_o), cols)

    def at(ref, lead, area):
        (r, nr), (c, nc) = area
        if not isinstance(r, int):
            r = pl.multiple_of(r, ROW)
        return ref.at[(*lead, pl.ds(r, nr), pl.ds(c, nc))]

    def colors(m):
        return "yzx" if mats[m][3] else "yz"

    def reach(m, color):
        src, out, _, is_in = mats[m]
        area = region(is_in, color, place[color])[0]
        for by in BOTH:
            links.send((m, "x1", color, by), at(src, (), area), at(out, (x, core), area), peer("x", by))

    def launch(m, color, off):
        _, out, _, is_in = mats[m]
        block = at(out, (spot("x", off), core), region(is_in, color, place[color])[0])
        for by in BOTH:
            links.send((m, "p1", color, off, by), block, block, peer(color, by))

    def relay(m, color, by):
        _, out, _, is_in = mats[m]
        xb = spot("x", -by)
        areas = region(is_in, color, place[color])
        links.arrive((m, "x1", color, by), at(out, (xb, core), areas[0]))
        part = at(out, (xb, core), areas[1] if by == 1 else areas[PAIR])
        links.send((m, "x2", color, by), part, part, peer("x", by))
        if color != "x":
            launch(m, color, -by)

    def far(m, color):
        _, out, _, is_in = mats[m]
        areas = region(is_in, color, place[color])
        for by in BOTH:
            links.arrive((m, "x2", color, by), at(out, (spot("x", PAIR), core), areas[1] if by == 1 else areas[PAIR]))
        if color != "x":
            launch(m, color, PAIR)

    def pass_on(m, color, off, by):
        _, out, _, is_in = mats[m]
        xb = spot("x", off)
        areas = region(is_in, color, spot(color, -by))
        links.arrive((m, "p1", color, off, by), at(out, (xb, core), areas[0]))
        part = at(out, (xb, core), areas[1] if by == 1 else areas[PAIR])
        links.send((m, "p2", color, off, by), part, part, peer(color, by))

    def close(m, color, off):
        _, out, _, is_in = mats[m]
        areas = region(is_in, color, spot(color, PAIR))
        for by in BOTH:
            links.arrive((m, "p2", color, off, by), at(out, (spot("x", off), core), areas[1] if by == 1 else areas[PAIR]))

    def hand(m, off):
        _, out, _, _ = mats[m]
        links.send((m, "d2d", off), out.at[spot("x", off), core], out.at[spot("x", off), core], twin)

    stages = {"reach": reach, "relay": relay, "far": far, "pass": pass_on, "close": close, "hand": hand}

    loads = []
    for m, (src, out, own, _) in enumerate(mats):
        load = pltpu.make_async_copy(src, own, lsem.at[0, m])
        load.start()
        loads.append(load)
    for k, device in enumerate(others):
        links.send(("sc", k), sc_in, sc_out.at[lax.axis_index("fsdp")], device)
    for m, (src, out, own, _) in enumerate(mats):
        links.send((m, "d2d", 0), src, out.at[x, core], twin)
    stores = []
    for m, (src, out, own, _) in enumerate(mats):
        loads[m].wait()
        store = pltpu.make_async_copy(own, out.at[x, core], lsem.at[1, m])
        store.start()
        stores.append(store)
    own_scale = pltpu.make_async_copy(sc_in, sc_out.at[lax.axis_index("fsdp")], lsem.at[PAIR, 0])
    own_scale.start()
    for kind, *task in order:
        stages[kind](*task)
    for m, (src, out, own, _) in enumerate(mats):
        for off in (0, -1, 1, PAIR):
            xb = spot("x", off)
            links.arrive((m, "d2d", off), out.at[xb, 1 - core])
        stores[m].wait()
    own_scale.wait()
    for k in range(7):
        source = lax.rem(lax.axis_index("fsdp") + 7 - k, ROW)
        links.arrive(("sc", k), sc_out.at[source])
    links.drain()


def gather_weights(scale_tile, w_in, w_out, starts=None, n_copies=320):
    any_space = pl.BlockSpec(memory_space=pltpu.HBM)
    wi = jax.ShapeDtypeStruct((SIDE, PAIR, *w_in.shape[1:]), w_in.dtype)
    wo = jax.ShapeDtypeStruct((SIDE, PAIR, *w_out.shape[1:]), w_out.dtype)
    return pl.pallas_call(
        functools.partial(gather_kernel, gather_order(*w_in.shape[1:], *w_out.shape[1:], starts or (0, 0, 0, 0))),
        out_shape=(jax.ShapeDtypeStruct((ROW, *scale_tile.shape), scale_tile.dtype), wi, wo, wi, wo),
        in_specs=[any_space] * 3,
        out_specs=[any_space] * 5,
        scratch_shapes=[
            pltpu.VMEM(w_in.shape, w_in.dtype),
            pltpu.VMEM(w_out.shape, w_out.dtype),
            pltpu.SemaphoreType.DMA((n_copies,)),
            pltpu.SemaphoreType.DMA((n_copies,)),
            pltpu.SemaphoreType.DMA((3, SIDE)),
        ],
        compiler_params=pltpu.CompilerParams(collective_id=0, has_side_effects=True, vmem_limit_bytes=12 << 20),
        name="gather_weights",
    )(scale_tile, w_in, w_out)


BF, F32 = jnp.bfloat16, jnp.float32


def product(a, b, contract=((1,), (0,))):
    return lax.dot_general(a, b, (contract, ((), ())), preferred_element_type=F32)


def lanes(start, size):
    return pl.ds(start if isinstance(start, int) else pl.multiple_of(start, LANE), size)


def layers_kernel(x_ref, dy_ref, gain_ref, cos_ref, sin_ref, turn_ref, wi_a, wo_a, wi_b, wo_b,
                  y_ref, gx_ref, ht_a, ht_b, z_a, z_b, mt_a, mt_b, yp_a, yp_b, sc_out,
                  wi, wo, z, om, h, hid, qr, kts, vts, ksl, scores, dscores, pcat, dscat,
                  dot_heads, qt, dht, dkv, omt, ht, dyt, sc, load_sems, own_sems, send_sems, recv_sems):
    seq, dim = x_ref.shape
    ff = (wi_a.shape[1] - dim - LANE) // PAIR
    x, y, zc, core = chip_position()
    twin = device_at(x, y, zc, 1 - core)
    announce([twin])
    links = Links(send_sems, recv_sems)
    stored, used = [], []
    loads = []
    for i, (src, dst) in enumerate(((wi_a, wi.at[0]), (wo_a, wo.at[0]), (wi_b, wi.at[1]), (wo_b, wo.at[1]))):
        copy = pltpu.make_async_copy(src, dst, load_sems.at[i])
        copy.start()
        loads.append(copy)

    def keep(src, dst):
        copy = pltpu.make_async_copy(src, dst, own_sems.at[len(used)])
        copy.start()
        used.append(copy)
        stored.append(copy)

    def settle():
        for copy in stored:
            copy.wait()
        stored.clear()
        links.drain()

    def share(key, src, out, place):
        keep(src, place(out, 0))
        links.send(key, src, place(out, 1), twin)

    z[:, :, wi.shape[PAIR]:] = jnp.zeros((PAIR, seq, z.shape[PAIR] - wi.shape[PAIR]), BF)
    entry = (x_ref, hid.at[0])
    kts[ALL] = jnp.zeros(kts.shape, BF)
    vts[ALL] = jnp.zeros(vts.shape, BF)

    def normalise(l, src):
        @pl.loop(0, seq // BAND)
        def _(r):
            rows = pl.ds(pl.multiple_of(r * BAND, BAND), BAND)
            v = src[rows].astype(F32)
            v = v - jnp.mean(v, axis=-1, keepdims=True)
            var = jnp.mean(v * v, axis=-1, keepdims=True)
            h[l, rows] = (v * lax.rsqrt(var + 1e-6) * gain_ref[l:l + 1]).astype(BF)

    def project(l):
        def part(at, size):
            z[l, :, lanes(at, size)] = product(h[l], wi[l, :, lanes(at, size)]).astype(BF)

        n = wi.shape[PAIR] // STRIP

        @pl.loop(0, n)
        def _(i):
            part(i * STRIP, STRIP)
        part(n * STRIP, wi.shape[PAIR] - n * STRIP)

    def heads(l):
        cos, sin = cos_ref[ALL], sin_ref[ALL]
        for g in range(dim // WIDE):
            q = z[l, :, g * WIDE:(g + 1) * WIDE]
            qr[l, :, g * WIDE:(g + 1) * WIDE] = ((q.astype(F32) * cos + product(q, turn_ref[ALL]) * sin) * 0.125).astype(BF)
        kv = z[l, :, dim:dim + LANE]
        turned = kv.astype(F32) * cos[:, :LANE] + product(kv, turn_ref[:LANE, :LANE]) * sin[:, :LANE]
        first = lax.broadcasted_iota(jnp.int32, turned.shape, 1) < HEAD
        key_lo = jnp.where(first, turned, 0.0)
        val_hi = jnp.where(first, 0.0, kv.astype(F32))
        return key_lo, pltpu.roll(key_lo, HEAD, 1), pltpu.roll(val_hi, HEAD, 1), val_hi

    def slot_rows(ref, lo, hi):
        zero = jnp.zeros((seq, LANE), BF)
        lo, hi = lo.astype(BF), hi.astype(BF)
        for i, (left, right) in enumerate(((lo, zero), (hi, zero), (zero, lo), (zero, hi))):
            ref[i * seq:(i + 1) * seq, :LANE] = left
            ref[i * seq:(i + 1) * seq, LANE:] = right

    def slot_cols(ref, lo):
        flat = lo.T[:HEAD].astype(BF)
        for i in range(SIDE):
            ref[HEAD * i:HEAD * (i + 1), i * seq:(i + 1) * seq] = flat

    def chances(rows, r, i):
        s = scores[rows, i * seq:(i + 1) * seq]
        at = lax.broadcasted_iota(jnp.int32, s.shape, 0) + r * BAND
        s = jnp.where(at >= lax.broadcasted_iota(jnp.int32, s.shape, 1), s, -1e30)
        e = jnp.exp(s - jnp.max(s, axis=-1, keepdims=True))
        return e * (1.0 / jnp.sum(e, axis=-1, keepdims=True))

    def attend(l):
        key_lo, _, val_lo, val_hi = heads(l)
        slot_cols(kts, key_lo)
        slot_rows(ksl, val_lo, val_hi)

        @pl.loop(0, dim // WIDE)
        def _(g):
            cols = lanes(g * WIDE, WIDE)
            scores[ALL] = product(qr[l, :, cols], kts[ALL])

            @pl.loop(0, seq // BAND)
            def _(r):
                rows = pl.ds(pl.multiple_of(r * BAND, BAND), BAND)
                for i in range(SIDE):
                    pcat[rows, i * seq:(i + 1) * seq] = chances(rows, r, i).astype(BF)
            om[:, cols] = product(pcat[ALL], ksl[ALL]).astype(BF)

    def mlp(l):
        @pl.loop(0, seq // BAND)
        def _(r):
            rows = pl.ds(pl.multiple_of(r * BAND, BAND), BAND)

            @pl.loop(0, ff // STRIP)
            def _(i):
                gate = z[l, rows, lanes(dim + LANE + i * STRIP, STRIP)].astype(F32)
                up = z[l, rows, lanes(dim + LANE + ff + i * STRIP, STRIP)].astype(F32)
                om[rows, lanes(dim + i * STRIP, STRIP)] = (gate * jax.nn.sigmoid(gate) * up).astype(BF)

    def put_out(l, dst):
        for n in range(dim // WIDE):
            cols = slice(n * WIDE, (n + 1) * WIDE)
            total = product(om[ALL], wo[l, :, cols])
            dst[:, cols] = (entry[l][:, cols].astype(F32) + total).astype(BF)

    def flip(src, dst, width):
        @pl.loop(0, width // WIDE)
        def _(i):
            dst[pl.ds(pl.multiple_of(i * WIDE, WIDE), WIDE)] = src(i * WIDE).T

    def backward(l, dy):
        flip(lambda at: dy[:, lanes(at, WIDE)], dyt, dim)

        @pl.loop(0, wo.shape[1] // dim)
        def _(n):
            rows = pl.ds(pl.multiple_of(n * dim, dim), dim)
            part = product(wo[l, rows], dyt[ALL]).astype(BF)
            om[:, lanes(n * dim, dim)] = part.T

            @pl.when(n == 0)
            def _():
                dot_heads[ALL] = part

        @pl.loop(0, seq // BAND)
        def _(r):
            rows = pl.ds(pl.multiple_of(r * BAND, BAND), BAND)

            @pl.loop(0, ff // STRIP)
            def _(i):
                gate_at, up_at = lanes(dim + LANE + i * STRIP, STRIP), lanes(dim + LANE + ff + i * STRIP, STRIP)
                gate, up = z[l, rows, gate_at].astype(F32), z[l, rows, up_at].astype(F32)
                d = om[rows, lanes(dim + i * STRIP, STRIP)].astype(F32)
                sig = jax.nn.sigmoid(gate)
                du = d * up
                z[l, rows, gate_at] = (du * sig + du * gate * (sig * (1.0 - sig))).astype(BF)
                z[l, rows, up_at] = (d * (gate * sig)).astype(BF)

        key_lo, key_hi, val_lo, val_hi = heads(l)
        slot_cols(kts, key_lo)
        slot_cols(vts, val_lo)
        slot_rows(ksl, key_lo, key_hi)
        dkv[ALL] = jnp.zeros(dkv.shape, F32)
        flip(lambda at: qr[l, :, lanes(at, WIDE)], qt, dim)

        @pl.loop(0, dim // WIDE)
        def _(g):
            cols = lanes(g * WIDE, WIDE)
            scores[ALL] = product(qr[l, :, cols], kts[ALL])
            dscores[ALL] = product(om[:, cols], vts[ALL])

            @pl.loop(0, seq // BAND)
            def _(r):
                rows = pl.ds(pl.multiple_of(r * BAND, BAND), BAND)
                for i in range(SIDE):
                    at = slice(i * seq, (i + 1) * seq)
                    p = chances(rows, r, i)
                    pcat[rows, at] = p.astype(BF)
                    pd = p * dscores[rows, at].astype(BF).astype(F32)
                    dscat[rows, at] = (pd - p * jnp.sum(pd, axis=-1, keepdims=True)).astype(BF)
            dq = product(dscat[ALL], ksl[ALL]).astype(BF)
            back = dq.astype(F32) * cos_ref[ALL] - product(dq, turn_ref[ALL]) * sin_ref[ALL]
            z[l, :, cols] = (back * 0.125).astype(BF)
            for i in range(SIDE):
                head = pl.ds(pl.multiple_of(g * WIDE + i * HEAD, HEAD), HEAD)
                at = slice(i * seq, (i + 1) * seq)
                dkv[:HEAD] += product(qt[head], dscat[:, at])
                dkv[HEAD:] += product(dot_heads[head], pcat[:, at])

        dkv_t = dkv[ALL].T
        dk = dkv_t.astype(BF)
        turned = dk.astype(F32) * cos_ref[:, :LANE] - product(dk, turn_ref[:LANE, :LANE]) * sin_ref[:, :LANE]
        first = lax.broadcasted_iota(jnp.int32, turned.shape, 1) < HEAD
        z[l, :, dim:dim + LANE] = jnp.where(first, turned, dkv_t).astype(BF)

    def backward_rows(l, dy, dst):
        n, width = wi.shape[PAIR] // 1408, 1408
        for i in range(n):
            at = slice(i * width, (i + 1) * width)
            part = product(wi[l, :, at], z[l, :, at], ((1,), (1,)))
            dht[ALL] = part if i == 0 else dht[ALL] + part
        for i in range(dim // WIDE):
            cols = slice(i * WIDE, (i + 1) * WIDE)
            h[l, :, cols] = dht[cols].T.astype(BF)
        sc[l] = jnp.zeros(sc.shape[1:], F32)

        @pl.loop(0, seq // BAND)
        def _(r):
            rows = pl.ds(pl.multiple_of(r * BAND, BAND), BAND)
            v = entry[l][rows].astype(F32)
            v = v - jnp.mean(v, axis=-1, keepdims=True)
            scale = lax.rsqrt(jnp.mean(v * v, axis=-1, keepdims=True) + 1e-6)
            hat = v * scale
            d = h[l, rows].astype(F32)
            each = (d * hat).reshape(SIDE, ROW, dim)
            sc[l] += (each[0] + each[1]) + (each[PAIR] + each[3])
            d = d * gain_ref[l:l + 1]
            d = scale * (d - jnp.mean(d, axis=-1, keepdims=True) - hat * jnp.mean(d * hat, axis=-1, keepdims=True))
            dst[rows] = (dy[rows].astype(F32) + d.astype(BF).astype(F32)).astype(BF)

    def give_rows(l, name, src, out):
        size = src.shape[0] // ROW
        for b in range(SIDE):
            mine = src.at[pl.ds(pl.multiple_of((PAIR * b + core) * size, BAND), size)]
            other = src.at[pl.ds(pl.multiple_of((PAIR * b + 1 - core) * size, BAND), size)]
            keep(mine, out.at[b, :, pl.ds(0, seq)])
            links.send((name, l, b), other, out.at[b, :, pl.ds(seq, seq)], twin)

    for l in range(PAIR):
        loads[PAIR * l].wait()
        normalise(l, entry[l])
        settle()
        flip(lambda at: h[l, :, lanes(at, WIDE)], ht, dim)
        project(l)
        attend(l)
        mlp(l)
        flip(lambda at: om[:, lanes(at, WIDE)], omt, om.shape[1])
        loads[PAIR * l + 1].wait()
        put_out(l, hid.at[0] if l == 0 else y_ref)
        give_rows(l, "ht", ht, (ht_a, ht_b)[l])
        give_rows(l, "mt", omt, (mt_a, mt_b)[l])
    share(("y", 1), dy_ref, yp_b, lambda out, far: out.at[pl.ds(far * seq, seq)])
    for l, dy, dst in ((1, dy_ref, hid.at[1]), (0, hid.at[1], gx_ref)):
        if l == 0:
            share(("y", 0), dy, yp_a, lambda out, far: out.at[pl.ds(far * seq, seq)])
        backward(l, dy)
        share(("z", l), z.at[l], (z_a, z_b)[l], lambda out, far: out.at[pl.ds(far * seq, seq)])
        backward_rows(l, dy, dst)
        share(("sc", l), sc.at[l], sc_out.at[l], lambda out, far: out.at[far])
    settle()
    for l in range(PAIR):
        for b in range(SIDE):
            links.arrive(("ht", l, b), (ht_a, ht_b)[l].at[b, :, pl.ds(seq, seq)])
            links.arrive(("mt", l, b), (mt_a, mt_b)[l].at[b, :, pl.ds(seq, seq)])
        links.arrive(("y", l), (yp_a, yp_b)[l].at[pl.ds(seq, seq)])
        links.arrive(("z", l), (z_a, z_b)[l].at[pl.ds(seq, seq)])
        links.arrive(("sc", l), sc_out.at[l, 1])


def run_layers(x, dy, gain, cos, sin, turn, weights):
    seq, dim = x.shape
    proj, cat = weights[0].shape[1], weights[1].shape[0]
    wide = proj + LANE
    any_space, vmem = pl.BlockSpec(memory_space=pltpu.HBM), pl.BlockSpec(memory_space=pltpu.VMEM)
    out = lambda *shape, dtype=BF: jax.ShapeDtypeStruct(shape, dtype)
    buffer = lambda *shape, dtype=BF: pltpu.VMEM(shape, dtype)
    pair = PAIR * seq
    return pl.pallas_call(
        layers_kernel,
        out_shape=(out(seq, dim), out(seq, dim), *[out(SIDE, dim // ROW, pair)] * PAIR, *[out(pair, wide)] * PAIR, *[out(SIDE, cat // ROW, pair)] * PAIR,
                   *[out(pair, dim)] * PAIR, out(PAIR, PAIR, ROW, dim, dtype=F32)),
        in_specs=[vmem] * 6 + [any_space] * SIDE,
        out_specs=[vmem] * PAIR + [any_space] * 9,
        scratch_shapes=[
            buffer(PAIR, dim, proj), buffer(PAIR, cat, dim), buffer(PAIR, seq, wide), buffer(seq, cat), buffer(PAIR, seq, dim),
            buffer(PAIR, seq, dim), buffer(PAIR, seq, dim),
            buffer(WIDE, SIDE * seq), buffer(WIDE, SIDE * seq), buffer(SIDE * seq, WIDE),
            buffer(seq, SIDE * seq, dtype=F32), buffer(seq, SIDE * seq, dtype=F32), buffer(seq, SIDE * seq), buffer(seq, SIDE * seq),
            buffer(dim, seq), buffer(dim, seq), buffer(dim, seq, dtype=F32), buffer(LANE, seq, dtype=F32),
            buffer(cat, seq), buffer(dim, seq), buffer(dim, seq), buffer(PAIR, ROW, dim, dtype=F32),
            pltpu.SemaphoreType.DMA((SIDE,)), pltpu.SemaphoreType.DMA((BAND,)), pltpu.SemaphoreType.DMA((BAND,)), pltpu.SemaphoreType.DMA((BAND,)),
        ],
        compiler_params=pltpu.CompilerParams(collective_id=PAIR, has_side_effects=True, vmem_limit_bytes=67043328),
        name="run_layers",
    )(x, dy, gain, cos, sin, turn, *weights)


NEXT_AXES = {"x": "yz", "y": "zx", "z": "xy"}
IN_CHAINS = [("x", 1)] * 3 + [("x", -1)] * 3 + [("z", 1)] * PAIR + [("z", -1)] * PAIR + [("y", 1)] * PAIR + [("y", -1)] * PAIR
OUT_CHAINS = [("x", 1), ("x", -1), ("z", 1), ("z", -1), ("y", 1), ("y", -1)]
CHAINS = [(color, by, True, i) for i, (color, by) in enumerate(IN_CHAINS)] + [(color, by, False, i) for i, (color, by) in enumerate(OUT_CHAINS)]
GROUPS = [("yz", True, 0, 3, 1), ("yz", True, 3, 3, -1), ("yz", True, 6, PAIR, 1), ("zy", True, ROW, PAIR, -1), ("zy", True, 10, SIDE, 1),
          ("yz", False, 0, 3, -1), ("zy", False, 3, 3, -1)]


def reduce_order(rows, rows_b, starts):
    rate = 11650.0
    tasks = []
    for l in range(PAIR):
        for b in range(SIDE):
            tasks.append((("rows", l, b), (9 * l, -9, b), 0.0, [], [], [], 0.9))
        for c, (color, by, is_in, i) in enumerate(CHAINS):
            axes = color + NEXT_AXES[color]
            full = 16 * LANE * (rows if is_in else rows_b) / rate
            chain = [("p1", l, c, s) for s in range(SIDE)] + [("p2", l, c, s) for s in (1, PAIR, 3)] + [("p3", l, c)]
            sends = [[((axes[0], by), full)]] * 3 + [[((axes[1], by), full / SIDE)]] * 3
            sends += [[((axes[PAIR], o), full / 16) for o in (1, -1, 1)], []]
            turn = sum(e[:PAIR] == (color, by) for e in IN_CHAINS[:i]) if is_in else 3
            if is_in:
                before = [("cols", l, c)]
                tasks.append((before[0], (9 * l, -9, turn), 0.0, [], [], [], 0.7))
            else:
                before = [("rows", l, b) for b in range(SIDE)]
            for j, task in enumerate(chain):
                needs = [(chain[j - 1], n) for n in range(len(sends[j - 1]))] if j else []
                start = starts[0][l] + starts[1][l] * turn if j == 0 else 0.0
                tasks.append((task, (l, j - ROW if j else -10, 0), start, needs, [] if j else before, sends[j], 0.3))
        for g, ((first, then), is_in, at, n, way) in enumerate(GROUPS):
            piece = n * LANE * (rows if is_in else rows_b) / rate
            members = [c for c, e in enumerate(CHAINS) if e[PAIR] == is_in and at <= e[3] < at + n]
            for s in range(5):
                needs = []
                if s:
                    needs = [(("ag", l, g, s - 1), k) for k in ((0,) if s == PAIR else (0, 1))]
                sends = ([((first, by), piece) for by in BOTH], [((first, way), piece)], [((then, by), SIDE * piece) for by in BOTH],
                         [((then, by), PAIR * piece) for by in BOTH], [])[s]
                after = [] if s else [("p3", l, c) for c in members]
                tasks.append((("ag", l, g, s), (l, s - 5, 0), 0.0, needs, after, sends, 0.3))
    return plan(tasks)


def reduce_kernel(order, *refs):
    ht, z, mt, yp, sc = refs[0:PAIR], refs[PAIR:SIDE], refs[SIDE:6], refs[6:ROW], refs[ROW]
    oa, ob, ga, gb = refs[9], refs[10], refs[11:13], refs[13:15]
    (wx, wy, wz, wb, rx, ry, rz, rb, sx, sy, sz, sb, tx, ty, tz, tb, fa, fb,
     hbuf, ybuf, scbuf, zbuf, mbuf, cols_out, rows_out, ssem, rsem, lsem, osem, isem, zsem, msem, gsem, bsem) = refs[15:]
    x, y, zc, core = chip_position()
    place = {"x": x, "y": y, "z": zc}
    work, ring1, ring2 = {"x": wx, "y": wy, "z": wz}, {"x": rx, "y": ry, "z": rz}, {"x": sx, "y": sy, "z": sz}
    last = {"x": tx, "y": ty, "z": tz}
    firsts = {color: [e[0] for e in IN_CHAINS].index(color) for color in "xyz"}
    counts = {color: sum(e[0] == color for e in IN_CHAINS) for color in "xyz"}
    quarter = z[0].shape[1] // SIDE
    rows_b = gb[0].shape[3]

    spots = {(axis, o): step(place[axis], o) for axis in "xyz" for o in range(SIDE)}

    def spot(axis, o):
        return spots[axis, o % SIDE]

    peers = {}
    for axis in "xyz":
        for o in range(1, SIDE):
            moved = {**place, axis: spot(axis, o)}
            peers[axis, o] = device_at(moved["x"], moved["y"], moved["z"], core)

    def peer(axis, o):
        return peers[axis, o % SIDE]

    col_order = [task for task in order if task[0] == "cols"]
    row_order = [task for task in order if task[0] == "rows"]
    whole = []
    for l in range(PAIR):
        for i, (src, dst) in enumerate(((ht[l], hbuf.at[l]), (yp[l], ybuf.at[l]), (sc.at[l], scbuf.at[l]))):
            copy = pltpu.make_async_copy(src, dst, isem.at[l, i])
            copy.start()
            whole.append(copy)
    pending = {}

    def fetch_cols(n):
        if n < len(col_order):
            _, l, c = col_order[n]
            for q in range(SIDE):
                copy = pltpu.make_async_copy(z[l].at[:, pl.ds(q * quarter + LANE * c, LANE)], zbuf.at[n % PAIR, :, pl.ds(q * LANE, LANE)], zsem.at[n % PAIR])
                copy.start()

    def fetch_rows(n):
        if n < len(row_order):
            _, l, b = row_order[n]
            copy = pltpu.make_async_copy(mt[l].at[b], mbuf.at[n % PAIR], msem.at[n % PAIR])
            copy.start()
            pending["m", n] = copy

    for n in range(PAIR):
        fetch_cols(n)
        fetch_rows(n)
    announce([peer(axis, by) for axis in "xyz" for by in AROUND])
    links = Links(ssem, rsem)
    local = {}
    for copy in whole:
        copy.wait()

    def cols(l, c):
        n = col_order.index(("cols", l, c))
        slot = n % PAIR
        pltpu.make_async_copy(zbuf.at[slot], zbuf.at[slot], zsem.at[slot]).wait()
        if n >= PAIR:
            settle("g", n - PAIR)
        total = product(hbuf[l].reshape(-1, hbuf.shape[-1]), zbuf[slot])
        size = cols_out.shape[3]
        for i in range(16):
            cols_out[slot, i // SIDE, i % SIDE] = total[i * size:(i + 1) * size]
        fetch_cols(n + PAIR)
        copy = pltpu.make_async_copy(cols_out.at[slot], ga[l].at[c], gsem.at[slot])
        copy.start()
        pending["g", n] = copy
        local["g", l, c] = n

    def rows(l, b):
        n = row_order.index(("rows", l, b))
        slot = n % PAIR
        pending["m", n].wait()
        if n >= PAIR:
            settle("b", n - PAIR)
        total = product(mbuf[slot], ybuf[l])
        size, spare = total.shape[0] // rows_b, 16 * rows_b - total.shape[0]
        for i in range(size):
            rows_out[slot, i // SIDE, i % SIDE] = total[i * rows_b:(i + 1) * rows_b]
        gain = jnp.sum(scbuf[l, 0] + scbuf[l, 1], axis=0, keepdims=True)
        at = lax.broadcasted_iota(jnp.int32, (spare, total.shape[1]), 0)
        rows_out[slot, 3, 3] = jnp.where(at == 0, gain, 0.0)
        fetch_rows(n + PAIR)
        copy = pltpu.make_async_copy(rows_out.at[slot], gb[l].at[b], bsem.at[slot])
        copy.start()
        pending["b", n] = copy

    def settle(kind, n):
        if (kind, n) in pending and not local.get((kind, n)):
            pending[kind, n].wait()
            local[kind, n] = True

    def block(l, c, b):
        color, _, is_in, i = CHAINS[c]
        if is_in:
            ref = ga[l].at[i]
            return ref.at[b] if color == "x" else ref.at[:, b] if color == "y" else ref.at[:, :, :, lanes(b * LANE, LANE)]
        at = pl.ds(i * LANE, LANE)
        ref = gb[l]
        return ref.at[b, :, :, :, at] if color == "x" else ref.at[:, b, :, :, at] if color == "y" else ref.at[:, :, b, :, at]

    def second(ref, c, b):
        color, _, is_in, _ = CHAINS[c]
        if color == "y":
            return ref.at[:, :, lanes(b * LANE, LANE)] if is_in else ref.at[:, b]
        return ref.at[b]

    def third(ref, c, b):
        color, _, is_in, _ = CHAINS[c]
        return ref.at[:, lanes(b * LANE, LANE)] if is_in and color == "x" else ref.at[b]

    def buf(table, flat, l, c, slots, slot):
        color, _, is_in, i = CHAINS[c]
        ref = table[color] if is_in else flat
        first = (l * (counts[color] if is_in else len(OUT_CHAINS)) + (i - firsts[color] if is_in else i)) * slots
        return ref.at[pl.ds(first, slots)] if slot is None else ref.at[first + slot]

    def load(l, c, b, dst, tag):
        copy = pltpu.make_async_copy(block(l, c, b), dst, lsem.at[l, c, tag])
        copy.start()
        local[l, c, tag] = copy

    def p1(l, c, s):
        color, by, is_in, i = CHAINS[c]
        r = [buf(ring1, rb, l, c, 3, k) for k in range(3)]
        w = [buf(work, wb, l, c, PAIR, k) for k in range(PAIR)]
        if s == 0:
            if is_in:
                settle("g", local["g", l, c])
            else:
                for b in range(SIDE):
                    settle("b", row_order.index(("rows", l, b)))
            links.send((l, c, "p1", 0), block(l, c, spot(color, -by)), r[0], peer(color, by), None, buf(ring1, rb, l, c, 3, None), (l, c, "p1"))
            load(l, c, spot(color, -PAIR * by), w[1], 0)
            load(l, c, spot(color, -3 * by), w[0], 1)
            return
        mine = (None, w[1], w[0], r[0])[s]
        links.arrive((l, c, "p1", s - 1), r[s - 1])
        local[l, c, s - 1].wait()
        add_into(mine, r[s - 1])
        if s < 3:
            links.send((l, c, "p1", s), mine, r[s], peer(color, by), None, buf(ring1, rb, l, c, 3, None), (l, c, "p1"))
            if s == 1:
                load(l, c, spot(color, 0), r[0], PAIR)
        else:
            p2(l, c, 0)

    def p2(l, c, s):
        color, by, _, _ = CHAINS[c]
        axis, beyond = NEXT_AXES[color]
        total = buf(ring1, rb, l, c, 3, 0)
        r = [buf(ring2, sb, l, c, 3, k) for k in range(3)]
        mine = second(total, c, spot(axis, -by * (1 + s)))
        if s:
            links.arrive((l, c, "p2", s - 1), r[s - 1])
            add_into(mine, r[s - 1])
        if s < 3:
            links.send((l, c, "p2", s), mine, r[s], peer(axis, by), None, buf(ring2, sb, l, c, 3, None), (l, c, "p2"))
        else:
            for slot, o in enumerate(AROUND):
                links.send((l, c, "p3", o), third(mine, c, spot(beyond, o)), buf(last, tb, l, c, 3, slot), peer(beyond, o), (l, c, "p3", 1), buf(last, tb, l, c, 3, None), (l, c, "p3"))

    def p3(l, c):
        color, _, is_in, i = CHAINS[c]
        axis, beyond = NEXT_AXES[color]
        t = [buf(last, tb, l, c, 3, k) for k in range(3)]
        links.arrive((l, c, "p3", 1), buf(last, tb, l, c, 3, None))
        mine = third(second(buf(ring1, rb, l, c, 3, 0), c, place[axis]), c, place[beyond])
        final = (fa if is_in else fb).at[l, :, pl.ds(LANE * i, LANE)]
        final[ALL] = (mine[ALL] + t[0][ALL]) + (t[1][ALL] + t[PAIR][ALL])

    def area(l, g, p, q):
        _, is_in, at, n, _ = GROUPS[g]
        if is_in:
            return oa.at[1 - l, p, :, lanes(q * quarter + LANE * at, LANE * n)]
        return ob.at[1 - l, p, q, :, pl.ds(LANE * at, LANE * n)]

    def line(l, g, at2, part):
        (first, _), is_in, _, _, _ = GROUPS[g]
        along = range(SIDE) if part is None else range(PAIR * part, PAIR * part + PAIR)
        span = pl.ds(along[0], len(along))
        if first == "y":
            return [area(l, g, span, at2)]
        return [area(l, g, at2, k) for k in along] if is_in else [area(l, g, at2, span)]

    def ag(l, g, s):
        (first, then), is_in, at, n, way = GROUPS[g]

        def piece(o):
            i, j = spot(first, o), spot(then, 0)
            return area(l, g, i, j) if first == "y" else area(l, g, j, i)

        if s == 0:
            src, dst = (fa if is_in else fb).at[l, :, pl.ds(LANE * at, LANE * n)], piece(0)
            for by in BOTH:
                links.send((l, g, "a1", by), src, dst, peer(first, by))
            copy = pltpu.make_async_copy(src, dst, osem.at[l, g])
            copy.start()
            local["own", l, g] = copy
        elif s == 1:
            for by in BOTH:
                landed = piece(-by)
                links.arrive((l, g, "a1", by), landed)
                if way == by:
                    links.send((l, g, "b1"), landed, landed, peer(first, by))
        elif s == PAIR:
            local["own", l, g].wait()
            links.arrive((l, g, "b1"), piece(PAIR))
            for k, part in enumerate(line(l, g, spot(then, 0), None)):
                for by in BOTH:
                    links.send((l, g, "a2", k, by), part, part, peer(then, by))
        elif s == 3:
            for by in BOTH:
                at2 = spot(then, -by)
                for k, part in enumerate(line(l, g, at2, None)):
                    links.arrive((l, g, "a2", k, by), part)
                for k, part in enumerate(line(l, g, at2, (1 - by) // PAIR)):
                    links.send((l, g, "a3", k, by), part, part, peer(then, by))
        else:
            for by in BOTH:
                for k, part in enumerate(line(l, g, spot(then, PAIR), (1 - by) // PAIR)):
                    links.arrive((l, g, "a3", k, by), part)

    stages = {"cols": cols, "rows": rows, "p1": p1, "p2": p2, "p3": p3, "ag": ag}
    for kind, *task in order:
        stages[kind](*task)
    for n in range(len(col_order)):
        if n >= len(col_order) - PAIR:
            settle("g", n)
    for n in range(len(row_order)):
        if n >= len(row_order) - PAIR:
            settle("b", n)
    links.drain()


def add_into(dst, src):
    lead = dst.shape[:-PAIR]
    if len(lead) == PAIR:
        @pl.loop(0, lead[0])
        def _(i):
            for j in range(lead[1]):
                dst[i, j] += src[i, j]
    elif len(lead) == 1:
        @pl.loop(0, lead[0])
        def _(i):
            dst[i] += src[i]
    else:
        dst[ALL] += src[ALL]


def reduce_gradients(h_rows, z_cols, m_rows, y_cols, scale_parts, starts=((0.0, 50.0), (0.0, 15.0))):
    hbm = pl.BlockSpec(memory_space=pltpu.HBM)
    rows, rows_out, dim, wide = h_rows[0].shape[1], m_rows[0].shape[1], y_cols[0].shape[1], z_cols[0].shape[1]
    pair = y_cols[0].shape[0]
    part, part_b = rows // SIDE, (rows_out + BAND) // 16
    n_in, n_out = len(IN_CHAINS), len(OUT_CHAINS)

    def buffers(slots, depth):
        shapes = {"x": ((SIDE, part, STRIP), (part, STRIP), (part, LANE)), "y": ((SIDE, part, STRIP), (SIDE, part, LANE), (part, LANE)),
                  "z": ((SIDE, SIDE, part, LANE), (SIDE, part, LANE), (part, LANE))}
        flat = ((SIDE, SIDE), (SIDE,), ())[depth]
        counts = {color: sum(e[0] == color for e in IN_CHAINS) for color in "xyz"}
        return [pltpu.VMEM((PAIR * counts[color] * slots, *shapes[color][depth]), F32) for color in "xyz"] + [
            pltpu.VMEM((PAIR * n_out * slots, *flat, part_b, LANE), F32)]

    out = lambda *shape: jax.ShapeDtypeStruct(shape, F32)
    sem = pltpu.SemaphoreType.DMA
    in_sums, out_sums, *_ = pl.pallas_call(
        functools.partial(reduce_kernel, reduce_order(part, part_b, starts)),
        out_shape=(out(PAIR, SIDE, part, wide), out(PAIR, SIDE, SIDE, part_b, dim), *[out(n_in, SIDE, SIDE, part, STRIP)] * PAIR, *[out(SIDE, SIDE, SIDE, part_b, dim)] * PAIR),
        in_specs=[hbm] * 9,
        out_specs=[hbm] * 6,
        scratch_shapes=[
            *buffers(PAIR, 0), *buffers(3, 0), *buffers(3, 1), *buffers(3, PAIR),
            pltpu.VMEM((PAIR, part, LANE * n_in), F32), pltpu.VMEM((PAIR, part_b, dim), F32),
            pltpu.VMEM((PAIR, *h_rows[0].shape), BF), pltpu.VMEM((PAIR, pair, dim), BF), pltpu.VMEM((PAIR, *scale_parts.shape[1:]), F32),
            pltpu.VMEM((PAIR, pair, STRIP), BF), pltpu.VMEM((PAIR, rows_out, pair), BF),
            pltpu.VMEM((PAIR, SIDE, SIDE, part, STRIP), F32), pltpu.VMEM((PAIR, SIDE, SIDE, part_b, dim), F32),
            sem((STRIP,)), sem((STRIP,)), sem((PAIR, n_in + n_out, 3)), sem((PAIR, len(GROUPS))), sem((PAIR, 3)), sem((PAIR,)), sem((PAIR,)), sem((PAIR,)), sem((PAIR,)),
        ],
        compiler_params=pltpu.CompilerParams(collective_id=1, has_side_effects=True, vmem_limit_bytes=67043328),
        name="reduce_gradients",
    )(*h_rows, *z_cols, *m_rows, *y_cols, scale_parts)
    return in_sums, out_sums


def rotary_tables(seq_len, head_dim):
    half_dim = head_dim // PAIR
    inv_freq = 10000.0 ** (-(jnp.arange(half_dim, dtype=jnp.float32) * 2.0 / head_dim))
    angles = jnp.arange(seq_len, dtype=jnp.float32)[:, None] * inv_freq[None, :]
    return jnp.cos(angles), jnp.sin(angles)


def solution(mesh):
    fsdp_size = mesh.shape["fsdp"]
    batch_spec = P(("dp", "fsdp"), None, None)
    scale_spec = P(None, "fsdp")
    weight_spec = P(None, "fsdp", None)

    def device_step(x_in, grad_y, norm_scale, w_in, w_out):
        n_layers = w_in.shape[0]
        seq_len, model_dim = x_in.shape[1:]
        proj_dim = w_in.shape[PAIR]
        ff_dim = w_out.shape[1] * fsdp_size - model_dim
        head_dim = (proj_dim - model_dim - PAIR * ff_dim) // PAIR
        rows, rows_out = norm_scale.shape[1], w_out.shape[1]
        scale_tile = jnp.pad(norm_scale.astype(jnp.float32), ((0, ROW - n_layers), (0, LANE - rows)))
        scales, *gathered = gather_weights(scale_tile, w_in, w_out)
        scale_full = scales[:, :n_layers, :rows].transpose(1, 0, PAIR).reshape(n_layers, model_dim)
        cos_tab, sin_tab = rotary_tables(seq_len, head_dim)
        cos_tab, sin_tab = jnp.tile(cos_tab, (1, ROW)), jnp.tile(sin_tab, (1, ROW))
        lane = jnp.arange(WIDE)
        down = lane[:, None] - lane[None, :]
        low = lane[None, :] % head_dim < head_dim // PAIR
        turn = jnp.where(low & (down == BAND), -1.0, jnp.where(~low & (down == -BAND), 1.0, 0.0)).astype(jnp.bfloat16)
        weights = [w.reshape(-1, w.shape[-1]) for w in gathered]
        hidden, grad_hidden, *rest = run_layers(x_in[0], grad_y[0], jnp.pad(scale_full, ((0, ROW - n_layers), (0, 0))), cos_tab, sin_tab, turn, weights)
        operands = [rest[PAIR * i:PAIR * i + PAIR][::-1] for i in range(SIDE)]
        in_sums, out_sums = reduce_gradients(*operands, rest[ROW][::-1])
        in_grads = in_sums.reshape(n_layers, rows, -1)[:, :, :proj_dim]
        out_rows = out_sums.reshape(n_layers, -1, model_dim)
        scale_grads = lax.dynamic_slice(out_rows[:, rows_out], (0, lax.axis_index("fsdp") * rows), (n_layers, rows))
        out_grads = out_rows[:, :rows_out]
        return hidden[None], grad_hidden[None], scale_grads, in_grads, out_grads

    return jax.shard_map(
        device_step,
        mesh=mesh,
        in_specs=(batch_spec, batch_spec, scale_spec, weight_spec, weight_spec),
        out_specs=(batch_spec, batch_spec, scale_spec, weight_spec, weight_spec),
        check_vma=False,
    )
```

```python
import functools
import jax
import jax.numpy as jnp
from jax import lax
from jax.experimental import pallas as pl
from jax.experimental.pallas import tpu as pltpu
from jax.sharding import PartitionSpec as P

MESH_ID = pl.DeviceIdType.MESH
BOTH = (1, -1)
AROUND = (1, -1, 2)
PARTS = (True, False)
ALL = ...
LANE, WIDE, STRIP, HEAD = 128, 256, 512, 64
ROW, BAND, SIDE, PAIR = 8, 32, 4, 2


class Links:
    def __init__(self, send_sems, recv_sems):
        self.send_sems, self.recv_sems = send_sems, recv_sems
        self.slots, self.batches, self.sent = {}, {}, {}

    def send(self, key, src, dst, device, landing=None, whole=None, batch=None):
        slot = self.slots.setdefault(landing or key, len(self.slots))
        leaving = self.batches.setdefault(batch or key, len(self.batches))
        copy = pltpu.make_async_remote_copy(
            src_ref=src, dst_ref=dst, send_sem=self.send_sems.at[leaving], recv_sem=self.recv_sems.at[slot],
            device_id=device, device_id_type=MESH_ID)
        copy.start()
        self.sent[batch or key] = (whole or src, leaving)

    def arrive(self, key, landed):
        slot = self.slots.setdefault(key, len(self.slots))
        pltpu.make_async_copy(landed, landed, self.recv_sems.at[slot]).wait()

    def drain(self):
        for left, leaving in self.sent.values():
            pltpu.make_async_copy(left, left, self.send_sems.at[leaving]).wait()
        self.sent.clear()


def rem(a, n):
    return a % n if isinstance(a, int) else lax.rem(a, n)


def chip_position():
    f, d = lax.axis_index("fsdp"), lax.axis_index("dp")
    return f // PAIR, rem(d, SIDE), d // SIDE, rem(f, PAIR)


def device_at(x, y, z, core):
    return (z * SIDE + y, x * PAIR + core)


def step(coord, by):
    return rem(coord + SIDE + by, SIDE)


def announce(devices):
    barrier = pltpu.get_barrier_semaphore()
    for device in devices:
        pl.semaphore_signal(barrier, inc=1, device_id=device, device_id_type=MESH_ID)
    pl.semaphore_wait(barrier, len(devices))


def plan(tasks, latency=2.5):
    free, landed, order, now = {}, {}, [], 0.0
    left = list(tasks)
    while left:
        best = None
        for place, (name, rank, start, needs, after, _, _) in enumerate(left):
            if all(n[0] in landed for n in needs) and all(n in landed for n in after):
                ready = max([start, now] + [landed[task][i] for task, i in needs])
                best = min(best or (ready, rank, place), (ready, rank, place))
        now, _, place = best
        name, _, _, _, _, sends, cost = left.pop(place)
        order.append(name)
        now += cost
        landed[name] = []
        for link, time in sends:
            free[link] = max(now, free.get(link, 0.0)) + time
            landed[name].append(free[link] + latency)
    return order


def forward_order(rows_i, cols_i, rows_o, cols_o, starts):
    rate = 23300.0
    tasks = []
    for m in range(SIDE):
        is_in = m % PAIR == 0
        edge = cols_i // LANE * SIDE // 9 // PAIR * WIDE
        size = {"y": rows_i // SIDE * edge, "x": rows_i * (cols_i - PAIR * edge)} if is_in else {"y": rows_o // SIDE * cols_o // PAIR}
        size["z"] = size["y"]
        for color in "yzx" if is_in else "yz":
            cost = size[color] / rate
            both = [(("x", by), cost) for by in BOTH]
            spread = [((color, by), cost) for by in BOTH] if color != "x" else []
            tasks.append((("reach", m, color), m, starts[m], [], [], both, 0.2))
            for i, by in enumerate(BOTH):
                tasks.append((("relay", m, color, by), m, 0.0, [(("reach", m, color), i)], [], [(("x", by), cost / PAIR)] + spread, 0.2))
            halves = [(("relay", m, color, by), 0) for by in BOTH]
            tasks.append((("far", m, color), m, 0.0, halves, [], spread, 0.2))
            if color == "x":
                continue
            for off, source, first in ((-1, ("relay", m, color, 1), 1), (1, ("relay", m, color, -1), 1), (PAIR, ("far", m, color), 0)):
                for i, by in enumerate(BOTH):
                    tasks.append((("pass", m, color, off, by), m, 0.0, [(source, first + i)], [], [((color, by), cost / PAIR)], 0.2))
                halves = [(("pass", m, color, off, by), 0) for by in BOTH]
                tasks.append((("close", m, color, off), m, 0.0, halves, [], [], 0.2))
        for off in (-1, 1, PAIR):
            last = [("close", m, color, off) for color in "yz"]
            if is_in:
                last.append(("far", m, "x") if off == PAIR else ("relay", m, "x", -off))
            tasks.append((("hand", m, off), m, 0.0, [], last, [("chip", (rows_i * cols_i if is_in else rows_o * cols_o) / 150000.0)], 0.2))
    before = []
    for l in range(PAIR):
        work = [(("norm", l), [], 0.8)] + [(("project", l, i), [PAIR * l], 1.4) for i in range(SIDE)]
        work += [(("attend", l), [], 4.0), (("mlp", l), [], 2.2), (("put", l), [PAIR * l + 1], 2.0)]
        for name, mats, cost in work:
            needs = [(("hand", m, off), 0) for m in mats for off in (-1, 1, PAIR)]
            tasks.append((name, 9, 0.0, needs, before, [], cost))
            before = [name]
    return plan(tasks)


def gather_stages(links, position, shard_i, shard_o, wi, wo, lsem):
    x, y, z, core = position
    twin = device_at(x, y, z, 1 - core)
    rows_i, cols_i = shard_i.shape[1:]
    rows_o, cols_o = shard_o.shape[1:]
    quarter_i, quarter_o = rows_i // SIDE, rows_o // SIDE
    third_i = cols_i // LANE * SIDE // 9 // PAIR * WIDE
    half_o = cols_o // PAIR
    cut_o = quarter_o // 16 * ROW + ROW if quarter_o % 16 else quarter_o // PAIR
    place = {"x": x, "y": y, "z": z}

    spots = {(axis, o): step(place[axis], o) for axis in "xyz" for o in range(SIDE)}

    def spot(axis, o):
        return spots[axis, o % SIDE]

    table = {}
    for axis in "xyz":
        for o in range(1, SIDE):
            moved = {**place, axis: spot(axis, o)}
            table[axis, o] = device_at(moved["x"], moved["y"], moved["z"], core)

    def peer(axis, o):
        return table[axis, o % SIDE]

    mats = []
    for l in range(PAIR):
        mats.append((shard_i.at[l], wi.at[l], rows_i, True))
        mats.append((shard_o.at[l], wo.at[l], rows_o, False))

    def region(is_in, color, q):
        if is_in:
            if color == "x":
                lo, hi = PAIR * third_i, cols_i
                rows = (0, rows_i)
            else:
                lo, hi = (0, third_i) if color == "y" else (third_i, PAIR * third_i)
                rows = (q * quarter_i, quarter_i)
            mid = lo + ((hi - lo) // LANE + 1) // PAIR * LANE
            return (rows, (lo, hi - lo)), (rows, (lo, mid - lo)), (rows, (mid, hi - mid))
        cols = (0, half_o) if color == "y" else (half_o, half_o)
        start = q * quarter_o
        return ((start, quarter_o), cols), ((start, cut_o), cols), ((start + cut_o, quarter_o - cut_o), cols)

    def at(m, xb, area):
        (r, nr), (c, nc) = area
        _, out, size, _ = mats[m]
        return out.at[pl.ds(pl.multiple_of((PAIR * xb + core) * size + r, ROW), nr), pl.ds(c, nc)]

    def block(m, xb, index):
        _, out, size, _ = mats[m]
        return out.at[pl.ds(pl.multiple_of((PAIR * xb + index) * size, BAND), size)]

    def colors(m):
        return "yzx" if mats[m][3] else "yz"

    def reach(m, color):
        src, _, _, is_in = mats[m]
        area = region(is_in, color, place[color])[0]
        for by in BOTH:
            links.send((m, "x1", color, by), src.at[pl.ds(pl.multiple_of(area[0][0], ROW), area[0][1]), pl.ds(*area[1])], at(m, x, area), peer("x", by))

    def launch(m, color, off):
        is_in = mats[m][3]
        moved = at(m, spot("x", off), region(is_in, color, place[color])[0])
        for by in BOTH:
            links.send((m, "p1", color, off, by), moved, moved, peer(color, by))

    def relay(m, color, by):
        is_in = mats[m][3]
        xb = spot("x", -by)
        areas = region(is_in, color, place[color])
        links.arrive((m, "x1", color, by), at(m, xb, areas[0]))
        part = at(m, xb, areas[1] if by == 1 else areas[PAIR])
        links.send((m, "x2", color, by), part, part, peer("x", by))
        if color != "x":
            launch(m, color, -by)

    def far(m, color):
        is_in = mats[m][3]
        areas = region(is_in, color, place[color])
        for by in BOTH:
            links.arrive((m, "x2", color, by), at(m, spot("x", PAIR), areas[1] if by == 1 else areas[PAIR]))
        if color != "x":
            launch(m, color, PAIR)

    def pass_on(m, color, off, by):
        is_in = mats[m][3]
        xb = spot("x", off)
        areas = region(is_in, color, spot(color, -by))
        links.arrive((m, "p1", color, off, by), at(m, xb, areas[0]))
        part = at(m, xb, areas[1] if by == 1 else areas[PAIR])
        links.send((m, "p2", color, off, by), part, part, peer(color, by))

    def close(m, color, off):
        is_in = mats[m][3]
        areas = region(is_in, color, spot(color, PAIR))
        for by in BOTH:
            links.arrive((m, "p2", color, off, by), at(m, spot("x", off), areas[1] if by == 1 else areas[PAIR]))

    def hand(m, off):
        whole = block(m, spot("x", off), core)
        links.send((m, "d2d", off), whole, whole, twin)

    owns = []

    def begin():
        for m, (src, _, _, _) in enumerate(mats):
            copy = pltpu.make_async_copy(src, block(m, x, core), lsem.at[m])
            copy.start()
            owns.append(copy)
            links.send((m, "d2d", 0), src, block(m, x, core), twin)

    def ready(m):
        owns[m].wait()
        for off in (0, -1, 1, PAIR):
            links.arrive((m, "d2d", off), block(m, spot("x", off), 1 - core))

    return begin, ready, peer, {"reach": reach, "relay": relay, "far": far, "pass": pass_on, "close": close, "hand": hand}


BF, F32 = jnp.bfloat16, jnp.float32


def product(a, b, contract=((1,), (0,))):
    return lax.dot_general(a, b, (contract, ((), ())), preferred_element_type=F32)


def lanes(start, size):
    return pl.ds(start if isinstance(start, int) else pl.multiple_of(start, LANE), size)


def layers_kernel(order, sc_ref, wi_ref, wo_ref, x_ref, dy_ref, cos_ref, sin_ref, turn_ref,
                  y_ref, gx_ref, ht_a, ht_b, z_a, z_b, mt_a, mt_b, yp_a, yp_b, sc_out,
                  wi, wo, z, om, h, hid, qr, kts, vts, ksl, scores, dscores, pcat, dscat,
                  dot_heads, qt, dht, dkv, omt, ht, dyt, sc, gains, gain_ref, load_sems, own_sems, send_sems, recv_sems,
                  share_send_sems, share_recv_sems):
    seq, dim = x_ref.shape
    ff = (wi.shape[PAIR] - dim - LANE) // PAIR
    position = chip_position()
    x, y, zc, core = position
    twin = device_at(x, y, zc, 1 - core)
    me = PAIR * x + core
    links, shared = Links(send_sems, recv_sems), Links(share_send_sems, share_recv_sems)
    stored, used = [], []
    begin, ready, peer, stages = gather_stages(links, position, wi_ref, wo_ref, wi, wo, load_sems)
    others = [(zc * SIDE + y, rem(me + k, ROW)) for k in range(1, ROW)]
    announce(others + [peer(axis, by) for axis in "yz" for by in BOTH])
    begin()
    for k, device in enumerate(others):
        links.send(("sc", k), sc_ref, gains.at[me], device)

    def keep(src, dst):
        copy = pltpu.make_async_copy(src, dst, own_sems.at[len(used)])
        copy.start()
        used.append(copy)
        stored.append(copy)

    def settle():
        for copy in stored:
            copy.wait()
        stored.clear()
        shared.drain()

    def share(key, src, out, place):
        keep(src, place(out, 0))
        shared.send(key, src, place(out, 1), twin)

    gains[me] = sc_ref[ALL]
    z[:, :, wi.shape[PAIR]:] = jnp.zeros((PAIR, seq, z.shape[PAIR] - wi.shape[PAIR]), BF)
    entry = (x_ref, hid.at[0])
    kts[ALL] = jnp.zeros(kts.shape, BF)
    vts[ALL] = jnp.zeros(vts.shape, BF)

    def normalise(l, src):
        @pl.loop(0, seq // BAND)
        def _(r):
            rows = pl.ds(pl.multiple_of(r * BAND, BAND), BAND)
            v = src[rows].astype(F32)
            v = v - jnp.mean(v, axis=-1, keepdims=True)
            var = jnp.mean(v * v, axis=-1, keepdims=True)
            h[l, rows] = (v * lax.rsqrt(var + 1e-6) * gain_ref[l:l + 1]).astype(BF)

    def project(l, quarter):
        def part(at, size):
            z[l, :, lanes(at, size)] = product(h[l], wi[l, :, lanes(at, size)]).astype(BF)

        n = wi.shape[PAIR] // STRIP

        @pl.loop(quarter * n // SIDE, (quarter + 1) * n // SIDE)
        def _(i):
            part(i * STRIP, STRIP)
        if quarter == 3:
            part(n * STRIP, wi.shape[PAIR] - n * STRIP)

    def heads(l):
        cos, sin = cos_ref[ALL], sin_ref[ALL]
        for g in range(dim // WIDE):
            q = z[l, :, g * WIDE:(g + 1) * WIDE]
            qr[l, :, g * WIDE:(g + 1) * WIDE] = ((q.astype(F32) * cos + product(q, turn_ref[ALL]) * sin) * 0.125).astype(BF)
        kv = z[l, :, dim:dim + LANE]
        turned = kv.astype(F32) * cos[:, :LANE] + product(kv, turn_ref[:LANE, :LANE]) * sin[:, :LANE]
        first = lax.broadcasted_iota(jnp.int32, turned.shape, 1) < HEAD
        key_lo = jnp.where(first, turned, 0.0)
        val_hi = jnp.where(first, 0.0, kv.astype(F32))
        return key_lo, pltpu.roll(key_lo, HEAD, 1), pltpu.roll(val_hi, HEAD, 1), val_hi

    def slot_rows(ref, lo, hi):
        zero = jnp.zeros((seq, LANE), BF)
        lo, hi = lo.astype(BF), hi.astype(BF)
        for i, (left, right) in enumerate(((lo, zero), (hi, zero), (zero, lo), (zero, hi))):
            ref[i * seq:(i + 1) * seq, :LANE] = left
            ref[i * seq:(i + 1) * seq, LANE:] = right

    def slot_cols(ref, lo):
        flat = lo.T[:HEAD].astype(BF)
        for i in range(SIDE):
            ref[HEAD * i:HEAD * (i + 1), i * seq:(i + 1) * seq] = flat

    def chances(rows, r, i):
        s = scores[rows, i * seq:(i + 1) * seq]
        at = lax.broadcasted_iota(jnp.int32, s.shape, 0) + r * BAND
        s = jnp.where(at >= lax.broadcasted_iota(jnp.int32, s.shape, 1), s, -1e30)
        e = jnp.exp(s - jnp.max(s, axis=-1, keepdims=True))
        return e * (1.0 / jnp.sum(e, axis=-1, keepdims=True))

    def attend(l):
        key_lo, _, val_lo, val_hi = heads(l)
        slot_cols(kts, key_lo)
        slot_rows(ksl, val_lo, val_hi)

        @pl.loop(0, dim // WIDE)
        def _(g):
            cols = lanes(g * WIDE, WIDE)
            scores[ALL] = product(qr[l, :, cols], kts[ALL])

            @pl.loop(0, seq // BAND)
            def _(r):
                rows = pl.ds(pl.multiple_of(r * BAND, BAND), BAND)
                for i in range(SIDE):
                    pcat[rows, i * seq:(i + 1) * seq] = chances(rows, r, i).astype(BF)
            om[:, cols] = product(pcat[ALL], ksl[ALL]).astype(BF)

    def mlp(l):
        @pl.loop(0, seq // BAND)
        def _(r):
            rows = pl.ds(pl.multiple_of(r * BAND, BAND), BAND)

            @pl.loop(0, ff // STRIP)
            def _(i):
                gate = z[l, rows, lanes(dim + LANE + i * STRIP, STRIP)].astype(F32)
                up = z[l, rows, lanes(dim + LANE + ff + i * STRIP, STRIP)].astype(F32)
                om[rows, lanes(dim + i * STRIP, STRIP)] = (gate * jax.nn.sigmoid(gate) * up).astype(BF)

    def put_out(l, dst):
        for n in range(dim // WIDE):
            cols = slice(n * WIDE, (n + 1) * WIDE)
            total = product(om[ALL], wo[l, :, cols])
            dst[:, cols] = (entry[l][:, cols].astype(F32) + total).astype(BF)

    def flip(src, dst, width):
        @pl.loop(0, width // WIDE)
        def _(i):
            dst[pl.ds(pl.multiple_of(i * WIDE, WIDE), WIDE)] = src(i * WIDE).T

    def backward(l, dy):
        flip(lambda at: dy[:, lanes(at, WIDE)], dyt, dim)

        @pl.loop(0, wo.shape[1] // dim)
        def _(n):
            rows = pl.ds(pl.multiple_of(n * dim, dim), dim)
            part = product(wo[l, rows], dyt[ALL]).astype(BF)
            om[:, lanes(n * dim, dim)] = part.T

            @pl.when(n == 0)
            def _():
                dot_heads[ALL] = part

        @pl.loop(0, seq // BAND)
        def _(r):
            rows = pl.ds(pl.multiple_of(r * BAND, BAND), BAND)

            @pl.loop(0, ff // STRIP)
            def _(i):
                gate_at, up_at = lanes(dim + LANE + i * STRIP, STRIP), lanes(dim + LANE + ff + i * STRIP, STRIP)
                gate, up = z[l, rows, gate_at].astype(F32), z[l, rows, up_at].astype(F32)
                d = om[rows, lanes(dim + i * STRIP, STRIP)].astype(F32)
                sig = jax.nn.sigmoid(gate)
                du = d * up
                z[l, rows, gate_at] = (du * sig + du * gate * (sig * (1.0 - sig))).astype(BF)
                z[l, rows, up_at] = (d * (gate * sig)).astype(BF)

        key_lo, key_hi, val_lo, val_hi = heads(l)
        slot_cols(kts, key_lo)
        slot_cols(vts, val_lo)
        slot_rows(ksl, key_lo, key_hi)
        dkv[ALL] = jnp.zeros(dkv.shape, F32)
        flip(lambda at: qr[l, :, lanes(at, WIDE)], qt, dim)

        @pl.loop(0, dim // WIDE)
        def _(g):
            cols = lanes(g * WIDE, WIDE)
            scores[ALL] = product(qr[l, :, cols], kts[ALL])
            dscores[ALL] = product(om[:, cols], vts[ALL])

            @pl.loop(0, seq // BAND)
            def _(r):
                rows = pl.ds(pl.multiple_of(r * BAND, BAND), BAND)
                for i in range(SIDE):
                    at = slice(i * seq, (i + 1) * seq)
                    p = chances(rows, r, i)
                    pcat[rows, at] = p.astype(BF)
                    pd = p * dscores[rows, at].astype(BF).astype(F32)
                    dscat[rows, at] = (pd - p * jnp.sum(pd, axis=-1, keepdims=True)).astype(BF)
            dq = product(dscat[ALL], ksl[ALL]).astype(BF)
            back = dq.astype(F32) * cos_ref[ALL] - product(dq, turn_ref[ALL]) * sin_ref[ALL]
            z[l, :, cols] = (back * 0.125).astype(BF)
            for i in range(SIDE):
                head = pl.ds(pl.multiple_of(g * WIDE + i * HEAD, HEAD), HEAD)
                at = slice(i * seq, (i + 1) * seq)
                dkv[:HEAD] += product(qt[head], dscat[:, at])
                dkv[HEAD:] += product(dot_heads[head], pcat[:, at])

        dkv_t = dkv[ALL].T
        dk = dkv_t.astype(BF)
        turned = dk.astype(F32) * cos_ref[:, :LANE] - product(dk, turn_ref[:LANE, :LANE]) * sin_ref[:, :LANE]
        first = lax.broadcasted_iota(jnp.int32, turned.shape, 1) < HEAD
        z[l, :, dim:dim + LANE] = jnp.where(first, turned, dkv_t).astype(BF)

    def backward_rows(l, dy, dst):
        n, width = wi.shape[PAIR] // 1408, 1408
        for i in range(n):
            at = slice(i * width, (i + 1) * width)
            part = product(wi[l, :, at], z[l, :, at], ((1,), (1,)))
            dht[ALL] = part if i == 0 else dht[ALL] + part
        for i in range(dim // WIDE):
            cols = slice(i * WIDE, (i + 1) * WIDE)
            h[l, :, cols] = dht[cols].T.astype(BF)
        sc[l] = jnp.zeros(sc.shape[1:], F32)

        @pl.loop(0, seq // BAND)
        def _(r):
            rows = pl.ds(pl.multiple_of(r * BAND, BAND), BAND)
            v = entry[l][rows].astype(F32)
            v = v - jnp.mean(v, axis=-1, keepdims=True)
            scale = lax.rsqrt(jnp.mean(v * v, axis=-1, keepdims=True) + 1e-6)
            hat = v * scale
            d = h[l, rows].astype(F32)
            each = (d * hat).reshape(SIDE, ROW, dim)
            sc[l] += (each[0] + each[1]) + (each[PAIR] + each[3])
            d = d * gain_ref[l:l + 1]
            d = scale * (d - jnp.mean(d, axis=-1, keepdims=True) - hat * jnp.mean(d * hat, axis=-1, keepdims=True))
            dst[rows] = (dy[rows].astype(F32) + d.astype(BF).astype(F32)).astype(BF)

    def give_rows(l, name, src, out):
        size = src.shape[0] // ROW
        for b in range(SIDE):
            mine = src.at[pl.ds(pl.multiple_of((PAIR * b + core) * size, BAND), size)]
            other = src.at[pl.ds(pl.multiple_of((PAIR * b + 1 - core) * size, BAND), size)]
            keep(mine, out.at[b, :, pl.ds(0, seq)])
            shared.send((name, l, b), other, out.at[b, :, pl.ds(seq, seq)], twin)

    def do_norm(l):
        if l == 0:
            for k, (_, f) in enumerate(others):
                links.arrive(("sc", k), gains.at[rem(me + 7 - k, ROW)])
            gain_ref[ALL] = jnp.sum(gains[ALL], axis=0)
        normalise(l, entry[l])
        settle()
        flip(lambda at: h[l, :, lanes(at, WIDE)], ht, dim)

    def do_project(l, i):
        if i == 0:
            ready(PAIR * l)
            give_rows(l, "ht", ht, (ht_a, ht_b)[l])
        project(l, i)

    def do_mlp(l):
        mlp(l)
        flip(lambda at: om[:, lanes(at, WIDE)], omt, om.shape[1])
        give_rows(l, "mt", omt, (mt_a, mt_b)[l])

    def do_put(l):
        ready(PAIR * l + 1)
        put_out(l, hid.at[0] if l == 0 else y_ref)

    stages.update(norm=do_norm, project=do_project, attend=attend, mlp=do_mlp, put=do_put)
    for kind, *task in order:
        stages[kind](*task)
    share(("y", 1), dy_ref, yp_b, lambda out, far: out.at[pl.ds(far * seq, seq)])
    for l, dy, dst in ((1, dy_ref, hid.at[1]), (0, hid.at[1], gx_ref)):
        if l == 0:
            share(("y", 0), dy, yp_a, lambda out, far: out.at[pl.ds(far * seq, seq)])
        backward(l, dy)
        share(("z", l), z.at[l], (z_a, z_b)[l], lambda out, far: out.at[pl.ds(far * seq, seq)])
        backward_rows(l, dy, dst)
        share(("scale", l), sc.at[l], sc_out.at[1 - l], lambda out, far: out.at[far])
    settle()
    for l in range(PAIR):
        for b in range(SIDE):
            shared.arrive(("ht", l, b), (ht_a, ht_b)[l].at[b, :, pl.ds(seq, seq)])
            shared.arrive(("mt", l, b), (mt_a, mt_b)[l].at[b, :, pl.ds(seq, seq)])
        shared.arrive(("y", l), (yp_a, yp_b)[l].at[pl.ds(seq, seq)])
        shared.arrive(("z", l), (z_a, z_b)[l].at[pl.ds(seq, seq)])
        shared.arrive(("scale", l), sc_out.at[1 - l, 1])
    links.drain()


def run_layers(x, dy, scale, w_in, w_out, cos, sin, turn, starts=(0.0, 10.0, 20.0, 30.0)):
    seq, dim = x.shape
    proj, cat = w_in.shape[PAIR], ROW * w_out.shape[1]
    wide = proj + LANE
    hbm, vmem = pl.BlockSpec(memory_space=pltpu.HBM), pl.BlockSpec(memory_space=pltpu.VMEM)
    out = lambda *shape, dtype=BF: jax.ShapeDtypeStruct(shape, dtype)
    buffer = lambda *shape, dtype=BF: pltpu.VMEM(shape, dtype)
    sem = pltpu.SemaphoreType.DMA
    pair = PAIR * seq
    return pl.pallas_call(
        functools.partial(layers_kernel, forward_order(*w_in.shape[1:], *w_out.shape[1:], starts)),
        out_shape=(out(seq, dim), out(seq, dim), *[out(SIDE, dim // ROW, pair)] * PAIR, *[out(pair, wide)] * PAIR, *[out(SIDE, cat // ROW, pair)] * PAIR,
                   *[out(pair, dim)] * PAIR, out(PAIR, PAIR, ROW, dim, dtype=F32)),
        in_specs=[vmem, hbm, hbm] + [vmem] * 5,
        out_specs=[vmem] * PAIR + [hbm] * 9,
        scratch_shapes=[
            buffer(PAIR, dim, proj), buffer(PAIR, cat, dim), buffer(PAIR, seq, wide), buffer(seq, cat), buffer(PAIR, seq, dim),
            buffer(PAIR, seq, dim), buffer(PAIR, seq, dim),
            buffer(WIDE, SIDE * seq), buffer(WIDE, SIDE * seq), buffer(SIDE * seq, WIDE),
            buffer(seq, SIDE * seq, dtype=F32), buffer(seq, SIDE * seq, dtype=F32), buffer(seq, SIDE * seq), buffer(seq, SIDE * seq),
            buffer(dim, seq), buffer(dim, seq), buffer(dim, seq, dtype=F32), buffer(LANE, seq, dtype=F32),
            buffer(cat, seq), buffer(dim, seq), buffer(dim, seq), buffer(PAIR, ROW, dim, dtype=F32),
            buffer(ROW, ROW, dim, dtype=F32), buffer(ROW, dim, dtype=F32),
            sem((SIDE,)), sem((BAND,)), sem((200,)), sem((200,)), sem((24,)), sem((24,)),
        ],
        compiler_params=pltpu.CompilerParams(collective_id=PAIR, has_side_effects=True, vmem_limit_bytes=67043328),
        name="run_layers",
    )(scale, w_in, w_out, x, dy, cos, sin, turn)


NEXT_AXES = {"x": "yz", "y": "zx", "z": "xy"}
IN_CHAINS = [("x", 1)] * 3 + [("x", -1)] * 3 + [("z", 1)] * PAIR + [("z", -1)] * PAIR + [("y", 1)] * PAIR + [("y", -1)] * PAIR
OUT_CHAINS = [("x", 1), ("x", -1), ("z", 1), ("z", -1), ("y", 1), ("y", -1)]
CHAINS = [(color, by, True, i) for i, (color, by) in enumerate(IN_CHAINS)] + [(color, by, False, i) for i, (color, by) in enumerate(OUT_CHAINS)]
GROUPS = [("yz", True, 0, 3, 1), ("yz", True, 3, 3, -1), ("yz", True, 6, PAIR, 1), ("zy", True, ROW, PAIR, -1), ("zy", True, 10, SIDE, 1),
          ("yz", False, 0, 3, -1), ("zy", False, 3, 3, -1)]


def reduce_order(rows, rows_b, starts):
    rate = 11650.0
    tasks = []
    for l in range(PAIR):
        for b in range(SIDE):
            tasks.append((("rows", l, b), (9 * l, -9, b), 0.0, [], [], [], 0.9))
        for c, (color, by, is_in, i) in enumerate(CHAINS):
            axes = color + NEXT_AXES[color]
            full = 16 * LANE * (rows if is_in else rows_b) / rate
            chain = [("p1", l, c, s) for s in range(SIDE)] + [("p2", l, c, s) for s in (1, PAIR, 3)] + [("p3", l, c)]
            sends = [[((axes[0], by), full)]] * 3 + [[((axes[1], by), full / SIDE)]] * 3
            sends += [[((axes[PAIR], o), full / 16) for o in (1, -1, 1)], []]
            turn = sum(e[:PAIR] == (color, by) for e in IN_CHAINS[:i]) if is_in else 3
            if is_in:
                before = [("cols", l, c)]
                tasks.append((before[0], (9 * l, -9, turn), 0.0, [], [], [], 0.7))
            else:
                before = [("rows", l, b) for b in range(SIDE)]
            for j, task in enumerate(chain):
                needs = [(chain[j - 1], n) for n in range(len(sends[j - 1]))] if j else []
                start = starts[0][l] + starts[1][l] * turn if j == 0 else 0.0
                tasks.append((task, (l, j - ROW if j else -10, 0), start, needs, [] if j else before, sends[j], 0.3))
        for g, ((first, then), is_in, at, n, way) in enumerate(GROUPS):
            piece = n * LANE * (rows if is_in else rows_b) / rate
            members = [c for c, e in enumerate(CHAINS) if e[PAIR] == is_in and at <= e[3] < at + n]
            for s in range(5):
                needs = []
                if s:
                    needs = [(("ag", l, g, s - 1), k) for k in ((0,) if s == PAIR else (0, 1))]
                sends = ([((first, by), piece) for by in BOTH], [((first, way), piece)], [((then, by), SIDE * piece) for by in BOTH],
                         [((then, by), PAIR * piece) for by in BOTH], [])[s]
                after = [] if s else [("p3", l, c) for c in members]
                tasks.append((("ag", l, g, s), (l, s - 5, 0), 0.0, needs, after, sends, 0.3))
    return plan(tasks)


def reduce_kernel(order, *refs):
    ht, z, mt, yp, sc = refs[0:PAIR], refs[PAIR:SIDE], refs[SIDE:6], refs[6:ROW], refs[ROW]
    oa, ob, ga, gb = refs[9], refs[10], refs[11:13], refs[13:15]
    (wx, wy, wz, wb, rx, ry, rz, rb, sx, sy, sz, sb, tx, ty, tz, tb, fa, fb,
     hbuf, ybuf, scbuf, zbuf, mbuf, cols_out, rows_out, ssem, rsem, lsem, osem, isem, zsem, msem, gsem, bsem) = refs[15:]
    x, y, zc, core = chip_position()
    place = {"x": x, "y": y, "z": zc}
    work, ring1, ring2 = {"x": wx, "y": wy, "z": wz}, {"x": rx, "y": ry, "z": rz}, {"x": sx, "y": sy, "z": sz}
    last = {"x": tx, "y": ty, "z": tz}
    firsts = {color: [e[0] for e in IN_CHAINS].index(color) for color in "xyz"}
    counts = {color: sum(e[0] == color for e in IN_CHAINS) for color in "xyz"}
    quarter = z[0].shape[1] // SIDE
    rows_b = gb[0].shape[3]

    spots = {(axis, o): step(place[axis], o) for axis in "xyz" for o in range(SIDE)}

    def spot(axis, o):
        return spots[axis, o % SIDE]

    peers = {}
    for axis in "xyz":
        for o in range(1, SIDE):
            moved = {**place, axis: spot(axis, o)}
            peers[axis, o] = device_at(moved["x"], moved["y"], moved["z"], core)

    def peer(axis, o):
        return peers[axis, o % SIDE]

    col_order = [task for task in order if task[0] == "cols"]
    row_order = [task for task in order if task[0] == "rows"]
    whole = []
    for l in range(PAIR):
        for i, (src, dst) in enumerate(((ht[l], hbuf.at[l]), (yp[l], ybuf.at[l]), (sc.at[l], scbuf.at[l]))):
            copy = pltpu.make_async_copy(src, dst, isem.at[l, i])
            copy.start()
            whole.append(copy)
    pending = {}

    def fetch_cols(n):
        if n < len(col_order):
            _, l, c = col_order[n]
            for q in range(SIDE):
                copy = pltpu.make_async_copy(z[l].at[:, pl.ds(q * quarter + LANE * c, LANE)], zbuf.at[n % PAIR, :, pl.ds(q * LANE, LANE)], zsem.at[n % PAIR])
                copy.start()

    def fetch_rows(n):
        if n < len(row_order):
            _, l, b = row_order[n]
            copy = pltpu.make_async_copy(mt[l].at[b], mbuf.at[n % PAIR], msem.at[n % PAIR])
            copy.start()
            pending["m", n] = copy

    for n in range(PAIR):
        fetch_cols(n)
        fetch_rows(n)
    announce([peer(axis, by) for axis in "xyz" for by in AROUND])
    links = Links(ssem, rsem)
    local = {}
    for copy in whole:
        copy.wait()

    def cols(l, c):
        n = col_order.index(("cols", l, c))
        slot = n % PAIR
        pltpu.make_async_copy(zbuf.at[slot], zbuf.at[slot], zsem.at[slot]).wait()
        if n >= PAIR:
            settle("g", n - PAIR)
        total = product(hbuf[l].reshape(-1, hbuf.shape[-1]), zbuf[slot])
        size = cols_out.shape[3]
        for i in range(16):
            cols_out[slot, i // SIDE, i % SIDE] = total[i * size:(i + 1) * size]
        fetch_cols(n + PAIR)
        copy = pltpu.make_async_copy(cols_out.at[slot], ga[l].at[c], gsem.at[slot])
        copy.start()
        pending["g", n] = copy
        local["g", l, c] = n

    def rows(l, b):
        n = row_order.index(("rows", l, b))
        slot = n % PAIR
        pending["m", n].wait()
        if n >= PAIR:
            settle("b", n - PAIR)
        total = product(mbuf[slot], ybuf[l])
        size, spare = total.shape[0] // rows_b, 16 * rows_b - total.shape[0]
        for i in range(size):
            rows_out[slot, i // SIDE, i % SIDE] = total[i * rows_b:(i + 1) * rows_b]
        gain = jnp.sum(scbuf[l, 0] + scbuf[l, 1], axis=0, keepdims=True)
        at = lax.broadcasted_iota(jnp.int32, (spare, total.shape[1]), 0)
        rows_out[slot, 3, 3] = jnp.where(at == 0, gain, 0.0)
        fetch_rows(n + PAIR)
        copy = pltpu.make_async_copy(rows_out.at[slot], gb[l].at[b], bsem.at[slot])
        copy.start()
        pending["b", n] = copy

    def settle(kind, n):
        if (kind, n) in pending and not local.get((kind, n)):
            pending[kind, n].wait()
            local[kind, n] = True

    def block(l, c, b):
        color, _, is_in, i = CHAINS[c]
        if is_in:
            ref = ga[l].at[i]
            return ref.at[b] if color == "x" else ref.at[:, b] if color == "y" else ref.at[:, :, :, lanes(b * LANE, LANE)]
        at = pl.ds(i * LANE, LANE)
        ref = gb[l]
        return ref.at[b, :, :, :, at] if color == "x" else ref.at[:, b, :, :, at] if color == "y" else ref.at[:, :, b, :, at]

    def second(ref, c, b):
        color, _, is_in, _ = CHAINS[c]
        if color == "y":
            return ref.at[:, :, lanes(b * LANE, LANE)] if is_in else ref.at[:, b]
        return ref.at[b]

    def third(ref, c, b):
        color, _, is_in, _ = CHAINS[c]
        return ref.at[:, lanes(b * LANE, LANE)] if is_in and color == "x" else ref.at[b]

    def buf(table, flat, l, c, slots, slot):
        color, _, is_in, i = CHAINS[c]
        ref = table[color] if is_in else flat
        first = (l * (counts[color] if is_in else len(OUT_CHAINS)) + (i - firsts[color] if is_in else i)) * slots
        return ref.at[pl.ds(first, slots)] if slot is None else ref.at[first + slot]

    def load(l, c, b, dst, tag):
        copy = pltpu.make_async_copy(block(l, c, b), dst, lsem.at[l, c, tag])
        copy.start()
        local[l, c, tag] = copy

    def p1(l, c, s):
        color, by, is_in, i = CHAINS[c]
        r = [buf(ring1, rb, l, c, 3, k) for k in range(3)]
        w = [buf(work, wb, l, c, PAIR, k) for k in range(PAIR)]
        if s == 0:
            if is_in:
                settle("g", local["g", l, c])
            else:
                for b in range(SIDE):
                    settle("b", row_order.index(("rows", l, b)))
            links.send((l, c, "p1", 0), block(l, c, spot(color, -by)), r[0], peer(color, by), None, buf(ring1, rb, l, c, 3, None), (l, c, "p1"))
            load(l, c, spot(color, -PAIR * by), w[1], 0)
            load(l, c, spot(color, -3 * by), w[0], 1)
            return
        mine = (None, w[1], w[0], r[0])[s]
        links.arrive((l, c, "p1", s - 1), r[s - 1])
        local[l, c, s - 1].wait()
        add_into(mine, r[s - 1])
        if s < 3:
            links.send((l, c, "p1", s), mine, r[s], peer(color, by), None, buf(ring1, rb, l, c, 3, None), (l, c, "p1"))
            if s == 1:
                load(l, c, spot(color, 0), r[0], PAIR)
        else:
            p2(l, c, 0)

    def p2(l, c, s):
        color, by, _, _ = CHAINS[c]
        axis, beyond = NEXT_AXES[color]
        total = buf(ring1, rb, l, c, 3, 0)
        r = [buf(ring2, sb, l, c, 3, k) for k in range(3)]
        mine = second(total, c, spot(axis, -by * (1 + s)))
        if s:
            links.arrive((l, c, "p2", s - 1), r[s - 1])
            add_into(mine, r[s - 1])
        if s < 3:
            links.send((l, c, "p2", s), mine, r[s], peer(axis, by), None, buf(ring2, sb, l, c, 3, None), (l, c, "p2"))
        else:
            for slot, o in enumerate(AROUND):
                links.send((l, c, "p3", o), third(mine, c, spot(beyond, o)), buf(last, tb, l, c, 3, slot), peer(beyond, o), (l, c, "p3", 1), buf(last, tb, l, c, 3, None), (l, c, "p3"))

    def p3(l, c):
        color, _, is_in, i = CHAINS[c]
        axis, beyond = NEXT_AXES[color]
        t = [buf(last, tb, l, c, 3, k) for k in range(3)]
        links.arrive((l, c, "p3", 1), buf(last, tb, l, c, 3, None))
        mine = third(second(buf(ring1, rb, l, c, 3, 0), c, place[axis]), c, place[beyond])
        final = (fa if is_in else fb).at[l, :, pl.ds(LANE * i, LANE)]
        final[ALL] = (mine[ALL] + t[0][ALL]) + (t[1][ALL] + t[PAIR][ALL])

    def area(l, g, p, q):
        _, is_in, at, n, _ = GROUPS[g]
        if is_in:
            return oa.at[1 - l, p, :, lanes(q * quarter + LANE * at, LANE * n)]
        return ob.at[1 - l, p, q, :, pl.ds(LANE * at, LANE * n)]

    def line(l, g, at2, part):
        (first, _), is_in, _, _, _ = GROUPS[g]
        along = range(SIDE) if part is None else range(PAIR * part, PAIR * part + PAIR)
        span = pl.ds(along[0], len(along))
        if first == "y":
            return [area(l, g, span, at2)]
        return [area(l, g, at2, k) for k in along] if is_in else [area(l, g, at2, span)]

    def ag(l, g, s):
        (first, then), is_in, at, n, way = GROUPS[g]

        def piece(o):
            i, j = spot(first, o), spot(then, 0)
            return area(l, g, i, j) if first == "y" else area(l, g, j, i)

        if s == 0:
            src, dst = (fa if is_in else fb).at[l, :, pl.ds(LANE * at, LANE * n)], piece(0)
            for by in BOTH:
                links.send((l, g, "a1", by), src, dst, peer(first, by))
            copy = pltpu.make_async_copy(src, dst, osem.at[l, g])
            copy.start()
            local["own", l, g] = copy
        elif s == 1:
            for by in BOTH:
                landed = piece(-by)
                links.arrive((l, g, "a1", by), landed)
                if way == by:
                    links.send((l, g, "b1"), landed, landed, peer(first, by))
        elif s == PAIR:
            local["own", l, g].wait()
            links.arrive((l, g, "b1"), piece(PAIR))
            for k, part in enumerate(line(l, g, spot(then, 0), None)):
                for by in BOTH:
                    links.send((l, g, "a2", k, by), part, part, peer(then, by))
        elif s == 3:
            for by in BOTH:
                at2 = spot(then, -by)
                for k, part in enumerate(line(l, g, at2, None)):
                    links.arrive((l, g, "a2", k, by), part)
                for k, part in enumerate(line(l, g, at2, (1 - by) // PAIR)):
                    links.send((l, g, "a3", k, by), part, part, peer(then, by))
        else:
            for by in BOTH:
                for k, part in enumerate(line(l, g, spot(then, PAIR), (1 - by) // PAIR)):
                    links.arrive((l, g, "a3", k, by), part)

    stages = {"cols": cols, "rows": rows, "p1": p1, "p2": p2, "p3": p3, "ag": ag}
    for kind, *task in order:
        stages[kind](*task)
    for n in range(len(col_order)):
        if n >= len(col_order) - PAIR:
            settle("g", n)
    for n in range(len(row_order)):
        if n >= len(row_order) - PAIR:
            settle("b", n)
    links.drain()


def add_into(dst, src):
    lead = dst.shape[:-PAIR]
    if len(lead) == PAIR:
        @pl.loop(0, lead[0])
        def _(i):
            for j in range(lead[1]):
                dst[i, j] += src[i, j]
    elif len(lead) == 1:
        @pl.loop(0, lead[0])
        def _(i):
            dst[i] += src[i]
    else:
        dst[ALL] += src[ALL]


def reduce_gradients(h_rows, z_cols, m_rows, y_cols, scale_parts, starts=((0.0, 50.0), (0.0, 15.0))):
    hbm = pl.BlockSpec(memory_space=pltpu.HBM)
    rows, rows_out, dim, wide = h_rows[0].shape[1], m_rows[0].shape[1], y_cols[0].shape[1], z_cols[0].shape[1]
    pair = y_cols[0].shape[0]
    part, part_b = rows // SIDE, (rows_out + BAND) // 16
    n_in, n_out = len(IN_CHAINS), len(OUT_CHAINS)

    def buffers(slots, depth):
        shapes = {"x": ((SIDE, part, STRIP), (part, STRIP), (part, LANE)), "y": ((SIDE, part, STRIP), (SIDE, part, LANE), (part, LANE)),
                  "z": ((SIDE, SIDE, part, LANE), (SIDE, part, LANE), (part, LANE))}
        flat = ((SIDE, SIDE), (SIDE,), ())[depth]
        counts = {color: sum(e[0] == color for e in IN_CHAINS) for color in "xyz"}
        return [pltpu.VMEM((PAIR * counts[color] * slots, *shapes[color][depth]), F32) for color in "xyz"] + [
            pltpu.VMEM((PAIR * n_out * slots, *flat, part_b, LANE), F32)]

    out = lambda *shape: jax.ShapeDtypeStruct(shape, F32)
    sem = pltpu.SemaphoreType.DMA
    in_sums, out_sums, *_ = pl.pallas_call(
        functools.partial(reduce_kernel, reduce_order(part, part_b, starts)),
        out_shape=(out(PAIR, SIDE, part, wide), out(PAIR, SIDE, SIDE, part_b, dim), *[out(n_in, SIDE, SIDE, part, STRIP)] * PAIR, *[out(SIDE, SIDE, SIDE, part_b, dim)] * PAIR),
        in_specs=[hbm] * 9,
        out_specs=[hbm] * 6,
        scratch_shapes=[
            *buffers(PAIR, 0), *buffers(3, 0), *buffers(3, 1), *buffers(3, PAIR),
            pltpu.VMEM((PAIR, part, LANE * n_in), F32), pltpu.VMEM((PAIR, part_b, dim), F32),
            pltpu.VMEM((PAIR, *h_rows[0].shape), BF), pltpu.VMEM((PAIR, pair, dim), BF), pltpu.VMEM((PAIR, *scale_parts.shape[1:]), F32),
            pltpu.VMEM((PAIR, pair, STRIP), BF), pltpu.VMEM((PAIR, rows_out, pair), BF),
            pltpu.VMEM((PAIR, SIDE, SIDE, part, STRIP), F32), pltpu.VMEM((PAIR, SIDE, SIDE, part_b, dim), F32),
            sem((STRIP,)), sem((STRIP,)), sem((PAIR, n_in + n_out, 3)), sem((PAIR, len(GROUPS))), sem((PAIR, 3)), sem((PAIR,)), sem((PAIR,)), sem((PAIR,)), sem((PAIR,)),
        ],
        compiler_params=pltpu.CompilerParams(collective_id=1, has_side_effects=True, vmem_limit_bytes=67043328),
        name="reduce_gradients",
    )(*h_rows, *z_cols, *m_rows, *y_cols, scale_parts)
    return in_sums, out_sums


def rotary_tables(seq_len, head_dim):
    half_dim = head_dim // PAIR
    inv_freq = 10000.0 ** (-(jnp.arange(half_dim, dtype=jnp.float32) * 2.0 / head_dim))
    angles = jnp.arange(seq_len, dtype=jnp.float32)[:, None] * inv_freq[None, :]
    return jnp.cos(angles), jnp.sin(angles)


def solution(mesh):
    fsdp_size = mesh.shape["fsdp"]
    batch_spec = P(("dp", "fsdp"), None, None)
    scale_spec = P(None, "fsdp")
    weight_spec = P(None, "fsdp", None)

    def device_step(x_in, grad_y, norm_scale, w_in, w_out):
        n_layers = w_in.shape[0]
        seq_len, model_dim = x_in.shape[1:]
        proj_dim = w_in.shape[PAIR]
        ff_dim = w_out.shape[1] * fsdp_size - model_dim
        head_dim = (proj_dim - model_dim - PAIR * ff_dim) // PAIR
        rows, rows_out = norm_scale.shape[1], w_out.shape[1]
        scale_rows = jnp.zeros((ROW, model_dim), jnp.float32)
        scale_rows = lax.dynamic_update_slice(scale_rows, norm_scale.astype(jnp.float32), (0, lax.axis_index("fsdp") * rows))
        cos_tab, sin_tab = rotary_tables(seq_len, head_dim)
        cos_tab, sin_tab = jnp.tile(cos_tab, (1, ROW)), jnp.tile(sin_tab, (1, ROW))
        lane = jnp.arange(WIDE)
        down = lane[:, None] - lane[None, :]
        low = lane[None, :] % head_dim < head_dim // PAIR
        turn = jnp.where(low & (down == BAND), -1.0, jnp.where(~low & (down == -BAND), 1.0, 0.0)).astype(jnp.bfloat16)
        hidden, grad_hidden, *rest = run_layers(x_in[0], grad_y[0], scale_rows, w_in, w_out, cos_tab, sin_tab, turn)
        operands = [rest[PAIR * i:PAIR * i + PAIR][::-1] for i in range(SIDE)]
        in_sums, out_sums = reduce_gradients(*operands, rest[ROW])
        in_grads = in_sums.reshape(n_layers, rows, -1)[:, :, :proj_dim]
        out_rows = out_sums.reshape(n_layers, -1, model_dim)
        scale_grads = lax.dynamic_slice(out_rows[:, rows_out], (0, lax.axis_index("fsdp") * rows), (n_layers, rows))
        out_grads = out_rows[:, :rows_out]
        return hidden[None], grad_hidden[None], scale_grads, in_grads, out_grads

    return jax.shard_map(
        device_step,
        mesh=mesh,
        in_specs=(batch_spec, batch_spec, scale_spec, weight_spec, weight_spec),
        out_specs=(batch_spec, batch_spec, scale_spec, weight_spec, weight_spec),
        check_vma=False,
    )
```

```python
import functools
import jax
import jax.numpy as jnp
from jax import lax
from jax.experimental import pallas as pl
from jax.experimental.pallas import tpu as pltpu
from jax.sharding import PartitionSpec as P

MESH_ID = pl.DeviceIdType.MESH
BOTH = (1, -1)
AROUND = (1, -1, 2)
PARTS = (True, False)
ALL = ...
LANE, WIDE, STRIP, HEAD = 128, 256, 512, 64
ROW, BAND, SIDE, PAIR = 8, 32, 4, 2


class Links:
    def __init__(self, send_sems, recv_sems):
        self.send_sems, self.recv_sems = send_sems, recv_sems
        self.slots, self.batches, self.sent = {}, {}, {}

    def send(self, key, src, dst, device, landing=None, whole=None, batch=None, lane=None):
        slot = self.slots.setdefault(landing or key, len(self.slots))
        leaving = self.batches.setdefault(batch or key, len(self.batches))
        copy = pltpu.make_async_remote_copy(
            src_ref=src, dst_ref=dst, send_sem=self.send_sems.at[leaving], recv_sem=self._landing(slot, lane),
            device_id=device, device_id_type=MESH_ID)
        copy.start()
        self.sent[batch or key] = (whole or src, leaving)

    def _landing(self, slot, lane):
        return self.recv_sems.at[slot] if lane is None else self.recv_sems.at[slot, lane]

    def arrive(self, key, landed, lane=None):
        slot = self.slots.setdefault(key, len(self.slots))
        pltpu.make_async_copy(landed, landed, self._landing(slot, lane)).wait()

    def drain(self):
        for left, leaving in self.sent.values():
            pltpu.make_async_copy(left, left, self.send_sems.at[leaving]).wait()
        self.sent.clear()


def rem(a, n):
    return a % n if isinstance(a, int) else lax.rem(a, n)


def chip_position():
    f, d = lax.axis_index("fsdp"), lax.axis_index("dp")
    return f // PAIR, rem(d, SIDE), d // SIDE, rem(f, PAIR)


def device_at(x, y, z, core):
    return (z * SIDE + y, x * PAIR + core)


def step(coord, by):
    return rem(coord + SIDE + by, SIDE)


def announce(devices):
    barrier = pltpu.get_barrier_semaphore()
    for device in devices:
        pl.semaphore_signal(barrier, inc=1, device_id=device, device_id_type=MESH_ID)
    pl.semaphore_wait(barrier, len(devices))


def plan(tasks, latency=2.5):
    free, landed, order, now = {}, {}, [], 0.0
    left = list(tasks)
    while left:
        best = None
        for place, (name, rank, start, needs, after, _, _) in enumerate(left):
            if all(n[0] in landed for n in needs) and all(n in landed for n in after):
                ready = max([start, now] + [landed[task][i] for task, i in needs])
                best = min(best or (ready, rank, place), (ready, rank, place))
        now, _, place = best
        name, _, _, _, _, sends, cost = left.pop(place)
        order.append(name)
        now += cost
        landed[name] = []
        for link, time in sends:
            free[link] = max(now, free.get(link, 0.0)) + time
            landed[name].append(free[link] + latency)
    return order


def forward_order(rows_i, cols_i, rows_o, cols_o, starts):
    rate = 23300.0
    tasks = []
    for m in range(SIDE):
        is_in = m % PAIR == 0
        edge = cols_i // LANE * SIDE // 9 // PAIR * WIDE
        size = {"y": rows_i // SIDE * edge, "x": rows_i * (cols_i - PAIR * edge)} if is_in else {"y": rows_o // SIDE * cols_o // PAIR}
        size["z"] = size["y"]
        for color in "yzx" if is_in else "yz":
            cost = size[color] / rate
            both = [(("x", by), cost) for by in BOTH]
            spread = [((color, by), cost) for by in BOTH] if color != "x" else []
            tasks.append((("reach", m, color), m, starts[m], [], [], both, 0.2))
            for i, by in enumerate(BOTH):
                tasks.append((("relay", m, color, by), m, 0.0, [(("reach", m, color), i)], [], [(("x", by), cost / PAIR)] + spread, 0.2))
            halves = [(("relay", m, color, by), 0) for by in BOTH]
            tasks.append((("far", m, color), m, 0.0, halves, [], spread, 0.2))
            if color == "x":
                continue
            for off, source, first in ((-1, ("relay", m, color, 1), 1), (1, ("relay", m, color, -1), 1), (PAIR, ("far", m, color), 0)):
                for i, by in enumerate(BOTH):
                    tasks.append((("pass", m, color, off, by), m, 0.0, [(source, first + i)], [], [((color, by), cost / PAIR)], 0.2))
                halves = [(("pass", m, color, off, by), 0) for by in BOTH]
                tasks.append((("close", m, color, off), m, 0.0, halves, [], [], 0.2))
        for off in (-1, 1, PAIR):
            last = [("close", m, color, off) for color in "yz"]
            if is_in:
                last.append(("far", m, "x") if off == PAIR else ("relay", m, "x", -off))
            tasks.append((("hand", m, off), m, 0.0, [], last, [("chip", (rows_i * cols_i if is_in else rows_o * cols_o) / 150000.0)], 0.2))
    before = []
    for l in range(PAIR):
        work = [(("norm", l), [], 0.8)] + [(("project", l, i), [PAIR * l], 1.4) for i in range(SIDE)]
        work += [(("attend", l), [], 4.0), (("mlp", l), [], 2.2), (("put", l), [PAIR * l + 1], 2.0)]
        for name, mats, cost in work:
            needs = [(("hand", m, off), 0) for m in mats for off in (-1, 1, PAIR)]
            tasks.append((name, 9, 0.0, needs, before, [], cost))
            before = [name]
    tasks.append((("give",), 9, 45.0, [], [], [], 0.3))
    return plan(tasks)


def gather_stages(links, position, shard_i, shard_o, wi, wo, lsem):
    x, y, z, core = position
    twin = device_at(x, y, z, 1 - core)
    rows_i, cols_i = shard_i.shape[1:]
    rows_o, cols_o = shard_o.shape[1:]
    quarter_i, quarter_o = rows_i // SIDE, rows_o // SIDE
    third_i = cols_i // LANE * SIDE // 9 // PAIR * WIDE
    half_o = cols_o // PAIR
    cut_o = quarter_o // 16 * ROW + ROW if quarter_o % 16 else quarter_o // PAIR
    place = {"x": x, "y": y, "z": z}

    spots = {(axis, o): step(place[axis], o) for axis in "xyz" for o in range(SIDE)}

    def spot(axis, o):
        return spots[axis, o % SIDE]

    table = {}
    for axis in "xyz":
        for o in range(1, SIDE):
            moved = {**place, axis: spot(axis, o)}
            table[axis, o] = device_at(moved["x"], moved["y"], moved["z"], core)

    def peer(axis, o):
        return table[axis, o % SIDE]

    mats = []
    for l in range(PAIR):
        mats.append((shard_i.at[l], wi.at[l], rows_i, True))
        mats.append((shard_o.at[l], wo.at[l], rows_o, False))

    def region(is_in, color, q):
        if is_in:
            if color == "x":
                lo, hi = PAIR * third_i, cols_i
                rows = (0, rows_i)
            else:
                lo, hi = (0, third_i) if color == "y" else (third_i, PAIR * third_i)
                rows = (q * quarter_i, quarter_i)
            mid = lo + ((hi - lo) // LANE + 1) // PAIR * LANE
            return (rows, (lo, hi - lo)), (rows, (lo, mid - lo)), (rows, (mid, hi - mid))
        cols = (0, half_o) if color == "y" else (half_o, half_o)
        start = q * quarter_o
        return ((start, quarter_o), cols), ((start, cut_o), cols), ((start + cut_o, quarter_o - cut_o), cols)

    def at(m, xb, area):
        (r, nr), (c, nc) = area
        _, out, size, _ = mats[m]
        return out.at[pl.ds(pl.multiple_of((PAIR * xb + core) * size + r, ROW), nr), pl.ds(c, nc)]

    def block(m, xb, index):
        _, out, size, _ = mats[m]
        return out.at[pl.ds(pl.multiple_of((PAIR * xb + index) * size, BAND), size)]

    def colors(m):
        return "yzx" if mats[m][3] else "yz"

    def reach(m, color):
        src, _, _, is_in = mats[m]
        area = region(is_in, color, place[color])[0]
        for by in BOTH:
            links.send((m, "x1", color, by), src.at[pl.ds(pl.multiple_of(area[0][0], ROW), area[0][1]), pl.ds(*area[1])], at(m, x, area), peer("x", by))

    def launch(m, color, off):
        is_in = mats[m][3]
        moved = at(m, spot("x", off), region(is_in, color, place[color])[0])
        for by in BOTH:
            links.send((m, "p1", color, off, by), moved, moved, peer(color, by))

    def relay(m, color, by):
        is_in = mats[m][3]
        xb = spot("x", -by)
        areas = region(is_in, color, place[color])
        links.arrive((m, "x1", color, by), at(m, xb, areas[0]))
        part = at(m, xb, areas[1] if by == 1 else areas[PAIR])
        links.send((m, "x2", color, by), part, part, peer("x", by))
        if color != "x":
            launch(m, color, -by)

    def far(m, color):
        is_in = mats[m][3]
        areas = region(is_in, color, place[color])
        for by in BOTH:
            links.arrive((m, "x2", color, by), at(m, spot("x", PAIR), areas[1] if by == 1 else areas[PAIR]))
        if color != "x":
            launch(m, color, PAIR)

    def pass_on(m, color, off, by):
        is_in = mats[m][3]
        xb = spot("x", off)
        areas = region(is_in, color, spot(color, -by))
        links.arrive((m, "p1", color, off, by), at(m, xb, areas[0]))
        part = at(m, xb, areas[1] if by == 1 else areas[PAIR])
        links.send((m, "p2", color, off, by), part, part, peer(color, by))

    def close(m, color, off):
        is_in = mats[m][3]
        areas = region(is_in, color, spot(color, PAIR))
        for by in BOTH:
            links.arrive((m, "p2", color, off, by), at(m, spot("x", off), areas[1] if by == 1 else areas[PAIR]))

    def hand(m, off):
        whole = block(m, spot("x", off), core)
        links.send((m, "d2d", off), whole, whole, twin)

    owns = []

    def begin():
        for m, (src, _, _, _) in enumerate(mats):
            copy = pltpu.make_async_copy(src, block(m, x, core), lsem.at[m])
            copy.start()
            owns.append(copy)
            links.send((m, "d2d", 0), src, block(m, x, core), twin)

    def ready(m):
        owns[m].wait()
        for off in (0, -1, 1, PAIR):
            links.arrive((m, "d2d", off), block(m, spot("x", off), 1 - core))

    return begin, ready, peer, {"reach": reach, "relay": relay, "far": far, "pass": pass_on, "close": close, "hand": hand}


BF, F32 = jnp.bfloat16, jnp.float32


def product(a, b, contract=((1,), (0,))):
    return lax.dot_general(a, b, (contract, ((), ())), preferred_element_type=F32)


def lanes(start, size):
    return pl.ds(start if isinstance(start, int) else pl.multiple_of(start, LANE), size)


def layers_kernel(order, sc_ref, wi_ref, wo_ref, x_ref, dy_ref, cos_ref, sin_ref, turn_ref,
                  y_ref, gx_ref, hy_a, hy_b, hz_a, hz_b, mx_a, mx_b, yx_a, yx_b, zy_b, zz_b, z_a, sc_out,
                  wi, wo, z, om, h, hid, qr, kts, vts, ksl, scores, dscores, pcat, dscat,
                  dot_heads, qt, dht, dkv, omt, ht, dyt, sc, gains, gain_ref, load_sems, own_sems, send_sems, recv_sems,
                  share_send_sems, share_recv_sems):
    seq, dim = x_ref.shape
    ff = (wi.shape[PAIR] - dim - LANE) // PAIR
    position = chip_position()
    x, y, zc, core = position
    twin = device_at(x, y, zc, 1 - core)
    me = PAIR * x + core
    links, shared = Links(send_sems, recv_sems), Links(share_send_sems, share_recv_sems)
    stored = []
    spots, _ = around(position)
    h_out, m_out, y_out, z_out = {"y": (hy_a, hy_b), "z": (hz_a, hz_b)}, (mx_a, mx_b), (yx_a, yx_b), {"y": zy_b, "z": zz_b}
    begin, ready, peer, stages = gather_stages(links, position, wi_ref, wo_ref, wi, wo, load_sems)
    others = [(zc * SIDE + y, rem(me + k, ROW)) for k in range(1, ROW)]

    def spot(axis, o):
        return spots[axis, o % SIDE]

    def device(axis, o, index):
        moved = {"x": x, "y": y, "z": zc, axis: spot(axis, o)}
        return device_at(moved["x"], moved["y"], moved["z"], index)

    announce(others + [device(axis, o, index) for axis in "yz" for o in AROUND for index in range(PAIR)])
    begin()
    for k, far in enumerate(others):
        links.send(("sc", k), sc_ref, gains.at[me], far)

    def keep(src, dst):
        copy = pltpu.make_async_copy(src, dst, own_sems.at[len(stored)])
        copy.start()
        stored.append(copy)

    def tokens(axis, o, index):
        return pl.ds(pl.multiple_of((PAIR * spot(axis, o) + index) * seq, seq), seq)

    def columns(axis, o):
        size = z.shape[PAIR] // ROW
        return lanes(((0 if axis == "y" else SIDE) + spot(axis, o)) * size, size)

    def send_h(l):
        for axis in "yz":
            out = h_out[axis][l].at[:, :, tokens(axis, 0, core)]
            for o in AROUND:
                for index in range(PAIR):
                    shared.send(("h", l, axis, o), ht.at[l, :, index], out, device(axis, o, index), batch=("h", l, axis, o, index), lane=core)
            shared.send(("h", l, axis), ht.at[l, :, 1 - core], out, twin, lane=0)
            keep(ht.at[l, :, core], out)

    def arrive_h(l):
        for axis in "yz":
            for o in AROUND:
                for index in range(PAIR):
                    shared.arrive(("h", l, axis, o), h_out[axis][l].at[:, :, tokens(axis, -o, index)], index)
            shared.arrive(("h", l, axis), h_out[axis][l].at[:, :, tokens(axis, 0, 1 - core)], 0)

    def row_block(l, o, index):
        size = omt.shape[1] // ROW
        return omt.at[l, pl.ds(pl.multiple_of((PAIR * spot("x", o) + index) * size, BAND), size)]

    def send_m(l):
        out = m_out[l].at[:, tokens("x", 0, core)]
        for o in AROUND:
            for index in range(PAIR):
                shared.send(("m", l, o), row_block(l, o, index), out, device("x", o, index), batch=("m", l, o, index), lane=core)
        shared.send(("m", l), row_block(l, 0, 1 - core), out, twin, lane=0)
        keep(row_block(l, 0, core), out)

    def arrive_m(l):
        for o in AROUND:
            for index in range(PAIR):
                shared.arrive(("m", l, o), m_out[l].at[:, tokens("x", -o, index)], index)
        shared.arrive(("m", l), m_out[l].at[:, tokens("x", 0, 1 - core)], 0)

    def send_y(l, src):
        out = y_out[l].at[tokens("x", 0, core)]
        for o in AROUND:
            shared.send(("y", l, o), src, out, device("x", o, core), lane=0)
        shared.send(("y", l), src, out, twin, lane=0)
        keep(src, out)

    def pass_y(l):
        for o in AROUND:
            landed = y_out[l].at[tokens("x", -o, core)]
            shared.arrive(("y", l, o), landed, 0)
            shared.send(("y", l, o, "pass"), landed, landed, twin, lane=0)

    def arrive_y(l):
        for o in AROUND:
            shared.arrive(("y", l, o, "pass"), y_out[l].at[tokens("x", -o, 1 - core)], 0)
        shared.arrive(("y", l), y_out[l].at[tokens("x", 0, 1 - core)], 0)

    def send_z(l):
        for axis in "yz":
            out = z_out[axis].at[tokens(axis, 0, core)]
            for o in AROUND:
                shared.send(("z", axis, o), z.at[l, :, columns(axis, o)], out, device(axis, o, core), lane=0)
            shared.send(("z", axis), z.at[l, :, columns(axis, 0)], out, twin, lane=0)
            keep(z.at[l, :, columns(axis, 0)], out)

    def pass_z():
        for axis in "yz":
            for o in AROUND:
                landed = z_out[axis].at[tokens(axis, -o, core)]
                shared.arrive(("z", axis, o), landed, 0)
                shared.send(("z", axis, o, "pass"), landed, landed, twin, lane=0)

    def arrive_z():
        for axis in "yz":
            for o in AROUND:
                shared.arrive(("z", axis, o, "pass"), z_out[axis].at[tokens(axis, -o, 1 - core)], 0)
            shared.arrive(("z", axis), z_out[axis].at[tokens(axis, 0, 1 - core)], 0)

    def send_scale(l):
        for k, far in enumerate(others):
            shared.send(("scale", l, k), sc.at[l], sc_out.at[l, me], far, lane=0)
        keep(sc.at[l], sc_out.at[l, me])

    def arrive_scale(l):
        for k in range(len(others)):
            shared.arrive(("scale", l, k), sc_out.at[l, rem(me + 7 - k, ROW)], 0)

    gains[me] = sc_ref[ALL]
    z[:, :, wi.shape[PAIR]:] = jnp.zeros((PAIR, seq, z.shape[PAIR] - wi.shape[PAIR]), BF)
    entry = (x_ref, hid.at[0])
    kts[ALL] = jnp.zeros(kts.shape, BF)
    vts[ALL] = jnp.zeros(vts.shape, BF)

    def normalise(l, src):
        @pl.loop(0, seq // BAND)
        def _(r):
            rows = pl.ds(pl.multiple_of(r * BAND, BAND), BAND)
            v = src[rows].astype(F32)
            v = v - jnp.mean(v, axis=-1, keepdims=True)
            var = jnp.mean(v * v, axis=-1, keepdims=True)
            h[l, rows] = (v * lax.rsqrt(var + 1e-6) * gain_ref[l:l + 1]).astype(BF)

    def project(l, quarter):
        def part(at, size):
            z[l, :, lanes(at, size)] = product(h[l], wi[l, :, lanes(at, size)]).astype(BF)

        n = wi.shape[PAIR] // STRIP

        @pl.loop(quarter * n // SIDE, (quarter + 1) * n // SIDE)
        def _(i):
            part(i * STRIP, STRIP)
        if quarter == 3:
            part(n * STRIP, wi.shape[PAIR] - n * STRIP)

    def heads(l):
        cos, sin = cos_ref[ALL], sin_ref[ALL]
        for g in range(dim // WIDE):
            q = z[l, :, g * WIDE:(g + 1) * WIDE]
            qr[l, :, g * WIDE:(g + 1) * WIDE] = ((q.astype(F32) * cos + product(q, turn_ref[ALL]) * sin) * 0.125).astype(BF)
        kv = z[l, :, dim:dim + LANE]
        turned = kv.astype(F32) * cos[:, :LANE] + product(kv, turn_ref[:LANE, :LANE]) * sin[:, :LANE]
        first = lax.broadcasted_iota(jnp.int32, turned.shape, 1) < HEAD
        key_lo = jnp.where(first, turned, 0.0)
        val_hi = jnp.where(first, 0.0, kv.astype(F32))
        return key_lo, pltpu.roll(key_lo, HEAD, 1), pltpu.roll(val_hi, HEAD, 1), val_hi

    def slot_rows(ref, lo, hi):
        zero = jnp.zeros((seq, LANE), BF)
        lo, hi = lo.astype(BF), hi.astype(BF)
        for i, (left, right) in enumerate(((lo, zero), (hi, zero), (zero, lo), (zero, hi))):
            ref[i * seq:(i + 1) * seq, :LANE] = left
            ref[i * seq:(i + 1) * seq, LANE:] = right

    def slot_cols(ref, lo):
        flat = lo.T[:HEAD].astype(BF)
        for i in range(SIDE):
            ref[HEAD * i:HEAD * (i + 1), i * seq:(i + 1) * seq] = flat

    def chances(rows, r, i):
        s = scores[rows, i * seq:(i + 1) * seq]
        at = lax.broadcasted_iota(jnp.int32, s.shape, 0) + r * BAND
        s = jnp.where(at >= lax.broadcasted_iota(jnp.int32, s.shape, 1), s, -1e30)
        e = jnp.exp(s - jnp.max(s, axis=-1, keepdims=True))
        return e * (1.0 / jnp.sum(e, axis=-1, keepdims=True))

    def attend(l):
        key_lo, _, val_lo, val_hi = heads(l)
        slot_cols(kts, key_lo)
        slot_rows(ksl, val_lo, val_hi)

        @pl.loop(0, dim // WIDE)
        def _(g):
            cols = lanes(g * WIDE, WIDE)
            scores[ALL] = product(qr[l, :, cols], kts[ALL])

            @pl.loop(0, seq // BAND)
            def _(r):
                rows = pl.ds(pl.multiple_of(r * BAND, BAND), BAND)
                for i in range(SIDE):
                    pcat[rows, i * seq:(i + 1) * seq] = chances(rows, r, i).astype(BF)
            om[:, cols] = product(pcat[ALL], ksl[ALL]).astype(BF)

    def mlp(l):
        @pl.loop(0, seq // BAND)
        def _(r):
            rows = pl.ds(pl.multiple_of(r * BAND, BAND), BAND)

            @pl.loop(0, ff // STRIP)
            def _(i):
                gate = z[l, rows, lanes(dim + LANE + i * STRIP, STRIP)].astype(F32)
                up = z[l, rows, lanes(dim + LANE + ff + i * STRIP, STRIP)].astype(F32)
                om[rows, lanes(dim + i * STRIP, STRIP)] = (gate * jax.nn.sigmoid(gate) * up).astype(BF)

    def put_out(l, dst):
        for n in range(dim // WIDE):
            cols = slice(n * WIDE, (n + 1) * WIDE)
            total = product(om[ALL], wo[l, :, cols])
            dst[:, cols] = (entry[l][:, cols].astype(F32) + total).astype(BF)

    def flip(src, dst, width):
        @pl.loop(0, width // WIDE)
        def _(i):
            dst[pl.ds(pl.multiple_of(i * WIDE, WIDE), WIDE)] = src(i * WIDE).T

    def backward(l, dy):
        flip(lambda at: dy[:, lanes(at, WIDE)], dyt, dim)

        @pl.loop(0, wo.shape[1] // dim)
        def _(n):
            rows = pl.ds(pl.multiple_of(n * dim, dim), dim)
            part = product(wo[l, rows], dyt[ALL]).astype(BF)
            om[:, lanes(n * dim, dim)] = part.T

            @pl.when(n == 0)
            def _():
                dot_heads[ALL] = part

        @pl.loop(0, seq // BAND)
        def _(r):
            rows = pl.ds(pl.multiple_of(r * BAND, BAND), BAND)

            @pl.loop(0, ff // STRIP)
            def _(i):
                gate_at, up_at = lanes(dim + LANE + i * STRIP, STRIP), lanes(dim + LANE + ff + i * STRIP, STRIP)
                gate, up = z[l, rows, gate_at].astype(F32), z[l, rows, up_at].astype(F32)
                d = om[rows, lanes(dim + i * STRIP, STRIP)].astype(F32)
                sig = jax.nn.sigmoid(gate)
                du = d * up
                z[l, rows, gate_at] = (du * sig + du * gate * (sig * (1.0 - sig))).astype(BF)
                z[l, rows, up_at] = (d * (gate * sig)).astype(BF)

        key_lo, key_hi, val_lo, val_hi = heads(l)
        slot_cols(kts, key_lo)
        slot_cols(vts, val_lo)
        slot_rows(ksl, key_lo, key_hi)
        dkv[ALL] = jnp.zeros(dkv.shape, F32)
        flip(lambda at: qr[l, :, lanes(at, WIDE)], qt, dim)

        @pl.loop(0, dim // WIDE)
        def _(g):
            cols = lanes(g * WIDE, WIDE)
            scores[ALL] = product(qr[l, :, cols], kts[ALL])
            dscores[ALL] = product(om[:, cols], vts[ALL])

            @pl.loop(0, seq // BAND)
            def _(r):
                rows = pl.ds(pl.multiple_of(r * BAND, BAND), BAND)
                for i in range(SIDE):
                    at = slice(i * seq, (i + 1) * seq)
                    p = chances(rows, r, i)
                    pcat[rows, at] = p.astype(BF)
                    pd = p * dscores[rows, at].astype(BF).astype(F32)
                    dscat[rows, at] = (pd - p * jnp.sum(pd, axis=-1, keepdims=True)).astype(BF)
            dq = product(dscat[ALL], ksl[ALL]).astype(BF)
            back = dq.astype(F32) * cos_ref[ALL] - product(dq, turn_ref[ALL]) * sin_ref[ALL]
            z[l, :, cols] = (back * 0.125).astype(BF)
            for i in range(SIDE):
                head = pl.ds(pl.multiple_of(g * WIDE + i * HEAD, HEAD), HEAD)
                at = slice(i * seq, (i + 1) * seq)
                dkv[:HEAD] += product(qt[head], dscat[:, at])
                dkv[HEAD:] += product(dot_heads[head], pcat[:, at])

        dkv_t = dkv[ALL].T
        dk = dkv_t.astype(BF)
        turned = dk.astype(F32) * cos_ref[:, :LANE] - product(dk, turn_ref[:LANE, :LANE]) * sin_ref[:, :LANE]
        first = lax.broadcasted_iota(jnp.int32, turned.shape, 1) < HEAD
        z[l, :, dim:dim + LANE] = jnp.where(first, turned, dkv_t).astype(BF)

    def backward_rows(l, dy, dst):
        n, width = wi.shape[PAIR] // 1408, 1408
        for i in range(n):
            at = slice(i * width, (i + 1) * width)
            part = product(wi[l, :, at], z[l, :, at], ((1,), (1,)))
            dht[ALL] = part if i == 0 else dht[ALL] + part
        for i in range(dim // WIDE):
            cols = slice(i * WIDE, (i + 1) * WIDE)
            h[l, :, cols] = dht[cols].T.astype(BF)
        sc[l] = jnp.zeros(sc.shape[1:], F32)

        @pl.loop(0, seq // BAND)
        def _(r):
            rows = pl.ds(pl.multiple_of(r * BAND, BAND), BAND)
            v = entry[l][rows].astype(F32)
            v = v - jnp.mean(v, axis=-1, keepdims=True)
            scale = lax.rsqrt(jnp.mean(v * v, axis=-1, keepdims=True) + 1e-6)
            hat = v * scale
            d = h[l, rows].astype(F32)
            each = (d * hat).reshape(SIDE, ROW, dim)
            sc[l] += (each[0] + each[1]) + (each[PAIR] + each[3])
            d = d * gain_ref[l:l + 1]
            d = scale * (d - jnp.mean(d, axis=-1, keepdims=True) - hat * jnp.mean(d * hat, axis=-1, keepdims=True))
            dst[rows] = (dy[rows].astype(F32) + d.astype(BF).astype(F32)).astype(BF)

    def do_norm(l):
        if l == 0:
            for k, (_, f) in enumerate(others):
                links.arrive(("sc", k), gains.at[rem(me + 7 - k, ROW)])
            gain_ref[ALL] = jnp.sum(gains[ALL], axis=0)
        normalise(l, entry[l])
        for i in range(dim // WIDE):
            flat = h[l, :, i * WIDE:(i + 1) * WIDE].T
            size = ht.shape[3]
            for b in range(ROW):
                lo, hi = max(b * size, i * WIDE), min((b + 1) * size, (i + 1) * WIDE)
                if lo < hi:
                    ht[l, b // PAIR, b % PAIR, lo - b * size:hi - b * size] = flat[lo - i * WIDE:hi - i * WIDE]

    def do_project(l, i):
        if i == 0:
            ready(PAIR * l)
        project(l, i)

    def do_mlp(l):
        mlp(l)
        flip(lambda at: om[:, lanes(at, WIDE)], omt.at[l], om.shape[1])
        if l == 0:
            send_m(l)

    def do_put(l):
        ready(PAIR * l + 1)
        put_out(l, hid.at[0] if l == 0 else y_ref)

    stages.update(norm=do_norm, project=do_project, attend=attend, mlp=do_mlp, put=do_put, give=lambda: send_y(1, dy_ref))
    for kind, *task in order:
        stages[kind](*task)
    send_h(0)
    send_h(1)
    send_m(1)
    middle = hid.at[1]
    backward(1, dy_ref)
    send_z(1)
    backward_rows(1, dy_ref, middle)
    send_y(0, middle)
    send_scale(1)
    pass_y(1)
    backward(0, middle)
    keep(z.at[0], z_a)
    pass_z()
    backward_rows(0, middle, gx_ref)
    send_scale(0)
    pass_y(0)
    for l in range(PAIR):
        arrive_h(l)
        arrive_m(l)
        arrive_scale(l)
        arrive_y(l)
    arrive_z()
    for copy in stored:
        copy.wait()
    shared.drain()
    links.drain()


def run_layers(x, dy, scale, w_in, w_out, cos, sin, turn, starts=(0.0, 10.0, 20.0, 30.0)):
    seq, dim = x.shape
    proj, cat = w_in.shape[PAIR], ROW * w_out.shape[1]
    wide = proj + LANE
    hbm, vmem = pl.BlockSpec(memory_space=pltpu.HBM), pl.BlockSpec(memory_space=pltpu.VMEM)
    out = lambda *shape, dtype=BF: jax.ShapeDtypeStruct(shape, dtype)
    buffer = lambda *shape, dtype=BF: pltpu.VMEM(shape, dtype)
    sem = pltpu.SemaphoreType.DMA
    line = ROW * seq
    return pl.pallas_call(
        functools.partial(layers_kernel, forward_order(*w_in.shape[1:], *w_out.shape[1:], starts)),
        out_shape=(out(seq, dim), out(seq, dim), *[out(SIDE, dim // ROW, line)] * SIDE, *[out(cat // ROW, line)] * PAIR, *[out(line, dim)] * PAIR,
                   *[out(line, wide // ROW)] * PAIR, out(seq, wide), out(PAIR, ROW, ROW, dim, dtype=F32)),
        in_specs=[vmem, hbm, hbm] + [vmem] * 5,
        out_specs=[vmem] * PAIR + [hbm] * 12,
        scratch_shapes=[
            buffer(PAIR, dim, proj), buffer(PAIR, cat, dim), buffer(PAIR, seq, wide), buffer(seq, cat), buffer(PAIR, seq, dim),
            buffer(PAIR, seq, dim), buffer(PAIR, seq, dim),
            buffer(WIDE, SIDE * seq), buffer(WIDE, SIDE * seq), buffer(SIDE * seq, WIDE),
            buffer(seq, SIDE * seq, dtype=F32), buffer(seq, SIDE * seq, dtype=F32), buffer(seq, SIDE * seq), buffer(seq, SIDE * seq),
            buffer(dim, seq), buffer(dim, seq), buffer(dim, seq, dtype=F32), buffer(LANE, seq, dtype=F32),
            buffer(PAIR, cat, seq), buffer(PAIR, SIDE, PAIR, dim // ROW, seq), buffer(dim, seq), buffer(PAIR, ROW, dim, dtype=F32),
            buffer(ROW, ROW, dim, dtype=F32), buffer(ROW, dim, dtype=F32),
            sem((SIDE,)), sem((16,)), sem((200,)), sem((200,)), sem((96,)), sem((96, PAIR)),
        ],
        compiler_params=pltpu.CompilerParams(collective_id=PAIR, has_side_effects=True, vmem_limit_bytes=67043328),
        name="run_layers",
    )(scale, w_in, w_out, x, dy, cos, sin, turn)


PARTS = (("i", "x", "z", "y", 0, STRIP), ("i", "x", "z", "y", STRIP, 384), ("i", "x", "y", "z", 0, STRIP), ("i", "x", "y", "z", STRIP, 384),
         ("o", "y", "z", "y", 0, 384), ("o", "z", "y", "z", 384, 384))


def reduce_order(rows, rows_b, starts):
    rate = 11650.0
    tasks = []
    moved = WIDE * 896 / (PAIR * rate)
    tasks.append((("swap",), (0, 0), 0.0, [], [], [((axis, by), moved * n) for axis in "yz" for by, n in ((1, 1), (-1, 1), (1, PAIR))] + [("chip", 0.8)] * PAIR, 0.5))
    for i, axis in enumerate("yz"):
        for j, o in enumerate(AROUND):
            tasks.append((("pass", axis, o), (0, 1), 0.0, [(("swap",), 3 * i + j)], [], [("chip", 1.6)], 0.2))
    for l in (1, 0):
        late = 1 - l
        for c, (kind, first, then, last, at, width) in enumerate(PARTS):
            needs, cost = [], 1.6 * width / STRIP
            if kind == "i" and l == 0:
                needs = [(("pass", last, o), 0) for o in AROUND]
            tasks.append((("make", l, c), (9 * late, -c), starts[late], needs, [], [], cost))
            full = SIDE * SIDE * (rows if kind == "i" else rows_b) * width / rate
            sends = [[((first, by), full / ROW) for by in BOTH], [((first, by), full / SIDE) for by in BOTH],
                     [((then, o), full / 16) for o in (1, -1, 1)], []]
            piece = full / 16
            sends += [[((then, by), piece) for by in BOTH], [((then, 1 - PAIR * (c % PAIR)), piece)], [((last, by), SIDE * piece) for by in BOTH],
                      [((last, by), PAIR * piece) for by in BOTH], []]
            for s in range(9):
                task = ("sum", l, c, s)
                needs = [(("sum", l, c, s - 1), k) for k in range(len(sends[s - 1]))] if s else []
                tasks.append((task, (late, -s), 0.0, needs, [("make", l, c)] if s == 0 else [("sum", l, c, s - 1)], sends[s], 0.3))
    return plan(tasks)


def reduce_kernel(order, *refs):
    hy, hz, mx, yx = refs[0:PAIR], refs[PAIR:SIDE], refs[SIDE:6], refs[6:ROW]
    zy1, zz1, z0, sc = refs[ROW:12]
    oa, ob = refs[12:14]
    n = len(PARTS)
    total, half, full, small, front = (refs[14 + k * n:14 + (k + 1) * n] for k in range(5))
    (hbuf, zbuf, mbuf, ybuf, scbuf, ssem, rsem, isem, osem, zsem) = refs[14 + 5 * n:]
    position = chip_position()
    x, y, zc, core = position
    place = {"x": x, "y": y, "z": zc}
    twin = device_at(x, y, zc, 1 - core)
    spots, peers = around(position)

    def spot(axis, o):
        return spots[axis, o % SIDE]

    def peer(axis, o):
        return peers[axis, o % SIDE]

    seq, wide = z0.shape
    own = wide // ROW
    loads = {}

    def load(key, src, dst):
        copy = pltpu.make_async_copy(src, dst, isem.at[len(loads)])
        copy.start()
        loads[key] = copy

    for l in (1, 0):
        if l:
            load(("z", 1, "y"), zy1, zbuf.at[1, 0])
            load(("z", 1, "z"), zz1, zbuf.at[1, 1])
        load(("h", l, "y"), hy[l], hbuf.at[l, 0])
        load(("h", l, "z"), hz[l], hbuf.at[l, 1])
        load(("m", l), mx[l], mbuf.at[l])
        load(("y", l), yx[l], ybuf.at[l])
        load(("s", l), sc.at[l], scbuf.at[l])
    done = set()

    def loaded(*keys):
        for key in keys:
            if key not in done:
                loads[key].wait()
                done.add(key)

    announce([peer(axis, o) for axis in "xyz" for o in AROUND] + [twin])
    links = Links(ssem, rsem)

    def columns(axis, o):
        return lanes(((0 if axis == "y" else SIDE) + spot(axis, o)) * own, own)

    def tokens(axis, o, index):
        return pl.ds(pl.multiple_of((PAIR * spot(axis, o) + index) * seq, seq), seq)

    def swap():
        for i, axis in enumerate("yz"):
            mine = zbuf.at[0, i, tokens(axis, 0, core)]
            for o in AROUND:
                links.send(("z", axis, o), z0.at[:, columns(axis, o)], mine, peer(axis, o))
            links.send(("near", axis), z0.at[:, columns(axis, 0)], mine, twin)
            load(("own", axis), z0.at[:, columns(axis, 0)], mine)

    def hand_on(axis, o):
        i = "yz".index(axis)
        landed = zbuf.at[0, i, tokens(axis, -o, core)]
        links.arrive(("z", axis, o), landed)
        links.send(("pass", axis, o), landed, landed, twin)

    def make(l, c):
        kind, first, then, last, at, width = PARTS[c]
        if kind == "i":
            i = "yz".index(last)
            loaded(("h", l, last))
            if l:
                loaded(("z", 1, last))
            elif ("joined", last) not in done:
                done.add(("joined", last))
                loaded(("own", last))
                links.arrive(("near", last), zbuf.at[0, i, tokens(last, 0, 1 - core)])
                for o in AROUND:
                    links.arrive(("pass", last, o), zbuf.at[0, i, tokens(last, -o, 1 - core)])
            size = total[c].shape[3]
            for lo in range(0, width, WIDE):
                hi = min(width, lo + WIDE)
                part = product(hbuf[l, i].reshape(-1, hbuf.shape[-1]), zbuf[l, i, :, at + lo:at + hi])
                for r in range(16):
                    total[c][l, r // SIDE, r % SIDE, :, lo:hi] = part[r * size:(r + 1) * size]
            return
        loaded(("m", l), ("y", l), ("s", l))
        part = product(mbuf[l], ybuf[l, :, at:at + width])
        size = total[c].shape[3]

        def put(r, value):
            total[c][(l, r // SIDE, r % SIDE) if first == "y" else (l, r % SIDE, r // SIDE)] = value

        for r in range(part.shape[0] // size):
            put(r, part[r * size:(r + 1) * size])
        gain = jnp.sum(jnp.sum(scbuf[l, :, :, at:at + width], axis=0), axis=0, keepdims=True)
        row = lax.broadcasted_iota(jnp.int32, (size, width), 0)
        put(15, jnp.where(row == 0, gain, 0.0))

    def area(l, c, o, whole):
        kind, first, then, last, at, width = PARTS[c]
        inner = (spot(then, whole) if isinstance(whole, int) else whole)
        outer = spot(last, o)
        if kind == "i":
            cols = lanes(((0 if last == "y" else SIDE) + outer) * own + at, width)
            return oa.at[l, inner, :, cols]
        cols = pl.ds(at, width)
        return ob.at[l, outer, inner, :, cols] if last == "y" else ob.at[l, inner, outer, :, cols]

    def add(l, c, s):
        kind, first, then, last, at, width = PARTS[c]
        t = total[c].at[l]
        way = 1 - PAIR * (c % PAIR)
        key = (l, c)
        if s == 0:
            far = t.at[spot(first, PAIR)]
            for k, by in enumerate(BOTH):
                links.send((*key, "half", by), far.at[pl.ds(PAIR * k, PAIR)], half[c].at[l, k], peer(first, by))
        elif s == 1:
            for k, by in enumerate(BOTH):
                links.arrive((*key, "half", by), half[c].at[l, k])
                mine = t.at[spot(first, by)]
                add_into(mine.at[pl.ds(PAIR * k, PAIR)], half[c].at[l, k])
                links.send((*key, "full", by), mine, full[c].at[l, k], peer(first, by))
        elif s == PAIR:
            mine = t.at[spot(first, 0)]
            for k, by in enumerate(BOTH):
                links.arrive((*key, "full", by), full[c].at[l, k])
                add_into(mine, full[c].at[l, k])
            for k, o in enumerate(AROUND):
                links.send((*key, "small", o), mine.at[spot(then, o)], small[c].at[l, k], peer(then, o), (*key, "small", 1), small[c].at[l], (*key, "small"))
        elif s == 3:
            links.arrive((*key, "small", 1), small[c].at[l])
            mine = t.at[spot(first, 0), spot(then, 0)]
            front[c][l] = (mine[ALL] + small[c][l, 0]) + (small[c][l, 1] + small[c][l, PAIR])
        elif s == SIDE:
            src, dst = front[c].at[l], area(l, c, 0, 0)
            for by in BOTH:
                links.send((*key, "a1", by), src, dst, peer(then, by))
            copy = pltpu.make_async_copy(src, dst, osem.at[l, c])
            copy.start()
            loads["front", l, c] = copy
        elif s == 5:
            for by in BOTH:
                landed = area(l, c, 0, -by)
                links.arrive((*key, "a1", by), landed)
                if way == by:
                    links.send((*key, "b1"), landed, landed, peer(then, by))
        elif s == 6:
            loaded(("front", l, c))
            links.arrive((*key, "b1"), area(l, c, 0, PAIR))
            line = area(l, c, 0, slice(None))
            for by in BOTH:
                links.send((*key, "a2", by), line, line, peer(last, by))
        elif s == 7:
            for k, by in enumerate(BOTH):
                links.arrive((*key, "a2", by), area(l, c, -by, slice(None)))
                part = area(l, c, -by, pl.ds(PAIR * k, PAIR))
                links.send((*key, "a3", by), part, part, peer(last, by))
        else:
            for k, by in enumerate(BOTH):
                links.arrive((*key, "a3", by), area(l, c, PAIR, pl.ds(PAIR * k, PAIR)))

    stages = {"swap": swap, "pass": hand_on, "make": make, "sum": add}
    for kind, *task in order:
        stages[kind](*task)
    links.drain()


def add_into(dst, src):
    @pl.loop(0, dst.shape[0])
    def _(i):
        if len(dst.shape) == SIDE:
            for j in range(dst.shape[1]):
                dst[i, j] += src[i, j]
        else:
            dst[i] += src[i]


def around(position):
    place, core = dict(zip("xyz", position)), position[3]
    spots = {(axis, o): step(place[axis], o) for axis in "xyz" for o in range(SIDE)}
    peers = {}
    for axis in "xyz":
        for o in range(1, SIDE):
            moved = {**place, axis: spots[axis, o]}
            peers[axis, o] = device_at(moved["x"], moved["y"], moved["z"], core)
    return spots, peers


def reduce_gradients(operands, starts=(0.0, 0.0)):
    hbm = pl.BlockSpec(memory_space=pltpu.HBM)
    h_rows, m_rows, y_cols, z_cols, z_own, scale_parts = operands
    part, part_b = h_rows[0].shape[1] // SIDE, (m_rows[0].shape[0] + BAND) // 16
    (line, dim), wide = y_cols[0].shape, z_own.shape[1]
    out = lambda *shape: jax.ShapeDtypeStruct(shape, F32)
    sem = pltpu.SemaphoreType.DMA

    def buffers(*lead):
        return [pltpu.VMEM((PAIR, *lead, part if e[0] == "i" else part_b, e[5]), F32) for e in PARTS]

    return pl.pallas_call(
        functools.partial(reduce_kernel, reduce_order(part, part_b, starts)),
        out_shape=(out(PAIR, SIDE, part, wide), out(PAIR, SIDE, SIDE, part_b, dim)),
        in_specs=[hbm] * 12,
        out_specs=[hbm] * PAIR,
        scratch_shapes=[
            *buffers(SIDE, SIDE), *buffers(PAIR, PAIR), *buffers(PAIR, SIDE), *buffers(3), *buffers(),
            pltpu.VMEM((PAIR, PAIR, *h_rows[0].shape), BF), pltpu.VMEM((PAIR, PAIR, line, wide // ROW), BF), pltpu.VMEM((PAIR, *m_rows[0].shape), BF),
            pltpu.VMEM((PAIR, line, dim), BF), pltpu.VMEM(scale_parts.shape, F32),
            sem((WIDE,)), sem((WIDE,)), sem((16,)), sem((PAIR, len(PARTS))), sem((PAIR,)),
        ],
        compiler_params=pltpu.CompilerParams(collective_id=1, has_side_effects=True, vmem_limit_bytes=67043328),
        name="reduce_gradients",
    )(*h_rows, *m_rows, *y_cols, *z_cols, z_own, scale_parts)


def rotary_tables(seq_len, head_dim):
    half_dim = head_dim // PAIR
    inv_freq = 10000.0 ** (-(jnp.arange(half_dim, dtype=jnp.float32) * 2.0 / head_dim))
    angles = jnp.arange(seq_len, dtype=jnp.float32)[:, None] * inv_freq[None, :]
    return jnp.cos(angles), jnp.sin(angles)


def solution(mesh):
    fsdp_size = mesh.shape["fsdp"]
    batch_spec = P(("dp", "fsdp"), None, None)
    scale_spec = P(None, "fsdp")
    weight_spec = P(None, "fsdp", None)

    def device_step(x_in, grad_y, norm_scale, w_in, w_out):
        n_layers = w_in.shape[0]
        seq_len, model_dim = x_in.shape[1:]
        proj_dim = w_in.shape[PAIR]
        ff_dim = w_out.shape[1] * fsdp_size - model_dim
        head_dim = (proj_dim - model_dim - PAIR * ff_dim) // PAIR
        rows, rows_out = norm_scale.shape[1], w_out.shape[1]
        scale_rows = jnp.zeros((ROW, model_dim), jnp.float32)
        scale_rows = lax.dynamic_update_slice(scale_rows, norm_scale.astype(jnp.float32), (0, lax.axis_index("fsdp") * rows))
        cos_tab, sin_tab = rotary_tables(seq_len, head_dim)
        cos_tab, sin_tab = jnp.tile(cos_tab, (1, ROW)), jnp.tile(sin_tab, (1, ROW))
        lane = jnp.arange(WIDE)
        down = lane[:, None] - lane[None, :]
        low = lane[None, :] % head_dim < head_dim // PAIR
        turn = jnp.where(low & (down == BAND), -1.0, jnp.where(~low & (down == -BAND), 1.0, 0.0)).astype(jnp.bfloat16)
        hidden, grad_hidden, *rest = run_layers(x_in[0], grad_y[0], scale_rows, w_in, w_out, cos_tab, sin_tab, turn)
        in_sums, out_sums = reduce_gradients((rest[0:SIDE], rest[SIDE:6], rest[6:ROW], rest[ROW:10], rest[10], rest[11]))
        in_grads = in_sums.reshape(n_layers, rows, -1)[:, :, :proj_dim]
        out_rows = out_sums.reshape(n_layers, -1, model_dim)
        scale_grads = lax.dynamic_slice(out_rows[:, rows_out], (0, lax.axis_index("fsdp") * rows), (n_layers, rows))
        out_grads = out_rows[:, :rows_out]
        return hidden[None], grad_hidden[None], scale_grads, in_grads, out_grads

    return jax.shard_map(
        device_step,
        mesh=mesh,
        in_specs=(batch_spec, batch_spec, scale_spec, weight_spec, weight_spec),
        out_specs=(batch_spec, batch_spec, scale_spec, weight_spec, weight_spec),
        check_vma=False,
    )
```

```python
import functools
import jax
import jax.numpy as jnp
from jax import lax
from jax.experimental import pallas as pl
from jax.experimental.pallas import tpu as pltpu
from jax.sharding import PartitionSpec as P

MESH_ID = pl.DeviceIdType.MESH
BOTH = (1, -1)
AROUND = (1, -1, 2)
PARTS = (True, False)
ALL, ZERO = ..., 0.0
LANE, WIDE, STRIP, HEAD = 128, 256, 512, 64
ROW, BAND, SIDE, PAIR = 8, 32, 4, 2


class Links:
    def __init__(self, send_sems, recv_sems):
        self.send_sems, self.recv_sems = send_sems, recv_sems
        self.slots, self.batches, self.sent = {}, {}, {}

    def send(self, key, src, dst, device, landing=None, whole=None, batch=None, lane=None):
        slot = self.slots.setdefault(landing or key, len(self.slots))
        leaving = self.batches.setdefault(batch or key, len(self.batches))
        copy = pltpu.make_async_remote_copy(
            src_ref=src, dst_ref=dst, send_sem=self.send_sems.at[leaving], recv_sem=self._landing(slot, lane),
            device_id=device, device_id_type=MESH_ID)
        copy.start()
        self.sent[batch or key] = (whole or src, leaving)

    def _landing(self, slot, lane):
        return self.recv_sems.at[slot] if lane is None else self.recv_sems.at[slot, lane]

    def arrive(self, key, landed, lane=None):
        slot = self.slots.setdefault(key, len(self.slots))
        pltpu.make_async_copy(landed, landed, self._landing(slot, lane)).wait()

    def drain(self):
        for left, leaving in self.sent.values():
            pltpu.make_async_copy(left, left, self.send_sems.at[leaving]).wait()
        self.sent.clear()


def rem(a, n):
    return a % n if isinstance(a, int) else lax.rem(a, n)


def chip_position():
    f, d = lax.axis_index("fsdp"), lax.axis_index("dp")
    return f // PAIR, rem(d, SIDE), d // SIDE, rem(f, PAIR)


def device_at(x, y, z, core):
    return (z * SIDE + y, x * PAIR + core)


def step(coord, by):
    return rem(coord + SIDE + by, SIDE)


def announce(devices):
    barrier = pltpu.get_barrier_semaphore()
    for device in devices:
        pl.semaphore_signal(barrier, inc=1, device_id=device, device_id_type=MESH_ID)
    pl.semaphore_wait(barrier, len(devices))


def plan(tasks, latency=2.5):
    free, landed, order, now = {}, {}, [], ZERO
    left = list(tasks)
    while left:
        best = None
        for place, (name, rank, start, needs, after, _, _) in enumerate(left):
            if all(n[0] in landed for n in needs) and all(n in landed for n in after):
                ready = max([start, now] + [landed[task][i] for task, i in needs])
                best = min(best or (ready, rank, place), (ready, rank, place))
        now, _, place = best
        name, _, _, _, _, sends, cost = left.pop(place)
        order.append(name)
        now += cost
        landed[name] = []
        for link, time in sends:
            free[link] = max(now, free.get(link, ZERO)) + time
            landed[name].append(free[link] + latency)
    return order


def layers_order(rows_i, cols_i, rows_o, cols_o, seq, starts):
    rate = 23300.0
    tasks = []
    for m in range(SIDE):
        is_in = m % PAIR == 0
        edge = cols_i // LANE * SIDE // 9 // PAIR * WIDE
        size = {"y": rows_i // SIDE * edge, "x": rows_i * (cols_i - PAIR * edge)} if is_in else {"y": rows_o // SIDE * cols_o // PAIR}
        size["z"] = size["y"]
        for color in "yzx" if is_in else "yz":
            cost = size[color] / rate
            both = [(("x", by), cost) for by in BOTH]
            spread = [((color, by), cost) for by in BOTH] if color != "x" else []
            tasks.append((("reach", m, color), m, starts[m], [], [], both, 0.2))
            for i, by in enumerate(BOTH):
                tasks.append((("relay", m, color, by), m, ZERO, [(("reach", m, color), i)], [], [(("x", by), cost / PAIR)] + spread, 0.2))
            halves = [(("relay", m, color, by), 0) for by in BOTH]
            tasks.append((("far", m, color), m, ZERO, halves, [], spread, 0.2))
            if color == "x":
                continue
            for off, source, first in ((-1, ("relay", m, color, 1), 1), (1, ("relay", m, color, -1), 1), (PAIR, ("far", m, color), 0)):
                for i, by in enumerate(BOTH):
                    tasks.append((("pass", m, color, off, by), m, ZERO, [(source, first + i)], [], [((color, by), cost / PAIR)], 0.2))
                halves = [(("pass", m, color, off, by), 0) for by in BOTH]
                tasks.append((("close", m, color, off), m, ZERO, halves, [], [], 0.2))
        for off in (-1, 1, PAIR):
            last = [("close", m, color, off) for color in "yz"]
            if is_in:
                last.append(("far", m, "x") if off == PAIR else ("relay", m, "x", -off))
            tasks.append((("hand", m, off), m, ZERO, [], last, [("chip", (rows_i * cols_i if is_in else rows_o * cols_o) / 150000.0)], 0.2))
    before = []

    def work(name, cost, mats=()):
        needs = [(("hand", m, off), 0) for m in mats for off in (-1, 1, PAIR)]
        tasks.append((name, 99, ZERO, needs, list(before), [], cost))
        before[:] = [name]

    for l in range(PAIR):
        work(("norm", l), 0.8)
        for i in range(SIDE):
            work(("project", l, i), 1.4, [PAIR * l])
        work(("attend", l), 4.0)
        work(("mlp", l), 2.2)
        work(("put", l), 2.0, [PAIR * l + 1])
    for l in (1, 0):
        work(("back_out", l), 4.0)
        work(("back_mlp", l), 3.5)
        work(("back_heads", l), 1.2)
        for g in range(3):
            work(("back_quad", l, g), 2.3)
        work(("back_keys", l), 0.5)
        for i in range(5):
            work(("back_in", l, i), 1.0)
        work(("back_norm", l), 1.2)
    def send(name, rank, start, after, sends):
        tasks.append((name, rank, start, [], [after] if after else [], sends, 0.4))

    def follow(name, rank, needs, sends):
        tasks.append((name, rank, ZERO, needs, [], sends, 0.2))

    def both(axis, size):
        return [((axis, by), size / rate) for by in BOTH]

    model = rows_i * ROW
    for l in (1, 0):
        for axis in "yz":
            name = ("send_h", l, axis)
            send(name, 20 - l, 58.0, ("norm", l), both(axis, seq * model))
            for i, by in enumerate(BOTH):
                for index in range(PAIR):
                    follow(("pass_h", l, axis, by, index), 10, [(name, i)], [((axis, by), seq * model / SIDE / rate)])
        name = ("send_m", l)
        send(name, 22 - l, ZERO, ("mlp", l), both("x", seq * rows_o) + both("x", PAIR * seq * rows_o))
        for i, by in enumerate(BOTH):
            for index in range(PAIR):
                follow(("pass_m", l, by, index), 11, [(name, i)], [(("x", by), seq * rows_o / PAIR / rate)])
        name = ("send_y", l)
        send(name, 12, 42.0, ("back_norm", 1) if l == 0 else None, both("x", seq * model))
        for i, by in enumerate(BOTH):
            follow(("pass_y", l, by), 12, [(name, i)], [(("x", by), seq * model / PAIR / rate)])
        follow(("far_y", l), 12, [(("pass_y", l, by), 0) for by in BOTH], [])
        for axis in "zy" if l else "z":
            name = ("send_z", l, axis)
            share = seq * (cols_i + LANE) / ROW
            send(name, 13, ZERO, ("back_mlp", l) if axis == "z" else ("back_keys", l), both(axis, share / PAIR) + both(axis, share))
            for i, by in enumerate(BOTH):
                follow(("pass_z", l, axis, by), 13, [(name, i)], [((axis, by), share / PAIR / rate)])
                follow(("twin_z", l, axis, by), 14, [(name, PAIR + i)], [])
            follow(("far_z", l, axis), 14, [(("pass_z", l, axis, by), 0) for by in BOTH], [])
        send(("send_scale", l), 15, ZERO, ("back_norm", l), [])
    send(("own_z",), 15, ZERO, ("back_keys", 0), [])
    return plan(tasks)


def gather_stages(links, position, shard_i, shard_o, wi, wo, lsem):
    x, y, z, core = position
    twin = device_at(x, y, z, 1 - core)
    rows_i, cols_i = shard_i.shape[1:]
    rows_o, cols_o = shard_o.shape[1:]
    quarter_i, quarter_o = rows_i // SIDE, rows_o // SIDE
    third_i = cols_i // LANE * SIDE // 9 // PAIR * WIDE
    half_o = cols_o // PAIR
    cut_o = quarter_o // 16 * ROW + ROW if quarter_o % 16 else quarter_o // PAIR
    place = {"x": x, "y": y, "z": z}

    spots = {(axis, o): step(place[axis], o) for axis in "xyz" for o in range(SIDE)}

    def spot(axis, o):
        return spots[axis, o % SIDE]

    table = {}
    for axis in "xyz":
        for o in range(1, SIDE):
            moved = {**place, axis: spot(axis, o)}
            table[axis, o] = device_at(moved["x"], moved["y"], moved["z"], core)

    def peer(axis, o):
        return table[axis, o % SIDE]

    mats = []
    for l in range(PAIR):
        mats.append((shard_i.at[l], wi.at[l], rows_i, True))
        mats.append((shard_o.at[l], wo.at[l], rows_o, False))

    def region(is_in, color, q):
        if is_in:
            if color == "x":
                lo, hi = PAIR * third_i, cols_i
                rows = (0, rows_i)
            else:
                lo, hi = (0, third_i) if color == "y" else (third_i, PAIR * third_i)
                rows = (q * quarter_i, quarter_i)
            mid = lo + ((hi - lo) // LANE + 1) // PAIR * LANE
            return (rows, (lo, hi - lo)), (rows, (lo, mid - lo)), (rows, (mid, hi - mid))
        cols = (0, half_o) if color == "y" else (half_o, half_o)
        start = q * quarter_o
        return ((start, quarter_o), cols), ((start, cut_o), cols), ((start + cut_o, quarter_o - cut_o), cols)

    def at(m, xb, area):
        (r, nr), (c, nc) = area
        _, out, size, _ = mats[m]
        return out.at[pl.ds(pl.multiple_of((PAIR * xb + core) * size + r, ROW), nr), pl.ds(c, nc)]

    def block(m, xb, index):
        _, out, size, _ = mats[m]
        return out.at[pl.ds(pl.multiple_of((PAIR * xb + index) * size, BAND), size)]

    def colors(m):
        return "yzx" if mats[m][3] else "yz"

    def reach(m, color):
        src, _, _, is_in = mats[m]
        area = region(is_in, color, place[color])[0]
        for by in BOTH:
            links.send((m, "x1", color, by), src.at[pl.ds(pl.multiple_of(area[0][0], ROW), area[0][1]), pl.ds(*area[1])], at(m, x, area), peer("x", by))

    def launch(m, color, off):
        is_in = mats[m][3]
        moved = at(m, spot("x", off), region(is_in, color, place[color])[0])
        for by in BOTH:
            links.send((m, "p1", color, off, by), moved, moved, peer(color, by))

    def relay(m, color, by):
        is_in = mats[m][3]
        xb = spot("x", -by)
        areas = region(is_in, color, place[color])
        links.arrive((m, "x1", color, by), at(m, xb, areas[0]))
        part = at(m, xb, areas[1] if by == 1 else areas[PAIR])
        links.send((m, "x2", color, by), part, part, peer("x", by))
        if color != "x":
            launch(m, color, -by)

    def far(m, color):
        is_in = mats[m][3]
        areas = region(is_in, color, place[color])
        for by in BOTH:
            links.arrive((m, "x2", color, by), at(m, spot("x", PAIR), areas[1] if by == 1 else areas[PAIR]))
        if color != "x":
            launch(m, color, PAIR)

    def pass_on(m, color, off, by):
        is_in = mats[m][3]
        xb = spot("x", off)
        areas = region(is_in, color, spot(color, -by))
        links.arrive((m, "p1", color, off, by), at(m, xb, areas[0]))
        part = at(m, xb, areas[1] if by == 1 else areas[PAIR])
        links.send((m, "p2", color, off, by), part, part, peer(color, by))

    def close(m, color, off):
        is_in = mats[m][3]
        areas = region(is_in, color, spot(color, PAIR))
        for by in BOTH:
            links.arrive((m, "p2", color, off, by), at(m, spot("x", off), areas[1] if by == 1 else areas[PAIR]))

    def hand(m, off):
        whole = block(m, spot("x", off), core)
        links.send((m, "d2d", off), whole, whole, twin)

    owns = []

    def begin():
        for m, (src, _, _, _) in enumerate(mats):
            copy = pltpu.make_async_copy(src, block(m, x, core), lsem.at[m])
            copy.start()
            owns.append(copy)
            links.send((m, "d2d", 0), src, block(m, x, core), twin)

    def ready(m):
        owns[m].wait()
        for off in (0, -1, 1, PAIR):
            links.arrive((m, "d2d", off), block(m, spot("x", off), 1 - core))

    return begin, ready, peer, {"reach": reach, "relay": relay, "far": far, "pass": pass_on, "close": close, "hand": hand}


BF, F32 = jnp.bfloat16, jnp.float32


def product(a, b, contract=((1,), (0,))):
    return lax.dot_general(a, b, (contract, ((), ())), preferred_element_type=F32)


def lanes(start, size):
    return pl.ds(start if isinstance(start, int) else pl.multiple_of(start, LANE), size)


def layers_kernel(order, sc_ref, wi_ref, wo_ref, x_ref, dy_ref, cos_ref, sin_ref, turn_ref,
                  y_ref, gx_ref, hy_a, hy_b, hz_a, hz_b, mx_a, mx_b, yx_a, yx_b, zy_b, zz_b, zz_a, z_a, sc_out, relay_m, relay_z,
                  wi, wo, z, om, h, hid, qr, kts, vts, ksl, scores, dscores, pcat, dscat,
                  dot_heads, qt, dht, dkv, omt, ht, dyt, sc, gains, gain_ref, load_sems, own_sems, send_sems, recv_sems,
                  share_send_sems, share_recv_sems):
    seq, dim = x_ref.shape
    ff = (wi.shape[PAIR] - dim - LANE) // PAIR
    position = chip_position()
    x, y, zc, core = position
    twin = device_at(x, y, zc, 1 - core)
    me = PAIR * x + core
    links, shared = Links(send_sems, recv_sems), Links(share_send_sems, share_recv_sems)
    stored = []
    spots, _ = around(position)
    h_out, m_out, y_out, z_out = {"y": (hy_a, hy_b), "z": (hz_a, hz_b)}, (mx_a, mx_b), (yx_a, yx_b), {(1, "y"): zy_b, (1, "z"): zz_b, (0, "z"): zz_a}
    middle = hid.at[1]
    begin, ready, peer, stages = gather_stages(links, position, wi_ref, wo_ref, wi, wo, load_sems)
    others = [(zc * SIDE + y, rem(me + k, ROW)) for k in range(1, ROW)]

    def spot(axis, o):
        return spots[axis, o % SIDE]

    def device(axis, o, index):
        moved = {"x": x, "y": y, "z": zc, axis: spot(axis, o)}
        return device_at(moved["x"], moved["y"], moved["z"], index)

    announce(others + [device(axis, o, index) for axis in "yz" for o in AROUND for index in range(PAIR)])
    begin()
    for k, far in enumerate(others):
        links.send(("sc", k), sc_ref, gains.at[me], far)

    def keep(src, dst):
        copy = pltpu.make_async_copy(src, dst, own_sems.at[len(stored)])
        copy.start()
        stored.append(copy)

    def tokens(axis, o, index):
        return pl.ds(pl.multiple_of((PAIR * spot(axis, o) + index) * seq, seq), seq)

    def columns(axis, o):
        size = z.shape[PAIR] // ROW
        return lanes(((0 if axis == "y" else SIDE) + spot(axis, o)) * size, size)

    def send_h(l, axis):
        out = h_out[axis][l].at[:, :, tokens(axis, 0, core)]
        for by in BOTH:
            for index in range(PAIR):
                shared.send(("h", l, axis, by), ht.at[l, :, index], out, device(axis, by, index), batch=("h", l, axis, by, index), lane=core)
        shared.send(("h", l, axis), ht.at[l, :, 1 - core], out, twin, lane=0)
        keep(ht.at[l, :, core], out)

    def pass_h(l, axis, by, index):
        out = h_out[axis][l]
        shared.arrive(("h", l, axis, by), out.at[:, :, tokens(axis, -by, index)], index)
        part = out.at[pl.ds(1 - by, PAIR), :, tokens(axis, -by, index)]
        shared.send(("h2", l, axis, by), part, part, device(axis, by, core), batch=("h2", l, axis, by, index), lane=index)

    def arrive_h(l):
        for axis in "yz":
            for by in BOTH:
                for index in range(PAIR):
                    shared.arrive(("h2", l, axis, by), h_out[axis][l].at[pl.ds(1 - by, PAIR), :, tokens(axis, PAIR, index)], index)
            shared.arrive(("h", l, axis), h_out[axis][l].at[:, :, tokens(axis, 0, 1 - core)], 0)

    def row_block(l, o, index, part=None):
        size = omt.shape[1] // ROW
        start = (PAIR * spot("x", o) + index) * size
        if part is not None:
            size = size // PAIR
            start = start + part * size
        return omt.at[l, pl.ds(pl.multiple_of(start, 16), size)]

    def row_half(k):
        size = m_out[0].shape[0] // PAIR
        return pl.ds(k * size, size)

    def send_m(l):
        out = m_out[l].at[:, tokens("x", 0, core)]
        for k, by in enumerate(BOTH):
            for index in range(PAIR):
                shared.send(("mr", l, by), row_block(l, PAIR, index, k), relay_m.at[l, k, core], device("x", by, index), batch=("mr", l, by, index), lane=core)
        for by in BOTH:
            for index in range(PAIR):
                shared.send(("m", l, by), row_block(l, by, index), out, device("x", by, index), batch=("m", l, by, index), lane=core)
        shared.send(("m", l), row_block(l, 0, 1 - core), out, twin, lane=0)
        keep(row_block(l, 0, core), out)

    def pass_m(l, by, index):
        k = (1 - by) // PAIR
        shared.arrive(("mr", l, by), relay_m.at[l, k, index], index)
        shared.send(("m2", l, by), relay_m.at[l, k, index], m_out[l].at[row_half(k), tokens("x", -by, index)], device("x", by, core),
                    batch=("m2", l, by, index), lane=index)

    def arrive_m(l):
        for k, by in enumerate(BOTH):
            for index in range(PAIR):
                shared.arrive(("m", l, by), m_out[l].at[:, tokens("x", -by, index)], index)
                shared.arrive(("m2", l, by), m_out[l].at[row_half(k), tokens("x", PAIR, index)], index)
        shared.arrive(("m", l), m_out[l].at[:, tokens("x", 0, 1 - core)], 0)

    def token_half(axis, o, k):
        return pl.ds(pl.multiple_of((PAIR * spot(axis, o) + core) * seq + k * (seq // PAIR), seq // PAIR), seq // PAIR)

    def send_y(l):
        src, out = (middle, dy_ref)[l], y_out[l].at[tokens("x", 0, core)]
        for by in BOTH:
            shared.send(("y", l, by), src, out, device("x", by, core), lane=0)
        shared.send(("y", l), src, out, twin, lane=0)
        keep(src, out)

    def pass_y(l, by):
        landed, part = y_out[l].at[tokens("x", -by, core)], y_out[l].at[token_half("x", -by, (1 - by) // PAIR)]
        shared.arrive(("y", l, by), landed, 0)
        shared.send(("y2", l, by), part, part, device("x", by, core), lane=0)
        shared.send(("yp", l, by), landed, landed, twin, lane=0)

    def far_y(l):
        for k, by in enumerate(BOTH):
            shared.arrive(("y2", l, by), y_out[l].at[token_half("x", PAIR, k)], 0)
        landed = y_out[l].at[tokens("x", PAIR, core)]
        shared.send(("yp", l, PAIR), landed, landed, twin, lane=0)

    def arrive_y(l):
        for o in AROUND:
            shared.arrive(("yp", l, o), y_out[l].at[tokens("x", -o, 1 - core)], 0)
        shared.arrive(("y", l), y_out[l].at[tokens("x", 0, 1 - core)], 0)

    def send_z(l, axis):
        out = z_out[l, axis].at[tokens(axis, 0, core)]
        for k, by in enumerate(BOTH):
            shared.send(("zr", l, axis, by), z.at[l, pl.ds(k * (seq // PAIR), seq // PAIR), columns(axis, PAIR)], relay_z.at[l, "yz".index(axis), k],
                        device(axis, by, core), lane=0)
        for by in BOTH:
            shared.send(("z", l, axis, by), z.at[l, :, columns(axis, by)], out, device(axis, by, core), lane=0)
        shared.send(("z", l, axis), z.at[l, :, columns(axis, 0)], out, twin, lane=0)
        keep(z.at[l, :, columns(axis, 0)], out)

    def pass_z(l, axis, by):
        k = (1 - by) // PAIR
        half = relay_z.at[l, "yz".index(axis), k]
        shared.arrive(("zr", l, axis, by), half, 0)
        shared.send(("z2", l, axis, by), half, z_out[l, axis].at[token_half(axis, -by, k)], device(axis, by, core), lane=0)

    def twin_z(l, axis, by):
        landed = z_out[l, axis].at[tokens(axis, -by, core)]
        shared.arrive(("z", l, axis, by), landed, 0)
        shared.send(("zp", l, axis, by), landed, landed, twin, lane=0)

    def far_z(l, axis):
        for k, by in enumerate(BOTH):
            shared.arrive(("z2", l, axis, by), z_out[l, axis].at[token_half(axis, PAIR, k)], 0)
        landed = z_out[l, axis].at[tokens(axis, PAIR, core)]
        shared.send(("zp", l, axis, PAIR), landed, landed, twin, lane=0)

    def arrive_z(l, axis):
        for o in AROUND:
            shared.arrive(("zp", l, axis, o), z_out[l, axis].at[tokens(axis, -o, 1 - core)], 0)
        shared.arrive(("z", l, axis), z_out[l, axis].at[tokens(axis, 0, 1 - core)], 0)

    def send_scale(l):
        for k, far in enumerate(others):
            shared.send(("scale", l, k), sc.at[l], sc_out.at[l, me], far, lane=0)
        keep(sc.at[l], sc_out.at[l, me])

    def arrive_scale(l):
        for k in range(len(others)):
            shared.arrive(("scale", l, k), sc_out.at[l, rem(me + 7 - k, ROW)], 0)

    gains[me] = sc_ref[ALL]
    z[:, :, wi.shape[PAIR]:] = jnp.zeros((PAIR, seq, z.shape[PAIR] - wi.shape[PAIR]), BF)
    entry = (x_ref, hid.at[0])
    kts[ALL] = jnp.zeros(kts.shape, BF)
    vts[ALL] = jnp.zeros(vts.shape, BF)

    def normalise(l, src):
        @pl.loop(0, seq // BAND)
        def _(r):
            rows = pl.ds(pl.multiple_of(r * BAND, BAND), BAND)
            v = src[rows].astype(F32)
            v = v - jnp.mean(v, axis=-1, keepdims=True)
            var = jnp.mean(v * v, axis=-1, keepdims=True)
            h[l, rows] = (v * lax.rsqrt(var + 1e-6) * gain_ref[l:l + 1]).astype(BF)

    def project(l, quarter):
        def part(at, size):
            z[l, :, lanes(at, size)] = product(h[l], wi[l, :, lanes(at, size)]).astype(BF)

        n = wi.shape[PAIR] // STRIP

        @pl.loop(quarter * n // SIDE, (quarter + 1) * n // SIDE)
        def _(i):
            part(i * STRIP, STRIP)
        if quarter == 3:
            part(n * STRIP, wi.shape[PAIR] - n * STRIP)

    def heads(l):
        cos, sin = cos_ref[ALL], sin_ref[ALL]
        for g in range(dim // WIDE):
            q = z[l, :, g * WIDE:(g + 1) * WIDE]
            qr[l, :, g * WIDE:(g + 1) * WIDE] = ((q.astype(F32) * cos + product(q, turn_ref[ALL]) * sin) * 0.125).astype(BF)
        kv = z[l, :, dim:dim + LANE]
        turned = kv.astype(F32) * cos[:, :LANE] + product(kv, turn_ref[:LANE, :LANE]) * sin[:, :LANE]
        first = lax.broadcasted_iota(jnp.int32, turned.shape, 1) < HEAD
        key_lo = jnp.where(first, turned, ZERO)
        val_hi = jnp.where(first, ZERO, kv.astype(F32))
        return key_lo, pltpu.roll(key_lo, HEAD, 1), pltpu.roll(val_hi, HEAD, 1), val_hi

    def slot_rows(ref, lo, hi):
        zero = jnp.zeros((seq, LANE), BF)
        lo, hi = lo.astype(BF), hi.astype(BF)
        for i, (left, right) in enumerate(((lo, zero), (hi, zero), (zero, lo), (zero, hi))):
            ref[i * seq:(i + 1) * seq, :LANE] = left
            ref[i * seq:(i + 1) * seq, LANE:] = right

    def slot_cols(ref, lo):
        flat = lo.T[:HEAD].astype(BF)
        for i in range(SIDE):
            ref[HEAD * i:HEAD * (i + 1), i * seq:(i + 1) * seq] = flat

    def chances(rows, r, i):
        s = scores[rows, i * seq:(i + 1) * seq]
        at = lax.broadcasted_iota(jnp.int32, s.shape, 0) + r * BAND
        s = jnp.where(at >= lax.broadcasted_iota(jnp.int32, s.shape, 1), s, -1e30)
        e = jnp.exp(s - jnp.max(s, axis=-1, keepdims=True))
        return e * (1.0 / jnp.sum(e, axis=-1, keepdims=True))

    def attend(l):
        key_lo, _, val_lo, val_hi = heads(l)
        slot_cols(kts, key_lo)
        slot_rows(ksl, val_lo, val_hi)

        @pl.loop(0, dim // WIDE)
        def _(g):
            cols = lanes(g * WIDE, WIDE)
            scores[ALL] = product(qr[l, :, cols], kts[ALL])

            @pl.loop(0, seq // BAND)
            def _(r):
                rows = pl.ds(pl.multiple_of(r * BAND, BAND), BAND)
                for i in range(SIDE):
                    pcat[rows, i * seq:(i + 1) * seq] = chances(rows, r, i).astype(BF)
            om[:, cols] = product(pcat[ALL], ksl[ALL]).astype(BF)

    def mlp(l):
        @pl.loop(0, seq // BAND)
        def _(r):
            rows = pl.ds(pl.multiple_of(r * BAND, BAND), BAND)

            @pl.loop(0, ff // STRIP)
            def _(i):
                gate = z[l, rows, lanes(dim + LANE + i * STRIP, STRIP)].astype(F32)
                up = z[l, rows, lanes(dim + LANE + ff + i * STRIP, STRIP)].astype(F32)
                om[rows, lanes(dim + i * STRIP, STRIP)] = (gate * jax.nn.sigmoid(gate) * up).astype(BF)

    def put_out(l, dst):
        for n in range(dim // WIDE):
            cols = slice(n * WIDE, (n + 1) * WIDE)
            total = product(om[ALL], wo[l, :, cols])
            dst[:, cols] = (entry[l][:, cols].astype(F32) + total).astype(BF)

    def flip(src, dst, width):
        @pl.loop(0, width // WIDE)
        def _(i):
            dst[pl.ds(pl.multiple_of(i * WIDE, WIDE), WIDE)] = src(i * WIDE).T

    upstream = (middle, dy_ref)

    def back_out(l):
        dy = upstream[l]
        flip(lambda at: dy[:, lanes(at, WIDE)], dyt, dim)

        @pl.loop(0, wo.shape[1] // dim)
        def _(n):
            rows = pl.ds(pl.multiple_of(n * dim, dim), dim)
            part = product(wo[l, rows], dyt[ALL]).astype(BF)
            om[:, lanes(n * dim, dim)] = part.T

            @pl.when(n == 0)
            def _():
                dot_heads[ALL] = part

    def back_mlp(l):
        @pl.loop(0, seq // BAND)
        def _(r):
            rows = pl.ds(pl.multiple_of(r * BAND, BAND), BAND)

            @pl.loop(0, ff // STRIP)
            def _(i):
                gate_at, up_at = lanes(dim + LANE + i * STRIP, STRIP), lanes(dim + LANE + ff + i * STRIP, STRIP)
                gate, up = z[l, rows, gate_at].astype(F32), z[l, rows, up_at].astype(F32)
                d = om[rows, lanes(dim + i * STRIP, STRIP)].astype(F32)
                sig = jax.nn.sigmoid(gate)
                du = d * up
                z[l, rows, gate_at] = (du * sig + du * gate * (sig * (1.0 - sig))).astype(BF)
                z[l, rows, up_at] = (d * (gate * sig)).astype(BF)

    def back_heads(l):
        key_lo, key_hi, val_lo, val_hi = heads(l)
        slot_cols(kts, key_lo)
        slot_cols(vts, val_lo)
        slot_rows(ksl, key_lo, key_hi)
        dkv[ALL] = jnp.zeros(dkv.shape, F32)
        flip(lambda at: qr[l, :, lanes(at, WIDE)], qt, dim)


    def back_quad(l, g):
        cols = pl.ds(g * WIDE, WIDE)
        scores[ALL] = product(qr[l, :, cols], kts[ALL])
        dscores[ALL] = product(om[:, cols], vts[ALL])

        @pl.loop(0, seq // BAND)
        def _(r):
            rows = pl.ds(pl.multiple_of(r * BAND, BAND), BAND)
            for i in range(SIDE):
                at = slice(i * seq, (i + 1) * seq)
                p = chances(rows, r, i)
                pcat[rows, at] = p.astype(BF)
                pd = p * dscores[rows, at].astype(BF).astype(F32)
                dscat[rows, at] = (pd - p * jnp.sum(pd, axis=-1, keepdims=True)).astype(BF)
        dq = product(dscat[ALL], ksl[ALL]).astype(BF)
        back = dq.astype(F32) * cos_ref[ALL] - product(dq, turn_ref[ALL]) * sin_ref[ALL]
        z[l, :, cols] = (back * 0.125).astype(BF)
        for i in range(SIDE):
            head = pl.ds(g * WIDE + i * HEAD, HEAD)
            at = slice(i * seq, (i + 1) * seq)
            dkv[:HEAD] += product(qt[head], dscat[:, at])
            dkv[HEAD:] += product(dot_heads[head], pcat[:, at])

    def back_keys(l):
        dkv_t = dkv[ALL].T
        dk = dkv_t.astype(BF)
        turned = dk.astype(F32) * cos_ref[:, :LANE] - product(dk, turn_ref[:LANE, :LANE]) * sin_ref[:, :LANE]
        first = lax.broadcasted_iota(jnp.int32, turned.shape, 1) < HEAD
        z[l, :, dim:dim + LANE] = jnp.where(first, turned, dkv_t).astype(BF)

    def back_in(l, i):
        width = wi.shape[PAIR] // 5
        at = slice(i * width, (i + 1) * width)
        part = product(wi[l, :, at], z[l, :, at], ((1,), (1,)))
        dht[ALL] = part if i == 0 else dht[ALL] + part

    def back_norm(l):
        dy, dst = upstream[l], (gx_ref, middle)[l]
        for i in range(dim // WIDE):
            cols = slice(i * WIDE, (i + 1) * WIDE)
            h[l, :, cols] = dht[cols].T.astype(BF)
        sc[l] = jnp.zeros(sc.shape[1:], F32)

        @pl.loop(0, seq // BAND)
        def _(r):
            rows = pl.ds(pl.multiple_of(r * BAND, BAND), BAND)
            v = entry[l][rows].astype(F32)
            v = v - jnp.mean(v, axis=-1, keepdims=True)
            scale = lax.rsqrt(jnp.mean(v * v, axis=-1, keepdims=True) + 1e-6)
            hat = v * scale
            d = h[l, rows].astype(F32)
            each = (d * hat).reshape(SIDE, ROW, dim)
            sc[l] += (each[0] + each[1]) + (each[PAIR] + each[3])
            d = d * gain_ref[l:l + 1]
            d = scale * (d - jnp.mean(d, axis=-1, keepdims=True) - hat * jnp.mean(d * hat, axis=-1, keepdims=True))
            dst[rows] = (dy[rows].astype(F32) + d.astype(BF).astype(F32)).astype(BF)

    def do_norm(l):
        if l == 0:
            for k, (_, f) in enumerate(others):
                links.arrive(("sc", k), gains.at[rem(me + 7 - k, ROW)])
            gain_ref[ALL] = jnp.sum(gains[ALL], axis=0)
        normalise(l, entry[l])
        for i in range(dim // WIDE):
            flat = h[l, :, i * WIDE:(i + 1) * WIDE].T
            size = ht.shape[3]
            for b in range(ROW):
                lo, hi = max(b * size, i * WIDE), min((b + 1) * size, (i + 1) * WIDE)
                if lo < hi:
                    ht[l, b // PAIR, b % PAIR, lo - b * size:hi - b * size] = flat[lo - i * WIDE:hi - i * WIDE]

    def do_project(l, i):
        if i == 0:
            ready(PAIR * l)
        project(l, i)

    def do_mlp(l):
        mlp(l)
        flip(lambda at: om[:, lanes(at, WIDE)], omt.at[l], om.shape[1])

    def do_put(l):
        ready(PAIR * l + 1)
        put_out(l, hid.at[0] if l == 0 else y_ref)

    stages.update(
        norm=do_norm, project=do_project, attend=attend, mlp=do_mlp, put=do_put, back_out=back_out, back_mlp=back_mlp, back_heads=back_heads,
        back_quad=back_quad, back_keys=back_keys, back_in=back_in, back_norm=back_norm, send_h=send_h, pass_h=pass_h, send_m=send_m,
        pass_m=pass_m, send_y=send_y, pass_y=pass_y, far_y=far_y, send_z=send_z, pass_z=pass_z, twin_z=twin_z, far_z=far_z,
        send_scale=send_scale, own_z=lambda: keep(z.at[0], z_a))
    for kind, *task in order:
        stages[kind](*task)
    for l in range(PAIR):
        arrive_h(l)
        arrive_m(l)
        arrive_scale(l)
        arrive_y(l)
    for l, axis in z_out:
        arrive_z(l, axis)
    for copy in stored:
        copy.wait()
    shared.drain()
    links.drain()


def run_layers(x, dy, scale, w_in, w_out, cos, sin, turn, starts=(ZERO, 10.0, 20.0, 30.0)):
    seq, dim = x.shape
    proj, cat = w_in.shape[PAIR], ROW * w_out.shape[1]
    wide = proj + LANE
    hbm, vmem = pl.BlockSpec(memory_space=pltpu.HBM), pl.BlockSpec(memory_space=pltpu.VMEM)
    out = lambda *shape, dtype=BF: jax.ShapeDtypeStruct(shape, dtype)
    buffer = lambda *shape, dtype=BF: pltpu.VMEM(shape, dtype)
    sem = pltpu.SemaphoreType.DMA
    line = ROW * seq
    return pl.pallas_call(
        functools.partial(layers_kernel, layers_order(*w_in.shape[1:], *w_out.shape[1:], seq, starts)),
        out_shape=(out(seq, dim), out(seq, dim), *[out(SIDE, dim // ROW, line)] * SIDE, *[out(cat // ROW, line)] * PAIR, *[out(line, dim)] * PAIR,
                   *[out(line, wide // ROW)] * 3, out(seq, wide), out(PAIR, ROW, ROW, dim, dtype=F32),
                   out(PAIR, PAIR, PAIR, cat // 16, seq), out(PAIR, PAIR, PAIR, seq // PAIR, wide // ROW)),
        in_specs=[vmem, hbm, hbm] + [vmem] * 5,
        out_specs=[vmem] * PAIR + [hbm] * 15,
        scratch_shapes=[
            buffer(PAIR, dim, proj), buffer(PAIR, cat, dim), buffer(PAIR, seq, wide), buffer(seq, cat), buffer(PAIR, seq, dim),
            buffer(PAIR, seq, dim), buffer(PAIR, seq, dim),
            buffer(WIDE, SIDE * seq), buffer(WIDE, SIDE * seq), buffer(SIDE * seq, WIDE),
            buffer(seq, SIDE * seq, dtype=F32), buffer(seq, SIDE * seq, dtype=F32), buffer(seq, SIDE * seq), buffer(seq, SIDE * seq),
            buffer(dim, seq), buffer(dim, seq), buffer(dim, seq, dtype=F32), buffer(LANE, seq, dtype=F32),
            buffer(PAIR, cat, seq), buffer(PAIR, SIDE, PAIR, dim // ROW, seq), buffer(dim, seq), buffer(PAIR, ROW, dim, dtype=F32),
            buffer(ROW, ROW, dim, dtype=F32), buffer(ROW, dim, dtype=F32),
            sem((SIDE,)), sem((16,)), sem((200,)), sem((200,)), sem((LANE,)), sem((LANE, PAIR)),
        ],
        compiler_params=pltpu.CompilerParams(collective_id=PAIR, has_side_effects=True, vmem_limit_bytes=67043328),
        name="run_layers",
    )(scale, w_in, w_out, x, dy, cos, sin, turn)


PARTS = (("i", "x", "z", "y", 0, STRIP), ("i", "x", "z", "y", STRIP, 384), ("i", "x", "y", "z", 0, STRIP), ("i", "x", "y", "z", STRIP, 384),
         ("o", "y", "z", "y", 0, 384), ("o", "z", "y", "z", 384, 384))


def reduce_order(rows, rows_b, starts):
    rate = 11650.0
    tasks = []
    share = WIDE * 896 / (PAIR * rate)
    tasks.append((("swap",), (0, 0), ZERO, [], [], [(("y", by), share / PAIR) for by in BOTH] + [(("y", by), share) for by in BOTH], 0.5))
    for i, by in enumerate(BOTH):
        tasks.append((("relay", by), (0, 1), ZERO, [(("swap",), i)], [], [(("y", by), share / PAIR)], 0.2))
        tasks.append((("near", by), (0, PAIR), ZERO, [(("swap",), PAIR + i)], [], [("chip", 1.6)], 0.2))
    tasks.append((("far",), (0, PAIR), ZERO, [(("relay", by), 0) for by in BOTH], [], [("chip", 1.6)], 0.2))
    for l in (1, 0):
        late = 1 - l
        for c, (kind, first, then, last, at, width) in enumerate(PARTS):
            needs, cost = [], 1.6 * width / STRIP
            if last == "y" and kind == "i" and l == 0:
                needs = [(("near", 1), 0), (("near", -1), 0), (("far",), 0)]
            tasks.append((("make", l, c), (9 * late, -c), starts[late], needs, [], [], cost))
            full = SIDE * SIDE * (rows if kind == "i" else rows_b) * width / rate
            sends = [[((first, by), full / ROW) for by in BOTH], [((first, by), full / SIDE) for by in BOTH],
                     [((then, o), full / 16) for o in (1, -1, 1)], []]
            piece = full / 16
            sends += [[((then, by), piece) for by in BOTH], [((then, 1 - PAIR * (c % PAIR)), piece)], [((last, by), SIDE * piece) for by in BOTH],
                      [((last, by), PAIR * piece) for by in BOTH], []]
            for s in range(9):
                task = ("sum", l, c, s)
                needs = [(("sum", l, c, s - 1), k) for k in range(len(sends[s - 1]))] if s else []
                tasks.append((task, (late, -s), ZERO, needs, [("make", l, c)] if s == 0 else [("sum", l, c, s - 1)], sends[s], 0.3))
    return plan(tasks)


def reduce_kernel(order, *refs):
    hy, hz, mx, yx = refs[0:PAIR], refs[PAIR:SIDE], refs[SIDE:6], refs[6:ROW]
    zy1, zz1, zz0, z0, sc = refs[ROW:13]
    oa, ob, relay = refs[13:16]
    n = len(PARTS)
    total, half, full, small, front = (refs[16 + k * n:16 + (k + 1) * n] for k in range(5))
    (hbuf, zbuf, mbuf, ybuf, scbuf, ssem, rsem, isem, osem, zsem) = refs[16 + 5 * n:]
    position = chip_position()
    x, y, zc, core = position
    place = {"x": x, "y": y, "z": zc}
    twin = device_at(x, y, zc, 1 - core)
    spots, peers = around(position)

    def spot(axis, o):
        return spots[axis, o % SIDE]

    def peer(axis, o):
        return peers[axis, o % SIDE]

    seq, wide = z0.shape
    own = wide // ROW
    loads = {}

    def load(key, src, dst):
        copy = pltpu.make_async_copy(src, dst, isem.at[len(loads)])
        copy.start()
        loads[key] = copy

    for l in (1, 0):
        if l:
            load(("z", 1, "y"), zy1, zbuf.at[1, 0])
            load(("z", 1, "z"), zz1, zbuf.at[1, 1])
        else:
            load(("z", 0, "z"), zz0, zbuf.at[0, 1])
        load(("h", l, "y"), hy[l], hbuf.at[l, 0])
        load(("h", l, "z"), hz[l], hbuf.at[l, 1])
        load(("m", l), mx[l], mbuf.at[l])
        load(("y", l), yx[l], ybuf.at[l])
        load(("s", l), sc.at[l], scbuf.at[l])
    done = set()

    def loaded(*keys):
        for key in keys:
            if key not in done:
                loads[key].wait()
                done.add(key)

    announce([peer(axis, o) for axis in "xyz" for o in AROUND] + [twin])
    links = Links(ssem, rsem)

    def columns(axis, o):
        return lanes(((0 if axis == "y" else SIDE) + spot(axis, o)) * own, own)

    def tokens(axis, o, index):
        return pl.ds(pl.multiple_of((PAIR * spot(axis, o) + index) * seq, seq), seq)

    def token_half(o, k):
        return pl.ds(pl.multiple_of((PAIR * spot("y", o) + core) * seq + k * (seq // PAIR), seq // PAIR), seq // PAIR)

    def swap():
        mine = zbuf.at[0, 0, tokens("y", 0, core)]
        for k, by in enumerate(BOTH):
            links.send(("zr", by), z0.at[pl.ds(k * (seq // PAIR), seq // PAIR), columns("y", PAIR)], relay.at[k], peer("y", by))
        for by in BOTH:
            links.send(("z", by), z0.at[:, columns("y", by)], mine, peer("y", by))
        links.send(("z",), z0.at[:, columns("y", 0)], mine, twin)
        load(("own",), z0.at[:, columns("y", 0)], mine)

    def pass_on(by):
        k = (1 - by) // PAIR
        links.arrive(("zr", by), relay.at[k])
        links.send(("z2", by), relay.at[k], zbuf.at[0, 0, token_half(-by, k)], peer("y", by))

    def near(by):
        landed = zbuf.at[0, 0, tokens("y", -by, core)]
        links.arrive(("z", by), landed)
        links.send(("zp", by), landed, landed, twin)

    def far():
        for k, by in enumerate(BOTH):
            links.arrive(("z2", by), zbuf.at[0, 0, token_half(PAIR, k)])
        landed = zbuf.at[0, 0, tokens("y", PAIR, core)]
        links.send(("zp", PAIR), landed, landed, twin)

    def make(l, c):
        kind, first, then, last, at, width = PARTS[c]
        if kind == "i":
            i = "yz".index(last)
            loaded(("h", l, last))
            if l or last == "z":
                loaded(("z", l, last))
            elif "joined" not in done:
                done.add("joined")
                loaded(("own",))
                links.arrive(("z",), zbuf.at[0, 0, tokens("y", 0, 1 - core)])
                for o in AROUND:
                    links.arrive(("zp", o), zbuf.at[0, 0, tokens("y", -o, 1 - core)])
            size = total[c].shape[3]
            for lo in range(0, width, WIDE):
                hi = min(width, lo + WIDE)
                part = product(hbuf[l, i].reshape(-1, hbuf.shape[-1]), zbuf[l, i, :, at + lo:at + hi])
                for r in range(16):
                    total[c][l, r // SIDE, r % SIDE, :, lo:hi] = part[r * size:(r + 1) * size]
            return
        loaded(("m", l), ("y", l), ("s", l))
        part = product(mbuf[l], ybuf[l, :, at:at + width])
        size = total[c].shape[3]

        def put(r, value):
            total[c][(l, r // SIDE, r % SIDE) if first == "y" else (l, r % SIDE, r // SIDE)] = value

        for r in range(part.shape[0] // size):
            put(r, part[r * size:(r + 1) * size])
        gain = jnp.sum(jnp.sum(scbuf[l, :, :, at:at + width], axis=0), axis=0, keepdims=True)
        row = lax.broadcasted_iota(jnp.int32, (size, width), 0)
        put(15, jnp.where(row == 0, gain, ZERO))

    def area(l, c, o, whole):
        kind, first, then, last, at, width = PARTS[c]
        inner = (spot(then, whole) if isinstance(whole, int) else whole)
        outer = spot(last, o)
        if kind == "i":
            cols = lanes(((0 if last == "y" else SIDE) + outer) * own + at, width)
            return oa.at[l, inner, :, cols]
        cols = pl.ds(at, width)
        return ob.at[l, outer, inner, :, cols] if last == "y" else ob.at[l, inner, outer, :, cols]

    def add(l, c, s):
        kind, first, then, last, at, width = PARTS[c]
        t = total[c].at[l]
        way = 1 - PAIR * (c % PAIR)
        key = (l, c)
        if s == 0:
            far = t.at[spot(first, PAIR)]
            for k, by in enumerate(BOTH):
                links.send((*key, "half", by), far.at[pl.ds(PAIR * k, PAIR)], half[c].at[l, k], peer(first, by))
        elif s == 1:
            for k, by in enumerate(BOTH):
                links.arrive((*key, "half", by), half[c].at[l, k])
                mine = t.at[spot(first, by)]
                add_into(mine.at[pl.ds(PAIR * k, PAIR)], half[c].at[l, k])
                links.send((*key, "full", by), mine, full[c].at[l, k], peer(first, by))
        elif s == PAIR:
            mine = t.at[spot(first, 0)]
            for k, by in enumerate(BOTH):
                links.arrive((*key, "full", by), full[c].at[l, k])
                add_into(mine, full[c].at[l, k])
            for k, o in enumerate(AROUND):
                links.send((*key, "small", o), mine.at[spot(then, o)], small[c].at[l, k], peer(then, o), (*key, "small", 1), small[c].at[l], (*key, "small"))
        elif s == 3:
            links.arrive((*key, "small", 1), small[c].at[l])
            mine = t.at[spot(first, 0), spot(then, 0)]
            front[c][l] = (mine[ALL] + small[c][l, 0]) + (small[c][l, 1] + small[c][l, PAIR])
        elif s == SIDE:
            src, dst = front[c].at[l], area(l, c, 0, 0)
            for by in BOTH:
                links.send((*key, "a1", by), src, dst, peer(then, by))
            copy = pltpu.make_async_copy(src, dst, osem.at[l, c])
            copy.start()
            loads["front", l, c] = copy
        elif s == 5:
            for by in BOTH:
                landed = area(l, c, 0, -by)
                links.arrive((*key, "a1", by), landed)
                if way == by:
                    links.send((*key, "b1"), landed, landed, peer(then, by))
        elif s == 6:
            loaded(("front", l, c))
            links.arrive((*key, "b1"), area(l, c, 0, PAIR))
            line = area(l, c, 0, slice(None))
            for by in BOTH:
                links.send((*key, "a2", by), line, line, peer(last, by))
        elif s == 7:
            for k, by in enumerate(BOTH):
                links.arrive((*key, "a2", by), area(l, c, -by, slice(None)))
                part = area(l, c, -by, pl.ds(PAIR * k, PAIR))
                links.send((*key, "a3", by), part, part, peer(last, by))
        else:
            for k, by in enumerate(BOTH):
                links.arrive((*key, "a3", by), area(l, c, PAIR, pl.ds(PAIR * k, PAIR)))

    stages = {"swap": swap, "relay": pass_on, "near": near, "far": far, "make": make, "sum": add}
    for kind, *task in order:
        stages[kind](*task)
    links.drain()


def add_into(dst, src):
    @pl.loop(0, dst.shape[0])
    def _(i):
        if len(dst.shape) == SIDE:
            for j in range(dst.shape[1]):
                dst[i, j] += src[i, j]
        else:
            dst[i] += src[i]


def around(position):
    place, core = dict(zip("xyz", position)), position[3]
    spots = {(axis, o): step(place[axis], o) for axis in "xyz" for o in range(SIDE)}
    peers = {}
    for axis in "xyz":
        for o in range(1, SIDE):
            moved = {**place, axis: spots[axis, o]}
            peers[axis, o] = device_at(moved["x"], moved["y"], moved["z"], core)
    return spots, peers


def reduce_gradients(operands, starts=(ZERO, ZERO)):
    hbm = pl.BlockSpec(memory_space=pltpu.HBM)
    h_rows, m_rows, y_cols, z_cols, z_own, scale_parts = operands
    part, part_b = h_rows[0].shape[1] // SIDE, (m_rows[0].shape[0] + BAND) // 16
    (line, dim), wide = y_cols[0].shape, z_own.shape[1]
    out = lambda *shape: jax.ShapeDtypeStruct(shape, F32)
    sem = pltpu.SemaphoreType.DMA

    def buffers(*lead):
        return [pltpu.VMEM((PAIR, *lead, part if e[0] == "i" else part_b, e[5]), F32) for e in PARTS]

    return pl.pallas_call(
        functools.partial(reduce_kernel, reduce_order(part, part_b, starts)),
        out_shape=(out(PAIR, SIDE, part, wide), out(PAIR, SIDE, SIDE, part_b, dim), jax.ShapeDtypeStruct((PAIR, z_own.shape[0] // PAIR, wide // ROW), BF)),
        in_specs=[hbm] * 13,
        out_specs=[hbm] * 3,
        scratch_shapes=[
            *buffers(SIDE, SIDE), *buffers(PAIR, PAIR), *buffers(PAIR, SIDE), *buffers(3), *buffers(),
            pltpu.VMEM((PAIR, PAIR, *h_rows[0].shape), BF), pltpu.VMEM((PAIR, PAIR, line, wide // ROW), BF), pltpu.VMEM((PAIR, *m_rows[0].shape), BF),
            pltpu.VMEM((PAIR, line, dim), BF), pltpu.VMEM(scale_parts.shape, F32),
            sem((WIDE,)), sem((WIDE,)), sem((16,)), sem((PAIR, len(PARTS))), sem((PAIR,)),
        ],
        compiler_params=pltpu.CompilerParams(collective_id=1, has_side_effects=True, vmem_limit_bytes=67043328),
        name="reduce_gradients",
    )(*h_rows, *m_rows, *y_cols, *z_cols, z_own, scale_parts)


def rotary_tables(seq_len, head_dim):
    half_dim = head_dim // PAIR
    inv_freq = 10000.0 ** (-(jnp.arange(half_dim, dtype=jnp.float32) * 2.0 / head_dim))
    angles = jnp.arange(seq_len, dtype=jnp.float32)[:, None] * inv_freq[None, :]
    return jnp.cos(angles), jnp.sin(angles)


def solution(mesh):
    fsdp_size = mesh.shape["fsdp"]
    batch_spec = P(("dp", "fsdp"), None, None)
    scale_spec = P(None, "fsdp")
    weight_spec = P(None, "fsdp", None)

    def device_step(x_in, grad_y, norm_scale, w_in, w_out):
        n_layers = w_in.shape[0]
        seq_len, model_dim = x_in.shape[1:]
        proj_dim = w_in.shape[PAIR]
        ff_dim = w_out.shape[1] * fsdp_size - model_dim
        head_dim = (proj_dim - model_dim - PAIR * ff_dim) // PAIR
        rows, rows_out = norm_scale.shape[1], w_out.shape[1]
        scale_rows = jnp.zeros((ROW, model_dim), jnp.float32)
        scale_rows = lax.dynamic_update_slice(scale_rows, norm_scale.astype(jnp.float32), (0, lax.axis_index("fsdp") * rows))
        cos_tab, sin_tab = rotary_tables(seq_len, head_dim)
        cos_tab, sin_tab = jnp.tile(cos_tab, (1, ROW)), jnp.tile(sin_tab, (1, ROW))
        lane = jnp.arange(WIDE)
        down = lane[:, None] - lane[None, :]
        low = lane[None, :] % head_dim < head_dim // PAIR
        turn = jnp.where(low & (down == BAND), -1.0, jnp.where(~low & (down == -BAND), 1.0, ZERO)).astype(jnp.bfloat16)
        hidden, grad_hidden, *rest = run_layers(x_in[0], grad_y[0], scale_rows, w_in, w_out, cos_tab, sin_tab, turn)
        in_sums, out_sums, _ = reduce_gradients((rest[0:SIDE], rest[SIDE:6], rest[6:ROW], rest[ROW:11], rest[11], rest[12]))
        in_grads = in_sums.reshape(n_layers, rows, -1)[:, :, :proj_dim]
        out_rows = out_sums.reshape(n_layers, -1, model_dim)
        scale_grads = lax.dynamic_slice(out_rows[:, rows_out], (0, lax.axis_index("fsdp") * rows), (n_layers, rows))
        out_grads = out_rows[:, :rows_out]
        return hidden[None], grad_hidden[None], scale_grads, in_grads, out_grads

    return jax.shard_map(
        device_step,
        mesh=mesh,
        in_specs=(batch_spec, batch_spec, scale_spec, weight_spec, weight_spec),
        out_specs=(batch_spec, batch_spec, scale_spec, weight_spec, weight_spec),
        check_vma=False,
    )
```

```python
import functools
import jax
import jax.numpy as jnp
from jax import lax
from jax.experimental import pallas as pl
from jax.experimental.pallas import tpu as pltpu
from jax.sharding import PartitionSpec as P

MESH_ID = pl.DeviceIdType.MESH
BOTH = (1, -1)
AROUND = (1, -1, 2)
PARTS = (True, False)
ALL, ZERO = ..., 0.0
LANE, WIDE, STRIP, HEAD = 128, 256, 512, 64
ROW, BAND, SIDE, PAIR = 8, 32, 4, 2


class Links:
    def __init__(self, send_sems, recv_sems):
        self.send_sems, self.recv_sems = send_sems, recv_sems
        self.slots, self.batches, self.sent = {}, {}, {}

    def send(self, key, src, dst, device, landing=None, whole=None, batch=None, lane=None):
        slot = self.slots.setdefault(landing or key, len(self.slots))
        leaving = self.batches.setdefault(batch or key, len(self.batches))
        copy = pltpu.make_async_remote_copy(
            src_ref=src, dst_ref=dst, send_sem=self.send_sems.at[leaving], recv_sem=self._landing(slot, lane),
            device_id=device, device_id_type=MESH_ID)
        copy.start()
        self.sent[batch or key] = (whole or src, leaving)

    def _landing(self, slot, lane):
        return self.recv_sems.at[slot] if lane is None else self.recv_sems.at[slot, lane]

    def arrive(self, key, landed, lane=None):
        slot = self.slots.setdefault(key, len(self.slots))
        pltpu.make_async_copy(landed, landed, self._landing(slot, lane)).wait()

    def drain(self):
        for left, leaving in self.sent.values():
            pltpu.make_async_copy(left, left, self.send_sems.at[leaving]).wait()
        self.sent.clear()


def rem(a, n):
    return a % n if isinstance(a, int) else lax.rem(a, n)


def chip_position():
    f, d = lax.axis_index("fsdp"), lax.axis_index("dp")
    return f // PAIR, rem(d, SIDE), d // SIDE, rem(f, PAIR)


def device_at(x, y, z, core):
    return (z * SIDE + y, x * PAIR + core)


def step(coord, by):
    return rem(coord + SIDE + by, SIDE)


def announce(devices):
    barrier = pltpu.get_barrier_semaphore()
    for device in devices:
        pl.semaphore_signal(barrier, inc=1, device_id=device, device_id_type=MESH_ID)
    pl.semaphore_wait(barrier, len(devices))


def plan(tasks, latency=2.5):
    free, landed, order, now = {}, {}, [], ZERO
    left = list(tasks)
    while left:
        best = None
        for place, (name, rank, start, needs, after, _, _) in enumerate(left):
            if all(n[0] in landed for n in needs) and all(n in landed for n in after):
                ready = max([start, now] + [landed[task][i] for task, i in needs])
                best = min(best or (ready, rank, place), (ready, rank, place))
        now, _, place = best
        name, _, _, _, _, sends, cost = left.pop(place)
        order.append(name)
        now += cost
        landed[name] = []
        for link, time in sends:
            free[link] = max(now, free.get(link, ZERO)) + time
            landed[name].append(free[link] + latency)
    return order


def layers_order(rows_i, cols_i, rows_o, cols_o, seq, starts):
    rate = 23300.0
    tasks = []
    for m in range(SIDE):
        is_in = m % PAIR == 0
        edge = cols_i // LANE * SIDE // 9 // PAIR * WIDE
        size = {"y": rows_i // SIDE * edge, "x": rows_i * (cols_i - PAIR * edge)} if is_in else {"y": rows_o // SIDE * cols_o // PAIR}
        size["z"] = size["y"]
        for color in "yzx" if is_in else "yz":
            cost = size[color] / rate
            both = [(("x", by), cost) for by in BOTH]
            spread = [((color, by), cost) for by in BOTH] if color != "x" else []
            tasks.append((("reach", m, color), m, starts[m], [], [], both, 0.2))
            for i, by in enumerate(BOTH):
                tasks.append((("relay", m, color, by), m, ZERO, [(("reach", m, color), i)], [], [(("x", by), cost / PAIR)] + spread, 0.2))
            halves = [(("relay", m, color, by), 0) for by in BOTH]
            tasks.append((("far", m, color), m, ZERO, halves, [], spread, 0.2))
            if color == "x":
                continue
            for off, source, first in ((-1, ("relay", m, color, 1), 1), (1, ("relay", m, color, -1), 1), (PAIR, ("far", m, color), 0)):
                for i, by in enumerate(BOTH):
                    tasks.append((("pass", m, color, off, by), m, ZERO, [(source, first + i)], [], [((color, by), cost / PAIR)], 0.2))
                halves = [(("pass", m, color, off, by), 0) for by in BOTH]
                tasks.append((("close", m, color, off), m, ZERO, halves, [], [], 0.2))
        for off in (-1, 1, PAIR):
            last = [("close", m, color, off) for color in "yz"]
            if is_in:
                last.append(("far", m, "x") if off == PAIR else ("relay", m, "x", -off))
            tasks.append((("hand", m, off), m, ZERO, [], last, [("chip", (rows_i * cols_i if is_in else rows_o * cols_o) / 150000.0)], 0.2))
    before = []

    def work(name, cost, mats=()):
        needs = [(("hand", m, off), 0) for m in mats for off in (-1, 1, PAIR)]
        tasks.append((name, 99, ZERO, needs, list(before), [], cost))
        before[:] = [name]

    for l in range(PAIR):
        work(("norm", l), 0.8)
        work(("project", l), 4.0, [PAIR * l])
        work(("attend", l), 3.0)
        work(("mlp", l), 2.4)
        work(("put", l), 1.6, [PAIR * l + 1])
    for l in (1, 0):
        work(("back_out", l), 2.9)
        work(("back_mlp", l), 2.0)
        work(("back_heads", l), 1.0)
        for g in range(3):
            work(("back_quad", l, g), 1.6)
        work(("back_keys", l), 0.2)
        for i in range(5):
            work(("back_in", l, i), 0.7)
        work(("back_norm", l), 1.0)
    def send(name, rank, start, after, sends):
        tasks.append((name, rank, start, [], [after] if after else [], sends, 0.4))

    def follow(name, rank, needs, sends):
        tasks.append((name, rank, ZERO, needs, [], sends, 0.2))

    def both(axis, size):
        return [((axis, by), size / rate) for by in BOTH]

    model = rows_i * ROW
    for l in (1, 0):
        for axis in "yz":
            name = ("send_h", l, axis)
            send(name, 20 - l, 58.0, ("norm", l), both(axis, seq * model))
            for i, by in enumerate(BOTH):
                for index in range(PAIR):
                    follow(("pass_h", l, axis, by, index), 10, [(name, i)], [((axis, by), seq * model / SIDE / rate)])
        name = ("send_m", l)
        send(name, 22 - l, ZERO, ("mlp", l), both("x", seq * rows_o) + both("x", PAIR * seq * rows_o))
        for i, by in enumerate(BOTH):
            for index in range(PAIR):
                follow(("pass_m", l, by, index), 11, [(name, i)], [(("x", by), seq * rows_o / PAIR / rate)])
        name = ("send_y", l)
        send(name, 12, 42.0, ("back_norm", 1) if l == 0 else None, both("x", seq * model))
        for i, by in enumerate(BOTH):
            follow(("pass_y", l, by), 12, [(name, i)], [(("x", by), seq * model / PAIR / rate)])
        follow(("far_y", l), 12, [(("pass_y", l, by), 0) for by in BOTH], [])
        for axis in "zy" if l else "z":
            name = ("send_z", l, axis)
            share = seq * (cols_i + LANE) / ROW
            send(name, 13, ZERO, ("back_mlp", l) if axis == "z" else ("back_keys", l), both(axis, share / PAIR) + both(axis, share))
            for i, by in enumerate(BOTH):
                follow(("pass_z", l, axis, by), 13, [(name, i)], [((axis, by), share / PAIR / rate)])
                follow(("twin_z", l, axis, by), 14, [(name, PAIR + i)], [])
            follow(("far_z", l, axis), 14, [(("pass_z", l, axis, by), 0) for by in BOTH], [])
        send(("send_scale", l), 15, ZERO, ("back_norm", l), [])
    send(("own_z",), 15, ZERO, ("back_keys", 0), [])
    return plan(tasks)


def gather_stages(links, position, shard_i, shard_o, wi, wo, lsem):
    x, y, z, core = position
    twin = device_at(x, y, z, 1 - core)
    rows_i, cols_i = shard_i.shape[1:]
    rows_o, cols_o = shard_o.shape[1:]
    quarter_i, quarter_o = rows_i // SIDE, rows_o // SIDE
    third_i = cols_i // LANE * SIDE // 9 // PAIR * WIDE
    half_o = cols_o // PAIR
    cut_o = quarter_o // 16 * ROW + ROW if quarter_o % 16 else quarter_o // PAIR
    place = {"x": x, "y": y, "z": z}

    spots = {(axis, o): step(place[axis], o) for axis in "xyz" for o in range(SIDE)}

    def spot(axis, o):
        return spots[axis, o % SIDE]

    table = {}
    for axis in "xyz":
        for o in range(1, SIDE):
            moved = {**place, axis: spot(axis, o)}
            table[axis, o] = device_at(moved["x"], moved["y"], moved["z"], core)

    def peer(axis, o):
        return table[axis, o % SIDE]

    mats = []
    for l in range(PAIR):
        mats.append((shard_i.at[l], wi.at[l], rows_i, True))
        mats.append((shard_o.at[l], wo.at[l], rows_o, False))

    def region(is_in, color, q):
        if is_in:
            if color == "x":
                lo, hi = PAIR * third_i, cols_i
                rows = (0, rows_i)
            else:
                lo, hi = (0, third_i) if color == "y" else (third_i, PAIR * third_i)
                rows = (q * quarter_i, quarter_i)
            mid = lo + ((hi - lo) // LANE + 1) // PAIR * LANE
            return (rows, (lo, hi - lo)), (rows, (lo, mid - lo)), (rows, (mid, hi - mid))
        cols = (0, half_o) if color == "y" else (half_o, half_o)
        start = q * quarter_o
        return ((start, quarter_o), cols), ((start, cut_o), cols), ((start + cut_o, quarter_o - cut_o), cols)

    def at(m, xb, area):
        (r, nr), (c, nc) = area
        _, out, size, _ = mats[m]
        return out.at[pl.ds(pl.multiple_of((PAIR * xb + core) * size + r, ROW), nr), pl.ds(c, nc)]

    def block(m, xb, index):
        _, out, size, _ = mats[m]
        return out.at[pl.ds(pl.multiple_of((PAIR * xb + index) * size, BAND), size)]

    def colors(m):
        return "yzx" if mats[m][3] else "yz"

    def reach(m, color):
        src, _, _, is_in = mats[m]
        area = region(is_in, color, place[color])[0]
        for by in BOTH:
            links.send((m, "x1", color, by), src.at[pl.ds(pl.multiple_of(area[0][0], ROW), area[0][1]), pl.ds(*area[1])], at(m, x, area), peer("x", by))

    def launch(m, color, off):
        is_in = mats[m][3]
        moved = at(m, spot("x", off), region(is_in, color, place[color])[0])
        for by in BOTH:
            links.send((m, "p1", color, off, by), moved, moved, peer(color, by))

    def relay(m, color, by):
        is_in = mats[m][3]
        xb = spot("x", -by)
        areas = region(is_in, color, place[color])
        links.arrive((m, "x1", color, by), at(m, xb, areas[0]))
        part = at(m, xb, areas[1] if by == 1 else areas[PAIR])
        links.send((m, "x2", color, by), part, part, peer("x", by))
        if color != "x":
            launch(m, color, -by)

    def far(m, color):
        is_in = mats[m][3]
        areas = region(is_in, color, place[color])
        for by in BOTH:
            links.arrive((m, "x2", color, by), at(m, spot("x", PAIR), areas[1] if by == 1 else areas[PAIR]))
        if color != "x":
            launch(m, color, PAIR)

    def pass_on(m, color, off, by):
        is_in = mats[m][3]
        xb = spot("x", off)
        areas = region(is_in, color, spot(color, -by))
        links.arrive((m, "p1", color, off, by), at(m, xb, areas[0]))
        part = at(m, xb, areas[1] if by == 1 else areas[PAIR])
        links.send((m, "p2", color, off, by), part, part, peer(color, by))

    def close(m, color, off):
        is_in = mats[m][3]
        areas = region(is_in, color, spot(color, PAIR))
        for by in BOTH:
            links.arrive((m, "p2", color, off, by), at(m, spot("x", off), areas[1] if by == 1 else areas[PAIR]))

    def hand(m, off):
        whole = block(m, spot("x", off), core)
        links.send((m, "d2d", off), whole, whole, twin)

    owns = []

    def begin():
        for m, (src, _, _, _) in enumerate(mats):
            copy = pltpu.make_async_copy(src, block(m, x, core), lsem.at[m])
            copy.start()
            owns.append(copy)
            links.send((m, "d2d", 0), src, block(m, x, core), twin)

    def ready(m):
        owns[m].wait()
        for off in (0, -1, 1, PAIR):
            links.arrive((m, "d2d", off), block(m, spot("x", off), 1 - core))

    return begin, ready, peer, {"reach": reach, "relay": relay, "far": far, "pass": pass_on, "close": close, "hand": hand}


BF, F32 = jnp.bfloat16, jnp.float32


def product(a, b, contract=((1,), (0,))):
    return lax.dot_general(a, b, (contract, ((), ())), preferred_element_type=F32)


def lanes(start, size):
    return pl.ds(start if isinstance(start, int) else pl.multiple_of(start, LANE), size)


def layers_kernel(order, sc_ref, wi_ref, wo_ref, x_ref, dy_ref, cos_ref, sin_ref, turn_ref,
                  y_ref, gx_ref, hy_a, hy_b, hz_a, hz_b, mx_a, mx_b, yx_a, yx_b, zy_b, zz_b, zz_a, z_a, sc_out, relay_m, relay_z,
                  wi, wo, z, om, h, hid, qr, kts, vsl, ksl, turned_q, turned_o, scores, dscores, pcat, dscat,
                  dot_heads, qt, dht, dkv, omt, ht, dyt, sc, gains, gain_ref, load_sems, own_sems, send_sems, recv_sems,
                  share_send_sems, share_recv_sems):
    seq, dim = x_ref.shape
    ff = (wi.shape[PAIR] - dim - LANE) // PAIR
    position = chip_position()
    x, y, zc, core = position
    twin = device_at(x, y, zc, 1 - core)
    me = PAIR * x + core
    links, shared = Links(send_sems, recv_sems), Links(share_send_sems, share_recv_sems)
    stored = []
    spots, _ = around(position)
    h_out, m_out, y_out, z_out = {"y": (hy_a, hy_b), "z": (hz_a, hz_b)}, (mx_a, mx_b), (yx_a, yx_b), {(1, "y"): zy_b, (1, "z"): zz_b, (0, "z"): zz_a}
    middle = hid.at[1]
    begin, ready, peer, stages = gather_stages(links, position, wi_ref, wo_ref, wi, wo, load_sems)
    others = [(zc * SIDE + y, rem(me + k, ROW)) for k in range(1, ROW)]

    def spot(axis, o):
        return spots[axis, o % SIDE]

    def device(axis, o, index):
        moved = {"x": x, "y": y, "z": zc, axis: spot(axis, o)}
        return device_at(moved["x"], moved["y"], moved["z"], index)

    announce(others + [device(axis, o, index) for axis in "yz" for o in AROUND for index in range(PAIR)])
    begin()
    for k, far in enumerate(others):
        links.send(("sc", k), sc_ref, gains.at[me], far)

    def keep(src, dst):
        copy = pltpu.make_async_copy(src, dst, own_sems.at[len(stored)])
        copy.start()
        stored.append(copy)

    def tokens(axis, o, index):
        return pl.ds(pl.multiple_of((PAIR * spot(axis, o) + index) * seq, seq), seq)

    def columns(axis, o):
        size = z.shape[PAIR] // ROW
        return lanes(((0 if axis == "y" else SIDE) + spot(axis, o)) * size, size)

    def send_h(l, axis):
        out = h_out[axis][l].at[:, :, tokens(axis, 0, core)]
        for by in BOTH:
            for index in range(PAIR):
                shared.send(("h", l, axis, by), ht.at[l, :, index], out, device(axis, by, index), batch=("h", l, axis, by, index), lane=core)
        shared.send(("h", l, axis), ht.at[l, :, 1 - core], out, twin, lane=0)
        keep(ht.at[l, :, core], out)

    def pass_h(l, axis, by, index):
        out = h_out[axis][l]
        shared.arrive(("h", l, axis, by), out.at[:, :, tokens(axis, -by, index)], index)
        part = out.at[pl.ds(1 - by, PAIR), :, tokens(axis, -by, index)]
        shared.send(("h2", l, axis, by), part, part, device(axis, by, core), batch=("h2", l, axis, by, index), lane=index)

    def arrive_h(l):
        for axis in "yz":
            for by in BOTH:
                for index in range(PAIR):
                    shared.arrive(("h2", l, axis, by), h_out[axis][l].at[pl.ds(1 - by, PAIR), :, tokens(axis, PAIR, index)], index)
            shared.arrive(("h", l, axis), h_out[axis][l].at[:, :, tokens(axis, 0, 1 - core)], 0)

    def row_block(l, o, index, part=None):
        size = omt.shape[1] // ROW
        start = (PAIR * spot("x", o) + index) * size
        if part is not None:
            size = size // PAIR
            start = start + part * size
        return omt.at[l, pl.ds(pl.multiple_of(start, 16), size)]

    def row_half(k):
        size = m_out[0].shape[0] // PAIR
        return pl.ds(k * size, size)

    def send_m(l):
        out = m_out[l].at[:, tokens("x", 0, core)]
        for k, by in enumerate(BOTH):
            for index in range(PAIR):
                shared.send(("mr", l, by), row_block(l, PAIR, index, k), relay_m.at[l, k, core], device("x", by, index), batch=("mr", l, by, index), lane=core)
        for by in BOTH:
            for index in range(PAIR):
                shared.send(("m", l, by), row_block(l, by, index), out, device("x", by, index), batch=("m", l, by, index), lane=core)
        shared.send(("m", l), row_block(l, 0, 1 - core), out, twin, lane=0)
        keep(row_block(l, 0, core), out)

    def pass_m(l, by, index):
        k = (1 - by) // PAIR
        shared.arrive(("mr", l, by), relay_m.at[l, k, index], index)
        shared.send(("m2", l, by), relay_m.at[l, k, index], m_out[l].at[row_half(k), tokens("x", -by, index)], device("x", by, core),
                    batch=("m2", l, by, index), lane=index)

    def arrive_m(l):
        for k, by in enumerate(BOTH):
            for index in range(PAIR):
                shared.arrive(("m", l, by), m_out[l].at[:, tokens("x", -by, index)], index)
                shared.arrive(("m2", l, by), m_out[l].at[row_half(k), tokens("x", PAIR, index)], index)
        shared.arrive(("m", l), m_out[l].at[:, tokens("x", 0, 1 - core)], 0)

    def token_half(axis, o, k):
        return pl.ds(pl.multiple_of((PAIR * spot(axis, o) + core) * seq + k * (seq // PAIR), seq // PAIR), seq // PAIR)

    def send_y(l):
        src, out = (middle, dy_ref)[l], y_out[l].at[tokens("x", 0, core)]
        for by in BOTH:
            shared.send(("y", l, by), src, out, device("x", by, core), lane=0)
        shared.send(("y", l), src, out, twin, lane=0)
        keep(src, out)

    def pass_y(l, by):
        landed, part = y_out[l].at[tokens("x", -by, core)], y_out[l].at[token_half("x", -by, (1 - by) // PAIR)]
        shared.arrive(("y", l, by), landed, 0)
        shared.send(("y2", l, by), part, part, device("x", by, core), lane=0)
        shared.send(("yp", l, by), landed, landed, twin, lane=0)

    def far_y(l):
        for k, by in enumerate(BOTH):
            shared.arrive(("y2", l, by), y_out[l].at[token_half("x", PAIR, k)], 0)
        landed = y_out[l].at[tokens("x", PAIR, core)]
        shared.send(("yp", l, PAIR), landed, landed, twin, lane=0)

    def arrive_y(l):
        for o in AROUND:
            shared.arrive(("yp", l, o), y_out[l].at[tokens("x", -o, 1 - core)], 0)
        shared.arrive(("y", l), y_out[l].at[tokens("x", 0, 1 - core)], 0)

    def send_z(l, axis):
        out = z_out[l, axis].at[tokens(axis, 0, core)]
        for k, by in enumerate(BOTH):
            shared.send(("zr", l, axis, by), z.at[l, pl.ds(k * (seq // PAIR), seq // PAIR), columns(axis, PAIR)], relay_z.at[l, "yz".index(axis), k],
                        device(axis, by, core), lane=0)
        for by in BOTH:
            shared.send(("z", l, axis, by), z.at[l, :, columns(axis, by)], out, device(axis, by, core), lane=0)
        shared.send(("z", l, axis), z.at[l, :, columns(axis, 0)], out, twin, lane=0)
        keep(z.at[l, :, columns(axis, 0)], out)

    def pass_z(l, axis, by):
        k = (1 - by) // PAIR
        half = relay_z.at[l, "yz".index(axis), k]
        shared.arrive(("zr", l, axis, by), half, 0)
        shared.send(("z2", l, axis, by), half, z_out[l, axis].at[token_half(axis, -by, k)], device(axis, by, core), lane=0)

    def twin_z(l, axis, by):
        landed = z_out[l, axis].at[tokens(axis, -by, core)]
        shared.arrive(("z", l, axis, by), landed, 0)
        shared.send(("zp", l, axis, by), landed, landed, twin, lane=0)

    def far_z(l, axis):
        for k, by in enumerate(BOTH):
            shared.arrive(("z2", l, axis, by), z_out[l, axis].at[token_half(axis, PAIR, k)], 0)
        landed = z_out[l, axis].at[tokens(axis, PAIR, core)]
        shared.send(("zp", l, axis, PAIR), landed, landed, twin, lane=0)

    def arrive_z(l, axis):
        for o in AROUND:
            shared.arrive(("zp", l, axis, o), z_out[l, axis].at[tokens(axis, -o, 1 - core)], 0)
        shared.arrive(("z", l, axis), z_out[l, axis].at[tokens(axis, 0, 1 - core)], 0)

    def send_scale(l):
        for k, far in enumerate(others):
            shared.send(("scale", l, k), sc.at[l], sc_out.at[l, me], far, lane=0)
        keep(sc.at[l], sc_out.at[l, me])

    def arrive_scale(l):
        for k in range(len(others)):
            shared.arrive(("scale", l, k), sc_out.at[l, rem(me + 7 - k, ROW)], 0)

    gains[me] = sc_ref[ALL]
    z[:, :, wi.shape[PAIR]:] = jnp.zeros((PAIR, seq, z.shape[PAIR] - wi.shape[PAIR]), BF)
    entry = (x_ref, hid.at[0])
    kts[ALL] = jnp.zeros(kts.shape, BF)
    pcat[ALL] = jnp.zeros(pcat.shape, BF)
    dscat[ALL] = jnp.zeros(dscat.shape, BF)

    def normalise(l, src):
        @pl.loop(0, seq // BAND, unroll=SIDE)
        def _(r):
            rows = pl.ds(pl.multiple_of(r * BAND, BAND), BAND)
            v = src[rows].astype(F32)
            v = v - jnp.mean(v, axis=-1, keepdims=True)
            var = jnp.mean(v * v, axis=-1, keepdims=True)
            h[l, rows] = (v * lax.rsqrt(var + 1e-6) * gain_ref[l:l + 1]).astype(BF)

    def project(l):
        strip = wi.shape[PAIR] // 5

        @pl.loop(0, 5)
        def _(i):
            at = lanes(i * strip, strip)
            z[l, :, at] = product(h[l], wi[l, :, at]).astype(BF)

    def heads(l):
        cos, sin = cos_ref[ALL], sin_ref[ALL]
        for g in range(dim // WIDE):
            q = z[l, :, g * WIDE:(g + 1) * WIDE]
            qr[l, :, g * WIDE:(g + 1) * WIDE] = ((q.astype(F32) * cos + product(q, turn_ref[ALL]) * sin) * 0.125).astype(BF)
        kv = z[l, :, dim:dim + LANE]
        turned = kv.astype(F32) * cos[:, :LANE] + product(kv, turn_ref[:LANE, :LANE]) * sin[:, :LANE]
        first = lax.broadcasted_iota(jnp.int32, turned.shape, 1) < HEAD
        key_lo = jnp.where(first, turned, ZERO)
        val_hi = jnp.where(first, ZERO, kv.astype(F32))
        return key_lo, pltpu.roll(key_lo, HEAD, 1), pltpu.roll(val_hi, HEAD, 1), val_hi

    def slot_rows(ref, lo, hi):
        zero = jnp.zeros((seq, LANE), BF)
        lo, hi = lo.astype(BF), hi.astype(BF)
        for i, (left, right) in enumerate(((lo, zero), (hi, zero), (zero, lo), (zero, hi))):
            ref[i * seq:(i + 1) * seq, :LANE] = left
            ref[i * seq:(i + 1) * seq, LANE:] = right

    def slot_cols(ref, lo):
        flat = lo.T[:HEAD].astype(BF)
        for i in range(SIDE):
            ref[HEAD * i:HEAD * (i + 1), i * seq:(i + 1) * seq] = flat

    def chances(i, half):
        n, at = LANE * (half + 1), slice(LANE * half, LANE * (half + 1))
        rows = pl.ds(pl.multiple_of(i * seq, seq), n)
        s = scores[rows, at]
        query = lax.broadcasted_iota(jnp.int32, s.shape, 1) + LANE * half
        s = jnp.where(query >= lax.broadcasted_iota(jnp.int32, s.shape, 0), s, -1e30)
        e = jnp.exp(s - jnp.max(s, axis=0, keepdims=True))
        return rows, at, e * (1.0 / jnp.sum(e, axis=0, keepdims=True))

    def attend(l):
        key_lo, key_hi, val_lo, _ = heads(l)
        slot_rows(ksl, key_lo, key_hi)
        slot_cols(kts, val_lo)
        flip(lambda at: qr[l, :, lanes(at, WIDE)], qt, dim)

        @pl.loop(0, dim // WIDE)
        def _(g):
            rows = pl.ds(pl.multiple_of(g * WIDE, WIDE), WIDE)
            scores[ALL] = product(ksl[ALL], qt[rows])

            @pl.loop(0, SIDE)
            def _(i):
                for half in range(PAIR):
                    keys, at, p = chances(i, half)
                    pcat[keys, at] = p.astype(BF)
            flat = product(kts[ALL], pcat[ALL]).astype(BF)
            omt[l, rows] = flat
            om[:, lanes(g * WIDE, WIDE)] = flat.T

    def mlp(l):
        @pl.loop(0, seq // BAND)
        def _(r):
            rows = pl.ds(pl.multiple_of(r * BAND, BAND), BAND)

            @pl.loop(0, ff // STRIP)
            def _(i):
                gate = z[l, rows, lanes(dim + LANE + i * STRIP, STRIP)].astype(F32)
                up = z[l, rows, lanes(dim + LANE + ff + i * STRIP, STRIP)].astype(F32)
                om[rows, lanes(dim + i * STRIP, STRIP)] = (gate * jax.nn.sigmoid(gate) * up).astype(BF)

    def put_out(l, dst):
        for n in range(dim // WIDE):
            cols = slice(n * WIDE, (n + 1) * WIDE)
            total = product(om[ALL], wo[l, :, cols])
            dst[:, cols] = (entry[l][:, cols].astype(F32) + total).astype(BF)

    def flip(src, dst, width, first=0):
        @pl.loop(first // WIDE, width // WIDE)
        def _(i):
            dst[pl.ds(pl.multiple_of(i * WIDE, WIDE), WIDE)] = src(i * WIDE).T

    upstream = (middle, dy_ref)

    def back_out(l):
        dy = upstream[l]
        flip(lambda at: dy[:, lanes(at, WIDE)], dyt, dim)

        @pl.loop(0, wo.shape[1] // dim)
        def _(n):
            rows = pl.ds(pl.multiple_of(n * dim, dim), dim)
            part = product(wo[l, rows], dyt[ALL]).astype(BF)
            om[:, lanes(n * dim, dim)] = part.T

            @pl.when(n == 0)
            def _():
                dot_heads[ALL] = part

    def back_mlp(l):
        @pl.loop(0, seq // BAND)
        def _(r):
            rows = pl.ds(pl.multiple_of(r * BAND, BAND), BAND)

            @pl.loop(0, ff // STRIP)
            def _(i):
                gate_at, up_at = lanes(dim + LANE + i * STRIP, STRIP), lanes(dim + LANE + ff + i * STRIP, STRIP)
                gate, up = z[l, rows, gate_at].astype(F32), z[l, rows, up_at].astype(F32)
                d = om[rows, lanes(dim + i * STRIP, STRIP)].astype(F32)
                sig = jax.nn.sigmoid(gate)
                du = d * up
                z[l, rows, gate_at] = (du * sig + du * gate * (sig * (1.0 - sig))).astype(BF)
                z[l, rows, up_at] = (d * (gate * sig)).astype(BF)

    def back_heads(l):
        key_lo, key_hi, val_lo, val_hi = heads(l)
        slot_rows(ksl, key_lo, key_hi)
        slot_rows(vsl, val_lo, val_hi)
        slot_cols(kts, key_lo)
        dkv[ALL] = jnp.zeros(dkv.shape, F32)
        flip(lambda at: qr[l, :, lanes(at, WIDE)], qt, dim)
        for at in range(0, dim, LANE):
            pair = slice(at, at + LANE)
            turned_q[:, pair] = pltpu.roll(qr[l, :, pair].astype(F32), HEAD, 1).astype(BF)
            turned_o[:, pair] = pltpu.roll(om[:, pair].astype(F32), HEAD, 1).astype(BF)

    def back_quad(l, g):
        cols = pl.ds(g * WIDE, WIDE)
        scores[ALL] = product(ksl[ALL], qt[cols])
        dscores[ALL] = product(vsl[ALL], dot_heads[cols])

        @pl.loop(0, SIDE)
        def _(i):
            for half in range(PAIR):
                keys, at, p = chances(i, half)
                pcat[keys, at] = p.astype(BF)
                pd = p * dscores[keys, at].astype(BF).astype(F32)
                dscat[keys, at] = (pd - p * jnp.sum(pd, axis=0, keepdims=True)).astype(BF)
        dq = product(kts[ALL], dscat[ALL]).astype(BF).T
        back = dq.astype(F32) * cos_ref[ALL] - product(dq, turn_ref[ALL]) * sin_ref[ALL]
        z[l, :, cols] = (back * 0.125).astype(BF)
        for i in range(SIDE):
            keys, pair = slice(i * seq, (i + 1) * seq), slice(g * WIDE + i // PAIR * LANE, g * WIDE + (i // PAIR + 1) * LANE)
            even = i % PAIR == 0
            dkv[0] += product(dscat[keys], qr[l, :, pair] if even else turned_q[:, pair])
            dkv[1] += product(pcat[keys], turned_o[:, pair] if even else om[:, pair])

    def back_keys(l):
        dk = dkv[0].astype(BF)
        turned = dk.astype(F32) * cos_ref[:, :LANE] - product(dk, turn_ref[:LANE, :LANE]) * sin_ref[:, :LANE]
        first = lax.broadcasted_iota(jnp.int32, turned.shape, 1) < HEAD
        z[l, :, dim:dim + LANE] = jnp.where(first, turned, dkv[1]).astype(BF)

    def back_in(l, i):
        width = wi.shape[PAIR] // 5
        at = slice(i * width, (i + 1) * width)
        part = product(wi[l, :, at], z[l, :, at], ((1,), (1,)))
        dht[ALL] = part if i == 0 else dht[ALL] + part

    def back_norm(l):
        dy, dst = upstream[l], (gx_ref, middle)[l]
        for i in range(dim // WIDE):
            cols = slice(i * WIDE, (i + 1) * WIDE)
            h[l, :, cols] = dht[cols].T.astype(BF)
        sc[l] = jnp.zeros(sc.shape[1:], F32)

        @pl.loop(0, seq // BAND, unroll=SIDE)
        def _(r):
            rows = pl.ds(pl.multiple_of(r * BAND, BAND), BAND)
            v = entry[l][rows].astype(F32)
            v = v - jnp.mean(v, axis=-1, keepdims=True)
            scale = lax.rsqrt(jnp.mean(v * v, axis=-1, keepdims=True) + 1e-6)
            hat = v * scale
            d = h[l, rows].astype(F32)
            each = (d * hat).reshape(SIDE, ROW, dim)
            sc[l] += (each[0] + each[1]) + (each[PAIR] + each[3])
            d = d * gain_ref[l:l + 1]
            d = scale * (d - jnp.mean(d, axis=-1, keepdims=True) - hat * jnp.mean(d * hat, axis=-1, keepdims=True))
            dst[rows] = (dy[rows].astype(F32) + d.astype(BF).astype(F32)).astype(BF)

    def do_norm(l):
        if l == 0:
            for k, (_, f) in enumerate(others):
                links.arrive(("sc", k), gains.at[rem(me + 7 - k, ROW)])
            gain_ref[ALL] = jnp.sum(gains[ALL], axis=0)
        normalise(l, entry[l])
        for i in range(dim // WIDE):
            flat = h[l, :, i * WIDE:(i + 1) * WIDE].T
            size = ht.shape[3]
            for b in range(ROW):
                lo, hi = max(b * size, i * WIDE), min((b + 1) * size, (i + 1) * WIDE)
                if lo < hi:
                    ht[l, b // PAIR, b % PAIR, lo - b * size:hi - b * size] = flat[lo - i * WIDE:hi - i * WIDE]

    def do_project(l):
        ready(PAIR * l)
        project(l)

    def do_mlp(l):
        mlp(l)
        flip(lambda at: om[:, lanes(at, WIDE)], omt.at[l], om.shape[1], dim)

    def do_put(l):
        ready(PAIR * l + 1)
        put_out(l, hid.at[0] if l == 0 else y_ref)

    stages.update(
        norm=do_norm, project=do_project, attend=attend, mlp=do_mlp, put=do_put, back_out=back_out, back_mlp=back_mlp, back_heads=back_heads,
        back_quad=back_quad, back_keys=back_keys, back_in=back_in, back_norm=back_norm, send_h=send_h, pass_h=pass_h, send_m=send_m,
        pass_m=pass_m, send_y=send_y, pass_y=pass_y, far_y=far_y, send_z=send_z, pass_z=pass_z, twin_z=twin_z, far_z=far_z,
        send_scale=send_scale, own_z=lambda: keep(z.at[0], z_a))
    for kind, *task in order:
        stages[kind](*task)
    for l in range(PAIR):
        arrive_h(l)
        arrive_m(l)
        arrive_scale(l)
        arrive_y(l)
    for l, axis in z_out:
        arrive_z(l, axis)
    for copy in stored:
        copy.wait()
    shared.drain()
    links.drain()


def run_layers(x, dy, scale, w_in, w_out, cos, sin, turn, starts=(ZERO, 10.0, 20.0, 30.0)):
    seq, dim = x.shape
    proj, cat = w_in.shape[PAIR], ROW * w_out.shape[1]
    wide = proj + LANE
    hbm, vmem = pl.BlockSpec(memory_space=pltpu.HBM), pl.BlockSpec(memory_space=pltpu.VMEM)
    out = lambda *shape, dtype=BF: jax.ShapeDtypeStruct(shape, dtype)
    buffer = lambda *shape, dtype=BF: pltpu.VMEM(shape, dtype)
    sem = pltpu.SemaphoreType.DMA
    line = ROW * seq
    return pl.pallas_call(
        functools.partial(layers_kernel, layers_order(*w_in.shape[1:], *w_out.shape[1:], seq, starts)),
        out_shape=(out(seq, dim), out(seq, dim), *[out(SIDE, dim // ROW, line)] * SIDE, *[out(cat // ROW, line)] * PAIR, *[out(line, dim)] * PAIR,
                   *[out(line, wide // ROW)] * 3, out(seq, wide), out(PAIR, ROW, ROW, dim, dtype=F32),
                   out(PAIR, PAIR, PAIR, cat // 16, seq), out(PAIR, PAIR, PAIR, seq // PAIR, wide // ROW)),
        in_specs=[vmem, hbm, hbm] + [vmem] * 5,
        out_specs=[vmem] * PAIR + [hbm] * 15,
        scratch_shapes=[
            buffer(PAIR, dim, proj), buffer(PAIR, cat, dim), buffer(PAIR, seq, wide), buffer(seq, cat), buffer(PAIR, seq, dim),
            buffer(PAIR, seq, dim), buffer(PAIR, seq, dim),
            buffer(WIDE, SIDE * seq), buffer(SIDE * seq, WIDE), buffer(SIDE * seq, WIDE), buffer(seq, dim), buffer(seq, dim),
            buffer(SIDE * seq, seq, dtype=F32), buffer(SIDE * seq, seq, dtype=F32), buffer(SIDE * seq, seq), buffer(SIDE * seq, seq),
            buffer(dim, seq), buffer(dim, seq), buffer(dim, seq, dtype=F32), buffer(PAIR, seq, LANE, dtype=F32),
            buffer(PAIR, cat, seq), buffer(PAIR, SIDE, PAIR, dim // ROW, seq), buffer(dim, seq), buffer(PAIR, ROW, dim, dtype=F32),
            buffer(ROW, ROW, dim, dtype=F32), buffer(ROW, dim, dtype=F32),
            sem((SIDE,)), sem((16,)), sem((200,)), sem((200,)), sem((LANE,)), sem((LANE, PAIR)),
        ],
        compiler_params=pltpu.CompilerParams(collective_id=PAIR, has_side_effects=True, vmem_limit_bytes=67043328),
        name="run_layers",
    )(scale, w_in, w_out, x, dy, cos, sin, turn)


PARTS = (("i", "x", "z", "y", 0, STRIP), ("i", "x", "z", "y", STRIP, 384), ("i", "x", "y", "z", 0, STRIP), ("i", "x", "y", "z", STRIP, 384),
         ("o", "y", "z", "y", 0, 384), ("o", "z", "y", "z", 384, 384))


def reduce_order(rows, rows_b, starts):
    rate = 11650.0
    tasks = []
    share = WIDE * 896 / (PAIR * rate)
    tasks.append((("swap",), (0, 0), ZERO, [], [], [(("y", by), share * n) for by, n in ((1, 1), (-1, 1), (1, PAIR))], 0.5))
    for i, o in enumerate(AROUND):
        tasks.append((("near", o), (0, PAIR), ZERO, [(("swap",), i)], [], [("chip", 1.6)], 0.2))
    for l in (1, 0):
        late = 1 - l
        for c, (kind, first, then, last, at, width) in enumerate(PARTS):
            needs, cost = [], 1.6 * width / STRIP
            if last == "y" and kind == "i" and l == 0:
                needs = [(("near", o), 0) for o in AROUND]
            tasks.append((("make", l, c), (9 * late, -c), starts[late], needs, [], [], cost))
            full = SIDE * SIDE * (rows if kind == "i" else rows_b) * width / rate
            sends = [[((first, by), full / ROW) for by in BOTH], [((first, by), full / SIDE) for by in BOTH],
                     [((then, o), full / 16) for o in (1, -1, 1)], []]
            piece = full / 16
            sends += [[((then, by), piece) for by in BOTH], [((then, 1 - PAIR * (c % PAIR)), piece)], [((last, by), SIDE * piece) for by in BOTH],
                      [((last, by), PAIR * piece) for by in BOTH], []]
            for s in range(9):
                task = ("sum", l, c, s)
                needs = [(("sum", l, c, s - 1), k) for k in range(len(sends[s - 1]))] if s else []
                tasks.append((task, (late, -s), ZERO, needs, [("make", l, c)] if s == 0 else [("sum", l, c, s - 1)], sends[s], 0.3))
    return plan(tasks)


def reduce_kernel(order, *refs):
    hy, hz, mx, yx = refs[0:PAIR], refs[PAIR:SIDE], refs[SIDE:6], refs[6:ROW]
    zy1, zz1, zz0, z0, sc = refs[ROW:13]
    oa, ob = refs[13:15]
    n = len(PARTS)
    total, half, full, small, front = (refs[15 + k * n:15 + (k + 1) * n] for k in range(5))
    (hbuf, zbuf, mbuf, ybuf, scbuf, ssem, rsem, isem, osem, zsem) = refs[15 + 5 * n:]
    position = chip_position()
    x, y, zc, core = position
    place = {"x": x, "y": y, "z": zc}
    twin = device_at(x, y, zc, 1 - core)
    spots, peers = around(position)

    def spot(axis, o):
        return spots[axis, o % SIDE]

    def peer(axis, o):
        return peers[axis, o % SIDE]

    seq, wide = z0.shape
    own = wide // ROW
    loads = {}

    def load(key, src, dst):
        copy = pltpu.make_async_copy(src, dst, isem.at[len(loads)])
        copy.start()
        loads[key] = copy

    for l in (1, 0):
        if l:
            load(("z", 1, "y"), zy1, zbuf.at[1, 0])
            load(("z", 1, "z"), zz1, zbuf.at[1, 1])
        else:
            load(("z", 0, "z"), zz0, zbuf.at[0, 1])
        load(("h", l, "y"), hy[l], hbuf.at[l, 0])
        load(("h", l, "z"), hz[l], hbuf.at[l, 1])
        load(("m", l), mx[l], mbuf.at[l])
        load(("y", l), yx[l], ybuf.at[l])
        load(("s", l), sc.at[l], scbuf.at[l])
    done = set()

    def loaded(*keys):
        for key in keys:
            if key not in done:
                loads[key].wait()
                done.add(key)

    announce([peer(axis, o) for axis in "xyz" for o in AROUND] + [twin])
    links = Links(ssem, rsem)

    def columns(axis, o):
        return lanes(((0 if axis == "y" else SIDE) + spot(axis, o)) * own, own)

    def tokens(axis, o, index):
        return pl.ds(pl.multiple_of((PAIR * spot(axis, o) + index) * seq, seq), seq)

    def swap():
        mine = zbuf.at[0, 0, tokens("y", 0, core)]
        for o in AROUND:
            links.send(("z", o), z0.at[:, columns("y", o)], mine, peer("y", o))
        links.send(("z",), z0.at[:, columns("y", 0)], mine, twin)
        load(("own",), z0.at[:, columns("y", 0)], mine)

    def near(o):
        landed = zbuf.at[0, 0, tokens("y", -o, core)]
        links.arrive(("z", o), landed)
        links.send(("zp", o), landed, landed, twin)

    def make(l, c):
        kind, first, then, last, at, width = PARTS[c]
        if kind == "i":
            i = "yz".index(last)
            loaded(("h", l, last))
            if l or last == "z":
                loaded(("z", l, last))
            elif "joined" not in done:
                done.add("joined")
                loaded(("own",))
                links.arrive(("z",), zbuf.at[0, 0, tokens("y", 0, 1 - core)])
                for o in AROUND:
                    links.arrive(("zp", o), zbuf.at[0, 0, tokens("y", -o, 1 - core)])
            size = total[c].shape[3]
            for lo in range(0, width, WIDE):
                hi = min(width, lo + WIDE)
                part = product(hbuf[l, i].reshape(-1, hbuf.shape[-1]), zbuf[l, i, :, at + lo:at + hi])
                for r in range(16):
                    total[c][l, r // SIDE, r % SIDE, :, lo:hi] = part[r * size:(r + 1) * size]
            return
        loaded(("m", l), ("y", l), ("s", l))
        part = product(mbuf[l], ybuf[l, :, at:at + width])
        size = total[c].shape[3]

        def put(r, value):
            total[c][(l, r // SIDE, r % SIDE) if first == "y" else (l, r % SIDE, r // SIDE)] = value

        for r in range(part.shape[0] // size):
            put(r, part[r * size:(r + 1) * size])
        gain = jnp.sum(jnp.sum(scbuf[l, :, :, at:at + width], axis=0), axis=0, keepdims=True)
        row = lax.broadcasted_iota(jnp.int32, (size, width), 0)
        put(15, jnp.where(row == 0, gain, ZERO))

    def area(l, c, o, whole):
        kind, first, then, last, at, width = PARTS[c]
        inner = (spot(then, whole) if isinstance(whole, int) else whole)
        outer = spot(last, o)
        if kind == "i":
            cols = lanes(((0 if last == "y" else SIDE) + outer) * own + at, width)
            return oa.at[l, inner, :, cols]
        cols = pl.ds(at, width)
        return ob.at[l, outer, inner, :, cols] if last == "y" else ob.at[l, inner, outer, :, cols]

    def add(l, c, s):
        kind, first, then, last, at, width = PARTS[c]
        t = total[c].at[l]
        way = 1 - PAIR * (c % PAIR)
        key = (l, c)
        if s == 0:
            far = t.at[spot(first, PAIR)]
            for k, by in enumerate(BOTH):
                links.send((*key, "half", by), far.at[pl.ds(PAIR * k, PAIR)], half[c].at[l, k], peer(first, by))
        elif s == 1:
            for k, by in enumerate(BOTH):
                links.arrive((*key, "half", by), half[c].at[l, k])
                mine = t.at[spot(first, by)]
                add_into(mine.at[pl.ds(PAIR * k, PAIR)], half[c].at[l, k])
                links.send((*key, "full", by), mine, full[c].at[l, k], peer(first, by))
        elif s == PAIR:
            mine = t.at[spot(first, 0)]
            for k, by in enumerate(BOTH):
                links.arrive((*key, "full", by), full[c].at[l, k])
                add_into(mine, full[c].at[l, k])
            for k, o in enumerate(AROUND):
                links.send((*key, "small", o), mine.at[spot(then, o)], small[c].at[l, k], peer(then, o), (*key, "small", 1), small[c].at[l], (*key, "small"))
        elif s == 3:
            links.arrive((*key, "small", 1), small[c].at[l])
            mine = t.at[spot(first, 0), spot(then, 0)]
            front[c][l] = (mine[ALL] + small[c][l, 0]) + (small[c][l, 1] + small[c][l, PAIR])
        elif s == SIDE:
            src, dst = front[c].at[l], area(l, c, 0, 0)
            for by in BOTH:
                links.send((*key, "a1", by), src, dst, peer(then, by))
            copy = pltpu.make_async_copy(src, dst, osem.at[l, c])
            copy.start()
            loads["front", l, c] = copy
        elif s == 5:
            for by in BOTH:
                landed = area(l, c, 0, -by)
                links.arrive((*key, "a1", by), landed)
                if way == by:
                    links.send((*key, "b1"), landed, landed, peer(then, by))
        elif s == 6:
            loaded(("front", l, c))
            links.arrive((*key, "b1"), area(l, c, 0, PAIR))
            line = area(l, c, 0, slice(None))
            for by in BOTH:
                links.send((*key, "a2", by), line, line, peer(last, by))
        elif s == 7:
            for k, by in enumerate(BOTH):
                links.arrive((*key, "a2", by), area(l, c, -by, slice(None)))
                part = area(l, c, -by, pl.ds(PAIR * k, PAIR))
                links.send((*key, "a3", by), part, part, peer(last, by))
        else:
            for k, by in enumerate(BOTH):
                links.arrive((*key, "a3", by), area(l, c, PAIR, pl.ds(PAIR * k, PAIR)))

    stages = {"swap": swap, "near": near, "make": make, "sum": add}
    for kind, *task in order:
        stages[kind](*task)
    links.drain()


def add_into(dst, src):
    @pl.loop(0, dst.shape[0])
    def _(i):
        if len(dst.shape) == SIDE:
            for j in range(dst.shape[1]):
                dst[i, j] += src[i, j]
        else:
            dst[i] += src[i]


def around(position):
    place, core = dict(zip("xyz", position)), position[3]
    spots = {(axis, o): step(place[axis], o) for axis in "xyz" for o in range(SIDE)}
    peers = {}
    for axis in "xyz":
        for o in range(1, SIDE):
            moved = {**place, axis: spots[axis, o]}
            peers[axis, o] = device_at(moved["x"], moved["y"], moved["z"], core)
    return spots, peers


def reduce_gradients(operands, starts=(ZERO, ZERO)):
    hbm = pl.BlockSpec(memory_space=pltpu.HBM)
    h_rows, m_rows, y_cols, z_cols, z_own, scale_parts = operands
    part, part_b = h_rows[0].shape[1] // SIDE, (m_rows[0].shape[0] + BAND) // 16
    (line, dim), wide = y_cols[0].shape, z_own.shape[1]
    out = lambda *shape: jax.ShapeDtypeStruct(shape, F32)
    sem = pltpu.SemaphoreType.DMA

    def buffers(*lead):
        return [pltpu.VMEM((PAIR, *lead, part if e[0] == "i" else part_b, e[5]), F32) for e in PARTS]

    return pl.pallas_call(
        functools.partial(reduce_kernel, reduce_order(part, part_b, starts)),
        out_shape=(out(PAIR, SIDE, part, wide), out(PAIR, SIDE, SIDE, part_b, dim)),
        in_specs=[hbm] * 13,
        out_specs=[hbm] * PAIR,
        scratch_shapes=[
            *buffers(SIDE, SIDE), *buffers(PAIR, PAIR), *buffers(PAIR, SIDE), *buffers(3), *buffers(),
            pltpu.VMEM((PAIR, PAIR, *h_rows[0].shape), BF), pltpu.VMEM((PAIR, PAIR, line, wide // ROW), BF), pltpu.VMEM((PAIR, *m_rows[0].shape), BF),
            pltpu.VMEM((PAIR, line, dim), BF), pltpu.VMEM(scale_parts.shape, F32),
            sem((WIDE,)), sem((WIDE,)), sem((16,)), sem((PAIR, len(PARTS))), sem((PAIR,)),
        ],
        compiler_params=pltpu.CompilerParams(collective_id=1, has_side_effects=True, vmem_limit_bytes=67043328),
        name="reduce_gradients",
    )(*h_rows, *m_rows, *y_cols, *z_cols, z_own, scale_parts)


def rotary_tables(seq_len, head_dim):
    half_dim = head_dim // PAIR
    inv_freq = 10000.0 ** (-(jnp.arange(half_dim, dtype=jnp.float32) * 2.0 / head_dim))
    angles = jnp.arange(seq_len, dtype=jnp.float32)[:, None] * inv_freq[None, :]
    return jnp.cos(angles), jnp.sin(angles)


def solution(mesh):
    fsdp_size = mesh.shape["fsdp"]
    batch_spec = P(("dp", "fsdp"), None, None)
    scale_spec = P(None, "fsdp")
    weight_spec = P(None, "fsdp", None)

    def device_step(x_in, grad_y, norm_scale, w_in, w_out):
        n_layers = w_in.shape[0]
        seq_len, model_dim = x_in.shape[1:]
        proj_dim = w_in.shape[PAIR]
        ff_dim = w_out.shape[1] * fsdp_size - model_dim
        head_dim = (proj_dim - model_dim - PAIR * ff_dim) // PAIR
        rows, rows_out = norm_scale.shape[1], w_out.shape[1]
        scale_rows = jnp.zeros((ROW, model_dim), jnp.float32)
        scale_rows = lax.dynamic_update_slice(scale_rows, norm_scale.astype(jnp.float32), (0, lax.axis_index("fsdp") * rows))
        cos_tab, sin_tab = rotary_tables(seq_len, head_dim)
        cos_tab, sin_tab = jnp.tile(cos_tab, (1, ROW)), jnp.tile(sin_tab, (1, ROW))
        lane = jnp.arange(WIDE)
        down = lane[:, None] - lane[None, :]
        low = lane[None, :] % head_dim < head_dim // PAIR
        turn = jnp.where(low & (down == BAND), -1.0, jnp.where(~low & (down == -BAND), 1.0, ZERO)).astype(jnp.bfloat16)
        hidden, grad_hidden, *rest = run_layers(x_in[0], grad_y[0], scale_rows, w_in, w_out, cos_tab, sin_tab, turn)
        in_sums, out_sums = reduce_gradients((rest[0:SIDE], rest[SIDE:6], rest[6:ROW], rest[ROW:11], rest[11], rest[12]))
        in_grads = in_sums.reshape(n_layers, rows, -1)[:, :, :proj_dim]
        out_rows = out_sums.reshape(n_layers, -1, model_dim)
        scale_grads = lax.dynamic_slice(out_rows[:, rows_out], (0, lax.axis_index("fsdp") * rows), (n_layers, rows))
        out_grads = out_rows[:, :rows_out]
        return hidden[None], grad_hidden[None], scale_grads, in_grads, out_grads

    return jax.shard_map(
        device_step,
        mesh=mesh,
        in_specs=(batch_spec, batch_spec, scale_spec, weight_spec, weight_spec),
        out_specs=(batch_spec, batch_spec, scale_spec, weight_spec, weight_spec),
        check_vma=False,
    )
```

```python
import functools
import jax
import jax.numpy as jnp
from jax import lax
from jax.experimental import pallas as pl
from jax.experimental.pallas import tpu as pltpu
from jax.sharding import PartitionSpec as P

MESH_ID = pl.DeviceIdType.MESH
BOTH = (1, -1)
AROUND = (1, -1, 2)
PARTS = (True, False)
ALL, ZERO = ..., 0.0
LANE, WIDE, STRIP, HEAD = 128, 256, 512, 64
ROW, BAND, SIDE, PAIR = 8, 32, 4, 2


class Links:
    def __init__(self, send_sems, recv_sems):
        self.send_sems, self.recv_sems = send_sems, recv_sems
        self.slots, self.batches, self.sent = {}, {}, {}

    def send(self, key, src, dst, device, landing=None, whole=None, batch=None, lane=None):
        slot = self.slots.setdefault(landing or key, len(self.slots))
        leaving = self.batches.setdefault(batch or key, len(self.batches))
        copy = pltpu.make_async_remote_copy(
            src_ref=src, dst_ref=dst, send_sem=self.send_sems.at[leaving], recv_sem=self._landing(slot, lane),
            device_id=device, device_id_type=MESH_ID)
        copy.start()
        self.sent[batch or key] = (whole or src, leaving)

    def _landing(self, slot, lane):
        return self.recv_sems.at[slot] if lane is None else self.recv_sems.at[slot, lane]

    def arrive(self, key, landed, lane=None):
        slot = self.slots.setdefault(key, len(self.slots))
        pltpu.make_async_copy(landed, landed, self._landing(slot, lane)).wait()

    def drain(self):
        for left, leaving in self.sent.values():
            pltpu.make_async_copy(left, left, self.send_sems.at[leaving]).wait()
        self.sent.clear()


def rem(a, n):
    return a % n if isinstance(a, int) else lax.rem(a, n)


def chip_position():
    f, d = lax.axis_index("fsdp"), lax.axis_index("dp")
    return f // PAIR, rem(d, SIDE), d // SIDE, rem(f, PAIR)


def device_at(x, y, z, core):
    return (z * SIDE + y, x * PAIR + core)


def step(coord, by):
    return rem(coord + SIDE + by, SIDE)


def announce(devices):
    barrier = pltpu.get_barrier_semaphore()
    for device in devices:
        pl.semaphore_signal(barrier, inc=1, device_id=device, device_id_type=MESH_ID)
    pl.semaphore_wait(barrier, len(devices))


def plan(tasks, latency=2.5):
    free, landed, order, now = {}, {}, [], ZERO
    left = list(tasks)
    while left:
        best = None
        for place, (name, rank, start, needs, after, _, _) in enumerate(left):
            if all(n[0] in landed for n in needs) and all(n in landed for n in after):
                ready = max([start, now] + [landed[task][i] for task, i in needs])
                best = min(best or (ready, rank, place), (ready, rank, place))
        now, _, place = best
        name, _, _, _, _, sends, cost = left.pop(place)
        order.append(name)
        now += cost
        landed[name] = []
        for link, time in sends:
            free[link] = max(now, free.get(link, ZERO)) + time
            landed[name].append(free[link] + latency)
    return order


def layers_order(rows_i, cols_i, rows_o, cols_o, seq, starts):
    rate = 23300.0
    tasks = []
    for m in range(SIDE):
        is_in = m % PAIR == 0
        edge = cols_i // LANE * SIDE // 9 // PAIR * WIDE
        size = {"y": rows_i // SIDE * edge, "x": rows_i * (cols_i - PAIR * edge)} if is_in else {"y": rows_o // SIDE * cols_o // PAIR}
        size["z"] = size["y"]
        for color in "yzx" if is_in else "yz":
            cost = size[color] / rate
            both = [(("x", by), cost) for by in BOTH]
            spread = [((color, by), cost) for by in BOTH] if color != "x" else []
            tasks.append((("reach", m, color), m, starts[m], [], [], both, 0.2))
            for i, by in enumerate(BOTH):
                tasks.append((("relay", m, color, by), m, ZERO, [(("reach", m, color), i)], [], [(("x", by), cost / PAIR)] + spread, 0.2))
            halves = [(("relay", m, color, by), 0) for by in BOTH]
            tasks.append((("far", m, color), m, ZERO, halves, [], spread, 0.2))
            if color == "x":
                continue
            for off, source, first in ((-1, ("relay", m, color, 1), 1), (1, ("relay", m, color, -1), 1), (PAIR, ("far", m, color), 0)):
                for i, by in enumerate(BOTH):
                    tasks.append((("pass", m, color, off, by), m, ZERO, [(source, first + i)], [], [((color, by), cost / PAIR)], 0.2))
                halves = [(("pass", m, color, off, by), 0) for by in BOTH]
                tasks.append((("close", m, color, off), m, ZERO, halves, [], [], 0.2))
        for off in (-1, 1, PAIR):
            last = [("close", m, color, off) for color in "yz"]
            if is_in:
                last.append(("far", m, "x") if off == PAIR else ("relay", m, "x", -off))
            tasks.append((("hand", m, off), m, ZERO, [], last, [("chip", (rows_i * cols_i if is_in else rows_o * cols_o) / 150000.0)], 0.2))
    before = []

    def work(name, cost, mats=()):
        needs = [(("hand", m, off), 0) for m in mats for off in (-1, 1, PAIR)]
        tasks.append((name, 99, ZERO, needs, list(before), [], cost))
        before[:] = [name]

    for l in range(PAIR):
        work(("norm", l), 0.8)
        work(("project", l), 4.0, [PAIR * l])
        work(("attend", l), 3.0)
        work(("mlp", l), 2.4)
        work(("put", l), 1.6, [PAIR * l + 1])
    for l in (1, 0):
        work(("back_out", l), 2.9)
        work(("back_mlp", l), 2.0)
        work(("back_heads", l), 1.0)
        work(("back_quad", l), 4.8)
        work(("back_keys", l), 0.2)
        for i in range(PAIR):
            work(("back_in", l, i), 1.3 + 0.7 * i)
        work(("back_norm", l), 1.0)
    def send(name, rank, start, after, sends):
        tasks.append((name, rank, start, [], [after] if after else [], sends, 0.4))

    def follow(name, rank, needs, sends):
        tasks.append((name, rank, ZERO, needs, [], sends, 0.2))

    def both(axis, size):
        return [((axis, by), size / rate) for by in BOTH]

    model = rows_i * ROW
    for l in (1, 0):
        for axis in "yz":
            name = ("send_h", l, axis)
            send(name, 20 - l, 58.0, ("norm", l), both(axis, seq * model))
            for i, by in enumerate(BOTH):
                for index in range(PAIR):
                    follow(("pass_h", l, axis, by, index), 10, [(name, i)], [((axis, by), seq * model / SIDE / rate)])
        name = ("send_m", l)
        send(name, 22 - l, ZERO, ("mlp", l), both("x", seq * rows_o) + both("x", PAIR * seq * rows_o))
        for i, by in enumerate(BOTH):
            for index in range(PAIR):
                follow(("pass_m", l, by, index), 11, [(name, i)], [(("x", by), seq * rows_o / PAIR / rate)])
        if l == 0:
            send(("own_y",), 15, ZERO, ("back_norm", 1), [])
            send(("send_scale", l), 15, ZERO, ("back_norm", l), [])
            continue
        name = ("send_y", l)
        send(name, 12, 42.0, None, both("x", seq * model))
        for i, by in enumerate(BOTH):
            follow(("pass_y", l, by), 12, [(name, i)], [(("x", by), seq * model / PAIR / rate)])
        follow(("far_y", l), 12, [(("pass_y", l, by), 0) for by in BOTH], [])
        for axis in "zy":
            name = ("send_z", l, axis)
            share = seq * (cols_i + LANE) / ROW
            send(name, 13, ZERO, ("back_mlp", l) if axis == "z" else ("back_keys", l), both(axis, share / PAIR) + both(axis, share))
            for i, by in enumerate(BOTH):
                follow(("pass_z", l, axis, by), 13, [(name, i)], [((axis, by), share / PAIR / rate)])
                follow(("twin_z", l, axis, by), 14, [(name, PAIR + i)], [])
            follow(("far_z", l, axis), 14, [(("pass_z", l, axis, by), 0) for by in BOTH], [])
        send(("send_scale", l), 15, ZERO, ("back_norm", l), [])
    send(("own_z",), 15, ZERO, ("back_keys", 0), [])
    return plan(tasks)


def gather_stages(links, position, shard_i, shard_o, wi, wo, lsem):
    x, y, z, core = position
    twin = device_at(x, y, z, 1 - core)
    rows_i, cols_i = shard_i.shape[1:]
    rows_o, cols_o = shard_o.shape[1:]
    quarter_i, quarter_o = rows_i // SIDE, rows_o // SIDE
    third_i = cols_i // LANE * SIDE // 9 // PAIR * WIDE
    half_o = cols_o // PAIR
    cut_o = quarter_o // 16 * ROW + ROW if quarter_o % 16 else quarter_o // PAIR
    place = {"x": x, "y": y, "z": z}

    spots = {(axis, o): step(place[axis], o) for axis in "xyz" for o in range(SIDE)}

    def spot(axis, o):
        return spots[axis, o % SIDE]

    table = {}
    for axis in "xyz":
        for o in range(1, SIDE):
            moved = {**place, axis: spot(axis, o)}
            table[axis, o] = device_at(moved["x"], moved["y"], moved["z"], core)

    def peer(axis, o):
        return table[axis, o % SIDE]

    mats = []
    for l in range(PAIR):
        mats.append((shard_i.at[l], wi.at[l], rows_i, True))
        mats.append((shard_o.at[l], wo.at[l], rows_o, False))

    def region(is_in, color, q):
        if is_in:
            if color == "x":
                lo, hi = PAIR * third_i, cols_i
                rows = (0, rows_i)
            else:
                lo, hi = (0, third_i) if color == "y" else (third_i, PAIR * third_i)
                rows = (q * quarter_i, quarter_i)
            mid = lo + ((hi - lo) // LANE + 1) // PAIR * LANE
            return (rows, (lo, hi - lo)), (rows, (lo, mid - lo)), (rows, (mid, hi - mid))
        cols = (0, half_o) if color == "y" else (half_o, half_o)
        start = q * quarter_o
        return ((start, quarter_o), cols), ((start, cut_o), cols), ((start + cut_o, quarter_o - cut_o), cols)

    def at(m, xb, area):
        (r, nr), (c, nc) = area
        _, out, size, _ = mats[m]
        return out.at[pl.ds(pl.multiple_of((PAIR * xb + core) * size + r, ROW), nr), pl.ds(c, nc)]

    def block(m, xb, index):
        _, out, size, _ = mats[m]
        return out.at[pl.ds(pl.multiple_of((PAIR * xb + index) * size, BAND), size)]

    def colors(m):
        return "yzx" if mats[m][3] else "yz"

    def reach(m, color):
        src, _, _, is_in = mats[m]
        area = region(is_in, color, place[color])[0]
        for by in BOTH:
            links.send((m, "x1", color, by), src.at[pl.ds(pl.multiple_of(area[0][0], ROW), area[0][1]), pl.ds(*area[1])], at(m, x, area), peer("x", by))

    def launch(m, color, off):
        is_in = mats[m][3]
        moved = at(m, spot("x", off), region(is_in, color, place[color])[0])
        for by in BOTH:
            links.send((m, "p1", color, off, by), moved, moved, peer(color, by))

    def relay(m, color, by):
        is_in = mats[m][3]
        xb = spot("x", -by)
        areas = region(is_in, color, place[color])
        links.arrive((m, "x1", color, by), at(m, xb, areas[0]))
        part = at(m, xb, areas[1] if by == 1 else areas[PAIR])
        links.send((m, "x2", color, by), part, part, peer("x", by))
        if color != "x":
            launch(m, color, -by)

    def far(m, color):
        is_in = mats[m][3]
        areas = region(is_in, color, place[color])
        for by in BOTH:
            links.arrive((m, "x2", color, by), at(m, spot("x", PAIR), areas[1] if by == 1 else areas[PAIR]))
        if color != "x":
            launch(m, color, PAIR)

    def pass_on(m, color, off, by):
        is_in = mats[m][3]
        xb = spot("x", off)
        areas = region(is_in, color, spot(color, -by))
        links.arrive((m, "p1", color, off, by), at(m, xb, areas[0]))
        part = at(m, xb, areas[1] if by == 1 else areas[PAIR])
        links.send((m, "p2", color, off, by), part, part, peer(color, by))

    def close(m, color, off):
        is_in = mats[m][3]
        areas = region(is_in, color, spot(color, PAIR))
        for by in BOTH:
            links.arrive((m, "p2", color, off, by), at(m, spot("x", off), areas[1] if by == 1 else areas[PAIR]))

    def hand(m, off):
        whole = block(m, spot("x", off), core)
        links.send((m, "d2d", off), whole, whole, twin)

    owns = []

    def begin():
        for m, (src, _, _, _) in enumerate(mats):
            copy = pltpu.make_async_copy(src, block(m, x, core), lsem.at[m])
            copy.start()
            owns.append(copy)
            links.send((m, "d2d", 0), src, block(m, x, core), twin)

    def ready(m):
        owns[m].wait()
        for off in (0, -1, 1, PAIR):
            links.arrive((m, "d2d", off), block(m, spot("x", off), 1 - core))

    return begin, ready, peer, {"reach": reach, "relay": relay, "far": far, "pass": pass_on, "close": close, "hand": hand}


BF, F32 = jnp.bfloat16, jnp.float32


def product(a, b, contract=((1,), (0,))):
    return lax.dot_general(a, b, (contract, ((), ())), preferred_element_type=F32)


def lanes(start, size):
    return pl.ds(start if isinstance(start, int) else pl.multiple_of(start, LANE), size)


def layers_kernel(order, sc_ref, wi_ref, wo_ref, x_ref, dy_ref, freq_ref,
                  y_ref, gx_ref, hy_a, hy_b, hz_a, hz_b, mx_a, mx_b, yx_b, zy_b, zz_b, z_a, dy_a, sc_out, relay_m, relay_z,
                  wi, wo, z, om, h, hid, qr, kts, vsl, ksl, turned_q, turned_o, scores, dscores, pcat, dscat, cos_ref, sin_ref, turn_ref,
                  dot_heads, qt, dht, dkv, omt, ht, dyt, sc, gains, gain_ref, load_sems, own_sems, send_sems, recv_sems,
                  share_send_sems, share_recv_sems):
    seq, dim = x_ref.shape
    ff = (wi.shape[PAIR] - dim - LANE) // PAIR
    position = chip_position()
    x, y, zc, core = position
    twin = device_at(x, y, zc, 1 - core)
    me = PAIR * x + core
    links, shared = Links(send_sems, recv_sems), Links(share_send_sems, share_recv_sems)
    stored = []
    spots, _ = around(position)
    h_out, m_out, y_out, z_out = {"y": (hy_a, hy_b), "z": (hz_a, hz_b)}, (mx_a, mx_b), {1: yx_b}, {(1, "y"): zy_b, (1, "z"): zz_b}
    middle = hid.at[1]
    begin, ready, peer, stages = gather_stages(links, position, wi_ref, wo_ref, wi, wo, load_sems)
    others = [(zc * SIDE + y, rem(me + k, ROW)) for k in range(1, ROW)]

    def spot(axis, o):
        return spots[axis, o % SIDE]

    def device(axis, o, index):
        moved = {"x": x, "y": y, "z": zc, axis: spot(axis, o)}
        return device_at(moved["x"], moved["y"], moved["z"], index)

    announce(others + [device(axis, o, index) for axis in "yz" for o in AROUND for index in range(PAIR)])
    begin()
    for k, far in enumerate(others):
        links.send(("sc", k), sc_ref, gains.at[me], far)

    def keep(src, dst):
        copy = pltpu.make_async_copy(src, dst, own_sems.at[len(stored)])
        copy.start()
        stored.append(copy)

    def tokens(axis, o, index):
        return pl.ds(pl.multiple_of((PAIR * spot(axis, o) + index) * seq, seq), seq)

    def columns(axis, o):
        size = z.shape[PAIR] // ROW
        return lanes(((0 if axis == "y" else SIDE) + spot(axis, o)) * size, size)

    def send_h(l, axis):
        out = h_out[axis][l].at[:, :, tokens(axis, 0, core)]
        for by in BOTH:
            for index in range(PAIR):
                shared.send(("h", l, axis, by), ht.at[l, :, index], out, device(axis, by, index), batch=("h", l, axis, by, index), lane=core)
        shared.send(("h", l, axis), ht.at[l, :, 1 - core], out, twin, lane=0)
        keep(ht.at[l, :, core], out)

    def pass_h(l, axis, by, index):
        out = h_out[axis][l]
        shared.arrive(("h", l, axis, by), out.at[:, :, tokens(axis, -by, index)], index)
        part = out.at[pl.ds(1 - by, PAIR), :, tokens(axis, -by, index)]
        shared.send(("h2", l, axis, by), part, part, device(axis, by, core), batch=("h2", l, axis, by, index), lane=index)

    def arrive_h(l):
        for axis in "yz":
            for by in BOTH:
                for index in range(PAIR):
                    shared.arrive(("h2", l, axis, by), h_out[axis][l].at[pl.ds(1 - by, PAIR), :, tokens(axis, PAIR, index)], index)
            shared.arrive(("h", l, axis), h_out[axis][l].at[:, :, tokens(axis, 0, 1 - core)], 0)

    def row_block(l, o, index, part=None):
        size = omt.shape[1] // ROW
        start = (PAIR * spot("x", o) + index) * size
        if part is not None:
            size = size // PAIR
            start = start + part * size
        return omt.at[l, pl.ds(pl.multiple_of(start, 16), size)]

    def row_half(k):
        size = m_out[0].shape[0] // PAIR
        return pl.ds(k * size, size)

    def send_m(l):
        out = m_out[l].at[:, tokens("x", 0, core)]
        for k, by in enumerate(BOTH):
            for index in range(PAIR):
                shared.send(("mr", l, by), row_block(l, PAIR, index, k), relay_m.at[l, k, core], device("x", by, index), batch=("mr", l, by, index), lane=core)
        for by in BOTH:
            for index in range(PAIR):
                shared.send(("m", l, by), row_block(l, by, index), out, device("x", by, index), batch=("m", l, by, index), lane=core)
        shared.send(("m", l), row_block(l, 0, 1 - core), out, twin, lane=0)
        keep(row_block(l, 0, core), out)

    def pass_m(l, by, index):
        k = (1 - by) // PAIR
        shared.arrive(("mr", l, by), relay_m.at[l, k, index], index)
        shared.send(("m2", l, by), relay_m.at[l, k, index], m_out[l].at[row_half(k), tokens("x", -by, index)], device("x", by, core),
                    batch=("m2", l, by, index), lane=index)

    def arrive_m(l):
        for k, by in enumerate(BOTH):
            for index in range(PAIR):
                shared.arrive(("m", l, by), m_out[l].at[:, tokens("x", -by, index)], index)
                shared.arrive(("m2", l, by), m_out[l].at[row_half(k), tokens("x", PAIR, index)], index)
        shared.arrive(("m", l), m_out[l].at[:, tokens("x", 0, 1 - core)], 0)

    def token_half(axis, o, k):
        return pl.ds(pl.multiple_of((PAIR * spot(axis, o) + core) * seq + k * (seq // PAIR), seq // PAIR), seq // PAIR)

    def send_y(l):
        src, out = dy_ref, y_out[l].at[tokens("x", 0, core)]
        for by in BOTH:
            shared.send(("y", l, by), src, out, device("x", by, core), lane=0)
        shared.send(("y", l), src, out, twin, lane=0)
        keep(src, out)

    def pass_y(l, by):
        landed, part = y_out[l].at[tokens("x", -by, core)], y_out[l].at[token_half("x", -by, (1 - by) // PAIR)]
        shared.arrive(("y", l, by), landed, 0)
        shared.send(("y2", l, by), part, part, device("x", by, core), lane=0)
        shared.send(("yp", l, by), landed, landed, twin, lane=0)

    def far_y(l):
        for k, by in enumerate(BOTH):
            shared.arrive(("y2", l, by), y_out[l].at[token_half("x", PAIR, k)], 0)
        landed = y_out[l].at[tokens("x", PAIR, core)]
        shared.send(("yp", l, PAIR), landed, landed, twin, lane=0)

    def arrive_y(l):
        for o in AROUND:
            shared.arrive(("yp", l, o), y_out[l].at[tokens("x", -o, 1 - core)], 0)
        shared.arrive(("y", l), y_out[l].at[tokens("x", 0, 1 - core)], 0)

    def send_z(l, axis):
        out = z_out[l, axis].at[tokens(axis, 0, core)]
        for k, by in enumerate(BOTH):
            shared.send(("zr", l, axis, by), z.at[l, pl.ds(k * (seq // PAIR), seq // PAIR), columns(axis, PAIR)], relay_z.at[l, "yz".index(axis), k],
                        device(axis, by, core), lane=0)
        for by in BOTH:
            shared.send(("z", l, axis, by), z.at[l, :, columns(axis, by)], out, device(axis, by, core), lane=0)
        shared.send(("z", l, axis), z.at[l, :, columns(axis, 0)], out, twin, lane=0)
        keep(z.at[l, :, columns(axis, 0)], out)

    def pass_z(l, axis, by):
        k = (1 - by) // PAIR
        half = relay_z.at[l, "yz".index(axis), k]
        shared.arrive(("zr", l, axis, by), half, 0)
        shared.send(("z2", l, axis, by), half, z_out[l, axis].at[token_half(axis, -by, k)], device(axis, by, core), lane=0)

    def twin_z(l, axis, by):
        landed = z_out[l, axis].at[tokens(axis, -by, core)]
        shared.arrive(("z", l, axis, by), landed, 0)
        shared.send(("zp", l, axis, by), landed, landed, twin, lane=0)

    def far_z(l, axis):
        for k, by in enumerate(BOTH):
            shared.arrive(("z2", l, axis, by), z_out[l, axis].at[token_half(axis, PAIR, k)], 0)
        landed = z_out[l, axis].at[tokens(axis, PAIR, core)]
        shared.send(("zp", l, axis, PAIR), landed, landed, twin, lane=0)

    def arrive_z(l, axis):
        for o in AROUND:
            shared.arrive(("zp", l, axis, o), z_out[l, axis].at[tokens(axis, -o, 1 - core)], 0)
        shared.arrive(("z", l, axis), z_out[l, axis].at[tokens(axis, 0, 1 - core)], 0)

    def send_scale(l):
        for k, far in enumerate(others):
            shared.send(("scale", l, k), sc.at[l], sc_out.at[l, me], far, lane=0)
        keep(sc.at[l], sc_out.at[l, me])

    def arrive_scale(l):
        for k in range(len(others)):
            shared.arrive(("scale", l, k), sc_out.at[l, rem(me + 7 - k, ROW)], 0)

    gains[me] = sc_ref[ALL]
    z[:, :, wi.shape[PAIR]:] = jnp.zeros((PAIR, seq, z.shape[PAIR] - wi.shape[PAIR]), BF)
    entry = (x_ref, hid.at[0])
    angle = lax.broadcasted_iota(jnp.int32, (seq, LANE), 0).astype(F32) * freq_ref[0:1]
    for half in range(PAIR):
        cos_ref[:, LANE * half:LANE * (half + 1)] = jnp.cos(angle)
        sin_ref[:, LANE * half:LANE * (half + 1)] = jnp.sin(angle)
    lane = lax.broadcasted_iota(jnp.int32, turn_ref.shape, 1)
    down = lax.broadcasted_iota(jnp.int32, turn_ref.shape, 0) - lane
    low = rem(lane, HEAD) < BAND
    turn_ref[ALL] = jnp.where(low & (down == BAND), -1.0, jnp.where(jnp.logical_not(low) & (down == -BAND), 1.0, ZERO)).astype(BF)
    kts[ALL] = jnp.zeros(kts.shape, BF)
    pcat[ALL] = jnp.zeros(pcat.shape, BF)
    dscat[ALL] = jnp.zeros(dscat.shape, BF)

    def normalise(l, src):
        @pl.loop(0, seq // BAND, unroll=SIDE)
        def _(r):
            rows = pl.ds(pl.multiple_of(r * BAND, BAND), BAND)
            v = src[rows].astype(F32)
            v = v - jnp.mean(v, axis=-1, keepdims=True)
            var = jnp.mean(v * v, axis=-1, keepdims=True)
            h[l, rows] = (v * lax.rsqrt(var + 1e-6) * gain_ref[l:l + 1]).astype(BF)

    def project(l):
        strip = wi.shape[PAIR] // 5

        @pl.loop(0, 5)
        def _(i):
            at = lanes(i * strip, strip)
            z[l, :, at] = product(h[l], wi[l, :, at]).astype(BF)

    def heads(l):
        cos, sin = cos_ref[ALL], sin_ref[ALL]
        for g in range(dim // WIDE):
            q = z[l, :, g * WIDE:(g + 1) * WIDE]
            qr[l, :, g * WIDE:(g + 1) * WIDE] = ((q.astype(F32) * cos + product(q, turn_ref[ALL]) * sin) * 0.125).astype(BF)
        kv = z[l, :, dim:dim + LANE]
        turned = kv.astype(F32) * cos[:, :LANE] + product(kv, turn_ref[:LANE, :LANE]) * sin[:, :LANE]
        first = lax.broadcasted_iota(jnp.int32, turned.shape, 1) < HEAD
        key_lo = jnp.where(first, turned, ZERO)
        val_hi = jnp.where(first, ZERO, kv.astype(F32))
        return key_lo, pltpu.roll(key_lo, HEAD, 1), pltpu.roll(val_hi, HEAD, 1), val_hi

    def slot_rows(ref, lo, hi):
        zero = jnp.zeros((seq, LANE), BF)
        lo, hi = lo.astype(BF), hi.astype(BF)
        for i, (left, right) in enumerate(((lo, zero), (hi, zero), (zero, lo), (zero, hi))):
            ref[i * seq:(i + 1) * seq, :LANE] = left
            ref[i * seq:(i + 1) * seq, LANE:] = right

    def slot_cols(ref, lo):
        flat = lo.T[:HEAD].astype(BF)
        for i in range(SIDE):
            ref[HEAD * i:HEAD * (i + 1), i * seq:(i + 1) * seq] = flat

    def chances(i, half):
        n, at = LANE * (half + 1), slice(LANE * half, LANE * (half + 1))
        rows = pl.ds(pl.multiple_of(i * seq, seq), n)
        s = scores[rows, at]
        query = lax.broadcasted_iota(jnp.int32, s.shape, 1) + LANE * half
        s = jnp.where(query >= lax.broadcasted_iota(jnp.int32, s.shape, 0), s, -1e30)
        e = jnp.exp(s - jnp.max(s, axis=0, keepdims=True))
        return rows, at, e * (1.0 / jnp.sum(e, axis=0, keepdims=True))

    def attend(l):
        key_lo, key_hi, val_lo, _ = heads(l)
        slot_rows(ksl, key_lo, key_hi)
        slot_cols(kts, val_lo)
        flip(lambda at: qr[l, :, lanes(at, WIDE)], qt, dim)

        @pl.loop(0, dim // WIDE)
        def _(g):
            rows = pl.ds(pl.multiple_of(g * WIDE, WIDE), WIDE)
            scores[ALL] = product(ksl[ALL], qt[rows])

            @pl.loop(0, SIDE)
            def _(i):
                for half in range(PAIR):
                    keys, at, p = chances(i, half)
                    pcat[keys, at] = p.astype(BF)
            flat = product(kts[ALL], pcat[ALL]).astype(BF)
            omt[l, rows] = flat
            om[:, lanes(g * WIDE, WIDE)] = flat.T

    def mlp(l):
        @pl.loop(0, seq // BAND)
        def _(r):
            rows = pl.ds(pl.multiple_of(r * BAND, BAND), BAND)

            @pl.loop(0, ff // STRIP)
            def _(i):
                gate = z[l, rows, lanes(dim + LANE + i * STRIP, STRIP)].astype(F32)
                up = z[l, rows, lanes(dim + LANE + ff + i * STRIP, STRIP)].astype(F32)
                om[rows, lanes(dim + i * STRIP, STRIP)] = (gate * jax.nn.sigmoid(gate) * up).astype(BF)

    def put_out(l, dst):
        for n in range(dim // WIDE):
            cols = slice(n * WIDE, (n + 1) * WIDE)
            total = product(om[ALL], wo[l, :, cols])
            dst[:, cols] = (entry[l][:, cols].astype(F32) + total).astype(BF)

    def flip(src, dst, width, first=0):
        @pl.loop(first // WIDE, width // WIDE)
        def _(i):
            dst[pl.ds(pl.multiple_of(i * WIDE, WIDE), WIDE)] = src(i * WIDE).T

    upstream = (middle, dy_ref)

    def back_out(l):
        dy = upstream[l]
        flip(lambda at: dy[:, lanes(at, WIDE)], dyt, dim)

        @pl.loop(0, wo.shape[1] // dim)
        def _(n):
            rows = pl.ds(pl.multiple_of(n * dim, dim), dim)
            part = product(wo[l, rows], dyt[ALL]).astype(BF)
            om[:, lanes(n * dim, dim)] = part.T

            @pl.when(n == 0)
            def _():
                dot_heads[ALL] = part

    def back_mlp(l):
        @pl.loop(0, seq // BAND)
        def _(r):
            rows = pl.ds(pl.multiple_of(r * BAND, BAND), BAND)

            @pl.loop(0, ff // STRIP)
            def _(i):
                gate_at, up_at = lanes(dim + LANE + i * STRIP, STRIP), lanes(dim + LANE + ff + i * STRIP, STRIP)
                gate, up = z[l, rows, gate_at].astype(F32), z[l, rows, up_at].astype(F32)
                d = om[rows, lanes(dim + i * STRIP, STRIP)].astype(F32)
                sig = jax.nn.sigmoid(gate)
                du = d * up
                z[l, rows, gate_at] = (du * sig + du * gate * (sig * (1.0 - sig))).astype(BF)
                z[l, rows, up_at] = (d * (gate * sig)).astype(BF)

    def back_heads(l):
        key_lo, key_hi, val_lo, val_hi = heads(l)
        slot_rows(ksl, key_lo, key_hi)
        slot_rows(vsl, val_lo, val_hi)
        slot_cols(kts, key_lo)
        dkv[ALL] = jnp.zeros(dkv.shape, F32)
        flip(lambda at: qr[l, :, lanes(at, WIDE)], qt, dim)
        for at in range(0, dim, LANE):
            pair = slice(at, at + LANE)
            turned_q[:, pair] = pltpu.roll(qr[l, :, pair].astype(F32), HEAD, 1).astype(BF)
            turned_o[:, pair] = pltpu.roll(om[:, pair].astype(F32), HEAD, 1).astype(BF)

    def back_quad(l):
        @pl.loop(0, dim // WIDE)
        def _(g):
            quad(l, g)

    def quad(l, g):
        cols = pl.ds(pl.multiple_of(g * WIDE, WIDE), WIDE)
        scores[ALL] = product(ksl[ALL], qt[cols])
        dscores[ALL] = product(vsl[ALL], dot_heads[cols])

        @pl.loop(0, SIDE)
        def _(i):
            for half in range(PAIR):
                keys, at, p = chances(i, half)
                pcat[keys, at] = p.astype(BF)
                pd = p * dscores[keys, at].astype(BF).astype(F32)
                dscat[keys, at] = (pd - p * jnp.sum(pd, axis=0, keepdims=True)).astype(BF)
        dq = product(kts[ALL], dscat[ALL]).astype(BF).T
        back = dq.astype(F32) * cos_ref[ALL] - product(dq, turn_ref[ALL]) * sin_ref[ALL]
        z[l, :, cols] = (back * 0.125).astype(BF)
        for i in range(SIDE):
            keys, pair = slice(i * seq, (i + 1) * seq), lanes(g * WIDE + i // PAIR * LANE, LANE)
            even = i % PAIR == 0
            dkv[0] += product(dscat[keys], qr[l, :, pair] if even else turned_q[:, pair])
            dkv[1] += product(pcat[keys], turned_o[:, pair] if even else om[:, pair])

    def back_keys(l):
        dk = dkv[0].astype(BF)
        turned = dk.astype(F32) * cos_ref[:, :LANE] - product(dk, turn_ref[:LANE, :LANE]) * sin_ref[:, :LANE]
        first = lax.broadcasted_iota(jnp.int32, turned.shape, 1) < HEAD
        z[l, :, dim:dim + LANE] = jnp.where(first, turned, dkv[1]).astype(BF)

    def back_in(l, half):
        width = wi.shape[PAIR] // 5
        if half == 0:
            dht[ALL] = jnp.zeros(dht.shape, F32)

        @pl.loop(PAIR * half, PAIR + 3 * half)
        def _(i):
            at = lanes(i * width, width)
            dht[ALL] += product(wi[l, :, at], z[l, :, at], ((1,), (1,)))

    def back_norm(l):
        dy, dst = upstream[l], (gx_ref, middle)[l]
        for i in range(dim // WIDE):
            cols = slice(i * WIDE, (i + 1) * WIDE)
            h[l, :, cols] = dht[cols].T.astype(BF)
        sc[l] = jnp.zeros(sc.shape[1:], F32)

        @pl.loop(0, seq // BAND, unroll=SIDE)
        def _(r):
            rows = pl.ds(pl.multiple_of(r * BAND, BAND), BAND)
            v = entry[l][rows].astype(F32)
            v = v - jnp.mean(v, axis=-1, keepdims=True)
            scale = lax.rsqrt(jnp.mean(v * v, axis=-1, keepdims=True) + 1e-6)
            hat = v * scale
            d = h[l, rows].astype(F32)
            each = (d * hat).reshape(SIDE, ROW, dim)
            sc[l] += (each[0] + each[1]) + (each[PAIR] + each[3])
            d = d * gain_ref[l:l + 1]
            d = scale * (d - jnp.mean(d, axis=-1, keepdims=True) - hat * jnp.mean(d * hat, axis=-1, keepdims=True))
            dst[rows] = (dy[rows].astype(F32) + d.astype(BF).astype(F32)).astype(BF)

    def do_norm(l):
        if l == 0:
            for k, (_, f) in enumerate(others):
                links.arrive(("sc", k), gains.at[rem(me + 7 - k, ROW)])
            gain_ref[ALL] = jnp.sum(gains[ALL], axis=0)
        normalise(l, entry[l])
        for i in range(dim // WIDE):
            flat = h[l, :, i * WIDE:(i + 1) * WIDE].T
            size = ht.shape[3]
            for b in range(ROW):
                lo, hi = max(b * size, i * WIDE), min((b + 1) * size, (i + 1) * WIDE)
                if lo < hi:
                    ht[l, b // PAIR, b % PAIR, lo - b * size:hi - b * size] = flat[lo - i * WIDE:hi - i * WIDE]

    def do_project(l):
        ready(PAIR * l)
        project(l)

    def do_mlp(l):
        mlp(l)
        flip(lambda at: om[:, lanes(at, WIDE)], omt.at[l], om.shape[1], dim)

    def do_put(l):
        ready(PAIR * l + 1)
        put_out(l, hid.at[0] if l == 0 else y_ref)

    stages.update(
        norm=do_norm, project=do_project, attend=attend, mlp=do_mlp, put=do_put, back_out=back_out, back_mlp=back_mlp, back_heads=back_heads,
        back_quad=back_quad, back_keys=back_keys, back_in=back_in, back_norm=back_norm, send_h=send_h, pass_h=pass_h, send_m=send_m,
        pass_m=pass_m, send_y=send_y, pass_y=pass_y, far_y=far_y, send_z=send_z, pass_z=pass_z, twin_z=twin_z, far_z=far_z,
        send_scale=send_scale, own_z=lambda: keep(z.at[0], z_a), own_y=lambda: keep(middle, dy_a))
    for kind, *task in order:
        stages[kind](*task)
    for l in range(PAIR):
        arrive_h(l)
        arrive_m(l)
        arrive_scale(l)
    arrive_y(1)
    for l, axis in z_out:
        arrive_z(l, axis)
    for copy in stored:
        copy.wait()
    shared.drain()
    links.drain()


def run_layers(x, dy, scale, w_in, w_out, freq, starts=(ZERO, 10.0, 20.0, 30.0)):
    seq, dim = x.shape
    proj, cat = w_in.shape[PAIR], ROW * w_out.shape[1]
    wide = proj + LANE
    hbm, vmem = pl.BlockSpec(memory_space=pltpu.HBM), pl.BlockSpec(memory_space=pltpu.VMEM)
    out = lambda *shape, dtype=BF: jax.ShapeDtypeStruct(shape, dtype)
    buffer = lambda *shape, dtype=BF: pltpu.VMEM(shape, dtype)
    sem = pltpu.SemaphoreType.DMA
    line = ROW * seq
    return pl.pallas_call(
        functools.partial(layers_kernel, layers_order(*w_in.shape[1:], *w_out.shape[1:], seq, starts)),
        out_shape=(out(seq, dim), out(seq, dim), *[out(SIDE, dim // ROW, line)] * SIDE, *[out(cat // ROW, line)] * PAIR, out(line, dim),
                   *[out(line, wide // ROW)] * PAIR, out(seq, wide), out(seq, dim), out(PAIR, ROW, ROW, dim, dtype=F32),
                   out(PAIR, PAIR, PAIR, cat // 16, seq), out(PAIR, PAIR, PAIR, seq // PAIR, wide // ROW)),
        in_specs=[vmem, hbm, hbm] + [vmem] * 3,
        out_specs=[vmem] * PAIR + [hbm] * 14,
        scratch_shapes=[
            buffer(PAIR, dim, proj), buffer(PAIR, cat, dim), buffer(PAIR, seq, wide), buffer(seq, cat), buffer(PAIR, seq, dim),
            buffer(PAIR, seq, dim), buffer(PAIR, seq, dim),
            buffer(WIDE, SIDE * seq), buffer(SIDE * seq, WIDE), buffer(SIDE * seq, WIDE), buffer(seq, dim), buffer(seq, dim),
            buffer(SIDE * seq, seq, dtype=F32), buffer(SIDE * seq, seq, dtype=F32), buffer(SIDE * seq, seq), buffer(SIDE * seq, seq),
            buffer(seq, WIDE, dtype=F32), buffer(seq, WIDE, dtype=F32), buffer(WIDE, WIDE),
            buffer(dim, seq), buffer(dim, seq), buffer(dim, seq, dtype=F32), buffer(PAIR, seq, LANE, dtype=F32),
            buffer(PAIR, cat, seq), buffer(PAIR, SIDE, PAIR, dim // ROW, seq), buffer(dim, seq), buffer(PAIR, ROW, dim, dtype=F32),
            buffer(ROW, ROW, dim, dtype=F32), buffer(ROW, dim, dtype=F32),
            sem((SIDE,)), sem((16,)), sem((200,)), sem((200,)), sem((LANE,)), sem((LANE, PAIR)),
        ],
        compiler_params=pltpu.CompilerParams(collective_id=PAIR, has_side_effects=True, vmem_limit_bytes=67043328),
        name="run_layers",
    )(scale, w_in, w_out, x, dy, freq)


PARTS = (("i", "x", "z", "y", 0, STRIP), ("i", "x", "z", "y", STRIP, 384), ("i", "x", "y", "z", 0, STRIP), ("i", "x", "y", "z", STRIP, 384),
         ("o", "y", "z", "y", 0, 384), ("o", "z", "y", "z", 384, 384))


def reduce_order(rows, rows_b, starts):
    rate = 11650.0
    tasks = []
    sizes = {"y": WIDE * 896 / (PAIR * rate), "z": WIDE * 896 / (PAIR * rate), "x": WIDE * 768 / (PAIR * rate)}
    for axis in "yzx":
        tasks.append((("swap", axis), (0, 0), starts[PAIR] if axis == "x" else ZERO, [], [], [((axis, by), sizes[axis] * n) for by, n in ((1, 1), (-1, 1), (1, PAIR))], 0.3))
        for i, o in enumerate(AROUND):
            tasks.append((("near", axis, o), (0, PAIR), ZERO, [(("swap", axis), i)], [], [("chip", 1.6)], 0.2))
    tasks.append((("fetch", 0), (5, 0), ZERO, [], [("make", 1, len(PARTS) - 1)], [], 0.2))
    for l in (1, 0):
        late = 1 - l
        for c, (kind, first, then, last, at, width) in enumerate(PARTS):
            needs, cost = [], 1.6 * width / STRIP
            if l == 0:
                needs = [(("near", last if kind == "i" else "x", o), 0) for o in AROUND]
            tasks.append((("make", l, c), (9 * late, c), starts[late], needs, [] if l else [("fetch", 0)], [], cost))
            full = SIDE * SIDE * (rows if kind == "i" else rows_b) * width / rate
            sends = [[((first, by), full / ROW) for by in BOTH], [((first, by), full / SIDE) for by in BOTH],
                     [((then, o), full / 16) for o in (1, -1, 1)], []]
            piece = full / 16
            sends += [[((then, by), piece) for by in BOTH], [((then, 1 - PAIR * (c % PAIR)), piece)], [((last, by), SIDE * piece) for by in BOTH],
                      [((last, by), PAIR * piece) for by in BOTH], []]
            for s in range(9):
                task = ("sum", l, c, s)
                needs = [(("sum", l, c, s - 1), k) for k in range(len(sends[s - 1]))] if s else []
                tasks.append((task, (late, -s), ZERO, needs, [("make", l, c)] if s == 0 else [("sum", l, c, s - 1)], sends[s], 0.3))
    return plan(tasks)


def reduce_kernel(order, *refs):
    hy, hz, mx = refs[0:PAIR], refs[PAIR:SIDE], refs[SIDE:6]
    yx1, zy1, zz1, z0, y0, sc = refs[6:12]
    oa, ob = refs[12:14]
    n = len(PARTS)
    total, half, full, small, front = (refs[14 + k * n:14 + (k + 1) * n] for k in range(5))
    (hbuf, zbuf, mbuf, ybuf, scbuf, ssem, rsem, isem, osem, zsem) = refs[14 + 5 * n:]
    position = chip_position()
    x, y, zc, core = position
    place = {"x": x, "y": y, "z": zc}
    twin = device_at(x, y, zc, 1 - core)
    spots, peers = around(position)

    def spot(axis, o):
        return spots[axis, o % SIDE]

    def peer(axis, o):
        return peers[axis, o % SIDE]

    seq, wide = z0.shape
    own = wide // ROW
    loads = {}

    def load(key, src, dst):
        copy = pltpu.make_async_copy(src, dst, isem.at[len(loads)])
        copy.start()
        loads[key] = copy

    def fetch(l):
        if l:
            load(("z", 1, "y"), zy1, zbuf.at[1, 0])
        load(("h", l, "y"), hy[l], hbuf.at[l, 0])
        if l:
            load(("z", 1, "z"), zz1, zbuf.at[1, 1])
        load(("h", l, "z"), hz[l], hbuf.at[l, 1])
        load(("m", l), mx[l], mbuf.at[l])
        if l:
            load(("y", 1), yx1, ybuf.at[1])
        load(("s", l), sc.at[l], scbuf.at[l])

    fetch(1)
    done = set()

    def loaded(*keys):
        for key in keys:
            if key not in done:
                loads[key].wait()
                done.add(key)

    announce([peer(axis, o) for axis in "xyz" for o in AROUND] + [twin])
    links = Links(ssem, rsem)

    def columns(axis, o):
        return lanes(((0 if axis == "y" else SIDE) + spot(axis, o)) * own, own)

    def tokens(axis, o, index):
        return pl.ds(pl.multiple_of((PAIR * spot(axis, o) + index) * seq, seq), seq)

    def target(axis):
        return ybuf.at[0] if axis == "x" else zbuf.at[0, "yz".index(axis)]

    def swap(axis):
        def part(o):
            return y0 if axis == "x" else z0.at[:, columns(axis, o)]

        mine = target(axis).at[tokens(axis, 0, core)]
        for o in AROUND:
            links.send(("swap", axis, o), part(o), mine, peer(axis, o))
        links.send(("swap", axis), part(0), mine, twin)
        load(("own", axis), part(0), mine)

    def near(axis, o):
        landed = target(axis).at[tokens(axis, -o, core)]
        links.arrive(("swap", axis, o), landed)
        links.send(("near", axis, o), landed, landed, twin)

    def joined(axis):
        if axis not in done:
            done.add(axis)
            loaded(("own", axis))
            links.arrive(("swap", axis), target(axis).at[tokens(axis, 0, 1 - core)])
            for o in AROUND:
                links.arrive(("near", axis, o), target(axis).at[tokens(axis, -o, 1 - core)])

    def make(l, c):
        kind, first, then, last, at, width = PARTS[c]
        if kind == "i":
            i = "yz".index(last)
            loaded(("h", l, last))
            if l:
                loaded(("z", l, last))
            else:
                joined(last)
            size = total[c].shape[3]
            for lo in range(0, width, WIDE):
                hi = min(width, lo + WIDE)
                part = product(hbuf[l, i].reshape(-1, hbuf.shape[-1]), zbuf[l, i, :, at + lo:at + hi])
                for r in range(16):
                    total[c][l, r // SIDE, r % SIDE, :, lo:hi] = part[r * size:(r + 1) * size]
            return
        loaded(("m", l), ("s", l))
        if l:
            loaded(("y", l))
        else:
            joined("x")
        part = product(mbuf[l], ybuf[l, :, at:at + width])
        size = total[c].shape[3]

        def put(r, value):
            total[c][(l, r // SIDE, r % SIDE) if first == "y" else (l, r % SIDE, r // SIDE)] = value

        for r in range(part.shape[0] // size):
            put(r, part[r * size:(r + 1) * size])
        gain = jnp.sum(jnp.sum(scbuf[l, :, :, at:at + width], axis=0), axis=0, keepdims=True)
        row = lax.broadcasted_iota(jnp.int32, (size, width), 0)
        put(15, jnp.where(row == 0, gain, ZERO))

    def area(l, c, o, whole):
        kind, first, then, last, at, width = PARTS[c]
        inner = (spot(then, whole) if isinstance(whole, int) else whole)
        outer = spot(last, o)
        if kind == "i":
            cols = lanes(((0 if last == "y" else SIDE) + outer) * own + at, width)
            return oa.at[l, inner, :, cols]
        cols = pl.ds(at, width)
        return ob.at[l, outer, inner, :, cols] if last == "y" else ob.at[l, inner, outer, :, cols]

    def add(l, c, s):
        kind, first, then, last, at, width = PARTS[c]
        t = total[c].at[l]
        way = 1 - PAIR * (c % PAIR)
        key = (l, c)
        if s == 0:
            far = t.at[spot(first, PAIR)]
            for k, by in enumerate(BOTH):
                links.send((*key, "half", by), far.at[pl.ds(PAIR * k, PAIR)], half[c].at[l, k], peer(first, by))
        elif s == 1:
            for k, by in enumerate(BOTH):
                links.arrive((*key, "half", by), half[c].at[l, k])
                mine = t.at[spot(first, by)]
                add_into(mine.at[pl.ds(PAIR * k, PAIR)], half[c].at[l, k])
                links.send((*key, "full", by), mine, full[c].at[l, k], peer(first, by))
        elif s == PAIR:
            mine = t.at[spot(first, 0)]
            for k, by in enumerate(BOTH):
                links.arrive((*key, "full", by), full[c].at[l, k])
                add_into(mine, full[c].at[l, k])
            for k, o in enumerate(AROUND):
                links.send((*key, "small", o), mine.at[spot(then, o)], small[c].at[l, k], peer(then, o), (*key, "small", 1), small[c].at[l], (*key, "small"))
        elif s == 3:
            links.arrive((*key, "small", 1), small[c].at[l])
            mine = t.at[spot(first, 0), spot(then, 0)]
            front[c][l] = (mine[ALL] + small[c][l, 0]) + (small[c][l, 1] + small[c][l, PAIR])
        elif s == SIDE:
            src, dst = front[c].at[l], area(l, c, 0, 0)
            for by in BOTH:
                links.send((*key, "a1", by), src, dst, peer(then, by))
            copy = pltpu.make_async_copy(src, dst, osem.at[l, c])
            copy.start()
            loads["front", l, c] = copy
        elif s == 5:
            for by in BOTH:
                landed = area(l, c, 0, -by)
                links.arrive((*key, "a1", by), landed)
                if way == by:
                    links.send((*key, "b1"), landed, landed, peer(then, by))
        elif s == 6:
            loaded(("front", l, c))
            links.arrive((*key, "b1"), area(l, c, 0, PAIR))
            line = area(l, c, 0, slice(None))
            for by in BOTH:
                links.send((*key, "a2", by), line, line, peer(last, by))
        elif s == 7:
            for k, by in enumerate(BOTH):
                links.arrive((*key, "a2", by), area(l, c, -by, slice(None)))
                part = area(l, c, -by, pl.ds(PAIR * k, PAIR))
                links.send((*key, "a3", by), part, part, peer(last, by))
        else:
            for k, by in enumerate(BOTH):
                links.arrive((*key, "a3", by), area(l, c, PAIR, pl.ds(PAIR * k, PAIR)))

    stages = {"swap": swap, "near": near, "fetch": fetch, "make": make, "sum": add}
    for kind, *task in order:
        stages[kind](*task)
    links.drain()


def add_into(dst, src):
    @pl.loop(0, dst.shape[0])
    def _(i):
        if len(dst.shape) == SIDE:
            for j in range(dst.shape[1]):
                dst[i, j] += src[i, j]
        else:
            dst[i] += src[i]


def around(position):
    place, core = dict(zip("xyz", position)), position[3]
    spots = {(axis, o): step(place[axis], o) for axis in "xyz" for o in range(SIDE)}
    peers = {}
    for axis in "xyz":
        for o in range(1, SIDE):
            moved = {**place, axis: spots[axis, o]}
            peers[axis, o] = device_at(moved["x"], moved["y"], moved["z"], core)
    return spots, peers


def reduce_gradients(operands, starts=(ZERO, ZERO, ZERO)):
    hbm = pl.BlockSpec(memory_space=pltpu.HBM)
    h_rows, m_rows, y_cols, z_cols, z_own, y_own, scale_parts = operands
    part, part_b = h_rows[0].shape[1] // SIDE, (m_rows[0].shape[0] + BAND) // 16
    (line, dim), wide = y_cols.shape, z_own.shape[1]
    out = lambda *shape: jax.ShapeDtypeStruct(shape, F32)
    sem = pltpu.SemaphoreType.DMA

    def buffers(*lead):
        return [pltpu.VMEM((PAIR, *lead, part if e[0] == "i" else part_b, e[5]), F32) for e in PARTS]

    return pl.pallas_call(
        functools.partial(reduce_kernel, reduce_order(part, part_b, starts)),
        out_shape=(out(PAIR, SIDE, part, wide), out(PAIR, SIDE, SIDE, part_b, dim)),
        in_specs=[hbm] * 12,
        out_specs=[hbm] * PAIR,
        scratch_shapes=[
            *buffers(SIDE, SIDE), *buffers(PAIR, PAIR), *buffers(PAIR, SIDE), *buffers(3), *buffers(),
            pltpu.VMEM((PAIR, PAIR, *h_rows[0].shape), BF), pltpu.VMEM((PAIR, PAIR, line, wide // ROW), BF), pltpu.VMEM((PAIR, *m_rows[0].shape), BF),
            pltpu.VMEM((PAIR, line, dim), BF), pltpu.VMEM(scale_parts.shape, F32),
            sem((WIDE,)), sem((WIDE,)), sem((BAND,)), sem((PAIR, len(PARTS))), sem((PAIR,)),
        ],
        compiler_params=pltpu.CompilerParams(collective_id=1, has_side_effects=True, vmem_limit_bytes=67043328),
        name="reduce_gradients",
    )(*h_rows, *m_rows, y_cols, *z_cols, z_own, y_own, scale_parts)


def solution(mesh):
    fsdp_size = mesh.shape["fsdp"]
    batch_spec = P(("dp", "fsdp"), None, None)
    scale_spec = P(None, "fsdp")
    weight_spec = P(None, "fsdp", None)

    def device_step(x_in, grad_y, norm_scale, w_in, w_out):
        n_layers = w_in.shape[0]
        seq_len, model_dim = x_in.shape[1:]
        proj_dim = w_in.shape[PAIR]
        ff_dim = w_out.shape[1] * fsdp_size - model_dim
        head_dim = (proj_dim - model_dim - PAIR * ff_dim) // PAIR
        rows, rows_out = norm_scale.shape[1], w_out.shape[1]
        scale_rows = jnp.zeros((ROW, model_dim), jnp.float32)
        scale_rows = lax.dynamic_update_slice(scale_rows, norm_scale.astype(jnp.float32), (0, lax.axis_index("fsdp") * rows))
        half_dim = head_dim // PAIR
        freq = 10000.0 ** (-(jnp.arange(half_dim, dtype=jnp.float32) * 2.0 / head_dim))
        freq = jnp.broadcast_to(jnp.tile(freq, LANE // half_dim), (ROW, LANE))
        hidden, grad_hidden, *rest = run_layers(x_in[0], grad_y[0], scale_rows, w_in, w_out, freq)
        in_sums, out_sums = reduce_gradients((rest[0:SIDE], rest[SIDE:6], rest[6], rest[7:9], rest[9], rest[10], rest[11]))
        in_grads = in_sums.reshape(n_layers, rows, -1)[:, :, :proj_dim]
        out_rows = out_sums.reshape(n_layers, -1, model_dim)
        scale_grads = lax.dynamic_slice(out_rows[:, rows_out], (0, lax.axis_index("fsdp") * rows), (n_layers, rows))
        out_grads = out_rows[:, :rows_out]
        return hidden[None], grad_hidden[None], scale_grads, in_grads, out_grads

    return jax.shard_map(
        device_step,
        mesh=mesh,
        in_specs=(batch_spec, batch_spec, scale_spec, weight_spec, weight_spec),
        out_specs=(batch_spec, batch_spec, scale_spec, weight_spec, weight_spec),
        check_vma=False,
    )
```

```python
import functools
import jax
import jax.numpy as jnp
import numpy as np
from jax import lax
from jax.experimental import pallas as pl
from jax.experimental.pallas import tpu as pltpu
from jax.sharding import PartitionSpec as P

MESH_ID = pl.DeviceIdType.MESH
BOTH = (1, -1)
AROUND = (1, -1, 2)
PARTS = (True, False)
ALL, ZERO = ..., 0.0
LANE, WIDE, STRIP, HEAD = 128, 256, 512, 64
ROW, BAND, SIDE, PAIR = 8, 32, 4, 2


class Links:
    def __init__(self, send_sems, recv_sems):
        self.send_sems, self.recv_sems = send_sems, recv_sems
        self.slots, self.batches, self.sent, self.count = {}, {}, {}, 0

    def _landing(self, key, lane):
        if key not in self.slots:
            self.slots[key] = self.count
            self.count += 1 if lane is None else PAIR
        return self.recv_sems.at[self.slots[key] + (0 if lane is None else lane)]

    def send(self, key, src, dst, device, landing=None, whole=None, batch=None, lane=None):
        leaving = self.batches.setdefault(batch or key, len(self.batches))
        copy = pltpu.make_async_remote_copy(
            src_ref=src, dst_ref=dst, send_sem=self.send_sems.at[leaving], recv_sem=self._landing(landing or key, lane),
            device_id=device, device_id_type=MESH_ID)
        copy.start()
        self.sent[batch or key] = (src if whole is None else whole, leaving)

    def arrive(self, key, landed, lane=None):
        pltpu.make_async_copy(landed, landed, self._landing(key, lane)).wait()

    def drain(self):
        for left, leaving in self.sent.values():
            pltpu.make_async_copy(left, left, self.send_sems.at[leaving]).wait()
        self.sent.clear()


def rem(a, n):
    return a % n if isinstance(a, int) else lax.rem(a, n)


def chip_position():
    f, d = lax.axis_index("fsdp"), lax.axis_index("dp")
    return f // PAIR, rem(d, SIDE), d // SIDE, rem(f, PAIR)


def device_at(x, y, z, core):
    return (z * SIDE + y, x * PAIR + core)


def step(coord, by):
    return rem(coord + SIDE + by, SIDE)


def announce(devices):
    barrier = pltpu.get_barrier_semaphore()
    for device in devices:
        pl.semaphore_signal(barrier, inc=1, device_id=device, device_id_type=MESH_ID)
    pl.semaphore_wait(barrier, len(devices))


def plan(tasks, latency=2.5):
    free, landed, order, now = {}, {}, [], ZERO
    left = list(tasks)
    while left:
        best = None
        for place, (name, rank, start, needs, after, _, _) in enumerate(left):
            if all(n[0] in landed for n in needs) and all(n in landed for n in after):
                ready = max([start, now] + [landed[task][i] for task, i in needs])
                best = min(best or (ready, rank, place), (ready, rank, place))
        now, _, place = best
        name, _, _, _, _, sends, cost = left.pop(place)
        order.append(name)
        now += cost
        landed[name] = []
        for link, time in sends:
            free[link] = max(now, free.get(link, ZERO)) + time
            landed[name].append(free[link] + latency)
    return order


def layers_order(rows_i, cols_i, rows_o, cols_o, seq, starts):
    rate = 23300.0
    tasks = []
    for m in range(SIDE):
        is_in = m % PAIR == 0
        edge = cols_i // LANE * SIDE // 9 // PAIR * WIDE
        size = {"y": rows_i // SIDE * edge, "x": rows_i * (cols_i - PAIR * edge)} if is_in else {"y": rows_o // SIDE * cols_o // PAIR}
        size["z"] = size["y"]
        for color in "yzx" if is_in else "yz":
            cost = size[color] / rate
            both = [(("x", by), cost) for by in BOTH]
            spread = [((color, by), cost) for by in BOTH] if color != "x" else []
            tasks.append((("reach", m, color), m, starts[m], [], [], both, 0.2))
            for i, by in enumerate(BOTH):
                tasks.append((("relay", m, color, by), m, ZERO, [(("reach", m, color), i)], [], [(("x", by), cost / PAIR)] + spread, 0.2))
            halves = [(("relay", m, color, by), 0) for by in BOTH]
            tasks.append((("far", m, color), m, ZERO, halves, [], spread, 0.2))
            if color == "x":
                continue
            for off, source, first in ((-1, ("relay", m, color, 1), 1), (1, ("relay", m, color, -1), 1), (PAIR, ("far", m, color), 0)):
                for i, by in enumerate(BOTH):
                    tasks.append((("pass", m, color, off, by), m, ZERO, [(source, first + i)], [], [((color, by), cost / PAIR)], 0.2))
                halves = [(("pass", m, color, off, by), 0) for by in BOTH]
                tasks.append((("close", m, color, off), m, ZERO, halves, [], [], 0.2))
        for off in (-1, 1, PAIR):
            last = [("close", m, color, off) for color in "yz"]
            if is_in:
                last.append(("far", m, "x") if off == PAIR else ("relay", m, "x", -off))
            tasks.append((("hand", m, off), m, ZERO, [], last, [("chip", (rows_i * cols_i if is_in else rows_o * cols_o) / 150000.0)], 0.2))
    before = []

    def work(name, cost, mats=()):
        needs = [(("hand", m, off), 0) for m in mats for off in (-1, 1, PAIR)]
        tasks.append((name, 99, ZERO, needs, list(before), [], cost))
        before[:] = [name]

    for l in range(PAIR):
        work(("norm", l), 0.8)
        work(("project", l), 4.0, [PAIR * l])
        work(("attend", l), 3.0)
        work(("mlp", l), 2.4)
        work(("put", l), 1.6, [PAIR * l + 1])
    for l in (1, 0):
        work(("back_out", l), 2.9)
        work(("back_mlp", l), 2.0)
        work(("back_heads", l), 1.0)
        work(("back_quad", l), 4.8)
        work(("back_keys", l), 0.2)
        for i in range(PAIR):
            work(("back_in", l, i), 1.3 + 0.7 * i)
        work(("back_norm", l), 1.0)
    def send(name, rank, start, after, sends):
        tasks.append((name, rank, start, [], [after] if after else [], sends, 0.4))

    def follow(name, rank, needs, sends):
        tasks.append((name, rank, ZERO, needs, [], sends, 0.2))

    def both(axis, size):
        return [((axis, by), size / rate) for by in BOTH]

    model = rows_i * ROW
    for l in (1, 0):
        for axis in "yz":
            name = ("send_h", l, axis)
            send(name, 20 - l, 58.0, ("norm", l), both(axis, seq * model))
            for i, by in enumerate(BOTH):
                for index in range(PAIR):
                    follow(("pass_h", l, axis, by, index), 10, [(name, i)], [((axis, by), seq * model / SIDE / rate)])
        name = ("send_m", l)
        send(name, 22 - l, ZERO, ("mlp", l), both("x", seq * rows_o) + both("x", PAIR * seq * rows_o))
        for i, by in enumerate(BOTH):
            for index in range(PAIR):
                follow(("pass_m", l, by, index), 11, [(name, i)], [(("x", by), seq * rows_o / PAIR / rate)])
        if l == 0:
            send(("own_y",), 15, ZERO, ("back_norm", 1), [])
            send(("send_scale", l), 15, ZERO, ("back_norm", l), [])
            continue
        name = ("send_y", l)
        send(name, 12, 42.0, None, both("x", seq * model))
        for i, by in enumerate(BOTH):
            follow(("pass_y", l, by), 12, [(name, i)], [(("x", by), seq * model / PAIR / rate)])
        follow(("far_y", l), 12, [(("pass_y", l, by), 0) for by in BOTH], [])
        for axis in "zy":
            name = ("send_z", l, axis)
            share = seq * (cols_i + LANE) / ROW
            send(name, 13, ZERO, ("back_mlp", l) if axis == "z" else ("back_keys", l), both(axis, share / PAIR) + both(axis, share))
            for i, by in enumerate(BOTH):
                follow(("pass_z", l, axis, by), 13, [(name, i)], [((axis, by), share / PAIR / rate)])
                follow(("twin_z", l, axis, by), 14, [(name, PAIR + i)], [])
            follow(("far_z", l, axis), 14, [(("pass_z", l, axis, by), 0) for by in BOTH], [])
        send(("send_scale", l), 15, ZERO, ("back_norm", l), [])
    send(("own_z",), 15, ZERO, ("back_keys", 0), [])
    return plan(tasks)


def gather_stages(links, position, shard_i, shard_o, wi, wo, lsem):
    x, y, z, core = position
    twin = device_at(x, y, z, 1 - core)
    rows_i, cols_i = shard_i.shape[1:]
    rows_o, cols_o = shard_o.shape[1:]
    quarter_i, quarter_o = rows_i // SIDE, rows_o // SIDE
    third_i = cols_i // LANE * SIDE // 9 // PAIR * WIDE
    half_o = cols_o // PAIR
    cut_o = quarter_o // 16 * ROW + ROW if quarter_o % 16 else quarter_o // PAIR
    place = {"x": x, "y": y, "z": z}

    spots = {(axis, o): step(place[axis], o) for axis in "xyz" for o in range(SIDE)}

    def spot(axis, o):
        return spots[axis, o % SIDE]

    table = {}
    for axis in "xyz":
        for o in range(1, SIDE):
            moved = {**place, axis: spot(axis, o)}
            table[axis, o] = device_at(moved["x"], moved["y"], moved["z"], core)

    def peer(axis, o):
        return table[axis, o % SIDE]

    mats = []
    for l in range(PAIR):
        mats.append((shard_i.at[l], wi.at[l], rows_i, True))
        mats.append((shard_o.at[l], wo.at[l], rows_o, False))

    def region(is_in, color, q):
        if is_in:
            if color == "x":
                lo, hi = PAIR * third_i, cols_i
                rows = (0, rows_i)
            else:
                lo, hi = (0, third_i) if color == "y" else (third_i, PAIR * third_i)
                rows = (q * quarter_i, quarter_i)
            mid = lo + ((hi - lo) // LANE + 1) // PAIR * LANE
            return (rows, (lo, hi - lo)), (rows, (lo, mid - lo)), (rows, (mid, hi - mid))
        cols = (0, half_o) if color == "y" else (half_o, half_o)
        start = q * quarter_o
        return ((start, quarter_o), cols), ((start, cut_o), cols), ((start + cut_o, quarter_o - cut_o), cols)

    def at(m, xb, area):
        (r, nr), (c, nc) = area
        _, out, size, _ = mats[m]
        return out.at[pl.ds(pl.multiple_of((PAIR * xb + core) * size + r, ROW), nr), pl.ds(c, nc)]

    def block(m, xb, index):
        _, out, size, _ = mats[m]
        return out.at[pl.ds(pl.multiple_of((PAIR * xb + index) * size, BAND), size)]

    def group(m, color):
        _, out, _, is_in = mats[m]
        (_, nr), (c, nc) = region(is_in, color, 0)[0]
        return dict(batch=(m, color), whole=out.at[pl.ds(0, nr * (3 if color == "x" else 12)), pl.ds(c, nc)])

    def reach(m, color):
        src, _, _, is_in = mats[m]
        area = region(is_in, color, place[color])[0]
        for by in BOTH:
            links.send((m, "x1", color, by), src.at[pl.ds(pl.multiple_of(area[0][0], ROW), area[0][1]), pl.ds(*area[1])], at(m, x, area), peer("x", by), **group(m, color))

    def launch(m, color, off):
        is_in = mats[m][3]
        moved = at(m, spot("x", off), region(is_in, color, place[color])[0])
        for by in BOTH:
            links.send((m, "p1", color, off, by), moved, moved, peer(color, by), **group(m, color))

    def relay(m, color, by):
        is_in = mats[m][3]
        xb = spot("x", -by)
        areas = region(is_in, color, place[color])
        links.arrive((m, "x1", color, by), at(m, xb, areas[0]))
        part = at(m, xb, areas[1] if by == 1 else areas[PAIR])
        links.send((m, "x2", color), part, part, peer("x", by), **group(m, color))
        if color != "x":
            launch(m, color, -by)

    def far(m, color):
        is_in = mats[m][3]
        links.arrive((m, "x2", color), at(m, spot("x", PAIR), region(is_in, color, place[color])[0]))
        if color != "x":
            launch(m, color, PAIR)

    def pass_on(m, color, off, by):
        is_in = mats[m][3]
        xb = spot("x", off)
        areas = region(is_in, color, spot(color, -by))
        links.arrive((m, "p1", color, off, by), at(m, xb, areas[0]))
        part = at(m, xb, areas[1] if by == 1 else areas[PAIR])
        links.send((m, "p2", color, off), part, part, peer(color, by), **group(m, color))

    def close(m, color, off):
        is_in = mats[m][3]
        links.arrive((m, "p2", color, off), at(m, spot("x", off), region(is_in, color, spot(color, PAIR))[0]))

    def four(m):
        _, out, size, _ = mats[m]
        return out.at[pl.ds(0, SIDE * size)]

    def give(m, src, dst):
        links.send((m, "chip"), src, dst, twin, batch=(m, "chip"), whole=four(m))

    def hand(m, off):
        whole = block(m, spot("x", off), core)
        give(m, whole, whole)

    owns = []

    def begin():
        for m, (src, _, _, _) in enumerate(mats):
            copy = pltpu.make_async_copy(src, block(m, x, core), lsem.at[m])
            copy.start()
            owns.append(copy)
            give(m, src, block(m, x, core))

    def ready(m):
        owns[m].wait()
        links.arrive((m, "chip"), four(m))

    return begin, ready, peer, {"reach": reach, "relay": relay, "far": far, "pass": pass_on, "close": close, "hand": hand}


BF, F32 = jnp.bfloat16, jnp.float32


def product(a, b, contract=((1,), (0,))):
    return lax.dot_general(a, b, (contract, ((), ())), preferred_element_type=F32)


def lanes(start, size):
    return pl.ds(start if isinstance(start, int) else pl.multiple_of(start, LANE), size)


def layers_kernel(order, sc_ref, wi_ref, wo_ref, x_ref, dy_ref, freq_ref,
                  y_ref, gx_ref, hy_a, hy_b, hz_a, hz_b, mx_a, mx_b, yx_b, zy_b, zz_b, z_a, dy_a, sc_out, relay_m, relay_z,
                  wi, wo, z, om, h, hid, qr, kts, vsl, ksl, turned_q, turned_o, scores, dscores, pcat, dscat, cos_ref, sin_ref, turn_ref,
                  dot_heads, qt, dht, dkv, omt, ht, dyt, sc, gains, own_gain, gain_ref, load_sems, own_sems, send_sems, recv_sems,
                  share_send_sems, share_recv_sems):
    seq, dim = x_ref.shape
    ff = (wi.shape[PAIR] - dim - LANE) // PAIR
    position = chip_position()
    x, y, zc, core = position
    twin = device_at(x, y, zc, 1 - core)
    me = PAIR * x + core
    links, shared = Links(send_sems, recv_sems), Links(share_send_sems, share_recv_sems)
    stored = []
    spots, _ = around(position)
    h_out, m_out, y_out, z_out = {"y": (hy_a, hy_b), "z": (hz_a, hz_b)}, (mx_a, mx_b), {1: yx_b}, {(1, "y"): zy_b, (1, "z"): zz_b}
    middle = hid.at[1]
    begin, ready, peer, stages = gather_stages(links, position, wi_ref, wo_ref, wi, wo, load_sems)
    others = [(zc * SIDE + y, rem(me + k, ROW)) for k in range(1, ROW)]

    def spot(axis, o):
        return spots[axis, o % SIDE]

    def device(axis, o, index):
        moved = {"x": x, "y": y, "z": zc, axis: spot(axis, o)}
        return device_at(moved["x"], moved["y"], moved["z"], index)

    own_gain[ALL] = jnp.zeros(own_gain.shape, F32)
    count = sc_ref.shape[1]
    for f in range(ROW):
        @pl.when(me == f)
        def _():
            own_gain[0:PAIR, f * count:(f + 1) * count] = sc_ref[ALL].astype(F32)
    announce(others + [device(axis, o, index) for axis in "yz" for o in AROUND for index in range(PAIR)])
    begin()
    for k, far in enumerate(others):
        links.send(("sc",), own_gain, gains.at[me], far, batch=("sc",), whole=gains.at[pl.ds(0, 7)])

    def keep(src, dst):
        copy = pltpu.make_async_copy(src, dst, own_sems.at[len(stored)])
        copy.start()
        stored.append(copy)

    def tokens(axis, o, index):
        return pl.ds(pl.multiple_of((PAIR * spot(axis, o) + index) * seq, seq), seq)

    def columns(axis, o):
        size = z.shape[PAIR] // ROW
        return lanes(((0 if axis == "y" else SIDE) + spot(axis, o)) * size, size)

    def several(batch, ref, n):
        whole = ref.at[pl.ds(0, n * seq)] if batch[0][0] in "yz" else ref.at[(slice(None),) * (len(ref.shape) - 1) + (pl.ds(0, n * seq),)]
        return dict(batch=batch, whole=whole)

    def send_h(l, axis):
        out = h_out[axis][l].at[:, :, tokens(axis, 0, core)]
        for by in BOTH:
            for index in range(PAIR):
                shared.send(("h", l, axis, by), ht.at[l, :, index], out, device(axis, by, index), lane=core, **several(("h", l, axis), h_out[axis][l], 7))
        shared.send(("h", l, axis), ht.at[l, :, 1 - core], out, twin, **several(("h", l, axis), h_out[axis][l], 7))
        keep(ht.at[l, :, core], out)

    def pass_h(l, axis, by, index):
        out = h_out[axis][l]
        shared.arrive(("h", l, axis, by), out.at[:, :, tokens(axis, -by, index)], index)
        part = out.at[pl.ds(1 - by, PAIR), :, tokens(axis, -by, index)]
        shared.send(("h", l, axis), part, part, device(axis, by, core), **several(("h", l, axis), out, 7))

    def arrive_h(l):
        for axis in "yz":
            shared.arrive(("h", l, axis), h_out[axis][l].at[:, :, pl.ds(0, 3 * seq)])

    def row_block(l, o, index, part=None):
        size = omt.shape[1] // ROW
        start = (PAIR * spot("x", o) + index) * size
        if part is not None:
            size = size // PAIR
            start = start + part * size
        return omt.at[l, pl.ds(pl.multiple_of(start, 16), size)]

    def row_half(k):
        size = m_out[0].shape[0] // PAIR
        return pl.ds(k * size, size)

    def send_m(l):
        out = m_out[l].at[:, tokens("x", 0, core)]
        for k, by in enumerate(BOTH):
            for index in range(PAIR):
                shared.send(("mr", l, by), row_block(l, PAIR, index, k), relay_m.at[l, k, core], device("x", by, index), lane=core, **several(("m", l), m_out[l], 7))
        for by in BOTH:
            for index in range(PAIR):
                shared.send(("m", l), row_block(l, by, index), out, device("x", by, index), **several(("m", l), m_out[l], 7))
        shared.send(("m", l), row_block(l, 0, 1 - core), out, twin, **several(("m", l), m_out[l], 7))
        keep(row_block(l, 0, core), out)

    def pass_m(l, by, index):
        k = (1 - by) // PAIR
        shared.arrive(("mr", l, by), relay_m.at[l, k, index], index)
        shared.send(("m", l), relay_m.at[l, k, index], m_out[l].at[row_half(k), tokens("x", -by, index)], device("x", by, core),
                    **several(("m2", l), m_out[l], PAIR))

    def arrive_m(l):
        shared.arrive(("m", l), m_out[l].at[:, pl.ds(0, 7 * seq)])

    def token_half(axis, o, k):
        return pl.ds(pl.multiple_of((PAIR * spot(axis, o) + core) * seq + k * (seq // PAIR), seq // PAIR), seq // PAIR)

    def send_y(l):
        src, out = dy_ref, y_out[l].at[tokens("x", 0, core)]
        for by in BOTH:
            shared.send(("y", l, by), src, out, device("x", by, core), **several(("y", l), y_out[l], 7))
        shared.send(("y", l), src, out, twin, **several(("y", l), y_out[l], 7))
        keep(src, out)

    def pass_y(l, by):
        landed, part = y_out[l].at[tokens("x", -by, core)], y_out[l].at[token_half("x", -by, (1 - by) // PAIR)]
        shared.arrive(("y", l, by), landed)
        shared.send(("y2", l), part, part, device("x", by, core), **several(("y", l), y_out[l], 7))
        shared.send(("y", l), landed, landed, twin, **several(("y", l), y_out[l], 7))

    def far_y(l):
        landed = y_out[l].at[tokens("x", PAIR, core)]
        shared.arrive(("y2", l), landed)
        shared.send(("y", l), landed, landed, twin, **several(("y", l), y_out[l], 7))

    def arrive_y(l):
        shared.arrive(("y", l), y_out[l].at[pl.ds(0, SIDE * seq)])

    def send_z(l, axis):
        out = z_out[l, axis].at[tokens(axis, 0, core)]
        for k, by in enumerate(BOTH):
            shared.send(("zr", l, axis, by), z.at[l, pl.ds(k * (seq // PAIR), seq // PAIR), columns(axis, PAIR)], relay_z.at[l, "yz".index(axis), k],
                        device(axis, by, core), **several(("z", l, axis), z_out[l, axis], ROW))
        for by in BOTH:
            shared.send(("z", l, axis, by), z.at[l, :, columns(axis, by)], out, device(axis, by, core), **several(("z", l, axis), z_out[l, axis], ROW))
        shared.send(("z", l, axis), z.at[l, :, columns(axis, 0)], out, twin, **several(("z", l, axis), z_out[l, axis], ROW))
        keep(z.at[l, :, columns(axis, 0)], out)

    def pass_z(l, axis, by):
        k = (1 - by) // PAIR
        half = relay_z.at[l, "yz".index(axis), k]
        shared.arrive(("zr", l, axis, by), half)
        shared.send(("z2", l, axis), half, z_out[l, axis].at[token_half(axis, -by, k)], device(axis, by, core), **several(("z", l, axis), z_out[l, axis], ROW))

    def twin_z(l, axis, by):
        landed = z_out[l, axis].at[tokens(axis, -by, core)]
        shared.arrive(("z", l, axis, by), landed)
        shared.send(("z", l, axis), landed, landed, twin, **several(("z", l, axis), z_out[l, axis], ROW))

    def far_z(l, axis):
        landed = z_out[l, axis].at[tokens(axis, PAIR, core)]
        shared.arrive(("z2", l, axis), landed)
        shared.send(("z", l, axis), landed, landed, twin, **several(("z", l, axis), z_out[l, axis], ROW))

    def arrive_z(l, axis):
        shared.arrive(("z", l, axis), z_out[l, axis].at[pl.ds(0, SIDE * seq)])

    def send_scale(l):
        for far in others:
            shared.send(("scale", l), sc.at[l], sc_out.at[l, me], far, batch=("scale", l), whole=sc_out.at[l, pl.ds(0, 7)])
        keep(sc.at[l], sc_out.at[l, me])

    def arrive_scale(l):
        shared.arrive(("scale", l), sc_out.at[l, pl.ds(0, 7)])

    gains[me] = own_gain[ALL]
    z[:, :, wi.shape[PAIR]:] = jnp.zeros((PAIR, seq, z.shape[PAIR] - wi.shape[PAIR]), BF)
    entry = (x_ref, hid.at[0])
    angle = lax.broadcasted_iota(jnp.int32, (seq, LANE), 0).astype(F32) * freq_ref[0:1]
    for half in range(PAIR):
        cos_ref[:, LANE * half:LANE * (half + 1)] = jnp.cos(angle)
        sin_ref[:, LANE * half:LANE * (half + 1)] = jnp.sin(angle)
    lane = lax.broadcasted_iota(jnp.int32, turn_ref.shape, 1)
    down = lax.broadcasted_iota(jnp.int32, turn_ref.shape, 0) - lane
    low = rem(lane, HEAD) < BAND
    turn_ref[ALL] = jnp.where(low & (down == BAND), -1.0, jnp.where(jnp.logical_not(low) & (down == -BAND), 1.0, ZERO)).astype(BF)
    kts[ALL] = jnp.zeros(kts.shape, BF)
    pcat[ALL] = jnp.zeros(pcat.shape, BF)
    dscat[ALL] = jnp.zeros(dscat.shape, BF)

    def normalise(l, src):
        @pl.loop(0, seq // BAND, unroll=SIDE)
        def _(r):
            rows = pl.ds(pl.multiple_of(r * BAND, BAND), BAND)
            v = src[rows].astype(F32)
            v = v - jnp.mean(v, axis=-1, keepdims=True)
            var = jnp.mean(v * v, axis=-1, keepdims=True)
            h[l, rows] = (v * lax.rsqrt(var + 1e-6) * gain_ref[l:l + 1]).astype(BF)

    def project(l):
        strip = wi.shape[PAIR] // 5

        @pl.loop(0, 5)
        def _(i):
            at = lanes(i * strip, strip)
            z[l, :, at] = product(h[l], wi[l, :, at]).astype(BF)

    def heads(l):
        cos, sin = cos_ref[ALL], sin_ref[ALL]
        for g in range(dim // WIDE):
            q = z[l, :, g * WIDE:(g + 1) * WIDE]
            qr[l, :, g * WIDE:(g + 1) * WIDE] = ((q.astype(F32) * cos + product(q, turn_ref[ALL]) * sin) * 0.125).astype(BF)
        kv = z[l, :, dim:dim + LANE]
        turned = kv.astype(F32) * cos[:, :LANE] + product(kv, turn_ref[:LANE, :LANE]) * sin[:, :LANE]
        first = lax.broadcasted_iota(jnp.int32, turned.shape, 1) < HEAD
        key_lo = jnp.where(first, turned, ZERO)
        val_hi = jnp.where(first, ZERO, kv.astype(F32))
        return key_lo, pltpu.roll(key_lo, HEAD, 1), pltpu.roll(val_hi, HEAD, 1), val_hi

    def slot_rows(ref, lo, hi):
        zero = jnp.zeros((seq, LANE), BF)
        lo, hi = lo.astype(BF), hi.astype(BF)
        for i, (left, right) in enumerate(((lo, zero), (hi, zero), (zero, lo), (zero, hi))):
            ref[i * seq:(i + 1) * seq, :LANE] = left
            ref[i * seq:(i + 1) * seq, LANE:] = right

    def slot_cols(ref, lo):
        flat = lo.T[:HEAD].astype(BF)
        for i in range(SIDE):
            ref[HEAD * i:HEAD * (i + 1), i * seq:(i + 1) * seq] = flat

    def chances(i, half):
        n, at = LANE * (half + 1), slice(LANE * half, LANE * (half + 1))
        rows = pl.ds(pl.multiple_of(i * seq, seq), n)
        s = scores[rows, at]
        query = lax.broadcasted_iota(jnp.int32, s.shape, 1) + LANE * half
        s = jnp.where(query >= lax.broadcasted_iota(jnp.int32, s.shape, 0), s, -1e30)
        e = jnp.exp(s - jnp.max(s, axis=0, keepdims=True))
        return rows, at, e * (1.0 / jnp.sum(e, axis=0, keepdims=True))

    def attend(l):
        key_lo, key_hi, val_lo, _ = heads(l)
        slot_rows(ksl, key_lo, key_hi)
        slot_cols(kts, val_lo)
        flip(lambda at: qr[l, :, lanes(at, WIDE)], qt, dim)

        @pl.loop(0, dim // WIDE)
        def _(g):
            rows = pl.ds(pl.multiple_of(g * WIDE, WIDE), WIDE)
            scores[ALL] = product(ksl[ALL], qt[rows])

            @pl.loop(0, SIDE)
            def _(i):
                for half in range(PAIR):
                    keys, at, p = chances(i, half)
                    pcat[keys, at] = p.astype(BF)
            flat = product(kts[ALL], pcat[ALL]).astype(BF)
            omt[l, rows] = flat
            om[:, lanes(g * WIDE, WIDE)] = flat.T

    def mlp(l):
        @pl.loop(0, seq // BAND)
        def _(r):
            rows = pl.ds(pl.multiple_of(r * BAND, BAND), BAND)

            @pl.loop(0, ff // STRIP)
            def _(i):
                gate = z[l, rows, lanes(dim + LANE + i * STRIP, STRIP)].astype(F32)
                up = z[l, rows, lanes(dim + LANE + ff + i * STRIP, STRIP)].astype(F32)
                om[rows, lanes(dim + i * STRIP, STRIP)] = (gate * jax.nn.sigmoid(gate) * up).astype(BF)

    def put_out(l, dst):
        for n in range(dim // WIDE):
            cols = slice(n * WIDE, (n + 1) * WIDE)
            total = product(om[ALL], wo[l, :, cols])
            dst[:, cols] = (entry[l][:, cols].astype(F32) + total).astype(BF)

    def flip(src, dst, width, first=0):
        @pl.loop(first // WIDE, width // WIDE)
        def _(i):
            dst[pl.ds(pl.multiple_of(i * WIDE, WIDE), WIDE)] = src(i * WIDE).T

    upstream = (middle, dy_ref)

    def back_out(l):
        dy = upstream[l]
        flip(lambda at: dy[:, lanes(at, WIDE)], dyt, dim)

        @pl.loop(0, wo.shape[1] // dim)
        def _(n):
            rows = pl.ds(pl.multiple_of(n * dim, dim), dim)
            part = product(wo[l, rows], dyt[ALL]).astype(BF)
            om[:, lanes(n * dim, dim)] = part.T

            @pl.when(n == 0)
            def _():
                dot_heads[ALL] = part

    def back_mlp(l):
        @pl.loop(0, seq // BAND)
        def _(r):
            rows = pl.ds(pl.multiple_of(r * BAND, BAND), BAND)

            @pl.loop(0, ff // STRIP)
            def _(i):
                gate_at, up_at = lanes(dim + LANE + i * STRIP, STRIP), lanes(dim + LANE + ff + i * STRIP, STRIP)
                gate, up = z[l, rows, gate_at].astype(F32), z[l, rows, up_at].astype(F32)
                d = om[rows, lanes(dim + i * STRIP, STRIP)].astype(F32)
                sig = jax.nn.sigmoid(gate)
                du = d * up
                z[l, rows, gate_at] = (du * sig + du * gate * (sig * (1.0 - sig))).astype(BF)
                z[l, rows, up_at] = (d * (gate * sig)).astype(BF)

    def back_heads(l):
        key_lo, key_hi, val_lo, val_hi = heads(l)
        slot_rows(ksl, key_lo, key_hi)
        slot_rows(vsl, val_lo, val_hi)
        slot_cols(kts, key_lo)
        dkv[ALL] = jnp.zeros(dkv.shape, F32)
        flip(lambda at: qr[l, :, lanes(at, WIDE)], qt, dim)
        for at in range(0, dim, LANE):
            pair = slice(at, at + LANE)
            turned_q[:, pair] = pltpu.roll(qr[l, :, pair].astype(F32), HEAD, 1).astype(BF)
            turned_o[:, pair] = pltpu.roll(om[:, pair].astype(F32), HEAD, 1).astype(BF)

    def back_quad(l):
        @pl.loop(0, dim // WIDE)
        def _(g):
            quad(l, g)

    def quad(l, g):
        cols = pl.ds(pl.multiple_of(g * WIDE, WIDE), WIDE)
        scores[ALL] = product(ksl[ALL], qt[cols])
        dscores[ALL] = product(vsl[ALL], dot_heads[cols])

        @pl.loop(0, SIDE)
        def _(i):
            for half in range(PAIR):
                keys, at, p = chances(i, half)
                pcat[keys, at] = p.astype(BF)
                pd = p * dscores[keys, at].astype(BF).astype(F32)
                dscat[keys, at] = (pd - p * jnp.sum(pd, axis=0, keepdims=True)).astype(BF)
        dq = product(kts[ALL], dscat[ALL]).astype(BF).T
        back = dq.astype(F32) * cos_ref[ALL] - product(dq, turn_ref[ALL]) * sin_ref[ALL]
        z[l, :, cols] = (back * 0.125).astype(BF)
        for i in range(SIDE):
            keys, pair = slice(i * seq, (i + 1) * seq), lanes(g * WIDE + i // PAIR * LANE, LANE)
            even = i % PAIR == 0
            dkv[0] += product(dscat[keys], qr[l, :, pair] if even else turned_q[:, pair])
            dkv[1] += product(pcat[keys], turned_o[:, pair] if even else om[:, pair])

    def back_keys(l):
        dk = dkv[0].astype(BF)
        turned = dk.astype(F32) * cos_ref[:, :LANE] - product(dk, turn_ref[:LANE, :LANE]) * sin_ref[:, :LANE]
        first = lax.broadcasted_iota(jnp.int32, turned.shape, 1) < HEAD
        z[l, :, dim:dim + LANE] = jnp.where(first, turned, dkv[1]).astype(BF)

    def back_in(l, half):
        width = wi.shape[PAIR] // 5
        at = slice(PAIR * half * width, (PAIR + 3 * half) * width)
        part = product(wi[l, :, at], z[l, :, at], ((1,), (1,)))
        dht[ALL] = dht[ALL] + part if half else part

    def back_norm(l):
        dy, dst = upstream[l], (gx_ref, middle)[l]
        for i in range(dim // WIDE):
            cols = slice(i * WIDE, (i + 1) * WIDE)
            h[l, :, cols] = dht[cols].T.astype(BF)
        sc[l] = jnp.zeros(sc.shape[1:], F32)

        @pl.loop(0, seq // BAND, unroll=SIDE)
        def _(r):
            rows = pl.ds(pl.multiple_of(r * BAND, BAND), BAND)
            v = entry[l][rows].astype(F32)
            v = v - jnp.mean(v, axis=-1, keepdims=True)
            scale = lax.rsqrt(jnp.mean(v * v, axis=-1, keepdims=True) + 1e-6)
            hat = v * scale
            d = h[l, rows].astype(F32)
            each = (d * hat).reshape(SIDE, ROW, dim)
            sc[l] += (each[0] + each[1]) + (each[PAIR] + each[3])
            d = d * gain_ref[l:l + 1]
            d = scale * (d - jnp.mean(d, axis=-1, keepdims=True) - hat * jnp.mean(d * hat, axis=-1, keepdims=True))
            dst[rows] = (dy[rows].astype(F32) + d.astype(BF).astype(F32)).astype(BF)

    def do_norm(l):
        if l == 0:
            links.arrive(("sc",), gains.at[pl.ds(0, 7)])
            gain_ref[ALL] = jnp.sum(gains[ALL], axis=0)
        normalise(l, entry[l])
        for i in range(dim // WIDE):
            flat = h[l, :, i * WIDE:(i + 1) * WIDE].T
            size = ht.shape[3]
            for b in range(ROW):
                lo, hi = max(b * size, i * WIDE), min((b + 1) * size, (i + 1) * WIDE)
                if lo < hi:
                    ht[l, b // PAIR, b % PAIR, lo - b * size:hi - b * size] = flat[lo - i * WIDE:hi - i * WIDE]

    def do_project(l):
        ready(PAIR * l)
        project(l)

    def do_mlp(l):
        mlp(l)
        flip(lambda at: om[:, lanes(at, WIDE)], omt.at[l], om.shape[1], dim)

    def do_put(l):
        ready(PAIR * l + 1)
        put_out(l, hid.at[0] if l == 0 else y_ref)

    stages.update(
        norm=do_norm, project=do_project, attend=attend, mlp=do_mlp, put=do_put, back_out=back_out, back_mlp=back_mlp, back_heads=back_heads,
        back_quad=back_quad, back_keys=back_keys, back_in=back_in, back_norm=back_norm, send_h=send_h, pass_h=pass_h, send_m=send_m,
        pass_m=pass_m, send_y=send_y, pass_y=pass_y, far_y=far_y, send_z=send_z, pass_z=pass_z, twin_z=twin_z, far_z=far_z,
        send_scale=send_scale, own_z=lambda: keep(z.at[0], z_a), own_y=lambda: keep(middle, dy_a))
    for kind, *task in order:
        stages[kind](*task)
    for l in range(PAIR):
        arrive_h(l)
        arrive_m(l)
        arrive_scale(l)
    arrive_y(1)
    for l, axis in z_out:
        arrive_z(l, axis)
    for copy in stored:
        copy.wait()
    shared.drain()
    links.drain()


def run_layers(x, dy, scale, w_in, w_out, freq, starts=(ZERO, 10.0, 20.0, 30.0)):
    seq, dim = x.shape
    proj, cat = w_in.shape[PAIR], ROW * w_out.shape[1]
    wide = proj + LANE
    hbm, vmem = pl.BlockSpec(memory_space=pltpu.HBM), pl.BlockSpec(memory_space=pltpu.VMEM)
    out = lambda *shape, dtype=BF: jax.ShapeDtypeStruct(shape, dtype)
    buffer = lambda *shape, dtype=BF: pltpu.VMEM(shape, dtype)
    sem = pltpu.SemaphoreType.DMA
    line = ROW * seq
    return pl.pallas_call(
        functools.partial(layers_kernel, layers_order(*w_in.shape[1:], *w_out.shape[1:], seq, starts)),
        out_shape=(out(seq, dim), out(seq, dim), *[out(SIDE, dim // ROW, line)] * SIDE, *[out(cat // ROW, line)] * PAIR, out(line, dim),
                   *[out(line, wide // ROW)] * PAIR, out(seq, wide), out(seq, dim), out(PAIR, ROW, ROW, dim, dtype=F32),
                   out(PAIR, PAIR, PAIR, cat // 16, seq), out(PAIR, PAIR, PAIR, seq // PAIR, wide // ROW)),
        in_specs=[vmem, hbm, hbm] + [vmem] * 3,
        out_specs=[vmem] * PAIR + [hbm] * 14,
        scratch_shapes=[
            buffer(PAIR, dim, proj), buffer(PAIR, cat, dim), buffer(PAIR, seq, wide), buffer(seq, cat), buffer(PAIR, seq, dim),
            buffer(PAIR, seq, dim), buffer(PAIR, seq, dim),
            buffer(WIDE, SIDE * seq), buffer(SIDE * seq, WIDE), buffer(SIDE * seq, WIDE), buffer(seq, dim), buffer(seq, dim),
            buffer(SIDE * seq, seq, dtype=F32), buffer(SIDE * seq, seq, dtype=F32), buffer(SIDE * seq, seq), buffer(SIDE * seq, seq),
            buffer(seq, WIDE, dtype=F32), buffer(seq, WIDE, dtype=F32), buffer(WIDE, WIDE),
            buffer(dim, seq), buffer(dim, seq), buffer(dim, seq, dtype=F32), buffer(PAIR, seq, LANE, dtype=F32),
            buffer(PAIR, cat, seq), buffer(PAIR, SIDE, PAIR, dim // ROW, seq), buffer(dim, seq), buffer(PAIR, ROW, dim, dtype=F32),
            buffer(ROW, ROW, dim, dtype=F32), buffer(ROW, dim, dtype=F32), buffer(ROW, dim, dtype=F32),
            sem((SIDE,)), sem((13,)), sem((15,)), sem((107,)), sem((13,)), sem((HEAD,)),
        ],
        compiler_params=pltpu.CompilerParams(collective_id=PAIR, has_side_effects=True, vmem_limit_bytes=67043328),
        name="run_layers",
    )(scale, w_in, w_out, x, dy, freq)


PARTS = (("i", "x", "z", "y", 0, STRIP), ("i", "x", "z", "y", STRIP, 384), ("i", "x", "y", "z", 0, STRIP), ("i", "x", "y", "z", STRIP, 384),
         ("o", "y", "z", "y", 0, 384), ("o", "z", "y", "z", 384, 384))


def reduce_order(rows, rows_b, starts):
    rate = 11650.0
    tasks = []
    sizes = {"y": WIDE * 896 / (PAIR * rate), "z": WIDE * 896 / (PAIR * rate), "x": WIDE * 768 / (PAIR * rate)}
    for axis in "yzx":
        tasks.append((("swap", axis), (0, 0), starts[PAIR] if axis == "x" else ZERO, [], [], [((axis, by), sizes[axis] * n) for by, n in ((1, 1), (-1, 1), (1, PAIR))], 0.3))
        for i, o in enumerate(AROUND):
            tasks.append((("near", axis, o), (0, PAIR), ZERO, [(("swap", axis), i)], [], [("chip", 1.6)], 0.2))
    tasks.append((("fetch", 0), (5, 0), ZERO, [], [("make", 1, len(PARTS) - 1)], [], 0.2))
    for l in (1, 0):
        late = 1 - l
        for c, (kind, first, then, last, at, width) in enumerate(PARTS):
            needs, cost = [], 1.6 * width / STRIP
            if l == 0:
                needs = [(("near", last if kind == "i" else "x", o), 0) for o in AROUND]
            tasks.append((("make", l, c), (9 * late, c), starts[late], needs, [] if l else [("fetch", 0)], [], cost))
            full = SIDE * SIDE * (rows if kind == "i" else rows_b) * width / rate
            sends = [[((first, by), full / ROW) for by in BOTH], [((first, by), full / SIDE) for by in BOTH],
                     [((then, o), full / 16) for o in (1, -1, 1)], []]
            piece = full / 16
            sends += [[((then, by), piece) for by in BOTH], [((then, 1 - PAIR * (c % PAIR)), piece)], [((last, by), SIDE * piece) for by in BOTH],
                      [((last, by), PAIR * piece) for by in BOTH], []]
            for s in range(9):
                task = ("sum", l, c, s)
                needs = [(("sum", l, c, s - 1), k) for k in range(len(sends[s - 1]))] if s else []
                tasks.append((task, (late, -s), ZERO, needs, [("make", l, c)] if s == 0 else [("sum", l, c, s - 1)], sends[s], 0.3))
    return plan(tasks)


def reduce_kernel(order, *refs):
    hy, hz, mx = refs[0:PAIR], refs[PAIR:SIDE], refs[SIDE:6]
    yx1, zy1, zz1, z0, y0, sc = refs[6:12]
    oa, ob = refs[12:14]
    n = len(PARTS)
    total, half, full, small, front = (refs[14 + k * n:14 + (k + 1) * n] for k in range(5))
    (hbuf, zbuf, mbuf, ybuf, scbuf, ssem, rsem, isem, osem) = refs[14 + 5 * n:]
    position = chip_position()
    x, y, zc, core = position
    place = {"x": x, "y": y, "z": zc}
    twin = device_at(x, y, zc, 1 - core)
    spots, peers = around(position)

    def spot(axis, o):
        return spots[axis, o % SIDE]

    def peer(axis, o):
        return peers[axis, o % SIDE]

    seq, wide = z0.shape
    own = wide // ROW
    loads, moving = {}, []

    def load(key, src, dst):
        copy = pltpu.make_async_copy(src, dst, isem.at[len(moving)])
        moving.append(key)
        copy.start()
        loads[key] = copy

    def fetch(l):
        if l:
            load(("z", 1, "y"), zy1, zbuf.at[1, 0])
        load(("h", l, "y"), hy[l], hbuf.at[l, 0])
        if l:
            load(("z", 1, "z"), zz1, zbuf.at[1, 1])
        load(("h", l, "z"), hz[l], hbuf.at[l, 1])
        load(("m", l), mx[l], mbuf.at[l])
        if l:
            load(("y", 1), yx1, ybuf.at[1])
        load(("s", l), sc.at[l], scbuf.at[l])

    fetch(1)
    done = set()

    def loaded(*keys):
        for key in keys:
            if key not in done:
                loads[key].wait()
                done.add(key)

    announce([peer(axis, o) for axis in "xyz" for o in AROUND] + [twin])
    links = Links(ssem, rsem)

    def columns(axis, o):
        return lanes(((0 if axis == "y" else SIDE) + spot(axis, o)) * own, own)

    def tokens(axis, o, index):
        return pl.ds(pl.multiple_of((PAIR * spot(axis, o) + index) * seq, seq), seq)

    def target(axis):
        return ybuf.at[0] if axis == "x" else zbuf.at[0, "yz".index(axis)]

    def seven(axis):
        return dict(batch=("swap", axis), whole=target(axis).at[pl.ds(0, 7 * seq)])

    def swap(axis):
        def part(o):
            return y0 if axis == "x" else z0.at[:, columns(axis, o)]

        mine = target(axis).at[tokens(axis, 0, core)]
        for o in AROUND:
            links.send(("swap", axis, o), part(o), mine, peer(axis, o), **seven(axis))
        links.send(("near", axis), part(0), mine, twin, **seven(axis))
        load(("own", axis), part(0), mine)

    def near(axis, o):
        landed = target(axis).at[tokens(axis, -o, core)]
        links.arrive(("swap", axis, o), landed)
        links.send(("near", axis), landed, landed, twin, **seven(axis))

    def joined(axis):
        if axis not in done:
            done.add(axis)
            loaded(("own", axis))
            links.arrive(("near", axis), target(axis).at[pl.ds(0, SIDE * seq)])

    def make(l, c):
        kind, first, then, last, at, width = PARTS[c]
        if kind == "i":
            i = "yz".index(last)
            loaded(("h", l, last))
            if l:
                loaded(("z", l, last))
            else:
                joined(last)
            size = total[c].shape[3]
            for lo in range(0, width, WIDE):
                hi = min(width, lo + WIDE)
                part = product(hbuf[l, i].reshape(-1, hbuf.shape[-1]), zbuf[l, i, :, at + lo:at + hi])
                for r in range(16):
                    total[c][l, r // SIDE, r % SIDE, :, lo:hi] = part[r * size:(r + 1) * size]
            return
        loaded(("m", l), ("s", l))
        if l:
            loaded(("y", l))
        else:
            joined("x")
        part = product(mbuf[l], ybuf[l, :, at:at + width])
        size = total[c].shape[3]

        def put(r, value):
            total[c][(l, r // SIDE, r % SIDE) if first == "y" else (l, r % SIDE, r // SIDE)] = value

        for r in range(part.shape[0] // size):
            put(r, part[r * size:(r + 1) * size])
        gain = jnp.sum(jnp.sum(scbuf[l, :, :, at:at + width], axis=0), axis=0, keepdims=True)
        row = lax.broadcasted_iota(jnp.int32, (size, width), 0)
        put(15, jnp.where(row == 0, gain, ZERO))

    def area(l, c, o, whole):
        kind, first, then, last, at, width = PARTS[c]
        inner = (spot(then, whole) if isinstance(whole, int) else whole)
        outer = spot(last, o)
        if kind == "i":
            cols = lanes(((0 if last == "y" else SIDE) + outer) * own + at, width)
            return oa.at[l, inner, :, cols]
        cols = pl.ds(at, width)
        return ob.at[l, outer, inner, :, cols] if last == "y" else ob.at[l, inner, outer, :, cols]

    def add(l, c, s):
        kind, first, then, last, at, width = PARTS[c]
        t = total[c].at[l]
        way = 1 - PAIR * (c % PAIR)
        sums = dict(batch=(l, c, 0), whole=t)
        wide_ones = dict(batch=(l, c, 1), whole=t.at[pl.ds(0, 3)])
        narrow = dict(batch=(l, c, PAIR), whole=t.at[0, pl.ds(0, PAIR)])
        if s == 0:
            far = t.at[spot(first, PAIR)]
            for k, by in enumerate(BOTH):
                links.send((l, c, "half"), far.at[pl.ds(PAIR * k, PAIR)], half[c].at[l, k], peer(first, by), **sums)
        elif s == 1:
            links.arrive((l, c, "half"), half[c].at[l])
            for k, by in enumerate(BOTH):
                mine = t.at[spot(first, by)]
                add_into(mine.at[pl.ds(PAIR * k, PAIR)], half[c].at[l, k])
                links.send((l, c, "full"), mine, full[c].at[l, k], peer(first, by), **sums)
        elif s == PAIR:
            mine = t.at[spot(first, 0)]
            links.arrive((l, c, "full"), full[c].at[l])
            for k in range(PAIR):
                add_into(mine, full[c].at[l, k])
            for k, o in enumerate(AROUND):
                links.send((l, c, "small"), mine.at[spot(then, o)], small[c].at[l, k], peer(then, o), **wide_ones)
        elif s == 3:
            links.arrive((l, c, "small"), small[c].at[l])
            mine = t.at[spot(first, 0), spot(then, 0)]
            front[c][l] = (mine[ALL] + small[c][l, 0]) + (small[c][l, 1] + small[c][l, PAIR])
        elif s == SIDE:
            src, dst = front[c].at[l], area(l, c, 0, 0)
            for by in BOTH:
                links.send((l, c, "a1"), src, dst, peer(then, by), **narrow)
            copy = pltpu.make_async_copy(src, dst, osem.at[l, c])
            copy.start()
            loads["front", l, c] = copy
        elif s == 5:
            links.arrive((l, c, "a1"), t.at[0, pl.ds(0, PAIR)])
            landed = area(l, c, 0, -way)
            links.send((l, c, "b1"), landed, landed, peer(then, way), **wide_ones)
        elif s == 6:
            loaded(("front", l, c))
            links.arrive((l, c, "b1"), area(l, c, 0, PAIR))
            line = area(l, c, 0, slice(None))
            for by in BOTH:
                links.send((l, c, "a2"), line, line, peer(last, by), **wide_ones)
        elif s == 7:
            links.arrive((l, c, "a2"), t.at[pl.ds(0, PAIR)])
            for k, by in enumerate(BOTH):
                part = area(l, c, -by, pl.ds(PAIR * k, PAIR))
                links.send((l, c, "a3"), part, part, peer(last, by), **sums)
        else:
            links.arrive((l, c, "a3"), area(l, c, PAIR, slice(None)))

    stages = {"swap": swap, "near": near, "fetch": fetch, "make": make, "sum": add}
    for kind, *task in order:
        stages[kind](*task)
    links.drain()


def add_into(dst, src):
    @pl.loop(0, dst.shape[0])
    def _(i):
        if len(dst.shape) == SIDE:
            for j in range(dst.shape[1]):
                dst[i, j] += src[i, j]
        else:
            dst[i] += src[i]


def around(position):
    place, core = dict(zip("xyz", position)), position[3]
    spots = {(axis, o): step(place[axis], o) for axis in "xyz" for o in range(SIDE)}
    peers = {}
    for axis in "xyz":
        for o in range(1, SIDE):
            moved = {**place, axis: spots[axis, o]}
            peers[axis, o] = device_at(moved["x"], moved["y"], moved["z"], core)
    return spots, peers


def reduce_gradients(operands, starts=(ZERO, ZERO, ZERO)):
    hbm = pl.BlockSpec(memory_space=pltpu.HBM)
    h_rows, m_rows, y_cols, z_cols, z_own, y_own, scale_parts = operands
    part, part_b = h_rows[0].shape[1] // SIDE, (m_rows[0].shape[0] + BAND) // 16
    (line, dim), wide = y_cols.shape, z_own.shape[1]
    out = lambda *shape: jax.ShapeDtypeStruct(shape, F32)
    sem = pltpu.SemaphoreType.DMA

    def buffers(*lead):
        return [pltpu.VMEM((PAIR, *lead, part if e[0] == "i" else part_b, e[5]), F32) for e in PARTS]

    return pl.pallas_call(
        functools.partial(reduce_kernel, reduce_order(part, part_b, starts)),
        out_shape=(out(PAIR, SIDE, part, wide), out(PAIR, SIDE, SIDE, part_b, dim)),
        in_specs=[hbm] * 12,
        out_specs=[hbm] * PAIR,
        scratch_shapes=[
            *buffers(SIDE, SIDE), *buffers(PAIR, PAIR), *buffers(PAIR, SIDE), *buffers(3), *buffers(),
            pltpu.VMEM((PAIR, PAIR, *h_rows[0].shape), BF), pltpu.VMEM((PAIR, PAIR, line, wide // ROW), BF), pltpu.VMEM((PAIR, *m_rows[0].shape), BF),
            pltpu.VMEM((PAIR, line, dim), BF), pltpu.VMEM(scale_parts.shape, F32),
            sem((39,)), sem((96,)), sem((14,)), sem((PAIR, len(PARTS))),
        ],
        compiler_params=pltpu.CompilerParams(collective_id=1, has_side_effects=True, vmem_limit_bytes=67043328),
        name="reduce_gradients",
    )(*h_rows, *m_rows, y_cols, *z_cols, z_own, y_own, scale_parts)


def solution(mesh):
    fsdp_size = mesh.shape["fsdp"]
    batch_spec = P(("dp", "fsdp"), None, None)
    scale_spec = P(None, "fsdp")
    weight_spec = P(None, "fsdp", None)

    def device_step(x_in, grad_y, norm_scale, w_in, w_out):
        n_layers = w_in.shape[0]
        seq_len, model_dim = x_in.shape[1:]
        proj_dim = w_in.shape[PAIR]
        ff_dim = w_out.shape[1] * fsdp_size - model_dim
        head_dim = (proj_dim - model_dim - PAIR * ff_dim) // PAIR
        rows, rows_out = norm_scale.shape[1], w_out.shape[1]
        half_dim = head_dim // PAIR
        freq = 10000.0 ** (-np.arange(half_dim, dtype=np.float32) * 2.0 / head_dim)
        freq = jnp.asarray(np.tile(freq.astype(np.float32), (ROW, LANE // half_dim)))
        hidden, grad_hidden, *rest = run_layers(x_in[0], grad_y[0], norm_scale, w_in, w_out, freq)
        in_sums, out_sums = reduce_gradients((rest[0:SIDE], rest[SIDE:6], rest[6], rest[7:9], rest[9], rest[10], rest[11]))
        in_grads = in_sums.reshape(n_layers, rows, -1)[:, :, :proj_dim]
        out_rows = out_sums.reshape(n_layers, -1, model_dim)
        scale_grads = lax.dynamic_slice(out_rows[:, rows_out], (0, lax.axis_index("fsdp") * rows), (n_layers, rows))
        out_grads = out_rows[:, :rows_out]
        return hidden[None], grad_hidden[None], scale_grads, in_grads, out_grads

    return jax.shard_map(
        device_step,
        mesh=mesh,
        in_specs=(batch_spec, batch_spec, scale_spec, weight_spec, weight_spec),
        out_specs=(batch_spec, batch_spec, scale_spec, weight_spec, weight_spec),
        check_vma=False,
    )
```

```python
import functools
import jax
import jax.numpy as jnp
import numpy as np
from jax import lax
from jax.experimental import pallas as pl
from jax.experimental.pallas import tpu as pltpu
from jax.sharding import PartitionSpec as P

MESH_ID = pl.DeviceIdType.MESH
BOTH = (1, -1)
AROUND = (1, -1, 2)
PARTS = (True, False)
ALL, ZERO = ..., 0.0
LANE, WIDE, STRIP, HEAD = 128, 256, 512, 64
ROW, BAND, SIDE, PAIR = 8, 32, 4, 2


class Links:
    def __init__(self, send_sems, recv_sems):
        self.send_sems, self.recv_sems = send_sems, recv_sems
        self.slots, self.batches, self.sent, self.count = {}, {}, {}, 0

    def _landing(self, key, lane):
        if key not in self.slots:
            self.slots[key] = self.count
            self.count += 1 if lane is None else PAIR
        return self.recv_sems.at[self.slots[key] + (0 if lane is None else lane)]

    def send(self, key, src, dst, device, landing=None, whole=None, batch=None, lane=None):
        leaving = self.batches.setdefault(batch or key, len(self.batches))
        copy = pltpu.make_async_remote_copy(
            src_ref=src, dst_ref=dst, send_sem=self.send_sems.at[leaving], recv_sem=self._landing(landing or key, lane),
            device_id=device, device_id_type=MESH_ID)
        copy.start()
        self.sent[batch or key] = (src if whole is None else whole, leaving)

    def arrive(self, key, landed, lane=None):
        pltpu.make_async_copy(landed, landed, self._landing(key, lane)).wait()

    def drain(self):
        for left, leaving in self.sent.values():
            pltpu.make_async_copy(left, left, self.send_sems.at[leaving]).wait()
        self.sent.clear()


def rem(a, n):
    return a % n if isinstance(a, int) else lax.rem(a, n)


def chip_position():
    f, d = lax.axis_index("fsdp"), lax.axis_index("dp")
    return f // PAIR, rem(d, SIDE), d // SIDE, rem(f, PAIR)


def device_at(x, y, z, core):
    return (z * SIDE + y, x * PAIR + core)


def step(coord, by):
    return rem(coord + SIDE + by, SIDE)


def announce(devices):
    barrier = pltpu.get_barrier_semaphore()
    for device in devices:
        pl.semaphore_signal(barrier, inc=1, device_id=device, device_id_type=MESH_ID)
    pl.semaphore_wait(barrier, len(devices))


def plan(tasks, latency=2.5):
    free, landed, order, now = {}, {}, [], ZERO
    left = list(tasks)
    while left:
        best = None
        for place, (name, rank, start, needs, after, _, _) in enumerate(left):
            if all(n[0] in landed for n in needs) and all(n in landed for n in after):
                ready = max([start, now] + [landed[task][i] for task, i in needs])
                best = min(best or (ready, rank, place), (ready, rank, place))
        now, _, place = best
        name, _, _, _, _, sends, cost = left.pop(place)
        order.append(name)
        now += cost
        landed[name] = []
        for link, time in sends:
            free[link] = max(now, free.get(link, ZERO)) + time
            landed[name].append(free[link] + latency)
    return order


def layers_order(rows_i, cols_i, rows_o, cols_o, seq, starts):
    rate = 23300.0
    tasks = []
    for m in range(SIDE):
        is_in = m % PAIR == 0
        edge = cols_i // LANE * SIDE // 9 // PAIR * WIDE
        size = {"y": rows_i // SIDE * edge, "x": rows_i * (cols_i - PAIR * edge)} if is_in else {"y": rows_o // SIDE * cols_o // PAIR}
        size["z"] = size["y"]
        colors = "yzx" if is_in else "yz"
        for color in colors:
            cost = size[color] / rate
            both = [(("x", by), cost) for by in BOTH]
            spread = [((color, by), cost) for by in BOTH] if color != "x" else []
            tasks.append((("reach", m, color), m, starts[m], [], [], both, 0.2))
            for i, by in enumerate(BOTH):
                tasks.append((("relay", m, color, by), m, ZERO, [(("reach", m, color), i)], [], [(("x", by), cost / PAIR)] + spread, 0.2))
            halves = [(("relay", m, color, by), 0) for by in BOTH]
            tasks.append((("far", m, color), m, ZERO, halves, [], spread, 0.2))
            if color == "x":
                continue
            for off, source, first in ((-1, ("relay", m, color, 1), 1), (1, ("relay", m, color, -1), 1), (PAIR, ("far", m, color), 0)):
                for i, by in enumerate(BOTH):
                    tasks.append((("pass", m, color, off, by), m, ZERO, [(source, first + i)], [], [((color, by), cost / PAIR)], 0.2))
                halves = [(("pass", m, color, off, by), 0) for by in BOTH]
                tasks.append((("close", m, color, off), m, ZERO, halves, [], [], 0.2))
        for color in colors:
            part = size[color] * (1 if color == "x" else SIDE)
            for off in (-1, 1, PAIR):
                last = (("far", m, "x") if off == PAIR else ("relay", m, "x", -off)) if color == "x" else ("close", m, color, off)
                tasks.append((("hand", m, color, off), m, ZERO, [], [last], [("chip", part / 150000.0)], 0.2))
    before = []

    def work(name, cost, mats=()):
        needs = [(("hand", m, color, off), 0) for m in mats for color in ("yz" if m % PAIR else "yzx") for off in (-1, 1, PAIR)]
        tasks.append((name, 99, ZERO, needs, list(before), [], cost))
        before[:] = [name]

    for l in range(PAIR):
        work(("norm", l), 0.8)
        work(("project", l), 4.0, [PAIR * l])
        work(("attend", l), 4.2)
        work(("mlp", l), 2.2)
        work(("put", l), 1.6, [PAIR * l + 1])
    for l in (1, 0):
        work(("back_out", l), 2.9)
        work(("back_mlp", l), 2.0)
        work(("back_heads", l), 1.0)
        work(("back_quad", l), 6.0)
        work(("back_keys", l), 0.2)
        for i in range(PAIR):
            work(("back_in", l, i), 1.3 + 0.6 * i)
        work(("back_norm", l), 1.0)
    def send(name, rank, start, after, sends):
        tasks.append((name, rank, start, [], [after] if after else [], sends, 0.4))

    def follow(name, rank, needs, sends):
        tasks.append((name, rank, ZERO, needs, [], sends, 0.2))

    def both(axis, size):
        return [((axis, by), size / rate) for by in BOTH]

    model = rows_i * ROW
    for l in (1, 0):
        for axis in "yz":
            name = ("send_h", l, axis)
            send(name, 20 - l, 58.0, ("norm", l), both(axis, seq * model))
            for i, by in enumerate(BOTH):
                for index in range(PAIR):
                    follow(("pass_h", l, axis, by, index), 10, [(name, i)], [((axis, by), seq * model / SIDE / rate)])
        name = ("send_m", l)
        send(name, 22 - l, ZERO, ("mlp", l), both("x", seq * rows_o) + both("x", PAIR * seq * rows_o))
        for i, by in enumerate(BOTH):
            for index in range(PAIR):
                follow(("pass_m", l, by, index), 11, [(name, i)], [(("x", by), seq * rows_o / PAIR / rate)])
        if l == 0:
            send(("own_y",), 15, ZERO, ("back_norm", 1), [])
            send(("send_scale", l), 15, ZERO, ("back_norm", l), [])
            continue
        name = ("send_y", l)
        send(name, 12, 42.0, None, both("x", seq * model))
        for i, by in enumerate(BOTH):
            follow(("pass_y", l, by), 12, [(name, i)], [(("x", by), seq * model / PAIR / rate)])
        follow(("far_y", l), 12, [(("pass_y", l, by), 0) for by in BOTH], [])
        for axis in "zy":
            name = ("send_z", l, axis)
            share = seq * (cols_i + LANE) / ROW
            send(name, 13, ZERO, ("back_mlp", l), both(axis, share / PAIR) + both(axis, share))
            if axis == "y":
                name = ("rest_z", l)
                send(name, 13, ZERO, ("back_keys", l), both(axis, share / ROW) + both(axis, share / SIDE))
            for i, by in enumerate(BOTH):
                follow(("pass_z", l, axis, by), 13, [(name, i)], [((axis, by), share / PAIR / rate)])
                follow(("twin_z", l, axis, by), 14, [(name, PAIR + i)], [])
            follow(("far_z", l, axis), 14, [(("pass_z", l, axis, by), 0) for by in BOTH], [])
        send(("send_scale", l), 15, ZERO, ("back_norm", l), [])
    send(("own_z",), 15, ZERO, ("back_keys", 0), [])
    return plan(tasks)


def gather_stages(links, position, shard_i, shard_o, wi, wo, lsem):
    x, y, z, core = position
    twin = device_at(x, y, z, 1 - core)
    rows_i, cols_i = shard_i.shape[1:]
    rows_o, cols_o = shard_o.shape[1:]
    quarter_i, quarter_o = rows_i // SIDE, rows_o // SIDE
    third_i = cols_i // LANE * SIDE // 9 // PAIR * WIDE
    half_o = cols_o // PAIR
    cut_o = quarter_o // 16 * ROW + ROW if quarter_o % 16 else quarter_o // PAIR
    place = {"x": x, "y": y, "z": z}

    spots = {(axis, o): step(place[axis], o) for axis in "xyz" for o in range(SIDE)}

    def spot(axis, o):
        return spots[axis, o % SIDE]

    table = {}
    for axis in "xyz":
        for o in range(1, SIDE):
            moved = {**place, axis: spot(axis, o)}
            table[axis, o] = device_at(moved["x"], moved["y"], moved["z"], core)

    def peer(axis, o):
        return table[axis, o % SIDE]

    mats = []
    for l in range(PAIR):
        mats.append((shard_i.at[l], wi.at[l], rows_i, True))
        mats.append((shard_o.at[l], wo.at[l], rows_o, False))

    def region(is_in, color, q):
        if is_in:
            if color == "x":
                lo, hi = PAIR * third_i, cols_i
                rows = (0, rows_i)
            else:
                lo, hi = (0, third_i) if color == "y" else (third_i, PAIR * third_i)
                rows = (q * quarter_i, quarter_i)
            mid = lo + ((hi - lo) // LANE + 1) // PAIR * LANE
            return (rows, (lo, hi - lo)), (rows, (lo, mid - lo)), (rows, (mid, hi - mid))
        cols = (0, half_o) if color == "y" else (half_o, half_o)
        start = q * quarter_o
        return ((start, quarter_o), cols), ((start, cut_o), cols), ((start + cut_o, quarter_o - cut_o), cols)

    def at(m, xb, area):
        (r, nr), (c, nc) = area
        _, out, size, _ = mats[m]
        return out.at[pl.ds(pl.multiple_of((PAIR * xb + core) * size + r, ROW), nr), pl.ds(c, nc)]

    def block(m, xb, index):
        _, out, size, _ = mats[m]
        return out.at[pl.ds(pl.multiple_of((PAIR * xb + index) * size, BAND), size)]

    def group(m, color):
        _, out, _, is_in = mats[m]
        (_, nr), (c, nc) = region(is_in, color, 0)[0]
        return dict(batch=(m, color), whole=out.at[pl.ds(0, nr * (3 if color == "x" else 12)), pl.ds(c, nc)])

    def reach(m, color):
        src, _, _, is_in = mats[m]
        area = region(is_in, color, place[color])[0]
        for by in BOTH:
            links.send((m, "x1", color, by), src.at[pl.ds(pl.multiple_of(area[0][0], ROW), area[0][1]), pl.ds(*area[1])], at(m, x, area), peer("x", by), **group(m, color))

    def launch(m, color, off):
        is_in = mats[m][3]
        moved = at(m, spot("x", off), region(is_in, color, place[color])[0])
        for by in BOTH:
            links.send((m, "p1", color, off, by), moved, moved, peer(color, by), **group(m, color))

    def relay(m, color, by):
        is_in = mats[m][3]
        xb = spot("x", -by)
        areas = region(is_in, color, place[color])
        links.arrive((m, "x1", color, by), at(m, xb, areas[0]))
        part = at(m, xb, areas[1] if by == 1 else areas[PAIR])
        links.send((m, "x2", color), part, part, peer("x", by), **group(m, color))
        if color != "x":
            launch(m, color, -by)

    def far(m, color):
        is_in = mats[m][3]
        links.arrive((m, "x2", color), at(m, spot("x", PAIR), region(is_in, color, place[color])[0]))
        if color != "x":
            launch(m, color, PAIR)

    def pass_on(m, color, off, by):
        is_in = mats[m][3]
        xb = spot("x", off)
        areas = region(is_in, color, spot(color, -by))
        links.arrive((m, "p1", color, off, by), at(m, xb, areas[0]))
        part = at(m, xb, areas[1] if by == 1 else areas[PAIR])
        links.send((m, "p2", color, off), part, part, peer(color, by), **group(m, color))

    def close(m, color, off):
        is_in = mats[m][3]
        links.arrive((m, "p2", color, off), at(m, spot("x", off), region(is_in, color, spot(color, PAIR))[0]))

    def four(m):
        _, out, size, _ = mats[m]
        return out.at[pl.ds(0, SIDE * size)]

    def give(m, src, dst):
        links.send((m, "chip"), src, dst, twin, batch=(m, "chip"), whole=four(m))

    def hand(m, color, off):
        _, out, size, is_in = mats[m]
        _, (c, nc) = region(is_in, color, 0)[0]
        rows = pl.ds(pl.multiple_of((PAIR * spot("x", off) + core) * size, BAND), size)
        part = out.at[rows, pl.ds(c, nc)]
        give(m, part, part)

    owns = []

    def begin():
        for m, (src, _, _, _) in enumerate(mats):
            copy = pltpu.make_async_copy(src, block(m, x, core), lsem.at[m])
            copy.start()
            owns.append(copy)
            give(m, src, block(m, x, core))

    def ready(m):
        owns[m].wait()
        links.arrive((m, "chip"), four(m))

    return begin, ready, peer, {"reach": reach, "relay": relay, "far": far, "pass": pass_on, "close": close, "hand": hand}


BF, F32 = jnp.bfloat16, jnp.float32


def product(a, b, contract=((1,), (0,))):
    return lax.dot_general(a, b, (contract, ((), ())), preferred_element_type=F32)


def lanes(start, size):
    return pl.ds(start if isinstance(start, int) else pl.multiple_of(start, LANE), size)


def layers_kernel(order, sc_ref, wi_ref, wo_ref, x_ref, dy_ref, freq_ref,
                  y_ref, gx_ref, hy_a, hy_b, hz_a, hz_b, mx_a, mx_b, yx_b, zy_b, zz_b, z_a, dy_a, sc_out, relay_m, relay_z,
                  wi, wo, z, om, h, hid, qr, kts, vsl, ksl, turned_q, turned_o, scores, dscores, pcat, dscat, cos_ref, sin_ref, turn_ref,
                  dot_heads, qt, dht, dkv, omt, ht, dyt, sc, gains, own_gain, gain_ref, load_sems, own_sems, send_sems, recv_sems,
                  share_send_sems, share_recv_sems):
    seq, dim = x_ref.shape
    ff = (wi.shape[PAIR] - dim - LANE) // PAIR
    position = chip_position()
    x, y, zc, core = position
    twin = device_at(x, y, zc, 1 - core)
    me = PAIR * x + core
    links, shared = Links(send_sems, recv_sems), Links(share_send_sems, share_recv_sems)
    stored = []
    spots, _ = around(position)
    h_out, m_out, y_out, z_out = {"y": (hy_a, hy_b), "z": (hz_a, hz_b)}, (mx_a, mx_b), {1: yx_b}, {(1, "y"): zy_b, (1, "z"): zz_b}
    middle = hid.at[1]
    begin, ready, peer, stages = gather_stages(links, position, wi_ref, wo_ref, wi, wo, load_sems)
    others = [(zc * SIDE + y, rem(me + k, ROW)) for k in range(1, ROW)]

    def spot(axis, o):
        return spots[axis, o % SIDE]

    def device(axis, o, index):
        moved = {"x": x, "y": y, "z": zc, axis: spot(axis, o)}
        return device_at(moved["x"], moved["y"], moved["z"], index)

    own_gain[ALL] = jnp.zeros(own_gain.shape, F32)
    count = sc_ref.shape[1]
    for f in range(ROW):
        @pl.when(me == f)
        def _():
            own_gain[0:PAIR, f * count:(f + 1) * count] = sc_ref[ALL].astype(F32)
    announce(others + [device(axis, o, index) for axis in "yz" for o in AROUND for index in range(PAIR)])
    begin()
    for k, far in enumerate(others):
        links.send(("sc",), own_gain, gains.at[me], far, batch=("sc",), whole=gains.at[pl.ds(0, 7)])

    def keep(src, dst):
        copy = pltpu.make_async_copy(src, dst, own_sems.at[len(stored)])
        copy.start()
        stored.append(copy)

    def tokens(axis, o, index):
        return pl.ds(pl.multiple_of((PAIR * spot(axis, o) + index) * seq, seq), seq)

    def columns(axis, o):
        size = z.shape[PAIR] // ROW
        return lanes(((0 if axis == "y" else SIDE) + spot(axis, o)) * size, size)

    def several(batch, ref, n):
        whole = ref.at[pl.ds(0, n * seq)] if batch[0][0] in "yz" else ref.at[(slice(None),) * (len(ref.shape) - 1) + (pl.ds(0, n * seq),)]
        return dict(batch=batch, whole=whole)

    def send_h(l, axis):
        out = h_out[axis][l].at[:, :, tokens(axis, 0, core)]
        for by in BOTH:
            for index in range(PAIR):
                shared.send(("h", l, axis, by), ht.at[l, :, index], out, device(axis, by, index), lane=core, **several(("h", l, axis), h_out[axis][l], 7))
        shared.send(("h", l, axis), ht.at[l, :, 1 - core], out, twin, **several(("h", l, axis), h_out[axis][l], 7))
        keep(ht.at[l, :, core], out)

    def pass_h(l, axis, by, index):
        out = h_out[axis][l]
        shared.arrive(("h", l, axis, by), out.at[:, :, tokens(axis, -by, index)], index)
        part = out.at[pl.ds(1 - by, PAIR), :, tokens(axis, -by, index)]
        shared.send(("h", l, axis), part, part, device(axis, by, core), **several(("h", l, axis), out, 7))

    def arrive_h(l):
        for axis in "yz":
            shared.arrive(("h", l, axis), h_out[axis][l].at[:, :, pl.ds(0, 3 * seq)])

    def row_block(l, o, index, part=None):
        size = omt.shape[1] // ROW
        start = (PAIR * spot("x", o) + index) * size
        if part is not None:
            size = size // PAIR
            start = start + part * size
        return omt.at[l, pl.ds(pl.multiple_of(start, 16), size)]

    def row_half(k):
        size = m_out[0].shape[0] // PAIR
        return pl.ds(k * size, size)

    def send_m(l):
        out = m_out[l].at[:, tokens("x", 0, core)]
        for k, by in enumerate(BOTH):
            for index in range(PAIR):
                shared.send(("mr", l, by), row_block(l, PAIR, index, k), relay_m.at[l, k, core], device("x", by, index), lane=core, **several(("m", l), m_out[l], 7))
        for by in BOTH:
            for index in range(PAIR):
                shared.send(("m", l), row_block(l, by, index), out, device("x", by, index), **several(("m", l), m_out[l], 7))
        shared.send(("m", l), row_block(l, 0, 1 - core), out, twin, **several(("m", l), m_out[l], 7))
        keep(row_block(l, 0, core), out)

    def pass_m(l, by, index):
        k = (1 - by) // PAIR
        shared.arrive(("mr", l, by), relay_m.at[l, k, index], index)
        shared.send(("m", l), relay_m.at[l, k, index], m_out[l].at[row_half(k), tokens("x", -by, index)], device("x", by, core),
                    **several(("m2", l), m_out[l], PAIR))

    def arrive_m(l):
        shared.arrive(("m", l), m_out[l].at[:, pl.ds(0, 7 * seq)])

    def token_half(axis, o, k):
        return pl.ds(pl.multiple_of((PAIR * spot(axis, o) + core) * seq + k * (seq // PAIR), seq // PAIR), seq // PAIR)

    def send_y(l):
        src, out = dy_ref, y_out[l].at[tokens("x", 0, core)]
        for by in BOTH:
            shared.send(("y", l, by), src, out, device("x", by, core), **several(("y", l), y_out[l], 7))
        shared.send(("y", l), src, out, twin, **several(("y", l), y_out[l], 7))
        keep(src, out)

    def pass_y(l, by):
        landed, part = y_out[l].at[tokens("x", -by, core)], y_out[l].at[token_half("x", -by, (1 - by) // PAIR)]
        shared.arrive(("y", l, by), landed)
        shared.send(("y2", l), part, part, device("x", by, core), **several(("y", l), y_out[l], 7))
        shared.send(("y", l), landed, landed, twin, **several(("y", l), y_out[l], 7))

    def far_y(l):
        landed = y_out[l].at[tokens("x", PAIR, core)]
        shared.arrive(("y2", l), landed)
        shared.send(("y", l), landed, landed, twin, **several(("y", l), y_out[l], 7))

    def arrive_y(l):
        shared.arrive(("y", l), y_out[l].at[pl.ds(0, SIDE * seq)])

    def push_z(l, axis, o, ready):
        out = z_out[l, axis].at[tokens(axis, 0, core)]
        batch = several(("z", l, axis), z_out[l, axis], ROW)

        def start():
            if o != PAIR:
                shared.send(("z", l, axis, o), z.at[l, :, columns(axis, o)], out, device(axis, o, core), **batch)
                return
            for k, by in enumerate(BOTH):
                shared.send(("zr", l, axis, by), z.at[l, pl.ds(k * (seq // PAIR), seq // PAIR), columns(axis, PAIR)], relay_z.at[l, "yz".index(axis), k],
                            device(axis, by, core), **batch)

        if ready is None:
            start()
        else:
            pl.when(ready)(start)

    def own_part(l, axis):
        out, mine = z_out[l, axis].at[tokens(axis, 0, core)], z.at[l, :, columns(axis, 0)]
        shared.send(("z", l, axis), mine, out, twin, **several(("z", l, axis), z_out[l, axis], ROW))
        keep(mine, out)

    def send_z(l, axis):
        for o in (PAIR, 1, -1):
            push_z(l, axis, o, spot(axis, o) != 0 if axis == "y" else None)
        if axis == "z":
            own_part(l, axis)

    def rest_z(l):
        for o in (PAIR, 1, -1):
            push_z(l, "y", o, spot("y", o) == 0)
        own_part(l, "y")

    def pass_z(l, axis, by):
        k = (1 - by) // PAIR
        half = relay_z.at[l, "yz".index(axis), k]
        shared.arrive(("zr", l, axis, by), half)
        shared.send(("z2", l, axis), half, z_out[l, axis].at[token_half(axis, -by, k)], device(axis, by, core), **several(("z", l, axis), z_out[l, axis], ROW))

    def twin_z(l, axis, by):
        landed = z_out[l, axis].at[tokens(axis, -by, core)]
        shared.arrive(("z", l, axis, by), landed)
        shared.send(("z", l, axis), landed, landed, twin, **several(("z", l, axis), z_out[l, axis], ROW))

    def far_z(l, axis):
        landed = z_out[l, axis].at[tokens(axis, PAIR, core)]
        shared.arrive(("z2", l, axis), landed)
        shared.send(("z", l, axis), landed, landed, twin, **several(("z", l, axis), z_out[l, axis], ROW))

    def arrive_z(l, axis):
        shared.arrive(("z", l, axis), z_out[l, axis].at[pl.ds(0, SIDE * seq)])

    def send_scale(l):
        for far in others:
            shared.send(("scale", l), sc.at[l], sc_out.at[l, me], far, batch=("scale", l), whole=sc_out.at[l, pl.ds(0, 7)])
        keep(sc.at[l], sc_out.at[l, me])

    def arrive_scale(l):
        shared.arrive(("scale", l), sc_out.at[l, pl.ds(0, 7)])

    gains[me] = own_gain[ALL]
    z[:, :, wi.shape[PAIR]:] = jnp.zeros((PAIR, seq, z.shape[PAIR] - wi.shape[PAIR]), BF)
    entry = (x_ref, hid.at[0])
    angle = lax.broadcasted_iota(jnp.int32, (seq, LANE), 0).astype(F32) * freq_ref[0:1]
    for half in range(PAIR):
        cos_ref[:, LANE * half:LANE * (half + 1)] = jnp.cos(angle)
        sin_ref[:, LANE * half:LANE * (half + 1)] = jnp.sin(angle)
    lane = lax.broadcasted_iota(jnp.int32, turn_ref.shape, 1)
    down = lax.broadcasted_iota(jnp.int32, turn_ref.shape, 0) - lane
    low = rem(lane, HEAD) < BAND
    turn_ref[ALL] = jnp.where(low & (down == BAND), -1.0, jnp.where(jnp.logical_not(low) & (down == -BAND), 1.0, ZERO)).astype(BF)
    kts[ALL] = jnp.zeros(kts.shape, BF)
    pcat[ALL] = jnp.zeros(pcat.shape, BF)
    dscat[ALL] = jnp.zeros(dscat.shape, BF)

    def normalise(l, src):
        @pl.loop(0, seq // BAND, unroll=SIDE)
        def _(r):
            rows = pl.ds(pl.multiple_of(r * BAND, BAND), BAND)
            v = src[rows].astype(F32)
            v = v - jnp.mean(v, axis=-1, keepdims=True)
            var = jnp.mean(v * v, axis=-1, keepdims=True)
            h[l, rows] = (v * lax.rsqrt(var + 1e-6) * gain_ref[l:l + 1]).astype(BF)

    def project(l):
        strip = wi.shape[PAIR] // 5

        @pl.loop(0, 5)
        def _(i):
            at = lanes(i * strip, strip)
            z[l, :, at] = product(h[l], wi[l, :, at]).astype(BF)

    def heads(l):
        cos, sin = cos_ref[ALL], sin_ref[ALL]
        for g in range(dim // WIDE):
            q = z[l, :, g * WIDE:(g + 1) * WIDE]
            qr[l, :, g * WIDE:(g + 1) * WIDE] = ((q.astype(F32) * cos + product(q, turn_ref[ALL]) * sin) * 0.125).astype(BF)
        kv = z[l, :, dim:dim + LANE]
        turned = kv.astype(F32) * cos[:, :LANE] + product(kv, turn_ref[:LANE, :LANE]) * sin[:, :LANE]
        first = lax.broadcasted_iota(jnp.int32, turned.shape, 1) < HEAD
        key_lo = jnp.where(first, turned, ZERO)
        val_hi = jnp.where(first, ZERO, kv.astype(F32))
        return key_lo, pltpu.roll(key_lo, HEAD, 1), pltpu.roll(val_hi, HEAD, 1), val_hi

    def slot_rows(ref, lo, hi):
        zero = jnp.zeros((seq, LANE), BF)
        lo, hi = lo.astype(BF), hi.astype(BF)
        for i, (left, right) in enumerate(((lo, zero), (hi, zero), (zero, lo), (zero, hi))):
            ref[i * seq:(i + 1) * seq, :LANE] = left
            ref[i * seq:(i + 1) * seq, LANE:] = right

    def slot_cols(ref, lo):
        flat = lo.T[:HEAD].astype(BF)
        for i in range(SIDE):
            ref[HEAD * i:HEAD * (i + 1), i * seq:(i + 1) * seq] = flat

    def chances(i, half):
        at = slice(LANE * half, LANE * (half + 1))
        blocks = [pl.ds(pl.multiple_of(i * seq + LANE * k, LANE), LANE) for k in range(half + 1)]
        s = [scores[keys, at] for keys in blocks]
        lower = lax.broadcasted_iota(jnp.int32, s[-1].shape, 1) >= lax.broadcasted_iota(jnp.int32, s[-1].shape, 0)
        s[-1] = jnp.where(lower, s[-1], -1e30)
        top = functools.reduce(jnp.maximum, [jnp.max(v, axis=0, keepdims=True) for v in s])
        e = [jnp.exp(v - top) for v in s]
        scale = 1.0 / sum(jnp.sum(v, axis=0, keepdims=True) for v in e)
        return at, [(keys, v * scale) for keys, v in zip(blocks, e)]

    def attend(l):
        key_lo, key_hi, val_lo, _ = heads(l)
        slot_rows(ksl, key_lo, key_hi)
        slot_cols(kts, val_lo)
        flip(lambda at: qr[l, :, lanes(at, WIDE)], qt, dim)

        @pl.loop(0, dim // WIDE)
        def _(g):
            rows = pl.ds(pl.multiple_of(g * WIDE, WIDE), WIDE)
            scores[ALL] = product(ksl[ALL], qt[rows])

            @pl.loop(0, SIDE)
            def _(i):
                for half in range(PAIR):
                    at, blocks = chances(i, half)
                    for keys, p in blocks:
                        pcat[keys, at] = p.astype(BF)
            flat = product(kts[ALL], pcat[ALL]).astype(BF)
            omt[l, rows] = flat
            om[:, lanes(g * WIDE, WIDE)] = flat.T

    def mlp(l):
        @pl.loop(0, seq // BAND)
        def _(r):
            rows = pl.ds(pl.multiple_of(r * BAND, BAND), BAND)

            @pl.loop(0, ff // STRIP)
            def _(i):
                gate = z[l, rows, lanes(dim + LANE + i * STRIP, STRIP)].astype(F32)
                up = z[l, rows, lanes(dim + LANE + ff + i * STRIP, STRIP)].astype(F32)
                om[rows, lanes(dim + i * STRIP, STRIP)] = (gate * jax.nn.sigmoid(gate) * up).astype(BF)

    def put_out(l, dst):
        for n in range(dim // WIDE):
            cols = slice(n * WIDE, (n + 1) * WIDE)
            total = product(om[ALL], wo[l, :, cols])
            dst[:, cols] = (entry[l][:, cols].astype(F32) + total).astype(BF)

    def flip(src, dst, width, first=0):
        @pl.loop(first // WIDE, width // WIDE)
        def _(i):
            dst[pl.ds(pl.multiple_of(i * WIDE, WIDE), WIDE)] = src(i * WIDE).T

    upstream = (middle, dy_ref)

    def back_out(l):
        dy = upstream[l]
        flip(lambda at: dy[:, lanes(at, WIDE)], dyt, dim)

        @pl.loop(0, wo.shape[1] // dim)
        def _(n):
            rows = pl.ds(pl.multiple_of(n * dim, dim), dim)
            part = product(wo[l, rows], dyt[ALL]).astype(BF)
            om[:, lanes(n * dim, dim)] = part.T

            @pl.when(n == 0)
            def _():
                dot_heads[ALL] = part

    def back_mlp(l):
        @pl.loop(0, seq // BAND)
        def _(r):
            rows = pl.ds(pl.multiple_of(r * BAND, BAND), BAND)

            @pl.loop(0, ff // STRIP)
            def _(i):
                gate_at, up_at = lanes(dim + LANE + i * STRIP, STRIP), lanes(dim + LANE + ff + i * STRIP, STRIP)
                gate, up = z[l, rows, gate_at].astype(F32), z[l, rows, up_at].astype(F32)
                d = om[rows, lanes(dim + i * STRIP, STRIP)].astype(F32)
                sig = jax.nn.sigmoid(gate)
                du = d * up
                z[l, rows, gate_at] = (du * sig + du * gate * (sig * (1.0 - sig))).astype(BF)
                z[l, rows, up_at] = (d * (gate * sig)).astype(BF)

    def back_heads(l):
        key_lo, key_hi, val_lo, val_hi = heads(l)
        slot_rows(ksl, key_lo, key_hi)
        slot_rows(vsl, val_lo, val_hi)
        slot_cols(kts, key_lo)
        dkv[ALL] = jnp.zeros(dkv.shape, F32)
        flip(lambda at: qr[l, :, lanes(at, WIDE)], qt, dim)
        for at in range(0, dim, LANE):
            pair = slice(at, at + LANE)
            turned_q[:, pair] = pltpu.roll(qr[l, :, pair].astype(F32), HEAD, 1).astype(BF)
            turned_o[:, pair] = pltpu.roll(om[:, pair].astype(F32), HEAD, 1).astype(BF)

    def back_quad(l):
        @pl.loop(0, dim // WIDE)
        def _(g):
            quad(l, g)

    def quad(l, g):
        cols = pl.ds(pl.multiple_of(g * WIDE, WIDE), WIDE)
        scores[ALL] = product(ksl[ALL], qt[cols])
        dscores[ALL] = product(vsl[ALL], dot_heads[cols])

        @pl.loop(0, SIDE)
        def _(i):
            for half in range(PAIR):
                at, blocks = chances(i, half)
                given = [p * dscores[keys, at].astype(BF).astype(F32) for keys, p in blocks]
                total = sum(jnp.sum(v, axis=0, keepdims=True) for v in given)
                for (keys, p), v in zip(blocks, given):
                    pcat[keys, at] = p.astype(BF)
                    dscat[keys, at] = (v - p * total).astype(BF)
        dq = product(kts[ALL], dscat[ALL]).astype(BF).T
        back = dq.astype(F32) * cos_ref[ALL] - product(dq, turn_ref[ALL]) * sin_ref[ALL]
        z[l, :, cols] = (back * 0.125).astype(BF)
        for i in range(SIDE):
            keys, pair = slice(i * seq, (i + 1) * seq), lanes(g * WIDE + i // PAIR * LANE, LANE)
            even = i % PAIR == 0
            dkv[0] += product(dscat[keys], qr[l, :, pair] if even else turned_q[:, pair])
            dkv[1] += product(pcat[keys], turned_o[:, pair] if even else om[:, pair])

    def back_keys(l):
        dk = dkv[0].astype(BF)
        turned = dk.astype(F32) * cos_ref[:, :LANE] - product(dk, turn_ref[:LANE, :LANE]) * sin_ref[:, :LANE]
        first = lax.broadcasted_iota(jnp.int32, turned.shape, 1) < HEAD
        z[l, :, dim:dim + LANE] = jnp.where(first, turned, dkv[1]).astype(BF)

    def back_in(l, half):
        width = wi.shape[PAIR] // 5
        at = slice(PAIR * half * width, (PAIR + 3 * half) * width)
        part = product(wi[l, :, at], z[l, :, at], ((1,), (1,)))
        dht[ALL] = dht[ALL] + part if half else part

    def back_norm(l):
        dy, dst = upstream[l], (gx_ref, middle)[l]
        for i in range(dim // WIDE):
            cols = slice(i * WIDE, (i + 1) * WIDE)
            h[l, :, cols] = dht[cols].T.astype(BF)
        sc[l] = jnp.zeros(sc.shape[1:], F32)

        @pl.loop(0, seq // BAND, unroll=SIDE)
        def _(r):
            rows = pl.ds(pl.multiple_of(r * BAND, BAND), BAND)
            v = entry[l][rows].astype(F32)
            v = v - jnp.mean(v, axis=-1, keepdims=True)
            scale = lax.rsqrt(jnp.mean(v * v, axis=-1, keepdims=True) + 1e-6)
            hat = v * scale
            d = h[l, rows].astype(F32)
            each = (d * hat).reshape(SIDE, ROW, dim)
            sc[l] += (each[0] + each[1]) + (each[PAIR] + each[3])
            d = d * gain_ref[l:l + 1]
            d = scale * (d - jnp.mean(d, axis=-1, keepdims=True) - hat * jnp.mean(d * hat, axis=-1, keepdims=True))
            dst[rows] = (dy[rows].astype(F32) + d.astype(BF).astype(F32)).astype(BF)

    def do_norm(l):
        if l == 0:
            links.arrive(("sc",), gains.at[pl.ds(0, 7)])
            gain_ref[ALL] = jnp.sum(gains[ALL], axis=0)
        normalise(l, entry[l])
        for i in range(dim // WIDE):
            flat = h[l, :, i * WIDE:(i + 1) * WIDE].T
            size = ht.shape[3]
            for b in range(ROW):
                lo, hi = max(b * size, i * WIDE), min((b + 1) * size, (i + 1) * WIDE)
                if lo < hi:
                    ht[l, b // PAIR, b % PAIR, lo - b * size:hi - b * size] = flat[lo - i * WIDE:hi - i * WIDE]

    def do_project(l):
        ready(PAIR * l)
        project(l)

    def do_mlp(l):
        mlp(l)
        flip(lambda at: om[:, lanes(at, WIDE)], omt.at[l], om.shape[1], dim)

    def do_put(l):
        ready(PAIR * l + 1)
        put_out(l, hid.at[0] if l == 0 else y_ref)

    stages.update(
        norm=do_norm, project=do_project, attend=attend, mlp=do_mlp, put=do_put, back_out=back_out, back_mlp=back_mlp, back_heads=back_heads,
        back_quad=back_quad, back_keys=back_keys, back_in=back_in, back_norm=back_norm, send_h=send_h, pass_h=pass_h, send_m=send_m,
        pass_m=pass_m, send_y=send_y, pass_y=pass_y, far_y=far_y, send_z=send_z, rest_z=rest_z, pass_z=pass_z, twin_z=twin_z, far_z=far_z,
        send_scale=send_scale, own_z=lambda: keep(z.at[0], z_a), own_y=lambda: keep(middle, dy_a))
    for kind, *task in order:
        stages[kind](*task)
    for l in range(PAIR):
        arrive_h(l)
        arrive_m(l)
        arrive_scale(l)
    arrive_y(1)
    for l, axis in z_out:
        arrive_z(l, axis)
    for copy in stored:
        copy.wait()
    shared.drain()
    links.drain()


def run_layers(x, dy, scale, w_in, w_out, freq, starts=(ZERO, 10.0, 20.0, 30.0)):
    seq, dim = x.shape
    proj, cat = w_in.shape[PAIR], ROW * w_out.shape[1]
    wide = proj + LANE
    hbm, vmem = pl.BlockSpec(memory_space=pltpu.HBM), pl.BlockSpec(memory_space=pltpu.VMEM)
    out = lambda *shape, dtype=BF: jax.ShapeDtypeStruct(shape, dtype)
    buffer = lambda *shape, dtype=BF: pltpu.VMEM(shape, dtype)
    sem = pltpu.SemaphoreType.DMA
    line = ROW * seq
    return pl.pallas_call(
        functools.partial(layers_kernel, layers_order(*w_in.shape[1:], *w_out.shape[1:], seq, starts)),
        out_shape=(out(seq, dim), out(seq, dim), *[out(SIDE, dim // ROW, line)] * SIDE, *[out(cat // ROW, line)] * PAIR, out(line, dim),
                   *[out(line, wide // ROW)] * PAIR, out(seq, wide), out(seq, dim), out(PAIR, ROW, ROW, dim, dtype=F32),
                   out(PAIR, PAIR, PAIR, cat // 16, seq), out(PAIR, PAIR, PAIR, seq // PAIR, wide // ROW)),
        in_specs=[vmem, hbm, hbm] + [vmem] * 3,
        out_specs=[vmem] * PAIR + [hbm] * 14,
        scratch_shapes=[
            buffer(PAIR, dim, proj), buffer(PAIR, cat, dim), buffer(PAIR, seq, wide), buffer(seq, cat), buffer(PAIR, seq, dim),
            buffer(PAIR, seq, dim), buffer(PAIR, seq, dim),
            buffer(WIDE, SIDE * seq), buffer(SIDE * seq, WIDE), buffer(SIDE * seq, WIDE), buffer(seq, dim), buffer(seq, dim),
            buffer(SIDE * seq, seq, dtype=F32), buffer(SIDE * seq, seq, dtype=F32), buffer(SIDE * seq, seq), buffer(SIDE * seq, seq),
            buffer(seq, WIDE, dtype=F32), buffer(seq, WIDE, dtype=F32), buffer(WIDE, WIDE),
            buffer(dim, seq), buffer(dim, seq), buffer(dim, seq, dtype=F32), buffer(PAIR, seq, LANE, dtype=F32),
            buffer(PAIR, cat, seq), buffer(PAIR, SIDE, PAIR, dim // ROW, seq), buffer(dim, seq), buffer(PAIR, ROW, dim, dtype=F32),
            buffer(ROW, ROW, dim, dtype=F32), buffer(ROW, dim, dtype=F32), buffer(ROW, dim, dtype=F32),
            sem((SIDE,)), sem((13,)), sem((15,)), sem((107,)), sem((13,)), sem((HEAD,)),
        ],
        compiler_params=pltpu.CompilerParams(collective_id=PAIR, has_side_effects=True, vmem_limit_bytes=67043328),
        name="run_layers",
    )(scale, w_in, w_out, x, dy, freq)


PARTS = (("i", "x", "z", "y", 0, STRIP), ("i", "x", "z", "y", STRIP, 384), ("i", "x", "y", "z", 0, STRIP), ("i", "x", "y", "z", STRIP, 384),
         ("o", "y", "z", "y", 0, 384), ("o", "z", "y", "z", 384, 384))


def reduce_order(rows, rows_b, starts):
    rate = 11650.0
    tasks = []
    sizes = {"y": WIDE * 896 / (PAIR * rate), "z": WIDE * 896 / (PAIR * rate), "x": WIDE * 768 / (PAIR * rate)}
    for axis in "yzx":
        tasks.append((("swap", axis), (0, 0), starts[PAIR] if axis == "x" else starts[3], [], [], [((axis, by), sizes[axis] * n) for by, n in ((1, 1), (-1, 1), (1, PAIR))], 0.3))
        for i, o in enumerate(AROUND):
            tasks.append((("near", axis, o), (0, PAIR), ZERO, [(("swap", axis), i)], [], [("chip", 1.6)], 0.2))
    tasks.append((("fetch", 0), (5, 0), ZERO, [], [("make", 1, len(PARTS) - 1)], [], 0.2))
    for l in (1, 0):
        late = 1 - l
        for c, (kind, first, then, last, at, width) in enumerate(PARTS):
            needs, cost = [], 1.6 * width / STRIP
            if l == 0:
                needs = [(("near", last if kind == "i" else "x", o), 0) for o in AROUND]
            tasks.append((("make", l, c), (9 * late, c), starts[late], needs, [] if l else [("fetch", 0)], [], cost))
            full = SIDE * SIDE * (rows if kind == "i" else rows_b) * width / rate
            sends = [[((first, by), full / ROW) for by in BOTH], [((first, by), full / SIDE) for by in BOTH],
                     [((then, o), full / 16) for o in (1, -1, 1)], []]
            piece = full / 16
            sends += [[((then, by), piece) for by in BOTH], [((then, 1 - PAIR * (c % PAIR)), piece)], [((last, by), SIDE * piece) for by in BOTH],
                      [((last, by), PAIR * piece) for by in BOTH], []]
            for s in range(9):
                task = ("sum", l, c, s)
                needs = [(("sum", l, c, s - 1), k) for k in range(len(sends[s - 1]))] if s else []
                tasks.append((task, (late, -s), ZERO, needs, [("make", l, c)] if s == 0 else [("sum", l, c, s - 1)], sends[s], 0.3))
    return plan(tasks)


def reduce_kernel(order, *refs):
    hy, hz, mx = refs[0:PAIR], refs[PAIR:SIDE], refs[SIDE:6]
    yx1, zy1, zz1, z0, y0, sc = refs[6:12]
    oa, ob = refs[12:14]
    n = len(PARTS)
    total, half, full, small, front = (refs[14 + k * n:14 + (k + 1) * n] for k in range(5))
    (hbuf, zbuf, mbuf, ybuf, scbuf, ssem, rsem, isem, osem) = refs[14 + 5 * n:]
    position = chip_position()
    x, y, zc, core = position
    place = {"x": x, "y": y, "z": zc}
    twin = device_at(x, y, zc, 1 - core)
    spots, peers = around(position)

    def spot(axis, o):
        return spots[axis, o % SIDE]

    def peer(axis, o):
        return peers[axis, o % SIDE]

    seq, wide = z0.shape
    own = wide // ROW
    loads, moving = {}, []

    def load(key, src, dst):
        copy = pltpu.make_async_copy(src, dst, isem.at[len(moving)])
        moving.append(key)
        copy.start()
        loads[key] = copy

    def fetch(l):
        if l:
            load(("z", 1, "y"), zy1, zbuf.at[1, 0])
        load(("h", l, "y"), hy[l], hbuf.at[l, 0])
        if l:
            load(("z", 1, "z"), zz1, zbuf.at[1, 1])
        load(("h", l, "z"), hz[l], hbuf.at[l, 1])
        load(("m", l), mx[l], mbuf.at[l])
        if l:
            load(("y", 1), yx1, ybuf.at[1])
        load(("s", l), sc.at[l], scbuf.at[l])

    fetch(1)
    done = set()

    def loaded(*keys):
        for key in keys:
            if key not in done:
                loads[key].wait()
                done.add(key)

    announce([peer(axis, o) for axis in "xyz" for o in AROUND] + [twin])
    links = Links(ssem, rsem)

    def columns(axis, o):
        return lanes(((0 if axis == "y" else SIDE) + spot(axis, o)) * own, own)

    def tokens(axis, o, index):
        return pl.ds(pl.multiple_of((PAIR * spot(axis, o) + index) * seq, seq), seq)

    def target(axis):
        return ybuf.at[0] if axis == "x" else zbuf.at[0, "yz".index(axis)]

    def seven(axis):
        return dict(batch=("swap", axis), whole=target(axis).at[pl.ds(0, 7 * seq)])

    def swap(axis):
        def part(o):
            return y0 if axis == "x" else z0.at[:, columns(axis, o)]

        mine = target(axis).at[tokens(axis, 0, core)]
        for o in AROUND:
            links.send(("swap", axis, o), part(o), mine, peer(axis, o), **seven(axis))
        links.send(("near", axis), part(0), mine, twin, **seven(axis))
        load(("own", axis), part(0), mine)

    def near(axis, o):
        landed = target(axis).at[tokens(axis, -o, core)]
        links.arrive(("swap", axis, o), landed)
        links.send(("near", axis), landed, landed, twin, **seven(axis))

    def joined(axis):
        if axis not in done:
            done.add(axis)
            loaded(("own", axis))
            links.arrive(("near", axis), target(axis).at[pl.ds(0, SIDE * seq)])

    def make(l, c):
        kind, first, then, last, at, width = PARTS[c]
        if kind == "i":
            i = "yz".index(last)
            loaded(("h", l, last))
            if l:
                loaded(("z", l, last))
            else:
                joined(last)
            size = total[c].shape[3]
            for lo in range(0, width, WIDE):
                hi = min(width, lo + WIDE)
                part = product(hbuf[l, i].reshape(-1, hbuf.shape[-1]), zbuf[l, i, :, at + lo:at + hi])
                for r in range(16):
                    total[c][l, r // SIDE, r % SIDE, :, lo:hi] = part[r * size:(r + 1) * size]
            return
        loaded(("m", l), ("s", l))
        if l:
            loaded(("y", l))
        else:
            joined("x")
        part = product(mbuf[l], ybuf[l, :, at:at + width])
        size = total[c].shape[3]

        def put(r, value):
            total[c][(l, r // SIDE, r % SIDE) if first == "y" else (l, r % SIDE, r // SIDE)] = value

        for r in range(part.shape[0] // size):
            put(r, part[r * size:(r + 1) * size])
        gain = jnp.sum(jnp.sum(scbuf[l, :, :, at:at + width], axis=0), axis=0, keepdims=True)
        row = lax.broadcasted_iota(jnp.int32, (size, width), 0)
        put(15, jnp.where(row == 0, gain, ZERO))

    def area(l, c, o, whole):
        kind, first, then, last, at, width = PARTS[c]
        inner = (spot(then, whole) if isinstance(whole, int) else whole)
        outer = spot(last, o)
        if kind == "i":
            cols = lanes(((0 if last == "y" else SIDE) + outer) * own + at, width)
            return oa.at[l, inner, :, cols]
        cols = pl.ds(at, width)
        return ob.at[l, outer, inner, :, cols] if last == "y" else ob.at[l, inner, outer, :, cols]

    def add(l, c, s):
        kind, first, then, last, at, width = PARTS[c]
        t = total[c].at[l]
        way = 1 - PAIR * (c % PAIR)
        sums = dict(batch=(l, c, 0), whole=t)
        wide_ones = dict(batch=(l, c, 1), whole=t.at[pl.ds(0, 3)])
        narrow = dict(batch=(l, c, PAIR), whole=t.at[0, pl.ds(0, PAIR)])
        if s == 0:
            far = t.at[spot(first, PAIR)]
            for k, by in enumerate(BOTH):
                links.send((l, c, "half"), far.at[pl.ds(PAIR * k, PAIR)], half[c].at[l, k], peer(first, by), **sums)
        elif s == 1:
            links.arrive((l, c, "half"), half[c].at[l])
            for k, by in enumerate(BOTH):
                mine = t.at[spot(first, by)]
                add_into(mine.at[pl.ds(PAIR * k, PAIR)], half[c].at[l, k])
                links.send((l, c, "full"), mine, full[c].at[l, k], peer(first, by), **sums)
        elif s == PAIR:
            mine = t.at[spot(first, 0)]
            links.arrive((l, c, "full"), full[c].at[l])
            for k in range(PAIR):
                add_into(mine, full[c].at[l, k])
            for k, o in enumerate(AROUND):
                links.send((l, c, "small"), mine.at[spot(then, o)], small[c].at[l, k], peer(then, o), **wide_ones)
        elif s == 3:
            links.arrive((l, c, "small"), small[c].at[l])
            mine = t.at[spot(first, 0), spot(then, 0)]
            front[c][l] = (mine[ALL] + small[c][l, 0]) + (small[c][l, 1] + small[c][l, PAIR])
        elif s == SIDE:
            src, dst = front[c].at[l], area(l, c, 0, 0)
            for by in BOTH:
                links.send((l, c, "a1"), src, dst, peer(then, by), **narrow)
            copy = pltpu.make_async_copy(src, dst, osem.at[l, c])
            copy.start()
            loads["front", l, c] = copy
        elif s == 5:
            links.arrive((l, c, "a1"), t.at[0, pl.ds(0, PAIR)])
            landed = area(l, c, 0, -way)
            links.send((l, c, "b1"), landed, landed, peer(then, way), **wide_ones)
        elif s == 6:
            loaded(("front", l, c))
            links.arrive((l, c, "b1"), area(l, c, 0, PAIR))
            line = area(l, c, 0, slice(None))
            for by in BOTH:
                links.send((l, c, "a2"), line, line, peer(last, by), **wide_ones)
        elif s == 7:
            links.arrive((l, c, "a2"), t.at[pl.ds(0, PAIR)])
            for k, by in enumerate(BOTH):
                part = area(l, c, -by, pl.ds(PAIR * k, PAIR))
                links.send((l, c, "a3"), part, part, peer(last, by), **sums)
        else:
            links.arrive((l, c, "a3"), area(l, c, PAIR, slice(None)))

    stages = {"swap": swap, "near": near, "fetch": fetch, "make": make, "sum": add}
    for kind, *task in order:
        stages[kind](*task)
    links.drain()


def add_into(dst, src):
    @pl.loop(0, dst.shape[0])
    def _(i):
        if len(dst.shape) == SIDE:
            for j in range(dst.shape[1]):
                dst[i, j] += src[i, j]
        else:
            dst[i] += src[i]


def around(position):
    place, core = dict(zip("xyz", position)), position[3]
    spots = {(axis, o): step(place[axis], o) for axis in "xyz" for o in range(SIDE)}
    peers = {}
    for axis in "xyz":
        for o in range(1, SIDE):
            moved = {**place, axis: spots[axis, o]}
            peers[axis, o] = device_at(moved["x"], moved["y"], moved["z"], core)
    return spots, peers


def reduce_gradients(operands, starts=(ZERO, ZERO, 20.0, ZERO)):
    hbm = pl.BlockSpec(memory_space=pltpu.HBM)
    h_rows, m_rows, y_cols, z_cols, z_own, y_own, scale_parts = operands
    part, part_b = h_rows[0].shape[1] // SIDE, (m_rows[0].shape[0] + BAND) // 16
    (line, dim), wide = y_cols.shape, z_own.shape[1]
    out = lambda *shape: jax.ShapeDtypeStruct(shape, F32)
    sem = pltpu.SemaphoreType.DMA

    def buffers(*lead):
        return [pltpu.VMEM((PAIR, *lead, part if e[0] == "i" else part_b, e[5]), F32) for e in PARTS]

    return pl.pallas_call(
        functools.partial(reduce_kernel, reduce_order(part, part_b, starts)),
        out_shape=(out(PAIR, SIDE, part, wide), out(PAIR, SIDE, SIDE, part_b, dim)),
        in_specs=[hbm] * 12,
        out_specs=[hbm] * PAIR,
        scratch_shapes=[
            *buffers(SIDE, SIDE), *buffers(PAIR, PAIR), *buffers(PAIR, SIDE), *buffers(3), *buffers(),
            pltpu.VMEM((PAIR, PAIR, *h_rows[0].shape), BF), pltpu.VMEM((PAIR, PAIR, line, wide // ROW), BF), pltpu.VMEM((PAIR, *m_rows[0].shape), BF),
            pltpu.VMEM((PAIR, line, dim), BF), pltpu.VMEM(scale_parts.shape, F32),
            sem((39,)), sem((96,)), sem((14,)), sem((PAIR, len(PARTS))),
        ],
        compiler_params=pltpu.CompilerParams(collective_id=1, has_side_effects=True, vmem_limit_bytes=67043328),
        name="reduce_gradients",
    )(*h_rows, *m_rows, y_cols, *z_cols, z_own, y_own, scale_parts)


def solution(mesh):
    fsdp_size = mesh.shape["fsdp"]
    batch_spec = P(("dp", "fsdp"), None, None)
    scale_spec = P(None, "fsdp")
    weight_spec = P(None, "fsdp", None)

    def device_step(x_in, grad_y, norm_scale, w_in, w_out):
        n_layers = w_in.shape[0]
        seq_len, model_dim = x_in.shape[1:]
        proj_dim = w_in.shape[PAIR]
        ff_dim = w_out.shape[1] * fsdp_size - model_dim
        head_dim = (proj_dim - model_dim - PAIR * ff_dim) // PAIR
        rows, rows_out = norm_scale.shape[1], w_out.shape[1]
        half_dim = head_dim // PAIR
        freq = 10000.0 ** (-np.arange(half_dim, dtype=np.float32) * 2.0 / head_dim)
        freq = jnp.asarray(np.tile(freq.astype(np.float32), (ROW, LANE // half_dim)))
        hidden, grad_hidden, *rest = run_layers(x_in[0], grad_y[0], norm_scale, w_in, w_out, freq)
        in_sums, out_sums = reduce_gradients((rest[0:SIDE], rest[SIDE:6], rest[6], rest[7:9], rest[9], rest[10], rest[11]))
        in_grads = in_sums.reshape(n_layers, rows, -1)[:, :, :proj_dim]
        out_rows = out_sums.reshape(n_layers, -1, model_dim)
        scale_grads = lax.dynamic_slice(out_rows[:, rows_out], (0, lax.axis_index("fsdp") * rows), (n_layers, rows))
        out_grads = out_rows[:, :rows_out]
        return hidden[None], grad_hidden[None], scale_grads, in_grads, out_grads

    return jax.shard_map(
        device_step,
        mesh=mesh,
        in_specs=(batch_spec, batch_spec, scale_spec, weight_spec, weight_spec),
        out_specs=(batch_spec, batch_spec, scale_spec, weight_spec, weight_spec),
        check_vma=False,
    )
```

```python
import functools
import jax
import jax.numpy as jnp
import numpy as np
from jax import lax
from jax.experimental import pallas as pl
from jax.experimental.pallas import tpu as pltpu
from jax.sharding import PartitionSpec as P

MESH_ID = pl.DeviceIdType.MESH
BOTH = (1, -1)
AROUND = (1, -1, 2)
PARTS = (True, False)
ALL, ZERO = ..., 0.0
LANE, WIDE, STRIP, HEAD = 128, 256, 512, 64
ROW, BAND, SIDE, PAIR = 8, 32, 4, 2


class Links:
    def __init__(self, send_sems, recv_sems):
        self.send_sems, self.recv_sems = send_sems, recv_sems
        self.slots, self.batches, self.sent, self.count = {}, {}, {}, 0

    def _landing(self, key, lane):
        if key not in self.slots:
            self.slots[key] = self.count
            self.count += 1 if lane is None else PAIR
        return self.recv_sems.at[self.slots[key] + (0 if lane is None else lane)]

    def send(self, key, src, dst, device, landing=None, whole=None, batch=None, lane=None):
        leaving = self.batches.setdefault(batch or key, len(self.batches))
        copy = pltpu.make_async_remote_copy(
            src_ref=src, dst_ref=dst, send_sem=self.send_sems.at[leaving], recv_sem=self._landing(landing or key, lane),
            device_id=device, device_id_type=MESH_ID)
        copy.start()
        self.sent[batch or key] = (src if whole is None else whole, leaving)

    def arrive(self, key, landed, lane=None):
        pltpu.make_async_copy(landed, landed, self._landing(key, lane)).wait()

    def drain(self):
        for left, leaving in self.sent.values():
            pltpu.make_async_copy(left, left, self.send_sems.at[leaving]).wait()
        self.sent.clear()


def rem(a, n):
    return a % n if isinstance(a, int) else lax.rem(a, n)


def chip_position():
    f, d = lax.axis_index("fsdp"), lax.axis_index("dp")
    return f // PAIR, rem(d, SIDE), d // SIDE, rem(f, PAIR)


def device_at(x, y, z, core):
    return (z * SIDE + y, x * PAIR + core)


def step(coord, by):
    return rem(coord + SIDE + by, SIDE)


def announce(devices):
    barrier = pltpu.get_barrier_semaphore()
    for device in devices:
        pl.semaphore_signal(barrier, inc=1, device_id=device, device_id_type=MESH_ID)
    pl.semaphore_wait(barrier, len(devices))


def plan(tasks, latency=2.5):
    free, landed, order, now = {}, {}, [], ZERO
    left = list(tasks)
    while left:
        best = None
        for place, (name, rank, start, needs, after, _, _) in enumerate(left):
            if all(n[0] in landed for n in needs) and all(n in landed for n in after):
                ready = max([start, now] + [landed[task][i] for task, i in needs])
                best = min(best or (ready, rank, place), (ready, rank, place))
        now, _, place = best
        name, _, _, _, _, sends, cost = left.pop(place)
        order.append(name)
        now += cost
        landed[name] = []
        for link, time in sends:
            free[link] = max(now, free.get(link, ZERO)) + time
            landed[name].append(free[link] + latency)
    return order


def layers_order(rows_i, cols_i, rows_o, cols_o, seq, starts):
    rate = 23300.0
    tasks = []
    for m in range(SIDE):
        is_in = m % PAIR == 0
        edge = cols_i // LANE * SIDE // 9 // PAIR * WIDE
        size = {"y": rows_i // SIDE * edge, "x": rows_i * (cols_i - PAIR * edge)} if is_in else {"y": rows_o // SIDE * cols_o // PAIR}
        size["z"] = size["y"]
        colors = "yzx" if is_in else "yz"
        for color in colors:
            cost = size[color] / rate
            both = [(("x", by), cost) for by in BOTH]
            spread = [((color, by), cost) for by in BOTH] if color != "x" else []
            tasks.append((("reach", m, color), m, starts[m], [], [], both, 0.2))
            for i, by in enumerate(BOTH):
                tasks.append((("relay", m, color, by), m, ZERO, [(("reach", m, color), i)], [], [(("x", by), cost / PAIR)] + spread, 0.2))
            halves = [(("relay", m, color, by), 0) for by in BOTH]
            tasks.append((("far", m, color), m, ZERO, halves, [], spread, 0.2))
            if color == "x":
                continue
            for off, source, first in ((-1, ("relay", m, color, 1), 1), (1, ("relay", m, color, -1), 1), (PAIR, ("far", m, color), 0)):
                for i, by in enumerate(BOTH):
                    tasks.append((("pass", m, color, off, by), m, ZERO, [(source, first + i)], [], [((color, by), cost / PAIR)], 0.2))
                halves = [(("pass", m, color, off, by), 0) for by in BOTH]
                tasks.append((("close", m, color, off), m, ZERO, halves, [], [], 0.2))
        for off in (-1, 1, PAIR):
            last = [("close", m, color, off) for color in "yz"]
            if is_in:
                last.append(("far", m, "x") if off == PAIR else ("relay", m, "x", -off))
            tasks.append((("hand", m, off), m, ZERO, [], last, [("chip", (rows_i * cols_i if is_in else rows_o * cols_o) / 150000.0)], 0.2))
    before = []

    def work(name, cost, mats=()):
        needs = [(("hand", m, off), 0) for m in mats for off in (-1, 1, PAIR)]
        tasks.append((name, 99, ZERO, needs, list(before), [], cost))
        before[:] = [name]

    for l in range(PAIR):
        work(("norm", l), 0.8)
        work(("project", l), 4.0, [PAIR * l])
        work(("attend", l), 4.2)
        work(("mlp", l), 2.2)
        work(("put", l), 1.6, [PAIR * l + 1])
    for l in (1, 0):
        work(("back_out", l), 2.9)
        work(("back_mlp", l), 2.0)
        work(("back_heads", l), 1.0)
        work(("back_quad", l), 6.0)
        work(("back_keys", l), 0.2)
        for i in range(PAIR):
            work(("back_in", l, i), 1.3 + 0.6 * i)
        work(("back_norm", l), 1.0)
    def send(name, rank, start, after, sends):
        tasks.append((name, rank, start, [], [after] if after else [], sends, 0.4))

    def follow(name, rank, needs, sends):
        tasks.append((name, rank, ZERO, needs, [], sends, 0.2))

    def both(axis, size):
        return [((axis, by), size / rate) for by in BOTH]

    model = rows_i * ROW
    for l in (1, 0):
        for axis in "yz":
            name = ("send_h", l, axis)
            send(name, 20 - l, 58.0, ("norm", l), both(axis, seq * model))
            for i, by in enumerate(BOTH):
                for index in range(PAIR):
                    follow(("pass_h", l, axis, by, index), 10, [(name, i)], [((axis, by), seq * model / SIDE / rate)])
        name = ("send_m", l)
        send(name, 22 - l, ZERO, ("mlp", l), both("x", seq * rows_o) + both("x", PAIR * seq * rows_o))
        for i, by in enumerate(BOTH):
            for index in range(PAIR):
                follow(("pass_m", l, by, index), 11, [(name, i)], [(("x", by), seq * rows_o / PAIR / rate)])
        if l == 0:
            send(("own_y",), 15, ZERO, ("back_norm", 1), [])
            send(("send_scale", l), 15, ZERO, ("back_norm", l), [])
            continue
        name = ("send_y", l)
        send(name, 12, 42.0, None, both("x", seq * model))
        for i, by in enumerate(BOTH):
            follow(("pass_y", l, by), 12, [(name, i)], [(("x", by), seq * model / PAIR / rate)])
        follow(("far_y", l), 12, [(("pass_y", l, by), 0) for by in BOTH], [])
        for axis in "zy":
            name = ("send_z", l, axis)
            share = seq * (cols_i + LANE) / ROW
            send(name, 13, ZERO, ("back_mlp", l), both(axis, share / PAIR) + both(axis, share))
            if axis == "y":
                name = ("rest_z", l)
                send(name, 13, ZERO, ("back_keys", l), both(axis, share / ROW) + both(axis, share / SIDE))
            for i, by in enumerate(BOTH):
                follow(("pass_z", l, axis, by), 13, [(name, i)], [((axis, by), share / PAIR / rate)])
                follow(("twin_z", l, axis, by), 14, [(name, PAIR + i)], [])
            follow(("far_z", l, axis), 14, [(("pass_z", l, axis, by), 0) for by in BOTH], [])
        send(("send_scale", l), 15, ZERO, ("back_norm", l), [])
    send(("own_z",), 15, ZERO, ("back_keys", 0), [])
    return plan(tasks)


def gather_stages(links, position, shard_i, shard_o, wi, wo, lsem):
    x, y, z, core = position
    twin = device_at(x, y, z, 1 - core)
    rows_i, cols_i = shard_i.shape[1:]
    rows_o, cols_o = shard_o.shape[1:]
    quarter_i, quarter_o = rows_i // SIDE, rows_o // SIDE
    third_i = cols_i // LANE * SIDE // 9 // PAIR * WIDE
    half_o = cols_o // PAIR
    cut_o = quarter_o // 16 * ROW + ROW if quarter_o % 16 else quarter_o // PAIR
    place = {"x": x, "y": y, "z": z}

    spots = {(axis, o): step(place[axis], o) for axis in "xyz" for o in range(SIDE)}

    def spot(axis, o):
        return spots[axis, o % SIDE]

    table = {}
    for axis in "xyz":
        for o in range(1, SIDE):
            moved = {**place, axis: spot(axis, o)}
            table[axis, o] = device_at(moved["x"], moved["y"], moved["z"], core)

    def peer(axis, o):
        return table[axis, o % SIDE]

    mats = []
    for l in range(PAIR):
        mats.append((shard_i.at[l], wi.at[l], rows_i, True))
        mats.append((shard_o.at[l], wo.at[l], rows_o, False))

    def region(is_in, color, q):
        if is_in:
            if color == "x":
                lo, hi = PAIR * third_i, cols_i
                rows = (0, rows_i)
            else:
                lo, hi = (0, third_i) if color == "y" else (third_i, PAIR * third_i)
                rows = (q * quarter_i, quarter_i)
            mid = lo + ((hi - lo) // LANE + 1) // PAIR * LANE
            return (rows, (lo, hi - lo)), (rows, (lo, mid - lo)), (rows, (mid, hi - mid))
        cols = (0, half_o) if color == "y" else (half_o, half_o)
        start = q * quarter_o
        return ((start, quarter_o), cols), ((start, cut_o), cols), ((start + cut_o, quarter_o - cut_o), cols)

    def at(m, xb, area):
        (r, nr), (c, nc) = area
        _, out, size, _ = mats[m]
        return out.at[pl.ds(pl.multiple_of((PAIR * xb + core) * size + r, ROW), nr), pl.ds(c, nc)]

    def block(m, xb, index):
        _, out, size, _ = mats[m]
        return out.at[pl.ds(pl.multiple_of((PAIR * xb + index) * size, BAND), size)]

    def group(m, color):
        _, out, _, is_in = mats[m]
        (_, nr), (c, nc) = region(is_in, color, 0)[0]
        return dict(batch=(m, color), whole=out.at[pl.ds(0, nr * (3 if color == "x" else 12)), pl.ds(c, nc)])

    def reach(m, color):
        src, _, _, is_in = mats[m]
        area = region(is_in, color, place[color])[0]
        for by in BOTH:
            links.send((m, "x1", color, by), src.at[pl.ds(pl.multiple_of(area[0][0], ROW), area[0][1]), pl.ds(*area[1])], at(m, x, area), peer("x", by), **group(m, color))

    def launch(m, color, off):
        is_in = mats[m][3]
        moved = at(m, spot("x", off), region(is_in, color, place[color])[0])
        for by in BOTH:
            links.send((m, "p1", color, off, by), moved, moved, peer(color, by), **group(m, color))

    def relay(m, color, by):
        is_in = mats[m][3]
        xb = spot("x", -by)
        areas = region(is_in, color, place[color])
        links.arrive((m, "x1", color, by), at(m, xb, areas[0]))
        part = at(m, xb, areas[1] if by == 1 else areas[PAIR])
        links.send((m, "x2", color), part, part, peer("x", by), **group(m, color))
        if color != "x":
            launch(m, color, -by)

    def far(m, color):
        is_in = mats[m][3]
        links.arrive((m, "x2", color), at(m, spot("x", PAIR), region(is_in, color, place[color])[0]))
        if color != "x":
            launch(m, color, PAIR)

    def pass_on(m, color, off, by):
        is_in = mats[m][3]
        xb = spot("x", off)
        areas = region(is_in, color, spot(color, -by))
        links.arrive((m, "p1", color, off, by), at(m, xb, areas[0]))
        part = at(m, xb, areas[1] if by == 1 else areas[PAIR])
        links.send((m, "p2", color, off), part, part, peer(color, by), **group(m, color))

    def close(m, color, off):
        is_in = mats[m][3]
        links.arrive((m, "p2", color, off), at(m, spot("x", off), region(is_in, color, spot(color, PAIR))[0]))

    def four(m):
        _, out, size, _ = mats[m]
        return out.at[pl.ds(0, SIDE * size)]

    def give(m, src, dst):
        links.send((m, "chip"), src, dst, twin, batch=(m, "chip"), whole=four(m))

    def hand(m, off):
        whole = block(m, spot("x", off), core)
        give(m, whole, whole)

    owns = []

    def begin():
        for m, (src, _, _, _) in enumerate(mats):
            copy = pltpu.make_async_copy(src, block(m, x, core), lsem.at[m])
            copy.start()
            owns.append(copy)
            give(m, src, block(m, x, core))

    def ready(m):
        owns[m].wait()
        links.arrive((m, "chip"), four(m))

    return begin, ready, peer, {"reach": reach, "relay": relay, "far": far, "pass": pass_on, "close": close, "hand": hand}


BF, F32 = jnp.bfloat16, jnp.float32


def product(a, b, contract=((1,), (0,))):
    return lax.dot_general(a, b, (contract, ((), ())), preferred_element_type=F32)


def lanes(start, size):
    return pl.ds(start if isinstance(start, int) else pl.multiple_of(start, LANE), size)


def layers_kernel(order, sc_ref, wi_ref, wo_ref, x_ref, dy_ref, freq_ref,
                  y_ref, gx_ref, hy_a, hy_b, hz_a, hz_b, mx_a, mx_b, yx_b, zy_b, zz_b, z_a, dy_a, sc_out, relay_m, relay_z,
                  wi, wo, z, om, h, hid, qr, kts, vsl, ksl, turned_q, turned_o, scores, dscores, pcat, dscat, cos_ref, sin_ref, turn_ref,
                  dot_heads, qt, dht, dkv, omt, ht, dyt, sc, gains, own_gain, gain_ref, load_sems, own_sems, send_sems, recv_sems,
                  share_send_sems, share_recv_sems):
    seq, dim = x_ref.shape
    ff = (wi.shape[PAIR] - dim - LANE) // PAIR
    position = chip_position()
    x, y, zc, core = position
    twin = device_at(x, y, zc, 1 - core)
    me = PAIR * x + core
    links, shared = Links(send_sems, recv_sems), Links(share_send_sems, share_recv_sems)
    stored = []
    spots, _ = around(position)
    h_out, m_out, y_out, z_out = {"y": (hy_a, hy_b), "z": (hz_a, hz_b)}, (mx_a, mx_b), {1: yx_b}, {(1, "y"): zy_b, (1, "z"): zz_b}
    middle = hid.at[1]
    begin, ready, peer, stages = gather_stages(links, position, wi_ref, wo_ref, wi, wo, load_sems)
    others = [(zc * SIDE + y, rem(me + k, ROW)) for k in range(1, ROW)]

    def spot(axis, o):
        return spots[axis, o % SIDE]

    def device(axis, o, index):
        moved = {"x": x, "y": y, "z": zc, axis: spot(axis, o)}
        return device_at(moved["x"], moved["y"], moved["z"], index)

    own_gain[ALL] = jnp.zeros(own_gain.shape, F32)
    count = sc_ref.shape[1]
    for f in range(ROW):
        @pl.when(me == f)
        def _():
            own_gain[0:PAIR, f * count:(f + 1) * count] = sc_ref[ALL].astype(F32)
    announce(others + [device(axis, o, index) for axis in "yz" for o in AROUND for index in range(PAIR)])
    begin()
    for k, far in enumerate(others):
        links.send(("sc",), own_gain, gains.at[me], far, batch=("sc",), whole=gains.at[pl.ds(0, 7)])

    def keep(src, dst):
        copy = pltpu.make_async_copy(src, dst, own_sems.at[len(stored)])
        copy.start()
        stored.append(copy)

    def tokens(axis, o, index):
        return pl.ds(pl.multiple_of((PAIR * spot(axis, o) + index) * seq, seq), seq)

    def columns(axis, o):
        size = z.shape[PAIR] // ROW
        return lanes(((0 if axis == "y" else SIDE) + spot(axis, o)) * size, size)

    def several(batch, ref, n):
        whole = ref.at[pl.ds(0, n * seq)] if batch[0][0] in "yz" else ref.at[(slice(None),) * (len(ref.shape) - 1) + (pl.ds(0, n * seq),)]
        return dict(batch=batch, whole=whole)

    def send_h(l, axis):
        out = h_out[axis][l].at[:, :, tokens(axis, 0, core)]
        for by in BOTH:
            for index in range(PAIR):
                shared.send(("h", l, axis, by), ht.at[l, :, index], out, device(axis, by, index), lane=core, **several(("h", l, axis), h_out[axis][l], 7))
        shared.send(("h", l, axis), ht.at[l, :, 1 - core], out, twin, **several(("h", l, axis), h_out[axis][l], 7))
        keep(ht.at[l, :, core], out)

    def pass_h(l, axis, by, index):
        out = h_out[axis][l]
        shared.arrive(("h", l, axis, by), out.at[:, :, tokens(axis, -by, index)], index)
        part = out.at[pl.ds(1 - by, PAIR), :, tokens(axis, -by, index)]
        shared.send(("h", l, axis), part, part, device(axis, by, core), **several(("h", l, axis), out, 7))

    def arrive_h(l):
        for axis in "yz":
            shared.arrive(("h", l, axis), h_out[axis][l].at[:, :, pl.ds(0, 3 * seq)])

    def row_block(l, o, index, part=None):
        size = omt.shape[1] // ROW
        start = (PAIR * spot("x", o) + index) * size
        if part is not None:
            size = size // PAIR
            start = start + part * size
        return omt.at[l, pl.ds(pl.multiple_of(start, 16), size)]

    def row_half(k):
        size = m_out[0].shape[0] // PAIR
        return pl.ds(k * size, size)

    def send_m(l):
        out = m_out[l].at[:, tokens("x", 0, core)]
        for k, by in enumerate(BOTH):
            for index in range(PAIR):
                shared.send(("mr", l, by), row_block(l, PAIR, index, k), relay_m.at[l, k, core], device("x", by, index), lane=core, **several(("m", l), m_out[l], 7))
        for by in BOTH:
            for index in range(PAIR):
                shared.send(("m", l), row_block(l, by, index), out, device("x", by, index), **several(("m", l), m_out[l], 7))
        shared.send(("m", l), row_block(l, 0, 1 - core), out, twin, **several(("m", l), m_out[l], 7))
        keep(row_block(l, 0, core), out)

    def pass_m(l, by, index):
        k = (1 - by) // PAIR
        shared.arrive(("mr", l, by), relay_m.at[l, k, index], index)
        shared.send(("m", l), relay_m.at[l, k, index], m_out[l].at[row_half(k), tokens("x", -by, index)], device("x", by, core),
                    **several(("m2", l), m_out[l], PAIR))

    def arrive_m(l):
        shared.arrive(("m", l), m_out[l].at[:, pl.ds(0, 7 * seq)])

    def token_half(axis, o, k):
        return pl.ds(pl.multiple_of((PAIR * spot(axis, o) + core) * seq + k * (seq // PAIR), seq // PAIR), seq // PAIR)

    def send_y(l):
        src, out = dy_ref, y_out[l].at[tokens("x", 0, core)]
        for by in BOTH:
            shared.send(("y", l, by), src, out, device("x", by, core), **several(("y", l), y_out[l], 7))
        shared.send(("y", l), src, out, twin, **several(("y", l), y_out[l], 7))
        keep(src, out)

    def pass_y(l, by):
        landed, part = y_out[l].at[tokens("x", -by, core)], y_out[l].at[token_half("x", -by, (1 - by) // PAIR)]
        shared.arrive(("y", l, by), landed)
        shared.send(("y2", l), part, part, device("x", by, core), **several(("y", l), y_out[l], 7))
        shared.send(("y", l), landed, landed, twin, **several(("y", l), y_out[l], 7))

    def far_y(l):
        landed = y_out[l].at[tokens("x", PAIR, core)]
        shared.arrive(("y2", l), landed)
        shared.send(("y", l), landed, landed, twin, **several(("y", l), y_out[l], 7))

    def arrive_y(l):
        shared.arrive(("y", l), y_out[l].at[pl.ds(0, SIDE * seq)])

    def push_z(l, axis, o, ready):
        out = z_out[l, axis].at[tokens(axis, 0, core)]
        batch = several(("z", l, axis), z_out[l, axis], ROW)

        def start():
            if o != PAIR:
                shared.send(("z", l, axis, o), z.at[l, :, columns(axis, o)], out, device(axis, o, core), **batch)
                return
            for k, by in enumerate(BOTH):
                shared.send(("zr", l, axis, by), z.at[l, pl.ds(k * (seq // PAIR), seq // PAIR), columns(axis, PAIR)], relay_z.at[l, "yz".index(axis), k],
                            device(axis, by, core), **batch)

        if ready is None:
            start()
        else:
            pl.when(ready)(start)

    def own_part(l, axis):
        out, mine = z_out[l, axis].at[tokens(axis, 0, core)], z.at[l, :, columns(axis, 0)]
        shared.send(("z", l, axis), mine, out, twin, **several(("z", l, axis), z_out[l, axis], ROW))
        keep(mine, out)

    def send_z(l, axis):
        for o in (PAIR, 1, -1):
            push_z(l, axis, o, spot(axis, o) != 0 if axis == "y" else None)
        if axis == "z":
            own_part(l, axis)

    def rest_z(l):
        for o in (PAIR, 1, -1):
            push_z(l, "y", o, spot("y", o) == 0)
        own_part(l, "y")

    def pass_z(l, axis, by):
        k = (1 - by) // PAIR
        half = relay_z.at[l, "yz".index(axis), k]
        shared.arrive(("zr", l, axis, by), half)
        shared.send(("z2", l, axis), half, z_out[l, axis].at[token_half(axis, -by, k)], device(axis, by, core), **several(("z", l, axis), z_out[l, axis], ROW))

    def twin_z(l, axis, by):
        landed = z_out[l, axis].at[tokens(axis, -by, core)]
        shared.arrive(("z", l, axis, by), landed)
        shared.send(("z", l, axis), landed, landed, twin, **several(("z", l, axis), z_out[l, axis], ROW))

    def far_z(l, axis):
        landed = z_out[l, axis].at[tokens(axis, PAIR, core)]
        shared.arrive(("z2", l, axis), landed)
        shared.send(("z", l, axis), landed, landed, twin, **several(("z", l, axis), z_out[l, axis], ROW))

    def arrive_z(l, axis):
        shared.arrive(("z", l, axis), z_out[l, axis].at[pl.ds(0, SIDE * seq)])

    def send_scale(l):
        for far in others:
            shared.send(("scale", l), sc.at[l], sc_out.at[l, me], far, batch=("scale", l), whole=sc_out.at[l, pl.ds(0, 7)])
        keep(sc.at[l], sc_out.at[l, me])

    def arrive_scale(l):
        shared.arrive(("scale", l), sc_out.at[l, pl.ds(0, 7)])

    gains[me] = own_gain[ALL]
    z[:, :, wi.shape[PAIR]:] = jnp.zeros((PAIR, seq, z.shape[PAIR] - wi.shape[PAIR]), BF)
    entry = (x_ref, hid.at[0])
    angle = lax.broadcasted_iota(jnp.int32, (seq, LANE), 0).astype(F32) * freq_ref[0:1]
    for half in range(PAIR):
        cos_ref[:, LANE * half:LANE * (half + 1)] = jnp.cos(angle)
        sin_ref[:, LANE * half:LANE * (half + 1)] = jnp.sin(angle)
    lane = lax.broadcasted_iota(jnp.int32, turn_ref.shape, 1)
    down = lax.broadcasted_iota(jnp.int32, turn_ref.shape, 0) - lane
    low = rem(lane, HEAD) < BAND
    turn_ref[ALL] = jnp.where(low & (down == BAND), -1.0, jnp.where(jnp.logical_not(low) & (down == -BAND), 1.0, ZERO)).astype(BF)
    kts[ALL] = jnp.zeros(kts.shape, BF)
    pcat[ALL] = jnp.zeros(pcat.shape, BF)
    dscat[ALL] = jnp.zeros(dscat.shape, BF)

    def normalise(l, src):
        @pl.loop(0, seq // BAND, unroll=SIDE)
        def _(r):
            rows = pl.ds(pl.multiple_of(r * BAND, BAND), BAND)
            v = src[rows].astype(F32)
            v = v - jnp.mean(v, axis=-1, keepdims=True)
            var = jnp.mean(v * v, axis=-1, keepdims=True)
            h[l, rows] = (v * lax.rsqrt(var + 1e-6) * gain_ref[l:l + 1]).astype(BF)

    def project(l):
        strip = wi.shape[PAIR] // 5

        @pl.loop(0, 5)
        def _(i):
            at = lanes(i * strip, strip)
            z[l, :, at] = product(h[l], wi[l, :, at]).astype(BF)

    def heads(l):
        cos, sin = cos_ref[ALL], sin_ref[ALL]
        for g in range(dim // WIDE):
            q = z[l, :, g * WIDE:(g + 1) * WIDE]
            qr[l, :, g * WIDE:(g + 1) * WIDE] = ((q.astype(F32) * cos + product(q, turn_ref[ALL]) * sin) * 0.125).astype(BF)
        kv = z[l, :, dim:dim + LANE]
        turned = kv.astype(F32) * cos[:, :LANE] + product(kv, turn_ref[:LANE, :LANE]) * sin[:, :LANE]
        first = lax.broadcasted_iota(jnp.int32, turned.shape, 1) < HEAD
        key_lo = jnp.where(first, turned, ZERO)
        val_hi = jnp.where(first, ZERO, kv.astype(F32))
        return key_lo, pltpu.roll(key_lo, HEAD, 1), pltpu.roll(val_hi, HEAD, 1), val_hi

    def slot_rows(ref, lo, hi):
        zero = jnp.zeros((seq, LANE), BF)
        lo, hi = lo.astype(BF), hi.astype(BF)
        for i, (left, right) in enumerate(((lo, zero), (hi, zero), (zero, lo), (zero, hi))):
            ref[i * seq:(i + 1) * seq, :LANE] = left
            ref[i * seq:(i + 1) * seq, LANE:] = right

    def slot_cols(ref, lo):
        flat = lo.T[:HEAD].astype(BF)
        for i in range(SIDE):
            ref[HEAD * i:HEAD * (i + 1), i * seq:(i + 1) * seq] = flat

    def chances(i, half):
        at = slice(LANE * half, LANE * (half + 1))
        blocks = [pl.ds(pl.multiple_of(i * seq + LANE * k, LANE), LANE) for k in range(half + 1)]
        s = [scores[keys, at] for keys in blocks]
        lower = lax.broadcasted_iota(jnp.int32, s[-1].shape, 1) >= lax.broadcasted_iota(jnp.int32, s[-1].shape, 0)
        s[-1] = jnp.where(lower, s[-1], -1e30)
        top = functools.reduce(jnp.maximum, [jnp.max(v, axis=0, keepdims=True) for v in s])
        e = [jnp.exp(v - top) for v in s]
        scale = 1.0 / sum(jnp.sum(v, axis=0, keepdims=True) for v in e)
        return at, [(keys, v * scale) for keys, v in zip(blocks, e)]

    def attend(l):
        key_lo, key_hi, val_lo, _ = heads(l)
        slot_rows(ksl, key_lo, key_hi)
        slot_cols(kts, val_lo)
        flip(lambda at: qr[l, :, lanes(at, WIDE)], qt, dim)

        @pl.loop(0, dim // WIDE)
        def _(g):
            rows = pl.ds(pl.multiple_of(g * WIDE, WIDE), WIDE)
            scores[ALL] = product(ksl[ALL], qt[rows])

            @pl.loop(0, SIDE)
            def _(i):
                for half in range(PAIR):
                    at, blocks = chances(i, half)
                    for keys, p in blocks:
                        pcat[keys, at] = p.astype(BF)
            flat = product(kts[ALL], pcat[ALL]).astype(BF)
            omt[l, rows] = flat
            om[:, lanes(g * WIDE, WIDE)] = flat.T

    def mlp(l):
        @pl.loop(0, seq // BAND)
        def _(r):
            rows = pl.ds(pl.multiple_of(r * BAND, BAND), BAND)

            @pl.loop(0, ff // STRIP)
            def _(i):
                gate = z[l, rows, lanes(dim + LANE + i * STRIP, STRIP)].astype(F32)
                up = z[l, rows, lanes(dim + LANE + ff + i * STRIP, STRIP)].astype(F32)
                om[rows, lanes(dim + i * STRIP, STRIP)] = (gate * jax.nn.sigmoid(gate) * up).astype(BF)

    def put_out(l, dst):
        for n in range(dim // WIDE):
            cols = slice(n * WIDE, (n + 1) * WIDE)
            total = product(om[ALL], wo[l, :, cols])
            dst[:, cols] = (entry[l][:, cols].astype(F32) + total).astype(BF)

    def flip(src, dst, width, first=0):
        @pl.loop(first // WIDE, width // WIDE)
        def _(i):
            dst[pl.ds(pl.multiple_of(i * WIDE, WIDE), WIDE)] = src(i * WIDE).T

    upstream = (middle, dy_ref)

    def back_out(l):
        dy = upstream[l]
        flip(lambda at: dy[:, lanes(at, WIDE)], dyt, dim)

        @pl.loop(0, wo.shape[1] // dim)
        def _(n):
            rows = pl.ds(pl.multiple_of(n * dim, dim), dim)
            part = product(wo[l, rows], dyt[ALL]).astype(BF)
            om[:, lanes(n * dim, dim)] = part.T

            @pl.when(n == 0)
            def _():
                dot_heads[ALL] = part

    def back_mlp(l):
        @pl.loop(0, seq // BAND)
        def _(r):
            rows = pl.ds(pl.multiple_of(r * BAND, BAND), BAND)

            @pl.loop(0, ff // STRIP)
            def _(i):
                gate_at, up_at = lanes(dim + LANE + i * STRIP, STRIP), lanes(dim + LANE + ff + i * STRIP, STRIP)
                gate, up = z[l, rows, gate_at].astype(F32), z[l, rows, up_at].astype(F32)
                d = om[rows, lanes(dim + i * STRIP, STRIP)].astype(F32)
                sig = jax.nn.sigmoid(gate)
                du = d * up
                z[l, rows, gate_at] = (du * sig + du * gate * (sig * (1.0 - sig))).astype(BF)
                z[l, rows, up_at] = (d * (gate * sig)).astype(BF)

    def back_heads(l):
        key_lo, key_hi, val_lo, val_hi = heads(l)
        slot_rows(ksl, key_lo, key_hi)
        slot_rows(vsl, val_lo, val_hi)
        slot_cols(kts, key_lo)
        dkv[ALL] = jnp.zeros(dkv.shape, F32)
        flip(lambda at: qr[l, :, lanes(at, WIDE)], qt, dim)
        for at in range(0, dim, LANE):
            pair = slice(at, at + LANE)
            turned_q[:, pair] = pltpu.roll(qr[l, :, pair].astype(F32), HEAD, 1).astype(BF)
            turned_o[:, pair] = pltpu.roll(om[:, pair].astype(F32), HEAD, 1).astype(BF)

    def back_quad(l):
        @pl.loop(0, dim // WIDE)
        def _(g):
            quad(l, g)

    def quad(l, g):
        cols = pl.ds(pl.multiple_of(g * WIDE, WIDE), WIDE)
        scores[ALL] = product(ksl[ALL], qt[cols])
        dscores[ALL] = product(vsl[ALL], dot_heads[cols])

        @pl.loop(0, SIDE)
        def _(i):
            for half in range(PAIR):
                at, blocks = chances(i, half)
                given = [p * dscores[keys, at].astype(BF).astype(F32) for keys, p in blocks]
                total = sum(jnp.sum(v, axis=0, keepdims=True) for v in given)
                for (keys, p), v in zip(blocks, given):
                    pcat[keys, at] = p.astype(BF)
                    dscat[keys, at] = (v - p * total).astype(BF)
        dq = product(kts[ALL], dscat[ALL]).astype(BF).T
        back = dq.astype(F32) * cos_ref[ALL] - product(dq, turn_ref[ALL]) * sin_ref[ALL]
        z[l, :, cols] = (back * 0.125).astype(BF)
        for i in range(SIDE):
            keys, pair = slice(i * seq, (i + 1) * seq), lanes(g * WIDE + i // PAIR * LANE, LANE)
            even = i % PAIR == 0
            dkv[0] += product(dscat[keys], qr[l, :, pair] if even else turned_q[:, pair])
            dkv[1] += product(pcat[keys], turned_o[:, pair] if even else om[:, pair])

    def back_keys(l):
        dk = dkv[0].astype(BF)
        turned = dk.astype(F32) * cos_ref[:, :LANE] - product(dk, turn_ref[:LANE, :LANE]) * sin_ref[:, :LANE]
        first = lax.broadcasted_iota(jnp.int32, turned.shape, 1) < HEAD
        z[l, :, dim:dim + LANE] = jnp.where(first, turned, dkv[1]).astype(BF)

    def back_in(l, half):
        width = wi.shape[PAIR] // 5
        at = slice(PAIR * half * width, (PAIR + 3 * half) * width)
        part = product(wi[l, :, at], z[l, :, at], ((1,), (1,)))
        dht[ALL] = dht[ALL] + part if half else part

    def back_norm(l):
        dy, dst = upstream[l], (gx_ref, middle)[l]
        for i in range(dim // WIDE):
            cols = slice(i * WIDE, (i + 1) * WIDE)
            h[l, :, cols] = dht[cols].T.astype(BF)
        sc[l] = jnp.zeros(sc.shape[1:], F32)

        @pl.loop(0, seq // BAND, unroll=SIDE)
        def _(r):
            rows = pl.ds(pl.multiple_of(r * BAND, BAND), BAND)
            v = entry[l][rows].astype(F32)
            v = v - jnp.mean(v, axis=-1, keepdims=True)
            scale = lax.rsqrt(jnp.mean(v * v, axis=-1, keepdims=True) + 1e-6)
            hat = v * scale
            d = h[l, rows].astype(F32)
            each = (d * hat).reshape(SIDE, ROW, dim)
            sc[l] += (each[0] + each[1]) + (each[PAIR] + each[3])
            d = d * gain_ref[l:l + 1]
            d = scale * (d - jnp.mean(d, axis=-1, keepdims=True) - hat * jnp.mean(d * hat, axis=-1, keepdims=True))
            dst[rows] = (dy[rows].astype(F32) + d.astype(BF).astype(F32)).astype(BF)

    def do_norm(l):
        if l == 0:
            links.arrive(("sc",), gains.at[pl.ds(0, 7)])
            gain_ref[ALL] = jnp.sum(gains[ALL], axis=0)
        normalise(l, entry[l])
        for i in range(dim // WIDE):
            flat = h[l, :, i * WIDE:(i + 1) * WIDE].T
            size = ht.shape[3]
            for b in range(ROW):
                lo, hi = max(b * size, i * WIDE), min((b + 1) * size, (i + 1) * WIDE)
                if lo < hi:
                    ht[l, b // PAIR, b % PAIR, lo - b * size:hi - b * size] = flat[lo - i * WIDE:hi - i * WIDE]

    def do_project(l):
        ready(PAIR * l)
        project(l)

    def do_mlp(l):
        mlp(l)
        flip(lambda at: om[:, lanes(at, WIDE)], omt.at[l], om.shape[1], dim)

    def do_put(l):
        ready(PAIR * l + 1)
        put_out(l, hid.at[0] if l == 0 else y_ref)

    stages.update(
        norm=do_norm, project=do_project, attend=attend, mlp=do_mlp, put=do_put, back_out=back_out, back_mlp=back_mlp, back_heads=back_heads,
        back_quad=back_quad, back_keys=back_keys, back_in=back_in, back_norm=back_norm, send_h=send_h, pass_h=pass_h, send_m=send_m,
        pass_m=pass_m, send_y=send_y, pass_y=pass_y, far_y=far_y, send_z=send_z, rest_z=rest_z, pass_z=pass_z, twin_z=twin_z, far_z=far_z,
        send_scale=send_scale, own_z=lambda: keep(z.at[0], z_a), own_y=lambda: keep(middle, dy_a))
    for kind, *task in order:
        stages[kind](*task)
    for l in range(PAIR):
        arrive_h(l)
        arrive_m(l)
        arrive_scale(l)
    arrive_y(1)
    for l, axis in z_out:
        arrive_z(l, axis)
    for copy in stored:
        copy.wait()
    shared.drain()
    links.drain()


def run_layers(x, dy, scale, w_in, w_out, freq, starts=(ZERO, 10.0, 20.0, 30.0)):
    seq, dim = x.shape
    proj, cat = w_in.shape[PAIR], ROW * w_out.shape[1]
    wide = proj + LANE
    hbm, vmem = pl.BlockSpec(memory_space=pltpu.HBM), pl.BlockSpec(memory_space=pltpu.VMEM)
    out = lambda *shape, dtype=BF: jax.ShapeDtypeStruct(shape, dtype)
    buffer = lambda *shape, dtype=BF: pltpu.VMEM(shape, dtype)
    sem = pltpu.SemaphoreType.DMA
    line = ROW * seq
    return pl.pallas_call(
        functools.partial(layers_kernel, layers_order(*w_in.shape[1:], *w_out.shape[1:], seq, starts)),
        out_shape=(out(seq, dim), out(seq, dim), *[out(SIDE, dim // ROW, line)] * SIDE, *[out(cat // ROW, line)] * PAIR, out(line, dim),
                   *[out(line, wide // ROW)] * PAIR, out(seq, wide), out(seq, dim), out(PAIR, ROW, ROW, dim, dtype=F32),
                   out(PAIR, PAIR, PAIR, cat // 16, seq), out(PAIR, PAIR, PAIR, seq // PAIR, wide // ROW)),
        in_specs=[vmem, hbm, hbm] + [vmem] * 3,
        out_specs=[vmem] * PAIR + [hbm] * 14,
        scratch_shapes=[
            buffer(PAIR, dim, proj), buffer(PAIR, cat, dim), buffer(PAIR, seq, wide), buffer(seq, cat), buffer(PAIR, seq, dim),
            buffer(PAIR, seq, dim), buffer(PAIR, seq, dim),
            buffer(WIDE, SIDE * seq), buffer(SIDE * seq, WIDE), buffer(SIDE * seq, WIDE), buffer(seq, dim), buffer(seq, dim),
            buffer(SIDE * seq, seq, dtype=F32), buffer(SIDE * seq, seq, dtype=F32), buffer(SIDE * seq, seq), buffer(SIDE * seq, seq),
            buffer(seq, WIDE, dtype=F32), buffer(seq, WIDE, dtype=F32), buffer(WIDE, WIDE),
            buffer(dim, seq), buffer(dim, seq), buffer(dim, seq, dtype=F32), buffer(PAIR, seq, LANE, dtype=F32),
            buffer(PAIR, cat, seq), buffer(PAIR, SIDE, PAIR, dim // ROW, seq), buffer(dim, seq), buffer(PAIR, ROW, dim, dtype=F32),
            buffer(ROW, ROW, dim, dtype=F32), buffer(ROW, dim, dtype=F32), buffer(ROW, dim, dtype=F32),
            sem((SIDE,)), sem((13,)), sem((15,)), sem((107,)), sem((13,)), sem((HEAD,)),
        ],
        compiler_params=pltpu.CompilerParams(collective_id=PAIR, has_side_effects=True, vmem_limit_bytes=67043328),
        name="run_layers",
    )(scale, w_in, w_out, x, dy, freq)


PARTS = (("i", "x", "z", "y", 0, STRIP), ("i", "x", "z", "y", STRIP, 384), ("i", "x", "y", "z", 0, STRIP), ("i", "x", "y", "z", STRIP, 384),
         ("o", "y", "z", "y", 0, 384), ("o", "z", "y", "z", 384, 384))


def reduce_order(rows, rows_b, starts):
    rate = 11650.0
    tasks = []
    sizes = {"y": WIDE * 896 / (PAIR * rate), "z": WIDE * 896 / (PAIR * rate), "x": WIDE * 768 / (PAIR * rate)}
    for axis in "yzx":
        tasks.append((("swap", axis), (0, 0), starts[PAIR] if axis == "x" else ZERO, [], [], [((axis, by), sizes[axis] * n) for by, n in ((1, 1), (-1, 1), (1, PAIR))], 0.3))
        for i, o in enumerate(AROUND):
            tasks.append((("near", axis, o), (0, PAIR), ZERO, [(("swap", axis), i)], [], [("chip", 1.6)], 0.2))
    tasks.append((("fetch", 0), (5, 0), ZERO, [], [("make", 1, len(PARTS) - 1)], [], 0.2))
    for l in (1, 0):
        late = 1 - l
        for c, (kind, first, then, last, at, width) in enumerate(PARTS):
            needs, cost = [], 1.6 * width / STRIP
            if l == 0:
                needs = [(("near", last if kind == "i" else "x", o), 0) for o in AROUND]
            tasks.append((("make", l, c), (9 * late, c), starts[late], needs, [] if l else [("fetch", 0)], [], cost))
            full = SIDE * SIDE * (rows if kind == "i" else rows_b) * width / rate
            sends = [[((first, by), full / ROW) for by in BOTH], [((first, by), full / SIDE) for by in BOTH],
                     [((then, o), full / 16) for o in (1, -1, 1)], []]
            piece = full / 16
            sends += [[((then, by), piece) for by in BOTH], [((then, 1 - PAIR * (c % PAIR)), piece)], [((last, by), SIDE * piece) for by in BOTH],
                      [((last, by), PAIR * piece) for by in BOTH], []]
            for s in range(9):
                task = ("sum", l, c, s)
                needs = [(("sum", l, c, s - 1), k) for k in range(len(sends[s - 1]))] if s else []
                tasks.append((task, (late, -s), ZERO, needs, [("make", l, c)] if s == 0 else [("sum", l, c, s - 1)], sends[s], 0.3))
    return plan(tasks)


def reduce_kernel(order, *refs):
    hy, hz, mx = refs[0:PAIR], refs[PAIR:SIDE], refs[SIDE:6]
    yx1, zy1, zz1, z0, y0, sc = refs[6:12]
    oa, ob = refs[12:14]
    n = len(PARTS)
    total, half, full, small, front = (refs[14 + k * n:14 + (k + 1) * n] for k in range(5))
    (hbuf, zbuf, mbuf, ybuf, scbuf, ssem, rsem, isem, osem) = refs[14 + 5 * n:]
    position = chip_position()
    x, y, zc, core = position
    place = {"x": x, "y": y, "z": zc}
    twin = device_at(x, y, zc, 1 - core)
    spots, peers = around(position)

    def spot(axis, o):
        return spots[axis, o % SIDE]

    def peer(axis, o):
        return peers[axis, o % SIDE]

    seq, wide = z0.shape
    own = wide // ROW
    loads, moving = {}, []

    def load(key, src, dst):
        copy = pltpu.make_async_copy(src, dst, isem.at[len(moving)])
        moving.append(key)
        copy.start()
        loads[key] = copy

    def fetch(l):
        if l:
            load(("z", 1, "y"), zy1, zbuf.at[1, 0])
        load(("h", l, "y"), hy[l], hbuf.at[l, 0])
        if l:
            load(("z", 1, "z"), zz1, zbuf.at[1, 1])
        load(("h", l, "z"), hz[l], hbuf.at[l, 1])
        load(("m", l), mx[l], mbuf.at[l])
        if l:
            load(("y", 1), yx1, ybuf.at[1])
        load(("s", l), sc.at[l], scbuf.at[l])

    fetch(1)
    done = set()

    def loaded(*keys):
        for key in keys:
            if key not in done:
                loads[key].wait()
                done.add(key)

    announce([peer(axis, o) for axis in "xyz" for o in AROUND] + [twin])
    links = Links(ssem, rsem)

    def columns(axis, o):
        return lanes(((0 if axis == "y" else SIDE) + spot(axis, o)) * own, own)

    def tokens(axis, o, index):
        return pl.ds(pl.multiple_of((PAIR * spot(axis, o) + index) * seq, seq), seq)

    def target(axis):
        return ybuf.at[0] if axis == "x" else zbuf.at[0, "yz".index(axis)]

    def seven(axis):
        return dict(batch=("swap", axis), whole=target(axis).at[pl.ds(0, 7 * seq)])

    def swap(axis):
        def part(o):
            return y0 if axis == "x" else z0.at[:, columns(axis, o)]

        mine = target(axis).at[tokens(axis, 0, core)]
        for o in AROUND:
            links.send(("swap", axis, o), part(o), mine, peer(axis, o), **seven(axis))
        links.send(("near", axis), part(0), mine, twin, **seven(axis))
        load(("own", axis), part(0), mine)

    def near(axis, o):
        landed = target(axis).at[tokens(axis, -o, core)]
        links.arrive(("swap", axis, o), landed)
        links.send(("near", axis), landed, landed, twin, **seven(axis))

    def joined(axis):
        if axis not in done:
            done.add(axis)
            loaded(("own", axis))
            links.arrive(("near", axis), target(axis).at[pl.ds(0, SIDE * seq)])

    def make(l, c):
        kind, first, then, last, at, width = PARTS[c]
        if kind == "i":
            i = "yz".index(last)
            loaded(("h", l, last))
            if l:
                loaded(("z", l, last))
            else:
                joined(last)
            size = total[c].shape[3]
            for lo in range(0, width, WIDE):
                hi = min(width, lo + WIDE)
                part = product(hbuf[l, i].reshape(-1, hbuf.shape[-1]), zbuf[l, i, :, at + lo:at + hi])
                for r in range(16):
                    total[c][l, r // SIDE, r % SIDE, :, lo:hi] = part[r * size:(r + 1) * size]
            return
        loaded(("m", l), ("s", l))
        if l:
            loaded(("y", l))
        else:
            joined("x")
        part = product(mbuf[l], ybuf[l, :, at:at + width])
        size = total[c].shape[3]

        def put(r, value):
            total[c][(l, r // SIDE, r % SIDE) if first == "y" else (l, r % SIDE, r // SIDE)] = value

        for r in range(part.shape[0] // size):
            put(r, part[r * size:(r + 1) * size])
        gain = jnp.sum(jnp.sum(scbuf[l, :, :, at:at + width], axis=0), axis=0, keepdims=True)
        row = lax.broadcasted_iota(jnp.int32, (size, width), 0)
        put(15, jnp.where(row == 0, gain, ZERO))

    def area(l, c, o, whole):
        kind, first, then, last, at, width = PARTS[c]
        inner = (spot(then, whole) if isinstance(whole, int) else whole)
        outer = spot(last, o)
        if kind == "i":
            cols = lanes(((0 if last == "y" else SIDE) + outer) * own + at, width)
            return oa.at[l, inner, :, cols]
        cols = pl.ds(at, width)
        return ob.at[l, outer, inner, :, cols] if last == "y" else ob.at[l, inner, outer, :, cols]

    def add(l, c, s):
        kind, first, then, last, at, width = PARTS[c]
        t = total[c].at[l]
        way = 1 - PAIR * (c % PAIR)
        sums = dict(batch=(l, c, 0), whole=t)
        wide_ones = dict(batch=(l, c, 1), whole=t.at[pl.ds(0, 3)])
        narrow = dict(batch=(l, c, PAIR), whole=t.at[0, pl.ds(0, PAIR)])
        if s == 0:
            far = t.at[spot(first, PAIR)]
            for k, by in enumerate(BOTH):
                links.send((l, c, "half"), far.at[pl.ds(PAIR * k, PAIR)], half[c].at[l, k], peer(first, by), **sums)
        elif s == 1:
            links.arrive((l, c, "half"), half[c].at[l])
            for k, by in enumerate(BOTH):
                mine = t.at[spot(first, by)]
                add_into(mine.at[pl.ds(PAIR * k, PAIR)], half[c].at[l, k])
                links.send((l, c, "full"), mine, full[c].at[l, k], peer(first, by), **sums)
        elif s == PAIR:
            mine = t.at[spot(first, 0)]
            links.arrive((l, c, "full"), full[c].at[l])
            for k in range(PAIR):
                add_into(mine, full[c].at[l, k])
            for k, o in enumerate(AROUND):
                links.send((l, c, "small"), mine.at[spot(then, o)], small[c].at[l, k], peer(then, o), **wide_ones)
        elif s == 3:
            links.arrive((l, c, "small"), small[c].at[l])
            mine = t.at[spot(first, 0), spot(then, 0)]
            front[c][l] = (mine[ALL] + small[c][l, 0]) + (small[c][l, 1] + small[c][l, PAIR])
        elif s == SIDE:
            src, dst = front[c].at[l], area(l, c, 0, 0)
            for by in BOTH:
                links.send((l, c, "a1"), src, dst, peer(then, by), **narrow)
            copy = pltpu.make_async_copy(src, dst, osem.at[l, c])
            copy.start()
            loads["front", l, c] = copy
        elif s == 5:
            links.arrive((l, c, "a1"), t.at[0, pl.ds(0, PAIR)])
            landed = area(l, c, 0, -way)
            links.send((l, c, "b1"), landed, landed, peer(then, way), **wide_ones)
        elif s == 6:
            loaded(("front", l, c))
            links.arrive((l, c, "b1"), area(l, c, 0, PAIR))
            line = area(l, c, 0, slice(None))
            for by in BOTH:
                links.send((l, c, "a2"), line, line, peer(last, by), **wide_ones)
        elif s == 7:
            links.arrive((l, c, "a2"), t.at[pl.ds(0, PAIR)])
            for k, by in enumerate(BOTH):
                part = area(l, c, -by, pl.ds(PAIR * k, PAIR))
                links.send((l, c, "a3"), part, part, peer(last, by), **sums)
        else:
            links.arrive((l, c, "a3"), area(l, c, PAIR, slice(None)))

    stages = {"swap": swap, "near": near, "fetch": fetch, "make": make, "sum": add}
    for kind, *task in order:
        stages[kind](*task)
    links.drain()


def add_into(dst, src):
    @pl.loop(0, dst.shape[0])
    def _(i):
        if len(dst.shape) == SIDE:
            for j in range(dst.shape[1]):
                dst[i, j] += src[i, j]
        else:
            dst[i] += src[i]


def around(position):
    place, core = dict(zip("xyz", position)), position[3]
    spots = {(axis, o): step(place[axis], o) for axis in "xyz" for o in range(SIDE)}
    peers = {}
    for axis in "xyz":
        for o in range(1, SIDE):
            moved = {**place, axis: spots[axis, o]}
            peers[axis, o] = device_at(moved["x"], moved["y"], moved["z"], core)
    return spots, peers


def reduce_gradients(operands, starts=(ZERO, ZERO, ZERO)):
    hbm = pl.BlockSpec(memory_space=pltpu.HBM)
    h_rows, m_rows, y_cols, z_cols, z_own, y_own, scale_parts = operands
    part, part_b = h_rows[0].shape[1] // SIDE, (m_rows[0].shape[0] + BAND) // 16
    (line, dim), wide = y_cols.shape, z_own.shape[1]
    out = lambda *shape: jax.ShapeDtypeStruct(shape, F32)
    sem = pltpu.SemaphoreType.DMA

    def buffers(*lead):
        return [pltpu.VMEM((PAIR, *lead, part if e[0] == "i" else part_b, e[5]), F32) for e in PARTS]

    return pl.pallas_call(
        functools.partial(reduce_kernel, reduce_order(part, part_b, starts)),
        out_shape=(out(PAIR, SIDE, part, wide), out(PAIR, SIDE, SIDE, part_b, dim)),
        in_specs=[hbm] * 12,
        out_specs=[hbm] * PAIR,
        scratch_shapes=[
            *buffers(SIDE, SIDE), *buffers(PAIR, PAIR), *buffers(PAIR, SIDE), *buffers(3), *buffers(),
            pltpu.VMEM((PAIR, PAIR, *h_rows[0].shape), BF), pltpu.VMEM((PAIR, PAIR, line, wide // ROW), BF), pltpu.VMEM((PAIR, *m_rows[0].shape), BF),
            pltpu.VMEM((PAIR, line, dim), BF), pltpu.VMEM(scale_parts.shape, F32),
            sem((39,)), sem((96,)), sem((14,)), sem((PAIR, len(PARTS))),
        ],
        compiler_params=pltpu.CompilerParams(collective_id=1, has_side_effects=True, vmem_limit_bytes=67043328),
        name="reduce_gradients",
    )(*h_rows, *m_rows, y_cols, *z_cols, z_own, y_own, scale_parts)


def solution(mesh):
    fsdp_size = mesh.shape["fsdp"]
    batch_spec = P(("dp", "fsdp"), None, None)
    scale_spec = P(None, "fsdp")
    weight_spec = P(None, "fsdp", None)

    def device_step(x_in, grad_y, norm_scale, w_in, w_out):
        n_layers = w_in.shape[0]
        seq_len, model_dim = x_in.shape[1:]
        proj_dim = w_in.shape[PAIR]
        ff_dim = w_out.shape[1] * fsdp_size - model_dim
        head_dim = (proj_dim - model_dim - PAIR * ff_dim) // PAIR
        rows, rows_out = norm_scale.shape[1], w_out.shape[1]
        half_dim = head_dim // PAIR
        freq = 10000.0 ** (-np.arange(half_dim, dtype=np.float32) * 2.0 / head_dim)
        freq = jnp.asarray(np.tile(freq.astype(np.float32), (ROW, LANE // half_dim)))
        hidden, grad_hidden, *rest = run_layers(x_in[0], grad_y[0], norm_scale, w_in, w_out, freq)
        in_sums, out_sums = reduce_gradients((rest[0:SIDE], rest[SIDE:6], rest[6], rest[7:9], rest[9], rest[10], rest[11]))
        in_grads = in_sums.reshape(n_layers, rows, -1)[:, :, :proj_dim]
        out_rows = out_sums.reshape(n_layers, -1, model_dim)
        scale_grads = lax.dynamic_slice(out_rows[:, rows_out], (0, lax.axis_index("fsdp") * rows), (n_layers, rows))
        out_grads = out_rows[:, :rows_out]
        return hidden[None], grad_hidden[None], scale_grads, in_grads, out_grads

    return jax.shard_map(
        device_step,
        mesh=mesh,
        in_specs=(batch_spec, batch_spec, scale_spec, weight_spec, weight_spec),
        out_specs=(batch_spec, batch_spec, scale_spec, weight_spec, weight_spec),
        check_vma=False,
    )
```

```python
import functools
import jax
import jax.numpy as jnp
import numpy as np
from jax import lax
from jax.experimental import pallas as pl
from jax.experimental.pallas import tpu as pltpu
from jax.sharding import PartitionSpec as P

MESH_ID = pl.DeviceIdType.MESH
BOTH = (1, -1)
AROUND = (1, -1, 2)
PARTS = (True, False)
ALL, ZERO = ..., 0.0
LANE, WIDE, STRIP, HEAD = 128, 256, 512, 64
ROW, BAND, SIDE, PAIR = 8, 32, 4, 2


class Links:
    def __init__(self, send_sems, recv_sems):
        self.send_sems, self.recv_sems = send_sems, recv_sems
        self.slots, self.batches, self.sent, self.count = {}, {}, {}, 0

    def _landing(self, key, lane):
        if key not in self.slots:
            self.slots[key] = self.count
            self.count += 1 if lane is None else PAIR
        return self.recv_sems.at[self.slots[key] + (0 if lane is None else lane)]

    def send(self, key, src, dst, device, landing=None, whole=None, batch=None, lane=None):
        leaving = self.batches.setdefault(batch or key, len(self.batches))
        copy = pltpu.make_async_remote_copy(
            src_ref=src, dst_ref=dst, send_sem=self.send_sems.at[leaving], recv_sem=self._landing(landing or key, lane),
            device_id=device, device_id_type=MESH_ID)
        copy.start()
        self.sent[batch or key] = (src if whole is None else whole, leaving)

    def arrive(self, key, landed, lane=None):
        pltpu.make_async_copy(landed, landed, self._landing(key, lane)).wait()

    def drain(self):
        for left, leaving in self.sent.values():
            pltpu.make_async_copy(left, left, self.send_sems.at[leaving]).wait()
        self.sent.clear()


def rem(a, n):
    return a % n if isinstance(a, int) else lax.rem(a, n)


def chip_position():
    f, d = lax.axis_index("fsdp"), lax.axis_index("dp")
    return f // PAIR, rem(d, SIDE), d // SIDE, rem(f, PAIR)


def device_at(x, y, z, core):
    return (z * SIDE + y, x * PAIR + core)


def step(coord, by):
    return rem(coord + SIDE + by, SIDE)


def announce(devices):
    barrier = pltpu.get_barrier_semaphore()
    for device in devices:
        pl.semaphore_signal(barrier, inc=1, device_id=device, device_id_type=MESH_ID)
    pl.semaphore_wait(barrier, len(devices))


def plan(tasks, latency=2.5):
    free, landed, order, now = {}, {}, [], ZERO
    left = list(tasks)
    while left:
        best = None
        for place, (name, rank, start, needs, after, _, _) in enumerate(left):
            if all(n[0] in landed for n in needs) and all(n in landed for n in after):
                ready = max([start, now] + [landed[task][i] for task, i in needs])
                best = min(best or (ready, rank, place), (ready, rank, place))
        now, _, place = best
        name, _, _, _, _, sends, cost = left.pop(place)
        order.append(name)
        now += cost
        landed[name] = []
        for link, time, *more in sends:
            free[link] = max(now, free.get(link, ZERO)) + time
            landed[name].append(free[link] + latency + sum(more))
    return order


def layers_order(rows_i, cols_i, rows_o, cols_o, seq, starts):
    rate = 23300.0
    tasks = []
    for m in range(SIDE):
        is_in = m % PAIR == 0
        edge = cols_i // LANE * SIDE // 9 // PAIR * WIDE
        size = {"y": rows_i // SIDE * edge, "x": rows_i * (cols_i - PAIR * edge)} if is_in else {"y": rows_o // SIDE * cols_o // PAIR}
        size["z"] = size["y"]
        colors = "yzx" if is_in else "yz"
        for color in colors:
            cost = size[color] / rate
            both = [(("x", by), cost) for by in BOTH]
            spread = [((color, by), cost) for by in BOTH] if color != "x" else []
            tasks.append((("reach", m, color), m, starts[m], [], [], both, 0.2))
            for i, by in enumerate(BOTH):
                tasks.append((("relay", m, color, by), m, ZERO, [(("reach", m, color), i)], [], [(("x", by), cost / PAIR)] + spread, 0.2))
            halves = [(("relay", m, color, by), 0) for by in BOTH]
            tasks.append((("far", m, color), m, ZERO, halves, [], spread, 0.2))
            if color == "x":
                continue
            for off, source, first in ((-1, ("relay", m, color, 1), 1), (1, ("relay", m, color, -1), 1), (PAIR, ("far", m, color), 0)):
                for i, by in enumerate(BOTH):
                    tasks.append((("pass", m, color, off, by), m, ZERO, [(source, first + i)], [], [((color, by), cost / PAIR)], 0.2))
                halves = [(("pass", m, color, off, by), 0) for by in BOTH]
                tasks.append((("close", m, color, off), m, ZERO, halves, [], [], 0.2))
        for off in (-1, 1, PAIR):
            last = [("close", m, color, off) for color in "yz"]
            if is_in:
                last.append(("far", m, "x") if off == PAIR else ("relay", m, "x", -off))
            tasks.append((("hand", m, off), m, ZERO, [], last, [("chip", (rows_i * cols_i if is_in else rows_o * cols_o) / 150000.0)], 0.2))
    before = []

    def work(name, cost, mats=()):
        needs = [(("hand", m, off), 0) for m in mats for off in (-1, 1, PAIR)]
        tasks.append((name, 99, ZERO, needs, list(before), [], cost))
        before[:] = [name]

    for l in range(PAIR):
        work(("norm", l), 0.8)
        work(("project", l), 4.0, [PAIR * l])
        work(("attend", l), 4.2)
        work(("mlp", l), 2.2)
        work(("put", l), 1.6, [PAIR * l + 1])
    for l in (1, 0):
        work(("back_out", l), 2.9)
        work(("back_mlp", l), 2.0)
        work(("back_heads", l), 1.0)
        work(("back_quad", l), 6.0)
        work(("back_keys", l), 0.2)
        for i in range(PAIR):
            work(("back_in", l, i), 1.3 + 0.6 * i)
        work(("back_norm", l), 1.0)
    def send(name, rank, start, after, sends):
        tasks.append((name, rank, start, [], [after] if after else [], sends, 0.4))

    def follow(name, rank, needs, sends):
        tasks.append((name, rank, ZERO, needs, [], sends, 0.2))

    def both(axis, size):
        return [((axis, by), size / rate, margin) for by in BOTH]

    model, margin = rows_i * ROW, 2.0
    for l in (1, 0):
        for axis in "yz":
            name = ("send_h", l, axis)
            send(name, 20 - l, 58.0, ("norm", l), both(axis, seq * model))
            for i, by in enumerate(BOTH):
                for index in range(PAIR):
                    follow(("pass_h", l, axis, by, index), 10, [(name, i)], [((axis, by), seq * model / SIDE / rate, margin)])
        name = ("send_m", l)
        send(name, 22 - l, ZERO, ("mlp", l), both("x", seq * rows_o) + both("x", PAIR * seq * rows_o))
        for i, by in enumerate(BOTH):
            for index in range(PAIR):
                follow(("pass_m", l, by, index), 11, [(name, i)], [(("x", by), seq * rows_o / PAIR / rate, margin)])
        if l == 0:
            send(("own_y",), 15, ZERO, ("back_norm", 1), [])
            send(("send_scale", l), 15, ZERO, ("back_norm", l), [])
            continue
        name = ("send_y", l)
        send(name, 12, 42.0, None, both("x", seq * model))
        for i, by in enumerate(BOTH):
            follow(("pass_y", l, by), 12, [(name, i)], [(("x", by), seq * model / PAIR / rate, margin)])
        follow(("far_y", l), 12, [(("pass_y", l, by), 0) for by in BOTH], [])
        for axis in "zy":
            name = ("send_z", l, axis)
            share = seq * (cols_i + LANE) / ROW
            send(name, 13, ZERO, ("back_mlp", l), both(axis, share / PAIR) + both(axis, share))
            if axis == "y":
                name = ("rest_z", l)
                send(name, 13, ZERO, ("back_keys", l), both(axis, share / ROW) + both(axis, share / SIDE))
            for i, by in enumerate(BOTH):
                follow(("pass_z", l, axis, by), 13, [(name, i)], [((axis, by), share / PAIR / rate, margin)])
                follow(("twin_z", l, axis, by), 14, [(name, PAIR + i)], [])
            follow(("far_z", l, axis), 14, [(("pass_z", l, axis, by), 0) for by in BOTH], [])
        send(("send_scale", l), 15, ZERO, ("back_norm", l), [])
    send(("own_z",), 15, ZERO, ("back_keys", 0), [])
    return plan(tasks)


def gather_stages(links, position, shard_i, shard_o, wi, wo, lsem):
    x, y, z, core = position
    twin = device_at(x, y, z, 1 - core)
    rows_i, cols_i = shard_i.shape[1:]
    rows_o, cols_o = shard_o.shape[1:]
    quarter_i, quarter_o = rows_i // SIDE, rows_o // SIDE
    third_i = cols_i // LANE * SIDE // 9 // PAIR * WIDE
    half_o = cols_o // PAIR
    cut_o = quarter_o // 16 * ROW + ROW if quarter_o % 16 else quarter_o // PAIR
    place = {"x": x, "y": y, "z": z}

    spots = {(axis, o): step(place[axis], o) for axis in "xyz" for o in range(SIDE)}

    def spot(axis, o):
        return spots[axis, o % SIDE]

    table = {}
    for axis in "xyz":
        for o in range(1, SIDE):
            moved = {**place, axis: spot(axis, o)}
            table[axis, o] = device_at(moved["x"], moved["y"], moved["z"], core)

    def peer(axis, o):
        return table[axis, o % SIDE]

    mats = []
    for l in range(PAIR):
        mats.append((shard_i.at[l], wi.at[l], rows_i, True))
        mats.append((shard_o.at[l], wo.at[l], rows_o, False))

    def region(is_in, color, q):
        if is_in:
            if color == "x":
                lo, hi = PAIR * third_i, cols_i
                rows = (0, rows_i)
            else:
                lo, hi = (0, third_i) if color == "y" else (third_i, PAIR * third_i)
                rows = (q * quarter_i, quarter_i)
            mid = lo + ((hi - lo) // LANE + 1) // PAIR * LANE
            return (rows, (lo, hi - lo)), (rows, (lo, mid - lo)), (rows, (mid, hi - mid))
        cols = (0, half_o) if color == "y" else (half_o, half_o)
        start = q * quarter_o
        return ((start, quarter_o), cols), ((start, cut_o), cols), ((start + cut_o, quarter_o - cut_o), cols)

    def at(m, xb, area):
        (r, nr), (c, nc) = area
        _, out, size, _ = mats[m]
        return out.at[pl.ds(pl.multiple_of((PAIR * xb + core) * size + r, ROW), nr), pl.ds(c, nc)]

    def block(m, xb, index):
        _, out, size, _ = mats[m]
        return out.at[pl.ds(pl.multiple_of((PAIR * xb + index) * size, BAND), size)]

    def group(m, color):
        _, out, _, is_in = mats[m]
        (_, nr), (c, nc) = region(is_in, color, 0)[0]
        return dict(batch=(m, color), whole=out.at[pl.ds(0, nr * (3 if color == "x" else 12)), pl.ds(c, nc)])

    def reach(m, color):
        src, _, _, is_in = mats[m]
        area = region(is_in, color, place[color])[0]
        for by in BOTH:
            links.send((m, "x1", color, by), src.at[pl.ds(pl.multiple_of(area[0][0], ROW), area[0][1]), pl.ds(*area[1])], at(m, x, area), peer("x", by), **group(m, color))

    def launch(m, color, off):
        is_in = mats[m][3]
        moved = at(m, spot("x", off), region(is_in, color, place[color])[0])
        for by in BOTH:
            links.send((m, "p1", color, off, by), moved, moved, peer(color, by), **group(m, color))

    def relay(m, color, by):
        is_in = mats[m][3]
        xb = spot("x", -by)
        areas = region(is_in, color, place[color])
        links.arrive((m, "x1", color, by), at(m, xb, areas[0]))
        part = at(m, xb, areas[1] if by == 1 else areas[PAIR])
        links.send((m, "x2", color), part, part, peer("x", by), **group(m, color))
        if color != "x":
            launch(m, color, -by)

    def far(m, color):
        is_in = mats[m][3]
        links.arrive((m, "x2", color), at(m, spot("x", PAIR), region(is_in, color, place[color])[0]))
        if color != "x":
            launch(m, color, PAIR)

    def pass_on(m, color, off, by):
        is_in = mats[m][3]
        xb = spot("x", off)
        areas = region(is_in, color, spot(color, -by))
        links.arrive((m, "p1", color, off, by), at(m, xb, areas[0]))
        part = at(m, xb, areas[1] if by == 1 else areas[PAIR])
        links.send((m, "p2", color, off), part, part, peer(color, by), **group(m, color))

    def close(m, color, off):
        is_in = mats[m][3]
        links.arrive((m, "p2", color, off), at(m, spot("x", off), region(is_in, color, spot(color, PAIR))[0]))

    def four(m):
        _, out, size, _ = mats[m]
        return out.at[pl.ds(0, SIDE * size)]

    def give(m, src, dst):
        links.send((m, "chip"), src, dst, twin, batch=(m, "chip"), whole=four(m))

    def hand(m, off):
        whole = block(m, spot("x", off), core)
        give(m, whole, whole)

    owns = []

    def begin():
        for m, (src, _, _, _) in enumerate(mats):
            copy = pltpu.make_async_copy(src, block(m, x, core), lsem.at[m])
            copy.start()
            owns.append(copy)
            give(m, src, block(m, x, core))

    def ready(m):
        owns[m].wait()
        links.arrive((m, "chip"), four(m))

    return begin, ready, peer, {"reach": reach, "relay": relay, "far": far, "pass": pass_on, "close": close, "hand": hand}


BF, F32 = jnp.bfloat16, jnp.float32


def product(a, b, contract=((1,), (0,))):
    return lax.dot_general(a, b, (contract, ((), ())), preferred_element_type=F32)


def lanes(start, size):
    return pl.ds(start if isinstance(start, int) else pl.multiple_of(start, LANE), size)


def layers_kernel(order, sc_ref, wi_ref, wo_ref, x_ref, dy_ref, freq_ref,
                  y_ref, gx_ref, hy_a, hy_b, hz_a, hz_b, mx_a, mx_b, yx_b, zy_b, zz_b, z_a, dy_a, sc_out, relay_m, relay_z,
                  wi, wo, z, om, h, hid, qr, kts, vsl, ksl, turned_q, turned_o, scores, dscores, pcat, dscat, cos_ref, sin_ref, turn_ref,
                  dot_heads, qt, dht, dkv, omt, ht, dyt, sc, gains, own_gain, gain_ref, load_sems, own_sems, send_sems, recv_sems,
                  share_send_sems, share_recv_sems):
    seq, dim = x_ref.shape
    ff = (wi.shape[PAIR] - dim - LANE) // PAIR
    position = chip_position()
    x, y, zc, core = position
    twin = device_at(x, y, zc, 1 - core)
    me = PAIR * x + core
    links, shared = Links(send_sems, recv_sems), Links(share_send_sems, share_recv_sems)
    stored = []
    spots, _ = around(position)
    h_out, m_out, y_out, z_out = {"y": (hy_a, hy_b), "z": (hz_a, hz_b)}, (mx_a, mx_b), {1: yx_b}, {(1, "y"): zy_b, (1, "z"): zz_b}
    middle = hid.at[1]
    begin, ready, peer, stages = gather_stages(links, position, wi_ref, wo_ref, wi, wo, load_sems)
    others = [(zc * SIDE + y, rem(me + k, ROW)) for k in range(1, ROW)]

    def spot(axis, o):
        return spots[axis, o % SIDE]

    def device(axis, o, index):
        moved = {"x": x, "y": y, "z": zc, axis: spot(axis, o)}
        return device_at(moved["x"], moved["y"], moved["z"], index)

    own_gain[ALL] = jnp.zeros(own_gain.shape, F32)
    count = sc_ref.shape[1]
    for f in range(ROW):
        @pl.when(me == f)
        def _():
            own_gain[0:PAIR, f * count:(f + 1) * count] = sc_ref[ALL].astype(F32)
    announce(others + [device(axis, o, index) for axis in "yz" for o in AROUND for index in range(PAIR)])
    begin()
    for k, far in enumerate(others):
        links.send(("sc",), own_gain, gains.at[me], far, batch=("sc",), whole=gains.at[pl.ds(0, 7)])

    def keep(src, dst):
        copy = pltpu.make_async_copy(src, dst, own_sems.at[len(stored)])
        copy.start()
        stored.append(copy)

    def tokens(axis, o, index):
        return pl.ds(pl.multiple_of((PAIR * spot(axis, o) + index) * seq, seq), seq)

    def place(axis, o, index):
        return PAIR * spot(axis, o) + index

    def columns(axis, o):
        size = z.shape[PAIR] // ROW
        return lanes(((0 if axis == "y" else SIDE) + spot(axis, o)) * size, size)

    def several(batch, ref, n):
        whole = ref.at[pl.ds(0, n * seq if batch[0][0] in "yz" else n)]
        return dict(batch=batch, whole=whole)

    def send_h(l, axis):
        out = h_out[axis][l].at[place(axis, 0, core)]
        for by in BOTH:
            for index in range(PAIR):
                shared.send(("h", l, axis, by), ht.at[l, :, index], out, device(axis, by, index), lane=core, **several(("h", l, axis), h_out[axis][l], 7))
        shared.send(("h", l, axis), ht.at[l, :, 1 - core], out, twin, **several(("h", l, axis), h_out[axis][l], 7))
        keep(ht.at[l, :, core], out)

    def pass_h(l, axis, by, index):
        out = h_out[axis][l]
        shared.arrive(("h", l, axis, by), out.at[place(axis, -by, index)], index)
        part = out.at[place(axis, -by, index), pl.ds(1 - by, PAIR)]
        shared.send(("h", l, axis), part, part, device(axis, by, core), **several(("h", l, axis), out, 7))

    def arrive_h(l):
        for axis in "yz":
            shared.arrive(("h", l, axis), h_out[axis][l].at[pl.ds(0, 3)])

    def row_block(l, o, index, part=None):
        size = omt.shape[1] // ROW
        start = (PAIR * spot("x", o) + index) * size
        if part is not None:
            size = size // PAIR
            start = start + part * size
        return omt.at[l, pl.ds(pl.multiple_of(start, 16), size)]

    def row_half(k):
        size = m_out[0].shape[1] // PAIR
        return pl.ds(k * size, size)

    def send_m(l):
        out = m_out[l].at[place("x", 0, core)]
        for k, by in enumerate(BOTH):
            for index in range(PAIR):
                shared.send(("mr", l, by), row_block(l, PAIR, index, k), relay_m.at[l, k, core], device("x", by, index), lane=core, **several(("m", l), m_out[l], 7))
        for by in BOTH:
            for index in range(PAIR):
                shared.send(("m", l), row_block(l, by, index), out, device("x", by, index), **several(("m", l), m_out[l], 7))
        shared.send(("m", l), row_block(l, 0, 1 - core), out, twin, **several(("m", l), m_out[l], 7))
        keep(row_block(l, 0, core), out)

    def pass_m(l, by, index):
        k = (1 - by) // PAIR
        shared.arrive(("mr", l, by), relay_m.at[l, k, index], index)
        shared.send(("m", l), relay_m.at[l, k, index], m_out[l].at[place("x", -by, index), row_half(k)], device("x", by, core),
                    **several(("m2", l), m_out[l], PAIR))

    def arrive_m(l):
        shared.arrive(("m", l), m_out[l].at[pl.ds(0, 7)])

    def token_half(axis, o, k):
        return pl.ds(pl.multiple_of((PAIR * spot(axis, o) + core) * seq + k * (seq // PAIR), seq // PAIR), seq // PAIR)

    def send_y(l):
        src, out = dy_ref, y_out[l].at[tokens("x", 0, core)]
        for by in BOTH:
            shared.send(("y", l, by), src, out, device("x", by, core), **several(("y", l), y_out[l], 7))
        shared.send(("y", l), src, out, twin, **several(("y", l), y_out[l], 7))
        keep(src, out)

    def pass_y(l, by):
        landed, part = y_out[l].at[tokens("x", -by, core)], y_out[l].at[token_half("x", -by, (1 - by) // PAIR)]
        shared.arrive(("y", l, by), landed)
        shared.send(("y2", l), part, part, device("x", by, core), **several(("y", l), y_out[l], 7))
        shared.send(("y", l), landed, landed, twin, **several(("y", l), y_out[l], 7))

    def far_y(l):
        landed = y_out[l].at[tokens("x", PAIR, core)]
        shared.arrive(("y2", l), landed)
        shared.send(("y", l), landed, landed, twin, **several(("y", l), y_out[l], 7))

    def arrive_y(l):
        shared.arrive(("y", l), y_out[l].at[pl.ds(0, SIDE * seq)])

    def push_z(l, axis, o, ready):
        out = z_out[l, axis].at[tokens(axis, 0, core)]
        batch = several(("z", l, axis), z_out[l, axis], ROW)

        def start():
            if o != PAIR:
                shared.send(("z", l, axis, o), z.at[l, :, columns(axis, o)], out, device(axis, o, core), **batch)
                return
            for k, by in enumerate(BOTH):
                shared.send(("zr", l, axis, by), z.at[l, pl.ds(k * (seq // PAIR), seq // PAIR), columns(axis, PAIR)], relay_z.at[l, "yz".index(axis), k],
                            device(axis, by, core), **batch)

        if ready is None:
            start()
        else:
            pl.when(ready)(start)

    def own_part(l, axis):
        out, mine = z_out[l, axis].at[tokens(axis, 0, core)], z.at[l, :, columns(axis, 0)]
        shared.send(("z", l, axis), mine, out, twin, **several(("z", l, axis), z_out[l, axis], ROW))
        keep(mine, out)

    def send_z(l, axis):
        for o in (PAIR, 1, -1):
            push_z(l, axis, o, spot(axis, o) != 0 if axis == "y" else None)
        if axis == "z":
            own_part(l, axis)

    def rest_z(l):
        for o in (PAIR, 1, -1):
            push_z(l, "y", o, spot("y", o) == 0)
        own_part(l, "y")

    def pass_z(l, axis, by):
        k = (1 - by) // PAIR
        half = relay_z.at[l, "yz".index(axis), k]
        shared.arrive(("zr", l, axis, by), half)
        shared.send(("z2", l, axis), half, z_out[l, axis].at[token_half(axis, -by, k)], device(axis, by, core), **several(("z", l, axis), z_out[l, axis], ROW))

    def twin_z(l, axis, by):
        landed = z_out[l, axis].at[tokens(axis, -by, core)]
        shared.arrive(("z", l, axis, by), landed)
        shared.send(("z", l, axis), landed, landed, twin, **several(("z", l, axis), z_out[l, axis], ROW))

    def far_z(l, axis):
        landed = z_out[l, axis].at[tokens(axis, PAIR, core)]
        shared.arrive(("z2", l, axis), landed)
        shared.send(("z", l, axis), landed, landed, twin, **several(("z", l, axis), z_out[l, axis], ROW))

    def arrive_z(l, axis):
        shared.arrive(("z", l, axis), z_out[l, axis].at[pl.ds(0, SIDE * seq)])

    def send_scale(l):
        for far in others:
            shared.send(("scale", l), sc.at[l], sc_out.at[l, me], far, batch=("scale", l), whole=sc_out.at[l, pl.ds(0, 7)])
        keep(sc.at[l], sc_out.at[l, me])

    def arrive_scale(l):
        shared.arrive(("scale", l), sc_out.at[l, pl.ds(0, 7)])

    gains[me] = own_gain[ALL]
    z[:, :, wi.shape[PAIR]:] = jnp.zeros((PAIR, seq, z.shape[PAIR] - wi.shape[PAIR]), BF)
    entry = (x_ref, hid.at[0])
    angle = lax.broadcasted_iota(jnp.int32, (seq, LANE), 0).astype(F32) * freq_ref[0:1]
    for half in range(PAIR):
        cos_ref[:, LANE * half:LANE * (half + 1)] = jnp.cos(angle)
        sin_ref[:, LANE * half:LANE * (half + 1)] = jnp.sin(angle)
    lane = lax.broadcasted_iota(jnp.int32, turn_ref.shape, 1)
    down = lax.broadcasted_iota(jnp.int32, turn_ref.shape, 0) - lane
    low = rem(lane, HEAD) < BAND
    turn_ref[ALL] = jnp.where(low & (down == BAND), -1.0, jnp.where(jnp.logical_not(low) & (down == -BAND), 1.0, ZERO)).astype(BF)
    kts[ALL] = jnp.zeros(kts.shape, BF)
    pcat[ALL] = jnp.zeros(pcat.shape, BF)
    dscat[ALL] = jnp.zeros(dscat.shape, BF)

    def normalise(l, src):
        @pl.loop(0, seq // BAND, unroll=SIDE)
        def _(r):
            rows = pl.ds(pl.multiple_of(r * BAND, BAND), BAND)
            v = src[rows].astype(F32)
            v = v - jnp.mean(v, axis=-1, keepdims=True)
            var = jnp.mean(v * v, axis=-1, keepdims=True)
            h[l, rows] = (v * lax.rsqrt(var + 1e-6) * gain_ref[l:l + 1]).astype(BF)

    def project(l):
        strip = wi.shape[PAIR] // 5

        @pl.loop(0, 5)
        def _(i):
            at = lanes(i * strip, strip)
            z[l, :, at] = product(h[l], wi[l, :, at]).astype(BF)

    def heads(l):
        cos, sin = cos_ref[ALL], sin_ref[ALL]
        for g in range(dim // WIDE):
            q = z[l, :, g * WIDE:(g + 1) * WIDE]
            qr[l, :, g * WIDE:(g + 1) * WIDE] = ((q.astype(F32) * cos + product(q, turn_ref[ALL]) * sin) * 0.125).astype(BF)
        kv = z[l, :, dim:dim + LANE]
        turned = kv.astype(F32) * cos[:, :LANE] + product(kv, turn_ref[:LANE, :LANE]) * sin[:, :LANE]
        first = lax.broadcasted_iota(jnp.int32, turned.shape, 1) < HEAD
        key_lo = jnp.where(first, turned, ZERO)
        val_hi = jnp.where(first, ZERO, kv.astype(F32))
        return key_lo, pltpu.roll(key_lo, HEAD, 1), pltpu.roll(val_hi, HEAD, 1), val_hi

    def slot_rows(ref, lo, hi):
        zero = jnp.zeros((seq, LANE), BF)
        lo, hi = lo.astype(BF), hi.astype(BF)
        for i, (left, right) in enumerate(((lo, zero), (hi, zero), (zero, lo), (zero, hi))):
            ref[i * seq:(i + 1) * seq, :LANE] = left
            ref[i * seq:(i + 1) * seq, LANE:] = right

    def slot_cols(ref, lo):
        flat = lo.T[:HEAD].astype(BF)
        for i in range(SIDE):
            ref[HEAD * i:HEAD * (i + 1), i * seq:(i + 1) * seq] = flat

    def chances(i, half):
        at = slice(LANE * half, LANE * (half + 1))
        blocks = [pl.ds(pl.multiple_of(i * seq + LANE * k, LANE), LANE) for k in range(half + 1)]
        s = [scores[keys, at] for keys in blocks]
        lower = lax.broadcasted_iota(jnp.int32, s[-1].shape, 1) >= lax.broadcasted_iota(jnp.int32, s[-1].shape, 0)
        s[-1] = jnp.where(lower, s[-1], -1e30)
        top = functools.reduce(jnp.maximum, [jnp.max(v, axis=0, keepdims=True) for v in s])
        e = [jnp.exp(v - top) for v in s]
        scale = 1.0 / sum(jnp.sum(v, axis=0, keepdims=True) for v in e)
        return at, [(keys, v * scale) for keys, v in zip(blocks, e)]

    def attend(l):
        key_lo, key_hi, val_lo, _ = heads(l)
        slot_rows(ksl, key_lo, key_hi)
        slot_cols(kts, val_lo)
        flip(lambda at: qr[l, :, lanes(at, WIDE)], qt, dim)

        @pl.loop(0, dim // WIDE)
        def _(g):
            rows = pl.ds(pl.multiple_of(g * WIDE, WIDE), WIDE)
            scores[ALL] = product(ksl[ALL], qt[rows])

            @pl.loop(0, SIDE)
            def _(i):
                for half in range(PAIR):
                    at, blocks = chances(i, half)
                    for keys, p in blocks:
                        pcat[keys, at] = p.astype(BF)
            flat = product(kts[ALL], pcat[ALL]).astype(BF)
            omt[l, rows] = flat
            om[:, lanes(g * WIDE, WIDE)] = flat.T

    def mlp(l):
        @pl.loop(0, seq // BAND)
        def _(r):
            rows = pl.ds(pl.multiple_of(r * BAND, BAND), BAND)

            @pl.loop(0, ff // STRIP)
            def _(i):
                gate = z[l, rows, lanes(dim + LANE + i * STRIP, STRIP)].astype(F32)
                up = z[l, rows, lanes(dim + LANE + ff + i * STRIP, STRIP)].astype(F32)
                om[rows, lanes(dim + i * STRIP, STRIP)] = (gate * jax.nn.sigmoid(gate) * up).astype(BF)

    def put_out(l, dst):
        for n in range(dim // WIDE):
            cols = slice(n * WIDE, (n + 1) * WIDE)
            total = product(om[ALL], wo[l, :, cols])
            dst[:, cols] = (entry[l][:, cols].astype(F32) + total).astype(BF)

    def flip(src, dst, width, first=0):
        @pl.loop(first // WIDE, width // WIDE)
        def _(i):
            dst[pl.ds(pl.multiple_of(i * WIDE, WIDE), WIDE)] = src(i * WIDE).T

    upstream = (middle, dy_ref)

    def back_out(l):
        dy = upstream[l]
        flip(lambda at: dy[:, lanes(at, WIDE)], dyt, dim)

        @pl.loop(0, wo.shape[1] // dim)
        def _(n):
            rows = pl.ds(pl.multiple_of(n * dim, dim), dim)
            part = product(wo[l, rows], dyt[ALL]).astype(BF)
            om[:, lanes(n * dim, dim)] = part.T

            @pl.when(n == 0)
            def _():
                dot_heads[ALL] = part

    def back_mlp(l):
        @pl.loop(0, seq // BAND)
        def _(r):
            rows = pl.ds(pl.multiple_of(r * BAND, BAND), BAND)

            @pl.loop(0, ff // STRIP)
            def _(i):
                gate_at, up_at = lanes(dim + LANE + i * STRIP, STRIP), lanes(dim + LANE + ff + i * STRIP, STRIP)
                gate, up = z[l, rows, gate_at].astype(F32), z[l, rows, up_at].astype(F32)
                d = om[rows, lanes(dim + i * STRIP, STRIP)].astype(F32)
                sig = jax.nn.sigmoid(gate)
                du = d * up
                z[l, rows, gate_at] = (du * sig + du * gate * (sig * (1.0 - sig))).astype(BF)
                z[l, rows, up_at] = (d * (gate * sig)).astype(BF)

    def back_heads(l):
        key_lo, key_hi, val_lo, val_hi = heads(l)
        slot_rows(ksl, key_lo, key_hi)
        slot_rows(vsl, val_lo, val_hi)
        slot_cols(kts, key_lo)
        dkv[ALL] = jnp.zeros(dkv.shape, F32)
        flip(lambda at: qr[l, :, lanes(at, WIDE)], qt, dim)
        for at in range(0, dim, LANE):
            pair = slice(at, at + LANE)
            turned_q[:, pair] = pltpu.roll(qr[l, :, pair].astype(F32), HEAD, 1).astype(BF)
            turned_o[:, pair] = pltpu.roll(om[:, pair].astype(F32), HEAD, 1).astype(BF)

    def back_quad(l):
        @pl.loop(0, dim // WIDE)
        def _(g):
            quad(l, g)

    def quad(l, g):
        cols = pl.ds(pl.multiple_of(g * WIDE, WIDE), WIDE)
        scores[ALL] = product(ksl[ALL], qt[cols])
        dscores[ALL] = product(vsl[ALL], dot_heads[cols])

        @pl.loop(0, SIDE)
        def _(i):
            for half in range(PAIR):
                at, blocks = chances(i, half)
                given = [p * dscores[keys, at].astype(BF).astype(F32) for keys, p in blocks]
                total = sum(jnp.sum(v, axis=0, keepdims=True) for v in given)
                for (keys, p), v in zip(blocks, given):
                    pcat[keys, at] = p.astype(BF)
                    dscat[keys, at] = (v - p * total).astype(BF)
        dq = product(kts[ALL], dscat[ALL]).astype(BF).T
        back = dq.astype(F32) * cos_ref[ALL] - product(dq, turn_ref[ALL]) * sin_ref[ALL]
        z[l, :, cols] = (back * 0.125).astype(BF)
        for i in range(SIDE):
            keys, pair = slice(i * seq, (i + 1) * seq), lanes(g * WIDE + i // PAIR * LANE, LANE)
            even = i % PAIR == 0
            dkv[0] += product(dscat[keys], qr[l, :, pair] if even else turned_q[:, pair])
            dkv[1] += product(pcat[keys], turned_o[:, pair] if even else om[:, pair])

    def back_keys(l):
        dk = dkv[0].astype(BF)
        turned = dk.astype(F32) * cos_ref[:, :LANE] - product(dk, turn_ref[:LANE, :LANE]) * sin_ref[:, :LANE]
        first = lax.broadcasted_iota(jnp.int32, turned.shape, 1) < HEAD
        z[l, :, dim:dim + LANE] = jnp.where(first, turned, dkv[1]).astype(BF)

    def back_in(l, half):
        width = wi.shape[PAIR] // 5
        at = slice(PAIR * half * width, (PAIR + 3 * half) * width)
        part = product(wi[l, :, at], z[l, :, at], ((1,), (1,)))
        dht[ALL] = dht[ALL] + part if half else part

    def back_norm(l):
        dy, dst = upstream[l], (gx_ref, middle)[l]
        for i in range(dim // WIDE):
            cols = slice(i * WIDE, (i + 1) * WIDE)
            h[l, :, cols] = dht[cols].T.astype(BF)
        sc[l] = jnp.zeros(sc.shape[1:], F32)

        @pl.loop(0, seq // BAND, unroll=SIDE)
        def _(r):
            rows = pl.ds(pl.multiple_of(r * BAND, BAND), BAND)
            v = entry[l][rows].astype(F32)
            v = v - jnp.mean(v, axis=-1, keepdims=True)
            scale = lax.rsqrt(jnp.mean(v * v, axis=-1, keepdims=True) + 1e-6)
            hat = v * scale
            d = h[l, rows].astype(F32)
            each = (d * hat).reshape(SIDE, ROW, dim)
            sc[l] += (each[0] + each[1]) + (each[PAIR] + each[3])
            d = d * gain_ref[l:l + 1]
            d = scale * (d - jnp.mean(d, axis=-1, keepdims=True) - hat * jnp.mean(d * hat, axis=-1, keepdims=True))
            dst[rows] = (dy[rows].astype(F32) + d.astype(BF).astype(F32)).astype(BF)

    def do_norm(l):
        if l == 0:
            links.arrive(("sc",), gains.at[pl.ds(0, 7)])
            gain_ref[ALL] = jnp.sum(gains[ALL], axis=0)
        normalise(l, entry[l])
        for i in range(dim // WIDE):
            flat = h[l, :, i * WIDE:(i + 1) * WIDE].T
            size = ht.shape[3]
            for b in range(ROW):
                lo, hi = max(b * size, i * WIDE), min((b + 1) * size, (i + 1) * WIDE)
                if lo < hi:
                    ht[l, b // PAIR, b % PAIR, lo - b * size:hi - b * size] = flat[lo - i * WIDE:hi - i * WIDE]

    def do_project(l):
        ready(PAIR * l)
        project(l)

    def do_mlp(l):
        mlp(l)
        flip(lambda at: om[:, lanes(at, WIDE)], omt.at[l], om.shape[1], dim)

    def do_put(l):
        ready(PAIR * l + 1)
        put_out(l, hid.at[0] if l == 0 else y_ref)

    stages.update(
        norm=do_norm, project=do_project, attend=attend, mlp=do_mlp, put=do_put, back_out=back_out, back_mlp=back_mlp, back_heads=back_heads,
        back_quad=back_quad, back_keys=back_keys, back_in=back_in, back_norm=back_norm, send_h=send_h, pass_h=pass_h, send_m=send_m,
        pass_m=pass_m, send_y=send_y, pass_y=pass_y, far_y=far_y, send_z=send_z, rest_z=rest_z, pass_z=pass_z, twin_z=twin_z, far_z=far_z,
        send_scale=send_scale, own_z=lambda: keep(z.at[0], z_a), own_y=lambda: keep(middle, dy_a))
    for kind, *task in order:
        stages[kind](*task)
    for l in range(PAIR):
        arrive_h(l)
        arrive_m(l)
        arrive_scale(l)
    arrive_y(1)
    for l, axis in z_out:
        arrive_z(l, axis)
    for copy in stored:
        copy.wait()
    shared.drain()
    links.drain()


def run_layers(x, dy, scale, w_in, w_out, freq, starts=(ZERO, 10.0, 20.0, 30.0)):
    seq, dim = x.shape
    proj, cat = w_in.shape[PAIR], ROW * w_out.shape[1]
    wide = proj + LANE
    hbm, vmem = pl.BlockSpec(memory_space=pltpu.HBM), pl.BlockSpec(memory_space=pltpu.VMEM)
    out = lambda *shape, dtype=BF: jax.ShapeDtypeStruct(shape, dtype)
    buffer = lambda *shape, dtype=BF: pltpu.VMEM(shape, dtype)
    sem = pltpu.SemaphoreType.DMA
    line = ROW * seq
    return pl.pallas_call(
        functools.partial(layers_kernel, layers_order(*w_in.shape[1:], *w_out.shape[1:], seq, starts)),
        out_shape=(out(seq, dim), out(seq, dim), *[out(ROW, SIDE, dim // ROW, seq)] * SIDE, *[out(ROW, cat // ROW, seq)] * PAIR, out(line, dim),
                   *[out(line, wide // ROW)] * PAIR, out(seq, wide), out(seq, dim), out(PAIR, ROW, ROW, dim, dtype=F32),
                   out(PAIR, PAIR, PAIR, cat // 16, seq), out(PAIR, PAIR, PAIR, seq // PAIR, wide // ROW)),
        in_specs=[vmem, hbm, hbm] + [vmem] * 3,
        out_specs=[vmem] * PAIR + [hbm] * 14,
        scratch_shapes=[
            buffer(PAIR, dim, proj), buffer(PAIR, cat, dim), buffer(PAIR, seq, wide), buffer(seq, cat), buffer(PAIR, seq, dim),
            buffer(PAIR, seq, dim), buffer(PAIR, seq, dim),
            buffer(WIDE, SIDE * seq), buffer(SIDE * seq, WIDE), buffer(SIDE * seq, WIDE), buffer(seq, dim), buffer(seq, dim),
            buffer(SIDE * seq, seq, dtype=F32), buffer(SIDE * seq, seq, dtype=F32), buffer(SIDE * seq, seq), buffer(SIDE * seq, seq),
            buffer(seq, WIDE, dtype=F32), buffer(seq, WIDE, dtype=F32), buffer(WIDE, WIDE),
            buffer(dim, seq), buffer(dim, seq), buffer(dim, seq, dtype=F32), buffer(PAIR, seq, LANE, dtype=F32),
            buffer(PAIR, cat, seq), buffer(PAIR, SIDE, PAIR, dim // ROW, seq), buffer(dim, seq), buffer(PAIR, ROW, dim, dtype=F32),
            buffer(ROW, ROW, dim, dtype=F32), buffer(ROW, dim, dtype=F32), buffer(ROW, dim, dtype=F32),
            sem((SIDE,)), sem((13,)), sem((15,)), sem((107,)), sem((13,)), sem((HEAD,)),
        ],
        compiler_params=pltpu.CompilerParams(collective_id=PAIR, has_side_effects=True, vmem_limit_bytes=67043328),
        name="run_layers",
    )(scale, w_in, w_out, x, dy, freq)


PARTS = (("i", "x", "z", "y", 0, STRIP), ("i", "x", "z", "y", STRIP, 384), ("i", "x", "y", "z", 0, STRIP), ("i", "x", "y", "z", STRIP, 384),
         ("o", "y", "z", "y", 0, 384), ("o", "z", "y", "z", 384, 384))


def reduce_order(rows, rows_b, starts):
    rate = 11650.0
    tasks = []
    sizes = {"y": WIDE * 896 / (PAIR * rate), "z": WIDE * 896 / (PAIR * rate), "x": WIDE * 768 / (PAIR * rate)}
    for axis in "yzx":
        tasks.append((("swap", axis), (0, 0), starts[PAIR] if axis == "x" else starts[3], [], [], [((axis, by), sizes[axis] * n) for by, n in ((1, 1), (-1, 1), (1, PAIR))], 0.3))
        for i, o in enumerate(AROUND):
            tasks.append((("near", axis, o), (0, PAIR), ZERO, [(("swap", axis), i)], [], [("chip", 1.6)], 0.2))
    tasks.append((("fetch", 0), (5, 0), ZERO, [], [("make", 1, len(PARTS) - 1)], [], 0.2))
    for l in (1, 0):
        late = 1 - l
        for c, (kind, first, then, last, at, width) in enumerate(PARTS):
            needs, cost = [], 1.6 * width / STRIP
            if l == 0:
                needs = [(("near", last if kind == "i" else "x", o), 0) for o in AROUND]
            tasks.append((("make", l, c), (9 * late, c), starts[late], needs, [] if l else [("fetch", 0)], [], cost))
            full = SIDE * SIDE * (rows if kind == "i" else rows_b) * width / rate
            sends = [[((first, by), full / ROW) for by in BOTH], [((first, by), full / SIDE) for by in BOTH],
                     [((then, o), full / 16) for o in (1, -1, 1)], []]
            piece = full / 16
            sends += [[((then, by), piece) for by in BOTH], [((then, 1 - PAIR * (c % PAIR)), piece)], [((last, by), SIDE * piece) for by in BOTH],
                      [((last, by), PAIR * piece) for by in BOTH], []]
            for s in range(9):
                task = ("sum", l, c, s)
                needs = [(("sum", l, c, s - 1), k) for k in range(len(sends[s - 1]))] if s else []
                tasks.append((task, (late, -s), ZERO, needs, [("make", l, c)] if s == 0 else [("sum", l, c, s - 1)], sends[s], 0.3))
    return plan(tasks)


def reduce_kernel(order, *refs):
    hy, hz, mx = refs[0:PAIR], refs[PAIR:SIDE], refs[SIDE:6]
    yx1, zy1, zz1, z0, y0, sc = refs[6:12]
    oa, ob = refs[12:14]
    n = len(PARTS)
    total, half, full, small, front = (refs[14 + k * n:14 + (k + 1) * n] for k in range(5))
    (hbuf, zbuf, mbuf, ybuf, scbuf, ssem, rsem, isem, osem) = refs[14 + 5 * n:]
    position = chip_position()
    x, y, zc, core = position
    place = {"x": x, "y": y, "z": zc}
    twin = device_at(x, y, zc, 1 - core)
    spots, peers = around(position)

    def spot(axis, o):
        return spots[axis, o % SIDE]

    def peer(axis, o):
        return peers[axis, o % SIDE]

    seq, wide = z0.shape
    own = wide // ROW
    loads, moving = {}, []

    def load(key, src, dst):
        copy = pltpu.make_async_copy(src, dst, isem.at[len(moving)])
        moving.append(key)
        copy.start()
        loads[key] = copy

    def fetch(l):
        if l:
            load(("z", 1, "y"), zy1, zbuf.at[1, 0])
        load(("h", l, "y"), hy[l], hbuf.at[l, 0])
        if l:
            load(("z", 1, "z"), zz1, zbuf.at[1, 1])
        load(("h", l, "z"), hz[l], hbuf.at[l, 1])
        load(("m", l), mx[l], mbuf.at[l])
        if l:
            load(("y", 1), yx1, ybuf.at[1])
        load(("s", l), sc.at[l], scbuf.at[l])

    fetch(1)
    done = set()

    def loaded(*keys):
        for key in keys:
            if key not in done:
                loads[key].wait()
                done.add(key)

    announce([peer(axis, o) for axis in "xyz" for o in AROUND] + [twin])
    links = Links(ssem, rsem)

    def columns(axis, o):
        return lanes(((0 if axis == "y" else SIDE) + spot(axis, o)) * own, own)

    def tokens(axis, o, index):
        return pl.ds(pl.multiple_of((PAIR * spot(axis, o) + index) * seq, seq), seq)

    def target(axis):
        return ybuf.at[0] if axis == "x" else zbuf.at[0, "yz".index(axis)]

    def seven(axis):
        return dict(batch=("swap", axis), whole=target(axis).at[pl.ds(0, 7 * seq)])

    def swap(axis):
        def part(o):
            return y0 if axis == "x" else z0.at[:, columns(axis, o)]

        mine = target(axis).at[tokens(axis, 0, core)]
        for o in AROUND:
            links.send(("swap", axis, o), part(o), mine, peer(axis, o), **seven(axis))
        links.send(("near", axis), part(0), mine, twin, **seven(axis))
        load(("own", axis), part(0), mine)

    def near(axis, o):
        landed = target(axis).at[tokens(axis, -o, core)]
        links.arrive(("swap", axis, o), landed)
        links.send(("near", axis), landed, landed, twin, **seven(axis))

    def joined(axis):
        if axis not in done:
            done.add(axis)
            loaded(("own", axis))
            links.arrive(("near", axis), target(axis).at[pl.ds(0, SIDE * seq)])

    def joined_lanes(ref, l, i):
        return jnp.concatenate([ref[l, i, k].reshape(-1, ref.shape[-1]) for k in range(ROW)], axis=1)

    def make(l, c):
        kind, first, then, last, at, width = PARTS[c]
        if kind == "i":
            i = "yz".index(last)
            loaded(("h", l, last))
            if l:
                loaded(("z", l, last))
            else:
                joined(last)
            size = total[c].shape[3]
            for lo in range(0, width, WIDE):
                hi = min(width, lo + WIDE)
                part = product(joined_lanes(hbuf, l, i), zbuf[l, i, :, at + lo:at + hi])
                for r in range(16):
                    total[c][l, r // SIDE, r % SIDE, :, lo:hi] = part[r * size:(r + 1) * size]
            return
        loaded(("m", l), ("s", l))
        if l:
            loaded(("y", l))
        else:
            joined("x")
        part = product(jnp.concatenate([mbuf[l, k] for k in range(ROW)], axis=1), ybuf[l, :, at:at + width])
        size = total[c].shape[3]

        def put(r, value):
            total[c][(l, r // SIDE, r % SIDE) if first == "y" else (l, r % SIDE, r // SIDE)] = value

        for r in range(part.shape[0] // size):
            put(r, part[r * size:(r + 1) * size])
        gain = jnp.sum(jnp.sum(scbuf[l, :, :, at:at + width], axis=0), axis=0, keepdims=True)
        row = lax.broadcasted_iota(jnp.int32, (size, width), 0)
        put(15, jnp.where(row == 0, gain, ZERO))

    def area(l, c, o, whole):
        kind, first, then, last, at, width = PARTS[c]
        inner = (spot(then, whole) if isinstance(whole, int) else whole)
        outer = spot(last, o)
        if kind == "i":
            cols = lanes(((0 if last == "y" else SIDE) + outer) * own + at, width)
            return oa.at[l, inner, :, cols]
        cols = pl.ds(at, width)
        return ob.at[l, outer, inner, :, cols] if last == "y" else ob.at[l, inner, outer, :, cols]

    def add(l, c, s):
        kind, first, then, last, at, width = PARTS[c]
        t = total[c].at[l]
        way = 1 - PAIR * (c % PAIR)
        sums = dict(batch=(l, c, 0), whole=t)
        wide_ones = dict(batch=(l, c, 1), whole=t.at[pl.ds(0, 3)])
        narrow = dict(batch=(l, c, PAIR), whole=t.at[0, pl.ds(0, PAIR)])
        if s == 0:
            far = t.at[spot(first, PAIR)]
            for k, by in enumerate(BOTH):
                links.send((l, c, "half"), far.at[pl.ds(PAIR * k, PAIR)], half[c].at[l, k], peer(first, by), **sums)
        elif s == 1:
            links.arrive((l, c, "half"), half[c].at[l])
            for k, by in enumerate(BOTH):
                mine = t.at[spot(first, by)]
                add_into(mine.at[pl.ds(PAIR * k, PAIR)], half[c].at[l, k])
                links.send((l, c, "full"), mine, full[c].at[l, k], peer(first, by), **sums)
        elif s == PAIR:
            mine = t.at[spot(first, 0)]
            links.arrive((l, c, "full"), full[c].at[l])
            for k in range(PAIR):
                add_into(mine, full[c].at[l, k])
            for k, o in enumerate(AROUND):
                links.send((l, c, "small"), mine.at[spot(then, o)], small[c].at[l, k], peer(then, o), **wide_ones)
        elif s == 3:
            links.arrive((l, c, "small"), small[c].at[l])
            mine = t.at[spot(first, 0), spot(then, 0)]
            front[c][l] = (mine[ALL] + small[c][l, 0]) + (small[c][l, 1] + small[c][l, PAIR])
        elif s == SIDE:
            src, dst = front[c].at[l], area(l, c, 0, 0)
            for by in BOTH:
                links.send((l, c, "a1"), src, dst, peer(then, by), **narrow)
            copy = pltpu.make_async_copy(src, dst, osem.at[l, c])
            copy.start()
            loads["front", l, c] = copy
        elif s == 5:
            links.arrive((l, c, "a1"), t.at[0, pl.ds(0, PAIR)])
            landed = area(l, c, 0, -way)
            links.send((l, c, "b1"), landed, landed, peer(then, way), **wide_ones)
        elif s == 6:
            loaded(("front", l, c))
            links.arrive((l, c, "b1"), area(l, c, 0, PAIR))
            line = area(l, c, 0, slice(None))
            for by in BOTH:
                links.send((l, c, "a2"), line, line, peer(last, by), **wide_ones)
        elif s == 7:
            links.arrive((l, c, "a2"), t.at[pl.ds(0, PAIR)])
            for k, by in enumerate(BOTH):
                part = area(l, c, -by, pl.ds(PAIR * k, PAIR))
                links.send((l, c, "a3"), part, part, peer(last, by), **sums)
        else:
            links.arrive((l, c, "a3"), area(l, c, PAIR, slice(None)))

    stages = {"swap": swap, "near": near, "fetch": fetch, "make": make, "sum": add}
    for kind, *task in order:
        stages[kind](*task)
    links.drain()


def add_into(dst, src):
    @pl.loop(0, dst.shape[0])
    def _(i):
        if len(dst.shape) == SIDE:
            for j in range(dst.shape[1]):
                dst[i, j] += src[i, j]
        else:
            dst[i] += src[i]


def around(position):
    place, core = dict(zip("xyz", position)), position[3]
    spots = {(axis, o): step(place[axis], o) for axis in "xyz" for o in range(SIDE)}
    peers = {}
    for axis in "xyz":
        for o in range(1, SIDE):
            moved = {**place, axis: spots[axis, o]}
            peers[axis, o] = device_at(moved["x"], moved["y"], moved["z"], core)
    return spots, peers


def reduce_gradients(operands, starts=(ZERO, ZERO, ZERO, ZERO)):
    hbm = pl.BlockSpec(memory_space=pltpu.HBM)
    h_rows, m_rows, y_cols, z_cols, z_own, y_own, scale_parts = operands
    part, part_b = h_rows[0].shape[PAIR] // SIDE, (m_rows[0].shape[1] + BAND) // 16
    (line, dim), wide = y_cols.shape, z_own.shape[1]
    out = lambda *shape: jax.ShapeDtypeStruct(shape, F32)
    sem = pltpu.SemaphoreType.DMA

    def buffers(*lead):
        return [pltpu.VMEM((PAIR, *lead, part if e[0] == "i" else part_b, e[5]), F32) for e in PARTS]

    return pl.pallas_call(
        functools.partial(reduce_kernel, reduce_order(part, part_b, starts)),
        out_shape=(out(PAIR, SIDE, part, wide), out(PAIR, SIDE, SIDE, part_b, dim)),
        in_specs=[hbm] * 12,
        out_specs=[hbm] * PAIR,
        scratch_shapes=[
            *buffers(SIDE, SIDE), *buffers(PAIR, PAIR), *buffers(PAIR, SIDE), *buffers(3), *buffers(),
            pltpu.VMEM((PAIR, PAIR, *h_rows[0].shape), BF), pltpu.VMEM((PAIR, PAIR, line, wide // ROW), BF), pltpu.VMEM((PAIR, *m_rows[0].shape), BF),
            pltpu.VMEM((PAIR, line, dim), BF), pltpu.VMEM(scale_parts.shape, F32),
            sem((39,)), sem((96,)), sem((14,)), sem((PAIR, len(PARTS))),
        ],
        compiler_params=pltpu.CompilerParams(collective_id=1, has_side_effects=True, vmem_limit_bytes=67043328),
        name="reduce_gradients",
    )(*h_rows, *m_rows, y_cols, *z_cols, z_own, y_own, scale_parts)


def solution(mesh):
    fsdp_size = mesh.shape["fsdp"]
    batch_spec = P(("dp", "fsdp"), None, None)
    scale_spec = P(None, "fsdp")
    weight_spec = P(None, "fsdp", None)

    def device_step(x_in, grad_y, norm_scale, w_in, w_out):
        n_layers = w_in.shape[0]
        seq_len, model_dim = x_in.shape[1:]
        proj_dim = w_in.shape[PAIR]
        ff_dim = w_out.shape[1] * fsdp_size - model_dim
        head_dim = (proj_dim - model_dim - PAIR * ff_dim) // PAIR
        rows, rows_out = norm_scale.shape[1], w_out.shape[1]
        half_dim = head_dim // PAIR
        freq = 10000.0 ** (-np.arange(half_dim, dtype=np.float32) * 2.0 / head_dim)
        freq = jnp.asarray(np.tile(freq.astype(np.float32), (ROW, LANE // half_dim)))
        hidden, grad_hidden, *rest = run_layers(x_in[0], grad_y[0], norm_scale, w_in, w_out, freq)
        in_sums, out_sums = reduce_gradients((rest[0:SIDE], rest[SIDE:6], rest[6], rest[7:9], rest[9], rest[10], rest[11]))
        in_grads = in_sums.reshape(n_layers, rows, -1)[:, :, :proj_dim]
        out_rows = out_sums.reshape(n_layers, -1, model_dim)
        scale_grads = lax.dynamic_slice(out_rows[:, rows_out], (0, lax.axis_index("fsdp") * rows), (n_layers, rows))
        out_grads = out_rows[:, :rows_out]
        return hidden[None], grad_hidden[None], scale_grads, in_grads, out_grads

    return jax.shard_map(
        device_step,
        mesh=mesh,
        in_specs=(batch_spec, batch_spec, scale_spec, weight_spec, weight_spec),
        out_specs=(batch_spec, batch_spec, scale_spec, weight_spec, weight_spec),
        check_vma=False,
    )
```

```python
import functools
import jax
import jax.numpy as jnp
import numpy as np
from jax import lax
from jax.experimental import pallas as pl
from jax.experimental.pallas import tpu as pltpu
from jax.sharding import PartitionSpec as P

MESH_ID = pl.DeviceIdType.MESH
BOTH = (1, -1)
AROUND = (1, -1, 2)
PARTS = (True, False)
ALL, ZERO = ..., 0.0
OTHERS = 7
QUICK, SHORT = 0.2, 0.3
LANE, WIDE, STRIP, HEAD = 128, 256, 512, 64
ROW, BAND, SIDE, TRIO, PAIR = 8, 32, 4, 3, 2


class Links:
    def __init__(self, send_sems, recv_sems):
        self.send_sems, self.recv_sems = send_sems, recv_sems
        self.slots, self.batches, self.sent, self.count = {}, {}, {}, 0

    def _landing(self, key, lane):
        if key not in self.slots:
            self.slots[key] = self.count
            self.count += 1 if lane is None else PAIR
        return self.recv_sems.at[self.slots[key] + (0 if lane is None else lane)]

    def send(self, key, src, dst, device, landing=None, whole=None, batch=None, lane=None):
        leaving = self.batches.setdefault(batch or key, len(self.batches))
        copy = pltpu.make_async_remote_copy(
            src_ref=src, dst_ref=dst, send_sem=self.send_sems.at[leaving], recv_sem=self._landing(landing or key, lane),
            device_id=device, device_id_type=MESH_ID)
        copy.start()
        self.sent[batch or key] = (src if whole is None else whole, leaving)

    def arrive(self, key, landed, lane=None):
        pltpu.make_async_copy(landed, landed, self._landing(key, lane)).wait()

    def drain(self):
        for left, leaving in self.sent.values():
            pltpu.make_async_copy(left, left, self.send_sems.at[leaving]).wait()
        self.sent.clear()


def rem(a, n):
    return a % n if isinstance(a, int) else lax.rem(a, n)


def chip_position():
    f, d = lax.axis_index("fsdp"), lax.axis_index("dp")
    return f // PAIR, rem(d, SIDE), d // SIDE, rem(f, PAIR)


def device_at(x, y, z, core):
    return (z * SIDE + y, x * PAIR + core)


def step(coord, by):
    return rem(coord + SIDE + by, SIDE)


def announce(devices):
    barrier = pltpu.get_barrier_semaphore()
    for device in devices:
        pl.semaphore_signal(barrier, inc=1, device_id=device, device_id_type=MESH_ID)
    pl.semaphore_wait(barrier, len(devices))


def plan(tasks, latency=2.5):
    free, landed, order, now = {}, {}, [], ZERO
    left = list(tasks)
    while left:
        best = None
        for place, (name, rank, start, needs, after, _, _) in enumerate(left):
            if all(n[0] in landed for n in needs) and all(n in landed for n in after):
                ready = max([start, now] + [landed[task][i] for task, i in needs])
                best = min(best or (ready, rank, place), (ready, rank, place))
        now, _, place = best
        name, _, _, _, _, sends, cost = left.pop(place)
        order.append(name)
        now += cost
        landed[name] = []
        for link, time, *more in sends:
            free[link] = max(now, free.get(link, ZERO)) + time
            landed[name].append(free[link] + latency + sum(more))
    return order


def layers_order(rows_i, cols_i, rows_o, cols_o, seq, starts):
    rate = 23300.0
    tasks = []
    for m in range(SIDE):
        is_in = m % PAIR == 0
        edge = cols_i // LANE * SIDE // 9 // PAIR * WIDE
        size = {"y": rows_i // SIDE * edge, "x": rows_i * (cols_i - PAIR * edge)} if is_in else {"y": rows_o // SIDE * cols_o // PAIR}
        size["z"] = size["y"]
        colors = "yzx" if is_in else "yz"
        for color in colors:
            cost = size[color] / rate
            both = [(("x", by), cost) for by in BOTH]
            spread = [((color, by), cost) for by in BOTH] if color != "x" else []
            tasks.append((("reach", m, color), m, starts[m], [], [], both, QUICK))
            for i, by in enumerate(BOTH):
                tasks.append((("relay", m, color, by), m, ZERO, [(("reach", m, color), i)], [], [(("x", by), cost / PAIR)] + spread, QUICK))
            halves = [(("relay", m, color, by), 0) for by in BOTH]
            tasks.append((("far", m, color), m, ZERO, halves, [], spread, QUICK))
            if color == "x":
                continue
            for off, source, first in ((-1, ("relay", m, color, 1), 1), (1, ("relay", m, color, -1), 1), (PAIR, ("far", m, color), 0)):
                for i, by in enumerate(BOTH):
                    tasks.append((("pass", m, color, off, by), m, ZERO, [(source, first + i)], [], [((color, by), cost / PAIR)], QUICK))
                halves = [(("pass", m, color, off, by), 0) for by in BOTH]
                tasks.append((("close", m, color, off), m, ZERO, halves, [], [], QUICK))
        for off in (-1, 1, PAIR):
            last = [("close", m, color, off) for color in "yz"]
            if is_in:
                last.append(("far", m, "x") if off == PAIR else ("relay", m, "x", -off))
            tasks.append((("hand", m, off), m, ZERO, [], last, [("chip", (rows_i * cols_i if is_in else rows_o * cols_o) / 150000.0)], QUICK))
    before = []

    def work(name, cost, mats=()):
        needs = [(("hand", m, off), 0) for m in mats for off in (-1, 1, PAIR)]
        tasks.append((name, 99, ZERO, needs, list(before), [], cost))
        before[:] = [name]

    for l in range(PAIR):
        work(("norm", l), 0.8)
        work(("project", l), 4.0, [PAIR * l])
        work(("attend", l), 4.2)
        work(("mlp", l), 2.2)
        work(("put", l), 1.6, [PAIR * l + 1])
    for l in (1, 0):
        work(("back_out", l), 2.9)
        work(("back_mlp", l), 2.0)
        work(("back_heads", l), 1.0)
        work(("back_quad", l), 6.0)
        work(("back_keys", l), QUICK)
        for i in range(PAIR):
            work(("back_in", l, i), 1.3 + 0.6 * i)
        work(("back_norm", l), 1.0)
    def send(name, rank, start, after, sends):
        tasks.append((name, rank, start, [], [after] if after else [], sends, 0.4))

    def follow(name, rank, needs, sends):
        tasks.append((name, rank, ZERO, needs, [], sends, QUICK))

    def both(axis, size):
        return [((axis, by), size / rate, margin) for by in BOTH]

    model, margin = rows_i * ROW, 2.0
    for l in (1, 0):
        for axis in "yz":
            name = ("send_h", l, axis)
            send(name, 20 - l, 58.0, ("norm", l), both(axis, seq * model))
            for i, by in enumerate(BOTH):
                for index in range(PAIR):
                    follow(("pass_h", l, axis, by, index), 10, [(name, i)], [((axis, by), seq * model / SIDE / rate, margin)])
        name = ("send_m", l)
        send(name, 22 - l, ZERO, ("mlp", l), both("x", seq * rows_o) + both("x", PAIR * seq * rows_o))
        for i, by in enumerate(BOTH):
            for index in range(PAIR):
                follow(("pass_m", l, by, index), 11, [(name, i)], [(("x", by), seq * rows_o / PAIR / rate, margin)])
        if l == 0:
            send(("own_y",), 15, ZERO, ("back_norm", 1), [])
            send(("send_scale", l), 15, ZERO, ("back_norm", l), [])
            continue
        name = ("send_y", l)
        send(name, 12, 42.0, None, both("x", seq * model))
        for i, by in enumerate(BOTH):
            follow(("pass_y", l, by), 12, [(name, i)], [(("x", by), seq * model / PAIR / rate, margin)])
        follow(("far_y", l), 12, [(("pass_y", l, by), 0) for by in BOTH], [])
        for axis in "zy":
            name = ("send_z", l, axis)
            share = seq * (cols_i + LANE) / ROW
            send(name, 13, ZERO, ("back_mlp", l), both(axis, share / PAIR) + both(axis, share))
            if axis == "y":
                name = ("rest_z", l)
                send(name, 13, ZERO, ("back_keys", l), both(axis, share / ROW) + both(axis, share / SIDE))
            for i, by in enumerate(BOTH):
                follow(("pass_z", l, axis, by), 13, [(name, i)], [((axis, by), share / PAIR / rate, margin)])
                follow(("twin_z", l, axis, by), 14, [(name, PAIR + i)], [])
            follow(("far_z", l, axis), 14, [(("pass_z", l, axis, by), 0) for by in BOTH], [])
        send(("send_scale", l), 15, ZERO, ("back_norm", l), [])
    send(("own_z",), 15, ZERO, ("back_keys", 0), [])
    send(("late_z",), 14, ZERO, ("back_mlp", 0), [])
    return plan(tasks)


def gather_stages(links, position, shard_i, shard_o, wi, wo, lsem):
    x, y, z, core = position
    twin = device_at(x, y, z, 1 - core)
    rows_i, cols_i = shard_i.shape[1:]
    rows_o, cols_o = shard_o.shape[1:]
    quarter_i, quarter_o = rows_i // SIDE, rows_o // SIDE
    third_i = cols_i // LANE * SIDE // 9 // PAIR * WIDE
    half_o = cols_o // PAIR
    cut_o = quarter_o // 16 * ROW + ROW if quarter_o % 16 else quarter_o // PAIR
    place = {"x": x, "y": y, "z": z}

    spots = {(axis, o): step(place[axis], o) for axis in "xyz" for o in range(SIDE)}

    def spot(axis, o):
        return spots[axis, o % SIDE]

    table = {}
    for axis in "xyz":
        for o in range(1, SIDE):
            moved = {**place, axis: spot(axis, o)}
            table[axis, o] = device_at(moved["x"], moved["y"], moved["z"], core)

    def peer(axis, o):
        return table[axis, o % SIDE]

    mats = []
    for l in range(PAIR):
        mats.append((shard_i.at[l], wi.at[l], rows_i, True))
        mats.append((shard_o.at[l], wo.at[l], rows_o, False))

    def region(is_in, color, q):
        if is_in:
            if color == "x":
                lo, hi = PAIR * third_i, cols_i
                rows = (0, rows_i)
            else:
                lo, hi = (0, third_i) if color == "y" else (third_i, PAIR * third_i)
                rows = (q * quarter_i, quarter_i)
            mid = lo + ((hi - lo) // LANE + 1) // PAIR * LANE
            return (rows, (lo, hi - lo)), (rows, (lo, mid - lo)), (rows, (mid, hi - mid))
        cols = (0, half_o) if color == "y" else (half_o, half_o)
        start = q * quarter_o
        return ((start, quarter_o), cols), ((start, cut_o), cols), ((start + cut_o, quarter_o - cut_o), cols)

    def at(m, xb, area):
        (r, nr), (c, nc) = area
        _, out, size, _ = mats[m]
        return out.at[pl.ds(pl.multiple_of((PAIR * xb + core) * size + r, ROW), nr), pl.ds(c, nc)]

    def block(m, xb, index):
        _, out, size, _ = mats[m]
        return out.at[pl.ds(pl.multiple_of((PAIR * xb + index) * size, BAND), size)]

    def group(m, color):
        _, out, _, is_in = mats[m]
        (_, nr), (c, nc) = region(is_in, color, 0)[0]
        return dict(batch=(m, color), whole=out.at[pl.ds(0, nr * (TRIO if color == "x" else 12)), pl.ds(c, nc)])

    def reach(m, color):
        src, _, _, is_in = mats[m]
        area = region(is_in, color, place[color])[0]
        for by in BOTH:
            links.send((m, "x1", color, by), src.at[pl.ds(pl.multiple_of(area[0][0], ROW), area[0][1]), pl.ds(*area[1])], at(m, x, area), peer("x", by), **group(m, color))

    def launch(m, color, off):
        is_in = mats[m][TRIO]
        moved = at(m, spot("x", off), region(is_in, color, place[color])[0])
        for by in BOTH:
            links.send((m, "p1", color, off, by), moved, moved, peer(color, by), **group(m, color))

    def relay(m, color, by):
        is_in = mats[m][TRIO]
        xb = spot("x", -by)
        areas = region(is_in, color, place[color])
        links.arrive((m, "x1", color, by), at(m, xb, areas[0]))
        part = at(m, xb, areas[1] if by == 1 else areas[PAIR])
        links.send((m, "x2", color), part, part, peer("x", by), **group(m, color))
        if color != "x":
            launch(m, color, -by)

    def far(m, color):
        is_in = mats[m][TRIO]
        links.arrive((m, "x2", color), at(m, spot("x", PAIR), region(is_in, color, place[color])[0]))
        if color != "x":
            launch(m, color, PAIR)

    def pass_on(m, color, off, by):
        is_in = mats[m][TRIO]
        xb = spot("x", off)
        areas = region(is_in, color, spot(color, -by))
        links.arrive((m, "p1", color, off, by), at(m, xb, areas[0]))
        part = at(m, xb, areas[1] if by == 1 else areas[PAIR])
        links.send((m, "p2", color, off), part, part, peer(color, by), **group(m, color))

    def close(m, color, off):
        is_in = mats[m][TRIO]
        links.arrive((m, "p2", color, off), at(m, spot("x", off), region(is_in, color, spot(color, PAIR))[0]))

    def four(m):
        _, out, size, _ = mats[m]
        return out.at[pl.ds(0, SIDE * size)]

    def give(m, src, dst):
        links.send((m, "chip"), src, dst, twin, batch=(m, "chip"), whole=four(m))

    def hand(m, off):
        whole = block(m, spot("x", off), core)
        give(m, whole, whole)

    owns = []

    def begin():
        for m, (src, _, _, _) in enumerate(mats):
            copy = pltpu.make_async_copy(src, block(m, x, core), lsem.at[m])
            copy.start()
            owns.append(copy)
            give(m, src, block(m, x, core))

    def ready(m):
        owns[m].wait()
        links.arrive((m, "chip"), four(m))

    return begin, ready, peer, {"reach": reach, "relay": relay, "far": far, "pass": pass_on, "close": close, "hand": hand}


BF, F32 = jnp.bfloat16, jnp.float32


def product(a, b, contract=((1,), (0,))):
    return lax.dot_general(a, b, (contract, ((), ())), preferred_element_type=F32)


def lanes(start, size):
    return pl.ds(start if isinstance(start, int) else pl.multiple_of(start, LANE), size)


def layers_kernel(order, sc_ref, wi_ref, wo_ref, x_ref, dy_ref, freq_ref,
                  y_ref, gx_ref, hy_a, hy_b, hz_a, hz_b, mx_a, mx_b, yx_b, zy_b, zz_b, zy_a, zz_a, z_a, dy_a, sc_out, relay_m, relay_z,
                  wi, wo, z, om, h, hid, qr, kts, vsl, ksl, turned_q, turned_o, scores, dscores, pcat, dscat, cos_ref, sin_ref, turn_ref,
                  dot_heads, qt, dht, dkv, omt, ht, dyt, sc, gains, own_gain, gain_ref, load_sems, own_sems, send_sems, recv_sems,
                  share_send_sems, share_recv_sems):
    seq, dim = x_ref.shape
    ff = (wi.shape[PAIR] - dim - LANE) // PAIR
    position = chip_position()
    x, y, zc, core = position
    twin = device_at(x, y, zc, 1 - core)
    me = PAIR * x + core
    links, shared = Links(send_sems, recv_sems), Links(share_send_sems, share_recv_sems)
    stored = []
    spots, _ = around(position)
    h_out, m_out, y_out, z_out = {"y": (hy_a, hy_b), "z": (hz_a, hz_b)}, (mx_a, mx_b), {1: yx_b}, {(1, "y"): zy_b, (1, "z"): zz_b}
    middle = hid.at[1]
    begin, ready, peer, stages = gather_stages(links, position, wi_ref, wo_ref, wi, wo, load_sems)
    others = [(zc * SIDE + y, rem(me + k, ROW)) for k in range(1, ROW)]

    def spot(axis, o):
        return spots[axis, o % SIDE]

    def device(axis, o, index):
        moved = {"x": x, "y": y, "z": zc, axis: spot(axis, o)}
        return device_at(moved["x"], moved["y"], moved["z"], index)

    own_gain[ALL] = jnp.zeros(own_gain.shape, F32)
    count = sc_ref.shape[1]
    for f in range(ROW):
        @pl.when(me == f)
        def _():
            own_gain[0:PAIR, f * count:(f + 1) * count] = sc_ref[ALL].astype(F32)
    announce(others + [device(axis, o, index) for axis in "yz" for o in AROUND for index in range(PAIR)])
    begin()
    for k, far in enumerate(others):
        links.send(("sc",), own_gain, gains.at[me], far, batch=("sc",), whole=gains.at[pl.ds(0, OTHERS)])

    def keep(src, dst):
        copy = pltpu.make_async_copy(src, dst, own_sems.at[len(stored)])
        copy.start()
        stored.append(copy)

    def tokens(axis, o, index):
        return pl.ds(pl.multiple_of((PAIR * spot(axis, o) + index) * seq, seq), seq)

    def place(axis, o, index):
        return PAIR * spot(axis, o) + index

    def columns(axis, o):
        size = z.shape[PAIR] // ROW
        return lanes(((0 if axis == "y" else SIDE) + spot(axis, o)) * size, size)

    def several(batch, ref, n):
        whole = ref.at[pl.ds(0, n * seq if batch[0][0] in "yz" else n)]
        return dict(batch=batch, whole=whole)

    def send_h(l, axis):
        out = h_out[axis][l].at[place(axis, 0, core)]
        for by in BOTH:
            for index in range(PAIR):
                shared.send(("h", l, axis, by), ht.at[l, :, index], out, device(axis, by, index), lane=core, **several(("h", l, axis), h_out[axis][l], OTHERS))
        shared.send(("h", l, axis), ht.at[l, :, 1 - core], out, twin, **several(("h", l, axis), h_out[axis][l], OTHERS))
        keep(ht.at[l, :, core], out)

    def pass_h(l, axis, by, index):
        out = h_out[axis][l]
        shared.arrive(("h", l, axis, by), out.at[place(axis, -by, index)], index)
        part = out.at[place(axis, -by, index), pl.ds(1 - by, PAIR)]
        shared.send(("h", l, axis), part, part, device(axis, by, core), **several(("h", l, axis), out, OTHERS))

    def arrive_h(l):
        for axis in "yz":
            shared.arrive(("h", l, axis), h_out[axis][l].at[pl.ds(0, TRIO)])

    def row_block(l, o, index, part=None):
        size = omt.shape[1] // ROW
        start = (PAIR * spot("x", o) + index) * size
        if part is not None:
            size = size // PAIR
            start = start + part * size
        return omt.at[l, pl.ds(pl.multiple_of(start, 16), size)]

    def row_half(k):
        size = m_out[0].shape[1] // PAIR
        return pl.ds(k * size, size)

    def send_m(l):
        out = m_out[l].at[place("x", 0, core)]
        for k, by in enumerate(BOTH):
            for index in range(PAIR):
                shared.send(("mr", l, by), row_block(l, PAIR, index, k), relay_m.at[l, k, core], device("x", by, index), lane=core, **several(("m", l), m_out[l], OTHERS))
        for by in BOTH:
            for index in range(PAIR):
                shared.send(("m", l), row_block(l, by, index), out, device("x", by, index), **several(("m", l), m_out[l], OTHERS))
        shared.send(("m", l), row_block(l, 0, 1 - core), out, twin, **several(("m", l), m_out[l], OTHERS))
        keep(row_block(l, 0, core), out)

    def pass_m(l, by, index):
        k = (1 - by) // PAIR
        shared.arrive(("mr", l, by), relay_m.at[l, k, index], index)
        shared.send(("m", l), relay_m.at[l, k, index], m_out[l].at[place("x", -by, index), row_half(k)], device("x", by, core),
                    **several(("m2", l), m_out[l], PAIR))

    def arrive_m(l):
        shared.arrive(("m", l), m_out[l].at[pl.ds(0, OTHERS)])

    def token_half(axis, o, k):
        return pl.ds(pl.multiple_of((PAIR * spot(axis, o) + core) * seq + k * (seq // PAIR), seq // PAIR), seq // PAIR)

    def send_y(l):
        src, out = dy_ref, y_out[l].at[tokens("x", 0, core)]
        for by in BOTH:
            shared.send(("y", l, by), src, out, device("x", by, core), **several(("y", l), y_out[l], OTHERS))
        shared.send(("y", l), src, out, twin, **several(("y", l), y_out[l], OTHERS))
        keep(src, out)

    def pass_y(l, by):
        landed, part = y_out[l].at[tokens("x", -by, core)], y_out[l].at[token_half("x", -by, (1 - by) // PAIR)]
        shared.arrive(("y", l, by), landed)
        shared.send(("y2", l), part, part, device("x", by, core), **several(("y", l), y_out[l], OTHERS))
        shared.send(("y", l), landed, landed, twin, **several(("y", l), y_out[l], OTHERS))

    def far_y(l):
        landed = y_out[l].at[tokens("x", PAIR, core)]
        shared.arrive(("y2", l), landed)
        shared.send(("y", l), landed, landed, twin, **several(("y", l), y_out[l], OTHERS))

    def arrive_y(l):
        shared.arrive(("y", l), y_out[l].at[pl.ds(0, SIDE * seq)])

    def push_z(l, axis, o, ready):
        out = z_out[l, axis].at[tokens(axis, 0, core)]
        batch = several(("z", l, axis), z_out[l, axis], ROW)

        def start():
            if o != PAIR:
                shared.send(("z", l, axis, o), z.at[l, :, columns(axis, o)], out, device(axis, o, core), **batch)
                return
            for k, by in enumerate(BOTH):
                shared.send(("zr", l, axis, by), z.at[l, pl.ds(k * (seq // PAIR), seq // PAIR), columns(axis, PAIR)], relay_z.at[l, "yz".index(axis), k],
                            device(axis, by, core), **batch)

        if ready is None:
            start()
        else:
            pl.when(ready)(start)

    def own_part(l, axis):
        out, mine = z_out[l, axis].at[tokens(axis, 0, core)], z.at[l, :, columns(axis, 0)]
        shared.send(("z", l, axis), mine, out, twin, **several(("z", l, axis), z_out[l, axis], ROW))
        keep(mine, out)

    def send_z(l, axis):
        for o in (PAIR, 1, -1):
            push_z(l, axis, o, spot(axis, o) != 0 if axis == "y" else None)
        if axis == "z":
            own_part(l, axis)

    def late_z():
        for axis, out in (("z", zz_a), ("y", zy_a)):
            for o in AROUND:
                def start():
                    shared.send(("late", axis), z.at[0, :, columns(axis, o)], out.at[tokens(axis, 0, core)], device(axis, o, core),
                                batch=("late", axis), whole=out.at[pl.ds(0, TRIO * seq)])

                if axis == "y":
                    pl.when(spot("y", o) != 0)(start)
                else:
                    start()

    def settle_late():
        shared.arrive(("late", "z"), zz_a.at[pl.ds(0, TRIO * seq)])
        _, leaving = shared.sent.pop(("late", "y"))

        def left(n):
            part = zy_a.at[pl.ds(0, n * seq)]
            pltpu.make_async_copy(part, part, share_send_sems.at[leaving]).wait()

        @pl.when(y == 0)
        def _():
            left(TRIO)

        @pl.when(y != 0)
        def _():
            left(PAIR)
            shared.arrive(("late", "y"), zy_a.at[pl.ds(0, TRIO * seq)])

    def rest_z(l):
        for o in (PAIR, 1, -1):
            push_z(l, "y", o, spot("y", o) == 0)
        own_part(l, "y")

    def pass_z(l, axis, by):
        k = (1 - by) // PAIR
        half = relay_z.at[l, "yz".index(axis), k]
        shared.arrive(("zr", l, axis, by), half)
        shared.send(("z2", l, axis), half, z_out[l, axis].at[token_half(axis, -by, k)], device(axis, by, core), **several(("z", l, axis), z_out[l, axis], ROW))

    def twin_z(l, axis, by):
        landed = z_out[l, axis].at[tokens(axis, -by, core)]
        shared.arrive(("z", l, axis, by), landed)
        shared.send(("z", l, axis), landed, landed, twin, **several(("z", l, axis), z_out[l, axis], ROW))

    def far_z(l, axis):
        landed = z_out[l, axis].at[tokens(axis, PAIR, core)]
        shared.arrive(("z2", l, axis), landed)
        shared.send(("z", l, axis), landed, landed, twin, **several(("z", l, axis), z_out[l, axis], ROW))

    def arrive_z(l, axis):
        shared.arrive(("z", l, axis), z_out[l, axis].at[pl.ds(0, SIDE * seq)])

    def send_scale(l):
        for far in others:
            shared.send(("scale", l), sc.at[l], sc_out.at[l, me], far, batch=("scale", l), whole=sc_out.at[l, pl.ds(0, OTHERS)])
        keep(sc.at[l], sc_out.at[l, me])

    def arrive_scale(l):
        shared.arrive(("scale", l), sc_out.at[l, pl.ds(0, OTHERS)])

    gains[me] = own_gain[ALL]
    z[:, :, wi.shape[PAIR]:] = jnp.zeros((PAIR, seq, z.shape[PAIR] - wi.shape[PAIR]), BF)
    entry = (x_ref, hid.at[0])
    angle = lax.broadcasted_iota(jnp.int32, (seq, LANE), 0).astype(F32) * freq_ref[0:1]
    for half in range(PAIR):
        cos_ref[:, LANE * half:LANE * (half + 1)] = jnp.cos(angle)
        sin_ref[:, LANE * half:LANE * (half + 1)] = jnp.sin(angle)
    lane = lax.broadcasted_iota(jnp.int32, turn_ref.shape, 1)
    down = lax.broadcasted_iota(jnp.int32, turn_ref.shape, 0) - lane
    low = rem(lane, HEAD) < BAND
    turn_ref[ALL] = jnp.where(low & (down == BAND), -1.0, jnp.where(jnp.logical_not(low) & (down == -BAND), 1.0, ZERO)).astype(BF)
    kts[ALL] = jnp.zeros(kts.shape, BF)
    pcat[ALL] = jnp.zeros(pcat.shape, BF)
    dscat[ALL] = jnp.zeros(dscat.shape, BF)

    def normalise(l, src):
        @pl.loop(0, seq // BAND, unroll=SIDE)
        def _(r):
            rows = pl.ds(pl.multiple_of(r * BAND, BAND), BAND)
            v = src[rows].astype(F32)
            v = v - jnp.mean(v, axis=-1, keepdims=True)
            var = jnp.mean(v * v, axis=-1, keepdims=True)
            h[l, rows] = (v * lax.rsqrt(var + 1e-6) * gain_ref[l:l + 1]).astype(BF)

    def project(l):
        strip = wi.shape[PAIR] // 5

        @pl.loop(0, 5)
        def _(i):
            at = lanes(i * strip, strip)
            z[l, :, at] = product(h[l], wi[l, :, at]).astype(BF)

    def heads(l):
        cos, sin = cos_ref[ALL], sin_ref[ALL]
        for g in range(dim // WIDE):
            q = z[l, :, g * WIDE:(g + 1) * WIDE]
            qr[l, :, g * WIDE:(g + 1) * WIDE] = ((q.astype(F32) * cos + product(q, turn_ref[ALL]) * sin) * 0.125).astype(BF)
        kv = z[l, :, dim:dim + LANE]
        turned = kv.astype(F32) * cos[:, :LANE] + product(kv, turn_ref[:LANE, :LANE]) * sin[:, :LANE]
        first = lax.broadcasted_iota(jnp.int32, turned.shape, 1) < HEAD
        key_lo = jnp.where(first, turned, ZERO)
        val_hi = jnp.where(first, ZERO, kv.astype(F32))
        return key_lo, pltpu.roll(key_lo, HEAD, 1), pltpu.roll(val_hi, HEAD, 1), val_hi

    def slot_rows(ref, lo, hi):
        zero = jnp.zeros((seq, LANE), BF)
        lo, hi = lo.astype(BF), hi.astype(BF)
        for i, (left, right) in enumerate(((lo, zero), (hi, zero), (zero, lo), (zero, hi))):
            ref[i * seq:(i + 1) * seq, :LANE] = left
            ref[i * seq:(i + 1) * seq, LANE:] = right

    def slot_cols(ref, lo):
        flat = lo.T[:HEAD].astype(BF)
        for i in range(SIDE):
            ref[HEAD * i:HEAD * (i + 1), i * seq:(i + 1) * seq] = flat

    def chances(i, half):
        at = slice(LANE * half, LANE * (half + 1))
        blocks = [pl.ds(pl.multiple_of(i * seq + LANE * k, LANE), LANE) for k in range(half + 1)]
        s = [scores[keys, at] for keys in blocks]
        lower = lax.broadcasted_iota(jnp.int32, s[-1].shape, 1) >= lax.broadcasted_iota(jnp.int32, s[-1].shape, 0)
        s[-1] = jnp.where(lower, s[-1], -1e30)
        top = functools.reduce(jnp.maximum, [jnp.max(v, axis=0, keepdims=True) for v in s])
        e = [jnp.exp(v - top) for v in s]
        scale = 1.0 / sum(jnp.sum(v, axis=0, keepdims=True) for v in e)
        return at, [(keys, v * scale) for keys, v in zip(blocks, e)]

    def attend(l):
        key_lo, key_hi, val_lo, _ = heads(l)
        slot_rows(ksl, key_lo, key_hi)
        slot_cols(kts, val_lo)
        flip(lambda at: qr[l, :, lanes(at, WIDE)], qt, dim)

        @pl.loop(0, dim // WIDE)
        def _(g):
            rows = pl.ds(pl.multiple_of(g * WIDE, WIDE), WIDE)
            scores[ALL] = product(ksl[ALL], qt[rows])

            @pl.loop(0, SIDE)
            def _(i):
                for half in range(PAIR):
                    at, blocks = chances(i, half)
                    for keys, p in blocks:
                        pcat[keys, at] = p.astype(BF)
            flat = product(kts[ALL], pcat[ALL]).astype(BF)
            omt[l, rows] = flat
            om[:, lanes(g * WIDE, WIDE)] = flat.T

    def mlp(l):
        @pl.loop(0, seq // BAND)
        def _(r):
            rows = pl.ds(pl.multiple_of(r * BAND, BAND), BAND)

            @pl.loop(0, ff // STRIP)
            def _(i):
                gate = z[l, rows, lanes(dim + LANE + i * STRIP, STRIP)].astype(F32)
                up = z[l, rows, lanes(dim + LANE + ff + i * STRIP, STRIP)].astype(F32)
                om[rows, lanes(dim + i * STRIP, STRIP)] = (gate * jax.nn.sigmoid(gate) * up).astype(BF)

    def put_out(l, dst):
        for n in range(dim // WIDE):
            cols = slice(n * WIDE, (n + 1) * WIDE)
            total = product(om[ALL], wo[l, :, cols])
            dst[:, cols] = (entry[l][:, cols].astype(F32) + total).astype(BF)

    def flip(src, dst, width, first=0):
        @pl.loop(first // WIDE, width // WIDE)
        def _(i):
            dst[pl.ds(pl.multiple_of(i * WIDE, WIDE), WIDE)] = src(i * WIDE).T

    upstream = (middle, dy_ref)

    def back_out(l):
        dy = upstream[l]
        flip(lambda at: dy[:, lanes(at, WIDE)], dyt, dim)

        @pl.loop(0, wo.shape[1] // dim)
        def _(n):
            rows = pl.ds(pl.multiple_of(n * dim, dim), dim)
            part = product(wo[l, rows], dyt[ALL]).astype(BF)
            om[:, lanes(n * dim, dim)] = part.T

            @pl.when(n == 0)
            def _():
                dot_heads[ALL] = part

    def back_mlp(l):
        @pl.loop(0, seq // BAND)
        def _(r):
            rows = pl.ds(pl.multiple_of(r * BAND, BAND), BAND)

            @pl.loop(0, ff // STRIP)
            def _(i):
                gate_at, up_at = lanes(dim + LANE + i * STRIP, STRIP), lanes(dim + LANE + ff + i * STRIP, STRIP)
                gate, up = z[l, rows, gate_at].astype(F32), z[l, rows, up_at].astype(F32)
                d = om[rows, lanes(dim + i * STRIP, STRIP)].astype(F32)
                sig = jax.nn.sigmoid(gate)
                du = d * up
                z[l, rows, gate_at] = (du * sig + du * gate * (sig * (1.0 - sig))).astype(BF)
                z[l, rows, up_at] = (d * (gate * sig)).astype(BF)

    def back_heads(l):
        key_lo, key_hi, val_lo, val_hi = heads(l)
        slot_rows(ksl, key_lo, key_hi)
        slot_rows(vsl, val_lo, val_hi)
        slot_cols(kts, key_lo)
        dkv[ALL] = jnp.zeros(dkv.shape, F32)
        flip(lambda at: qr[l, :, lanes(at, WIDE)], qt, dim)
        for at in range(0, dim, LANE):
            pair = slice(at, at + LANE)
            turned_q[:, pair] = pltpu.roll(qr[l, :, pair].astype(F32), HEAD, 1).astype(BF)
            turned_o[:, pair] = pltpu.roll(om[:, pair].astype(F32), HEAD, 1).astype(BF)

    def back_quad(l):
        @pl.loop(0, dim // WIDE)
        def _(g):
            quad(l, g)

    def quad(l, g):
        cols = pl.ds(pl.multiple_of(g * WIDE, WIDE), WIDE)
        scores[ALL] = product(ksl[ALL], qt[cols])
        dscores[ALL] = product(vsl[ALL], dot_heads[cols])

        @pl.loop(0, SIDE)
        def _(i):
            for half in range(PAIR):
                at, blocks = chances(i, half)
                given = [p * dscores[keys, at].astype(BF).astype(F32) for keys, p in blocks]
                total = sum(jnp.sum(v, axis=0, keepdims=True) for v in given)
                for (keys, p), v in zip(blocks, given):
                    pcat[keys, at] = p.astype(BF)
                    dscat[keys, at] = (v - p * total).astype(BF)
        dq = product(kts[ALL], dscat[ALL]).astype(BF).T
        back = dq.astype(F32) * cos_ref[ALL] - product(dq, turn_ref[ALL]) * sin_ref[ALL]
        z[l, :, cols] = (back * 0.125).astype(BF)
        for i in range(SIDE):
            keys, pair = slice(i * seq, (i + 1) * seq), lanes(g * WIDE + i // PAIR * LANE, LANE)
            even = i % PAIR == 0
            dkv[0] += product(dscat[keys], qr[l, :, pair] if even else turned_q[:, pair])
            dkv[1] += product(pcat[keys], turned_o[:, pair] if even else om[:, pair])

    def back_keys(l):
        dk = dkv[0].astype(BF)
        turned = dk.astype(F32) * cos_ref[:, :LANE] - product(dk, turn_ref[:LANE, :LANE]) * sin_ref[:, :LANE]
        first = lax.broadcasted_iota(jnp.int32, turned.shape, 1) < HEAD
        z[l, :, dim:dim + LANE] = jnp.where(first, turned, dkv[1]).astype(BF)

    def back_in(l, half):
        width = wi.shape[PAIR] // 5
        at = slice(PAIR * half * width, (PAIR + TRIO * half) * width)
        part = product(wi[l, :, at], z[l, :, at], ((1,), (1,)))
        dht[ALL] = dht[ALL] + part if half else part

    def back_norm(l):
        dy, dst = upstream[l], (gx_ref, middle)[l]
        for i in range(dim // WIDE):
            cols = slice(i * WIDE, (i + 1) * WIDE)
            h[l, :, cols] = dht[cols].T.astype(BF)
        sc[l] = jnp.zeros(sc.shape[1:], F32)

        @pl.loop(0, seq // BAND, unroll=SIDE)
        def _(r):
            rows = pl.ds(pl.multiple_of(r * BAND, BAND), BAND)
            v = entry[l][rows].astype(F32)
            v = v - jnp.mean(v, axis=-1, keepdims=True)
            scale = lax.rsqrt(jnp.mean(v * v, axis=-1, keepdims=True) + 1e-6)
            hat = v * scale
            d = h[l, rows].astype(F32)
            each = (d * hat).reshape(SIDE, ROW, dim)
            sc[l] += (each[0] + each[1]) + (each[PAIR] + each[TRIO])
            d = d * gain_ref[l:l + 1]
            d = scale * (d - jnp.mean(d, axis=-1, keepdims=True) - hat * jnp.mean(d * hat, axis=-1, keepdims=True))
            dst[rows] = (dy[rows].astype(F32) + d.astype(BF).astype(F32)).astype(BF)

    def do_norm(l):
        if l == 0:
            links.arrive(("sc",), gains.at[pl.ds(0, OTHERS)])
            gain_ref[ALL] = jnp.sum(gains[ALL], axis=0)
        normalise(l, entry[l])
        for i in range(dim // WIDE):
            flat = h[l, :, i * WIDE:(i + 1) * WIDE].T
            size = ht.shape[TRIO]
            for b in range(ROW):
                lo, hi = max(b * size, i * WIDE), min((b + 1) * size, (i + 1) * WIDE)
                if lo < hi:
                    ht[l, b // PAIR, b % PAIR, lo - b * size:hi - b * size] = flat[lo - i * WIDE:hi - i * WIDE]

    def do_project(l):
        ready(PAIR * l)
        project(l)

    def do_mlp(l):
        mlp(l)
        flip(lambda at: om[:, lanes(at, WIDE)], omt.at[l], om.shape[1], dim)

    def do_put(l):
        ready(PAIR * l + 1)
        put_out(l, hid.at[0] if l == 0 else y_ref)

    stages.update(
        norm=do_norm, project=do_project, attend=attend, mlp=do_mlp, put=do_put, back_out=back_out, back_mlp=back_mlp, back_heads=back_heads,
        back_quad=back_quad, back_keys=back_keys, back_in=back_in, back_norm=back_norm, send_h=send_h, pass_h=pass_h, send_m=send_m,
        pass_m=pass_m, send_y=send_y, pass_y=pass_y, far_y=far_y, send_z=send_z, rest_z=rest_z, late_z=late_z, pass_z=pass_z, twin_z=twin_z, far_z=far_z,
        send_scale=send_scale, own_z=lambda: keep(z.at[0], z_a), own_y=lambda: keep(middle, dy_a))
    for kind, *task in order:
        stages[kind](*task)
    for l in range(PAIR):
        arrive_h(l)
        arrive_m(l)
        arrive_scale(l)
    arrive_y(1)
    for l, axis in z_out:
        arrive_z(l, axis)
    settle_late()
    for copy in stored:
        copy.wait()
    shared.drain()
    links.drain()


def run_layers(x, dy, scale, w_in, w_out, freq, starts=(ZERO, 10.0, 20.0, 30.0)):
    seq, dim = x.shape
    proj, cat = w_in.shape[PAIR], ROW * w_out.shape[1]
    wide = proj + LANE
    hbm, vmem = pl.BlockSpec(memory_space=pltpu.HBM), pl.BlockSpec(memory_space=pltpu.VMEM)
    out = lambda *shape, dtype=BF: jax.ShapeDtypeStruct(shape, dtype)
    buffer = lambda *shape, dtype=BF: pltpu.VMEM(shape, dtype)
    sem = pltpu.SemaphoreType.DMA
    line = ROW * seq
    return pl.pallas_call(
        functools.partial(layers_kernel, layers_order(*w_in.shape[1:], *w_out.shape[1:], seq, starts)),
        out_shape=(out(seq, dim), out(seq, dim), *[out(ROW, SIDE, dim // ROW, seq)] * SIDE, *[out(ROW, cat // ROW, seq)] * PAIR, out(line, dim),
                   *[out(line, wide // ROW)] * SIDE, out(seq, wide), out(seq, dim), out(PAIR, ROW, ROW, dim, dtype=F32),
                   out(PAIR, PAIR, PAIR, cat // 16, seq), out(PAIR, PAIR, PAIR, seq // PAIR, wide // ROW)),
        in_specs=[vmem, hbm, hbm] + [vmem] * TRIO,
        out_specs=[vmem] * PAIR + [hbm] * 16,
        scratch_shapes=[
            buffer(PAIR, dim, proj), buffer(PAIR, cat, dim), buffer(PAIR, seq, wide), buffer(seq, cat), buffer(PAIR, seq, dim),
            buffer(PAIR, seq, dim), buffer(PAIR, seq, dim),
            buffer(WIDE, SIDE * seq), buffer(SIDE * seq, WIDE), buffer(SIDE * seq, WIDE), buffer(seq, dim), buffer(seq, dim),
            buffer(SIDE * seq, seq, dtype=F32), buffer(SIDE * seq, seq, dtype=F32), buffer(SIDE * seq, seq), buffer(SIDE * seq, seq),
            buffer(seq, WIDE, dtype=F32), buffer(seq, WIDE, dtype=F32), buffer(WIDE, WIDE),
            buffer(dim, seq), buffer(dim, seq), buffer(dim, seq, dtype=F32), buffer(PAIR, seq, LANE, dtype=F32),
            buffer(PAIR, cat, seq), buffer(PAIR, SIDE, PAIR, dim // ROW, seq), buffer(dim, seq), buffer(PAIR, ROW, dim, dtype=F32),
            buffer(ROW, ROW, dim, dtype=F32), buffer(ROW, dim, dtype=F32), buffer(ROW, dim, dtype=F32),
            sem((SIDE,)), sem((13,)), sem((15,)), sem((107,)), sem((15,)), sem((HEAD,)),
        ],
        compiler_params=pltpu.CompilerParams(collective_id=PAIR, has_side_effects=True, vmem_limit_bytes=67043328),
        name="run_layers",
    )(scale, w_in, w_out, x, dy, freq)


PARTS = (("i", "x", "z", "y", 0, STRIP), ("i", "x", "z", "y", STRIP, 384), ("i", "x", "y", "z", 0, STRIP), ("i", "x", "y", "z", STRIP, 384),
         ("o", "y", "z", "y", 0, 384), ("o", "z", "y", "z", 384, 384))


def reduce_order(rows, rows_b, starts):
    rate = 11650.0
    tasks = []
    sizes = {"y": WIDE * 896 / (PAIR * rate), "z": WIDE * 896 / (PAIR * rate), "x": WIDE * 768 / (PAIR * rate)}
    tasks.append((("swap", "x"), (0, 0), starts[PAIR], [], [], [(("x", by), sizes["x"] * n) for by, n in ((1, 1), (-1, 1), (1, PAIR))], SHORT))
    tasks.append((("swap", "z"), (0, 0), starts[TRIO], [], [], [("chip", 1.6)] * SIDE, 0.4))
    tasks.append((("swap", "y"), (0, 0), starts[TRIO], [], [], [(("y", by), sizes["y"] * n / PAIR) for by, n in ((1, 1), (-1, 1), (1, PAIR))] + [("chip", 1.6)] * SIDE, 0.4))
    for axis in "yx":
        for i, o in enumerate(AROUND):
            tasks.append((("near", axis, o), (0, PAIR), ZERO, [(("swap", axis), i)], [], [("chip", 1.6)], QUICK))
    tasks.append((("fetch", 0), (5, 0), ZERO, [], [("make", 1, len(PARTS) - 1)], [], QUICK))
    for l in (1, 0):
        late = 1 - l
        for c, (kind, first, then, last, at, width) in enumerate(PARTS):
            needs, cost = [], 1.6 * width / STRIP
            if l == 0:
                needs = [(("swap", "z"), k) for k in range(SIDE)] if (kind, last) == ("i", "z") else [
                    (("near", last if kind == "i" else "x", o), 0) for o in AROUND]
            tasks.append((("make", l, c), (9 * late, c), starts[late], needs, [] if l else [("fetch", 0)], [], cost))
            full = SIDE * SIDE * (rows if kind == "i" else rows_b) * width / rate
            sends = [[((first, by), full / ROW) for by in BOTH], [((first, by), full / SIDE) for by in BOTH],
                     [((then, o), full / 16) for o in (1, -1, 1)], []]
            piece = full / 16
            sends += [[((then, by), piece) for by in BOTH], [((then, 1 - PAIR * (c % PAIR)), piece)], [((last, by), SIDE * piece) for by in BOTH],
                      [((last, by), PAIR * piece) for by in BOTH], []]
            for s in range(9):
                task = ("sum", l, c, s)
                needs = [(("sum", l, c, s - 1), k) for k in range(len(sends[s - 1]))] if s else []
                tasks.append((task, (late, -s), ZERO, needs, [("make", l, c)] if s == 0 else [("sum", l, c, s - 1)], sends[s], SHORT))
    return plan(tasks)


def reduce_kernel(order, *refs):
    hy, hz, mx = refs[0:PAIR], refs[PAIR:SIDE], refs[SIDE:6]
    yx1, zy1, zz1, zy0, zz0, z0, y0, sc = refs[6:14]
    oa, ob = refs[14:16]
    n = len(PARTS)
    total, half, full, small, front = (refs[16 + k * n:16 + (k + 1) * n] for k in range(5))
    (hbuf, zbuf, mbuf, ybuf, scbuf, ssem, rsem, isem, osem, fsem) = refs[16 + 5 * n:]
    position = chip_position()
    x, y, zc, core = position
    place = {"x": x, "y": y, "z": zc}
    twin = device_at(x, y, zc, 1 - core)
    spots, peers = around(position)

    def spot(axis, o):
        return spots[axis, o % SIDE]

    def peer(axis, o):
        return peers[axis, o % SIDE]

    seq, wide = z0.shape
    own = wide // ROW
    loads, moving = {}, []

    def load(key, src, dst):
        copy = pltpu.make_async_copy(src, dst, isem.at[len(moving)])
        moving.append(key)
        copy.start()
        loads[key] = copy

    def fetch(l):
        if l:
            load(("z", 1, "y"), zy1, zbuf.at[1, 0])
        load(("h", l, "y"), hy[l], hbuf.at[l, 0])
        if l:
            load(("z", 1, "z"), zz1, zbuf.at[1, 1])
        load(("h", l, "z"), hz[l], hbuf.at[l, 1])
        load(("m", l), mx[l], mbuf.at[l])
        if l:
            load(("y", 1), yx1, ybuf.at[1])
        load(("s", l), sc.at[l], scbuf.at[l])

    fetch(1)
    done = set()

    def loaded(*keys):
        for key in keys:
            if key not in done:
                loads[key].wait()
                done.add(key)

    announce([peer(axis, o) for axis in "xyz" for o in AROUND] + [twin])
    links = Links(ssem, rsem)

    def columns(axis, o):
        return lanes(((0 if axis == "y" else SIDE) + spot(axis, o)) * own, own)

    def tokens(axis, o, index):
        return pl.ds(pl.multiple_of((PAIR * spot(axis, o) + index) * seq, seq), seq)

    def target(axis):
        return ybuf.at[0] if axis == "x" else zbuf.at[0, "yz".index(axis)]

    def seven(axis, n):
        return dict(batch=("swap", axis), whole=target(axis).at[pl.ds(0, n * seq)])

    batches = {axis: seven(axis, OTHERS if axis == "x" else SIDE) for axis in "xyz"}

    def to_twin(axis, src, o):
        near_core = device_at(x, y, zc, 1 - core)
        links.send(("near", axis), src, target(axis).at[tokens(axis, -o, core)], near_core, **batches[axis])

    def swap(axis):
        def part(o):
            return y0 if axis == "x" else z0.at[:, columns(axis, o)]

        mine = target(axis).at[tokens(axis, 0, core)]
        if axis == "x":
            for o in AROUND:
                links.send(("swap", axis, o), y0, mine, peer(axis, o), **batches[axis])
        elif axis == "y":
            for o in AROUND:
                @pl.when(spot("y", o) == 0)
                def _():
                    links.send(("swap", axis, o), part(o), mine, device_at(x, spot("y", o), zc, core), batch=("first",), whole=mine)
        to_twin(axis, part(0), 0)
        load(("own", axis), part(0), mine)
        if axis == "z":
            for o in AROUND:
                landed = zz0.at[tokens(axis, -o, core)]
                to_twin(axis, landed, o)
                load(("far", axis, o), landed, target(axis).at[tokens(axis, -o, core)])
        if axis == "y":
            @pl.when(y != 0)
            def _():
                for k, o in enumerate(AROUND):
                    landed = zy0.at[tokens(axis, -o, core)]
                    to_twin(axis, landed, o)
                    pltpu.make_async_copy(landed, target(axis).at[tokens(axis, -o, core)], fsem.at[k]).start()

    def near(axis, o):
        def go():
            landed = target(axis).at[tokens(axis, -o, core)]
            links.arrive(("swap", axis, o), landed)
            to_twin(axis, landed, o)

        if axis == "x":
            go()
        else:
            pl.when(y == 0)(go)

    def joined(axis):
        if axis not in done:
            done.add(axis)
            loaded(("own", axis))
            if axis == "z":
                loaded(*[("far", axis, o) for o in AROUND])
            if axis == "y":
                @pl.when(y != 0)
                def _():
                    for k, o in enumerate(AROUND):
                        landed = target(axis).at[tokens(axis, -o, core)]
                        pltpu.make_async_copy(landed, landed, fsem.at[k]).wait()
            links.arrive(("near", axis), target(axis).at[pl.ds(0, SIDE * seq)])

    def joined_lanes(ref, l, i):
        return jnp.concatenate([ref[l, i, k].reshape(-1, ref.shape[-1]) for k in range(ROW)], axis=1)

    def make(l, c):
        kind, first, then, last, at, width = PARTS[c]
        if kind == "i":
            i = "yz".index(last)
            loaded(("h", l, last))
            if l:
                loaded(("z", l, last))
            else:
                joined(last)
            size = total[c].shape[TRIO]
            for lo in range(0, width, WIDE):
                hi = min(width, lo + WIDE)
                part = product(joined_lanes(hbuf, l, i), zbuf[l, i, :, at + lo:at + hi])
                for r in range(16):
                    total[c][l, r // SIDE, r % SIDE, :, lo:hi] = part[r * size:(r + 1) * size]
            return
        loaded(("m", l), ("s", l))
        if l:
            loaded(("y", l))
        else:
            joined("x")
        part = product(jnp.concatenate([mbuf[l, k] for k in range(ROW)], axis=1), ybuf[l, :, at:at + width])
        size = total[c].shape[TRIO]

        def put(r, value):
            total[c][(l, r // SIDE, r % SIDE) if first == "y" else (l, r % SIDE, r // SIDE)] = value

        for r in range(part.shape[0] // size):
            put(r, part[r * size:(r + 1) * size])
        gain = jnp.sum(jnp.sum(scbuf[l, :, :, at:at + width], axis=0), axis=0, keepdims=True)
        row = lax.broadcasted_iota(jnp.int32, (size, width), 0)
        put(15, jnp.where(row == 0, gain, ZERO))

    def area(l, c, o, whole):
        kind, first, then, last, at, width = PARTS[c]
        inner = (spot(then, whole) if isinstance(whole, int) else whole)
        outer = spot(last, o)
        if kind == "i":
            cols = lanes(((0 if last == "y" else SIDE) + outer) * own + at, width)
            return oa.at[l, inner, :, cols]
        cols = pl.ds(at, width)
        return ob.at[l, outer, inner, :, cols] if last == "y" else ob.at[l, inner, outer, :, cols]

    def add(l, c, s):
        kind, first, then, last, at, width = PARTS[c]
        t = total[c].at[l]
        way = 1 - PAIR * (c % PAIR)
        sums = dict(batch=(l, c, 0), whole=t)
        wide_ones = dict(batch=(l, c, 1), whole=t.at[pl.ds(0, TRIO)])
        narrow = dict(batch=(l, c, PAIR), whole=t.at[0, pl.ds(0, PAIR)])
        if s == 0:
            far = t.at[spot(first, PAIR)]
            for k, by in enumerate(BOTH):
                links.send((l, c, "half"), far.at[pl.ds(PAIR * k, PAIR)], half[c].at[l, k], peer(first, by), **sums)
        elif s == 1:
            links.arrive((l, c, "half"), half[c].at[l])
            for k, by in enumerate(BOTH):
                mine = t.at[spot(first, by)]
                add_into(mine.at[pl.ds(PAIR * k, PAIR)], half[c].at[l, k])
                links.send((l, c, "full"), mine, full[c].at[l, k], peer(first, by), **sums)
        elif s == PAIR:
            mine = t.at[spot(first, 0)]
            links.arrive((l, c, "full"), full[c].at[l])
            for k in range(PAIR):
                add_into(mine, full[c].at[l, k])
            for k, o in enumerate(AROUND):
                links.send((l, c, "small"), mine.at[spot(then, o)], small[c].at[l, k], peer(then, o), **wide_ones)
        elif s == TRIO:
            links.arrive((l, c, "small"), small[c].at[l])
            mine = t.at[spot(first, 0), spot(then, 0)]
            front[c][l] = (mine[ALL] + small[c][l, 0]) + (small[c][l, 1] + small[c][l, PAIR])
        elif s == SIDE:
            src, dst = front[c].at[l], area(l, c, 0, 0)
            for by in BOTH:
                links.send((l, c, "a1"), src, dst, peer(then, by), **narrow)
            copy = pltpu.make_async_copy(src, dst, osem.at[l, c])
            copy.start()
            loads["front", l, c] = copy
        elif s == 5:
            links.arrive((l, c, "a1"), t.at[0, pl.ds(0, PAIR)])
            landed = area(l, c, 0, -way)
            links.send((l, c, "b1"), landed, landed, peer(then, way), **wide_ones)
        elif s == 6:
            loaded(("front", l, c))
            links.arrive((l, c, "b1"), area(l, c, 0, PAIR))
            line = area(l, c, 0, slice(None))
            for by in BOTH:
                links.send((l, c, "a2"), line, line, peer(last, by), **wide_ones)
        elif s == OTHERS:
            links.arrive((l, c, "a2"), t.at[pl.ds(0, PAIR)])
            for k, by in enumerate(BOTH):
                part = area(l, c, -by, pl.ds(PAIR * k, PAIR))
                links.send((l, c, "a3"), part, part, peer(last, by), **sums)
        else:
            links.arrive((l, c, "a3"), area(l, c, PAIR, slice(None)))

    stages = {"swap": swap, "near": near, "fetch": fetch, "make": make, "sum": add}
    for kind, *task in order:
        stages[kind](*task)
    _, leaving = links.sent.pop(("first",))

    @pl.when(y != 0)
    def _():
        mine = target("y").at[tokens("y", 0, core)]
        pltpu.make_async_copy(mine, mine, ssem.at[leaving]).wait()

    links.drain()


def add_into(dst, src):
    @pl.loop(0, dst.shape[0])
    def _(i):
        if len(dst.shape) == SIDE:
            for j in range(dst.shape[1]):
                dst[i, j] += src[i, j]
        else:
            dst[i] += src[i]


def around(position):
    place, core = dict(zip("xyz", position)), position[TRIO]
    spots = {(axis, o): step(place[axis], o) for axis in "xyz" for o in range(SIDE)}
    peers = {}
    for axis in "xyz":
        for o in range(1, SIDE):
            moved = {**place, axis: spots[axis, o]}
            peers[axis, o] = device_at(moved["x"], moved["y"], moved["z"], core)
    return spots, peers


def reduce_gradients(operands, starts=(ZERO, ZERO, 8.0, ZERO)):
    hbm = pl.BlockSpec(memory_space=pltpu.HBM)
    h_rows, m_rows, y_cols, z_cols, z_own, y_own, scale_parts = operands
    part, part_b = h_rows[0].shape[PAIR] // SIDE, (m_rows[0].shape[1] + BAND) // 16
    (line, dim), wide = y_cols.shape, z_own.shape[1]
    out = lambda *shape: jax.ShapeDtypeStruct(shape, F32)
    sem = pltpu.SemaphoreType.DMA

    def buffers(*lead):
        return [pltpu.VMEM((PAIR, *lead, part if e[0] == "i" else part_b, e[5]), F32) for e in PARTS]

    return pl.pallas_call(
        functools.partial(reduce_kernel, reduce_order(part, part_b, starts)),
        out_shape=(out(PAIR, SIDE, part, wide), out(PAIR, SIDE, SIDE, part_b, dim)),
        in_specs=[hbm] * 14,
        out_specs=[hbm] * PAIR,
        scratch_shapes=[
            *buffers(SIDE, SIDE), *buffers(PAIR, PAIR), *buffers(PAIR, SIDE), *buffers(TRIO), *buffers(),
            pltpu.VMEM((PAIR, PAIR, *h_rows[0].shape), BF), pltpu.VMEM((PAIR, PAIR, line, wide // ROW), BF), pltpu.VMEM((PAIR, *m_rows[0].shape), BF),
            pltpu.VMEM((PAIR, line, dim), BF), pltpu.VMEM(scale_parts.shape, F32),
            sem((40,)), sem((96,)), sem((17,)), sem((PAIR, len(PARTS))), sem((TRIO,)),
        ],
        compiler_params=pltpu.CompilerParams(collective_id=1, has_side_effects=True, vmem_limit_bytes=67043328),
        name="reduce_gradients",
    )(*h_rows, *m_rows, y_cols, *z_cols, z_own, y_own, scale_parts)


def solution(mesh):
    fsdp_size = mesh.shape["fsdp"]
    batch_spec = P(("dp", "fsdp"), None, None)
    scale_spec = P(None, "fsdp")
    weight_spec = P(None, "fsdp", None)

    def device_step(x_in, grad_y, norm_scale, w_in, w_out):
        n_layers = w_in.shape[0]
        seq_len, model_dim = x_in.shape[1:]
        proj_dim = w_in.shape[PAIR]
        ff_dim = w_out.shape[1] * fsdp_size - model_dim
        head_dim = (proj_dim - model_dim - PAIR * ff_dim) // PAIR
        rows, rows_out = norm_scale.shape[1], w_out.shape[1]
        half_dim = head_dim // PAIR
        freq = 10000.0 ** (-np.arange(half_dim, dtype=np.float32) * 2.0 / head_dim)
        freq = jnp.asarray(np.tile(freq.astype(np.float32), (ROW, LANE // half_dim)))
        hidden, grad_hidden, *rest = run_layers(x_in[0], grad_y[0], norm_scale, w_in, w_out, freq)
        in_sums, out_sums = reduce_gradients((rest[0:SIDE], rest[SIDE:6], rest[6], rest[OTHERS:11], rest[11], rest[12], rest[13]))
        in_grads = in_sums.reshape(n_layers, rows, -1)[:, :, :proj_dim]
        out_rows = out_sums.reshape(n_layers, -1, model_dim)
        scale_grads = lax.dynamic_slice(out_rows[:, rows_out], (0, lax.axis_index("fsdp") * rows), (n_layers, rows))
        out_grads = out_rows[:, :rows_out]
        return hidden[None], grad_hidden[None], scale_grads, in_grads, out_grads

    return jax.shard_map(
        device_step,
        mesh=mesh,
        in_specs=(batch_spec, batch_spec, scale_spec, weight_spec, weight_spec),
        out_specs=(batch_spec, batch_spec, scale_spec, weight_spec, weight_spec),
        check_vma=False,
    )
```

```python
import functools
import jax
import jax.numpy as jnp
import numpy as np
from jax import lax
from jax.experimental import pallas as pl
from jax.experimental.pallas import tpu as pltpu
from jax.sharding import PartitionSpec as P

MESH_ID = pl.DeviceIdType.MESH
BOTH = (1, -1)
AROUND = (1, -1, 2)
PARTS = (True, False)
ALL, ZERO = ..., 0.0
OTHERS = 7
QUICK, SHORT = 0.2, 0.3
LANE, WIDE, STRIP, HEAD = 128, 256, 512, 64
ROW, BAND, SIDE, TRIO, PAIR = 8, 32, 4, 3, 2


class Links:
    def __init__(self, send_sems, recv_sems):
        self.send_sems, self.recv_sems = send_sems, recv_sems
        self.slots, self.batches, self.sent, self.count = {}, {}, {}, 0

    def _landing(self, key, lane):
        if key not in self.slots:
            self.slots[key] = self.count
            self.count += 1 if lane is None else PAIR
        return self.recv_sems.at[self.slots[key] + (0 if lane is None else lane)]

    def send(self, key, src, dst, device, landing=None, whole=None, batch=None, lane=None):
        leaving = self.batches.setdefault(batch or key, len(self.batches))
        copy = pltpu.make_async_remote_copy(
            src_ref=src, dst_ref=dst, send_sem=self.send_sems.at[leaving], recv_sem=self._landing(landing or key, lane),
            device_id=device, device_id_type=MESH_ID)
        copy.start()
        self.sent[batch or key] = (src if whole is None else whole, leaving)

    def arrive(self, key, landed, lane=None):
        pltpu.make_async_copy(landed, landed, self._landing(key, lane)).wait()

    def drain(self):
        for left, leaving in self.sent.values():
            pltpu.make_async_copy(left, left, self.send_sems.at[leaving]).wait()
        self.sent.clear()


def rem(a, n):
    return a % n if isinstance(a, int) else lax.rem(a, n)


def chip_position():
    f, d = lax.axis_index("fsdp"), lax.axis_index("dp")
    return f // PAIR, rem(d, SIDE), d // SIDE, rem(f, PAIR)


def device_at(x, y, z, core):
    return (z * SIDE + y, x * PAIR + core)


def step(coord, by):
    return rem(coord + SIDE + by, SIDE)


def announce(devices):
    barrier = pltpu.get_barrier_semaphore()
    for device in devices:
        pl.semaphore_signal(barrier, inc=1, device_id=device, device_id_type=MESH_ID)
    pl.semaphore_wait(barrier, len(devices))


def plan(tasks, latency=2.5):
    free, landed, order, now = {}, {}, [], ZERO
    left = list(tasks)
    while left:
        best = None
        for place, (name, rank, start, needs, after, _, _) in enumerate(left):
            if all(n[0] in landed for n in needs) and all(n in landed for n in after):
                ready = max([start, now] + [landed[task][i] for task, i in needs])
                best = min(best or (ready, rank, place), (ready, rank, place))
        now, _, place = best
        name, _, _, _, _, sends, cost = left.pop(place)
        order.append(name)
        now += cost
        landed[name] = []
        for link, time, *more in sends:
            free[link] = max(now, free.get(link, ZERO)) + time
            landed[name].append(free[link] + latency + sum(more))
    return order


def layers_order(rows_i, cols_i, rows_o, cols_o, seq, starts):
    rate = 23300.0
    tasks = []
    for m in range(SIDE):
        is_in = m % PAIR == 0
        edge = cols_i // LANE * SIDE // 9 // PAIR * WIDE
        size = {"y": rows_i // SIDE * edge, "x": rows_i * (cols_i - PAIR * edge)} if is_in else {"y": rows_o // SIDE * cols_o // PAIR}
        size["z"] = size["y"]
        colors = "yzx" if is_in else "yz"
        for color in colors:
            cost = size[color] / rate
            both = [(("x", by), cost) for by in BOTH]
            spread = [((color, by), cost) for by in BOTH] if color != "x" else []
            tasks.append((("reach", m, color), m, starts[m], [], [], both, QUICK))
            for i, by in enumerate(BOTH):
                tasks.append((("relay", m, color, by), m, ZERO, [(("reach", m, color), i)], [], [(("x", by), cost / PAIR)] + spread, QUICK))
            halves = [(("relay", m, color, by), 0) for by in BOTH]
            tasks.append((("far", m, color), m, ZERO, halves, [], spread, QUICK))
            if color == "x":
                continue
            for off, source, first in ((-1, ("relay", m, color, 1), 1), (1, ("relay", m, color, -1), 1), (PAIR, ("far", m, color), 0)):
                for i, by in enumerate(BOTH):
                    tasks.append((("pass", m, color, off, by), m, ZERO, [(source, first + i)], [], [((color, by), cost / PAIR)], QUICK))
                halves = [(("pass", m, color, off, by), 0) for by in BOTH]
                tasks.append((("close", m, color, off), m, ZERO, halves, [], [], QUICK))
        for off in (-1, 1, PAIR):
            last = [("close", m, color, off) for color in "yz"]
            if is_in:
                last.append(("far", m, "x") if off == PAIR else ("relay", m, "x", -off))
            tasks.append((("hand", m, off), m, ZERO, [], last, [("chip", (rows_i * cols_i if is_in else rows_o * cols_o) / 150000.0)], QUICK))
    before = []

    def work(name, cost, mats=()):
        needs = [(("hand", m, off), 0) for m in mats for off in (-1, 1, PAIR)]
        tasks.append((name, 99, ZERO, needs, list(before), [], cost))
        before[:] = [name]

    for l in range(PAIR):
        work(("norm", l), 0.8)
        work(("project", l), 4.0, [PAIR * l])
        work(("attend", l), 4.2)
        work(("mlp", l), 2.2)
        work(("put", l), 1.6, [PAIR * l + 1])
    for l in (1, 0):
        work(("back_out", l), 2.9)
        work(("back_mlp", l), 2.0)
        work(("back_heads", l), 1.0)
        work(("back_quad", l), 6.0)
        work(("back_keys", l), QUICK)
        for i in range(PAIR):
            work(("back_in", l, i), 1.3 + 0.6 * i)
        work(("back_norm", l), 1.0)
    def send(name, rank, start, after, sends):
        tasks.append((name, rank, start, [], [after] if after else [], sends, 0.4))

    def follow(name, rank, needs, sends):
        tasks.append((name, rank, ZERO, needs, [], sends, QUICK))

    def both(axis, size):
        return [((axis, by), size / rate, margin) for by in BOTH]

    model, margin = rows_i * ROW, 2.0
    for l in (1, 0):
        for axis in "yz":
            name = ("send_h", l, axis)
            send(name, 20 - l, 58.0, ("norm", l), both(axis, seq * model))
            for i, by in enumerate(BOTH):
                for index in range(PAIR):
                    follow(("pass_h", l, axis, by, index), 10, [(name, i)], [((axis, by), seq * model / SIDE / rate, margin)])
        name = ("send_m", l)
        send(name, 22 - l, ZERO, ("mlp", l), both("x", seq * rows_o) + both("x", PAIR * seq * rows_o))
        for i, by in enumerate(BOTH):
            for index in range(PAIR):
                follow(("pass_m", l, by, index), 11, [(name, i)], [(("x", by), seq * rows_o / PAIR / rate, margin)])
        if l == 0:
            send(("own_y",), 15, ZERO, ("back_norm", 1), [])
            send(("send_scale", l), 15, ZERO, ("back_norm", l), [])
            continue
        name = ("send_y", l)
        send(name, 12, 42.0, None, both("x", seq * model))
        for i, by in enumerate(BOTH):
            follow(("pass_y", l, by), 12, [(name, i)], [(("x", by), seq * model / PAIR / rate, margin)])
        follow(("far_y", l), 12, [(("pass_y", l, by), 0) for by in BOTH], [])
        for axis in "zy":
            name = ("send_z", l, axis)
            share = seq * (cols_i + LANE) / ROW
            send(name, 13, ZERO, ("back_mlp", l), both(axis, share / PAIR) + both(axis, share))
            if axis == "y":
                name = ("rest_z", l)
                send(name, 13, ZERO, ("back_keys", l), both(axis, share / ROW) + both(axis, share / SIDE))
            for i, by in enumerate(BOTH):
                follow(("pass_z", l, axis, by), 13, [(name, i)], [((axis, by), share / PAIR / rate, margin)])
                follow(("twin_z", l, axis, by), 14, [(name, PAIR + i)], [])
            follow(("far_z", l, axis), 14, [(("pass_z", l, axis, by), 0) for by in BOTH], [])
        send(("send_scale", l), 15, ZERO, ("back_norm", l), [])
    send(("own_z",), 15, ZERO, ("back_keys", 0), [])
    return plan(tasks)


def gather_stages(links, position, shard_i, shard_o, wi, wo, lsem):
    x, y, z, core = position
    twin = device_at(x, y, z, 1 - core)
    rows_i, cols_i = shard_i.shape[1:]
    rows_o, cols_o = shard_o.shape[1:]
    quarter_i, quarter_o = rows_i // SIDE, rows_o // SIDE
    third_i = cols_i // LANE * SIDE // 9 // PAIR * WIDE
    half_o = cols_o // PAIR
    cut_o = quarter_o // 16 * ROW + ROW if quarter_o % 16 else quarter_o // PAIR
    place = {"x": x, "y": y, "z": z}

    spots = {(axis, o): step(place[axis], o) for axis in "xyz" for o in range(SIDE)}

    def spot(axis, o):
        return spots[axis, o % SIDE]

    table = {}
    for axis in "xyz":
        for o in range(1, SIDE):
            moved = {**place, axis: spot(axis, o)}
            table[axis, o] = device_at(moved["x"], moved["y"], moved["z"], core)

    def peer(axis, o):
        return table[axis, o % SIDE]

    mats = []
    for l in range(PAIR):
        mats.append((shard_i.at[l], wi.at[l], rows_i, True))
        mats.append((shard_o.at[l], wo.at[l], rows_o, False))

    def region(is_in, color, q):
        if is_in:
            if color == "x":
                lo, hi = PAIR * third_i, cols_i
                rows = (0, rows_i)
            else:
                lo, hi = (0, third_i) if color == "y" else (third_i, PAIR * third_i)
                rows = (q * quarter_i, quarter_i)
            mid = lo + ((hi - lo) // LANE + 1) // PAIR * LANE
            return (rows, (lo, hi - lo)), (rows, (lo, mid - lo)), (rows, (mid, hi - mid))
        cols = (0, half_o) if color == "y" else (half_o, half_o)
        start = q * quarter_o
        return ((start, quarter_o), cols), ((start, cut_o), cols), ((start + cut_o, quarter_o - cut_o), cols)

    def at(m, xb, area):
        (r, nr), (c, nc) = area
        _, out, size, _ = mats[m]
        return out.at[pl.ds(pl.multiple_of((PAIR * xb + core) * size + r, ROW), nr), pl.ds(c, nc)]

    def block(m, xb, index):
        _, out, size, _ = mats[m]
        return out.at[pl.ds(pl.multiple_of((PAIR * xb + index) * size, BAND), size)]

    def group(m, color):
        _, out, _, is_in = mats[m]
        (_, nr), (c, nc) = region(is_in, color, 0)[0]
        return dict(batch=(m, color), whole=out.at[pl.ds(0, nr * (TRIO if color == "x" else 12)), pl.ds(c, nc)])

    def reach(m, color):
        src, _, _, is_in = mats[m]
        area = region(is_in, color, place[color])[0]
        for by in BOTH:
            links.send((m, "x1", color, by), src.at[pl.ds(pl.multiple_of(area[0][0], ROW), area[0][1]), pl.ds(*area[1])], at(m, x, area), peer("x", by), **group(m, color))

    def launch(m, color, off):
        is_in = mats[m][TRIO]
        moved = at(m, spot("x", off), region(is_in, color, place[color])[0])
        for by in BOTH:
            links.send((m, "p1", color, off, by), moved, moved, peer(color, by), **group(m, color))

    def relay(m, color, by):
        is_in = mats[m][TRIO]
        xb = spot("x", -by)
        areas = region(is_in, color, place[color])
        links.arrive((m, "x1", color, by), at(m, xb, areas[0]))
        part = at(m, xb, areas[1] if by == 1 else areas[PAIR])
        links.send((m, "x2", color), part, part, peer("x", by), **group(m, color))
        if color != "x":
            launch(m, color, -by)

    def far(m, color):
        is_in = mats[m][TRIO]
        links.arrive((m, "x2", color), at(m, spot("x", PAIR), region(is_in, color, place[color])[0]))
        if color != "x":
            launch(m, color, PAIR)

    def pass_on(m, color, off, by):
        is_in = mats[m][TRIO]
        xb = spot("x", off)
        areas = region(is_in, color, spot(color, -by))
        links.arrive((m, "p1", color, off, by), at(m, xb, areas[0]))
        part = at(m, xb, areas[1] if by == 1 else areas[PAIR])
        links.send((m, "p2", color, off), part, part, peer(color, by), **group(m, color))

    def close(m, color, off):
        is_in = mats[m][TRIO]
        links.arrive((m, "p2", color, off), at(m, spot("x", off), region(is_in, color, spot(color, PAIR))[0]))

    def four(m):
        _, out, size, _ = mats[m]
        return out.at[pl.ds(0, SIDE * size)]

    def give(m, src, dst):
        links.send((m, "chip"), src, dst, twin, batch=(m, "chip"), whole=four(m))

    def hand(m, off):
        whole = block(m, spot("x", off), core)
        give(m, whole, whole)

    owns = []

    def begin():
        for m, (src, _, _, _) in enumerate(mats):
            copy = pltpu.make_async_copy(src, block(m, x, core), lsem.at[m])
            copy.start()
            owns.append(copy)
            give(m, src, block(m, x, core))

    def ready(m):
        owns[m].wait()
        links.arrive((m, "chip"), four(m))

    return begin, ready, peer, {"reach": reach, "relay": relay, "far": far, "pass": pass_on, "close": close, "hand": hand}


BF, F32 = jnp.bfloat16, jnp.float32


def product(a, b, contract=((1,), (0,))):
    return lax.dot_general(a, b, (contract, ((), ())), preferred_element_type=F32)


def lanes(start, size):
    return pl.ds(start if isinstance(start, int) else pl.multiple_of(start, LANE), size)


def layers_kernel(order, sc_ref, wi_ref, wo_ref, x_ref, dy_ref, freq_ref,
                  y_ref, gx_ref, hy_a, hy_b, hz_a, hz_b, mx_a, mx_b, yx_b, zy_b, zz_b, z_a, dy_a, sc_out, relay_m, relay_z,
                  wi, wo, z, om, h, hid, qr, kts, vsl, ksl, turned_q, turned_o, scores, dscores, pcat, dscat, cos_ref, sin_ref, turn_ref,
                  dot_heads, qt, dht, dkv, omt, ht, dyt, sc, gains, own_gain, gain_ref, load_sems, own_sems, send_sems, recv_sems,
                  share_send_sems, share_recv_sems):
    seq, dim = x_ref.shape
    ff = (wi.shape[PAIR] - dim - LANE) // PAIR
    position = chip_position()
    x, y, zc, core = position
    twin = device_at(x, y, zc, 1 - core)
    me = PAIR * x + core
    links, shared = Links(send_sems, recv_sems), Links(share_send_sems, share_recv_sems)
    stored = []
    spots, _ = around(position)
    h_out, m_out, y_out, z_out = {"y": (hy_a, hy_b), "z": (hz_a, hz_b)}, (mx_a, mx_b), {1: yx_b}, {(1, "y"): zy_b, (1, "z"): zz_b}
    middle = hid.at[1]
    begin, ready, peer, stages = gather_stages(links, position, wi_ref, wo_ref, wi, wo, load_sems)
    others = [(zc * SIDE + y, rem(me + k, ROW)) for k in range(1, ROW)]

    def spot(axis, o):
        return spots[axis, o % SIDE]

    def device(axis, o, index):
        moved = {"x": x, "y": y, "z": zc, axis: spot(axis, o)}
        return device_at(moved["x"], moved["y"], moved["z"], index)

    own_gain[ALL] = jnp.zeros(own_gain.shape, F32)
    count = sc_ref.shape[1]
    for f in range(ROW):
        @pl.when(me == f)
        def _():
            own_gain[0:PAIR, f * count:(f + 1) * count] = sc_ref[ALL].astype(F32)
    announce(others + [device(axis, o, index) for axis in "yz" for o in AROUND for index in range(PAIR)])
    begin()
    for k, far in enumerate(others):
        links.send(("sc",), own_gain, gains.at[me], far, batch=("sc",), whole=gains.at[pl.ds(0, OTHERS)])

    def keep(src, dst):
        copy = pltpu.make_async_copy(src, dst, own_sems.at[len(stored)])
        copy.start()
        stored.append(copy)

    def tokens(axis, o, index):
        return pl.ds(pl.multiple_of((PAIR * spot(axis, o) + index) * seq, seq), seq)

    def place(axis, o, index):
        return PAIR * spot(axis, o) + index

    def columns(axis, o):
        size = z.shape[PAIR] // ROW
        return lanes(((0 if axis == "y" else SIDE) + spot(axis, o)) * size, size)

    def several(batch, ref, n):
        whole = ref.at[pl.ds(0, n * seq if batch[0][0] in "yz" else n)]
        return dict(batch=batch, whole=whole)

    def send_h(l, axis):
        out = h_out[axis][l].at[place(axis, 0, core)]
        for by in BOTH:
            for index in range(PAIR):
                shared.send(("h", l, axis, by), ht.at[l, :, index], out, device(axis, by, index), lane=core, **several(("h", l, axis), h_out[axis][l], OTHERS))
        shared.send(("h", l, axis), ht.at[l, :, 1 - core], out, twin, **several(("h", l, axis), h_out[axis][l], OTHERS))
        keep(ht.at[l, :, core], out)

    def pass_h(l, axis, by, index):
        out = h_out[axis][l]
        shared.arrive(("h", l, axis, by), out.at[place(axis, -by, index)], index)
        part = out.at[place(axis, -by, index), pl.ds(1 - by, PAIR)]
        shared.send(("h", l, axis), part, part, device(axis, by, core), **several(("h", l, axis), out, OTHERS))

    def arrive_h(l):
        for axis in "yz":
            shared.arrive(("h", l, axis), h_out[axis][l].at[pl.ds(0, TRIO)])

    def row_block(l, o, index, part=None):
        size = omt.shape[1] // ROW
        start = (PAIR * spot("x", o) + index) * size
        if part is not None:
            size = size // PAIR
            start = start + part * size
        return omt.at[l, pl.ds(pl.multiple_of(start, 16), size)]

    def row_half(k):
        size = m_out[0].shape[1] // PAIR
        return pl.ds(k * size, size)

    def send_m(l):
        out = m_out[l].at[place("x", 0, core)]
        for k, by in enumerate(BOTH):
            for index in range(PAIR):
                shared.send(("mr", l, by), row_block(l, PAIR, index, k), relay_m.at[l, k, core], device("x", by, index), lane=core, **several(("m", l), m_out[l], OTHERS))
        for by in BOTH:
            for index in range(PAIR):
                shared.send(("m", l), row_block(l, by, index), out, device("x", by, index), **several(("m", l), m_out[l], OTHERS))
        shared.send(("m", l), row_block(l, 0, 1 - core), out, twin, **several(("m", l), m_out[l], OTHERS))
        keep(row_block(l, 0, core), out)

    def pass_m(l, by, index):
        k = (1 - by) // PAIR
        shared.arrive(("mr", l, by), relay_m.at[l, k, index], index)
        shared.send(("m", l), relay_m.at[l, k, index], m_out[l].at[place("x", -by, index), row_half(k)], device("x", by, core),
                    **several(("m2", l), m_out[l], PAIR))

    def arrive_m(l):
        shared.arrive(("m", l), m_out[l].at[pl.ds(0, OTHERS)])

    def token_half(axis, o, k):
        return pl.ds(pl.multiple_of((PAIR * spot(axis, o) + core) * seq + k * (seq // PAIR), seq // PAIR), seq // PAIR)

    def send_y(l):
        src, out = dy_ref, y_out[l].at[tokens("x", 0, core)]
        for by in BOTH:
            shared.send(("y", l, by), src, out, device("x", by, core), **several(("y", l), y_out[l], OTHERS))
        shared.send(("y", l), src, out, twin, **several(("y", l), y_out[l], OTHERS))
        keep(src, out)

    def pass_y(l, by):
        landed, part = y_out[l].at[tokens("x", -by, core)], y_out[l].at[token_half("x", -by, (1 - by) // PAIR)]
        shared.arrive(("y", l, by), landed)
        shared.send(("y2", l), part, part, device("x", by, core), **several(("y", l), y_out[l], OTHERS))
        shared.send(("y", l), landed, landed, twin, **several(("y", l), y_out[l], OTHERS))

    def far_y(l):
        landed = y_out[l].at[tokens("x", PAIR, core)]
        shared.arrive(("y2", l), landed)
        shared.send(("y", l), landed, landed, twin, **several(("y", l), y_out[l], OTHERS))

    def arrive_y(l):
        shared.arrive(("y", l), y_out[l].at[pl.ds(0, SIDE * seq)])

    def push_z(l, axis, o, ready):
        out = z_out[l, axis].at[tokens(axis, 0, core)]
        batch = several(("z", l, axis), z_out[l, axis], ROW)

        def start():
            if o != PAIR:
                shared.send(("z", l, axis, o), z.at[l, :, columns(axis, o)], out, device(axis, o, core), **batch)
                return
            for k, by in enumerate(BOTH):
                shared.send(("zr", l, axis, by), z.at[l, pl.ds(k * (seq // PAIR), seq // PAIR), columns(axis, PAIR)], relay_z.at[l, "yz".index(axis), k],
                            device(axis, by, core), **batch)

        if ready is None:
            start()
        else:
            pl.when(ready)(start)

    def own_part(l, axis):
        out, mine = z_out[l, axis].at[tokens(axis, 0, core)], z.at[l, :, columns(axis, 0)]
        shared.send(("z", l, axis), mine, out, twin, **several(("z", l, axis), z_out[l, axis], ROW))
        keep(mine, out)

    def send_z(l, axis):
        for o in (PAIR, 1, -1):
            push_z(l, axis, o, spot(axis, o) != 0 if axis == "y" else None)
        if axis == "z":
            own_part(l, axis)

    def rest_z(l):
        for o in (PAIR, 1, -1):
            push_z(l, "y", o, spot("y", o) == 0)
        own_part(l, "y")

    def pass_z(l, axis, by):
        k = (1 - by) // PAIR
        half = relay_z.at[l, "yz".index(axis), k]
        shared.arrive(("zr", l, axis, by), half)
        shared.send(("z2", l, axis), half, z_out[l, axis].at[token_half(axis, -by, k)], device(axis, by, core), **several(("z", l, axis), z_out[l, axis], ROW))

    def twin_z(l, axis, by):
        landed = z_out[l, axis].at[tokens(axis, -by, core)]
        shared.arrive(("z", l, axis, by), landed)
        shared.send(("z", l, axis), landed, landed, twin, **several(("z", l, axis), z_out[l, axis], ROW))

    def far_z(l, axis):
        landed = z_out[l, axis].at[tokens(axis, PAIR, core)]
        shared.arrive(("z2", l, axis), landed)
        shared.send(("z", l, axis), landed, landed, twin, **several(("z", l, axis), z_out[l, axis], ROW))

    def arrive_z(l, axis):
        shared.arrive(("z", l, axis), z_out[l, axis].at[pl.ds(0, SIDE * seq)])

    def send_scale(l):
        for far in others:
            shared.send(("scale", l), sc.at[l], sc_out.at[l, me], far, batch=("scale", l), whole=sc_out.at[l, pl.ds(0, OTHERS)])
        keep(sc.at[l], sc_out.at[l, me])

    def arrive_scale(l):
        shared.arrive(("scale", l), sc_out.at[l, pl.ds(0, OTHERS)])

    gains[me] = own_gain[ALL]
    z[:, :, wi.shape[PAIR]:] = jnp.zeros((PAIR, seq, z.shape[PAIR] - wi.shape[PAIR]), BF)
    entry = (x_ref, hid.at[0])
    angle = lax.broadcasted_iota(jnp.int32, (seq, LANE), 0).astype(F32) * freq_ref[0:1]
    for half in range(PAIR):
        cos_ref[:, LANE * half:LANE * (half + 1)] = jnp.cos(angle)
        sin_ref[:, LANE * half:LANE * (half + 1)] = jnp.sin(angle)
    lane = lax.broadcasted_iota(jnp.int32, turn_ref.shape, 1)
    down = lax.broadcasted_iota(jnp.int32, turn_ref.shape, 0) - lane
    low = rem(lane, HEAD) < BAND
    turn_ref[ALL] = jnp.where(low & (down == BAND), -1.0, jnp.where(jnp.logical_not(low) & (down == -BAND), 1.0, ZERO)).astype(BF)
    kts[ALL] = jnp.zeros(kts.shape, BF)
    pcat[ALL] = jnp.zeros(pcat.shape, BF)
    dscat[ALL] = jnp.zeros(dscat.shape, BF)

    def normalise(l, src):
        @pl.loop(0, seq // BAND, unroll=SIDE)
        def _(r):
            rows = pl.ds(pl.multiple_of(r * BAND, BAND), BAND)
            v = src[rows].astype(F32)
            v = v - jnp.mean(v, axis=-1, keepdims=True)
            var = jnp.mean(v * v, axis=-1, keepdims=True)
            h[l, rows] = (v * lax.rsqrt(var + 1e-6) * gain_ref[l:l + 1]).astype(BF)

    def project(l):
        strip = wi.shape[PAIR] // 5

        @pl.loop(0, 5)
        def _(i):
            at = lanes(i * strip, strip)
            z[l, :, at] = product(h[l], wi[l, :, at]).astype(BF)

    def heads(l):
        cos, sin = cos_ref[ALL], sin_ref[ALL]
        for g in range(dim // WIDE):
            q = z[l, :, g * WIDE:(g + 1) * WIDE]
            qr[l, :, g * WIDE:(g + 1) * WIDE] = ((q.astype(F32) * cos + product(q, turn_ref[ALL]) * sin) * 0.125).astype(BF)
        kv = z[l, :, dim:dim + LANE]
        turned = kv.astype(F32) * cos[:, :LANE] + product(kv, turn_ref[:LANE, :LANE]) * sin[:, :LANE]
        first = lax.broadcasted_iota(jnp.int32, turned.shape, 1) < HEAD
        key_lo = jnp.where(first, turned, ZERO)
        val_hi = jnp.where(first, ZERO, kv.astype(F32))
        return key_lo, pltpu.roll(key_lo, HEAD, 1), pltpu.roll(val_hi, HEAD, 1), val_hi

    def slot_rows(ref, lo, hi):
        zero = jnp.zeros((seq, LANE), BF)
        lo, hi = lo.astype(BF), hi.astype(BF)
        for i, (left, right) in enumerate(((lo, zero), (hi, zero), (zero, lo), (zero, hi))):
            ref[i * seq:(i + 1) * seq, :LANE] = left
            ref[i * seq:(i + 1) * seq, LANE:] = right

    def slot_cols(ref, lo):
        flat = lo.T[:HEAD].astype(BF)
        for i in range(SIDE):
            ref[HEAD * i:HEAD * (i + 1), i * seq:(i + 1) * seq] = flat

    def chances(i, half):
        at = slice(LANE * half, LANE * (half + 1))
        blocks = [pl.ds(pl.multiple_of(i * seq + LANE * k, LANE), LANE) for k in range(half + 1)]
        s = [scores[keys, at] for keys in blocks]
        lower = lax.broadcasted_iota(jnp.int32, s[-1].shape, 1) >= lax.broadcasted_iota(jnp.int32, s[-1].shape, 0)
        s[-1] = jnp.where(lower, s[-1], -1e30)
        top = functools.reduce(jnp.maximum, [jnp.max(v, axis=0, keepdims=True) for v in s])
        e = [jnp.exp(v - top) for v in s]
        scale = 1.0 / sum(jnp.sum(v, axis=0, keepdims=True) for v in e)
        return at, [(keys, v * scale) for keys, v in zip(blocks, e)]

    def attend(l):
        key_lo, key_hi, val_lo, _ = heads(l)
        slot_rows(ksl, key_lo, key_hi)
        slot_cols(kts, val_lo)
        flip(lambda at: qr[l, :, lanes(at, WIDE)], qt, dim)

        @pl.loop(0, dim // WIDE)
        def _(g):
            rows = pl.ds(pl.multiple_of(g * WIDE, WIDE), WIDE)
            scores[ALL] = product(ksl[ALL], qt[rows])

            @pl.loop(0, SIDE)
            def _(i):
                for half in range(PAIR):
                    at, blocks = chances(i, half)
                    for keys, p in blocks:
                        pcat[keys, at] = p.astype(BF)
            flat = product(kts[ALL], pcat[ALL]).astype(BF)
            omt[l, rows] = flat
            om[:, lanes(g * WIDE, WIDE)] = flat.T

    def mlp(l):
        @pl.loop(0, seq // BAND)
        def _(r):
            rows = pl.ds(pl.multiple_of(r * BAND, BAND), BAND)

            @pl.loop(0, ff // STRIP)
            def _(i):
                gate = z[l, rows, lanes(dim + LANE + i * STRIP, STRIP)].astype(F32)
                up = z[l, rows, lanes(dim + LANE + ff + i * STRIP, STRIP)].astype(F32)
                om[rows, lanes(dim + i * STRIP, STRIP)] = (gate * jax.nn.sigmoid(gate) * up).astype(BF)

    def put_out(l, dst):
        for n in range(dim // WIDE):
            cols = slice(n * WIDE, (n + 1) * WIDE)
            total = product(om[ALL], wo[l, :, cols])
            dst[:, cols] = (entry[l][:, cols].astype(F32) + total).astype(BF)

    def flip(src, dst, width, first=0):
        @pl.loop(first // WIDE, width // WIDE)
        def _(i):
            dst[pl.ds(pl.multiple_of(i * WIDE, WIDE), WIDE)] = src(i * WIDE).T

    upstream = (middle, dy_ref)

    def back_out(l):
        dy = upstream[l]
        flip(lambda at: dy[:, lanes(at, WIDE)], dyt, dim)

        @pl.loop(0, wo.shape[1] // dim)
        def _(n):
            rows = pl.ds(pl.multiple_of(n * dim, dim), dim)
            part = product(wo[l, rows], dyt[ALL]).astype(BF)
            om[:, lanes(n * dim, dim)] = part.T

            @pl.when(n == 0)
            def _():
                dot_heads[ALL] = part

    def back_mlp(l):
        @pl.loop(0, seq // BAND)
        def _(r):
            rows = pl.ds(pl.multiple_of(r * BAND, BAND), BAND)

            @pl.loop(0, ff // STRIP)
            def _(i):
                gate_at, up_at = lanes(dim + LANE + i * STRIP, STRIP), lanes(dim + LANE + ff + i * STRIP, STRIP)
                gate, up = z[l, rows, gate_at].astype(F32), z[l, rows, up_at].astype(F32)
                d = om[rows, lanes(dim + i * STRIP, STRIP)].astype(F32)
                sig = jax.nn.sigmoid(gate)
                du = d * up
                z[l, rows, gate_at] = (du * sig + du * gate * (sig * (1.0 - sig))).astype(BF)
                z[l, rows, up_at] = (d * (gate * sig)).astype(BF)

    def back_heads(l):
        key_lo, key_hi, val_lo, val_hi = heads(l)
        slot_rows(ksl, key_lo, key_hi)
        slot_rows(vsl, val_lo, val_hi)
        slot_cols(kts, key_lo)
        dkv[ALL] = jnp.zeros(dkv.shape, F32)
        flip(lambda at: qr[l, :, lanes(at, WIDE)], qt, dim)
        for at in range(0, dim, LANE):
            pair = slice(at, at + LANE)
            turned_q[:, pair] = pltpu.roll(qr[l, :, pair].astype(F32), HEAD, 1).astype(BF)
            turned_o[:, pair] = pltpu.roll(om[:, pair].astype(F32), HEAD, 1).astype(BF)

    def back_quad(l):
        @pl.loop(0, dim // WIDE)
        def _(g):
            quad(l, g)

    def quad(l, g):
        cols = pl.ds(pl.multiple_of(g * WIDE, WIDE), WIDE)
        scores[ALL] = product(ksl[ALL], qt[cols])
        dscores[ALL] = product(vsl[ALL], dot_heads[cols])

        @pl.loop(0, SIDE)
        def _(i):
            for half in range(PAIR):
                at, blocks = chances(i, half)
                given = [p * dscores[keys, at].astype(BF).astype(F32) for keys, p in blocks]
                total = sum(jnp.sum(v, axis=0, keepdims=True) for v in given)
                for (keys, p), v in zip(blocks, given):
                    pcat[keys, at] = p.astype(BF)
                    dscat[keys, at] = (v - p * total).astype(BF)
        dq = product(kts[ALL], dscat[ALL]).astype(BF).T
        back = dq.astype(F32) * cos_ref[ALL] - product(dq, turn_ref[ALL]) * sin_ref[ALL]
        z[l, :, cols] = (back * 0.125).astype(BF)
        for i in range(SIDE):
            keys, pair = slice(i * seq, (i + 1) * seq), lanes(g * WIDE + i // PAIR * LANE, LANE)
            even = i % PAIR == 0
            dkv[0] += product(dscat[keys], qr[l, :, pair] if even else turned_q[:, pair])
            dkv[1] += product(pcat[keys], turned_o[:, pair] if even else om[:, pair])

    def back_keys(l):
        dk = dkv[0].astype(BF)
        turned = dk.astype(F32) * cos_ref[:, :LANE] - product(dk, turn_ref[:LANE, :LANE]) * sin_ref[:, :LANE]
        first = lax.broadcasted_iota(jnp.int32, turned.shape, 1) < HEAD
        z[l, :, dim:dim + LANE] = jnp.where(first, turned, dkv[1]).astype(BF)

    def back_in(l, half):
        width = wi.shape[PAIR] // 5
        at = slice(PAIR * half * width, (PAIR + TRIO * half) * width)
        part = product(wi[l, :, at], z[l, :, at], ((1,), (1,)))
        dht[ALL] = dht[ALL] + part if half else part

    def back_norm(l):
        dy, dst = upstream[l], (gx_ref, middle)[l]
        for i in range(dim // WIDE):
            cols = slice(i * WIDE, (i + 1) * WIDE)
            h[l, :, cols] = dht[cols].T.astype(BF)
        sc[l] = jnp.zeros(sc.shape[1:], F32)

        @pl.loop(0, seq // BAND, unroll=SIDE)
        def _(r):
            rows = pl.ds(pl.multiple_of(r * BAND, BAND), BAND)
            v = entry[l][rows].astype(F32)
            v = v - jnp.mean(v, axis=-1, keepdims=True)
            scale = lax.rsqrt(jnp.mean(v * v, axis=-1, keepdims=True) + 1e-6)
            hat = v * scale
            d = h[l, rows].astype(F32)
            each = (d * hat).reshape(SIDE, ROW, dim)
            sc[l] += (each[0] + each[1]) + (each[PAIR] + each[TRIO])
            d = d * gain_ref[l:l + 1]
            d = scale * (d - jnp.mean(d, axis=-1, keepdims=True) - hat * jnp.mean(d * hat, axis=-1, keepdims=True))
            dst[rows] = (dy[rows].astype(F32) + d.astype(BF).astype(F32)).astype(BF)

    def do_norm(l):
        if l == 0:
            links.arrive(("sc",), gains.at[pl.ds(0, OTHERS)])
            gain_ref[ALL] = jnp.sum(gains[ALL], axis=0)
        normalise(l, entry[l])
        for i in range(dim // WIDE):
            flat = h[l, :, i * WIDE:(i + 1) * WIDE].T
            size = ht.shape[TRIO]
            for b in range(ROW):
                lo, hi = max(b * size, i * WIDE), min((b + 1) * size, (i + 1) * WIDE)
                if lo < hi:
                    ht[l, b // PAIR, b % PAIR, lo - b * size:hi - b * size] = flat[lo - i * WIDE:hi - i * WIDE]

    def do_project(l):
        ready(PAIR * l)
        project(l)

    def do_mlp(l):
        mlp(l)
        flip(lambda at: om[:, lanes(at, WIDE)], omt.at[l], om.shape[1], dim)

    def do_put(l):
        ready(PAIR * l + 1)
        put_out(l, hid.at[0] if l == 0 else y_ref)

    stages.update(
        norm=do_norm, project=do_project, attend=attend, mlp=do_mlp, put=do_put, back_out=back_out, back_mlp=back_mlp, back_heads=back_heads,
        back_quad=back_quad, back_keys=back_keys, back_in=back_in, back_norm=back_norm, send_h=send_h, pass_h=pass_h, send_m=send_m,
        pass_m=pass_m, send_y=send_y, pass_y=pass_y, far_y=far_y, send_z=send_z, rest_z=rest_z, pass_z=pass_z, twin_z=twin_z, far_z=far_z,
        send_scale=send_scale, own_z=lambda: keep(z.at[0], z_a), own_y=lambda: keep(middle, dy_a))
    for kind, *task in order:
        stages[kind](*task)
    for l in range(PAIR):
        arrive_h(l)
        arrive_m(l)
        arrive_scale(l)
    arrive_y(1)
    for l, axis in z_out:
        arrive_z(l, axis)
    for copy in stored:
        copy.wait()
    shared.drain()
    links.drain()


def run_layers(x, dy, scale, w_in, w_out, freq, starts=(ZERO, 10.0, 20.0, 30.0)):
    seq, dim = x.shape
    proj, cat = w_in.shape[PAIR], ROW * w_out.shape[1]
    wide = proj + LANE
    hbm, vmem = pl.BlockSpec(memory_space=pltpu.HBM), pl.BlockSpec(memory_space=pltpu.VMEM)
    out = lambda *shape, dtype=BF: jax.ShapeDtypeStruct(shape, dtype)
    buffer = lambda *shape, dtype=BF: pltpu.VMEM(shape, dtype)
    sem = pltpu.SemaphoreType.DMA
    line = ROW * seq
    return pl.pallas_call(
        functools.partial(layers_kernel, layers_order(*w_in.shape[1:], *w_out.shape[1:], seq, starts)),
        out_shape=(out(seq, dim), out(seq, dim), *[out(ROW, SIDE, dim // ROW, seq)] * SIDE, *[out(ROW, cat // ROW, seq)] * PAIR, out(line, dim),
                   *[out(line, wide // ROW)] * PAIR, out(seq, wide), out(seq, dim), out(PAIR, ROW, ROW, dim, dtype=F32),
                   out(PAIR, PAIR, PAIR, cat // 16, seq), out(PAIR, PAIR, PAIR, seq // PAIR, wide // ROW)),
        in_specs=[vmem, hbm, hbm] + [vmem] * TRIO,
        out_specs=[vmem] * PAIR + [hbm] * 14,
        scratch_shapes=[
            buffer(PAIR, dim, proj), buffer(PAIR, cat, dim), buffer(PAIR, seq, wide), buffer(seq, cat), buffer(PAIR, seq, dim),
            buffer(PAIR, seq, dim), buffer(PAIR, seq, dim),
            buffer(WIDE, SIDE * seq), buffer(SIDE * seq, WIDE), buffer(SIDE * seq, WIDE), buffer(seq, dim), buffer(seq, dim),
            buffer(SIDE * seq, seq, dtype=F32), buffer(SIDE * seq, seq, dtype=F32), buffer(SIDE * seq, seq), buffer(SIDE * seq, seq),
            buffer(seq, WIDE, dtype=F32), buffer(seq, WIDE, dtype=F32), buffer(WIDE, WIDE),
            buffer(dim, seq), buffer(dim, seq), buffer(dim, seq, dtype=F32), buffer(PAIR, seq, LANE, dtype=F32),
            buffer(PAIR, cat, seq), buffer(PAIR, SIDE, PAIR, dim // ROW, seq), buffer(dim, seq), buffer(PAIR, ROW, dim, dtype=F32),
            buffer(ROW, ROW, dim, dtype=F32), buffer(ROW, dim, dtype=F32), buffer(ROW, dim, dtype=F32),
            sem((SIDE,)), sem((13,)), sem((15,)), sem((107,)), sem((13,)), sem((HEAD,)),
        ],
        compiler_params=pltpu.CompilerParams(collective_id=PAIR, has_side_effects=True, vmem_limit_bytes=67043328),
        name="run_layers",
    )(scale, w_in, w_out, x, dy, freq)


PARTS = (("i", "x", "z", "y", 0, STRIP), ("i", "x", "z", "y", STRIP, 384), ("i", "x", "y", "z", 0, STRIP), ("i", "x", "y", "z", STRIP, 384),
         ("o", "y", "z", "y", 0, 384), ("o", "z", "y", "z", 384, 384))


def reduce_order(rows, rows_b, starts):
    rate = 11650.0
    tasks = []
    sizes = {"y": WIDE * 896 / (PAIR * rate), "z": WIDE * 896 / (PAIR * rate), "x": WIDE * 768 / (PAIR * rate)}
    for axis in "yzx":
        size = sizes[axis]
        tasks.append((("swap", axis), (0, 0), starts[PAIR] if axis == "x" else starts[TRIO], [], [],
                      [((axis, by), size * n) for by, n in ((-1, 0.5), (1, 1), (-1, 1), (1, 1))], SHORT))
        tasks.append((("relay", axis), (0, 0), ZERO, [(("swap", axis), 0)], [], [((axis, -1), size / PAIR)], SHORT))
        for o, needs in ((1, [(("swap", axis), 1)]), (-1, [(("swap", axis), PAIR)]), (PAIR, [(("swap", axis), TRIO), (("relay", axis), 0)])):
            tasks.append((("near", axis, o), (0, PAIR), ZERO, needs, [], [("chip", 1.6)], QUICK))
    tasks.append((("fetch", 0), (5, 0), ZERO, [], [("make", 1, len(PARTS) - 1)], [], QUICK))
    for l in (1, 0):
        late = 1 - l
        for c, (kind, first, then, last, at, width) in enumerate(PARTS):
            needs, cost = [], 1.6 * width / STRIP
            if l == 0:
                needs = [(("near", last if kind == "i" else "x", o), 0) for o in AROUND]
            tasks.append((("make", l, c), (9 * late, c), starts[late], needs, [] if l else [("fetch", 0)], [], cost))
            full = SIDE * SIDE * (rows if kind == "i" else rows_b) * width / rate
            sends = [[((first, by), full / ROW) for by in BOTH], [((first, by), full / SIDE) for by in BOTH],
                     [((then, o), full / 16) for o in (1, -1, 1)], []]
            piece = full / 16
            sends += [[((then, by), piece) for by in BOTH], [((then, 1 - PAIR * (c % PAIR)), piece)], [((last, by), SIDE * piece) for by in BOTH],
                      [((last, by), PAIR * piece) for by in BOTH], []]
            for s in range(9):
                task = ("sum", l, c, s)
                needs = [(("sum", l, c, s - 1), k) for k in range(len(sends[s - 1]))] if s else []
                tasks.append((task, (late, -s), ZERO, needs, [("make", l, c)] if s == 0 else [("sum", l, c, s - 1)], sends[s], SHORT))
    return plan(tasks)


def reduce_kernel(order, *refs):
    hy, hz, mx = refs[0:PAIR], refs[PAIR:SIDE], refs[SIDE:6]
    yx1, zy1, zz1, z0, y0, sc = refs[6:12]
    oa, ob = refs[12:14]
    n = len(PARTS)
    total, half, full, small, front = (refs[14 + k * n:14 + (k + 1) * n] for k in range(5))
    (hbuf, zbuf, mbuf, ybuf, scbuf, rz, ry, ssem, rsem, isem, osem) = refs[14 + 5 * n:]
    position = chip_position()
    x, y, zc, core = position
    place = {"x": x, "y": y, "z": zc}
    twin = device_at(x, y, zc, 1 - core)
    spots, peers = around(position)

    def spot(axis, o):
        return spots[axis, o % SIDE]

    def peer(axis, o):
        return peers[axis, o % SIDE]

    seq, wide = z0.shape
    own = wide // ROW
    loads, moving = {}, []

    def load(key, src, dst):
        copy = pltpu.make_async_copy(src, dst, isem.at[len(moving)])
        moving.append(key)
        copy.start()
        loads[key] = copy

    def fetch(l):
        if l:
            load(("z", 1, "y"), zy1, zbuf.at[1, 0])
        load(("h", l, "y"), hy[l], hbuf.at[l, 0])
        if l:
            load(("z", 1, "z"), zz1, zbuf.at[1, 1])
        load(("h", l, "z"), hz[l], hbuf.at[l, 1])
        load(("m", l), mx[l], mbuf.at[l])
        if l:
            load(("y", 1), yx1, ybuf.at[1])
        load(("s", l), sc.at[l], scbuf.at[l])

    fetch(1)
    done = set()

    def loaded(*keys):
        for key in keys:
            if key not in done:
                loads[key].wait()
                done.add(key)

    announce([peer(axis, o) for axis in "xyz" for o in AROUND] + [twin])
    links = Links(ssem, rsem)

    def columns(axis, o):
        return lanes(((0 if axis == "y" else SIDE) + spot(axis, o)) * own, own)

    def tokens(axis, o, index):
        return pl.ds(pl.multiple_of((PAIR * spot(axis, o) + index) * seq, seq), seq)

    def target(axis):
        return ybuf.at[0] if axis == "x" else zbuf.at[0, "yz".index(axis)]

    def leaving(axis):
        return dict(batch=("swap", axis), whole=target(axis).at[pl.ds(0, OTHERS * seq + seq // PAIR)])

    def half_at(axis, o, k):
        start = (PAIR * spot(axis, o) + core) * seq + k * (seq // PAIR)
        return target(axis).at[pl.ds(pl.multiple_of(start, seq // PAIR), seq // PAIR)]

    def relay_of(axis):
        return ry if axis == "x" else rz.at["yz".index(axis)]

    def swap(axis):
        def part(o, rows=slice(None)):
            return y0.at[rows] if axis == "x" else z0.at[rows, columns(axis, o)]

        mine = target(axis).at[tokens(axis, 0, core)]
        links.send(("relay", axis), part(PAIR, pl.ds(seq // PAIR, seq // PAIR)), relay_of(axis), peer(axis, -1), **leaving(axis))
        for by in BOTH:
            links.send(("swap", axis, by), part(by), mine, peer(axis, by), **leaving(axis))
        links.send(("swap", axis, PAIR), part(PAIR, pl.ds(0, seq // PAIR)), half_at(axis, 0, 0), peer(axis, PAIR), **leaving(axis))
        links.send(("near", axis), part(0), mine, twin, **leaving(axis))
        load(("own", axis), part(0), mine)

    def relay(axis):
        links.arrive(("relay", axis), relay_of(axis))
        links.send(("relayed", axis), relay_of(axis), half_at(axis, 1, 1), peer(axis, -1), **leaving(axis))

    def near(axis, o):
        landed = target(axis).at[tokens(axis, -o, core)]
        if o == PAIR:
            links.arrive(("swap", axis, PAIR), half_at(axis, PAIR, 0))
            links.arrive(("relayed", axis), half_at(axis, PAIR, 1))
        else:
            links.arrive(("swap", axis, o), landed)
        links.send(("near", axis), landed, landed, twin, **leaving(axis))

    def joined(axis):
        if axis not in done:
            done.add(axis)
            loaded(("own", axis))
            links.arrive(("near", axis), target(axis).at[pl.ds(0, SIDE * seq)])

    def joined_lanes(ref, l, i):
        return jnp.concatenate([ref[l, i, k].reshape(-1, ref.shape[-1]) for k in range(ROW)], axis=1)

    def make(l, c):
        kind, first, then, last, at, width = PARTS[c]
        if kind == "i":
            i = "yz".index(last)
            loaded(("h", l, last))
            if l:
                loaded(("z", l, last))
            else:
                joined(last)
            size = total[c].shape[TRIO]
            for lo in range(0, width, WIDE):
                hi = min(width, lo + WIDE)
                part = product(joined_lanes(hbuf, l, i), zbuf[l, i, :, at + lo:at + hi])
                for r in range(16):
                    total[c][l, r // SIDE, r % SIDE, :, lo:hi] = part[r * size:(r + 1) * size]
            return
        loaded(("m", l), ("s", l))
        if l:
            loaded(("y", l))
        else:
            joined("x")
        part = product(jnp.concatenate([mbuf[l, k] for k in range(ROW)], axis=1), ybuf[l, :, at:at + width])
        size = total[c].shape[TRIO]

        def put(r, value):
            total[c][(l, r // SIDE, r % SIDE) if first == "y" else (l, r % SIDE, r // SIDE)] = value

        for r in range(part.shape[0] // size):
            put(r, part[r * size:(r + 1) * size])
        gain = jnp.sum(jnp.sum(scbuf[l, :, :, at:at + width], axis=0), axis=0, keepdims=True)
        row = lax.broadcasted_iota(jnp.int32, (size, width), 0)
        put(15, jnp.where(row == 0, gain, ZERO))

    def area(l, c, o, whole):
        kind, first, then, last, at, width = PARTS[c]
        inner = (spot(then, whole) if isinstance(whole, int) else whole)
        outer = spot(last, o)
        if kind == "i":
            cols = lanes(((0 if last == "y" else SIDE) + outer) * own + at, width)
            return oa.at[l, inner, :, cols]
        cols = pl.ds(at, width)
        return ob.at[l, outer, inner, :, cols] if last == "y" else ob.at[l, inner, outer, :, cols]

    def add(l, c, s):
        kind, first, then, last, at, width = PARTS[c]
        t = total[c].at[l]
        way = 1 - PAIR * (c % PAIR)
        sums = dict(batch=(l, c, 0), whole=t)
        wide_ones = dict(batch=(l, c, 1), whole=t.at[pl.ds(0, TRIO)])
        narrow = dict(batch=(l, c, PAIR), whole=t.at[0, pl.ds(0, PAIR)])
        if s == 0:
            far = t.at[spot(first, PAIR)]
            for k, by in enumerate(BOTH):
                links.send((l, c, "half"), far.at[pl.ds(PAIR * k, PAIR)], half[c].at[l, k], peer(first, by), **sums)
        elif s == 1:
            links.arrive((l, c, "half"), half[c].at[l])
            for k, by in enumerate(BOTH):
                mine = t.at[spot(first, by)]
                add_into(mine.at[pl.ds(PAIR * k, PAIR)], half[c].at[l, k])
                links.send((l, c, "full"), mine, full[c].at[l, k], peer(first, by), **sums)
        elif s == PAIR:
            mine = t.at[spot(first, 0)]
            links.arrive((l, c, "full"), full[c].at[l])
            for k in range(PAIR):
                add_into(mine, full[c].at[l, k])
            for k, o in enumerate(AROUND):
                links.send((l, c, "small"), mine.at[spot(then, o)], small[c].at[l, k], peer(then, o), **wide_ones)
        elif s == TRIO:
            links.arrive((l, c, "small"), small[c].at[l])
            mine = t.at[spot(first, 0), spot(then, 0)]
            front[c][l] = (mine[ALL] + small[c][l, 0]) + (small[c][l, 1] + small[c][l, PAIR])
        elif s == SIDE:
            src, dst = front[c].at[l], area(l, c, 0, 0)
            for by in BOTH:
                links.send((l, c, "a1"), src, dst, peer(then, by), **narrow)
            copy = pltpu.make_async_copy(src, dst, osem.at[l, c])
            copy.start()
            loads["front", l, c] = copy
        elif s == 5:
            links.arrive((l, c, "a1"), t.at[0, pl.ds(0, PAIR)])
            landed = area(l, c, 0, -way)
            links.send((l, c, "b1"), landed, landed, peer(then, way), **wide_ones)
        elif s == 6:
            loaded(("front", l, c))
            links.arrive((l, c, "b1"), area(l, c, 0, PAIR))
            line = area(l, c, 0, slice(None))
            for by in BOTH:
                links.send((l, c, "a2"), line, line, peer(last, by), **wide_ones)
        elif s == OTHERS:
            links.arrive((l, c, "a2"), t.at[pl.ds(0, PAIR)])
            for k, by in enumerate(BOTH):
                part = area(l, c, -by, pl.ds(PAIR * k, PAIR))
                links.send((l, c, "a3"), part, part, peer(last, by), **sums)
        else:
            links.arrive((l, c, "a3"), area(l, c, PAIR, slice(None)))

    stages = {"swap": swap, "relay": relay, "near": near, "fetch": fetch, "make": make, "sum": add}
    for kind, *task in order:
        stages[kind](*task)
    links.drain()


def add_into(dst, src):
    @pl.loop(0, dst.shape[0])
    def _(i):
        if len(dst.shape) == SIDE:
            for j in range(dst.shape[1]):
                dst[i, j] += src[i, j]
        else:
            dst[i] += src[i]


def around(position):
    place, core = dict(zip("xyz", position)), position[TRIO]
    spots = {(axis, o): step(place[axis], o) for axis in "xyz" for o in range(SIDE)}
    peers = {}
    for axis in "xyz":
        for o in range(1, SIDE):
            moved = {**place, axis: spots[axis, o]}
            peers[axis, o] = device_at(moved["x"], moved["y"], moved["z"], core)
    return spots, peers


def reduce_gradients(operands, starts=(ZERO, ZERO, 20.0, 3.0)):
    hbm = pl.BlockSpec(memory_space=pltpu.HBM)
    h_rows, m_rows, y_cols, z_cols, z_own, y_own, scale_parts = operands
    part, part_b = h_rows[0].shape[PAIR] // SIDE, (m_rows[0].shape[1] + BAND) // 16
    (line, dim), wide = y_cols.shape, z_own.shape[1]
    out = lambda *shape: jax.ShapeDtypeStruct(shape, F32)
    sem = pltpu.SemaphoreType.DMA

    def buffers(*lead):
        return [pltpu.VMEM((PAIR, *lead, part if e[0] == "i" else part_b, e[5]), F32) for e in PARTS]

    return pl.pallas_call(
        functools.partial(reduce_kernel, reduce_order(part, part_b, starts)),
        out_shape=(out(PAIR, SIDE, part, wide), out(PAIR, SIDE, SIDE, part_b, dim)),
        in_specs=[hbm] * 12,
        out_specs=[hbm] * PAIR,
        scratch_shapes=[
            *buffers(SIDE, SIDE), *buffers(PAIR, PAIR), *buffers(PAIR, SIDE), *buffers(TRIO), *buffers(),
            pltpu.VMEM((PAIR, PAIR, *h_rows[0].shape), BF), pltpu.VMEM((PAIR, PAIR, line, wide // ROW), BF), pltpu.VMEM((PAIR, *m_rows[0].shape), BF),
            pltpu.VMEM((PAIR, line, dim), BF), pltpu.VMEM(scale_parts.shape, F32),
            pltpu.VMEM((PAIR, z_own.shape[0] // PAIR, wide // ROW), BF), pltpu.VMEM((y_own.shape[0] // PAIR, dim), BF),
            sem((39,)), sem((102,)), sem((14,)), sem((PAIR, len(PARTS))),
        ],
        compiler_params=pltpu.CompilerParams(collective_id=1, has_side_effects=True, vmem_limit_bytes=67043328),
        name="reduce_gradients",
    )(*h_rows, *m_rows, y_cols, *z_cols, z_own, y_own, scale_parts)


def solution(mesh):
    fsdp_size = mesh.shape["fsdp"]
    batch_spec = P(("dp", "fsdp"), None, None)
    scale_spec = P(None, "fsdp")
    weight_spec = P(None, "fsdp", None)

    def device_step(x_in, grad_y, norm_scale, w_in, w_out):
        n_layers = w_in.shape[0]
        seq_len, model_dim = x_in.shape[1:]
        proj_dim = w_in.shape[PAIR]
        ff_dim = w_out.shape[1] * fsdp_size - model_dim
        head_dim = (proj_dim - model_dim - PAIR * ff_dim) // PAIR
        rows, rows_out = norm_scale.shape[1], w_out.shape[1]
        half_dim = head_dim // PAIR
        freq = 10000.0 ** (-np.arange(half_dim, dtype=np.float32) * 2.0 / head_dim)
        freq = jnp.asarray(np.tile(freq.astype(np.float32), (ROW, LANE // half_dim)))
        hidden, grad_hidden, *rest = run_layers(x_in[0], grad_y[0], norm_scale, w_in, w_out, freq)
        in_sums, out_sums = reduce_gradients((rest[0:SIDE], rest[SIDE:6], rest[6], rest[OTHERS:9], rest[9], rest[10], rest[11]))
        in_grads = in_sums.reshape(n_layers, rows, -1)[:, :, :proj_dim]
        out_rows = out_sums.reshape(n_layers, -1, model_dim)
        scale_grads = lax.dynamic_slice(out_rows[:, rows_out], (0, lax.axis_index("fsdp") * rows), (n_layers, rows))
        out_grads = out_rows[:, :rows_out]
        return hidden[None], grad_hidden[None], scale_grads, in_grads, out_grads

    return jax.shard_map(
        device_step,
        mesh=mesh,
        in_specs=(batch_spec, batch_spec, scale_spec, weight_spec, weight_spec),
        out_specs=(batch_spec, batch_spec, scale_spec, weight_spec, weight_spec),
        check_vma=False,
    )
```

```python
import functools
import jax
import jax.numpy as jnp
import numpy as np
from jax import lax
from jax.experimental import pallas as pl
from jax.experimental.pallas import tpu as pltpu
from jax.sharding import PartitionSpec as P

MESH_ID = pl.DeviceIdType.MESH
BOTH = (1, -1)
AROUND = (1, -1, 2)
PARTS = (True, False)
ALL, ZERO = ..., 0.0
OTHERS = 7
QUICK, SHORT = 0.2, 0.3
LANE, WIDE, STRIP, HEAD = 128, 256, 512, 64
ROW, BAND, SIDE, TRIO, PAIR = 8, 32, 4, 3, 2


class Links:
    def __init__(self, send_sems, recv_sems):
        self.send_sems, self.recv_sems = send_sems, recv_sems
        self.slots, self.batches, self.sent, self.count = {}, {}, {}, 0

    def _landing(self, key, lane):
        if key not in self.slots:
            self.slots[key] = self.count
            self.count += 1 if lane is None else PAIR
        return self.recv_sems.at[self.slots[key] + (0 if lane is None else lane)]

    def send(self, key, src, dst, device, landing=None, whole=None, batch=None, lane=None):
        leaving = self.batches.setdefault(batch or key, len(self.batches))
        copy = pltpu.make_async_remote_copy(
            src_ref=src, dst_ref=dst, send_sem=self.send_sems.at[leaving], recv_sem=self._landing(landing or key, lane),
            device_id=device, device_id_type=MESH_ID)
        copy.start()
        self.sent[batch or key] = (src if whole is None else whole, leaving)

    def arrive(self, key, landed, lane=None):
        pltpu.make_async_copy(landed, landed, self._landing(key, lane)).wait()

    def drain(self):
        for left, leaving in self.sent.values():
            pltpu.make_async_copy(left, left, self.send_sems.at[leaving]).wait()
        self.sent.clear()


def rem(a, n):
    return a % n if isinstance(a, int) else lax.rem(a, n)


def chip_position():
    f, d = lax.axis_index("fsdp"), lax.axis_index("dp")
    return f // PAIR, rem(d, SIDE), d // SIDE, rem(f, PAIR)


def device_at(x, y, z, core):
    return (z * SIDE + y, x * PAIR + core)


def step(coord, by):
    return rem(coord + SIDE + by, SIDE)


def announce(devices):
    barrier = pltpu.get_barrier_semaphore()
    for device in devices:
        pl.semaphore_signal(barrier, inc=1, device_id=device, device_id_type=MESH_ID)
    pl.semaphore_wait(barrier, len(devices))


def plan(tasks, latency=2.5):
    free, landed, order, now = {}, {}, [], ZERO
    left = list(tasks)
    while left:
        best = None
        for place, (name, rank, start, needs, after, _, _) in enumerate(left):
            if all(n[0] in landed for n in needs) and all(n in landed for n in after):
                ready = max([start, now] + [landed[task][i] for task, i in needs])
                best = min(best or (ready, rank, place), (ready, rank, place))
        now, _, place = best
        name, _, _, _, _, sends, cost = left.pop(place)
        order.append(name)
        now += cost
        landed[name] = []
        for link, time, *more in sends:
            free[link] = max(now, free.get(link, ZERO)) + time
            landed[name].append(free[link] + latency + sum(more))
    return order


def layers_order(rows_i, cols_i, rows_o, cols_o, seq, starts):
    rate = 23300.0
    tasks = []
    for m in range(SIDE):
        is_in = m % PAIR == 0
        edge = cols_i // LANE * SIDE // 9 // PAIR * WIDE
        size = {"y": rows_i // SIDE * edge, "x": rows_i * (cols_i - PAIR * edge)} if is_in else {"y": rows_o // SIDE * cols_o // PAIR}
        size["z"] = size["y"]
        colors = "yzx" if is_in else "yz"
        tasks.append((("lend", m), 5, 3.0 + SIDE * m, [], [], [("chip", (rows_i * cols_i if is_in else rows_o * cols_o) / 150000.0)], QUICK))
        for color in colors:
            cost = size[color] / rate
            both = [(("x", by), cost) for by in BOTH]
            spread = [((color, by), cost) for by in BOTH] if color != "x" else []
            tasks.append((("reach", m, color), m, starts[m], [], [], both, QUICK))
            for i, by in enumerate(BOTH):
                tasks.append((("relay", m, color, by), m, ZERO, [(("reach", m, color), i)], [], [(("x", by), cost / PAIR)] + spread, QUICK))
            halves = [(("relay", m, color, by), 0) for by in BOTH]
            tasks.append((("far", m, color), m, ZERO, halves, [], spread, QUICK))
            if color == "x":
                continue
            for off, source, first in ((-1, ("relay", m, color, 1), 1), (1, ("relay", m, color, -1), 1), (PAIR, ("far", m, color), 0)):
                for i, by in enumerate(BOTH):
                    tasks.append((("pass", m, color, off, by), m, ZERO, [(source, first + i)], [], [((color, by), cost / PAIR)], QUICK))
                halves = [(("pass", m, color, off, by), 0) for by in BOTH]
                tasks.append((("close", m, color, off), m, ZERO, halves, [], [], QUICK))
        for off in (-1, 1, PAIR):
            last = [("close", m, color, off) for color in "yz"]
            if is_in:
                last.append(("far", m, "x") if off == PAIR else ("relay", m, "x", -off))
            tasks.append((("hand", m, off), m, ZERO, [], last, [("chip", (rows_i * cols_i if is_in else rows_o * cols_o) / 150000.0)], QUICK))
    before = []

    def work(name, cost, mats=()):
        needs = [(("hand", m, off), 0) for m in mats for off in (-1, 1, PAIR)] + [(("lend", m), 0) for m in mats]
        tasks.append((name, 99, ZERO, needs, list(before), [], cost))
        before[:] = [name]

    for l in range(PAIR):
        work(("norm", l), 0.8)
        work(("project", l), 4.0, [PAIR * l])
        work(("attend", l), 4.2)
        work(("mlp", l), 2.2)
        work(("put", l), 1.6, [PAIR * l + 1])
    for l in (1, 0):
        work(("back_out", l), 2.9)
        work(("back_mlp", l), 2.0)
        work(("back_heads", l), 1.0)
        work(("back_quad", l), 6.0)
        work(("back_keys", l), QUICK)
        for i in range(PAIR):
            work(("back_in", l, i), 1.3 + 0.6 * i)
        work(("back_norm", l), 1.0)
    def send(name, rank, start, after, sends):
        tasks.append((name, rank, start, [], [after] if after else [], sends, 0.4))

    def follow(name, rank, needs, sends):
        tasks.append((name, rank, ZERO, needs, [], sends, QUICK))

    def both(axis, size):
        return [((axis, by), size / rate, margin) for by in BOTH]

    model, margin = rows_i * ROW, 2.0
    for l in (1, 0):
        for axis in "yz":
            name = ("send_h", l, axis)
            send(name, 20 - l, 58.0, ("norm", l), both(axis, seq * model))
            for i, by in enumerate(BOTH):
                for index in range(PAIR):
                    follow(("pass_h", l, axis, by, index), 10, [(name, i)], [((axis, by), seq * model / SIDE / rate, margin)])
        name = ("send_m", l)
        send(name, 22 - l, ZERO, ("mlp", l), both("x", seq * rows_o) + both("x", PAIR * seq * rows_o))
        for i, by in enumerate(BOTH):
            for index in range(PAIR):
                follow(("pass_m", l, by, index), 11, [(name, i)], [(("x", by), seq * rows_o / PAIR / rate, margin)])
        if l == 0:
            send(("own_y",), 15, ZERO, ("back_norm", 1), [])
            send(("send_scale", l), 15, ZERO, ("back_norm", l), [])
            continue
        name = ("send_y", l)
        send(name, 12, 42.0, None, both("x", seq * model))
        for i, by in enumerate(BOTH):
            follow(("pass_y", l, by), 12, [(name, i)], [(("x", by), seq * model / PAIR / rate, margin)])
        follow(("far_y", l), 12, [(("pass_y", l, by), 0) for by in BOTH], [])
        for axis in "zy":
            name = ("send_z", l, axis)
            share = seq * (cols_i + LANE) / ROW
            send(name, 13, ZERO, ("back_mlp", l), both(axis, share / PAIR) + both(axis, share))
            if axis == "y":
                name = ("rest_z", l)
                send(name, 13, ZERO, ("back_keys", l), both(axis, share / ROW) + both(axis, share / SIDE))
            for i, by in enumerate(BOTH):
                follow(("pass_z", l, axis, by), 13, [(name, i)], [((axis, by), share / PAIR / rate, margin)])
                follow(("twin_z", l, axis, by), 14, [(name, PAIR + i)], [])
            follow(("far_z", l, axis), 14, [(("pass_z", l, axis, by), 0) for by in BOTH], [])
        send(("send_scale", l), 15, ZERO, ("back_norm", l), [])
    send(("own_z",), 15, ZERO, ("back_keys", 0), [])
    return plan(tasks)


def gather_stages(links, position, shard_i, shard_o, wi, wo, lsem):
    x, y, z, core = position
    twin = device_at(x, y, z, 1 - core)
    rows_i, cols_i = shard_i.shape[1:]
    rows_o, cols_o = shard_o.shape[1:]
    quarter_i, quarter_o = rows_i // SIDE, rows_o // SIDE
    third_i = cols_i // LANE * SIDE // 9 // PAIR * WIDE
    half_o = cols_o // PAIR
    cut_o = quarter_o // 16 * ROW + ROW if quarter_o % 16 else quarter_o // PAIR
    place = {"x": x, "y": y, "z": z}

    spots = {(axis, o): step(place[axis], o) for axis in "xyz" for o in range(SIDE)}

    def spot(axis, o):
        return spots[axis, o % SIDE]

    table = {}
    for axis in "xyz":
        for o in range(1, SIDE):
            moved = {**place, axis: spot(axis, o)}
            table[axis, o] = device_at(moved["x"], moved["y"], moved["z"], core)

    def peer(axis, o):
        return table[axis, o % SIDE]

    mats = []
    for l in range(PAIR):
        mats.append((shard_i.at[l], wi.at[l], rows_i, True))
        mats.append((shard_o.at[l], wo.at[l], rows_o, False))

    def region(is_in, color, q):
        if is_in:
            if color == "x":
                lo, hi = PAIR * third_i, cols_i
                rows = (0, rows_i)
            else:
                lo, hi = (0, third_i) if color == "y" else (third_i, PAIR * third_i)
                rows = (q * quarter_i, quarter_i)
            mid = lo + ((hi - lo) // LANE + 1) // PAIR * LANE
            return (rows, (lo, hi - lo)), (rows, (lo, mid - lo)), (rows, (mid, hi - mid))
        cols = (0, half_o) if color == "y" else (half_o, half_o)
        start = q * quarter_o
        return ((start, quarter_o), cols), ((start, cut_o), cols), ((start + cut_o, quarter_o - cut_o), cols)

    def at(m, xb, area):
        (r, nr), (c, nc) = area
        _, out, size, _ = mats[m]
        return out.at[pl.ds(pl.multiple_of((PAIR * xb + core) * size + r, ROW), nr), pl.ds(c, nc)]

    def block(m, xb, index):
        _, out, size, _ = mats[m]
        return out.at[pl.ds(pl.multiple_of((PAIR * xb + index) * size, BAND), size)]

    def group(m, color):
        _, out, _, is_in = mats[m]
        (_, nr), (c, nc) = region(is_in, color, 0)[0]
        return dict(batch=(m, color), whole=out.at[pl.ds(0, nr * (TRIO if color == "x" else 12)), pl.ds(c, nc)])

    def reach(m, color):
        src, _, _, is_in = mats[m]
        area = region(is_in, color, place[color])[0]
        for by in BOTH:
            links.send((m, "x1", color, by), src.at[pl.ds(pl.multiple_of(area[0][0], ROW), area[0][1]), pl.ds(*area[1])], at(m, x, area), peer("x", by), **group(m, color))

    def launch(m, color, off):
        is_in = mats[m][TRIO]
        moved = at(m, spot("x", off), region(is_in, color, place[color])[0])
        for by in BOTH:
            links.send((m, "p1", color, off, by), moved, moved, peer(color, by), **group(m, color))

    def relay(m, color, by):
        is_in = mats[m][TRIO]
        xb = spot("x", -by)
        areas = region(is_in, color, place[color])
        links.arrive((m, "x1", color, by), at(m, xb, areas[0]))
        part = at(m, xb, areas[1] if by == 1 else areas[PAIR])
        links.send((m, "x2", color), part, part, peer("x", by), **group(m, color))
        if color != "x":
            launch(m, color, -by)

    def far(m, color):
        is_in = mats[m][TRIO]
        links.arrive((m, "x2", color), at(m, spot("x", PAIR), region(is_in, color, place[color])[0]))
        if color != "x":
            launch(m, color, PAIR)

    def pass_on(m, color, off, by):
        is_in = mats[m][TRIO]
        xb = spot("x", off)
        areas = region(is_in, color, spot(color, -by))
        links.arrive((m, "p1", color, off, by), at(m, xb, areas[0]))
        part = at(m, xb, areas[1] if by == 1 else areas[PAIR])
        links.send((m, "p2", color, off), part, part, peer(color, by), **group(m, color))

    def close(m, color, off):
        is_in = mats[m][TRIO]
        links.arrive((m, "p2", color, off), at(m, spot("x", off), region(is_in, color, spot(color, PAIR))[0]))

    def four(m):
        _, out, size, _ = mats[m]
        return out.at[pl.ds(0, SIDE * size)]

    def give(m, src, dst):
        links.send((m, "chip"), src, dst, twin, batch=(m, "chip"), whole=four(m))

    def hand(m, off):
        whole = block(m, spot("x", off), core)
        give(m, whole, whole)

    owns = []

    def begin():
        for m, (src, _, _, _) in enumerate(mats):
            copy = pltpu.make_async_copy(src, block(m, x, core), lsem.at[m])
            copy.start()
            owns.append(copy)

    def lend(m):
        give(m, mats[m][0], block(m, x, core))

    def ready(m):
        owns[m].wait()
        links.arrive((m, "chip"), four(m))

    return begin, ready, peer, {"reach": reach, "relay": relay, "far": far, "pass": pass_on, "close": close, "hand": hand, "lend": lend}


BF, F32 = jnp.bfloat16, jnp.float32


def product(a, b, contract=((1,), (0,))):
    return lax.dot_general(a, b, (contract, ((), ())), preferred_element_type=F32)


def lanes(start, size):
    return pl.ds(start if isinstance(start, int) else pl.multiple_of(start, LANE), size)


def layers_kernel(order, sc_ref, wi_ref, wo_ref, x_ref, dy_ref, freq_ref,
                  y_ref, gx_ref, hy_a, hy_b, hz_a, hz_b, mx_a, mx_b, yx_b, zy_b, zz_b, z_a, dy_a, sc_out, relay_m, relay_z,
                  wi, wo, z, om, h, hid, qr, kts, vsl, ksl, turned_q, turned_o, scores, dscores, pcat, dscat, cos_ref, sin_ref, turn_ref,
                  dot_heads, qt, dht, dkv, omt, ht, dyt, sc, gains, own_gain, gain_ref, load_sems, own_sems, send_sems, recv_sems,
                  share_send_sems, share_recv_sems):
    seq, dim = x_ref.shape
    ff = (wi.shape[PAIR] - dim - LANE) // PAIR
    position = chip_position()
    x, y, zc, core = position
    twin = device_at(x, y, zc, 1 - core)
    me = PAIR * x + core
    links, shared = Links(send_sems, recv_sems), Links(share_send_sems, share_recv_sems)
    stored = []
    spots, _ = around(position)
    h_out, m_out, y_out, z_out = {"y": (hy_a, hy_b), "z": (hz_a, hz_b)}, (mx_a, mx_b), {1: yx_b}, {(1, "y"): zy_b, (1, "z"): zz_b}
    middle = hid.at[1]
    begin, ready, peer, stages = gather_stages(links, position, wi_ref, wo_ref, wi, wo, load_sems)
    others = [(zc * SIDE + y, rem(me + k, ROW)) for k in range(1, ROW)]

    def spot(axis, o):
        return spots[axis, o % SIDE]

    def device(axis, o, index):
        moved = {"x": x, "y": y, "z": zc, axis: spot(axis, o)}
        return device_at(moved["x"], moved["y"], moved["z"], index)

    own_gain[ALL] = jnp.zeros(own_gain.shape, F32)
    count = sc_ref.shape[1]
    for f in range(ROW):
        @pl.when(me == f)
        def _():
            own_gain[0:PAIR, f * count:(f + 1) * count] = sc_ref[ALL].astype(F32)
    announce(others + [device(axis, o, index) for axis in "yz" for o in AROUND for index in range(PAIR)])
    begin()
    for k, far in enumerate(others):
        links.send(("sc",), own_gain, gains.at[me], far, batch=("sc",), whole=gains.at[pl.ds(0, OTHERS)])

    def keep(src, dst):
        copy = pltpu.make_async_copy(src, dst, own_sems.at[len(stored)])
        copy.start()
        stored.append(copy)

    def tokens(axis, o, index):
        return pl.ds(pl.multiple_of((PAIR * spot(axis, o) + index) * seq, seq), seq)

    def place(axis, o, index):
        return PAIR * spot(axis, o) + index

    def columns(axis, o):
        size = z.shape[PAIR] // ROW
        return lanes(((0 if axis == "y" else SIDE) + spot(axis, o)) * size, size)

    def several(batch, ref, n):
        whole = ref.at[pl.ds(0, n * seq if batch[0][0] in "yz" else n)]
        return dict(batch=batch, whole=whole)

    def send_h(l, axis):
        out = h_out[axis][l].at[place(axis, 0, core)]
        for by in BOTH:
            for index in range(PAIR):
                shared.send(("h", l, axis, by), ht.at[l, :, index], out, device(axis, by, index), lane=core, **several(("h", l, axis), h_out[axis][l], OTHERS))
        shared.send(("h", l, axis), ht.at[l, :, 1 - core], out, twin, **several(("h", l, axis), h_out[axis][l], OTHERS))
        keep(ht.at[l, :, core], out)

    def pass_h(l, axis, by, index):
        out = h_out[axis][l]
        shared.arrive(("h", l, axis, by), out.at[place(axis, -by, index)], index)
        part = out.at[place(axis, -by, index), pl.ds(1 - by, PAIR)]
        shared.send(("h", l, axis), part, part, device(axis, by, core), **several(("h", l, axis), out, OTHERS))

    def arrive_h(l):
        for axis in "yz":
            shared.arrive(("h", l, axis), h_out[axis][l].at[pl.ds(0, TRIO)])

    def row_block(l, o, index, part=None):
        size = omt.shape[1] // ROW
        start = (PAIR * spot("x", o) + index) * size
        if part is not None:
            size = size // PAIR
            start = start + part * size
        return omt.at[l, pl.ds(pl.multiple_of(start, 16), size)]

    def row_half(k):
        size = m_out[0].shape[1] // PAIR
        return pl.ds(k * size, size)

    def send_m(l):
        out = m_out[l].at[place("x", 0, core)]
        for k, by in enumerate(BOTH):
            for index in range(PAIR):
                shared.send(("mr", l, by), row_block(l, PAIR, index, k), relay_m.at[l, k, core], device("x", by, index), lane=core, **several(("m", l), m_out[l], OTHERS))
        for by in BOTH:
            for index in range(PAIR):
                shared.send(("m", l), row_block(l, by, index), out, device("x", by, index), **several(("m", l), m_out[l], OTHERS))
        shared.send(("m", l), row_block(l, 0, 1 - core), out, twin, **several(("m", l), m_out[l], OTHERS))
        keep(row_block(l, 0, core), out)

    def pass_m(l, by, index):
        k = (1 - by) // PAIR
        shared.arrive(("mr", l, by), relay_m.at[l, k, index], index)
        shared.send(("m", l), relay_m.at[l, k, index], m_out[l].at[place("x", -by, index), row_half(k)], device("x", by, core),
                    **several(("m2", l), m_out[l], PAIR))

    def arrive_m(l):
        shared.arrive(("m", l), m_out[l].at[pl.ds(0, OTHERS)])

    def token_half(axis, o, k):
        return pl.ds(pl.multiple_of((PAIR * spot(axis, o) + core) * seq + k * (seq // PAIR), seq // PAIR), seq // PAIR)

    def send_y(l):
        src, out = dy_ref, y_out[l].at[tokens("x", 0, core)]
        for by in BOTH:
            shared.send(("y", l, by), src, out, device("x", by, core), **several(("y", l), y_out[l], OTHERS))
        shared.send(("y", l), src, out, twin, **several(("y", l), y_out[l], OTHERS))
        keep(src, out)

    def pass_y(l, by):
        landed, part = y_out[l].at[tokens("x", -by, core)], y_out[l].at[token_half("x", -by, (1 - by) // PAIR)]
        shared.arrive(("y", l, by), landed)
        shared.send(("y2", l), part, part, device("x", by, core), **several(("y", l), y_out[l], OTHERS))
        shared.send(("y", l), landed, landed, twin, **several(("y", l), y_out[l], OTHERS))

    def far_y(l):
        landed = y_out[l].at[tokens("x", PAIR, core)]
        shared.arrive(("y2", l), landed)
        shared.send(("y", l), landed, landed, twin, **several(("y", l), y_out[l], OTHERS))

    def arrive_y(l):
        shared.arrive(("y", l), y_out[l].at[pl.ds(0, SIDE * seq)])

    def push_z(l, axis, o, ready):
        out = z_out[l, axis].at[tokens(axis, 0, core)]
        batch = several(("z", l, axis), z_out[l, axis], ROW)

        def start():
            if o != PAIR:
                shared.send(("z", l, axis, o), z.at[l, :, columns(axis, o)], out, device(axis, o, core), **batch)
                return
            for k, by in enumerate(BOTH):
                shared.send(("zr", l, axis, by), z.at[l, pl.ds(k * (seq // PAIR), seq // PAIR), columns(axis, PAIR)], relay_z.at[l, "yz".index(axis), k],
                            device(axis, by, core), **batch)

        if ready is None:
            start()
        else:
            pl.when(ready)(start)

    def own_part(l, axis):
        out, mine = z_out[l, axis].at[tokens(axis, 0, core)], z.at[l, :, columns(axis, 0)]
        shared.send(("z", l, axis), mine, out, twin, **several(("z", l, axis), z_out[l, axis], ROW))
        keep(mine, out)

    def send_z(l, axis):
        for o in (PAIR, 1, -1):
            push_z(l, axis, o, spot(axis, o) != 0 if axis == "y" else None)
        if axis == "z":
            own_part(l, axis)

    def rest_z(l):
        for o in (PAIR, 1, -1):
            push_z(l, "y", o, spot("y", o) == 0)
        own_part(l, "y")

    def pass_z(l, axis, by):
        k = (1 - by) // PAIR
        half = relay_z.at[l, "yz".index(axis), k]
        shared.arrive(("zr", l, axis, by), half)
        shared.send(("z2", l, axis), half, z_out[l, axis].at[token_half(axis, -by, k)], device(axis, by, core), **several(("z", l, axis), z_out[l, axis], ROW))

    def twin_z(l, axis, by):
        landed = z_out[l, axis].at[tokens(axis, -by, core)]
        shared.arrive(("z", l, axis, by), landed)
        shared.send(("z", l, axis), landed, landed, twin, **several(("z", l, axis), z_out[l, axis], ROW))

    def far_z(l, axis):
        landed = z_out[l, axis].at[tokens(axis, PAIR, core)]
        shared.arrive(("z2", l, axis), landed)
        shared.send(("z", l, axis), landed, landed, twin, **several(("z", l, axis), z_out[l, axis], ROW))

    def arrive_z(l, axis):
        shared.arrive(("z", l, axis), z_out[l, axis].at[pl.ds(0, SIDE * seq)])

    def send_scale(l):
        for far in others:
            shared.send(("scale", l), sc.at[l], sc_out.at[l, me], far, batch=("scale", l), whole=sc_out.at[l, pl.ds(0, OTHERS)])
        keep(sc.at[l], sc_out.at[l, me])

    def arrive_scale(l):
        shared.arrive(("scale", l), sc_out.at[l, pl.ds(0, OTHERS)])

    gains[me] = own_gain[ALL]
    z[:, :, wi.shape[PAIR]:] = jnp.zeros((PAIR, seq, z.shape[PAIR] - wi.shape[PAIR]), BF)
    entry = (x_ref, hid.at[0])
    angle = lax.broadcasted_iota(jnp.int32, (seq, LANE), 0).astype(F32) * freq_ref[0:1]
    for half in range(PAIR):
        cos_ref[:, LANE * half:LANE * (half + 1)] = jnp.cos(angle)
        sin_ref[:, LANE * half:LANE * (half + 1)] = jnp.sin(angle)
    lane = lax.broadcasted_iota(jnp.int32, turn_ref.shape, 1)
    down = lax.broadcasted_iota(jnp.int32, turn_ref.shape, 0) - lane
    low = rem(lane, HEAD) < BAND
    turn_ref[ALL] = jnp.where(low & (down == BAND), -1.0, jnp.where(jnp.logical_not(low) & (down == -BAND), 1.0, ZERO)).astype(BF)
    kts[ALL] = jnp.zeros(kts.shape, BF)
    pcat[ALL] = jnp.zeros(pcat.shape, BF)
    dscat[ALL] = jnp.zeros(dscat.shape, BF)

    def normalise(l, src):
        @pl.loop(0, seq // BAND, unroll=SIDE)
        def _(r):
            rows = pl.ds(pl.multiple_of(r * BAND, BAND), BAND)
            v = src[rows].astype(F32)
            v = v - jnp.mean(v, axis=-1, keepdims=True)
            var = jnp.mean(v * v, axis=-1, keepdims=True)
            h[l, rows] = (v * lax.rsqrt(var + 1e-6) * gain_ref[l:l + 1]).astype(BF)

    def project(l):
        strip = wi.shape[PAIR] // 5

        @pl.loop(0, 5)
        def _(i):
            at = lanes(i * strip, strip)
            z[l, :, at] = product(h[l], wi[l, :, at]).astype(BF)

    def heads(l):
        cos, sin = cos_ref[ALL], sin_ref[ALL]
        for g in range(dim // WIDE):
            q = z[l, :, g * WIDE:(g + 1) * WIDE]
            qr[l, :, g * WIDE:(g + 1) * WIDE] = ((q.astype(F32) * cos + product(q, turn_ref[ALL]) * sin) * 0.125).astype(BF)
        kv = z[l, :, dim:dim + LANE]
        turned = kv.astype(F32) * cos[:, :LANE] + product(kv, turn_ref[:LANE, :LANE]) * sin[:, :LANE]
        first = lax.broadcasted_iota(jnp.int32, turned.shape, 1) < HEAD
        key_lo = jnp.where(first, turned, ZERO)
        val_hi = jnp.where(first, ZERO, kv.astype(F32))
        return key_lo, pltpu.roll(key_lo, HEAD, 1), pltpu.roll(val_hi, HEAD, 1), val_hi

    def slot_rows(ref, lo, hi):
        zero = jnp.zeros((seq, LANE), BF)
        lo, hi = lo.astype(BF), hi.astype(BF)
        for i, (left, right) in enumerate(((lo, zero), (hi, zero), (zero, lo), (zero, hi))):
            ref[i * seq:(i + 1) * seq, :LANE] = left
            ref[i * seq:(i + 1) * seq, LANE:] = right

    def slot_cols(ref, lo):
        flat = lo.T[:HEAD].astype(BF)
        for i in range(SIDE):
            ref[HEAD * i:HEAD * (i + 1), i * seq:(i + 1) * seq] = flat

    def chances(i, half):
        at = slice(LANE * half, LANE * (half + 1))
        blocks = [pl.ds(pl.multiple_of(i * seq + LANE * k, LANE), LANE) for k in range(half + 1)]
        s = [scores[keys, at] for keys in blocks]
        lower = lax.broadcasted_iota(jnp.int32, s[-1].shape, 1) >= lax.broadcasted_iota(jnp.int32, s[-1].shape, 0)
        s[-1] = jnp.where(lower, s[-1], -1e30)
        top = functools.reduce(jnp.maximum, [jnp.max(v, axis=0, keepdims=True) for v in s])
        e = [jnp.exp(v - top) for v in s]
        scale = 1.0 / sum(jnp.sum(v, axis=0, keepdims=True) for v in e)
        return at, [(keys, v * scale) for keys, v in zip(blocks, e)]

    def attend(l):
        key_lo, key_hi, val_lo, _ = heads(l)
        slot_rows(ksl, key_lo, key_hi)
        slot_cols(kts, val_lo)
        flip(lambda at: qr[l, :, lanes(at, WIDE)], qt, dim)

        @pl.loop(0, dim // WIDE)
        def _(g):
            rows = pl.ds(pl.multiple_of(g * WIDE, WIDE), WIDE)
            scores[ALL] = product(ksl[ALL], qt[rows])

            @pl.loop(0, SIDE)
            def _(i):
                for half in range(PAIR):
                    at, blocks = chances(i, half)
                    for keys, p in blocks:
                        pcat[keys, at] = p.astype(BF)
            flat = product(kts[ALL], pcat[ALL]).astype(BF)
            omt[l, rows] = flat
            om[:, lanes(g * WIDE, WIDE)] = flat.T

    def mlp(l):
        @pl.loop(0, seq // BAND)
        def _(r):
            rows = pl.ds(pl.multiple_of(r * BAND, BAND), BAND)

            @pl.loop(0, ff // STRIP)
            def _(i):
                gate = z[l, rows, lanes(dim + LANE + i * STRIP, STRIP)].astype(F32)
                up = z[l, rows, lanes(dim + LANE + ff + i * STRIP, STRIP)].astype(F32)
                om[rows, lanes(dim + i * STRIP, STRIP)] = (gate * jax.nn.sigmoid(gate) * up).astype(BF)

    def put_out(l, dst):
        for n in range(dim // WIDE):
            cols = slice(n * WIDE, (n + 1) * WIDE)
            total = product(om[ALL], wo[l, :, cols])
            dst[:, cols] = (entry[l][:, cols].astype(F32) + total).astype(BF)

    def flip(src, dst, width, first=0):
        @pl.loop(first // WIDE, width // WIDE)
        def _(i):
            dst[pl.ds(pl.multiple_of(i * WIDE, WIDE), WIDE)] = src(i * WIDE).T

    upstream = (middle, dy_ref)

    def back_out(l):
        dy = upstream[l]
        flip(lambda at: dy[:, lanes(at, WIDE)], dyt, dim)

        @pl.loop(0, wo.shape[1] // dim)
        def _(n):
            rows = pl.ds(pl.multiple_of(n * dim, dim), dim)
            part = product(wo[l, rows], dyt[ALL]).astype(BF)
            om[:, lanes(n * dim, dim)] = part.T

            @pl.when(n == 0)
            def _():
                dot_heads[ALL] = part

    def back_mlp(l):
        @pl.loop(0, seq // BAND)
        def _(r):
            rows = pl.ds(pl.multiple_of(r * BAND, BAND), BAND)

            @pl.loop(0, ff // STRIP)
            def _(i):
                gate_at, up_at = lanes(dim + LANE + i * STRIP, STRIP), lanes(dim + LANE + ff + i * STRIP, STRIP)
                gate, up = z[l, rows, gate_at].astype(F32), z[l, rows, up_at].astype(F32)
                d = om[rows, lanes(dim + i * STRIP, STRIP)].astype(F32)
                sig = jax.nn.sigmoid(gate)
                du = d * up
                z[l, rows, gate_at] = (du * sig + du * gate * (sig * (1.0 - sig))).astype(BF)
                z[l, rows, up_at] = (d * (gate * sig)).astype(BF)

    def back_heads(l):
        key_lo, key_hi, val_lo, val_hi = heads(l)
        slot_rows(ksl, key_lo, key_hi)
        slot_rows(vsl, val_lo, val_hi)
        slot_cols(kts, key_lo)
        dkv[ALL] = jnp.zeros(dkv.shape, F32)
        flip(lambda at: qr[l, :, lanes(at, WIDE)], qt, dim)
        for at in range(0, dim, LANE):
            pair = slice(at, at + LANE)
            turned_q[:, pair] = pltpu.roll(qr[l, :, pair].astype(F32), HEAD, 1).astype(BF)
            turned_o[:, pair] = pltpu.roll(om[:, pair].astype(F32), HEAD, 1).astype(BF)

    def back_quad(l):
        @pl.loop(0, dim // WIDE)
        def _(g):
            quad(l, g)

    def quad(l, g):
        cols = pl.ds(pl.multiple_of(g * WIDE, WIDE), WIDE)
        scores[ALL] = product(ksl[ALL], qt[cols])
        dscores[ALL] = product(vsl[ALL], dot_heads[cols])

        @pl.loop(0, SIDE)
        def _(i):
            for half in range(PAIR):
                at, blocks = chances(i, half)
                given = [p * dscores[keys, at].astype(BF).astype(F32) for keys, p in blocks]
                total = sum(jnp.sum(v, axis=0, keepdims=True) for v in given)
                for (keys, p), v in zip(blocks, given):
                    pcat[keys, at] = p.astype(BF)
                    dscat[keys, at] = (v - p * total).astype(BF)
        dq = product(kts[ALL], dscat[ALL]).astype(BF).T
        back = dq.astype(F32) * cos_ref[ALL] - product(dq, turn_ref[ALL]) * sin_ref[ALL]
        z[l, :, cols] = (back * 0.125).astype(BF)
        def pieces(left, even, odd):
            for i in range(SIDE):
                pair = lanes(g * WIDE + i // PAIR * LANE, LANE)
                yield product(left[i * seq:(i + 1) * seq, :], odd(pair) if i % PAIR else even(pair))

        dkv[0] += sum(pieces(dscat, lambda at: qr[l, :, at], lambda at: turned_q[:, at]))
        dkv[1] += sum(pieces(pcat, lambda at: turned_o[:, at], lambda at: om[:, at]))

    def back_keys(l):
        dk = dkv[0].astype(BF)
        turned = dk.astype(F32) * cos_ref[:, :LANE] - product(dk, turn_ref[:LANE, :LANE]) * sin_ref[:, :LANE]
        first = lax.broadcasted_iota(jnp.int32, turned.shape, 1) < HEAD
        z[l, :, dim:dim + LANE] = jnp.where(first, turned, dkv[1]).astype(BF)

    def back_in(l, half):
        width = wi.shape[PAIR] // 5
        at = slice(PAIR * half * width, (PAIR + TRIO * half) * width)
        part = product(wi[l, :, at], z[l, :, at], ((1,), (1,)))
        dht[ALL] = dht[ALL] + part if half else part

    def back_norm(l):
        dy, dst = upstream[l], (gx_ref, middle)[l]
        for i in range(dim // WIDE):
            cols = slice(i * WIDE, (i + 1) * WIDE)
            h[l, :, cols] = dht[cols].T.astype(BF)
        sc[l] = jnp.zeros(sc.shape[1:], F32)

        @pl.loop(0, seq // BAND, unroll=SIDE)
        def _(r):
            rows = pl.ds(pl.multiple_of(r * BAND, BAND), BAND)
            v = entry[l][rows].astype(F32)
            v = v - jnp.mean(v, axis=-1, keepdims=True)
            scale = lax.rsqrt(jnp.mean(v * v, axis=-1, keepdims=True) + 1e-6)
            hat = v * scale
            d = h[l, rows].astype(F32)
            each = (d * hat).reshape(SIDE, ROW, dim)
            sc[l] += (each[0] + each[1]) + (each[PAIR] + each[TRIO])
            d = d * gain_ref[l:l + 1]
            d = scale * (d - jnp.mean(d, axis=-1, keepdims=True) - hat * jnp.mean(d * hat, axis=-1, keepdims=True))
            dst[rows] = (dy[rows].astype(F32) + d.astype(BF).astype(F32)).astype(BF)

    def do_norm(l):
        if l == 0:
            links.arrive(("sc",), gains.at[pl.ds(0, OTHERS)])
            gain_ref[ALL] = jnp.sum(gains[ALL], axis=0)
        normalise(l, entry[l])
        for i in range(dim // WIDE):
            flat = h[l, :, i * WIDE:(i + 1) * WIDE].T
            size = ht.shape[TRIO]
            for b in range(ROW):
                lo, hi = max(b * size, i * WIDE), min((b + 1) * size, (i + 1) * WIDE)
                if lo < hi:
                    ht[l, b // PAIR, b % PAIR, lo - b * size:hi - b * size] = flat[lo - i * WIDE:hi - i * WIDE]

    def do_project(l):
        ready(PAIR * l)
        project(l)

    def do_mlp(l):
        mlp(l)
        flip(lambda at: om[:, lanes(at, WIDE)], omt.at[l], om.shape[1], dim)

    def do_put(l):
        ready(PAIR * l + 1)
        put_out(l, hid.at[0] if l == 0 else y_ref)

    stages.update(
        norm=do_norm, project=do_project, attend=attend, mlp=do_mlp, put=do_put, back_out=back_out, back_mlp=back_mlp, back_heads=back_heads,
        back_quad=back_quad, back_keys=back_keys, back_in=back_in, back_norm=back_norm, send_h=send_h, pass_h=pass_h, send_m=send_m,
        pass_m=pass_m, send_y=send_y, pass_y=pass_y, far_y=far_y, send_z=send_z, rest_z=rest_z, pass_z=pass_z, twin_z=twin_z, far_z=far_z,
        send_scale=send_scale, own_z=lambda: keep(z.at[0], z_a), own_y=lambda: keep(middle, dy_a))
    for kind, *task in order:
        stages[kind](*task)
    for l in range(PAIR):
        arrive_h(l)
        arrive_m(l)
        arrive_scale(l)
    arrive_y(1)
    for l, axis in z_out:
        arrive_z(l, axis)
    for copy in stored:
        copy.wait()
    shared.drain()
    links.drain()


def run_layers(x, dy, scale, w_in, w_out, freq, starts=(ZERO, 10.0, 20.0, 30.0)):
    seq, dim = x.shape
    proj, cat = w_in.shape[PAIR], ROW * w_out.shape[1]
    wide = proj + LANE
    hbm, vmem = pl.BlockSpec(memory_space=pltpu.HBM), pl.BlockSpec(memory_space=pltpu.VMEM)
    out = lambda *shape, dtype=BF: jax.ShapeDtypeStruct(shape, dtype)
    buffer = lambda *shape, dtype=BF: pltpu.VMEM(shape, dtype)
    sem = pltpu.SemaphoreType.DMA
    line = ROW * seq
    return pl.pallas_call(
        functools.partial(layers_kernel, layers_order(*w_in.shape[1:], *w_out.shape[1:], seq, starts)),
        out_shape=(out(seq, dim), out(seq, dim), *[out(ROW, SIDE, dim // ROW, seq)] * SIDE, *[out(ROW, cat // ROW, seq)] * PAIR, out(line, dim),
                   *[out(line, wide // ROW)] * PAIR, out(seq, wide), out(seq, dim), out(PAIR, ROW, ROW, dim, dtype=F32),
                   out(PAIR, PAIR, PAIR, cat // 16, seq), out(PAIR, PAIR, PAIR, seq // PAIR, wide // ROW)),
        in_specs=[vmem, hbm, hbm] + [vmem] * TRIO,
        out_specs=[vmem] * PAIR + [hbm] * 14,
        scratch_shapes=[
            buffer(PAIR, dim, proj), buffer(PAIR, cat, dim), buffer(PAIR, seq, wide), buffer(seq, cat), buffer(PAIR, seq, dim),
            buffer(PAIR, seq, dim), buffer(PAIR, seq, dim),
            buffer(WIDE, SIDE * seq), buffer(SIDE * seq, WIDE), buffer(SIDE * seq, WIDE), buffer(seq, dim), buffer(seq, dim),
            buffer(SIDE * seq, seq, dtype=F32), buffer(SIDE * seq, seq, dtype=F32), buffer(SIDE * seq, seq), buffer(SIDE * seq, seq),
            buffer(seq, WIDE, dtype=F32), buffer(seq, WIDE, dtype=F32), buffer(WIDE, WIDE),
            buffer(dim, seq), buffer(dim, seq), buffer(dim, seq, dtype=F32), buffer(PAIR, seq, LANE, dtype=F32),
            buffer(PAIR, cat, seq), buffer(PAIR, SIDE, PAIR, dim // ROW, seq), buffer(dim, seq), buffer(PAIR, ROW, dim, dtype=F32),
            buffer(ROW, ROW, dim, dtype=F32), buffer(ROW, dim, dtype=F32), buffer(ROW, dim, dtype=F32),
            sem((SIDE,)), sem((13,)), sem((15,)), sem((107,)), sem((13,)), sem((HEAD,)),
        ],
        compiler_params=pltpu.CompilerParams(collective_id=PAIR, has_side_effects=True, vmem_limit_bytes=67043328),
        name="run_layers",
    )(scale, w_in, w_out, x, dy, freq)


PARTS = (("i", "x", "z", "y", 0, STRIP), ("i", "x", "z", "y", STRIP, 384), ("i", "x", "y", "z", 0, STRIP), ("i", "x", "y", "z", STRIP, 384),
         ("o", "y", "z", "y", 0, 384), ("o", "z", "y", "z", 384, 384))


def reduce_order(rows, rows_b, starts):
    rate = 11650.0
    tasks = []
    sizes = {"y": WIDE * 896 / (PAIR * rate), "z": WIDE * 896 / (PAIR * rate), "x": WIDE * 768 / (PAIR * rate)}
    for axis in "yzx":
        size = sizes[axis]
        tasks.append((("swap", axis), (0, 0), starts[PAIR] if axis == "x" else starts[TRIO], [], [],
                      [((axis, by), size * n) for by, n in ((-1, 0.5), (1, 1), (-1, 1), (1, 1))], SHORT))
        tasks.append((("relay", axis), (0, 0), ZERO, [(("swap", axis), 0)], [], [((axis, -1), size / PAIR)], SHORT))
        for o, needs in ((1, [(("swap", axis), 1)]), (-1, [(("swap", axis), PAIR)]), (PAIR, [(("swap", axis), TRIO), (("relay", axis), 0)])):
            tasks.append((("near", axis, o), (0, PAIR), ZERO, needs, [], [("chip", 1.6)], QUICK))
    tasks.append((("fetch", 0), (5, 0), ZERO, [], [("make", 1, len(PARTS) - 1)], [], QUICK))
    for l in (1, 0):
        late = 1 - l
        for c, (kind, first, then, last, at, width) in enumerate(PARTS):
            needs, cost = [], 1.6 * width / STRIP
            if l == 0:
                needs = [(("near", last if kind == "i" else "x", o), 0) for o in AROUND]
            tasks.append((("make", l, c), (9 * late, c), starts[late], needs, [] if l else [("fetch", 0)], [], cost))
            full = SIDE * SIDE * (rows if kind == "i" else rows_b) * width / rate
            sends = [[((first, by), full / ROW) for by in BOTH], [((first, by), full / SIDE) for by in BOTH],
                     [((then, o), full / 16) for o in (1, -1, 1)], []]
            piece = full / 16
            sends += [[((then, by), piece) for by in BOTH], [((then, 1 - PAIR * (c % PAIR)), piece)], [((last, by), SIDE * piece) for by in BOTH],
                      [((last, by), PAIR * piece) for by in BOTH], []]
            for s in range(9):
                task = ("sum", l, c, s)
                needs = [(("sum", l, c, s - 1), k) for k in range(len(sends[s - 1]))] if s else []
                tasks.append((task, (late, -s), ZERO, needs, [("make", l, c)] if s == 0 else [("sum", l, c, s - 1)], sends[s], SHORT))
    return plan(tasks)


def reduce_kernel(order, *refs):
    hy, hz, mx = refs[0:PAIR], refs[PAIR:SIDE], refs[SIDE:6]
    yx1, zy1, zz1, z0, y0, sc = refs[6:12]
    oa, ob = refs[12:14]
    n = len(PARTS)
    total, half, full, small, front = (refs[14 + k * n:14 + (k + 1) * n] for k in range(5))
    (hbuf, zbuf, mbuf, ybuf, scbuf, rz, ry, ssem, rsem, isem, osem) = refs[14 + 5 * n:]
    position = chip_position()
    x, y, zc, core = position
    place = {"x": x, "y": y, "z": zc}
    twin = device_at(x, y, zc, 1 - core)
    spots, peers = around(position)

    def spot(axis, o):
        return spots[axis, o % SIDE]

    def peer(axis, o):
        return peers[axis, o % SIDE]

    seq, wide = z0.shape
    own = wide // ROW
    loads, moving = {}, []

    def load(key, src, dst):
        copy = pltpu.make_async_copy(src, dst, isem.at[len(moving)])
        moving.append(key)
        copy.start()
        loads[key] = copy

    def fetch(l):
        if l:
            load(("z", 1, "y"), zy1, zbuf.at[1, 0])
        load(("h", l, "y"), hy[l], hbuf.at[l, 0])
        if l:
            load(("z", 1, "z"), zz1, zbuf.at[1, 1])
        load(("h", l, "z"), hz[l], hbuf.at[l, 1])
        load(("m", l), mx[l], mbuf.at[l])
        if l:
            load(("y", 1), yx1, ybuf.at[1])
        load(("s", l), sc.at[l], scbuf.at[l])

    fetch(1)
    done = set()

    def loaded(*keys):
        for key in keys:
            if key not in done:
                loads[key].wait()
                done.add(key)

    announce([peer(axis, o) for axis in "xyz" for o in AROUND] + [twin])
    links = Links(ssem, rsem)

    def columns(axis, o):
        return lanes(((0 if axis == "y" else SIDE) + spot(axis, o)) * own, own)

    def tokens(axis, o, index):
        return pl.ds(pl.multiple_of((PAIR * spot(axis, o) + index) * seq, seq), seq)

    def target(axis):
        return ybuf.at[0] if axis == "x" else zbuf.at[0, "yz".index(axis)]

    def leaving(axis):
        return dict(batch=("swap", axis), whole=target(axis).at[pl.ds(0, OTHERS * seq + seq // PAIR)])

    def half_at(axis, o, k):
        start = (PAIR * spot(axis, o) + core) * seq + k * (seq // PAIR)
        return target(axis).at[pl.ds(pl.multiple_of(start, seq // PAIR), seq // PAIR)]

    def relay_of(axis):
        return ry if axis == "x" else rz.at["yz".index(axis)]

    def swap(axis):
        def part(o, rows=slice(None)):
            return y0.at[rows] if axis == "x" else z0.at[rows, columns(axis, o)]

        mine = target(axis).at[tokens(axis, 0, core)]
        links.send(("relay", axis), part(PAIR, pl.ds(seq // PAIR, seq // PAIR)), relay_of(axis), peer(axis, -1), **leaving(axis))
        for by in BOTH:
            links.send(("swap", axis, by), part(by), mine, peer(axis, by), **leaving(axis))
        links.send(("swap", axis, PAIR), part(PAIR, pl.ds(0, seq // PAIR)), half_at(axis, 0, 0), peer(axis, PAIR), **leaving(axis))
        links.send(("near", axis), part(0), mine, twin, **leaving(axis))
        load(("own", axis), part(0), mine)

    def relay(axis):
        links.arrive(("relay", axis), relay_of(axis))
        links.send(("relayed", axis), relay_of(axis), half_at(axis, 1, 1), peer(axis, -1), **leaving(axis))

    def near(axis, o):
        landed = target(axis).at[tokens(axis, -o, core)]
        if o == PAIR:
            links.arrive(("swap", axis, PAIR), half_at(axis, PAIR, 0))
            links.arrive(("relayed", axis), half_at(axis, PAIR, 1))
        else:
            links.arrive(("swap", axis, o), landed)
        links.send(("near", axis), landed, landed, twin, **leaving(axis))

    def joined(axis):
        if axis not in done:
            done.add(axis)
            loaded(("own", axis))
            links.arrive(("near", axis), target(axis).at[pl.ds(0, SIDE * seq)])

    def joined_lanes(ref, l, i):
        return jnp.concatenate([ref[l, i, k].reshape(-1, ref.shape[-1]) for k in range(ROW)], axis=1)

    def make(l, c):
        kind, first, then, last, at, width = PARTS[c]
        if kind == "i":
            i = "yz".index(last)
            loaded(("h", l, last))
            if l:
                loaded(("z", l, last))
            else:
                joined(last)
            size = total[c].shape[TRIO]
            for lo in range(0, width, WIDE):
                hi = min(width, lo + WIDE)
                part = product(joined_lanes(hbuf, l, i), zbuf[l, i, :, at + lo:at + hi])
                for r in range(16):
                    total[c][l, r // SIDE, r % SIDE, :, lo:hi] = part[r * size:(r + 1) * size]
            return
        loaded(("m", l), ("s", l))
        if l:
            loaded(("y", l))
        else:
            joined("x")
        part = product(jnp.concatenate([mbuf[l, k] for k in range(ROW)], axis=1), ybuf[l, :, at:at + width])
        size = total[c].shape[TRIO]

        def put(r, value):
            total[c][(l, r // SIDE, r % SIDE) if first == "y" else (l, r % SIDE, r // SIDE)] = value

        for r in range(part.shape[0] // size):
            put(r, part[r * size:(r + 1) * size])
        gain = jnp.sum(jnp.sum(scbuf[l, :, :, at:at + width], axis=0), axis=0, keepdims=True)
        row = lax.broadcasted_iota(jnp.int32, (size, width), 0)
        put(15, jnp.where(row == 0, gain, ZERO))

    def area(l, c, o, whole):
        kind, first, then, last, at, width = PARTS[c]
        inner = (spot(then, whole) if isinstance(whole, int) else whole)
        outer = spot(last, o)
        if kind == "i":
            cols = lanes(((0 if last == "y" else SIDE) + outer) * own + at, width)
            return oa.at[l, inner, :, cols]
        cols = pl.ds(at, width)
        return ob.at[l, outer, inner, :, cols] if last == "y" else ob.at[l, inner, outer, :, cols]

    def add(l, c, s):
        kind, first, then, last, at, width = PARTS[c]
        t = total[c].at[l]
        way = 1 - PAIR * (c % PAIR)
        sums = dict(batch=(l, c, 0), whole=t)
        wide_ones = dict(batch=(l, c, 1), whole=t.at[pl.ds(0, TRIO)])
        narrow = dict(batch=(l, c, PAIR), whole=t.at[0, pl.ds(0, PAIR)])
        if s == 0:
            far = t.at[spot(first, PAIR)]
            for k, by in enumerate(BOTH):
                links.send((l, c, "half"), far.at[pl.ds(PAIR * k, PAIR)], half[c].at[l, k], peer(first, by), **sums)
        elif s == 1:
            links.arrive((l, c, "half"), half[c].at[l])
            for k, by in enumerate(BOTH):
                mine = t.at[spot(first, by)]
                add_into(mine.at[pl.ds(PAIR * k, PAIR)], half[c].at[l, k])
                links.send((l, c, "full"), mine, full[c].at[l, k], peer(first, by), **sums)
        elif s == PAIR:
            mine = t.at[spot(first, 0)]
            links.arrive((l, c, "full"), full[c].at[l])
            for k in range(PAIR):
                add_into(mine, full[c].at[l, k])
            for k, o in enumerate(AROUND):
                links.send((l, c, "small"), mine.at[spot(then, o)], small[c].at[l, k], peer(then, o), **wide_ones)
        elif s == TRIO:
            links.arrive((l, c, "small"), small[c].at[l])
            mine = t.at[spot(first, 0), spot(then, 0)]
            front[c][l] = (mine[ALL] + small[c][l, 0]) + (small[c][l, 1] + small[c][l, PAIR])
        elif s == SIDE:
            src, dst = front[c].at[l], area(l, c, 0, 0)
            for by in BOTH:
                links.send((l, c, "a1"), src, dst, peer(then, by), **narrow)
            copy = pltpu.make_async_copy(src, dst, osem.at[l, c])
            copy.start()
            loads["front", l, c] = copy
        elif s == 5:
            links.arrive((l, c, "a1"), t.at[0, pl.ds(0, PAIR)])
            landed = area(l, c, 0, -way)
            links.send((l, c, "b1"), landed, landed, peer(then, way), **wide_ones)
        elif s == 6:
            loaded(("front", l, c))
            links.arrive((l, c, "b1"), area(l, c, 0, PAIR))
            line = area(l, c, 0, slice(None))
            for by in BOTH:
                links.send((l, c, "a2"), line, line, peer(last, by), **wide_ones)
        elif s == OTHERS:
            links.arrive((l, c, "a2"), t.at[pl.ds(0, PAIR)])
            for k, by in enumerate(BOTH):
                part = area(l, c, -by, pl.ds(PAIR * k, PAIR))
                links.send((l, c, "a3"), part, part, peer(last, by), **sums)
        else:
            links.arrive((l, c, "a3"), area(l, c, PAIR, slice(None)))

    stages = {"swap": swap, "relay": relay, "near": near, "fetch": fetch, "make": make, "sum": add}
    for kind, *task in order:
        stages[kind](*task)
    links.drain()


def add_into(dst, src):
    @pl.loop(0, dst.shape[0])
    def _(i):
        if len(dst.shape) == SIDE:
            for j in range(dst.shape[1]):
                dst[i, j] += src[i, j]
        else:
            dst[i] += src[i]


def around(position):
    place, core = dict(zip("xyz", position)), position[TRIO]
    spots = {(axis, o): step(place[axis], o) for axis in "xyz" for o in range(SIDE)}
    peers = {}
    for axis in "xyz":
        for o in range(1, SIDE):
            moved = {**place, axis: spots[axis, o]}
            peers[axis, o] = device_at(moved["x"], moved["y"], moved["z"], core)
    return spots, peers


def reduce_gradients(operands, starts=(ZERO, ZERO, 20.0, 3.0)):
    hbm = pl.BlockSpec(memory_space=pltpu.HBM)
    h_rows, m_rows, y_cols, z_cols, z_own, y_own, scale_parts = operands
    part, part_b = h_rows[0].shape[PAIR] // SIDE, (m_rows[0].shape[1] + BAND) // 16
    (line, dim), wide = y_cols.shape, z_own.shape[1]
    out = lambda *shape: jax.ShapeDtypeStruct(shape, F32)
    sem = pltpu.SemaphoreType.DMA

    def buffers(*lead):
        return [pltpu.VMEM((PAIR, *lead, part if e[0] == "i" else part_b, e[5]), F32) for e in PARTS]

    return pl.pallas_call(
        functools.partial(reduce_kernel, reduce_order(part, part_b, starts)),
        out_shape=(out(PAIR, SIDE, part, wide), out(PAIR, SIDE, SIDE, part_b, dim)),
        in_specs=[hbm] * 12,
        out_specs=[hbm] * PAIR,
        scratch_shapes=[
            *buffers(SIDE, SIDE), *buffers(PAIR, PAIR), *buffers(PAIR, SIDE), *buffers(TRIO), *buffers(),
            pltpu.VMEM((PAIR, PAIR, *h_rows[0].shape), BF), pltpu.VMEM((PAIR, PAIR, line, wide // ROW), BF), pltpu.VMEM((PAIR, *m_rows[0].shape), BF),
            pltpu.VMEM((PAIR, line, dim), BF), pltpu.VMEM(scale_parts.shape, F32),
            pltpu.VMEM((PAIR, z_own.shape[0] // PAIR, wide // ROW), BF), pltpu.VMEM((y_own.shape[0] // PAIR, dim), BF),
            sem((39,)), sem((102,)), sem((14,)), sem((PAIR, len(PARTS))),
        ],
        compiler_params=pltpu.CompilerParams(collective_id=1, has_side_effects=True, vmem_limit_bytes=67043328),
        name="reduce_gradients",
    )(*h_rows, *m_rows, y_cols, *z_cols, z_own, y_own, scale_parts)


def finish_kernel(count, in_ref, out_ref, y_ref, gx_ref, in_grad, out_grad, y_out, gx_out, scale_out, in_buf, out_buf, y_buf, gx_buf, came, left):
    moves = [(out_ref.at[l, p], out_buf.at[l, pl.ds(SIDE * p, SIDE)]) for l in range(PAIR) for p in range(SIDE)]
    moves += [(y_ref, y_buf), (gx_ref, gx_buf)]
    size, width = in_buf.shape[PAIR:]
    moves += [(in_ref.at[l, p, :, pl.ds(0, width)], in_buf.at[l, p]) for l in range(PAIR) for p in range(SIDE)]
    loads = [pltpu.make_async_copy(src, dst, came.at[k]) for k, (src, dst) in enumerate(moves)]
    for copy in loads:
        copy.start()
    stores = []

    def store(src, dst):
        copy = pltpu.make_async_copy(src, dst, left.at[len(stores)])
        copy.start()
        stores.append(copy)

    for l in range(PAIR):
        for p in range(SIDE):
            loads[SIDE * l + p].wait()
        store(out_buf.at[l, pl.ds(0, 15)], out_grad.at[l])
    for k, (src, dst) in enumerate(((y_buf, y_out), (gx_buf, gx_out))):
        loads[ROW + k].wait()
        store(src, dst)
    me = lax.axis_index("fsdp")
    for l in range(PAIR):
        for f in range(ROW):
            @pl.when(me == f)
            def _():
                scale_out[l:l + 1] = out_buf[l, 15, 0:1, f * count:(f + 1) * count]
    for l in range(PAIR):
        for p in range(SIDE):
            loads[10 + SIDE * l + p].wait()
            store(in_buf.at[l, p], in_grad.at[l, pl.ds(p * size, size)])
    for copy in stores:
        copy.wait()


def finish(in_sums, out_sums, y, gx, rows, proj):
    hbm = pl.BlockSpec(memory_space=pltpu.HBM)
    out = lambda *shape, dtype=F32: jax.ShapeDtypeStruct(shape, dtype)
    size, (depth, dim) = in_sums.shape[PAIR], out_sums.shape[TRIO:]
    in_grad, out_grad, y_out, gx_out, scale = pl.pallas_call(
        functools.partial(finish_kernel, rows),
        out_shape=(out(PAIR, rows, proj), out(PAIR, 15, depth, dim), out(*y.shape, dtype=BF), out(*gx.shape, dtype=BF), out(PAIR, rows)),
        in_specs=[hbm] * SIDE,
        out_specs=[hbm] * SIDE + [pl.BlockSpec(memory_space=pltpu.VMEM)],
        scratch_shapes=[
            pltpu.VMEM((PAIR, SIDE, size, proj), F32), pltpu.VMEM((PAIR, 16, depth, dim), F32), pltpu.VMEM(y.shape, BF), pltpu.VMEM(gx.shape, BF),
            pltpu.SemaphoreType.DMA((18,)), pltpu.SemaphoreType.DMA((12,)),
        ],
        compiler_params=pltpu.CompilerParams(vmem_limit_bytes=67043328),
        name="finish",
    )(in_sums, out_sums, y, gx)
    return y_out[None], gx_out[None], scale, in_grad, out_grad.reshape(PAIR, 15 * depth, dim)


def solution(mesh):
    fsdp_size = mesh.shape["fsdp"]
    batch_spec = P(("dp", "fsdp"), None, None)
    scale_spec = P(None, "fsdp")
    weight_spec = P(None, "fsdp", None)

    def device_step(x_in, grad_y, norm_scale, w_in, w_out):
        n_layers = w_in.shape[0]
        seq_len, model_dim = x_in.shape[1:]
        proj_dim = w_in.shape[PAIR]
        ff_dim = w_out.shape[1] * fsdp_size - model_dim
        head_dim = (proj_dim - model_dim - PAIR * ff_dim) // PAIR
        rows, rows_out = norm_scale.shape[1], w_out.shape[1]
        half_dim = head_dim // PAIR
        freq = 10000.0 ** (-np.arange(half_dim, dtype=np.float32) * 2.0 / head_dim)
        freq = jnp.asarray(np.tile(freq.astype(np.float32), (ROW, LANE // half_dim)))
        hidden, grad_hidden, *rest = run_layers(x_in[0], grad_y[0], norm_scale, w_in, w_out, freq)
        in_sums, out_sums = reduce_gradients((rest[0:SIDE], rest[SIDE:6], rest[6], rest[OTHERS:9], rest[9], rest[10], rest[11]))
        return finish(in_sums, out_sums, hidden, grad_hidden, rows, proj_dim)

    return jax.shard_map(
        device_step,
        mesh=mesh,
        in_specs=(batch_spec, batch_spec, scale_spec, weight_spec, weight_spec),
        out_specs=(batch_spec, batch_spec, scale_spec, weight_spec, weight_spec),
        check_vma=False,
    )
```

```python
import functools
import jax
import jax.numpy as jnp
import numpy as np
from jax import lax
from jax.experimental import pallas as pl
from jax.experimental.pallas import tpu as pltpu
from jax.sharding import PartitionSpec as P

MESH_ID = pl.DeviceIdType.MESH
BOTH = (1, -1)
AROUND = (1, -1, 2)
PARTS = (True, False)
ALL, ZERO = ..., 0.0
OTHERS = 7
QUICK, SHORT = 0.2, 0.3
LANE, WIDE, STRIP, HEAD = 128, 256, 512, 64
ROW, BAND, SIDE, TRIO, PAIR = 8, 32, 4, 3, 2


class Links:
    def __init__(self, send_sems, recv_sems):
        self.send_sems, self.recv_sems = send_sems, recv_sems
        self.slots, self.batches, self.sent, self.count = {}, {}, {}, 0

    def _landing(self, key, lane):
        if key not in self.slots:
            self.slots[key] = self.count
            self.count += 1 if lane is None else PAIR
        return self.recv_sems.at[self.slots[key] + (0 if lane is None else lane)]

    def send(self, key, src, dst, device, landing=None, whole=None, batch=None, lane=None):
        leaving = self.batches.setdefault(batch or key, len(self.batches))
        copy = pltpu.make_async_remote_copy(
            src_ref=src, dst_ref=dst, send_sem=self.send_sems.at[leaving], recv_sem=self._landing(landing or key, lane),
            device_id=device, device_id_type=MESH_ID)
        copy.start()
        self.sent[batch or key] = (src if whole is None else whole, leaving)

    def arrive(self, key, landed, lane=None):
        pltpu.make_async_copy(landed, landed, self._landing(key, lane)).wait()

    def drain(self):
        for left, leaving in self.sent.values():
            pltpu.make_async_copy(left, left, self.send_sems.at[leaving]).wait()
        self.sent.clear()


def rem(a, n):
    return a % n if isinstance(a, int) else lax.rem(a, n)


def chip_position():
    f, d = lax.axis_index("fsdp"), lax.axis_index("dp")
    return f // PAIR, rem(d, SIDE), d // SIDE, rem(f, PAIR)


def device_at(x, y, z, core):
    return (z * SIDE + y, x * PAIR + core)


def step(coord, by):
    return rem(coord + SIDE + by, SIDE)


def announce(devices):
    barrier = pltpu.get_barrier_semaphore()
    for device in devices:
        pl.semaphore_signal(barrier, inc=1, device_id=device, device_id_type=MESH_ID)
    pl.semaphore_wait(barrier, len(devices))


def plan(tasks, latency=2.5):
    free, landed, order, now = {}, {}, [], ZERO
    left = list(tasks)
    while left:
        best = None
        for place, (name, rank, start, needs, after, _, _) in enumerate(left):
            if all(n[0] in landed for n in needs) and all(n in landed for n in after):
                ready = max([start, now] + [landed[task][i] for task, i in needs])
                best = min(best or (ready, rank, place), (ready, rank, place))
        now, _, place = best
        name, _, _, _, _, sends, cost = left.pop(place)
        order.append(name)
        now += cost
        landed[name] = []
        for link, time, *more in sends:
            free[link] = max(now, free.get(link, ZERO)) + time
            landed[name].append(free[link] + latency + sum(more))
    return order


def layers_order(rows_i, cols_i, rows_o, cols_o, seq, starts):
    rate = 23300.0
    tasks = []
    for m in range(SIDE):
        is_in = m % PAIR == 0
        edge = cols_i // LANE * SIDE // 9 // PAIR * WIDE
        size = {"y": rows_i // SIDE * edge, "x": rows_i * (cols_i - PAIR * edge)} if is_in else {"y": rows_o // SIDE * cols_o // PAIR}
        size["z"] = size["y"]
        colors = "yzx" if is_in else "yz"
        tasks.append((("lend", m), 5, 3.0 + SIDE * m, [], [], [("chip", (rows_i * cols_i if is_in else rows_o * cols_o) / 150000.0)], QUICK))
        for color in colors:
            cost = size[color] / rate
            both = [(("x", by), cost) for by in BOTH]
            spread = [((color, by), cost) for by in BOTH] if color != "x" else []
            tasks.append((("reach", m, color), m, starts[m], [], [], both, QUICK))
            for i, by in enumerate(BOTH):
                tasks.append((("relay", m, color, by), m, ZERO, [(("reach", m, color), i)], [], [(("x", by), cost / PAIR)] + spread, QUICK))
            halves = [(("relay", m, color, by), 0) for by in BOTH]
            tasks.append((("far", m, color), m, ZERO, halves, [], spread, QUICK))
            if color == "x":
                continue
            for off, source, first in ((-1, ("relay", m, color, 1), 1), (1, ("relay", m, color, -1), 1), (PAIR, ("far", m, color), 0)):
                for i, by in enumerate(BOTH):
                    tasks.append((("pass", m, color, off, by), m, ZERO, [(source, first + i)], [], [((color, by), cost / PAIR)], QUICK))
                halves = [(("pass", m, color, off, by), 0) for by in BOTH]
                tasks.append((("close", m, color, off), m, ZERO, halves, [], [], QUICK))
        for off in (-1, 1, PAIR):
            last = [("close", m, color, off) for color in "yz"]
            if is_in:
                last.append(("far", m, "x") if off == PAIR else ("relay", m, "x", -off))
            tasks.append((("hand", m, off), m, ZERO, [], last, [("chip", (rows_i * cols_i if is_in else rows_o * cols_o) / 150000.0)], QUICK))
    before = []

    def work(name, cost, mats=()):
        needs = [(("hand", m, off), 0) for m in mats for off in (-1, 1, PAIR)] + [(("lend", m), 0) for m in mats]
        tasks.append((name, 99, ZERO, needs, list(before), [], cost))
        before[:] = [name]

    for l in range(PAIR):
        work(("norm", l), 0.8)
        work(("project", l), 4.0, [PAIR * l])
        work(("attend", l), 4.2)
        work(("mlp", l), 2.2)
        work(("put", l), 1.6, [PAIR * l + 1])
    for l in (1, 0):
        work(("back_out", l), 2.9)
        work(("back_mlp", l), 2.0)
        work(("back_heads", l), 1.0)
        work(("back_quad", l), 6.0)
        work(("back_keys", l), QUICK)
        for i in range(PAIR):
            work(("back_in", l, i), 1.3 + 0.6 * i)
        work(("back_norm", l), 1.0)
    def send(name, rank, start, after, sends):
        tasks.append((name, rank, start, [], [after] if after else [], sends, 0.4))

    def follow(name, rank, needs, sends):
        tasks.append((name, rank, ZERO, needs, [], sends, QUICK))

    def both(axis, size):
        return [((axis, by), size / rate, margin) for by in BOTH]

    model, margin = rows_i * ROW, 2.0
    for l in (1, 0):
        for axis in "yz":
            send(("send_h", l, axis), 20 - l, 58.0, ("norm", l), both(axis, seq * model) + both(axis, seq * model))
        send(("send_m", l), 22 - l, ZERO, ("mlp", l), both("x", PAIR * seq * rows_o) + both("x", PAIR * seq * rows_o))
        if l == 0:
            send(("own_y",), 15, ZERO, ("back_norm", 1), [])
            send(("send_scale", l), 15, ZERO, ("back_norm", l), [])
            continue
        name = ("send_y", l)
        send(name, 12, 42.0, None, both("x", seq * model))
        for i, by in enumerate(BOTH):
            follow(("pass_y", l, by), 12, [(name, i)], [(("x", by), seq * model / PAIR / rate, margin)])
        follow(("far_y", l), 12, [(("pass_y", l, by), 0) for by in BOTH], [])
        for axis in "zy":
            name = ("send_z", l, axis)
            share = seq * (cols_i + LANE) / ROW
            send(name, 13, ZERO, ("back_mlp", l), both(axis, share / PAIR) + both(axis, share))
            if axis == "y":
                name = ("rest_z", l)
                send(name, 13, ZERO, ("back_keys", l), both(axis, share / ROW) + both(axis, share / SIDE))
            for i, by in enumerate(BOTH):
                follow(("pass_z", l, axis, by), 13, [(name, i)], [((axis, by), share / PAIR / rate, margin)])
                follow(("twin_z", l, axis, by), 14, [(name, PAIR + i)], [])
            follow(("far_z", l, axis), 14, [(("pass_z", l, axis, by), 0) for by in BOTH], [])
        send(("send_scale", l), 15, ZERO, ("back_norm", l), [])
    send(("own_z",), 15, ZERO, ("back_keys", 0), [])
    return plan(tasks)


def gather_stages(links, position, shard_i, shard_o, wi, wo, lsem):
    x, y, z, core = position
    twin = device_at(x, y, z, 1 - core)
    rows_i, cols_i = shard_i.shape[1:]
    rows_o, cols_o = shard_o.shape[1:]
    quarter_i, quarter_o = rows_i // SIDE, rows_o // SIDE
    third_i = cols_i // LANE * SIDE // 9 // PAIR * WIDE
    half_o = cols_o // PAIR
    cut_o = quarter_o // 16 * ROW + ROW if quarter_o % 16 else quarter_o // PAIR
    place = {"x": x, "y": y, "z": z}

    spots = {(axis, o): step(place[axis], o) for axis in "xyz" for o in range(SIDE)}

    def spot(axis, o):
        return spots[axis, o % SIDE]

    table = {}
    for axis in "xyz":
        for o in range(1, SIDE):
            moved = {**place, axis: spot(axis, o)}
            table[axis, o] = device_at(moved["x"], moved["y"], moved["z"], core)

    def peer(axis, o):
        return table[axis, o % SIDE]

    mats = []
    for l in range(PAIR):
        mats.append((shard_i.at[l], wi.at[l], rows_i, True))
        mats.append((shard_o.at[l], wo.at[l], rows_o, False))

    def region(is_in, color, q):
        if is_in:
            if color == "x":
                lo, hi = PAIR * third_i, cols_i
                rows = (0, rows_i)
            else:
                lo, hi = (0, third_i) if color == "y" else (third_i, PAIR * third_i)
                rows = (q * quarter_i, quarter_i)
            mid = lo + ((hi - lo) // LANE + 1) // PAIR * LANE
            return (rows, (lo, hi - lo)), (rows, (lo, mid - lo)), (rows, (mid, hi - mid))
        cols = (0, half_o) if color == "y" else (half_o, half_o)
        start = q * quarter_o
        return ((start, quarter_o), cols), ((start, cut_o), cols), ((start + cut_o, quarter_o - cut_o), cols)

    def at(m, xb, area):
        (r, nr), (c, nc) = area
        _, out, size, _ = mats[m]
        return out.at[pl.ds(pl.multiple_of((PAIR * xb + core) * size + r, ROW), nr), pl.ds(c, nc)]

    def block(m, xb, index):
        _, out, size, _ = mats[m]
        return out.at[pl.ds(pl.multiple_of((PAIR * xb + index) * size, BAND), size)]

    def group(m, color):
        _, out, _, is_in = mats[m]
        (_, nr), (c, nc) = region(is_in, color, 0)[0]
        return dict(batch=(m, color), whole=out.at[pl.ds(0, nr * (TRIO if color == "x" else 12)), pl.ds(c, nc)])

    def reach(m, color):
        src, _, _, is_in = mats[m]
        area = region(is_in, color, place[color])[0]
        for by in BOTH:
            links.send((m, "x1", color, by), src.at[pl.ds(pl.multiple_of(area[0][0], ROW), area[0][1]), pl.ds(*area[1])], at(m, x, area), peer("x", by), **group(m, color))

    def launch(m, color, off):
        is_in = mats[m][TRIO]
        moved = at(m, spot("x", off), region(is_in, color, place[color])[0])
        for by in BOTH:
            links.send((m, "p1", color, off, by), moved, moved, peer(color, by), **group(m, color))

    def relay(m, color, by):
        is_in = mats[m][TRIO]
        xb = spot("x", -by)
        areas = region(is_in, color, place[color])
        links.arrive((m, "x1", color, by), at(m, xb, areas[0]))
        part = at(m, xb, areas[1] if by == 1 else areas[PAIR])
        links.send((m, "x2", color), part, part, peer("x", by), **group(m, color))
        if color != "x":
            launch(m, color, -by)

    def far(m, color):
        is_in = mats[m][TRIO]
        links.arrive((m, "x2", color), at(m, spot("x", PAIR), region(is_in, color, place[color])[0]))
        if color != "x":
            launch(m, color, PAIR)

    def pass_on(m, color, off, by):
        is_in = mats[m][TRIO]
        xb = spot("x", off)
        areas = region(is_in, color, spot(color, -by))
        links.arrive((m, "p1", color, off, by), at(m, xb, areas[0]))
        part = at(m, xb, areas[1] if by == 1 else areas[PAIR])
        links.send((m, "p2", color, off), part, part, peer(color, by), **group(m, color))

    def close(m, color, off):
        is_in = mats[m][TRIO]
        links.arrive((m, "p2", color, off), at(m, spot("x", off), region(is_in, color, spot(color, PAIR))[0]))

    def four(m):
        _, out, size, _ = mats[m]
        return out.at[pl.ds(0, SIDE * size)]

    def give(m, src, dst):
        links.send((m, "chip"), src, dst, twin, batch=(m, "chip"), whole=four(m))

    def hand(m, off):
        whole = block(m, spot("x", off), core)
        give(m, whole, whole)

    owns = []

    def begin():
        for m, (src, _, _, _) in enumerate(mats):
            copy = pltpu.make_async_copy(src, block(m, x, core), lsem.at[m])
            copy.start()
            owns.append(copy)

    def lend(m):
        give(m, mats[m][0], block(m, x, core))

    def ready(m):
        owns[m].wait()
        links.arrive((m, "chip"), four(m))

    return begin, ready, peer, {"reach": reach, "relay": relay, "far": far, "pass": pass_on, "close": close, "hand": hand, "lend": lend}


BF, F32 = jnp.bfloat16, jnp.float32


def product(a, b, contract=((1,), (0,))):
    return lax.dot_general(a, b, (contract, ((), ())), preferred_element_type=F32)


def lanes(start, size):
    return pl.ds(start if isinstance(start, int) else pl.multiple_of(start, LANE), size)


def layers_kernel(order, sc_ref, wi_ref, wo_ref, x_ref, dy_ref, freq_ref,
                  y_ref, gx_ref, hy_a, hy_b, hz_a, hz_b, mx_a, mx_b, yx_b, zy_b, zz_b, z_a, dy_a, sc_out, relay_z,
                  wi, wo, z, om, h, hid, qr, kts, vsl, ksl, turned_q, turned_o, scores, dscores, pcat, dscat, cos_ref, sin_ref, turn_ref,
                  dot_heads, qt, dht, dkv, omt, ht, dyt, sc, gains, own_gain, gain_ref, load_sems, own_sems, send_sems, recv_sems,
                  share_send_sems, share_recv_sems):
    seq, dim = x_ref.shape
    ff = (wi.shape[PAIR] - dim - LANE) // PAIR
    position = chip_position()
    x, y, zc, core = position
    twin = device_at(x, y, zc, 1 - core)
    me = PAIR * x + core
    links, shared = Links(send_sems, recv_sems), Links(share_send_sems, share_recv_sems)
    stored = []
    spots, _ = around(position)
    h_out, m_out, y_out, z_out = {"y": (hy_a, hy_b), "z": (hz_a, hz_b)}, (mx_a, mx_b), {1: yx_b}, {(1, "y"): zy_b, (1, "z"): zz_b}
    middle = hid.at[1]
    begin, ready, peer, stages = gather_stages(links, position, wi_ref, wo_ref, wi, wo, load_sems)
    others = [(zc * SIDE + y, rem(me + k, ROW)) for k in range(1, ROW)]

    def spot(axis, o):
        return spots[axis, o % SIDE]

    def device(axis, o, index):
        moved = {"x": x, "y": y, "z": zc, axis: spot(axis, o)}
        return device_at(moved["x"], moved["y"], moved["z"], index)

    own_gain[ALL] = jnp.zeros(own_gain.shape, F32)
    count = sc_ref.shape[1]
    for f in range(ROW):
        @pl.when(me == f)
        def _():
            own_gain[0:PAIR, f * count:(f + 1) * count] = sc_ref[ALL].astype(F32)
    announce(others + [device(axis, o, index) for axis in "yz" for o in AROUND for index in range(PAIR)])
    begin()
    for k, far in enumerate(others):
        links.send(("sc",), own_gain, gains.at[me], far, batch=("sc",), whole=gains.at[pl.ds(0, OTHERS)])

    def keep(src, dst):
        copy = pltpu.make_async_copy(src, dst, own_sems.at[len(stored)])
        copy.start()
        stored.append(copy)

    def tokens(axis, o, index):
        return pl.ds(pl.multiple_of((PAIR * spot(axis, o) + index) * seq, seq), seq)

    def place(axis, o, index):
        return PAIR * spot(axis, o) + index

    def columns(axis, o):
        size = z.shape[PAIR] // ROW
        return lanes(((0 if axis == "y" else SIDE) + spot(axis, o)) * size, size)

    def several(batch, ref, n):
        whole = ref.at[pl.ds(0, n * seq if batch[0][0] in "yz" else n)]
        return dict(batch=batch, whole=whole)

    def send_h(l, axis):
        out, batch = h_out[axis][l].at[place(axis, 0, core)], several(("h", l, axis), h_out[axis][l], OTHERS)
        for o in AROUND:
            for index in range(PAIR):
                shared.send(("h", l, axis), ht.at[l, :, index], out, device(axis, o, index), **batch)
        shared.send(("h", l, axis), ht.at[l, :, 1 - core], out, twin, **batch)
        keep(ht.at[l, :, core], out)

    def arrive_h(l):
        for axis in "yz":
            shared.arrive(("h", l, axis), h_out[axis][l].at[pl.ds(0, OTHERS)])

    def row_block(l, o, index):
        size = omt.shape[1] // ROW
        return omt.at[l, pl.ds(pl.multiple_of((PAIR * spot("x", o) + index) * size, BAND), size)]

    def send_m(l):
        out, batch = m_out[l].at[place("x", 0, core)], several(("m", l), m_out[l], OTHERS)
        for o in AROUND:
            for index in range(PAIR):
                shared.send(("m", l), row_block(l, o, index), out, device("x", o, index), **batch)
        shared.send(("m", l), row_block(l, 0, 1 - core), out, twin, **batch)
        keep(row_block(l, 0, core), out)

    def arrive_m(l):
        shared.arrive(("m", l), m_out[l].at[pl.ds(0, OTHERS)])

    def token_half(axis, o, k):
        return pl.ds(pl.multiple_of((PAIR * spot(axis, o) + core) * seq + k * (seq // PAIR), seq // PAIR), seq // PAIR)

    def send_y(l):
        src, out = dy_ref, y_out[l].at[tokens("x", 0, core)]
        for by in BOTH:
            shared.send(("y", l, by), src, out, device("x", by, core), **several(("y", l), y_out[l], OTHERS))
        shared.send(("y", l), src, out, twin, **several(("y", l), y_out[l], OTHERS))
        keep(src, out)

    def pass_y(l, by):
        landed, part = y_out[l].at[tokens("x", -by, core)], y_out[l].at[token_half("x", -by, (1 - by) // PAIR)]
        shared.arrive(("y", l, by), landed)
        shared.send(("y2", l), part, part, device("x", by, core), **several(("y", l), y_out[l], OTHERS))
        shared.send(("y", l), landed, landed, twin, **several(("y", l), y_out[l], OTHERS))

    def far_y(l):
        landed = y_out[l].at[tokens("x", PAIR, core)]
        shared.arrive(("y2", l), landed)
        shared.send(("y", l), landed, landed, twin, **several(("y", l), y_out[l], OTHERS))

    def arrive_y(l):
        shared.arrive(("y", l), y_out[l].at[pl.ds(0, SIDE * seq)])

    def push_z(l, axis, o, ready):
        out = z_out[l, axis].at[tokens(axis, 0, core)]
        batch = several(("z", l, axis), z_out[l, axis], ROW)

        def start():
            if o != PAIR:
                shared.send(("z", l, axis, o), z.at[l, :, columns(axis, o)], out, device(axis, o, core), **batch)
                return
            for k, by in enumerate(BOTH):
                shared.send(("zr", l, axis, by), z.at[l, pl.ds(k * (seq // PAIR), seq // PAIR), columns(axis, PAIR)], relay_z.at[l, "yz".index(axis), k],
                            device(axis, by, core), **batch)

        if ready is None:
            start()
        else:
            pl.when(ready)(start)

    def own_part(l, axis):
        out, mine = z_out[l, axis].at[tokens(axis, 0, core)], z.at[l, :, columns(axis, 0)]
        shared.send(("z", l, axis), mine, out, twin, **several(("z", l, axis), z_out[l, axis], ROW))
        keep(mine, out)

    def send_z(l, axis):
        for o in (PAIR, 1, -1):
            push_z(l, axis, o, spot(axis, o) != 0 if axis == "y" else None)
        if axis == "z":
            own_part(l, axis)

    def rest_z(l):
        for o in (PAIR, 1, -1):
            push_z(l, "y", o, spot("y", o) == 0)
        own_part(l, "y")

    def pass_z(l, axis, by):
        k = (1 - by) // PAIR
        half = relay_z.at[l, "yz".index(axis), k]
        shared.arrive(("zr", l, axis, by), half)
        shared.send(("z2", l, axis), half, z_out[l, axis].at[token_half(axis, -by, k)], device(axis, by, core), **several(("z", l, axis), z_out[l, axis], ROW))

    def twin_z(l, axis, by):
        landed = z_out[l, axis].at[tokens(axis, -by, core)]
        shared.arrive(("z", l, axis, by), landed)
        shared.send(("z", l, axis), landed, landed, twin, **several(("z", l, axis), z_out[l, axis], ROW))

    def far_z(l, axis):
        landed = z_out[l, axis].at[tokens(axis, PAIR, core)]
        shared.arrive(("z2", l, axis), landed)
        shared.send(("z", l, axis), landed, landed, twin, **several(("z", l, axis), z_out[l, axis], ROW))

    def arrive_z(l, axis):
        shared.arrive(("z", l, axis), z_out[l, axis].at[pl.ds(0, SIDE * seq)])

    def send_scale(l):
        for far in others:
            shared.send(("scale", l), sc.at[l], sc_out.at[l, me], far, batch=("scale", l), whole=sc_out.at[l, pl.ds(0, OTHERS)])
        keep(sc.at[l], sc_out.at[l, me])

    def arrive_scale(l):
        shared.arrive(("scale", l), sc_out.at[l, pl.ds(0, OTHERS)])

    gains[me] = own_gain[ALL]
    z[:, :, wi.shape[PAIR]:] = jnp.zeros((PAIR, seq, z.shape[PAIR] - wi.shape[PAIR]), BF)
    entry = (x_ref, hid.at[0])
    angle = lax.broadcasted_iota(jnp.int32, (seq, LANE), 0).astype(F32) * freq_ref[0:1]
    for half in range(PAIR):
        cos_ref[:, LANE * half:LANE * (half + 1)] = jnp.cos(angle)
        sin_ref[:, LANE * half:LANE * (half + 1)] = jnp.sin(angle)
    lane = lax.broadcasted_iota(jnp.int32, turn_ref.shape, 1)
    down = lax.broadcasted_iota(jnp.int32, turn_ref.shape, 0) - lane
    low = rem(lane, HEAD) < BAND
    turn_ref[ALL] = jnp.where(low & (down == BAND), -1.0, jnp.where(jnp.logical_not(low) & (down == -BAND), 1.0, ZERO)).astype(BF)
    kts[ALL] = jnp.zeros(kts.shape, BF)
    pcat[ALL] = jnp.zeros(pcat.shape, BF)
    dscat[ALL] = jnp.zeros(dscat.shape, BF)

    def normalise(l, src):
        @pl.loop(0, seq // BAND, unroll=SIDE)
        def _(r):
            rows = pl.ds(pl.multiple_of(r * BAND, BAND), BAND)
            v = src[rows].astype(F32)
            v = v - jnp.mean(v, axis=-1, keepdims=True)
            var = jnp.mean(v * v, axis=-1, keepdims=True)
            h[l, rows] = (v * lax.rsqrt(var + 1e-6) * gain_ref[l:l + 1]).astype(BF)

    def project(l):
        strip = wi.shape[PAIR] // 5

        @pl.loop(0, 5)
        def _(i):
            at = lanes(i * strip, strip)
            z[l, :, at] = product(h[l], wi[l, :, at]).astype(BF)

    def heads(l):
        cos, sin = cos_ref[ALL], sin_ref[ALL]
        for g in range(dim // WIDE):
            q = z[l, :, g * WIDE:(g + 1) * WIDE]
            qr[l, :, g * WIDE:(g + 1) * WIDE] = ((q.astype(F32) * cos + product(q, turn_ref[ALL]) * sin) * 0.125).astype(BF)
        kv = z[l, :, dim:dim + LANE]
        turned = kv.astype(F32) * cos[:, :LANE] + product(kv, turn_ref[:LANE, :LANE]) * sin[:, :LANE]
        first = lax.broadcasted_iota(jnp.int32, turned.shape, 1) < HEAD
        key_lo = jnp.where(first, turned, ZERO)
        val_hi = jnp.where(first, ZERO, kv.astype(F32))
        return key_lo, pltpu.roll(key_lo, HEAD, 1), pltpu.roll(val_hi, HEAD, 1), val_hi

    def slot_rows(ref, lo, hi):
        zero = jnp.zeros((seq, LANE), BF)
        lo, hi = lo.astype(BF), hi.astype(BF)
        for i, (left, right) in enumerate(((lo, zero), (hi, zero), (zero, lo), (zero, hi))):
            ref[i * seq:(i + 1) * seq, :LANE] = left
            ref[i * seq:(i + 1) * seq, LANE:] = right

    def slot_cols(ref, lo):
        flat = lo.T[:HEAD].astype(BF)
        for i in range(SIDE):
            ref[HEAD * i:HEAD * (i + 1), i * seq:(i + 1) * seq] = flat

    def chances(i, half):
        at = slice(LANE * half, LANE * (half + 1))
        blocks = [pl.ds(pl.multiple_of(i * seq + LANE * k, LANE), LANE) for k in range(half + 1)]
        s = [scores[keys, at] for keys in blocks]
        lower = lax.broadcasted_iota(jnp.int32, s[-1].shape, 1) >= lax.broadcasted_iota(jnp.int32, s[-1].shape, 0)
        s[-1] = jnp.where(lower, s[-1], -1e30)
        top = functools.reduce(jnp.maximum, [jnp.max(v, axis=0, keepdims=True) for v in s])
        e = [jnp.exp(v - top) for v in s]
        scale = 1.0 / sum(jnp.sum(v, axis=0, keepdims=True) for v in e)
        return at, [(keys, v * scale) for keys, v in zip(blocks, e)]

    def attend(l):
        key_lo, key_hi, val_lo, _ = heads(l)
        slot_rows(ksl, key_lo, key_hi)
        slot_cols(kts, val_lo)
        flip(lambda at: qr[l, :, lanes(at, WIDE)], qt, dim)

        @pl.loop(0, dim // WIDE)
        def _(g):
            rows = pl.ds(pl.multiple_of(g * WIDE, WIDE), WIDE)
            scores[ALL] = product(ksl[ALL], qt[rows])

            @pl.loop(0, SIDE)
            def _(i):
                for half in range(PAIR):
                    at, blocks = chances(i, half)
                    for keys, p in blocks:
                        pcat[keys, at] = p.astype(BF)
            flat = product(kts[ALL], pcat[ALL]).astype(BF)
            omt[l, rows] = flat
            om[:, lanes(g * WIDE, WIDE)] = flat.T

    def mlp(l):
        @pl.loop(0, seq // BAND)
        def _(r):
            rows = pl.ds(pl.multiple_of(r * BAND, BAND), BAND)

            @pl.loop(0, ff // STRIP)
            def _(i):
                gate = z[l, rows, lanes(dim + LANE + i * STRIP, STRIP)].astype(F32)
                up = z[l, rows, lanes(dim + LANE + ff + i * STRIP, STRIP)].astype(F32)
                om[rows, lanes(dim + i * STRIP, STRIP)] = (gate * jax.nn.sigmoid(gate) * up).astype(BF)

    def put_out(l, dst):
        for n in range(dim // WIDE):
            cols = slice(n * WIDE, (n + 1) * WIDE)
            total = product(om[ALL], wo[l, :, cols])
            dst[:, cols] = (entry[l][:, cols].astype(F32) + total).astype(BF)

    def flip(src, dst, width, first=0):
        @pl.loop(first // WIDE, width // WIDE)
        def _(i):
            dst[pl.ds(pl.multiple_of(i * WIDE, WIDE), WIDE)] = src(i * WIDE).T

    upstream = (middle, dy_ref)

    def back_out(l):
        dy = upstream[l]
        flip(lambda at: dy[:, lanes(at, WIDE)], dyt, dim)

        @pl.loop(0, wo.shape[1] // dim)
        def _(n):
            rows = pl.ds(pl.multiple_of(n * dim, dim), dim)
            part = product(wo[l, rows], dyt[ALL]).astype(BF)
            om[:, lanes(n * dim, dim)] = part.T

            @pl.when(n == 0)
            def _():
                dot_heads[ALL] = part

    def back_mlp(l):
        @pl.loop(0, seq // BAND)
        def _(r):
            rows = pl.ds(pl.multiple_of(r * BAND, BAND), BAND)

            @pl.loop(0, ff // STRIP)
            def _(i):
                gate_at, up_at = lanes(dim + LANE + i * STRIP, STRIP), lanes(dim + LANE + ff + i * STRIP, STRIP)
                gate, up = z[l, rows, gate_at].astype(F32), z[l, rows, up_at].astype(F32)
                d = om[rows, lanes(dim + i * STRIP, STRIP)].astype(F32)
                sig = jax.nn.sigmoid(gate)
                du = d * up
                z[l, rows, gate_at] = (du * sig + du * gate * (sig * (1.0 - sig))).astype(BF)
                z[l, rows, up_at] = (d * (gate * sig)).astype(BF)

    def back_heads(l):
        key_lo, key_hi, val_lo, val_hi = heads(l)
        slot_rows(ksl, key_lo, key_hi)
        slot_rows(vsl, val_lo, val_hi)
        slot_cols(kts, key_lo)
        dkv[ALL] = jnp.zeros(dkv.shape, F32)
        flip(lambda at: qr[l, :, lanes(at, WIDE)], qt, dim)
        for at in range(0, dim, LANE):
            pair = slice(at, at + LANE)
            turned_q[:, pair] = pltpu.roll(qr[l, :, pair].astype(F32), HEAD, 1).astype(BF)
            turned_o[:, pair] = pltpu.roll(om[:, pair].astype(F32), HEAD, 1).astype(BF)

    def back_quad(l):
        @pl.loop(0, dim // WIDE)
        def _(g):
            quad(l, g)

    def quad(l, g):
        cols = pl.ds(pl.multiple_of(g * WIDE, WIDE), WIDE)
        scores[ALL] = product(ksl[ALL], qt[cols])
        dscores[ALL] = product(vsl[ALL], dot_heads[cols])

        @pl.loop(0, SIDE)
        def _(i):
            for half in range(PAIR):
                at, blocks = chances(i, half)
                given = [p * dscores[keys, at].astype(BF).astype(F32) for keys, p in blocks]
                total = sum(jnp.sum(v, axis=0, keepdims=True) for v in given)
                for (keys, p), v in zip(blocks, given):
                    pcat[keys, at] = p.astype(BF)
                    dscat[keys, at] = (v - p * total).astype(BF)
        dq = product(kts[ALL], dscat[ALL]).astype(BF).T
        back = dq.astype(F32) * cos_ref[ALL] - product(dq, turn_ref[ALL]) * sin_ref[ALL]
        z[l, :, cols] = (back * 0.125).astype(BF)
        def pieces(left, even, odd):
            for i in range(SIDE):
                pair = lanes(g * WIDE + i // PAIR * LANE, LANE)
                yield product(left[i * seq:(i + 1) * seq, :], odd(pair) if i % PAIR else even(pair))

        dkv[0] += sum(pieces(dscat, lambda at: qr[l, :, at], lambda at: turned_q[:, at]))
        dkv[1] += sum(pieces(pcat, lambda at: turned_o[:, at], lambda at: om[:, at]))

    def back_keys(l):
        dk = dkv[0].astype(BF)
        turned = dk.astype(F32) * cos_ref[:, :LANE] - product(dk, turn_ref[:LANE, :LANE]) * sin_ref[:, :LANE]
        first = lax.broadcasted_iota(jnp.int32, turned.shape, 1) < HEAD
        z[l, :, dim:dim + LANE] = jnp.where(first, turned, dkv[1]).astype(BF)

    def back_in(l, half):
        width = wi.shape[PAIR] // 5
        at = slice(PAIR * half * width, (PAIR + TRIO * half) * width)
        part = product(wi[l, :, at], z[l, :, at], ((1,), (1,)))
        dht[ALL] = dht[ALL] + part if half else part

    def back_norm(l):
        dy, dst = upstream[l], (gx_ref, middle)[l]
        for i in range(dim // WIDE):
            cols = slice(i * WIDE, (i + 1) * WIDE)
            h[l, :, cols] = dht[cols].T.astype(BF)
        sc[l] = jnp.zeros(sc.shape[1:], F32)

        @pl.loop(0, seq // BAND, unroll=SIDE)
        def _(r):
            rows = pl.ds(pl.multiple_of(r * BAND, BAND), BAND)
            v = entry[l][rows].astype(F32)
            v = v - jnp.mean(v, axis=-1, keepdims=True)
            scale = lax.rsqrt(jnp.mean(v * v, axis=-1, keepdims=True) + 1e-6)
            hat = v * scale
            d = h[l, rows].astype(F32)
            each = (d * hat).reshape(SIDE, ROW, dim)
            sc[l] += (each[0] + each[1]) + (each[PAIR] + each[TRIO])
            d = d * gain_ref[l:l + 1]
            d = scale * (d - jnp.mean(d, axis=-1, keepdims=True) - hat * jnp.mean(d * hat, axis=-1, keepdims=True))
            dst[rows] = (dy[rows].astype(F32) + d.astype(BF).astype(F32)).astype(BF)

    def do_norm(l):
        if l == 0:
            links.arrive(("sc",), gains.at[pl.ds(0, OTHERS)])
            gain_ref[ALL] = jnp.sum(gains[ALL], axis=0)
        normalise(l, entry[l])
        for i in range(dim // WIDE):
            flat = h[l, :, i * WIDE:(i + 1) * WIDE].T
            size = ht.shape[TRIO]
            for b in range(ROW):
                lo, hi = max(b * size, i * WIDE), min((b + 1) * size, (i + 1) * WIDE)
                if lo < hi:
                    ht[l, b // PAIR, b % PAIR, lo - b * size:hi - b * size] = flat[lo - i * WIDE:hi - i * WIDE]

    def do_project(l):
        ready(PAIR * l)
        project(l)

    def do_mlp(l):
        mlp(l)
        flip(lambda at: om[:, lanes(at, WIDE)], omt.at[l], om.shape[1], dim)

    def do_put(l):
        ready(PAIR * l + 1)
        put_out(l, hid.at[0] if l == 0 else y_ref)

    stages.update(
        norm=do_norm, project=do_project, attend=attend, mlp=do_mlp, put=do_put, back_out=back_out, back_mlp=back_mlp, back_heads=back_heads,
        back_quad=back_quad, back_keys=back_keys, back_in=back_in, back_norm=back_norm, send_h=send_h, send_m=send_m, send_y=send_y, pass_y=pass_y, far_y=far_y, send_z=send_z, rest_z=rest_z, pass_z=pass_z, twin_z=twin_z, far_z=far_z,
        send_scale=send_scale, own_z=lambda: keep(z.at[0], z_a), own_y=lambda: keep(middle, dy_a))
    for kind, *task in order:
        stages[kind](*task)
    for l in range(PAIR):
        arrive_h(l)
        arrive_m(l)
        arrive_scale(l)
    arrive_y(1)
    for l, axis in z_out:
        arrive_z(l, axis)
    for copy in stored:
        copy.wait()
    shared.drain()
    links.drain()


def run_layers(x, dy, scale, w_in, w_out, freq, starts=(ZERO, 10.0, 20.0, 30.0)):
    seq, dim = x.shape
    proj, cat = w_in.shape[PAIR], ROW * w_out.shape[1]
    wide = proj + LANE
    hbm, vmem = pl.BlockSpec(memory_space=pltpu.HBM), pl.BlockSpec(memory_space=pltpu.VMEM)
    out = lambda *shape, dtype=BF: jax.ShapeDtypeStruct(shape, dtype)
    buffer = lambda *shape, dtype=BF: pltpu.VMEM(shape, dtype)
    sem = pltpu.SemaphoreType.DMA
    line = ROW * seq
    return pl.pallas_call(
        functools.partial(layers_kernel, layers_order(*w_in.shape[1:], *w_out.shape[1:], seq, starts)),
        out_shape=(out(seq, dim), out(seq, dim), *[out(ROW, SIDE, dim // ROW, seq)] * SIDE, *[out(ROW, cat // ROW, seq)] * PAIR, out(line, dim),
                   *[out(line, wide // ROW)] * PAIR, out(seq, wide), out(seq, dim), out(PAIR, ROW, ROW, dim, dtype=F32),
                   out(PAIR, PAIR, PAIR, seq // PAIR, wide // ROW)),
        in_specs=[vmem, hbm, hbm] + [vmem] * TRIO,
        out_specs=[vmem] * PAIR + [hbm] * 13,
        scratch_shapes=[
            buffer(PAIR, dim, proj), buffer(PAIR, cat, dim), buffer(PAIR, seq, wide), buffer(seq, cat), buffer(PAIR, seq, dim),
            buffer(PAIR, seq, dim), buffer(PAIR, seq, dim),
            buffer(WIDE, SIDE * seq), buffer(SIDE * seq, WIDE), buffer(SIDE * seq, WIDE), buffer(seq, dim), buffer(seq, dim),
            buffer(SIDE * seq, seq, dtype=F32), buffer(SIDE * seq, seq, dtype=F32), buffer(SIDE * seq, seq), buffer(SIDE * seq, seq),
            buffer(seq, WIDE, dtype=F32), buffer(seq, WIDE, dtype=F32), buffer(WIDE, WIDE),
            buffer(dim, seq), buffer(dim, seq), buffer(dim, seq, dtype=F32), buffer(PAIR, seq, LANE, dtype=F32),
            buffer(PAIR, cat, seq), buffer(PAIR, SIDE, PAIR, dim // ROW, seq), buffer(dim, seq), buffer(PAIR, ROW, dim, dtype=F32),
            buffer(ROW, ROW, dim, dtype=F32), buffer(ROW, dim, dtype=F32), buffer(ROW, dim, dtype=F32),
            sem((SIDE,)), sem((13,)), sem((15,)), sem((107,)), sem((11,)), sem((24,)),
        ],
        compiler_params=pltpu.CompilerParams(collective_id=PAIR, has_side_effects=True, vmem_limit_bytes=67043328),
        name="run_layers",
    )(scale, w_in, w_out, x, dy, freq)


PARTS = (("i", "x", "z", "y", 0, STRIP), ("i", "x", "z", "y", STRIP, 384), ("i", "x", "y", "z", 0, STRIP), ("i", "x", "y", "z", STRIP, 384),
         ("o", "y", "z", "y", 0, 384), ("o", "z", "y", "z", 384, 384))


def reduce_order(rows, rows_b, starts):
    rate = 11650.0
    tasks = []
    sizes = {"y": WIDE * 896 / (PAIR * rate), "z": WIDE * 896 / (PAIR * rate), "x": WIDE * 768 / (PAIR * rate)}
    for axis in "yzx":
        size = sizes[axis]
        tasks.append((("swap", axis), (0, 0), starts[PAIR] if axis == "x" else starts[TRIO], [], [],
                      [((axis, by), size * n) for by, n in ((-1, 0.5), (1, 1), (-1, 1), (1, 1))], SHORT))
        tasks.append((("relay", axis), (0, 0), ZERO, [(("swap", axis), 0)], [], [((axis, -1), size / PAIR)], SHORT))
        for o, needs in ((1, [(("swap", axis), 1)]), (-1, [(("swap", axis), PAIR)]), (PAIR, [(("swap", axis), TRIO), (("relay", axis), 0)])):
            tasks.append((("near", axis, o), (0, PAIR), ZERO, needs, [], [("chip", 1.6)], QUICK))
    tasks.append((("fetch", 0), (5, 0), ZERO, [], [("make", 1, len(PARTS) - 1)], [], QUICK))
    for l in (1, 0):
        late = 1 - l
        for c, (kind, first, then, last, at, width) in enumerate(PARTS):
            needs, cost = [], 1.6 * width / STRIP
            if l == 0:
                needs = [(("near", last if kind == "i" else "x", o), 0) for o in AROUND]
            tasks.append((("make", l, c), (9 * late, c), starts[late], needs, [] if l else [("fetch", 0)], [], cost))
            full = SIDE * SIDE * (rows if kind == "i" else rows_b) * width / rate
            sends = [[((first, by), full / ROW) for by in BOTH], [((first, by), full / SIDE) for by in BOTH],
                     [((then, o), full / 16) for o in (1, -1, 1)], []]
            piece = full / 16
            sends += [[((then, o), piece) for o in (1, -1, 1)], [((last, by), SIDE * piece) for by in BOTH],
                      [((last, by), PAIR * piece) for by in BOTH], []]
            for s in range(ROW):
                task = ("sum", l, c, s)
                needs = [(("sum", l, c, s - 1), k) for k in range(len(sends[s - 1]))] if s else []
                tasks.append((task, (late, -s), ZERO, needs, [("make", l, c)] if s == 0 else [("sum", l, c, s - 1)], sends[s], SHORT))
    return plan(tasks)


def reduce_kernel(order, *refs):
    hy, hz, mx = refs[0:PAIR], refs[PAIR:SIDE], refs[SIDE:6]
    yx1, zy1, zz1, z0, y0, sc = refs[6:12]
    oa, ob = refs[12:14]
    n = len(PARTS)
    total, half, full, small, front = (refs[14 + k * n:14 + (k + 1) * n] for k in range(5))
    (hbuf, zbuf, mbuf, ybuf, scbuf, rz, ry, ssem, rsem, isem, osem) = refs[14 + 5 * n:]
    position = chip_position()
    x, y, zc, core = position
    place = {"x": x, "y": y, "z": zc}
    twin = device_at(x, y, zc, 1 - core)
    spots, peers = around(position)

    def spot(axis, o):
        return spots[axis, o % SIDE]

    def peer(axis, o):
        return peers[axis, o % SIDE]

    seq, wide = z0.shape
    own = wide // ROW
    loads, moving = {}, []

    def load(key, src, dst):
        copy = pltpu.make_async_copy(src, dst, isem.at[len(moving)])
        moving.append(key)
        copy.start()
        loads[key] = copy

    def fetch(l):
        if l:
            load(("z", 1, "y"), zy1, zbuf.at[1, 0])
        load(("h", l, "y"), hy[l], hbuf.at[l, 0])
        if l:
            load(("z", 1, "z"), zz1, zbuf.at[1, 1])
        load(("h", l, "z"), hz[l], hbuf.at[l, 1])
        load(("m", l), mx[l], mbuf.at[l])
        if l:
            load(("y", 1), yx1, ybuf.at[1])
        load(("s", l), sc.at[l], scbuf.at[l])

    fetch(1)
    done = set()

    def loaded(*keys):
        for key in keys:
            if key not in done:
                loads[key].wait()
                done.add(key)

    announce([peer(axis, o) for axis in "xyz" for o in AROUND] + [twin])
    links = Links(ssem, rsem)

    def columns(axis, o):
        return lanes(((0 if axis == "y" else SIDE) + spot(axis, o)) * own, own)

    def tokens(axis, o, index):
        return pl.ds(pl.multiple_of((PAIR * spot(axis, o) + index) * seq, seq), seq)

    def target(axis):
        return ybuf.at[0] if axis == "x" else zbuf.at[0, "yz".index(axis)]

    def leaving(axis):
        return dict(batch=("swap", axis), whole=target(axis).at[pl.ds(0, OTHERS * seq + seq // PAIR)])

    def half_at(axis, o, k):
        start = (PAIR * spot(axis, o) + core) * seq + k * (seq // PAIR)
        return target(axis).at[pl.ds(pl.multiple_of(start, seq // PAIR), seq // PAIR)]

    def relay_of(axis):
        return ry if axis == "x" else rz.at["yz".index(axis)]

    def swap(axis):
        def part(o, rows=slice(None)):
            return y0.at[rows] if axis == "x" else z0.at[rows, columns(axis, o)]

        mine = target(axis).at[tokens(axis, 0, core)]
        links.send(("relay", axis), part(PAIR, pl.ds(seq // PAIR, seq // PAIR)), relay_of(axis), peer(axis, -1), **leaving(axis))
        for by in BOTH:
            links.send(("swap", axis, by), part(by), mine, peer(axis, by), **leaving(axis))
        links.send(("swap", axis, PAIR), part(PAIR, pl.ds(0, seq // PAIR)), half_at(axis, 0, 0), peer(axis, PAIR), **leaving(axis))
        links.send(("near", axis), part(0), mine, twin, **leaving(axis))
        load(("own", axis), part(0), mine)

    def relay(axis):
        links.arrive(("relay", axis), relay_of(axis))
        links.send(("relayed", axis), relay_of(axis), half_at(axis, 1, 1), peer(axis, -1), **leaving(axis))

    def near(axis, o):
        landed = target(axis).at[tokens(axis, -o, core)]
        if o == PAIR:
            links.arrive(("swap", axis, PAIR), half_at(axis, PAIR, 0))
            links.arrive(("relayed", axis), half_at(axis, PAIR, 1))
        else:
            links.arrive(("swap", axis, o), landed)
        links.send(("near", axis), landed, landed, twin, **leaving(axis))

    def joined(axis):
        if axis not in done:
            done.add(axis)
            loaded(("own", axis))
            links.arrive(("near", axis), target(axis).at[pl.ds(0, SIDE * seq)])

    def joined_lanes(ref, l, i):
        return jnp.concatenate([ref[l, i, k].reshape(-1, ref.shape[-1]) for k in range(ROW)], axis=1)

    def make(l, c):
        kind, first, then, last, at, width = PARTS[c]
        if kind == "i":
            i = "yz".index(last)
            loaded(("h", l, last))
            if l:
                loaded(("z", l, last))
            else:
                joined(last)
            size = total[c].shape[TRIO]
            for lo in range(0, width, WIDE):
                hi = min(width, lo + WIDE)
                part = product(joined_lanes(hbuf, l, i), zbuf[l, i, :, at + lo:at + hi])
                for r in range(16):
                    total[c][l, r // SIDE, r % SIDE, :, lo:hi] = part[r * size:(r + 1) * size]
            return
        loaded(("m", l), ("s", l))
        if l:
            loaded(("y", l))
        else:
            joined("x")
        part = product(jnp.concatenate([mbuf[l, k] for k in range(ROW)], axis=1), ybuf[l, :, at:at + width])
        size = total[c].shape[TRIO]

        def put(r, value):
            total[c][(l, r // SIDE, r % SIDE) if first == "y" else (l, r % SIDE, r // SIDE)] = value

        for r in range(part.shape[0] // size):
            put(r, part[r * size:(r + 1) * size])
        gain = jnp.sum(jnp.sum(scbuf[l, :, :, at:at + width], axis=0), axis=0, keepdims=True)
        row = lax.broadcasted_iota(jnp.int32, (size, width), 0)
        put(15, jnp.where(row == 0, gain, ZERO))

    def area(l, c, o, whole):
        kind, first, then, last, at, width = PARTS[c]
        inner = (spot(then, whole) if isinstance(whole, int) else whole)
        outer = spot(last, o)
        if kind == "i":
            cols = lanes(((0 if last == "y" else SIDE) + outer) * own + at, width)
            return oa.at[l, inner, :, cols]
        cols = pl.ds(at, width)
        return ob.at[l, outer, inner, :, cols] if last == "y" else ob.at[l, inner, outer, :, cols]

    def add(l, c, s):
        kind, first, then, last, at, width = PARTS[c]
        t = total[c].at[l]
        sums = dict(batch=(l, c, 0), whole=t)
        lines = dict(batch=(l, c, 1), whole=t.at[pl.ds(0, PAIR)])
        singles = dict(batch=(l, c, PAIR), whole=t.at[pl.ds(0, PAIR), pl.ds(0, TRIO)])
        if s == 0:
            far = t.at[spot(first, PAIR)]
            for k, by in enumerate(BOTH):
                links.send((l, c, "half"), far.at[pl.ds(PAIR * k, PAIR)], half[c].at[l, k], peer(first, by), **sums)
        elif s == 1:
            links.arrive((l, c, "half"), half[c].at[l])
            for k, by in enumerate(BOTH):
                mine = t.at[spot(first, by)]
                add_into(mine.at[pl.ds(PAIR * k, PAIR)], half[c].at[l, k])
                links.send((l, c, "full"), mine, full[c].at[l, k], peer(first, by), **sums)
        elif s == PAIR:
            mine = t.at[spot(first, 0)]
            links.arrive((l, c, "full"), full[c].at[l])
            for k in range(PAIR):
                add_into(mine, full[c].at[l, k])
            for k, o in enumerate(AROUND):
                links.send((l, c, "small"), mine.at[spot(then, o)], small[c].at[l, k], peer(then, o), **singles)
        elif s == TRIO:
            links.arrive((l, c, "small"), small[c].at[l])
            mine = t.at[spot(first, 0), spot(then, 0)]
            front[c][l] = (mine[ALL] + small[c][l, 0]) + (small[c][l, 1] + small[c][l, PAIR])
        elif s == SIDE:
            src, dst = front[c].at[l], area(l, c, 0, 0)
            for o in AROUND:
                links.send((l, c, "a1"), src, dst, peer(then, o), **singles)
            copy = pltpu.make_async_copy(src, dst, osem.at[l, c])
            copy.start()
            loads["front", l, c] = copy
        elif s == 5:
            loaded(("front", l, c))
            links.arrive((l, c, "a1"), t.at[0, pl.ds(0, TRIO)])
            line = area(l, c, 0, slice(None))
            for by in BOTH:
                links.send((l, c, "a2"), line, line, peer(last, by), **lines)
        elif s == 6:
            links.arrive((l, c, "a2"), t.at[pl.ds(0, PAIR)])
            for k, by in enumerate(BOTH):
                part = area(l, c, -by, pl.ds(PAIR * k, PAIR))
                links.send((l, c, "a3"), part, part, peer(last, by), **sums)
        else:
            links.arrive((l, c, "a3"), area(l, c, PAIR, slice(None)))

    stages = {"swap": swap, "relay": relay, "near": near, "fetch": fetch, "make": make, "sum": add}
    for kind, *task in order:
        stages[kind](*task)
    links.drain()


def add_into(dst, src):
    @pl.loop(0, dst.shape[0])
    def _(i):
        if len(dst.shape) == SIDE:
            for j in range(dst.shape[1]):
                dst[i, j] += src[i, j]
        else:
            dst[i] += src[i]


def around(position):
    place, core = dict(zip("xyz", position)), position[TRIO]
    spots = {(axis, o): step(place[axis], o) for axis in "xyz" for o in range(SIDE)}
    peers = {}
    for axis in "xyz":
        for o in range(1, SIDE):
            moved = {**place, axis: spots[axis, o]}
            peers[axis, o] = device_at(moved["x"], moved["y"], moved["z"], core)
    return spots, peers


def reduce_gradients(operands, starts=(ZERO, ZERO, 20.0, 3.0)):
    hbm = pl.BlockSpec(memory_space=pltpu.HBM)
    h_rows, m_rows, y_cols, z_cols, z_own, y_own, scale_parts = operands
    part, part_b = h_rows[0].shape[PAIR] // SIDE, (m_rows[0].shape[1] + BAND) // 16
    (line, dim), wide = y_cols.shape, z_own.shape[1]
    out = lambda *shape: jax.ShapeDtypeStruct(shape, F32)
    sem = pltpu.SemaphoreType.DMA

    def buffers(*lead):
        return [pltpu.VMEM((PAIR, *lead, part if e[0] == "i" else part_b, e[5]), F32) for e in PARTS]

    return pl.pallas_call(
        functools.partial(reduce_kernel, reduce_order(part, part_b, starts)),
        out_shape=(out(PAIR, SIDE, part, wide), out(PAIR, SIDE, SIDE, part_b, dim)),
        in_specs=[hbm] * 12,
        out_specs=[hbm] * PAIR,
        scratch_shapes=[
            *buffers(SIDE, SIDE), *buffers(PAIR, PAIR), *buffers(PAIR, SIDE), *buffers(TRIO), *buffers(),
            pltpu.VMEM((PAIR, PAIR, *h_rows[0].shape), BF), pltpu.VMEM((PAIR, PAIR, line, wide // ROW), BF), pltpu.VMEM((PAIR, *m_rows[0].shape), BF),
            pltpu.VMEM((PAIR, line, dim), BF), pltpu.VMEM(scale_parts.shape, F32),
            pltpu.VMEM((PAIR, z_own.shape[0] // PAIR, wide // ROW), BF), pltpu.VMEM((y_own.shape[0] // PAIR, dim), BF),
            sem((39,)), sem((90,)), sem((14,)), sem((PAIR, len(PARTS))),
        ],
        compiler_params=pltpu.CompilerParams(collective_id=1, has_side_effects=True, vmem_limit_bytes=67043328),
        name="reduce_gradients",
    )(*h_rows, *m_rows, y_cols, *z_cols, z_own, y_own, scale_parts)


def finish_kernel(count, in_ref, out_ref, y_ref, gx_ref, in_grad, out_grad, y_out, gx_out, scale_out, in_buf, out_buf, y_buf, gx_buf, came, left):
    moves = [(out_ref.at[l, p], out_buf.at[l, pl.ds(SIDE * p, SIDE)]) for l in range(PAIR) for p in range(SIDE)]
    moves += [(y_ref, y_buf), (gx_ref, gx_buf)]
    size, width = in_buf.shape[PAIR:]
    moves += [(in_ref.at[l, p, :, pl.ds(0, width)], in_buf.at[l, p]) for l in range(PAIR) for p in range(SIDE)]
    loads = [pltpu.make_async_copy(src, dst, came.at[k]) for k, (src, dst) in enumerate(moves)]
    for copy in loads:
        copy.start()
    stores = []

    def store(src, dst):
        copy = pltpu.make_async_copy(src, dst, left.at[len(stores)])
        copy.start()
        stores.append(copy)

    for l in range(PAIR):
        for p in range(SIDE):
            loads[SIDE * l + p].wait()
        store(out_buf.at[l, pl.ds(0, 15)], out_grad.at[l])
    for k, (src, dst) in enumerate(((y_buf, y_out), (gx_buf, gx_out))):
        loads[ROW + k].wait()
        store(src, dst)
    me = lax.axis_index("fsdp")
    for l in range(PAIR):
        for f in range(ROW):
            @pl.when(me == f)
            def _():
                scale_out[l:l + 1] = out_buf[l, 15, 0:1, f * count:(f + 1) * count]
    for l in range(PAIR):
        for p in range(SIDE):
            loads[10 + SIDE * l + p].wait()
            store(in_buf.at[l, p], in_grad.at[l, pl.ds(p * size, size)])
    for copy in stores:
        copy.wait()


def finish(in_sums, out_sums, y, gx, rows, proj):
    hbm = pl.BlockSpec(memory_space=pltpu.HBM)
    out = lambda *shape, dtype=F32: jax.ShapeDtypeStruct(shape, dtype)
    size, (depth, dim) = in_sums.shape[PAIR], out_sums.shape[TRIO:]
    in_grad, out_grad, y_out, gx_out, scale = pl.pallas_call(
        functools.partial(finish_kernel, rows),
        out_shape=(out(PAIR, rows, proj), out(PAIR, 15, depth, dim), out(*y.shape, dtype=BF), out(*gx.shape, dtype=BF), out(PAIR, rows)),
        in_specs=[hbm] * SIDE,
        out_specs=[hbm] * SIDE + [pl.BlockSpec(memory_space=pltpu.VMEM)],
        scratch_shapes=[
            pltpu.VMEM((PAIR, SIDE, size, proj), F32), pltpu.VMEM((PAIR, 16, depth, dim), F32), pltpu.VMEM(y.shape, BF), pltpu.VMEM(gx.shape, BF),
            pltpu.SemaphoreType.DMA((18,)), pltpu.SemaphoreType.DMA((12,)),
        ],
        compiler_params=pltpu.CompilerParams(vmem_limit_bytes=67043328),
        name="finish",
    )(in_sums, out_sums, y, gx)
    return y_out[None], gx_out[None], scale, in_grad, out_grad.reshape(PAIR, 15 * depth, dim)


def solution(mesh):
    fsdp_size = mesh.shape["fsdp"]
    batch_spec = P(("dp", "fsdp"), None, None)
    scale_spec = P(None, "fsdp")
    weight_spec = P(None, "fsdp", None)

    def device_step(x_in, grad_y, norm_scale, w_in, w_out):
        n_layers = w_in.shape[0]
        seq_len, model_dim = x_in.shape[1:]
        proj_dim = w_in.shape[PAIR]
        ff_dim = w_out.shape[1] * fsdp_size - model_dim
        head_dim = (proj_dim - model_dim - PAIR * ff_dim) // PAIR
        rows, rows_out = norm_scale.shape[1], w_out.shape[1]
        half_dim = head_dim // PAIR
        freq = 10000.0 ** (-np.arange(half_dim, dtype=np.float32) * 2.0 / head_dim)
        freq = jnp.asarray(np.tile(freq.astype(np.float32), (ROW, LANE // half_dim)))
        hidden, grad_hidden, *rest = run_layers(x_in[0], grad_y[0], norm_scale, w_in, w_out, freq)
        in_sums, out_sums = reduce_gradients((rest[0:SIDE], rest[SIDE:6], rest[6], rest[OTHERS:9], rest[9], rest[10], rest[11]))
        return finish(in_sums, out_sums, hidden, grad_hidden, rows, proj_dim)

    return jax.shard_map(
        device_step,
        mesh=mesh,
        in_specs=(batch_spec, batch_spec, scale_spec, weight_spec, weight_spec),
        out_specs=(batch_spec, batch_spec, scale_spec, weight_spec, weight_spec),
        check_vma=False,
    )
```

```python
import functools
import jax
import jax.numpy as jnp
import numpy as np
from jax import lax
from jax.experimental import pallas as pl
from jax.experimental.pallas import tpu as pltpu
from jax.sharding import PartitionSpec as P

MESH_ID = pl.DeviceIdType.MESH
BOTH = (1, -1)
AROUND = (1, -1, 2)
PARTS = (True, False)
ALL, ZERO = ..., 0.0
OTHERS = 7
QUICK, SHORT = 0.2, 0.3
LANE, WIDE, STRIP, HEAD = 128, 256, 512, 64
ROW, BAND, SIDE, TRIO, PAIR = 8, 32, 4, 3, 2


class Links:
    def __init__(self, send_sems, recv_sems):
        self.send_sems, self.recv_sems = send_sems, recv_sems
        self.slots, self.batches, self.sent, self.count = {}, {}, {}, 0

    def _landing(self, key, lane):
        if key not in self.slots:
            self.slots[key] = self.count
            self.count += 1 if lane is None else PAIR
        return self.recv_sems.at[self.slots[key] + (0 if lane is None else lane)]

    def send(self, key, src, dst, device, landing=None, whole=None, batch=None, lane=None):
        leaving = self.batches.setdefault(batch or key, len(self.batches))
        copy = pltpu.make_async_remote_copy(
            src_ref=src, dst_ref=dst, send_sem=self.send_sems.at[leaving], recv_sem=self._landing(landing or key, lane),
            device_id=device, device_id_type=MESH_ID)
        copy.start()
        self.sent[batch or key] = (src if whole is None else whole, leaving)

    def arrive(self, key, landed, lane=None):
        pltpu.make_async_copy(landed, landed, self._landing(key, lane)).wait()

    def drain(self):
        for left, leaving in self.sent.values():
            pltpu.make_async_copy(left, left, self.send_sems.at[leaving]).wait()
        self.sent.clear()


def rem(a, n):
    return a % n if isinstance(a, int) else lax.rem(a, n)


def chip_position():
    f, d = lax.axis_index("fsdp"), lax.axis_index("dp")
    return f // PAIR, rem(d, SIDE), d // SIDE, rem(f, PAIR)


def device_at(x, y, z, core):
    return (z * SIDE + y, x * PAIR + core)


def step(coord, by):
    return rem(coord + SIDE + by, SIDE)


def announce(devices):
    barrier = pltpu.get_barrier_semaphore()
    for device in devices:
        pl.semaphore_signal(barrier, inc=1, device_id=device, device_id_type=MESH_ID)
    pl.semaphore_wait(barrier, len(devices))


def plan(tasks, latency=2.5):
    free, landed, order, now = {}, {}, [], ZERO
    left = list(tasks)
    while left:
        best = None
        for place, (name, rank, start, needs, after, _, _) in enumerate(left):
            if all(n[0] in landed for n in needs) and all(n in landed for n in after):
                ready = max([start, now] + [landed[task][i] for task, i in needs])
                best = min(best or (ready, rank, place), (ready, rank, place))
        now, _, place = best
        name, _, _, _, _, sends, cost = left.pop(place)
        order.append(name)
        now += cost
        landed[name] = []
        for link, time, *more in sends:
            free[link] = max(now, free.get(link, ZERO)) + time
            landed[name].append(free[link] + latency + sum(more))
    return order


def layers_order(rows_i, cols_i, rows_o, cols_o, seq, starts):
    rate = 23300.0
    tasks = []
    for m in range(SIDE):
        is_in = m % PAIR == 0
        edge = cols_i // LANE * SIDE // 9 // PAIR * WIDE
        size = {"y": rows_i // SIDE * edge, "x": rows_i * (cols_i - PAIR * edge)} if is_in else {"y": rows_o // SIDE * cols_o // PAIR}
        size["z"] = size["y"]
        colors = "yzx" if is_in else "yz"
        tasks.append((("lend", m), 5, 3.0 + SIDE * m, [], [], [("chip", (rows_i * cols_i if is_in else rows_o * cols_o) / 150000.0)], QUICK))
        for color in colors:
            cost = size[color] / rate
            both = [(("x", by), cost) for by in BOTH]
            spread = [((color, by), cost) for by in BOTH] if color != "x" else []
            tasks.append((("reach", m, color), m, starts[m], [], [], both, QUICK))
            for i, by in enumerate(BOTH):
                tasks.append((("relay", m, color, by), m, ZERO, [(("reach", m, color), i)], [], [(("x", by), cost / PAIR)] + spread, QUICK))
            halves = [(("relay", m, color, by), 0) for by in BOTH]
            tasks.append((("far", m, color), m, ZERO, halves, [], spread, QUICK))
            if color == "x":
                continue
            for off, source, first in ((-1, ("relay", m, color, 1), 1), (1, ("relay", m, color, -1), 1), (PAIR, ("far", m, color), 0)):
                for i, by in enumerate(BOTH):
                    tasks.append((("pass", m, color, off, by), m, ZERO, [(source, first + i)], [], [((color, by), cost / PAIR)], QUICK))
                halves = [(("pass", m, color, off, by), 0) for by in BOTH]
                tasks.append((("close", m, color, off), m, ZERO, halves, [], [], QUICK))
        for off in (-1, 1, PAIR):
            last = [("close", m, color, off) for color in "yz"]
            if is_in:
                last.append(("far", m, "x") if off == PAIR else ("relay", m, "x", -off))
            tasks.append((("hand", m, off), m, ZERO, [], last, [("chip", (rows_i * cols_i if is_in else rows_o * cols_o) / 150000.0)], QUICK))
    before = []

    def work(name, cost, mats=()):
        needs = [(("hand", m, off), 0) for m in mats for off in (-1, 1, PAIR)] + [(("lend", m), 0) for m in mats]
        tasks.append((name, 99, ZERO, needs, list(before), [], cost))
        before[:] = [name]

    for l in range(PAIR):
        work(("norm", l), 0.8)
        work(("project", l), 4.0, [PAIR * l])
        work(("attend", l), 4.2)
        work(("mlp", l), 2.2)
        work(("put", l), 1.6, [PAIR * l + 1])
    for l in (1, 0):
        work(("back_out", l), 2.9)
        work(("back_mlp", l), 2.0)
        work(("back_heads", l), 1.0)
        work(("back_quad", l), 6.0)
        work(("back_keys", l), QUICK)
        for i in range(PAIR):
            work(("back_in", l, i), 1.3 + 0.6 * i)
        work(("back_norm", l), 1.0)
    def send(name, rank, start, after, sends):
        tasks.append((name, rank, start, [], [after] if after else [], sends, 0.4))

    def follow(name, rank, needs, sends):
        tasks.append((name, rank, ZERO, needs, [], sends, QUICK))

    def both(axis, size):
        return [((axis, by), size / rate, margin) for by in BOTH]

    model, margin = rows_i * ROW, 2.0
    for l in (1, 0):
        for axis in "yz":
            send(("send_h", l, axis), 20 - l, 58.0, ("back_keys" if l else "norm", l), both(axis, seq * model) + both(axis, seq * model))
        send(("send_m", l), 22 - l, ZERO, ("mlp", l), both("x", PAIR * seq * rows_o) + both("x", PAIR * seq * rows_o))
        if l == 0:
            send(("own_y",), 15, ZERO, ("back_norm", 1), [])
            send(("send_scale", l), 15, ZERO, ("back_norm", l), [])
            continue
        name = ("send_y", l)
        send(name, 12, 42.0, None, both("x", seq * model))
        for i, by in enumerate(BOTH):
            follow(("pass_y", l, by), 12, [(name, i)], [(("x", by), seq * model / PAIR / rate, margin)])
        follow(("far_y", l), 12, [(("pass_y", l, by), 0) for by in BOTH], [])
        for axis in "zy":
            name = ("send_z", l, axis)
            share = seq * (cols_i + LANE) / ROW
            send(name, 13, ZERO, ("back_mlp", l), both(axis, share / PAIR) + both(axis, share))
            if axis == "y":
                name = ("rest_z", l)
                send(name, 13, ZERO, ("back_keys", l), both(axis, share / ROW) + both(axis, share / SIDE))
            for i, by in enumerate(BOTH):
                follow(("pass_z", l, axis, by), 13, [(name, i)], [((axis, by), share / PAIR / rate, margin)])
                follow(("twin_z", l, axis, by), 14, [(name, PAIR + i)], [])
            follow(("far_z", l, axis), 14, [(("pass_z", l, axis, by), 0) for by in BOTH], [])
        send(("send_scale", l), 15, ZERO, ("back_norm", l), [])
    send(("own_z",), 15, ZERO, ("back_keys", 0), [])
    return plan(tasks)


def gather_stages(links, position, shard_i, shard_o, wi, wo, lsem):
    x, y, z, core = position
    twin = device_at(x, y, z, 1 - core)
    rows_i, cols_i = shard_i.shape[1:]
    rows_o, cols_o = shard_o.shape[1:]
    quarter_i, quarter_o = rows_i // SIDE, rows_o // SIDE
    third_i = cols_i // LANE * SIDE // 9 // PAIR * WIDE
    half_o = cols_o // PAIR
    cut_o = quarter_o // 16 * ROW + ROW if quarter_o % 16 else quarter_o // PAIR
    place = {"x": x, "y": y, "z": z}

    spots = {(axis, o): step(place[axis], o) for axis in "xyz" for o in range(SIDE)}

    def spot(axis, o):
        return spots[axis, o % SIDE]

    table = {}
    for axis in "xyz":
        for o in range(1, SIDE):
            moved = {**place, axis: spot(axis, o)}
            table[axis, o] = device_at(moved["x"], moved["y"], moved["z"], core)

    def peer(axis, o):
        return table[axis, o % SIDE]

    mats = []
    for l in range(PAIR):
        mats.append((shard_i.at[l], wi.at[l], rows_i, True))
        mats.append((shard_o.at[l], wo.at[l], rows_o, False))

    def region(is_in, color, q):
        if is_in:
            if color == "x":
                lo, hi = PAIR * third_i, cols_i
                rows = (0, rows_i)
            else:
                lo, hi = (0, third_i) if color == "y" else (third_i, PAIR * third_i)
                rows = (q * quarter_i, quarter_i)
            mid = lo + ((hi - lo) // LANE + 1) // PAIR * LANE
            return (rows, (lo, hi - lo)), (rows, (lo, mid - lo)), (rows, (mid, hi - mid))
        cols = (0, half_o) if color == "y" else (half_o, half_o)
        start = q * quarter_o
        return ((start, quarter_o), cols), ((start, cut_o), cols), ((start + cut_o, quarter_o - cut_o), cols)

    def at(m, xb, area):
        (r, nr), (c, nc) = area
        _, out, size, _ = mats[m]
        return out.at[pl.ds(pl.multiple_of((PAIR * xb + core) * size + r, ROW), nr), pl.ds(c, nc)]

    def block(m, xb, index):
        _, out, size, _ = mats[m]
        return out.at[pl.ds(pl.multiple_of((PAIR * xb + index) * size, BAND), size)]

    def group(m, color):
        _, out, _, is_in = mats[m]
        (_, nr), (c, nc) = region(is_in, color, 0)[0]
        return dict(batch=(m, color), whole=out.at[pl.ds(0, nr * (TRIO if color == "x" else 12)), pl.ds(c, nc)])

    def reach(m, color):
        src, _, _, is_in = mats[m]
        area = region(is_in, color, place[color])[0]
        for by in BOTH:
            links.send((m, "x1", color, by), src.at[pl.ds(pl.multiple_of(area[0][0], ROW), area[0][1]), pl.ds(*area[1])], at(m, x, area), peer("x", by), **group(m, color))

    def launch(m, color, off):
        is_in = mats[m][TRIO]
        moved = at(m, spot("x", off), region(is_in, color, place[color])[0])
        for by in BOTH:
            links.send((m, "p1", color, off, by), moved, moved, peer(color, by), **group(m, color))

    def relay(m, color, by):
        is_in = mats[m][TRIO]
        xb = spot("x", -by)
        areas = region(is_in, color, place[color])
        links.arrive((m, "x1", color, by), at(m, xb, areas[0]))
        part = at(m, xb, areas[1] if by == 1 else areas[PAIR])
        links.send((m, "x2", color), part, part, peer("x", by), **group(m, color))
        if color != "x":
            launch(m, color, -by)

    def far(m, color):
        is_in = mats[m][TRIO]
        links.arrive((m, "x2", color), at(m, spot("x", PAIR), region(is_in, color, place[color])[0]))
        if color != "x":
            launch(m, color, PAIR)

    def pass_on(m, color, off, by):
        is_in = mats[m][TRIO]
        xb = spot("x", off)
        areas = region(is_in, color, spot(color, -by))
        links.arrive((m, "p1", color, off, by), at(m, xb, areas[0]))
        part = at(m, xb, areas[1] if by == 1 else areas[PAIR])
        links.send((m, "p2", color, off), part, part, peer(color, by), **group(m, color))

    def close(m, color, off):
        is_in = mats[m][TRIO]
        links.arrive((m, "p2", color, off), at(m, spot("x", off), region(is_in, color, spot(color, PAIR))[0]))

    def four(m):
        _, out, size, _ = mats[m]
        return out.at[pl.ds(0, SIDE * size)]

    def give(m, src, dst):
        links.send((m, "chip"), src, dst, twin, batch=(m, "chip"), whole=four(m))

    def hand(m, off):
        whole = block(m, spot("x", off), core)
        give(m, whole, whole)

    owns = []

    def begin():
        for m, (src, _, _, _) in enumerate(mats):
            copy = pltpu.make_async_copy(src, block(m, x, core), lsem.at[m])
            copy.start()
            owns.append(copy)

    def lend(m):
        give(m, mats[m][0], block(m, x, core))

    def ready(m):
        owns[m].wait()
        links.arrive((m, "chip"), four(m))

    return begin, ready, peer, {"reach": reach, "relay": relay, "far": far, "pass": pass_on, "close": close, "hand": hand, "lend": lend}


BF, F32 = jnp.bfloat16, jnp.float32


def product(a, b, contract=((1,), (0,))):
    return lax.dot_general(a, b, (contract, ((), ())), preferred_element_type=F32)


def lanes(start, size):
    return pl.ds(start if isinstance(start, int) else pl.multiple_of(start, LANE), size)


def layers_kernel(order, sc_ref, wi_ref, wo_ref, x_ref, dy_ref, freq_ref,
                  y_ref, gx_ref, hy_a, hy_b, hz_a, hz_b, mx_a, mx_b, yx_b, zy_b, zz_b, z_a, dy_a, sc_out, relay_z,
                  wi, wo, z, om, h, hid, qr, kts, vsl, ksl, turned_q, turned_o, scores, dscores, pcat, dscat, cos_ref, sin_ref, turn_ref,
                  dot_heads, qt, dht, dkv, omt, ht, dyt, sc, gains, own_gain, gain_ref, load_sems, own_sems, send_sems, recv_sems,
                  share_send_sems, share_recv_sems):
    seq, dim = x_ref.shape
    ff = (wi.shape[PAIR] - dim - LANE) // PAIR
    position = chip_position()
    x, y, zc, core = position
    twin = device_at(x, y, zc, 1 - core)
    me = PAIR * x + core
    links, shared = Links(send_sems, recv_sems), Links(share_send_sems, share_recv_sems)
    stored = []
    spots, _ = around(position)
    h_out, m_out, y_out, z_out = {"y": (hy_a, hy_b), "z": (hz_a, hz_b)}, (mx_a, mx_b), {1: yx_b}, {(1, "y"): zy_b, (1, "z"): zz_b}
    middle = hid.at[1]
    begin, ready, peer, stages = gather_stages(links, position, wi_ref, wo_ref, wi, wo, load_sems)
    others = [(zc * SIDE + y, rem(me + k, ROW)) for k in range(1, ROW)]

    def spot(axis, o):
        return spots[axis, o % SIDE]

    def device(axis, o, index):
        moved = {"x": x, "y": y, "z": zc, axis: spot(axis, o)}
        return device_at(moved["x"], moved["y"], moved["z"], index)

    own_gain[ALL] = jnp.zeros(own_gain.shape, F32)
    count = sc_ref.shape[1]
    for f in range(ROW):
        @pl.when(me == f)
        def _():
            own_gain[0:PAIR, f * count:(f + 1) * count] = sc_ref[ALL].astype(F32)
    announce(others + [device(axis, o, index) for axis in "yz" for o in AROUND for index in range(PAIR)])
    begin()
    for k, far in enumerate(others):
        links.send(("sc",), own_gain, gains.at[me], far, batch=("sc",), whole=gains.at[pl.ds(0, OTHERS)])

    def keep(src, dst):
        copy = pltpu.make_async_copy(src, dst, own_sems.at[len(stored)])
        copy.start()
        stored.append(copy)

    def tokens(axis, o, index):
        return pl.ds(pl.multiple_of((PAIR * spot(axis, o) + index) * seq, seq), seq)

    def place(axis, o, index):
        return PAIR * spot(axis, o) + index

    def columns(axis, o):
        size = z.shape[PAIR] // ROW
        return lanes(((0 if axis == "y" else SIDE) + spot(axis, o)) * size, size)

    def several(batch, ref, n):
        whole = ref.at[pl.ds(0, n * seq if batch[0][0] in "yz" else n)]
        return dict(batch=batch, whole=whole)

    def send_h(l, axis):
        out, batch = h_out[axis][l].at[place(axis, 0, core)], several(("h", l, axis), h_out[axis][l], OTHERS)
        for o in AROUND:
            for index in range(PAIR):
                shared.send(("h", l, axis), ht.at[l, :, index], out, device(axis, o, index), **batch)
        shared.send(("h", l, axis), ht.at[l, :, 1 - core], out, twin, **batch)
        keep(ht.at[l, :, core], out)

    def arrive_h(l):
        for axis in "yz":
            shared.arrive(("h", l, axis), h_out[axis][l].at[pl.ds(0, OTHERS)])

    def row_block(l, o, index):
        size = omt.shape[1] // ROW
        return omt.at[l, pl.ds(pl.multiple_of((PAIR * spot("x", o) + index) * size, BAND), size)]

    def send_m(l):
        out, batch = m_out[l].at[place("x", 0, core)], several(("m", l), m_out[l], OTHERS)
        for o in AROUND:
            for index in range(PAIR):
                shared.send(("m", l), row_block(l, o, index), out, device("x", o, index), **batch)
        shared.send(("m", l), row_block(l, 0, 1 - core), out, twin, **batch)
        keep(row_block(l, 0, core), out)

    def arrive_m(l):
        shared.arrive(("m", l), m_out[l].at[pl.ds(0, OTHERS)])

    def token_half(axis, o, k):
        return pl.ds(pl.multiple_of((PAIR * spot(axis, o) + core) * seq + k * (seq // PAIR), seq // PAIR), seq // PAIR)

    def send_y(l):
        src, out = dy_ref, y_out[l].at[tokens("x", 0, core)]
        for by in BOTH:
            shared.send(("y", l, by), src, out, device("x", by, core), **several(("y", l), y_out[l], OTHERS))
        shared.send(("y", l), src, out, twin, **several(("y", l), y_out[l], OTHERS))
        keep(src, out)

    def pass_y(l, by):
        landed, part = y_out[l].at[tokens("x", -by, core)], y_out[l].at[token_half("x", -by, (1 - by) // PAIR)]
        shared.arrive(("y", l, by), landed)
        shared.send(("y2", l), part, part, device("x", by, core), **several(("y", l), y_out[l], OTHERS))
        shared.send(("y", l), landed, landed, twin, **several(("y", l), y_out[l], OTHERS))

    def far_y(l):
        landed = y_out[l].at[tokens("x", PAIR, core)]
        shared.arrive(("y2", l), landed)
        shared.send(("y", l), landed, landed, twin, **several(("y", l), y_out[l], OTHERS))

    def arrive_y(l):
        shared.arrive(("y", l), y_out[l].at[pl.ds(0, SIDE * seq)])

    def push_z(l, axis, o, ready):
        out = z_out[l, axis].at[tokens(axis, 0, core)]
        batch = several(("z", l, axis), z_out[l, axis], ROW)

        def start():
            if o != PAIR:
                shared.send(("z", l, axis, o), z.at[l, :, columns(axis, o)], out, device(axis, o, core), **batch)
                return
            for k, by in enumerate(BOTH):
                shared.send(("zr", l, axis, by), z.at[l, pl.ds(k * (seq // PAIR), seq // PAIR), columns(axis, PAIR)], relay_z.at[l, "yz".index(axis), k],
                            device(axis, by, core), **batch)

        if ready is None:
            start()
        else:
            pl.when(ready)(start)

    def own_part(l, axis):
        out, mine = z_out[l, axis].at[tokens(axis, 0, core)], z.at[l, :, columns(axis, 0)]
        shared.send(("z", l, axis), mine, out, twin, **several(("z", l, axis), z_out[l, axis], ROW))
        keep(mine, out)

    def send_z(l, axis):
        for o in (PAIR, 1, -1):
            push_z(l, axis, o, spot(axis, o) != 0 if axis == "y" else None)
        if axis == "z":
            own_part(l, axis)

    def rest_z(l):
        for o in (PAIR, 1, -1):
            push_z(l, "y", o, spot("y", o) == 0)
        own_part(l, "y")

    def pass_z(l, axis, by):
        k = (1 - by) // PAIR
        half = relay_z.at[l, "yz".index(axis), k]
        shared.arrive(("zr", l, axis, by), half)
        shared.send(("z2", l, axis), half, z_out[l, axis].at[token_half(axis, -by, k)], device(axis, by, core), **several(("z", l, axis), z_out[l, axis], ROW))

    def twin_z(l, axis, by):
        landed = z_out[l, axis].at[tokens(axis, -by, core)]
        shared.arrive(("z", l, axis, by), landed)
        shared.send(("z", l, axis), landed, landed, twin, **several(("z", l, axis), z_out[l, axis], ROW))

    def far_z(l, axis):
        landed = z_out[l, axis].at[tokens(axis, PAIR, core)]
        shared.arrive(("z2", l, axis), landed)
        shared.send(("z", l, axis), landed, landed, twin, **several(("z", l, axis), z_out[l, axis], ROW))

    def arrive_z(l, axis):
        shared.arrive(("z", l, axis), z_out[l, axis].at[pl.ds(0, SIDE * seq)])

    def send_scale(l):
        for far in others:
            shared.send(("scale", l), sc.at[l], sc_out.at[l, me], far, batch=("scale", l), whole=sc_out.at[l, pl.ds(0, OTHERS)])
        keep(sc.at[l], sc_out.at[l, me])

    def arrive_scale(l):
        shared.arrive(("scale", l), sc_out.at[l, pl.ds(0, OTHERS)])

    gains[me] = own_gain[ALL]
    z[:, :, wi.shape[PAIR]:] = jnp.zeros((PAIR, seq, z.shape[PAIR] - wi.shape[PAIR]), BF)
    entry = (x_ref, hid.at[0])
    angle = lax.broadcasted_iota(jnp.int32, (seq, LANE), 0).astype(F32) * freq_ref[0:1]
    for half in range(PAIR):
        cos_ref[:, LANE * half:LANE * (half + 1)] = jnp.cos(angle)
        sin_ref[:, LANE * half:LANE * (half + 1)] = jnp.sin(angle)
    lane = lax.broadcasted_iota(jnp.int32, turn_ref.shape, 1)
    down = lax.broadcasted_iota(jnp.int32, turn_ref.shape, 0) - lane
    low = rem(lane, HEAD) < BAND
    turn_ref[ALL] = jnp.where(low & (down == BAND), -1.0, jnp.where(jnp.logical_not(low) & (down == -BAND), 1.0, ZERO)).astype(BF)
    kts[ALL] = jnp.zeros(kts.shape, BF)
    pcat[ALL] = jnp.zeros(pcat.shape, BF)
    dscat[ALL] = jnp.zeros(dscat.shape, BF)

    def normalise(l, src):
        @pl.loop(0, seq // BAND, unroll=SIDE)
        def _(r):
            rows = pl.ds(pl.multiple_of(r * BAND, BAND), BAND)
            v = src[rows].astype(F32)
            v = v - jnp.mean(v, axis=-1, keepdims=True)
            var = jnp.mean(v * v, axis=-1, keepdims=True)
            h[l, rows] = (v * lax.rsqrt(var + 1e-6) * gain_ref[l:l + 1]).astype(BF)

    def project(l):
        strip = wi.shape[PAIR] // 5

        @pl.loop(0, 5)
        def _(i):
            at = lanes(i * strip, strip)
            z[l, :, at] = product(h[l], wi[l, :, at]).astype(BF)

    def heads(l):
        cos, sin = cos_ref[ALL], sin_ref[ALL]
        for g in range(dim // WIDE):
            q = z[l, :, g * WIDE:(g + 1) * WIDE]
            qr[l, :, g * WIDE:(g + 1) * WIDE] = ((q.astype(F32) * cos + product(q, turn_ref[ALL]) * sin) * 0.125).astype(BF)
        kv = z[l, :, dim:dim + LANE]
        turned = kv.astype(F32) * cos[:, :LANE] + product(kv, turn_ref[:LANE, :LANE]) * sin[:, :LANE]
        first = lax.broadcasted_iota(jnp.int32, turned.shape, 1) < HEAD
        key_lo = jnp.where(first, turned, ZERO)
        val_hi = jnp.where(first, ZERO, kv.astype(F32))
        return key_lo, pltpu.roll(key_lo, HEAD, 1), pltpu.roll(val_hi, HEAD, 1), val_hi

    def slot_rows(ref, lo, hi):
        zero = jnp.zeros((seq, LANE), BF)
        lo, hi = lo.astype(BF), hi.astype(BF)
        for i, (left, right) in enumerate(((lo, zero), (hi, zero), (zero, lo), (zero, hi))):
            ref[i * seq:(i + 1) * seq, :LANE] = left
            ref[i * seq:(i + 1) * seq, LANE:] = right

    def slot_cols(ref, lo):
        flat = lo.T[:HEAD].astype(BF)
        for i in range(SIDE):
            ref[HEAD * i:HEAD * (i + 1), i * seq:(i + 1) * seq] = flat

    def chances(i, half):
        at = slice(LANE * half, LANE * (half + 1))
        blocks = [pl.ds(pl.multiple_of(i * seq + LANE * k, LANE), LANE) for k in range(half + 1)]
        s = [scores[keys, at] for keys in blocks]
        lower = lax.broadcasted_iota(jnp.int32, s[-1].shape, 1) >= lax.broadcasted_iota(jnp.int32, s[-1].shape, 0)
        s[-1] = jnp.where(lower, s[-1], -1e30)
        top = functools.reduce(jnp.maximum, [jnp.max(v, axis=0, keepdims=True) for v in s])
        e = [jnp.exp(v - top) for v in s]
        scale = 1.0 / sum(jnp.sum(v, axis=0, keepdims=True) for v in e)
        return at, [(keys, v * scale) for keys, v in zip(blocks, e)]

    def attend(l):
        key_lo, key_hi, val_lo, _ = heads(l)
        slot_rows(ksl, key_lo, key_hi)
        slot_cols(kts, val_lo)
        flip(lambda at: qr[l, :, lanes(at, WIDE)], qt, dim)

        @pl.loop(0, dim // WIDE)
        def _(g):
            rows = pl.ds(pl.multiple_of(g * WIDE, WIDE), WIDE)
            scores[ALL] = product(ksl[ALL], qt[rows])

            @pl.loop(0, SIDE)
            def _(i):
                for half in range(PAIR):
                    at, blocks = chances(i, half)
                    for keys, p in blocks:
                        pcat[keys, at] = p.astype(BF)
            flat = product(kts[ALL], pcat[ALL]).astype(BF)
            omt[l, rows] = flat
            om[:, lanes(g * WIDE, WIDE)] = flat.T

    def mlp(l):
        @pl.loop(0, seq // BAND)
        def _(r):
            rows = pl.ds(pl.multiple_of(r * BAND, BAND), BAND)

            @pl.loop(0, ff // STRIP)
            def _(i):
                gate = z[l, rows, lanes(dim + LANE + i * STRIP, STRIP)].astype(F32)
                up = z[l, rows, lanes(dim + LANE + ff + i * STRIP, STRIP)].astype(F32)
                om[rows, lanes(dim + i * STRIP, STRIP)] = (gate * jax.nn.sigmoid(gate) * up).astype(BF)

    def put_out(l, dst):
        for n in range(dim // WIDE):
            cols = slice(n * WIDE, (n + 1) * WIDE)
            total = product(om[ALL], wo[l, :, cols])
            dst[:, cols] = (entry[l][:, cols].astype(F32) + total).astype(BF)

    def flip(src, dst, width, first=0):
        @pl.loop(first // WIDE, width // WIDE)
        def _(i):
            dst[pl.ds(pl.multiple_of(i * WIDE, WIDE), WIDE)] = src(i * WIDE).T

    upstream = (middle, dy_ref)

    def back_out(l):
        dy = upstream[l]
        flip(lambda at: dy[:, lanes(at, WIDE)], dyt, dim)

        @pl.loop(0, wo.shape[1] // dim)
        def _(n):
            rows = pl.ds(pl.multiple_of(n * dim, dim), dim)
            part = product(wo[l, rows], dyt[ALL]).astype(BF)
            om[:, lanes(n * dim, dim)] = part.T

            @pl.when(n == 0)
            def _():
                dot_heads[ALL] = part

    def back_mlp(l):
        @pl.loop(0, seq // BAND)
        def _(r):
            rows = pl.ds(pl.multiple_of(r * BAND, BAND), BAND)

            @pl.loop(0, ff // STRIP)
            def _(i):
                gate_at, up_at = lanes(dim + LANE + i * STRIP, STRIP), lanes(dim + LANE + ff + i * STRIP, STRIP)
                gate, up = z[l, rows, gate_at].astype(F32), z[l, rows, up_at].astype(F32)
                d = om[rows, lanes(dim + i * STRIP, STRIP)].astype(F32)
                sig = jax.nn.sigmoid(gate)
                du = d * up
                z[l, rows, gate_at] = (du * sig + du * gate * (sig * (1.0 - sig))).astype(BF)
                z[l, rows, up_at] = (d * (gate * sig)).astype(BF)

    def back_heads(l):
        key_lo, key_hi, val_lo, val_hi = heads(l)
        slot_rows(ksl, key_lo, key_hi)
        slot_rows(vsl, val_lo, val_hi)
        slot_cols(kts, key_lo)
        dkv[ALL] = jnp.zeros(dkv.shape, F32)
        flip(lambda at: qr[l, :, lanes(at, WIDE)], qt, dim)
        for at in range(0, dim, LANE):
            pair = slice(at, at + LANE)
            turned_q[:, pair] = pltpu.roll(qr[l, :, pair].astype(F32), HEAD, 1).astype(BF)
            turned_o[:, pair] = pltpu.roll(om[:, pair].astype(F32), HEAD, 1).astype(BF)

    def back_quad(l):
        @pl.loop(0, dim // WIDE)
        def _(g):
            quad(l, g)

    def quad(l, g):
        cols = pl.ds(pl.multiple_of(g * WIDE, WIDE), WIDE)
        scores[ALL] = product(ksl[ALL], qt[cols])
        dscores[ALL] = product(vsl[ALL], dot_heads[cols])

        @pl.loop(0, SIDE)
        def _(i):
            for half in range(PAIR):
                at, blocks = chances(i, half)
                given = [p * dscores[keys, at].astype(BF).astype(F32) for keys, p in blocks]
                total = sum(jnp.sum(v, axis=0, keepdims=True) for v in given)
                for (keys, p), v in zip(blocks, given):
                    pcat[keys, at] = p.astype(BF)
                    dscat[keys, at] = (v - p * total).astype(BF)
        dq = product(kts[ALL], dscat[ALL]).astype(BF).T
        back = dq.astype(F32) * cos_ref[ALL] - product(dq, turn_ref[ALL]) * sin_ref[ALL]
        z[l, :, cols] = (back * 0.125).astype(BF)
        def pieces(left, even, odd):
            for i in range(SIDE):
                pair = lanes(g * WIDE + i // PAIR * LANE, LANE)
                yield product(left[i * seq:(i + 1) * seq, :], odd(pair) if i % PAIR else even(pair))

        dkv[0] += sum(pieces(dscat, lambda at: qr[l, :, at], lambda at: turned_q[:, at]))
        dkv[1] += sum(pieces(pcat, lambda at: turned_o[:, at], lambda at: om[:, at]))

    def back_keys(l):
        dk = dkv[0].astype(BF)
        turned = dk.astype(F32) * cos_ref[:, :LANE] - product(dk, turn_ref[:LANE, :LANE]) * sin_ref[:, :LANE]
        first = lax.broadcasted_iota(jnp.int32, turned.shape, 1) < HEAD
        z[l, :, dim:dim + LANE] = jnp.where(first, turned, dkv[1]).astype(BF)

    def back_in(l, half):
        width = wi.shape[PAIR] // 5
        at = slice(PAIR * half * width, (PAIR + TRIO * half) * width)
        part = product(wi[l, :, at], z[l, :, at], ((1,), (1,)))
        dht[ALL] = dht[ALL] + part if half else part

    def back_norm(l):
        dy, dst = upstream[l], (gx_ref, middle)[l]
        for i in range(dim // WIDE):
            cols = slice(i * WIDE, (i + 1) * WIDE)
            h[l, :, cols] = dht[cols].T.astype(BF)
        sc[l] = jnp.zeros(sc.shape[1:], F32)

        @pl.loop(0, seq // BAND, unroll=SIDE)
        def _(r):
            rows = pl.ds(pl.multiple_of(r * BAND, BAND), BAND)
            v = entry[l][rows].astype(F32)
            v = v - jnp.mean(v, axis=-1, keepdims=True)
            scale = lax.rsqrt(jnp.mean(v * v, axis=-1, keepdims=True) + 1e-6)
            hat = v * scale
            d = h[l, rows].astype(F32)
            each = (d * hat).reshape(SIDE, ROW, dim)
            sc[l] += (each[0] + each[1]) + (each[PAIR] + each[TRIO])
            d = d * gain_ref[l:l + 1]
            d = scale * (d - jnp.mean(d, axis=-1, keepdims=True) - hat * jnp.mean(d * hat, axis=-1, keepdims=True))
            dst[rows] = (dy[rows].astype(F32) + d.astype(BF).astype(F32)).astype(BF)

    def do_norm(l):
        if l == 0:
            links.arrive(("sc",), gains.at[pl.ds(0, OTHERS)])
            gain_ref[ALL] = jnp.sum(gains[ALL], axis=0)
        normalise(l, entry[l])
        for i in range(dim // WIDE):
            flat = h[l, :, i * WIDE:(i + 1) * WIDE].T
            size = ht.shape[TRIO]
            for b in range(ROW):
                lo, hi = max(b * size, i * WIDE), min((b + 1) * size, (i + 1) * WIDE)
                if lo < hi:
                    ht[l, b // PAIR, b % PAIR, lo - b * size:hi - b * size] = flat[lo - i * WIDE:hi - i * WIDE]

    def do_project(l):
        ready(PAIR * l)
        project(l)

    def do_mlp(l):
        mlp(l)
        flip(lambda at: om[:, lanes(at, WIDE)], omt.at[l], om.shape[1], dim)

    def do_put(l):
        ready(PAIR * l + 1)
        put_out(l, hid.at[0] if l == 0 else y_ref)

    stages.update(
        norm=do_norm, project=do_project, attend=attend, mlp=do_mlp, put=do_put, back_out=back_out, back_mlp=back_mlp, back_heads=back_heads,
        back_quad=back_quad, back_keys=back_keys, back_in=back_in, back_norm=back_norm, send_h=send_h, send_m=send_m, send_y=send_y, pass_y=pass_y, far_y=far_y, send_z=send_z, rest_z=rest_z, pass_z=pass_z, twin_z=twin_z, far_z=far_z,
        send_scale=send_scale, own_z=lambda: keep(z.at[0], z_a), own_y=lambda: keep(middle, dy_a))
    for kind, *task in order:
        stages[kind](*task)
    for l in range(PAIR):
        arrive_h(l)
        arrive_m(l)
        arrive_scale(l)
    arrive_y(1)
    for l, axis in z_out:
        arrive_z(l, axis)
    for copy in stored:
        copy.wait()
    shared.drain()
    links.drain()


def run_layers(x, dy, scale, w_in, w_out, freq, starts=(ZERO, 10.0, 20.0, 30.0)):
    seq, dim = x.shape
    proj, cat = w_in.shape[PAIR], ROW * w_out.shape[1]
    wide = proj + LANE
    hbm, vmem = pl.BlockSpec(memory_space=pltpu.HBM), pl.BlockSpec(memory_space=pltpu.VMEM)
    out = lambda *shape, dtype=BF: jax.ShapeDtypeStruct(shape, dtype)
    buffer = lambda *shape, dtype=BF: pltpu.VMEM(shape, dtype)
    sem = pltpu.SemaphoreType.DMA
    line = ROW * seq
    return pl.pallas_call(
        functools.partial(layers_kernel, layers_order(*w_in.shape[1:], *w_out.shape[1:], seq, starts)),
        out_shape=(out(seq, dim), out(seq, dim), *[out(ROW, SIDE, dim // ROW, seq)] * SIDE, *[out(ROW, cat // ROW, seq)] * PAIR, out(line, dim),
                   *[out(line, wide // ROW)] * PAIR, out(seq, wide), out(seq, dim), out(PAIR, ROW, ROW, dim, dtype=F32),
                   out(PAIR, PAIR, PAIR, seq // PAIR, wide // ROW)),
        in_specs=[vmem, hbm, hbm] + [vmem] * TRIO,
        out_specs=[vmem] * PAIR + [hbm] * 13,
        scratch_shapes=[
            buffer(PAIR, dim, proj), buffer(PAIR, cat, dim), buffer(PAIR, seq, wide), buffer(seq, cat), buffer(PAIR, seq, dim),
            buffer(PAIR, seq, dim), buffer(PAIR, seq, dim),
            buffer(WIDE, SIDE * seq), buffer(SIDE * seq, WIDE), buffer(SIDE * seq, WIDE), buffer(seq, dim), buffer(seq, dim),
            buffer(SIDE * seq, seq, dtype=F32), buffer(SIDE * seq, seq, dtype=F32), buffer(SIDE * seq, seq), buffer(SIDE * seq, seq),
            buffer(seq, WIDE, dtype=F32), buffer(seq, WIDE, dtype=F32), buffer(WIDE, WIDE),
            buffer(dim, seq), buffer(dim, seq), buffer(dim, seq, dtype=F32), buffer(PAIR, seq, LANE, dtype=F32),
            buffer(PAIR, cat, seq), buffer(PAIR, SIDE, PAIR, dim // ROW, seq), buffer(dim, seq), buffer(PAIR, ROW, dim, dtype=F32),
            buffer(ROW, ROW, dim, dtype=F32), buffer(ROW, dim, dtype=F32), buffer(ROW, dim, dtype=F32),
            sem((SIDE,)), sem((13,)), sem((15,)), sem((107,)), sem((11,)), sem((24,)),
        ],
        compiler_params=pltpu.CompilerParams(collective_id=PAIR, has_side_effects=True, vmem_limit_bytes=67043328),
        name="run_layers",
    )(scale, w_in, w_out, x, dy, freq)


PARTS = (("i", "x", "z", "y", 0, STRIP), ("i", "x", "z", "y", STRIP, 384), ("i", "x", "y", "z", 0, STRIP), ("i", "x", "y", "z", STRIP, 384),
         ("o", "y", "z", "y", 0, 384), ("o", "z", "y", "z", 384, 384))


def reduce_order(rows, rows_b, starts):
    rate = 11650.0
    tasks = []
    sizes = {"y": WIDE * 896 / (PAIR * rate), "z": WIDE * 896 / (PAIR * rate), "x": WIDE * 768 / (PAIR * rate)}
    for axis in "yzx":
        size = sizes[axis]
        tasks.append((("swap", axis), (0, 0), starts[PAIR] if axis == "x" else starts[TRIO], [], [],
                      [((axis, by), size * n) for by, n in ((-1, 0.5), (1, 1), (-1, 1), (1, 1))], SHORT))
        tasks.append((("relay", axis), (0, 0), ZERO, [(("swap", axis), 0)], [], [((axis, -1), size / PAIR)], SHORT))
        for o, needs in ((1, [(("swap", axis), 1)]), (-1, [(("swap", axis), PAIR)]), (PAIR, [(("swap", axis), TRIO), (("relay", axis), 0)])):
            tasks.append((("near", axis, o), (0, PAIR), ZERO, needs, [], [("chip", 1.6)], QUICK))
    tasks.append((("fetch", 0), (5, 0), ZERO, [], [("make", 1, len(PARTS) - 1)], [], QUICK))
    for l in (1, 0):
        late = 1 - l
        for c, (kind, first, then, last, at, width) in enumerate(PARTS):
            needs, cost = [], 1.6 * width / STRIP
            if l == 0:
                needs = [(("near", last if kind == "i" else "x", o), 0) for o in AROUND]
            tasks.append((("make", l, c), (9 * late, c), starts[late], needs, [] if l else [("fetch", 0)], [], cost))
            full = SIDE * SIDE * (rows if kind == "i" else rows_b) * width / rate
            sends = [[((first, by), full / ROW) for by in BOTH], [((first, by), full / SIDE) for by in BOTH],
                     [((then, o), full / 16) for o in (1, -1, 1)], []]
            piece = full / 16
            sends += [[((then, o), piece) for o in (1, -1, 1)], [((last, by), SIDE * piece) for by in BOTH],
                      [((last, by), PAIR * piece) for by in BOTH], []]
            for s in range(ROW):
                task = ("sum", l, c, s)
                needs = [(("sum", l, c, s - 1), k) for k in range(len(sends[s - 1]))] if s else []
                tasks.append((task, (late, -s), ZERO, needs, [("make", l, c)] if s == 0 else [("sum", l, c, s - 1)], sends[s], SHORT))
    return plan(tasks)


def reduce_kernel(order, *refs):
    hy, hz, mx = refs[0:PAIR], refs[PAIR:SIDE], refs[SIDE:6]
    yx1, zy1, zz1, z0, y0, sc = refs[6:12]
    oa, ob = refs[12:14]
    n = len(PARTS)
    total, half, full, small, front = (refs[14 + k * n:14 + (k + 1) * n] for k in range(5))
    (hbuf, zbuf, mbuf, ybuf, scbuf, rz, ry, ssem, rsem, isem, osem) = refs[14 + 5 * n:]
    position = chip_position()
    x, y, zc, core = position
    place = {"x": x, "y": y, "z": zc}
    twin = device_at(x, y, zc, 1 - core)
    spots, peers = around(position)

    def spot(axis, o):
        return spots[axis, o % SIDE]

    def peer(axis, o):
        return peers[axis, o % SIDE]

    seq, wide = z0.shape
    own = wide // ROW
    loads, moving = {}, []

    def load(key, src, dst):
        copy = pltpu.make_async_copy(src, dst, isem.at[len(moving)])
        moving.append(key)
        copy.start()
        loads[key] = copy

    def fetch(l):
        if l:
            load(("z", 1, "y"), zy1, zbuf.at[1, 0])
        load(("h", l, "y"), hy[l], hbuf.at[l, 0])
        if l:
            load(("z", 1, "z"), zz1, zbuf.at[1, 1])
        load(("h", l, "z"), hz[l], hbuf.at[l, 1])
        load(("m", l), mx[l], mbuf.at[l])
        if l:
            load(("y", 1), yx1, ybuf.at[1])
        load(("s", l), sc.at[l], scbuf.at[l])

    fetch(1)
    done = set()

    def loaded(*keys):
        for key in keys:
            if key not in done:
                loads[key].wait()
                done.add(key)

    announce([peer(axis, o) for axis in "xyz" for o in AROUND] + [twin])
    links = Links(ssem, rsem)

    def columns(axis, o):
        return lanes(((0 if axis == "y" else SIDE) + spot(axis, o)) * own, own)

    def tokens(axis, o, index):
        return pl.ds(pl.multiple_of((PAIR * spot(axis, o) + index) * seq, seq), seq)

    def target(axis):
        return ybuf.at[0] if axis == "x" else zbuf.at[0, "yz".index(axis)]

    def leaving(axis):
        return dict(batch=("swap", axis), whole=target(axis).at[pl.ds(0, OTHERS * seq + seq // PAIR)])

    def half_at(axis, o, k):
        start = (PAIR * spot(axis, o) + core) * seq + k * (seq // PAIR)
        return target(axis).at[pl.ds(pl.multiple_of(start, seq // PAIR), seq // PAIR)]

    def relay_of(axis):
        return ry if axis == "x" else rz.at["yz".index(axis)]

    def swap(axis):
        def part(o, rows=slice(None)):
            return y0.at[rows] if axis == "x" else z0.at[rows, columns(axis, o)]

        mine = target(axis).at[tokens(axis, 0, core)]
        links.send(("relay", axis), part(PAIR, pl.ds(seq // PAIR, seq // PAIR)), relay_of(axis), peer(axis, -1), **leaving(axis))
        for by in BOTH:
            links.send(("swap", axis, by), part(by), mine, peer(axis, by), **leaving(axis))
        links.send(("swap", axis, PAIR), part(PAIR, pl.ds(0, seq // PAIR)), half_at(axis, 0, 0), peer(axis, PAIR), **leaving(axis))
        links.send(("near", axis), part(0), mine, twin, **leaving(axis))
        load(("own", axis), part(0), mine)

    def relay(axis):
        links.arrive(("relay", axis), relay_of(axis))
        links.send(("relayed", axis), relay_of(axis), half_at(axis, 1, 1), peer(axis, -1), **leaving(axis))

    def near(axis, o):
        landed = target(axis).at[tokens(axis, -o, core)]
        if o == PAIR:
            links.arrive(("swap", axis, PAIR), half_at(axis, PAIR, 0))
            links.arrive(("relayed", axis), half_at(axis, PAIR, 1))
        else:
            links.arrive(("swap", axis, o), landed)
        links.send(("near", axis), landed, landed, twin, **leaving(axis))

    def joined(axis):
        if axis not in done:
            done.add(axis)
            loaded(("own", axis))
            links.arrive(("near", axis), target(axis).at[pl.ds(0, SIDE * seq)])

    def joined_lanes(ref, l, i):
        return jnp.concatenate([ref[l, i, k].reshape(-1, ref.shape[-1]) for k in range(ROW)], axis=1)

    def make(l, c):
        kind, first, then, last, at, width = PARTS[c]
        if kind == "i":
            i = "yz".index(last)
            loaded(("h", l, last))
            if l:
                loaded(("z", l, last))
            else:
                joined(last)
            size = total[c].shape[TRIO]
            for lo in range(0, width, WIDE):
                hi = min(width, lo + WIDE)
                part = product(joined_lanes(hbuf, l, i), zbuf[l, i, :, at + lo:at + hi])
                for r in range(16):
                    total[c][l, r // SIDE, r % SIDE, :, lo:hi] = part[r * size:(r + 1) * size]
            return
        loaded(("m", l), ("s", l))
        if l:
            loaded(("y", l))
        else:
            joined("x")
        part = product(jnp.concatenate([mbuf[l, k] for k in range(ROW)], axis=1), ybuf[l, :, at:at + width])
        size = total[c].shape[TRIO]

        def put(r, value):
            total[c][(l, r // SIDE, r % SIDE) if first == "y" else (l, r % SIDE, r // SIDE)] = value

        for r in range(part.shape[0] // size):
            put(r, part[r * size:(r + 1) * size])
        gain = jnp.sum(jnp.sum(scbuf[l, :, :, at:at + width], axis=0), axis=0, keepdims=True)
        row = lax.broadcasted_iota(jnp.int32, (size, width), 0)
        put(15, jnp.where(row == 0, gain, ZERO))

    def area(l, c, o, whole):
        kind, first, then, last, at, width = PARTS[c]
        inner = (spot(then, whole) if isinstance(whole, int) else whole)
        outer = spot(last, o)
        if kind == "i":
            cols = lanes(((0 if last == "y" else SIDE) + outer) * own + at, width)
            return oa.at[l, inner, :, cols]
        cols = pl.ds(at, width)
        return ob.at[l, outer, inner, :, cols] if last == "y" else ob.at[l, inner, outer, :, cols]

    def add(l, c, s):
        kind, first, then, last, at, width = PARTS[c]
        t = total[c].at[l]
        sums = dict(batch=(l, c, 0), whole=t)
        lines = dict(batch=(l, c, 1), whole=t.at[pl.ds(0, PAIR)])
        singles = dict(batch=(l, c, PAIR), whole=t.at[pl.ds(0, PAIR), pl.ds(0, TRIO)])
        if s == 0:
            far = t.at[spot(first, PAIR)]
            for k, by in enumerate(BOTH):
                links.send((l, c, "half"), far.at[pl.ds(PAIR * k, PAIR)], half[c].at[l, k], peer(first, by), **sums)
        elif s == 1:
            links.arrive((l, c, "half"), half[c].at[l])
            for k, by in enumerate(BOTH):
                mine = t.at[spot(first, by)]
                add_into(mine.at[pl.ds(PAIR * k, PAIR)], half[c].at[l, k])
                links.send((l, c, "full"), mine, full[c].at[l, k], peer(first, by), **sums)
        elif s == PAIR:
            mine = t.at[spot(first, 0)]
            links.arrive((l, c, "full"), full[c].at[l])
            for k in range(PAIR):
                add_into(mine, full[c].at[l, k])
            for k, o in enumerate(AROUND):
                links.send((l, c, "small"), mine.at[spot(then, o)], small[c].at[l, k], peer(then, o), **singles)
        elif s == TRIO:
            links.arrive((l, c, "small"), small[c].at[l])
            mine = t.at[spot(first, 0), spot(then, 0)]
            front[c][l] = (mine[ALL] + small[c][l, 0]) + (small[c][l, 1] + small[c][l, PAIR])
        elif s == SIDE:
            src, dst = front[c].at[l], area(l, c, 0, 0)
            for o in AROUND:
                links.send((l, c, "a1"), src, dst, peer(then, o), **singles)
            copy = pltpu.make_async_copy(src, dst, osem.at[l, c])
            copy.start()
            loads["front", l, c] = copy
        elif s == 5:
            loaded(("front", l, c))
            links.arrive((l, c, "a1"), t.at[0, pl.ds(0, TRIO)])
            line = area(l, c, 0, slice(None))
            for by in BOTH:
                links.send((l, c, "a2"), line, line, peer(last, by), **lines)
        elif s == 6:
            links.arrive((l, c, "a2"), t.at[pl.ds(0, PAIR)])
            for k, by in enumerate(BOTH):
                part = area(l, c, -by, pl.ds(PAIR * k, PAIR))
                links.send((l, c, "a3"), part, part, peer(last, by), **sums)
        else:
            links.arrive((l, c, "a3"), area(l, c, PAIR, slice(None)))

    stages = {"swap": swap, "relay": relay, "near": near, "fetch": fetch, "make": make, "sum": add}
    for kind, *task in order:
        stages[kind](*task)
    links.drain()


def add_into(dst, src):
    @pl.loop(0, dst.shape[0])
    def _(i):
        if len(dst.shape) == SIDE:
            for j in range(dst.shape[1]):
                dst[i, j] += src[i, j]
        else:
            dst[i] += src[i]


def around(position):
    place, core = dict(zip("xyz", position)), position[TRIO]
    spots = {(axis, o): step(place[axis], o) for axis in "xyz" for o in range(SIDE)}
    peers = {}
    for axis in "xyz":
        for o in range(1, SIDE):
            moved = {**place, axis: spots[axis, o]}
            peers[axis, o] = device_at(moved["x"], moved["y"], moved["z"], core)
    return spots, peers


def reduce_gradients(operands, starts=(ZERO, ZERO, 20.0, 3.0)):
    hbm = pl.BlockSpec(memory_space=pltpu.HBM)
    h_rows, m_rows, y_cols, z_cols, z_own, y_own, scale_parts = operands
    part, part_b = h_rows[0].shape[PAIR] // SIDE, (m_rows[0].shape[1] + BAND) // 16
    (line, dim), wide = y_cols.shape, z_own.shape[1]
    out = lambda *shape: jax.ShapeDtypeStruct(shape, F32)
    sem = pltpu.SemaphoreType.DMA

    def buffers(*lead):
        return [pltpu.VMEM((PAIR, *lead, part if e[0] == "i" else part_b, e[5]), F32) for e in PARTS]

    return pl.pallas_call(
        functools.partial(reduce_kernel, reduce_order(part, part_b, starts)),
        out_shape=(out(PAIR, SIDE, part, wide), out(PAIR, SIDE, SIDE, part_b, dim)),
        in_specs=[hbm] * 12,
        out_specs=[hbm] * PAIR,
        scratch_shapes=[
            *buffers(SIDE, SIDE), *buffers(PAIR, PAIR), *buffers(PAIR, SIDE), *buffers(TRIO), *buffers(),
            pltpu.VMEM((PAIR, PAIR, *h_rows[0].shape), BF), pltpu.VMEM((PAIR, PAIR, line, wide // ROW), BF), pltpu.VMEM((PAIR, *m_rows[0].shape), BF),
            pltpu.VMEM((PAIR, line, dim), BF), pltpu.VMEM(scale_parts.shape, F32),
            pltpu.VMEM((PAIR, z_own.shape[0] // PAIR, wide // ROW), BF), pltpu.VMEM((y_own.shape[0] // PAIR, dim), BF),
            sem((39,)), sem((90,)), sem((14,)), sem((PAIR, len(PARTS))),
        ],
        compiler_params=pltpu.CompilerParams(collective_id=1, has_side_effects=True, vmem_limit_bytes=67043328),
        name="reduce_gradients",
    )(*h_rows, *m_rows, y_cols, *z_cols, z_own, y_own, scale_parts)


def finish_kernel(count, in_ref, out_ref, y_ref, gx_ref, in_grad, out_grad, y_out, gx_out, scale_out, in_buf, out_buf, y_buf, gx_buf, came, left):
    moves = [(out_ref.at[l, p], out_buf.at[l, pl.ds(SIDE * p, SIDE)]) for l in range(PAIR) for p in range(SIDE)]
    moves += [(y_ref, y_buf), (gx_ref, gx_buf)]
    size, width = in_buf.shape[PAIR:]
    moves += [(in_ref.at[l, p, :, pl.ds(0, width)], in_buf.at[l, p]) for l in range(PAIR) for p in range(SIDE)]
    loads = [pltpu.make_async_copy(src, dst, came.at[k]) for k, (src, dst) in enumerate(moves)]
    for copy in loads:
        copy.start()
    stores = []

    def store(src, dst):
        copy = pltpu.make_async_copy(src, dst, left.at[len(stores)])
        copy.start()
        stores.append(copy)

    for l in range(PAIR):
        for p in range(SIDE):
            loads[SIDE * l + p].wait()
        store(out_buf.at[l, pl.ds(0, 15)], out_grad.at[l])
    for k, (src, dst) in enumerate(((y_buf, y_out), (gx_buf, gx_out))):
        loads[ROW + k].wait()
        store(src, dst)
    me = lax.axis_index("fsdp")
    for l in range(PAIR):
        for f in range(ROW):
            @pl.when(me == f)
            def _():
                scale_out[l:l + 1] = out_buf[l, 15, 0:1, f * count:(f + 1) * count]
    for l in range(PAIR):
        for p in range(SIDE):
            loads[10 + SIDE * l + p].wait()
            store(in_buf.at[l, p], in_grad.at[l, pl.ds(p * size, size)])
    for copy in stores:
        copy.wait()


def finish(in_sums, out_sums, y, gx, rows, proj):
    hbm = pl.BlockSpec(memory_space=pltpu.HBM)
    out = lambda *shape, dtype=F32: jax.ShapeDtypeStruct(shape, dtype)
    size, (depth, dim) = in_sums.shape[PAIR], out_sums.shape[TRIO:]
    in_grad, out_grad, y_out, gx_out, scale = pl.pallas_call(
        functools.partial(finish_kernel, rows),
        out_shape=(out(PAIR, rows, proj), out(PAIR, 15, depth, dim), out(*y.shape, dtype=BF), out(*gx.shape, dtype=BF), out(PAIR, rows)),
        in_specs=[hbm] * SIDE,
        out_specs=[hbm] * SIDE + [pl.BlockSpec(memory_space=pltpu.VMEM)],
        scratch_shapes=[
            pltpu.VMEM((PAIR, SIDE, size, proj), F32), pltpu.VMEM((PAIR, 16, depth, dim), F32), pltpu.VMEM(y.shape, BF), pltpu.VMEM(gx.shape, BF),
            pltpu.SemaphoreType.DMA((18,)), pltpu.SemaphoreType.DMA((12,)),
        ],
        compiler_params=pltpu.CompilerParams(vmem_limit_bytes=67043328),
        name="finish",
    )(in_sums, out_sums, y, gx)
    return y_out[None], gx_out[None], scale, in_grad, out_grad.reshape(PAIR, 15 * depth, dim)


def solution(mesh):
    fsdp_size = mesh.shape["fsdp"]
    batch_spec = P(("dp", "fsdp"), None, None)
    scale_spec = P(None, "fsdp")
    weight_spec = P(None, "fsdp", None)

    def device_step(x_in, grad_y, norm_scale, w_in, w_out):
        n_layers = w_in.shape[0]
        seq_len, model_dim = x_in.shape[1:]
        proj_dim = w_in.shape[PAIR]
        ff_dim = w_out.shape[1] * fsdp_size - model_dim
        head_dim = (proj_dim - model_dim - PAIR * ff_dim) // PAIR
        rows, rows_out = norm_scale.shape[1], w_out.shape[1]
        half_dim = head_dim // PAIR
        freq = 10000.0 ** (-np.arange(half_dim, dtype=np.float32) * 2.0 / head_dim)
        freq = jnp.asarray(np.tile(freq.astype(np.float32), (ROW, LANE // half_dim)))
        hidden, grad_hidden, *rest = run_layers(x_in[0], grad_y[0], norm_scale, w_in, w_out, freq)
        in_sums, out_sums = reduce_gradients((rest[0:SIDE], rest[SIDE:6], rest[6], rest[OTHERS:9], rest[9], rest[10], rest[11]))
        return finish(in_sums, out_sums, hidden, grad_hidden, rows, proj_dim)

    return jax.shard_map(
        device_step,
        mesh=mesh,
        in_specs=(batch_spec, batch_spec, scale_spec, weight_spec, weight_spec),
        out_specs=(batch_spec, batch_spec, scale_spec, weight_spec, weight_spec),
        check_vma=False,
    )
```

```python
import functools
import jax
import jax.numpy as jnp
import numpy as np
from jax import lax
from jax.experimental import pallas as pl
from jax.experimental.pallas import tpu as pltpu
from jax.sharding import PartitionSpec as P

MESH_ID = pl.DeviceIdType.MESH
BOTH = (1, -1)
AROUND = (1, -1, 2)
PARTS = (True, False)
ALL, ZERO = ..., 0.0
OTHERS = 7
QUICK, SHORT = 0.2, 0.3
LANE, WIDE, STRIP, HEAD = 128, 256, 512, 64
ROW, BAND, SIDE, TRIO, PAIR = 8, 32, 4, 3, 2


class Links:
    def __init__(self, send_sems, recv_sems):
        self.send_sems, self.recv_sems = send_sems, recv_sems
        self.slots, self.batches, self.sent, self.count = {}, {}, {}, 0

    def _landing(self, key, lane):
        if key not in self.slots:
            self.slots[key] = self.count
            self.count += 1 if lane is None else PAIR
        return self.recv_sems.at[self.slots[key] + (0 if lane is None else lane)]

    def send(self, key, src, dst, device, landing=None, whole=None, batch=None, lane=None):
        leaving = self.batches.setdefault(batch or key, len(self.batches))
        copy = pltpu.make_async_remote_copy(
            src_ref=src, dst_ref=dst, send_sem=self.send_sems.at[leaving], recv_sem=self._landing(landing or key, lane),
            device_id=device, device_id_type=MESH_ID)
        copy.start()
        self.sent[batch or key] = (src if whole is None else whole, leaving)

    def arrive(self, key, landed, lane=None):
        pltpu.make_async_copy(landed, landed, self._landing(key, lane)).wait()

    def drain(self):
        for left, leaving in self.sent.values():
            pltpu.make_async_copy(left, left, self.send_sems.at[leaving]).wait()
        self.sent.clear()


def rem(a, n):
    return a % n if isinstance(a, int) else lax.rem(a, n)


def chip_position():
    f, d = lax.axis_index("fsdp"), lax.axis_index("dp")
    return f // PAIR, rem(d, SIDE), d // SIDE, rem(f, PAIR)


def device_at(x, y, z, core):
    return (z * SIDE + y, x * PAIR + core)


def step(coord, by):
    return rem(coord + SIDE + by, SIDE)


def announce(devices):
    barrier = pltpu.get_barrier_semaphore()
    for device in devices:
        pl.semaphore_signal(barrier, inc=1, device_id=device, device_id_type=MESH_ID)
    pl.semaphore_wait(barrier, len(devices))


def plan(tasks, latency=2.5):
    free, landed, order, now = {}, {}, [], ZERO
    left = list(tasks)
    while left:
        best = None
        for place, (name, rank, start, needs, after, _, _) in enumerate(left):
            if all(n[0] in landed for n in needs) and all(n in landed for n in after):
                ready = max([start, now] + [landed[task][i] for task, i in needs])
                best = min(best or (ready, rank, place), (ready, rank, place))
        now, _, place = best
        name, _, _, _, _, sends, cost = left.pop(place)
        order.append(name)
        now += cost
        landed[name] = []
        for link, time, *more in sends:
            free[link] = max(now, free.get(link, ZERO)) + time
            landed[name].append(free[link] + latency + sum(more))
    return order


def layers_order(rows_i, cols_i, rows_o, cols_o, seq, starts):
    rate = 23300.0
    tasks = []
    for m in range(SIDE):
        is_in = m % PAIR == 0
        edge = cols_i // LANE * SIDE // 9 // PAIR * WIDE
        size = {"y": rows_i // SIDE * edge, "x": rows_i * (cols_i - PAIR * edge)} if is_in else {"y": rows_o // SIDE * cols_o // PAIR}
        size["z"] = size["y"]
        colors = "yzx" if is_in else "yz"
        tasks.append((("lend", m), 5, 3.0 + SIDE * m, [], [], [("chip", (rows_i * cols_i if is_in else rows_o * cols_o) / 150000.0)], QUICK))
        for color in colors:
            cost = size[color] / rate
            both = [(("x", by), cost) for by in BOTH]
            spread = [((color, by), cost) for by in BOTH] if color != "x" else []
            tasks.append((("reach", m, color), m, starts[m], [], [], both, QUICK))
            for i, by in enumerate(BOTH):
                tasks.append((("relay", m, color, by), m, ZERO, [(("reach", m, color), i)], [], [(("x", by), cost / PAIR)] + spread, QUICK))
            halves = [(("relay", m, color, by), 0) for by in BOTH]
            tasks.append((("far", m, color), m, ZERO, halves, [], spread, QUICK))
            if color == "x":
                continue
            for off, source, first in ((-1, ("relay", m, color, 1), 1), (1, ("relay", m, color, -1), 1), (PAIR, ("far", m, color), 0)):
                for i, by in enumerate(BOTH):
                    tasks.append((("pass", m, color, off, by), m, ZERO, [(source, first + i)], [], [((color, by), cost / PAIR)], QUICK))
                halves = [(("pass", m, color, off, by), 0) for by in BOTH]
                tasks.append((("close", m, color, off), m, ZERO, halves, [], [], QUICK))
        for off in (-1, 1, PAIR):
            last = [("close", m, color, off) for color in "yz"]
            if is_in:
                last.append(("far", m, "x") if off == PAIR else ("relay", m, "x", -off))
            tasks.append((("hand", m, off), m, ZERO, [], last, [("chip", (rows_i * cols_i if is_in else rows_o * cols_o) / 150000.0)], QUICK))
    before = []

    def work(name, cost, mats=()):
        needs = [(("hand", m, off), 0) for m in mats for off in (-1, 1, PAIR)] + [(("lend", m), 0) for m in mats]
        tasks.append((name, 99, ZERO, needs, list(before), [], cost))
        before[:] = [name]

    for l in range(PAIR):
        work(("norm", l), 0.8)
        work(("project", l), 4.0, [PAIR * l])
        work(("attend", l), 4.2)
        work(("mlp", l), 2.2)
        work(("put", l), 1.6, [PAIR * l + 1])
    for l in (1, 0):
        work(("back_out", l), 2.9)
        work(("back_mlp", l), 2.0)
        work(("back_heads", l), 1.0)
        work(("back_quad", l), 6.0)
        work(("back_keys", l), QUICK)
        for i in range(PAIR):
            work(("back_in", l, i), 1.3 + 0.6 * i)
        work(("back_norm", l), 1.0)
    def send(name, rank, start, after, sends):
        tasks.append((name, rank, start, [], [after] if after else [], sends, 0.4))

    def follow(name, rank, needs, sends):
        tasks.append((name, rank, ZERO, needs, [], sends, QUICK))

    def both(axis, size):
        return [((axis, by), size / rate, margin) for by in BOTH]

    model, margin = rows_i * ROW, 0.5
    for l in (1, 0):
        for axis in "yz":
            name = ("send_h", l, axis)
            send(name, 20 - l, 58.0, ("norm", l), both(axis, seq * model))
            for i, by in enumerate(BOTH):
                for index in range(PAIR):
                    follow(("pass_h", l, axis, by, index), 10, [(name, i)], [((axis, by), seq * model / SIDE / rate, margin)])
        send(("send_m", l), 22 - l, ZERO, ("mlp", l), both("x", PAIR * seq * rows_o) + both("x", PAIR * seq * rows_o))
        if l == 0:
            send(("own_y",), 15, ZERO, ("back_norm", 1), [])
            send(("send_scale", l), 15, ZERO, ("back_norm", l), [])
            continue
        name = ("send_y", l)
        send(name, 12, 42.0, None, both("x", seq * model))
        for i, by in enumerate(BOTH):
            follow(("pass_y", l, by), 12, [(name, i)], [(("x", by), seq * model / PAIR / rate, margin)])
        follow(("far_y", l), 12, [(("pass_y", l, by), 0) for by in BOTH], [])
        for axis in "zy":
            name = ("send_z", l, axis)
            share = seq * (cols_i + LANE) / ROW
            send(name, 13, ZERO, ("back_mlp", l), both(axis, share / PAIR) + both(axis, share))
            if axis == "y":
                name = ("rest_z", l)
                send(name, 13, ZERO, ("back_keys", l), both(axis, share / ROW) + both(axis, share / SIDE))
            for i, by in enumerate(BOTH):
                follow(("pass_z", l, axis, by), 13, [(name, i)], [((axis, by), share / PAIR / rate, margin)])
                follow(("twin_z", l, axis, by), 14, [(name, PAIR + i)], [])
            follow(("far_z", l, axis), 14, [(("pass_z", l, axis, by), 0) for by in BOTH], [])
        send(("send_scale", l), 15, ZERO, ("back_norm", l), [])
    send(("own_z",), 15, ZERO, ("back_keys", 0), [])
    return plan(tasks)


def gather_stages(links, position, shard_i, shard_o, wi, wo, lsem):
    x, y, z, core = position
    twin = device_at(x, y, z, 1 - core)
    rows_i, cols_i = shard_i.shape[1:]
    rows_o, cols_o = shard_o.shape[1:]
    quarter_i, quarter_o = rows_i // SIDE, rows_o // SIDE
    third_i = cols_i // LANE * SIDE // 9 // PAIR * WIDE
    half_o = cols_o // PAIR
    cut_o = quarter_o // 16 * ROW + ROW if quarter_o % 16 else quarter_o // PAIR
    place = {"x": x, "y": y, "z": z}

    spots = {(axis, o): step(place[axis], o) for axis in "xyz" for o in range(SIDE)}

    def spot(axis, o):
        return spots[axis, o % SIDE]

    table = {}
    for axis in "xyz":
        for o in range(1, SIDE):
            moved = {**place, axis: spot(axis, o)}
            table[axis, o] = device_at(moved["x"], moved["y"], moved["z"], core)

    def peer(axis, o):
        return table[axis, o % SIDE]

    mats = []
    for l in range(PAIR):
        mats.append((shard_i.at[l], wi.at[l], rows_i, True))
        mats.append((shard_o.at[l], wo.at[l], rows_o, False))

    def region(is_in, color, q):
        if is_in:
            if color == "x":
                lo, hi = PAIR * third_i, cols_i
                rows = (0, rows_i)
            else:
                lo, hi = (0, third_i) if color == "y" else (third_i, PAIR * third_i)
                rows = (q * quarter_i, quarter_i)
            mid = lo + ((hi - lo) // LANE + 1) // PAIR * LANE
            return (rows, (lo, hi - lo)), (rows, (lo, mid - lo)), (rows, (mid, hi - mid))
        cols = (0, half_o) if color == "y" else (half_o, half_o)
        start = q * quarter_o
        return ((start, quarter_o), cols), ((start, cut_o), cols), ((start + cut_o, quarter_o - cut_o), cols)

    def at(m, xb, area):
        (r, nr), (c, nc) = area
        _, out, size, _ = mats[m]
        return out.at[pl.ds(pl.multiple_of((PAIR * xb + core) * size + r, ROW), nr), pl.ds(c, nc)]

    def block(m, xb, index):
        _, out, size, _ = mats[m]
        return out.at[pl.ds(pl.multiple_of((PAIR * xb + index) * size, BAND), size)]

    def group(m, color):
        _, out, _, is_in = mats[m]
        (_, nr), (c, nc) = region(is_in, color, 0)[0]
        return dict(batch=(m, color), whole=out.at[pl.ds(0, nr * (TRIO if color == "x" else 12)), pl.ds(c, nc)])

    def reach(m, color):
        src, _, _, is_in = mats[m]
        area = region(is_in, color, place[color])[0]
        for by in BOTH:
            links.send((m, "x1", color, by), src.at[pl.ds(pl.multiple_of(area[0][0], ROW), area[0][1]), pl.ds(*area[1])], at(m, x, area), peer("x", by), **group(m, color))

    def launch(m, color, off):
        is_in = mats[m][TRIO]
        moved = at(m, spot("x", off), region(is_in, color, place[color])[0])
        for by in BOTH:
            links.send((m, "p1", color, off, by), moved, moved, peer(color, by), **group(m, color))

    def relay(m, color, by):
        is_in = mats[m][TRIO]
        xb = spot("x", -by)
        areas = region(is_in, color, place[color])
        links.arrive((m, "x1", color, by), at(m, xb, areas[0]))
        part = at(m, xb, areas[1] if by == 1 else areas[PAIR])
        links.send((m, "x2", color), part, part, peer("x", by), **group(m, color))
        if color != "x":
            launch(m, color, -by)

    def far(m, color):
        is_in = mats[m][TRIO]
        links.arrive((m, "x2", color), at(m, spot("x", PAIR), region(is_in, color, place[color])[0]))
        if color != "x":
            launch(m, color, PAIR)

    def pass_on(m, color, off, by):
        is_in = mats[m][TRIO]
        xb = spot("x", off)
        areas = region(is_in, color, spot(color, -by))
        links.arrive((m, "p1", color, off, by), at(m, xb, areas[0]))
        part = at(m, xb, areas[1] if by == 1 else areas[PAIR])
        links.send((m, "p2", color, off), part, part, peer(color, by), **group(m, color))

    def close(m, color, off):
        is_in = mats[m][TRIO]
        links.arrive((m, "p2", color, off), at(m, spot("x", off), region(is_in, color, spot(color, PAIR))[0]))

    def four(m):
        _, out, size, _ = mats[m]
        return out.at[pl.ds(0, SIDE * size)]

    def give(m, src, dst):
        links.send((m, "chip"), src, dst, twin, batch=(m, "chip"), whole=four(m))

    def hand(m, off):
        whole = block(m, spot("x", off), core)
        give(m, whole, whole)

    owns = []

    def begin():
        for m, (src, _, _, _) in enumerate(mats):
            copy = pltpu.make_async_copy(src, block(m, x, core), lsem.at[m])
            copy.start()
            owns.append(copy)

    def lend(m):
        give(m, mats[m][0], block(m, x, core))

    def ready(m):
        owns[m].wait()
        links.arrive((m, "chip"), four(m))

    return begin, ready, peer, {"reach": reach, "relay": relay, "far": far, "pass": pass_on, "close": close, "hand": hand, "lend": lend}


BF, F32 = jnp.bfloat16, jnp.float32


def product(a, b, contract=((1,), (0,))):
    return lax.dot_general(a, b, (contract, ((), ())), preferred_element_type=F32)


def lanes(start, size):
    return pl.ds(start if isinstance(start, int) else pl.multiple_of(start, LANE), size)


def layers_kernel(order, sc_ref, wi_ref, wo_ref, x_ref, dy_ref, freq_ref,
                  y_ref, gx_ref, hy_a, hy_b, hz_a, hz_b, mx_a, mx_b, yx_b, zy_b, zz_b, z_a, dy_a, sc_out, relay_z,
                  wi, wo, z, om, h, hid, qr, kts, vsl, ksl, turned_q, turned_o, scores, dscores, pcat, dscat, cos_ref, sin_ref, turn_ref,
                  dot_heads, qt, dht, dkv, omt, ht, dyt, sc, gains, own_gain, gain_ref, load_sems, own_sems, send_sems, recv_sems,
                  share_send_sems, share_recv_sems):
    seq, dim = x_ref.shape
    ff = (wi.shape[PAIR] - dim - LANE) // PAIR
    position = chip_position()
    x, y, zc, core = position
    twin = device_at(x, y, zc, 1 - core)
    me = PAIR * x + core
    links, shared = Links(send_sems, recv_sems), Links(share_send_sems, share_recv_sems)
    stored = []
    spots, _ = around(position)
    h_out, m_out, y_out, z_out = {"y": (hy_a, hy_b), "z": (hz_a, hz_b)}, (mx_a, mx_b), {1: yx_b}, {(1, "y"): zy_b, (1, "z"): zz_b}
    middle = hid.at[1]
    begin, ready, peer, stages = gather_stages(links, position, wi_ref, wo_ref, wi, wo, load_sems)
    others = [(zc * SIDE + y, rem(me + k, ROW)) for k in range(1, ROW)]

    def spot(axis, o):
        return spots[axis, o % SIDE]

    def device(axis, o, index):
        moved = {"x": x, "y": y, "z": zc, axis: spot(axis, o)}
        return device_at(moved["x"], moved["y"], moved["z"], index)

    own_gain[ALL] = jnp.zeros(own_gain.shape, F32)
    count = sc_ref.shape[1]
    for f in range(ROW):
        @pl.when(me == f)
        def _():
            own_gain[0:PAIR, f * count:(f + 1) * count] = sc_ref[ALL].astype(F32)
    announce(others + [device(axis, o, index) for axis in "yz" for o in AROUND for index in range(PAIR)])
    begin()
    for k, far in enumerate(others):
        links.send(("sc",), own_gain, gains.at[me], far, batch=("sc",), whole=gains.at[pl.ds(0, OTHERS)])

    def keep(src, dst):
        copy = pltpu.make_async_copy(src, dst, own_sems.at[len(stored)])
        copy.start()
        stored.append(copy)

    def tokens(axis, o, index):
        return pl.ds(pl.multiple_of((PAIR * spot(axis, o) + index) * seq, seq), seq)

    def place(axis, o, index):
        return PAIR * spot(axis, o) + index

    def columns(axis, o):
        size = z.shape[PAIR] // ROW
        return lanes(((0 if axis == "y" else SIDE) + spot(axis, o)) * size, size)

    def several(batch, ref, n):
        whole = ref.at[pl.ds(0, n * seq if batch[0][0] in "yz" else n)]
        return dict(batch=batch, whole=whole)

    def send_h(l, axis):
        out = h_out[axis][l].at[place(axis, 0, core)]
        for by in BOTH:
            for index in range(PAIR):
                shared.send(("h", l, axis, by), ht.at[l, :, index], out, device(axis, by, index), lane=core, **several(("h", l, axis), h_out[axis][l], OTHERS))
        shared.send(("h", l, axis), ht.at[l, :, 1 - core], out, twin, **several(("h", l, axis), h_out[axis][l], OTHERS))
        keep(ht.at[l, :, core], out)

    def pass_h(l, axis, by, index):
        out = h_out[axis][l]
        shared.arrive(("h", l, axis, by), out.at[place(axis, -by, index)], index)
        part = out.at[place(axis, -by, index), pl.ds(1 - by, PAIR)]
        shared.send(("h", l, axis), part, part, device(axis, by, core), **several(("h", l, axis), out, OTHERS))

    def arrive_h(l):
        for axis in "yz":
            shared.arrive(("h", l, axis), h_out[axis][l].at[pl.ds(0, TRIO)])

    def row_block(l, o, index):
        size = omt.shape[1] // ROW
        return omt.at[l, pl.ds(pl.multiple_of((PAIR * spot("x", o) + index) * size, BAND), size)]

    def send_m(l):
        out, batch = m_out[l].at[place("x", 0, core)], several(("m", l), m_out[l], OTHERS)
        for o in AROUND:
            for index in range(PAIR):
                shared.send(("m", l), row_block(l, o, index), out, device("x", o, index), **batch)
        shared.send(("m", l), row_block(l, 0, 1 - core), out, twin, **batch)
        keep(row_block(l, 0, core), out)

    def arrive_m(l):
        shared.arrive(("m", l), m_out[l].at[pl.ds(0, OTHERS)])

    def token_half(axis, o, k):
        return pl.ds(pl.multiple_of((PAIR * spot(axis, o) + core) * seq + k * (seq // PAIR), seq // PAIR), seq // PAIR)

    def send_y(l):
        src, out = dy_ref, y_out[l].at[tokens("x", 0, core)]
        for by in BOTH:
            shared.send(("y", l, by), src, out, device("x", by, core), **several(("y", l), y_out[l], OTHERS))
        shared.send(("y", l), src, out, twin, **several(("y", l), y_out[l], OTHERS))
        keep(src, out)

    def pass_y(l, by):
        landed, part = y_out[l].at[tokens("x", -by, core)], y_out[l].at[token_half("x", -by, (1 - by) // PAIR)]
        shared.arrive(("y", l, by), landed)
        shared.send(("y2", l), part, part, device("x", by, core), **several(("y", l), y_out[l], OTHERS))
        shared.send(("y", l), landed, landed, twin, **several(("y", l), y_out[l], OTHERS))

    def far_y(l):
        landed = y_out[l].at[tokens("x", PAIR, core)]
        shared.arrive(("y2", l), landed)
        shared.send(("y", l), landed, landed, twin, **several(("y", l), y_out[l], OTHERS))

    def arrive_y(l):
        shared.arrive(("y", l), y_out[l].at[pl.ds(0, SIDE * seq)])

    def push_z(l, axis, o, ready):
        out = z_out[l, axis].at[tokens(axis, 0, core)]
        batch = several(("z", l, axis), z_out[l, axis], ROW)

        def start():
            if o != PAIR:
                shared.send(("z", l, axis, o), z.at[l, :, columns(axis, o)], out, device(axis, o, core), **batch)
                return
            for k, by in enumerate(BOTH):
                shared.send(("zr", l, axis, by), z.at[l, pl.ds(k * (seq // PAIR), seq // PAIR), columns(axis, PAIR)], relay_z.at[l, "yz".index(axis), k],
                            device(axis, by, core), **batch)

        if ready is None:
            start()
        else:
            pl.when(ready)(start)

    def own_part(l, axis):
        out, mine = z_out[l, axis].at[tokens(axis, 0, core)], z.at[l, :, columns(axis, 0)]
        shared.send(("z", l, axis), mine, out, twin, **several(("z", l, axis), z_out[l, axis], ROW))
        keep(mine, out)

    def send_z(l, axis):
        for o in (PAIR, 1, -1):
            push_z(l, axis, o, spot(axis, o) != 0 if axis == "y" else None)
        if axis == "z":
            own_part(l, axis)

    def rest_z(l):
        for o in (PAIR, 1, -1):
            push_z(l, "y", o, spot("y", o) == 0)
        own_part(l, "y")

    def pass_z(l, axis, by):
        k = (1 - by) // PAIR
        half = relay_z.at[l, "yz".index(axis), k]
        shared.arrive(("zr", l, axis, by), half)
        shared.send(("z2", l, axis), half, z_out[l, axis].at[token_half(axis, -by, k)], device(axis, by, core), **several(("z", l, axis), z_out[l, axis], ROW))

    def twin_z(l, axis, by):
        landed = z_out[l, axis].at[tokens(axis, -by, core)]
        shared.arrive(("z", l, axis, by), landed)
        shared.send(("z", l, axis), landed, landed, twin, **several(("z", l, axis), z_out[l, axis], ROW))

    def far_z(l, axis):
        landed = z_out[l, axis].at[tokens(axis, PAIR, core)]
        shared.arrive(("z2", l, axis), landed)
        shared.send(("z", l, axis), landed, landed, twin, **several(("z", l, axis), z_out[l, axis], ROW))

    def arrive_z(l, axis):
        shared.arrive(("z", l, axis), z_out[l, axis].at[pl.ds(0, SIDE * seq)])

    def send_scale(l):
        for far in others:
            shared.send(("scale", l), sc.at[l], sc_out.at[l, me], far, batch=("scale", l), whole=sc_out.at[l, pl.ds(0, OTHERS)])
        keep(sc.at[l], sc_out.at[l, me])

    def arrive_scale(l):
        shared.arrive(("scale", l), sc_out.at[l, pl.ds(0, OTHERS)])

    gains[me] = own_gain[ALL]
    z[:, :, wi.shape[PAIR]:] = jnp.zeros((PAIR, seq, z.shape[PAIR] - wi.shape[PAIR]), BF)
    entry = (x_ref, hid.at[0])
    angle = lax.broadcasted_iota(jnp.int32, (seq, LANE), 0).astype(F32) * freq_ref[0:1]
    for half in range(PAIR):
        cos_ref[:, LANE * half:LANE * (half + 1)] = jnp.cos(angle)
        sin_ref[:, LANE * half:LANE * (half + 1)] = jnp.sin(angle)
    lane = lax.broadcasted_iota(jnp.int32, turn_ref.shape, 1)
    down = lax.broadcasted_iota(jnp.int32, turn_ref.shape, 0) - lane
    low = rem(lane, HEAD) < BAND
    turn_ref[ALL] = jnp.where(low & (down == BAND), -1.0, jnp.where(jnp.logical_not(low) & (down == -BAND), 1.0, ZERO)).astype(BF)
    kts[ALL] = jnp.zeros(kts.shape, BF)
    pcat[ALL] = jnp.zeros(pcat.shape, BF)
    dscat[ALL] = jnp.zeros(dscat.shape, BF)

    def normalise(l, src):
        @pl.loop(0, seq // BAND, unroll=SIDE)
        def _(r):
            rows = pl.ds(pl.multiple_of(r * BAND, BAND), BAND)
            v = src[rows].astype(F32)
            v = v - jnp.mean(v, axis=-1, keepdims=True)
            var = jnp.mean(v * v, axis=-1, keepdims=True)
            h[l, rows] = (v * lax.rsqrt(var + 1e-6) * gain_ref[l:l + 1]).astype(BF)

    def project(l):
        strip = wi.shape[PAIR] // 5

        @pl.loop(0, 5)
        def _(i):
            at = lanes(i * strip, strip)
            z[l, :, at] = product(h[l], wi[l, :, at]).astype(BF)

    def heads(l):
        cos, sin = cos_ref[ALL], sin_ref[ALL]
        for g in range(dim // WIDE):
            q = z[l, :, g * WIDE:(g + 1) * WIDE]
            qr[l, :, g * WIDE:(g + 1) * WIDE] = ((q.astype(F32) * cos + product(q, turn_ref[ALL]) * sin) * 0.125).astype(BF)
        kv = z[l, :, dim:dim + LANE]
        turned = kv.astype(F32) * cos[:, :LANE] + product(kv, turn_ref[:LANE, :LANE]) * sin[:, :LANE]
        first = lax.broadcasted_iota(jnp.int32, turned.shape, 1) < HEAD
        key_lo = jnp.where(first, turned, ZERO)
        val_hi = jnp.where(first, ZERO, kv.astype(F32))
        return key_lo, pltpu.roll(key_lo, HEAD, 1), pltpu.roll(val_hi, HEAD, 1), val_hi

    def slot_rows(ref, lo, hi):
        zero = jnp.zeros((seq, LANE), BF)
        lo, hi = lo.astype(BF), hi.astype(BF)
        for i, (left, right) in enumerate(((lo, zero), (hi, zero), (zero, lo), (zero, hi))):
            ref[i * seq:(i + 1) * seq, :LANE] = left
            ref[i * seq:(i + 1) * seq, LANE:] = right

    def slot_cols(ref, lo):
        flat = lo.T[:HEAD].astype(BF)
        for i in range(SIDE):
            ref[HEAD * i:HEAD * (i + 1), i * seq:(i + 1) * seq] = flat

    def chances(i, half):
        at = slice(LANE * half, LANE * (half + 1))
        blocks = [pl.ds(pl.multiple_of(i * seq + LANE * k, LANE), LANE) for k in range(half + 1)]
        s = [scores[keys, at] for keys in blocks]
        lower = lax.broadcasted_iota(jnp.int32, s[-1].shape, 1) >= lax.broadcasted_iota(jnp.int32, s[-1].shape, 0)
        s[-1] = jnp.where(lower, s[-1], -1e30)
        top = functools.reduce(jnp.maximum, [jnp.max(v, axis=0, keepdims=True) for v in s])
        e = [jnp.exp(v - top) for v in s]
        scale = 1.0 / sum(jnp.sum(v, axis=0, keepdims=True) for v in e)
        return at, [(keys, v * scale) for keys, v in zip(blocks, e)]

    def attend(l):
        key_lo, key_hi, val_lo, _ = heads(l)
        slot_rows(ksl, key_lo, key_hi)
        slot_cols(kts, val_lo)
        flip(lambda at: qr[l, :, lanes(at, WIDE)], qt, dim)

        @pl.loop(0, dim // WIDE)
        def _(g):
            rows = pl.ds(pl.multiple_of(g * WIDE, WIDE), WIDE)
            scores[ALL] = product(ksl[ALL], qt[rows])

            @pl.loop(0, SIDE)
            def _(i):
                for half in range(PAIR):
                    at, blocks = chances(i, half)
                    for keys, p in blocks:
                        pcat[keys, at] = p.astype(BF)
            flat = product(kts[ALL], pcat[ALL]).astype(BF)
            omt[l, rows] = flat
            om[:, lanes(g * WIDE, WIDE)] = flat.T

    def mlp(l):
        @pl.loop(0, seq // BAND)
        def _(r):
            rows = pl.ds(pl.multiple_of(r * BAND, BAND), BAND)

            @pl.loop(0, ff // STRIP)
            def _(i):
                gate = z[l, rows, lanes(dim + LANE + i * STRIP, STRIP)].astype(F32)
                up = z[l, rows, lanes(dim + LANE + ff + i * STRIP, STRIP)].astype(F32)
                om[rows, lanes(dim + i * STRIP, STRIP)] = (gate * jax.nn.sigmoid(gate) * up).astype(BF)

    def put_out(l, dst):
        for n in range(dim // WIDE):
            cols = slice(n * WIDE, (n + 1) * WIDE)
            total = product(om[ALL], wo[l, :, cols])
            dst[:, cols] = (entry[l][:, cols].astype(F32) + total).astype(BF)

    def flip(src, dst, width, first=0):
        @pl.loop(first // WIDE, width // WIDE)
        def _(i):
            dst[pl.ds(pl.multiple_of(i * WIDE, WIDE), WIDE)] = src(i * WIDE).T

    upstream = (middle, dy_ref)

    def back_out(l):
        dy = upstream[l]
        flip(lambda at: dy[:, lanes(at, WIDE)], dyt, dim)

        @pl.loop(0, wo.shape[1] // dim)
        def _(n):
            rows = pl.ds(pl.multiple_of(n * dim, dim), dim)
            part = product(wo[l, rows], dyt[ALL]).astype(BF)
            om[:, lanes(n * dim, dim)] = part.T

            @pl.when(n == 0)
            def _():
                dot_heads[ALL] = part

    def back_mlp(l):
        @pl.loop(0, seq // BAND)
        def _(r):
            rows = pl.ds(pl.multiple_of(r * BAND, BAND), BAND)

            @pl.loop(0, ff // STRIP)
            def _(i):
                gate_at, up_at = lanes(dim + LANE + i * STRIP, STRIP), lanes(dim + LANE + ff + i * STRIP, STRIP)
                gate, up = z[l, rows, gate_at].astype(F32), z[l, rows, up_at].astype(F32)
                d = om[rows, lanes(dim + i * STRIP, STRIP)].astype(F32)
                sig = jax.nn.sigmoid(gate)
                du = d * up
                z[l, rows, gate_at] = (du * sig + du * gate * (sig * (1.0 - sig))).astype(BF)
                z[l, rows, up_at] = (d * (gate * sig)).astype(BF)

    def back_heads(l):
        key_lo, key_hi, val_lo, val_hi = heads(l)
        slot_rows(ksl, key_lo, key_hi)
        slot_rows(vsl, val_lo, val_hi)
        slot_cols(kts, key_lo)
        dkv[ALL] = jnp.zeros(dkv.shape, F32)
        flip(lambda at: qr[l, :, lanes(at, WIDE)], qt, dim)
        for at in range(0, dim, LANE):
            pair = slice(at, at + LANE)
            turned_q[:, pair] = pltpu.roll(qr[l, :, pair].astype(F32), HEAD, 1).astype(BF)
            turned_o[:, pair] = pltpu.roll(om[:, pair].astype(F32), HEAD, 1).astype(BF)

    def back_quad(l):
        @pl.loop(0, dim // WIDE)
        def _(g):
            quad(l, g)

    def quad(l, g):
        cols = pl.ds(pl.multiple_of(g * WIDE, WIDE), WIDE)
        scores[ALL] = product(ksl[ALL], qt[cols])
        dscores[ALL] = product(vsl[ALL], dot_heads[cols])

        @pl.loop(0, SIDE)
        def _(i):
            for half in range(PAIR):
                at, blocks = chances(i, half)
                given = [p * dscores[keys, at].astype(BF).astype(F32) for keys, p in blocks]
                total = sum(jnp.sum(v, axis=0, keepdims=True) for v in given)
                for (keys, p), v in zip(blocks, given):
                    pcat[keys, at] = p.astype(BF)
                    dscat[keys, at] = (v - p * total).astype(BF)
        dq = product(kts[ALL], dscat[ALL]).astype(BF).T
        back = dq.astype(F32) * cos_ref[ALL] - product(dq, turn_ref[ALL]) * sin_ref[ALL]
        z[l, :, cols] = (back * 0.125).astype(BF)
        def pieces(left, even, odd):
            for i in range(SIDE):
                pair = lanes(g * WIDE + i // PAIR * LANE, LANE)
                yield product(left[i * seq:(i + 1) * seq, :], odd(pair) if i % PAIR else even(pair))

        dkv[0] += sum(pieces(dscat, lambda at: qr[l, :, at], lambda at: turned_q[:, at]))
        dkv[1] += sum(pieces(pcat, lambda at: turned_o[:, at], lambda at: om[:, at]))

    def back_keys(l):
        dk = dkv[0].astype(BF)
        turned = dk.astype(F32) * cos_ref[:, :LANE] - product(dk, turn_ref[:LANE, :LANE]) * sin_ref[:, :LANE]
        first = lax.broadcasted_iota(jnp.int32, turned.shape, 1) < HEAD
        z[l, :, dim:dim + LANE] = jnp.where(first, turned, dkv[1]).astype(BF)

    def back_in(l, half):
        width = wi.shape[PAIR] // 5
        at = slice(PAIR * half * width, (PAIR + TRIO * half) * width)
        part = product(wi[l, :, at], z[l, :, at], ((1,), (1,)))
        dht[ALL] = dht[ALL] + part if half else part

    def back_norm(l):
        dy, dst = upstream[l], (gx_ref, middle)[l]
        for i in range(dim // WIDE):
            cols = slice(i * WIDE, (i + 1) * WIDE)
            h[l, :, cols] = dht[cols].T.astype(BF)
        sc[l] = jnp.zeros(sc.shape[1:], F32)

        @pl.loop(0, seq // BAND, unroll=SIDE)
        def _(r):
            rows = pl.ds(pl.multiple_of(r * BAND, BAND), BAND)
            v = entry[l][rows].astype(F32)
            v = v - jnp.mean(v, axis=-1, keepdims=True)
            scale = lax.rsqrt(jnp.mean(v * v, axis=-1, keepdims=True) + 1e-6)
            hat = v * scale
            d = h[l, rows].astype(F32)
            each = (d * hat).reshape(SIDE, ROW, dim)
            sc[l] += (each[0] + each[1]) + (each[PAIR] + each[TRIO])
            d = d * gain_ref[l:l + 1]
            d = scale * (d - jnp.mean(d, axis=-1, keepdims=True) - hat * jnp.mean(d * hat, axis=-1, keepdims=True))
            dst[rows] = (dy[rows].astype(F32) + d.astype(BF).astype(F32)).astype(BF)

    def do_norm(l):
        if l == 0:
            links.arrive(("sc",), gains.at[pl.ds(0, OTHERS)])
            gain_ref[ALL] = jnp.sum(gains[ALL], axis=0)
        normalise(l, entry[l])
        for i in range(dim // WIDE):
            flat = h[l, :, i * WIDE:(i + 1) * WIDE].T
            size = ht.shape[TRIO]
            for b in range(ROW):
                lo, hi = max(b * size, i * WIDE), min((b + 1) * size, (i + 1) * WIDE)
                if lo < hi:
                    ht[l, b // PAIR, b % PAIR, lo - b * size:hi - b * size] = flat[lo - i * WIDE:hi - i * WIDE]

    def do_project(l):
        ready(PAIR * l)
        project(l)

    def do_mlp(l):
        mlp(l)
        flip(lambda at: om[:, lanes(at, WIDE)], omt.at[l], om.shape[1], dim)

    def do_put(l):
        ready(PAIR * l + 1)
        put_out(l, hid.at[0] if l == 0 else y_ref)

    stages.update(
        norm=do_norm, project=do_project, attend=attend, mlp=do_mlp, put=do_put, back_out=back_out, back_mlp=back_mlp, back_heads=back_heads,
        back_quad=back_quad, back_keys=back_keys, back_in=back_in, back_norm=back_norm, send_h=send_h, pass_h=pass_h, send_m=send_m, send_y=send_y, pass_y=pass_y, far_y=far_y, send_z=send_z, rest_z=rest_z, pass_z=pass_z, twin_z=twin_z, far_z=far_z,
        send_scale=send_scale, own_z=lambda: keep(z.at[0], z_a), own_y=lambda: keep(middle, dy_a))
    for kind, *task in order:
        stages[kind](*task)
    for l in range(PAIR):
        arrive_h(l)
        arrive_m(l)
        arrive_scale(l)
    arrive_y(1)
    for l, axis in z_out:
        arrive_z(l, axis)
    for copy in stored:
        copy.wait()
    shared.drain()
    links.drain()


def run_layers(x, dy, scale, w_in, w_out, freq, starts=(ZERO, 10.0, 20.0, 30.0)):
    seq, dim = x.shape
    proj, cat = w_in.shape[PAIR], ROW * w_out.shape[1]
    wide = proj + LANE
    hbm, vmem = pl.BlockSpec(memory_space=pltpu.HBM), pl.BlockSpec(memory_space=pltpu.VMEM)
    out = lambda *shape, dtype=BF: jax.ShapeDtypeStruct(shape, dtype)
    buffer = lambda *shape, dtype=BF: pltpu.VMEM(shape, dtype)
    sem = pltpu.SemaphoreType.DMA
    line = ROW * seq
    return pl.pallas_call(
        functools.partial(layers_kernel, layers_order(*w_in.shape[1:], *w_out.shape[1:], seq, starts)),
        out_shape=(out(seq, dim), out(seq, dim), *[out(ROW, SIDE, dim // ROW, seq)] * SIDE, *[out(ROW, cat // ROW, seq)] * PAIR, out(line, dim),
                   *[out(line, wide // ROW)] * PAIR, out(seq, wide), out(seq, dim), out(PAIR, ROW, ROW, dim, dtype=F32),
                   out(PAIR, PAIR, PAIR, seq // PAIR, wide // ROW)),
        in_specs=[vmem, hbm, hbm] + [vmem] * TRIO,
        out_specs=[vmem] * PAIR + [hbm] * 13,
        scratch_shapes=[
            buffer(PAIR, dim, proj), buffer(PAIR, cat, dim), buffer(PAIR, seq, wide), buffer(seq, cat), buffer(PAIR, seq, dim),
            buffer(PAIR, seq, dim), buffer(PAIR, seq, dim),
            buffer(WIDE, SIDE * seq), buffer(SIDE * seq, WIDE), buffer(SIDE * seq, WIDE), buffer(seq, dim), buffer(seq, dim),
            buffer(SIDE * seq, seq, dtype=F32), buffer(SIDE * seq, seq, dtype=F32), buffer(SIDE * seq, seq), buffer(SIDE * seq, seq),
            buffer(seq, WIDE, dtype=F32), buffer(seq, WIDE, dtype=F32), buffer(WIDE, WIDE),
            buffer(dim, seq), buffer(dim, seq), buffer(dim, seq, dtype=F32), buffer(PAIR, seq, LANE, dtype=F32),
            buffer(PAIR, cat, seq), buffer(PAIR, SIDE, PAIR, dim // ROW, seq), buffer(dim, seq), buffer(PAIR, ROW, dim, dtype=F32),
            buffer(ROW, ROW, dim, dtype=F32), buffer(ROW, dim, dtype=F32), buffer(ROW, dim, dtype=F32),
            sem((SIDE,)), sem((13,)), sem((15,)), sem((107,)), sem((11,)), sem((40,)),
        ],
        compiler_params=pltpu.CompilerParams(collective_id=PAIR, has_side_effects=True, vmem_limit_bytes=67043328),
        name="run_layers",
    )(scale, w_in, w_out, x, dy, freq)


PARTS = (("i", "x", "z", "y", 0, STRIP), ("i", "x", "z", "y", STRIP, 384), ("i", "x", "y", "z", 0, STRIP), ("i", "x", "y", "z", STRIP, 384),
         ("o", "y", "z", "y", 0, 384), ("o", "z", "y", "z", 384, 384))


def reduce_order(rows, rows_b, starts):
    rate = 11650.0
    tasks = []
    sizes = {"y": WIDE * 896 / (PAIR * rate), "z": WIDE * 896 / (PAIR * rate), "x": WIDE * 768 / (PAIR * rate)}
    for axis in "yzx":
        size = sizes[axis]
        tasks.append((("swap", axis), (0, 0), starts[PAIR] if axis == "x" else starts[TRIO], [], [],
                      [((axis, by), size * n) for by, n in ((-1, 0.5), (1, 1), (-1, 1), (1, 1))], SHORT))
        tasks.append((("relay", axis), (0, 0), ZERO, [(("swap", axis), 0)], [], [((axis, -1), size / PAIR)], SHORT))
        for o, needs in ((1, [(("swap", axis), 1)]), (-1, [(("swap", axis), PAIR)]), (PAIR, [(("swap", axis), TRIO), (("relay", axis), 0)])):
            tasks.append((("near", axis, o), (0, PAIR), ZERO, needs, [], [("chip", 1.6)], QUICK))
    tasks.append((("fetch", 0), (5, 0), ZERO, [], [("make", 1, len(PARTS) - 1)], [], QUICK))
    for l in (1, 0):
        late = 1 - l
        for c, (kind, first, then, last, at, width) in enumerate(PARTS):
            needs, cost = [], 1.6 * width / STRIP
            if l == 0:
                needs = [(("near", last if kind == "i" else "x", o), 0) for o in AROUND]
            tasks.append((("make", l, c), (9 * late, c), starts[late], needs, [] if l else [("fetch", 0)], [], cost))
            full = SIDE * SIDE * (rows if kind == "i" else rows_b) * width / rate
            sends = [[((first, by), full / ROW) for by in BOTH], [((first, by), full / SIDE) for by in BOTH],
                     [((then, o), full / 16) for o in (1, -1, 1)], []]
            piece = full / 16
            sends += [[((then, o), piece) for o in (1, -1, 1)], [((last, by), SIDE * piece) for by in BOTH],
                      [((last, by), PAIR * piece) for by in BOTH], []]
            for s in range(ROW):
                task = ("sum", l, c, s)
                needs = [(("sum", l, c, s - 1), k) for k in range(len(sends[s - 1]))] if s else []
                tasks.append((task, (late, -s), ZERO, needs, [("make", l, c)] if s == 0 else [("sum", l, c, s - 1)], sends[s], SHORT))
    return plan(tasks)


def reduce_kernel(order, *refs):
    hy, hz, mx = refs[0:PAIR], refs[PAIR:SIDE], refs[SIDE:6]
    yx1, zy1, zz1, z0, y0, sc = refs[6:12]
    oa, ob = refs[12:14]
    n = len(PARTS)
    total, half, full, small, front = (refs[14 + k * n:14 + (k + 1) * n] for k in range(5))
    (hbuf, zbuf, mbuf, ybuf, scbuf, rz, ry, ssem, rsem, isem, osem) = refs[14 + 5 * n:]
    position = chip_position()
    x, y, zc, core = position
    place = {"x": x, "y": y, "z": zc}
    twin = device_at(x, y, zc, 1 - core)
    spots, peers = around(position)

    def spot(axis, o):
        return spots[axis, o % SIDE]

    def peer(axis, o):
        return peers[axis, o % SIDE]

    seq, wide = z0.shape
    own = wide // ROW
    loads, moving = {}, []

    def load(key, src, dst):
        copy = pltpu.make_async_copy(src, dst, isem.at[len(moving)])
        moving.append(key)
        copy.start()
        loads[key] = copy

    def fetch(l):
        if l:
            load(("z", 1, "y"), zy1, zbuf.at[1, 0])
        load(("h", l, "y"), hy[l], hbuf.at[l, 0])
        if l:
            load(("z", 1, "z"), zz1, zbuf.at[1, 1])
        load(("h", l, "z"), hz[l], hbuf.at[l, 1])
        load(("m", l), mx[l], mbuf.at[l])
        if l:
            load(("y", 1), yx1, ybuf.at[1])
        load(("s", l), sc.at[l], scbuf.at[l])

    fetch(1)
    done = set()

    def loaded(*keys):
        for key in keys:
            if key not in done:
                loads[key].wait()
                done.add(key)

    announce([peer(axis, o) for axis in "xyz" for o in AROUND] + [twin])
    links = Links(ssem, rsem)

    def columns(axis, o):
        return lanes(((0 if axis == "y" else SIDE) + spot(axis, o)) * own, own)

    def tokens(axis, o, index):
        return pl.ds(pl.multiple_of((PAIR * spot(axis, o) + index) * seq, seq), seq)

    def target(axis):
        return ybuf.at[0] if axis == "x" else zbuf.at[0, "yz".index(axis)]

    def leaving(axis):
        return dict(batch=("swap", axis), whole=target(axis).at[pl.ds(0, OTHERS * seq + seq // PAIR)])

    def half_at(axis, o, k):
        start = (PAIR * spot(axis, o) + core) * seq + k * (seq // PAIR)
        return target(axis).at[pl.ds(pl.multiple_of(start, seq // PAIR), seq // PAIR)]

    def relay_of(axis):
        return ry if axis == "x" else rz.at["yz".index(axis)]

    def swap(axis):
        def part(o, rows=slice(None)):
            return y0.at[rows] if axis == "x" else z0.at[rows, columns(axis, o)]

        mine = target(axis).at[tokens(axis, 0, core)]
        links.send(("relay", axis), part(PAIR, pl.ds(seq // PAIR, seq // PAIR)), relay_of(axis), peer(axis, -1), **leaving(axis))
        for by in BOTH:
            links.send(("swap", axis, by), part(by), mine, peer(axis, by), **leaving(axis))
        links.send(("swap", axis, PAIR), part(PAIR, pl.ds(0, seq // PAIR)), half_at(axis, 0, 0), peer(axis, PAIR), **leaving(axis))
        links.send(("near", axis), part(0), mine, twin, **leaving(axis))
        load(("own", axis), part(0), mine)

    def relay(axis):
        links.arrive(("relay", axis), relay_of(axis))
        links.send(("relayed", axis), relay_of(axis), half_at(axis, 1, 1), peer(axis, -1), **leaving(axis))

    def near(axis, o):
        landed = target(axis).at[tokens(axis, -o, core)]
        if o == PAIR:
            links.arrive(("swap", axis, PAIR), half_at(axis, PAIR, 0))
            links.arrive(("relayed", axis), half_at(axis, PAIR, 1))
        else:
            links.arrive(("swap", axis, o), landed)
        links.send(("near", axis), landed, landed, twin, **leaving(axis))

    def joined(axis):
        if axis not in done:
            done.add(axis)
            loaded(("own", axis))
            links.arrive(("near", axis), target(axis).at[pl.ds(0, SIDE * seq)])

    def joined_lanes(ref, l, i):
        return jnp.concatenate([ref[l, i, k].reshape(-1, ref.shape[-1]) for k in range(ROW)], axis=1)

    def make(l, c):
        kind, first, then, last, at, width = PARTS[c]
        if kind == "i":
            i = "yz".index(last)
            loaded(("h", l, last))
            if l:
                loaded(("z", l, last))
            else:
                joined(last)
            size = total[c].shape[TRIO]
            for lo in range(0, width, WIDE):
                hi = min(width, lo + WIDE)
                part = product(joined_lanes(hbuf, l, i), zbuf[l, i, :, at + lo:at + hi])
                for r in range(16):
                    total[c][l, r // SIDE, r % SIDE, :, lo:hi] = part[r * size:(r + 1) * size]
            return
        loaded(("m", l), ("s", l))
        if l:
            loaded(("y", l))
        else:
            joined("x")
        part = product(jnp.concatenate([mbuf[l, k] for k in range(ROW)], axis=1), ybuf[l, :, at:at + width])
        size = total[c].shape[TRIO]

        def put(r, value):
            total[c][(l, r // SIDE, r % SIDE) if first == "y" else (l, r % SIDE, r // SIDE)] = value

        for r in range(part.shape[0] // size):
            put(r, part[r * size:(r + 1) * size])
        gain = jnp.sum(jnp.sum(scbuf[l, :, :, at:at + width], axis=0), axis=0, keepdims=True)
        row = lax.broadcasted_iota(jnp.int32, (size, width), 0)
        put(15, jnp.where(row == 0, gain, ZERO))

    def area(l, c, o, whole):
        kind, first, then, last, at, width = PARTS[c]
        inner = (spot(then, whole) if isinstance(whole, int) else whole)
        outer = spot(last, o)
        if kind == "i":
            cols = lanes(((0 if last == "y" else SIDE) + outer) * own + at, width)
            return oa.at[l, inner, :, cols]
        cols = pl.ds(at, width)
        return ob.at[l, outer, inner, :, cols] if last == "y" else ob.at[l, inner, outer, :, cols]

    def add(l, c, s):
        kind, first, then, last, at, width = PARTS[c]
        t = total[c].at[l]
        sums = dict(batch=(l, c, 0), whole=t)
        lines = dict(batch=(l, c, 1), whole=t.at[pl.ds(0, PAIR)])
        singles = dict(batch=(l, c, PAIR), whole=t.at[pl.ds(0, PAIR), pl.ds(0, TRIO)])
        if s == 0:
            far = t.at[spot(first, PAIR)]
            for k, by in enumerate(BOTH):
                links.send((l, c, "half"), far.at[pl.ds(PAIR * k, PAIR)], half[c].at[l, k], peer(first, by), **sums)
        elif s == 1:
            links.arrive((l, c, "half"), half[c].at[l])
            for k, by in enumerate(BOTH):
                mine = t.at[spot(first, by)]
                add_into(mine.at[pl.ds(PAIR * k, PAIR)], half[c].at[l, k])
                links.send((l, c, "full"), mine, full[c].at[l, k], peer(first, by), **sums)
        elif s == PAIR:
            mine = t.at[spot(first, 0)]
            links.arrive((l, c, "full"), full[c].at[l])
            for k in range(PAIR):
                add_into(mine, full[c].at[l, k])
            for k, o in enumerate(AROUND):
                links.send((l, c, "small"), mine.at[spot(then, o)], small[c].at[l, k], peer(then, o), **singles)
        elif s == TRIO:
            links.arrive((l, c, "small"), small[c].at[l])
            mine = t.at[spot(first, 0), spot(then, 0)]
            front[c][l] = (mine[ALL] + small[c][l, 0]) + (small[c][l, 1] + small[c][l, PAIR])
        elif s == SIDE:
            src, dst = front[c].at[l], area(l, c, 0, 0)
            for o in AROUND:
                links.send((l, c, "a1"), src, dst, peer(then, o), **singles)
            copy = pltpu.make_async_copy(src, dst, osem.at[l, c])
            copy.start()
            loads["front", l, c] = copy
        elif s == 5:
            loaded(("front", l, c))
            links.arrive((l, c, "a1"), t.at[0, pl.ds(0, TRIO)])
            line = area(l, c, 0, slice(None))
            for by in BOTH:
                links.send((l, c, "a2"), line, line, peer(last, by), **lines)
        elif s == 6:
            links.arrive((l, c, "a2"), t.at[pl.ds(0, PAIR)])
            for k, by in enumerate(BOTH):
                part = area(l, c, -by, pl.ds(PAIR * k, PAIR))
                links.send((l, c, "a3"), part, part, peer(last, by), **sums)
        else:
            links.arrive((l, c, "a3"), area(l, c, PAIR, slice(None)))

    stages = {"swap": swap, "relay": relay, "near": near, "fetch": fetch, "make": make, "sum": add}
    for kind, *task in order:
        stages[kind](*task)
    links.drain()


def add_into(dst, src):
    @pl.loop(0, dst.shape[0])
    def _(i):
        if len(dst.shape) == SIDE:
            for j in range(dst.shape[1]):
                dst[i, j] += src[i, j]
        else:
            dst[i] += src[i]


def around(position):
    place, core = dict(zip("xyz", position)), position[TRIO]
    spots = {(axis, o): step(place[axis], o) for axis in "xyz" for o in range(SIDE)}
    peers = {}
    for axis in "xyz":
        for o in range(1, SIDE):
            moved = {**place, axis: spots[axis, o]}
            peers[axis, o] = device_at(moved["x"], moved["y"], moved["z"], core)
    return spots, peers


def reduce_gradients(operands, starts=(ZERO, ZERO, 20.0, 3.0)):
    hbm = pl.BlockSpec(memory_space=pltpu.HBM)
    h_rows, m_rows, y_cols, z_cols, z_own, y_own, scale_parts = operands
    part, part_b = h_rows[0].shape[PAIR] // SIDE, (m_rows[0].shape[1] + BAND) // 16
    (line, dim), wide = y_cols.shape, z_own.shape[1]
    out = lambda *shape: jax.ShapeDtypeStruct(shape, F32)
    sem = pltpu.SemaphoreType.DMA

    def buffers(*lead):
        return [pltpu.VMEM((PAIR, *lead, part if e[0] == "i" else part_b, e[5]), F32) for e in PARTS]

    return pl.pallas_call(
        functools.partial(reduce_kernel, reduce_order(part, part_b, starts)),
        out_shape=(out(PAIR, SIDE, part, wide), out(PAIR, SIDE, SIDE, part_b, dim)),
        in_specs=[hbm] * 12,
        out_specs=[hbm] * PAIR,
        scratch_shapes=[
            *buffers(SIDE, SIDE), *buffers(PAIR, PAIR), *buffers(PAIR, SIDE), *buffers(TRIO), *buffers(),
            pltpu.VMEM((PAIR, PAIR, *h_rows[0].shape), BF), pltpu.VMEM((PAIR, PAIR, line, wide // ROW), BF), pltpu.VMEM((PAIR, *m_rows[0].shape), BF),
            pltpu.VMEM((PAIR, line, dim), BF), pltpu.VMEM(scale_parts.shape, F32),
            pltpu.VMEM((PAIR, z_own.shape[0] // PAIR, wide // ROW), BF), pltpu.VMEM((y_own.shape[0] // PAIR, dim), BF),
            sem((39,)), sem((90,)), sem((14,)), sem((PAIR, len(PARTS))),
        ],
        compiler_params=pltpu.CompilerParams(collective_id=1, has_side_effects=True, vmem_limit_bytes=67043328),
        name="reduce_gradients",
    )(*h_rows, *m_rows, y_cols, *z_cols, z_own, y_own, scale_parts)


def finish_kernel(count, in_ref, out_ref, y_ref, gx_ref, in_grad, out_grad, y_out, gx_out, scale_out, in_buf, out_buf, y_buf, gx_buf, came, left):
    moves = [(out_ref.at[l, p], out_buf.at[l, pl.ds(SIDE * p, SIDE)]) for l in range(PAIR) for p in range(SIDE)]
    moves += [(y_ref, y_buf), (gx_ref, gx_buf)]
    size, width = in_buf.shape[PAIR:]
    moves += [(in_ref.at[l, p, :, pl.ds(0, width)], in_buf.at[l, p]) for l in range(PAIR) for p in range(SIDE)]
    loads = [pltpu.make_async_copy(src, dst, came.at[k]) for k, (src, dst) in enumerate(moves)]
    for copy in loads:
        copy.start()
    stores = []

    def store(src, dst):
        copy = pltpu.make_async_copy(src, dst, left.at[len(stores)])
        copy.start()
        stores.append(copy)

    for l in range(PAIR):
        for p in range(SIDE):
            loads[SIDE * l + p].wait()
        store(out_buf.at[l, pl.ds(0, 15)], out_grad.at[l])
    for k, (src, dst) in enumerate(((y_buf, y_out), (gx_buf, gx_out))):
        loads[ROW + k].wait()
        store(src, dst)
    me = lax.axis_index("fsdp")
    for l in range(PAIR):
        for f in range(ROW):
            @pl.when(me == f)
            def _():
                scale_out[l:l + 1] = out_buf[l, 15, 0:1, f * count:(f + 1) * count]
    for l in range(PAIR):
        for p in range(SIDE):
            loads[10 + SIDE * l + p].wait()
            store(in_buf.at[l, p], in_grad.at[l, pl.ds(p * size, size)])
    for copy in stores:
        copy.wait()


def finish(in_sums, out_sums, y, gx, rows, proj):
    hbm = pl.BlockSpec(memory_space=pltpu.HBM)
    out = lambda *shape, dtype=F32: jax.ShapeDtypeStruct(shape, dtype)
    size, (depth, dim) = in_sums.shape[PAIR], out_sums.shape[TRIO:]
    in_grad, out_grad, y_out, gx_out, scale = pl.pallas_call(
        functools.partial(finish_kernel, rows),
        out_shape=(out(PAIR, rows, proj), out(PAIR, 15, depth, dim), out(*y.shape, dtype=BF), out(*gx.shape, dtype=BF), out(PAIR, rows)),
        in_specs=[hbm] * SIDE,
        out_specs=[hbm] * SIDE + [pl.BlockSpec(memory_space=pltpu.VMEM)],
        scratch_shapes=[
            pltpu.VMEM((PAIR, SIDE, size, proj), F32), pltpu.VMEM((PAIR, 16, depth, dim), F32), pltpu.VMEM(y.shape, BF), pltpu.VMEM(gx.shape, BF),
            pltpu.SemaphoreType.DMA((18,)), pltpu.SemaphoreType.DMA((12,)),
        ],
        compiler_params=pltpu.CompilerParams(vmem_limit_bytes=67043328),
        name="finish",
    )(in_sums, out_sums, y, gx)
    return y_out[None], gx_out[None], scale, in_grad, out_grad.reshape(PAIR, 15 * depth, dim)


def solution(mesh):
    fsdp_size = mesh.shape["fsdp"]
    batch_spec = P(("dp", "fsdp"), None, None)
    scale_spec = P(None, "fsdp")
    weight_spec = P(None, "fsdp", None)

    def device_step(x_in, grad_y, norm_scale, w_in, w_out):
        n_layers = w_in.shape[0]
        seq_len, model_dim = x_in.shape[1:]
        proj_dim = w_in.shape[PAIR]
        ff_dim = w_out.shape[1] * fsdp_size - model_dim
        head_dim = (proj_dim - model_dim - PAIR * ff_dim) // PAIR
        rows, rows_out = norm_scale.shape[1], w_out.shape[1]
        half_dim = head_dim // PAIR
        freq = 10000.0 ** (-np.arange(half_dim, dtype=np.float32) * 2.0 / head_dim)
        freq = jnp.asarray(np.tile(freq.astype(np.float32), (ROW, LANE // half_dim)))
        hidden, grad_hidden, *rest = run_layers(x_in[0], grad_y[0], norm_scale, w_in, w_out, freq)
        in_sums, out_sums = reduce_gradients((rest[0:SIDE], rest[SIDE:6], rest[6], rest[OTHERS:9], rest[9], rest[10], rest[11]))
        return finish(in_sums, out_sums, hidden, grad_hidden, rows, proj_dim)

    return jax.shard_map(
        device_step,
        mesh=mesh,
        in_specs=(batch_spec, batch_spec, scale_spec, weight_spec, weight_spec),
        out_specs=(batch_spec, batch_spec, scale_spec, weight_spec, weight_spec),
        check_vma=False,
    )
```

```python
import functools
import jax
import jax.numpy as jnp
import numpy as np
from jax import lax
from jax.experimental import pallas as pl
from jax.experimental.pallas import tpu as pltpu
from jax.sharding import PartitionSpec as P

MESH_ID = pl.DeviceIdType.MESH
BOTH = (1, -1)
AROUND = (1, -1, 2)
PARTS = (True, False)
ALL, ZERO = ..., 0.0
OTHERS = 7
QUICK, SHORT = 0.2, 0.3
LANE, WIDE, STRIP, HEAD = 128, 256, 512, 64
ROW, BAND, SIDE, TRIO, PAIR = 8, 32, 4, 3, 2


class Links:
    def __init__(self, send_sems, recv_sems):
        self.send_sems, self.recv_sems = send_sems, recv_sems
        self.slots, self.batches, self.sent, self.count = {}, {}, {}, 0

    def _landing(self, key, lane):
        if key not in self.slots:
            self.slots[key] = self.count
            self.count += 1 if lane is None else PAIR
        return self.recv_sems.at[self.slots[key] + (0 if lane is None else lane)]

    def send(self, key, src, dst, device, landing=None, whole=None, batch=None, lane=None):
        leaving = self.batches.setdefault(batch or key, len(self.batches))
        copy = pltpu.make_async_remote_copy(
            src_ref=src, dst_ref=dst, send_sem=self.send_sems.at[leaving], recv_sem=self._landing(landing or key, lane),
            device_id=device, device_id_type=MESH_ID)
        copy.start()
        self.sent[batch or key] = (src if whole is None else whole, leaving)

    def arrive(self, key, landed, lane=None):
        pltpu.make_async_copy(landed, landed, self._landing(key, lane)).wait()

    def drain(self):
        for left, leaving in self.sent.values():
            pltpu.make_async_copy(left, left, self.send_sems.at[leaving]).wait()
        self.sent.clear()


def rem(a, n):
    return a % n if isinstance(a, int) else lax.rem(a, n)


def chip_position():
    f, d = lax.axis_index("fsdp"), lax.axis_index("dp")
    return f // PAIR, rem(d, SIDE), d // SIDE, rem(f, PAIR)


def device_at(x, y, z, core):
    return (z * SIDE + y, x * PAIR + core)


def step(coord, by):
    return rem(coord + SIDE + by, SIDE)


def announce(devices):
    barrier = pltpu.get_barrier_semaphore()
    for device in devices:
        pl.semaphore_signal(barrier, inc=1, device_id=device, device_id_type=MESH_ID)
    pl.semaphore_wait(barrier, len(devices))


def plan(tasks, latency=2.5):
    free, landed, order, now = {}, {}, [], ZERO
    left = list(tasks)
    while left:
        best = None
        for place, (name, rank, start, needs, after, _, _) in enumerate(left):
            if all(n[0] in landed for n in needs) and all(n in landed for n in after):
                ready = max([start, now] + [landed[task][i] for task, i in needs])
                best = min(best or (ready, rank, place), (ready, rank, place))
        now, _, place = best
        name, _, _, _, _, sends, cost = left.pop(place)
        order.append(name)
        now += cost
        landed[name] = []
        for link, time, *more in sends:
            free[link] = max(now, free.get(link, ZERO)) + time
            landed[name].append(free[link] + latency + sum(more))
    return order


def layers_order(rows_i, cols_i, rows_o, cols_o, seq, starts):
    rate = 23300.0
    tasks = []
    for m in range(SIDE):
        is_in = m % PAIR == 0
        edge = cols_i // LANE * SIDE // 9 // PAIR * WIDE
        size = {"y": rows_i // SIDE * edge, "x": rows_i * (cols_i - PAIR * edge)} if is_in else {"y": rows_o // SIDE * cols_o // PAIR}
        size["z"] = size["y"]
        colors = "yzx" if is_in else "yz"
        tasks.append((("lend", m), 5, 3.0 + SIDE * m, [], [], [("chip", (rows_i * cols_i if is_in else rows_o * cols_o) / 200000.0)], QUICK))
        for color in colors:
            cost = size[color] / rate
            both = [(("x", by), cost) for by in BOTH]
            spread = [((color, by), cost) for by in BOTH] if color != "x" else []
            tasks.append((("reach", m, color), m, starts[m], [], [], both, QUICK))
            for i, by in enumerate(BOTH):
                tasks.append((("relay", m, color, by), m, ZERO, [(("reach", m, color), i)], [], [(("x", by), cost / PAIR)] + spread, QUICK))
            halves = [(("relay", m, color, by), 0) for by in BOTH]
            tasks.append((("far", m, color), m, ZERO, halves, [], spread, QUICK))
            if color == "x":
                continue
            for off, source, first in ((-1, ("relay", m, color, 1), 1), (1, ("relay", m, color, -1), 1), (PAIR, ("far", m, color), 0)):
                for i, by in enumerate(BOTH):
                    tasks.append((("pass", m, color, off, by), m, ZERO, [(source, first + i)], [], [((color, by), cost / PAIR)], QUICK))
                halves = [(("pass", m, color, off, by), 0) for by in BOTH]
                tasks.append((("close", m, color, off), m, ZERO, halves, [], [], QUICK))
        for off in (-1, 1, PAIR):
            last = [("close", m, color, off) for color in "yz"]
            if is_in:
                last.append(("far", m, "x") if off == PAIR else ("relay", m, "x", -off))
            tasks.append((("hand", m, off), m, ZERO, [], last, [("chip", (rows_i * cols_i if is_in else rows_o * cols_o) / 200000.0)], QUICK))
    before = []

    def work(name, cost, mats=()):
        needs = [(("hand", m, off), 0) for m in mats for off in (-1, 1, PAIR)] + [(("lend", m), 0) for m in mats]
        tasks.append((name, 99, ZERO, needs, list(before), [], cost))
        before[:] = [name]

    for l in range(PAIR):
        work(("norm", l), 0.8)
        work(("project", l), 4.0, [PAIR * l])
        work(("attend", l), 4.2)
        work(("mlp", l), 2.2)
        work(("put", l), 1.6, [PAIR * l + 1])
    for l in (1, 0):
        work(("back_out", l), 2.9)
        work(("back_mlp", l), 2.0)
        work(("back_heads", l), 1.0)
        work(("back_quad", l), 6.0)
        work(("back_keys", l), QUICK)
        for i in range(PAIR):
            work(("back_in", l, i), 1.3 + 0.6 * i)
        work(("back_norm", l), 1.0)
    def send(name, rank, start, after, sends):
        tasks.append((name, rank, start, [], [after] if after else [], sends, 0.4))

    def follow(name, rank, needs, sends):
        tasks.append((name, rank, ZERO, needs, [], sends, QUICK))

    def both(axis, size):
        return [((axis, by), size / rate, margin) for by in BOTH]

    model, margin = rows_i * ROW, 0.5
    for l in (1, 0):
        for axis in "yz":
            name = ("send_h", l, axis)
            send(name, 20 - l, 58.0, ("norm", l), both(axis, seq * model))
            for i, by in enumerate(BOTH):
                for index in range(PAIR):
                    follow(("pass_h", l, axis, by, index), 10, [(name, i)], [((axis, by), seq * model / SIDE / rate, margin)])
        send(("send_m", l), 22 - l, ZERO, ("mlp", l), both("x", PAIR * seq * rows_o) + both("x", PAIR * seq * rows_o))
        if l == 0:
            send(("own_y",), 15, ZERO, ("back_norm", 1), [])
            send(("send_scale", l), 15, ZERO, ("back_norm", l), [])
            continue
        name = ("send_y", l)
        send(name, 12, 42.0, None, both("x", seq * model))
        for i, by in enumerate(BOTH):
            follow(("pass_y", l, by), 12, [(name, i)], [(("x", by), seq * model / PAIR / rate, margin)])
        follow(("far_y", l), 12, [(("pass_y", l, by), 0) for by in BOTH], [])
        for axis in "zy":
            name = ("send_z", l, axis)
            share = seq * (cols_i + LANE) / ROW
            send(name, 13, ZERO, ("back_mlp", l), both(axis, share / PAIR) + both(axis, share))
            if axis == "y":
                name = ("rest_z", l)
                send(name, 13, ZERO, ("back_keys", l), both(axis, share / ROW) + both(axis, share / SIDE))
            for i, by in enumerate(BOTH):
                follow(("pass_z", l, axis, by), 13, [(name, i)], [((axis, by), share / PAIR / rate, margin)])
                follow(("twin_z", l, axis, by), 14, [(name, PAIR + i)], [])
            follow(("far_z", l, axis), 14, [(("pass_z", l, axis, by), 0) for by in BOTH], [])
        send(("send_scale", l), 15, ZERO, ("back_norm", l), [])
    send(("own_z",), 15, ZERO, ("back_keys", 0), [])
    return plan(tasks)


def gather_stages(links, position, shard_i, shard_o, wi, wo, lsem):
    x, y, z, core = position
    twin = device_at(x, y, z, 1 - core)
    rows_i, cols_i = shard_i.shape[1:]
    rows_o, cols_o = shard_o.shape[1:]
    quarter_i, quarter_o = rows_i // SIDE, rows_o // SIDE
    third_i = cols_i // LANE * SIDE // 9 // PAIR * WIDE
    half_o = cols_o // PAIR
    cut_o = quarter_o // 16 * ROW + ROW if quarter_o % 16 else quarter_o // PAIR
    place = {"x": x, "y": y, "z": z}

    spots = {(axis, o): step(place[axis], o) for axis in "xyz" for o in range(SIDE)}

    def spot(axis, o):
        return spots[axis, o % SIDE]

    table = {}
    for axis in "xyz":
        for o in range(1, SIDE):
            moved = {**place, axis: spot(axis, o)}
            table[axis, o] = device_at(moved["x"], moved["y"], moved["z"], core)

    def peer(axis, o):
        return table[axis, o % SIDE]

    mats = []
    for l in range(PAIR):
        mats.append((shard_i.at[l], wi.at[l], rows_i, True))
        mats.append((shard_o.at[l], wo.at[l], rows_o, False))

    def region(is_in, color, q):
        if is_in:
            if color == "x":
                lo, hi = PAIR * third_i, cols_i
                rows = (0, rows_i)
            else:
                lo, hi = (0, third_i) if color == "y" else (third_i, PAIR * third_i)
                rows = (q * quarter_i, quarter_i)
            mid = lo + ((hi - lo) // LANE + 1) // PAIR * LANE
            return (rows, (lo, hi - lo)), (rows, (lo, mid - lo)), (rows, (mid, hi - mid))
        cols = (0, half_o) if color == "y" else (half_o, half_o)
        start = q * quarter_o
        return ((start, quarter_o), cols), ((start, cut_o), cols), ((start + cut_o, quarter_o - cut_o), cols)

    def at(m, xb, area):
        (r, nr), (c, nc) = area
        _, out, size, _ = mats[m]
        return out.at[pl.ds(pl.multiple_of((PAIR * xb + core) * size + r, ROW), nr), pl.ds(c, nc)]

    def block(m, xb, index):
        _, out, size, _ = mats[m]
        return out.at[pl.ds(pl.multiple_of((PAIR * xb + index) * size, BAND), size)]

    def group(m, color):
        _, out, _, is_in = mats[m]
        (_, nr), (c, nc) = region(is_in, color, 0)[0]
        return dict(batch=(m, color), whole=out.at[pl.ds(0, nr * (TRIO if color == "x" else 12)), pl.ds(c, nc)])

    def reach(m, color):
        src, _, _, is_in = mats[m]
        area = region(is_in, color, place[color])[0]
        for by in BOTH:
            links.send((m, "x1", color, by), src.at[pl.ds(pl.multiple_of(area[0][0], ROW), area[0][1]), pl.ds(*area[1])], at(m, x, area), peer("x", by), **group(m, color))

    def launch(m, color, off):
        is_in = mats[m][TRIO]
        moved = at(m, spot("x", off), region(is_in, color, place[color])[0])
        for by in BOTH:
            links.send((m, "p1", color, off, by), moved, moved, peer(color, by), **group(m, color))

    def relay(m, color, by):
        is_in = mats[m][TRIO]
        xb = spot("x", -by)
        areas = region(is_in, color, place[color])
        links.arrive((m, "x1", color, by), at(m, xb, areas[0]))
        part = at(m, xb, areas[1] if by == 1 else areas[PAIR])
        links.send((m, "x2", color), part, part, peer("x", by), **group(m, color))
        if color != "x":
            launch(m, color, -by)

    def far(m, color):
        is_in = mats[m][TRIO]
        links.arrive((m, "x2", color), at(m, spot("x", PAIR), region(is_in, color, place[color])[0]))
        if color != "x":
            launch(m, color, PAIR)

    def pass_on(m, color, off, by):
        is_in = mats[m][TRIO]
        xb = spot("x", off)
        areas = region(is_in, color, spot(color, -by))
        links.arrive((m, "p1", color, off, by), at(m, xb, areas[0]))
        part = at(m, xb, areas[1] if by == 1 else areas[PAIR])
        links.send((m, "p2", color, off), part, part, peer(color, by), **group(m, color))

    def close(m, color, off):
        is_in = mats[m][TRIO]
        links.arrive((m, "p2", color, off), at(m, spot("x", off), region(is_in, color, spot(color, PAIR))[0]))

    def four(m):
        _, out, size, _ = mats[m]
        return out.at[pl.ds(0, SIDE * size)]

    def give(m, src, dst):
        links.send((m, "chip"), src, dst, twin, batch=(m, "chip"), whole=four(m))

    def hand(m, off):
        whole = block(m, spot("x", off), core)
        give(m, whole, whole)

    owns = []

    def begin():
        for m, (src, _, _, _) in enumerate(mats):
            copy = pltpu.make_async_copy(src, block(m, x, core), lsem.at[m])
            copy.start()
            owns.append(copy)

    def lend(m):
        give(m, mats[m][0], block(m, x, core))

    def ready(m):
        owns[m].wait()
        links.arrive((m, "chip"), four(m))

    return begin, ready, peer, {"reach": reach, "relay": relay, "far": far, "pass": pass_on, "close": close, "hand": hand, "lend": lend}


BF, F32 = jnp.bfloat16, jnp.float32


def product(a, b, contract=((1,), (0,))):
    return lax.dot_general(a, b, (contract, ((), ())), preferred_element_type=F32)


def lanes(start, size):
    return pl.ds(start if isinstance(start, int) else pl.multiple_of(start, LANE), size)


def layers_kernel(order, sc_ref, wi_ref, wo_ref, x_ref, dy_ref, freq_ref,
                  y_ref, gx_ref, hy_a, hy_b, hz_a, hz_b, mx_a, mx_b, yx_b, zy_b, zz_b, z_a, dy_a, sc_out, relay_z,
                  wi, wo, z, om, h, hid, qr, kts, vsl, ksl, turned_q, turned_o, scores, dscores, pcat, dscat, cos_ref, sin_ref, turn_ref,
                  dot_heads, qt, dht, dkv, omt, ht, dyt, sc, gains, own_gain, gain_ref, load_sems, own_sems, send_sems, recv_sems,
                  share_send_sems, share_recv_sems):
    seq, dim = x_ref.shape
    ff = (wi.shape[PAIR] - dim - LANE) // PAIR
    position = chip_position()
    x, y, zc, core = position
    twin = device_at(x, y, zc, 1 - core)
    me = PAIR * x + core
    links, shared = Links(send_sems, recv_sems), Links(share_send_sems, share_recv_sems)
    stored = []
    spots, _ = around(position)
    h_out, m_out, y_out, z_out = {"y": (hy_a, hy_b), "z": (hz_a, hz_b)}, (mx_a, mx_b), {1: yx_b}, {(1, "y"): zy_b, (1, "z"): zz_b}
    middle = hid.at[1]
    begin, ready, peer, stages = gather_stages(links, position, wi_ref, wo_ref, wi, wo, load_sems)
    others = [(zc * SIDE + y, rem(me + k, ROW)) for k in range(1, ROW)]

    def spot(axis, o):
        return spots[axis, o % SIDE]

    def device(axis, o, index):
        moved = {"x": x, "y": y, "z": zc, axis: spot(axis, o)}
        return device_at(moved["x"], moved["y"], moved["z"], index)

    own_gain[ALL] = jnp.zeros(own_gain.shape, F32)
    count = sc_ref.shape[1]
    for f in range(ROW):
        @pl.when(me == f)
        def _():
            own_gain[0:PAIR, f * count:(f + 1) * count] = sc_ref[ALL].astype(F32)
    announce(others + [device(axis, o, index) for axis in "yz" for o in AROUND for index in range(PAIR)])
    begin()
    for k, far in enumerate(others):
        links.send(("sc",), own_gain, gains.at[me], far, batch=("sc",), whole=gains.at[pl.ds(0, OTHERS)])

    def keep(src, dst):
        copy = pltpu.make_async_copy(src, dst, own_sems.at[len(stored)])
        copy.start()
        stored.append(copy)

    def tokens(axis, o, index):
        return pl.ds(pl.multiple_of((PAIR * spot(axis, o) + index) * seq, seq), seq)

    def place(axis, o, index):
        return PAIR * spot(axis, o) + index

    def columns(axis, o):
        size = z.shape[PAIR] // ROW
        return lanes(((0 if axis == "y" else SIDE) + spot(axis, o)) * size, size)

    def several(batch, ref, n):
        whole = ref.at[pl.ds(0, n * seq if batch[0][0] in "yz" else n)]
        return dict(batch=batch, whole=whole)

    def send_h(l, axis):
        out = h_out[axis][l].at[place(axis, 0, core)]
        for by in BOTH:
            for index in range(PAIR):
                shared.send(("h", l, axis, by), ht.at[l, :, index], out, device(axis, by, index), lane=core, **several(("h", l, axis), h_out[axis][l], OTHERS))
        shared.send(("h", l, axis), ht.at[l, :, 1 - core], out, twin, **several(("h", l, axis), h_out[axis][l], OTHERS))
        keep(ht.at[l, :, core], out)

    def pass_h(l, axis, by, index):
        out = h_out[axis][l]
        shared.arrive(("h", l, axis, by), out.at[place(axis, -by, index)], index)
        part = out.at[place(axis, -by, index), pl.ds(1 - by, PAIR)]
        shared.send(("h", l, axis), part, part, device(axis, by, core), **several(("h", l, axis), out, OTHERS))

    def arrive_h(l):
        for axis in "yz":
            shared.arrive(("h", l, axis), h_out[axis][l].at[pl.ds(0, TRIO)])

    def row_block(l, o, index):
        size = omt.shape[1] // ROW
        return omt.at[l, pl.ds(pl.multiple_of((PAIR * spot("x", o) + index) * size, BAND), size)]

    def send_m(l):
        out, batch = m_out[l].at[place("x", 0, core)], several(("m", l), m_out[l], OTHERS)
        for o in AROUND:
            for index in range(PAIR):
                shared.send(("m", l), row_block(l, o, index), out, device("x", o, index), **batch)
        shared.send(("m", l), row_block(l, 0, 1 - core), out, twin, **batch)
        keep(row_block(l, 0, core), out)

    def arrive_m(l):
        shared.arrive(("m", l), m_out[l].at[pl.ds(0, OTHERS)])

    def token_half(axis, o, k):
        return pl.ds(pl.multiple_of((PAIR * spot(axis, o) + core) * seq + k * (seq // PAIR), seq // PAIR), seq // PAIR)

    def send_y(l):
        src, out = dy_ref, y_out[l].at[tokens("x", 0, core)]
        for by in BOTH:
            shared.send(("y", l, by), src, out, device("x", by, core), **several(("y", l), y_out[l], OTHERS))
        shared.send(("y", l), src, out, twin, **several(("y", l), y_out[l], OTHERS))
        keep(src, out)

    def pass_y(l, by):
        landed, part = y_out[l].at[tokens("x", -by, core)], y_out[l].at[token_half("x", -by, (1 - by) // PAIR)]
        shared.arrive(("y", l, by), landed)
        shared.send(("y2", l), part, part, device("x", by, core), **several(("y", l), y_out[l], OTHERS))
        shared.send(("y", l), landed, landed, twin, **several(("y", l), y_out[l], OTHERS))

    def far_y(l):
        landed = y_out[l].at[tokens("x", PAIR, core)]
        shared.arrive(("y2", l), landed)
        shared.send(("y", l), landed, landed, twin, **several(("y", l), y_out[l], OTHERS))

    def arrive_y(l):
        shared.arrive(("y", l), y_out[l].at[pl.ds(0, SIDE * seq)])

    def push_z(l, axis, o, ready):
        out = z_out[l, axis].at[tokens(axis, 0, core)]
        batch = several(("z", l, axis), z_out[l, axis], ROW)

        def start():
            if o != PAIR:
                shared.send(("z", l, axis, o), z.at[l, :, columns(axis, o)], out, device(axis, o, core), **batch)
                return
            for k, by in enumerate(BOTH):
                shared.send(("zr", l, axis, by), z.at[l, pl.ds(k * (seq // PAIR), seq // PAIR), columns(axis, PAIR)], relay_z.at[l, "yz".index(axis), k],
                            device(axis, by, core), **batch)

        if ready is None:
            start()
        else:
            pl.when(ready)(start)

    def own_part(l, axis):
        out, mine = z_out[l, axis].at[tokens(axis, 0, core)], z.at[l, :, columns(axis, 0)]
        shared.send(("z", l, axis), mine, out, twin, **several(("z", l, axis), z_out[l, axis], ROW))
        keep(mine, out)

    def send_z(l, axis):
        for o in (PAIR, 1, -1):
            push_z(l, axis, o, spot(axis, o) != 0 if axis == "y" else None)
        if axis == "z":
            own_part(l, axis)

    def rest_z(l):
        for o in (PAIR, 1, -1):
            push_z(l, "y", o, spot("y", o) == 0)
        own_part(l, "y")

    def pass_z(l, axis, by):
        k = (1 - by) // PAIR
        half = relay_z.at[l, "yz".index(axis), k]
        shared.arrive(("zr", l, axis, by), half)
        shared.send(("z2", l, axis), half, z_out[l, axis].at[token_half(axis, -by, k)], device(axis, by, core), **several(("z", l, axis), z_out[l, axis], ROW))

    def twin_z(l, axis, by):
        landed = z_out[l, axis].at[tokens(axis, -by, core)]
        shared.arrive(("z", l, axis, by), landed)
        shared.send(("z", l, axis), landed, landed, twin, **several(("z", l, axis), z_out[l, axis], ROW))

    def far_z(l, axis):
        landed = z_out[l, axis].at[tokens(axis, PAIR, core)]
        shared.arrive(("z2", l, axis), landed)
        shared.send(("z", l, axis), landed, landed, twin, **several(("z", l, axis), z_out[l, axis], ROW))

    def arrive_z(l, axis):
        shared.arrive(("z", l, axis), z_out[l, axis].at[pl.ds(0, SIDE * seq)])

    def send_scale(l):
        for far in others:
            shared.send(("scale", l), sc.at[l], sc_out.at[l, me], far, batch=("scale", l), whole=sc_out.at[l, pl.ds(0, OTHERS)])
        keep(sc.at[l], sc_out.at[l, me])

    def arrive_scale(l):
        shared.arrive(("scale", l), sc_out.at[l, pl.ds(0, OTHERS)])

    gains[me] = own_gain[ALL]
    z[:, :, wi.shape[PAIR]:] = jnp.zeros((PAIR, seq, z.shape[PAIR] - wi.shape[PAIR]), BF)
    entry = (x_ref, hid.at[0])
    angle = lax.broadcasted_iota(jnp.int32, (seq, LANE), 0).astype(F32) * freq_ref[0:1]
    for half in range(PAIR):
        cos_ref[:, LANE * half:LANE * (half + 1)] = jnp.cos(angle)
        sin_ref[:, LANE * half:LANE * (half + 1)] = jnp.sin(angle)
    lane = lax.broadcasted_iota(jnp.int32, turn_ref.shape, 1)
    down = lax.broadcasted_iota(jnp.int32, turn_ref.shape, 0) - lane
    low = rem(lane, HEAD) < BAND
    turn_ref[ALL] = jnp.where(low & (down == BAND), -1.0, jnp.where(jnp.logical_not(low) & (down == -BAND), 1.0, ZERO)).astype(BF)
    kts[ALL] = jnp.zeros(kts.shape, BF)
    pcat[ALL] = jnp.zeros(pcat.shape, BF)
    dscat[ALL] = jnp.zeros(dscat.shape, BF)

    def normalise(l, src):
        @pl.loop(0, seq // BAND, unroll=SIDE)
        def _(r):
            rows = pl.ds(pl.multiple_of(r * BAND, BAND), BAND)
            v = src[rows].astype(F32)
            v = v - jnp.mean(v, axis=-1, keepdims=True)
            var = jnp.mean(v * v, axis=-1, keepdims=True)
            h[l, rows] = (v * lax.rsqrt(var + 1e-6) * gain_ref[l:l + 1]).astype(BF)

    def project(l):
        strip = wi.shape[PAIR] // 5

        @pl.loop(0, 5)
        def _(i):
            at = lanes(i * strip, strip)
            z[l, :, at] = product(h[l], wi[l, :, at]).astype(BF)

    def heads(l):
        cos, sin = cos_ref[ALL], sin_ref[ALL]
        for g in range(dim // WIDE):
            q = z[l, :, g * WIDE:(g + 1) * WIDE]
            qr[l, :, g * WIDE:(g + 1) * WIDE] = ((q.astype(F32) * cos + product(q, turn_ref[ALL]) * sin) * 0.125).astype(BF)
        kv = z[l, :, dim:dim + LANE]
        turned = kv.astype(F32) * cos[:, :LANE] + product(kv, turn_ref[:LANE, :LANE]) * sin[:, :LANE]
        first = lax.broadcasted_iota(jnp.int32, turned.shape, 1) < HEAD
        key_lo = jnp.where(first, turned, ZERO)
        val_hi = jnp.where(first, ZERO, kv.astype(F32))
        return key_lo, pltpu.roll(key_lo, HEAD, 1), pltpu.roll(val_hi, HEAD, 1), val_hi

    def slot_rows(ref, lo, hi):
        zero = jnp.zeros((seq, LANE), BF)
        lo, hi = lo.astype(BF), hi.astype(BF)
        for i, (left, right) in enumerate(((lo, zero), (hi, zero), (zero, lo), (zero, hi))):
            ref[i * seq:(i + 1) * seq, :LANE] = left
            ref[i * seq:(i + 1) * seq, LANE:] = right

    def slot_cols(ref, lo):
        flat = lo.T[:HEAD].astype(BF)
        for i in range(SIDE):
            ref[HEAD * i:HEAD * (i + 1), i * seq:(i + 1) * seq] = flat

    def chances(i, half):
        at = slice(LANE * half, LANE * (half + 1))
        blocks = [pl.ds(pl.multiple_of(i * seq + LANE * k, LANE), LANE) for k in range(half + 1)]
        s = [scores[keys, at] for keys in blocks]
        lower = lax.broadcasted_iota(jnp.int32, s[-1].shape, 1) >= lax.broadcasted_iota(jnp.int32, s[-1].shape, 0)
        s[-1] = jnp.where(lower, s[-1], -1e30)
        top = functools.reduce(jnp.maximum, [jnp.max(v, axis=0, keepdims=True) for v in s])
        e = [jnp.exp(v - top) for v in s]
        scale = 1.0 / sum(jnp.sum(v, axis=0, keepdims=True) for v in e)
        return at, [(keys, v * scale) for keys, v in zip(blocks, e)]

    def attend(l):
        key_lo, key_hi, val_lo, _ = heads(l)
        slot_rows(ksl, key_lo, key_hi)
        slot_cols(kts, val_lo)
        flip(lambda at: qr[l, :, lanes(at, WIDE)], qt, dim)

        @pl.loop(0, dim // WIDE)
        def _(g):
            rows = pl.ds(pl.multiple_of(g * WIDE, WIDE), WIDE)
            scores[ALL] = product(ksl[ALL], qt[rows])

            @pl.loop(0, SIDE)
            def _(i):
                for half in range(PAIR):
                    at, blocks = chances(i, half)
                    for keys, p in blocks:
                        pcat[keys, at] = p.astype(BF)
            flat = product(kts[ALL], pcat[ALL]).astype(BF)
            omt[l, rows] = flat
            om[:, lanes(g * WIDE, WIDE)] = flat.T

    def mlp(l):
        @pl.loop(0, seq // BAND)
        def _(r):
            rows = pl.ds(pl.multiple_of(r * BAND, BAND), BAND)

            @pl.loop(0, ff // STRIP)
            def _(i):
                gate = z[l, rows, lanes(dim + LANE + i * STRIP, STRIP)].astype(F32)
                up = z[l, rows, lanes(dim + LANE + ff + i * STRIP, STRIP)].astype(F32)
                om[rows, lanes(dim + i * STRIP, STRIP)] = (gate * jax.nn.sigmoid(gate) * up).astype(BF)

    def put_out(l, dst):
        for n in range(dim // WIDE):
            cols = slice(n * WIDE, (n + 1) * WIDE)
            total = product(om[ALL], wo[l, :, cols])
            dst[:, cols] = (entry[l][:, cols].astype(F32) + total).astype(BF)

    def flip(src, dst, width, first=0):
        @pl.loop(first // WIDE, width // WIDE)
        def _(i):
            dst[pl.ds(pl.multiple_of(i * WIDE, WIDE), WIDE)] = src(i * WIDE).T

    upstream = (middle, dy_ref)

    def back_out(l):
        dy = upstream[l]
        flip(lambda at: dy[:, lanes(at, WIDE)], dyt, dim)

        @pl.loop(0, wo.shape[1] // dim)
        def _(n):
            rows = pl.ds(pl.multiple_of(n * dim, dim), dim)
            part = product(wo[l, rows], dyt[ALL]).astype(BF)
            om[:, lanes(n * dim, dim)] = part.T

            @pl.when(n == 0)
            def _():
                dot_heads[ALL] = part

    def back_mlp(l):
        @pl.loop(0, seq // BAND)
        def _(r):
            rows = pl.ds(pl.multiple_of(r * BAND, BAND), BAND)

            @pl.loop(0, ff // STRIP)
            def _(i):
                gate_at, up_at = lanes(dim + LANE + i * STRIP, STRIP), lanes(dim + LANE + ff + i * STRIP, STRIP)
                gate, up = z[l, rows, gate_at].astype(F32), z[l, rows, up_at].astype(F32)
                d = om[rows, lanes(dim + i * STRIP, STRIP)].astype(F32)
                sig = jax.nn.sigmoid(gate)
                du = d * up
                z[l, rows, gate_at] = (du * sig + du * gate * (sig * (1.0 - sig))).astype(BF)
                z[l, rows, up_at] = (d * (gate * sig)).astype(BF)

    def back_heads(l):
        key_lo, key_hi, val_lo, val_hi = heads(l)
        slot_rows(ksl, key_lo, key_hi)
        slot_rows(vsl, val_lo, val_hi)
        slot_cols(kts, key_lo)
        dkv[ALL] = jnp.zeros(dkv.shape, F32)
        flip(lambda at: qr[l, :, lanes(at, WIDE)], qt, dim)
        for at in range(0, dim, LANE):
            pair = slice(at, at + LANE)
            turned_q[:, pair] = pltpu.roll(qr[l, :, pair].astype(F32), HEAD, 1).astype(BF)
            turned_o[:, pair] = pltpu.roll(om[:, pair].astype(F32), HEAD, 1).astype(BF)

    def back_quad(l):
        @pl.loop(0, dim // WIDE)
        def _(g):
            quad(l, g)

    def quad(l, g):
        cols = pl.ds(pl.multiple_of(g * WIDE, WIDE), WIDE)
        scores[ALL] = product(ksl[ALL], qt[cols])
        dscores[ALL] = product(vsl[ALL], dot_heads[cols])

        @pl.loop(0, SIDE)
        def _(i):
            for half in range(PAIR):
                at, blocks = chances(i, half)
                given = [p * dscores[keys, at].astype(BF).astype(F32) for keys, p in blocks]
                total = sum(jnp.sum(v, axis=0, keepdims=True) for v in given)
                for (keys, p), v in zip(blocks, given):
                    pcat[keys, at] = p.astype(BF)
                    dscat[keys, at] = (v - p * total).astype(BF)
        dq = product(kts[ALL], dscat[ALL]).astype(BF).T
        back = dq.astype(F32) * cos_ref[ALL] - product(dq, turn_ref[ALL]) * sin_ref[ALL]
        z[l, :, cols] = (back * 0.125).astype(BF)
        def pieces(left, even, odd):
            for i in range(SIDE):
                pair = lanes(g * WIDE + i // PAIR * LANE, LANE)
                yield product(left[i * seq:(i + 1) * seq, :], odd(pair) if i % PAIR else even(pair))

        dkv[0] += sum(pieces(dscat, lambda at: qr[l, :, at], lambda at: turned_q[:, at]))
        dkv[1] += sum(pieces(pcat, lambda at: turned_o[:, at], lambda at: om[:, at]))

    def back_keys(l):
        dk = dkv[0].astype(BF)
        turned = dk.astype(F32) * cos_ref[:, :LANE] - product(dk, turn_ref[:LANE, :LANE]) * sin_ref[:, :LANE]
        first = lax.broadcasted_iota(jnp.int32, turned.shape, 1) < HEAD
        z[l, :, dim:dim + LANE] = jnp.where(first, turned, dkv[1]).astype(BF)

    def back_in(l, half):
        width = wi.shape[PAIR] // 5
        at = slice(PAIR * half * width, (PAIR + TRIO * half) * width)
        part = product(wi[l, :, at], z[l, :, at], ((1,), (1,)))
        dht[ALL] = dht[ALL] + part if half else part

    def back_norm(l):
        dy, dst = upstream[l], (gx_ref, middle)[l]
        for i in range(dim // WIDE):
            cols = slice(i * WIDE, (i + 1) * WIDE)
            h[l, :, cols] = dht[cols].T.astype(BF)
        sc[l] = jnp.zeros(sc.shape[1:], F32)

        @pl.loop(0, seq // BAND, unroll=SIDE)
        def _(r):
            rows = pl.ds(pl.multiple_of(r * BAND, BAND), BAND)
            v = entry[l][rows].astype(F32)
            v = v - jnp.mean(v, axis=-1, keepdims=True)
            scale = lax.rsqrt(jnp.mean(v * v, axis=-1, keepdims=True) + 1e-6)
            hat = v * scale
            d = h[l, rows].astype(F32)
            each = (d * hat).reshape(SIDE, ROW, dim)
            sc[l] += (each[0] + each[1]) + (each[PAIR] + each[TRIO])
            d = d * gain_ref[l:l + 1]
            d = scale * (d - jnp.mean(d, axis=-1, keepdims=True) - hat * jnp.mean(d * hat, axis=-1, keepdims=True))
            dst[rows] = (dy[rows].astype(F32) + d.astype(BF).astype(F32)).astype(BF)

    def do_norm(l):
        if l == 0:
            links.arrive(("sc",), gains.at[pl.ds(0, OTHERS)])
            gain_ref[ALL] = jnp.sum(gains[ALL], axis=0)
        normalise(l, entry[l])
        for i in range(dim // WIDE):
            flat = h[l, :, i * WIDE:(i + 1) * WIDE].T
            size = ht.shape[TRIO]
            for b in range(ROW):
                lo, hi = max(b * size, i * WIDE), min((b + 1) * size, (i + 1) * WIDE)
                if lo < hi:
                    ht[l, b // PAIR, b % PAIR, lo - b * size:hi - b * size] = flat[lo - i * WIDE:hi - i * WIDE]

    def do_project(l):
        ready(PAIR * l)
        project(l)

    def do_mlp(l):
        mlp(l)
        flip(lambda at: om[:, lanes(at, WIDE)], omt.at[l], om.shape[1], dim)

    def do_put(l):
        ready(PAIR * l + 1)
        put_out(l, hid.at[0] if l == 0 else y_ref)

    stages.update(
        norm=do_norm, project=do_project, attend=attend, mlp=do_mlp, put=do_put, back_out=back_out, back_mlp=back_mlp, back_heads=back_heads,
        back_quad=back_quad, back_keys=back_keys, back_in=back_in, back_norm=back_norm, send_h=send_h, pass_h=pass_h, send_m=send_m, send_y=send_y, pass_y=pass_y, far_y=far_y, send_z=send_z, rest_z=rest_z, pass_z=pass_z, twin_z=twin_z, far_z=far_z,
        send_scale=send_scale, own_z=lambda: keep(z.at[0], z_a), own_y=lambda: keep(middle, dy_a))
    for kind, *task in order:
        stages[kind](*task)
    for l in range(PAIR):
        arrive_h(l)
        arrive_m(l)
        arrive_scale(l)
    arrive_y(1)
    for l, axis in z_out:
        arrive_z(l, axis)
    for copy in stored:
        copy.wait()
    shared.drain()
    links.drain()


def run_layers(x, dy, scale, w_in, w_out, freq, starts=(ZERO, 10.0, 20.0, 30.0)):
    seq, dim = x.shape
    proj, cat = w_in.shape[PAIR], ROW * w_out.shape[1]
    wide = proj + LANE
    hbm, vmem = pl.BlockSpec(memory_space=pltpu.HBM), pl.BlockSpec(memory_space=pltpu.VMEM)
    out = lambda *shape, dtype=BF: jax.ShapeDtypeStruct(shape, dtype)
    buffer = lambda *shape, dtype=BF: pltpu.VMEM(shape, dtype)
    sem = pltpu.SemaphoreType.DMA
    line = ROW * seq
    return pl.pallas_call(
        functools.partial(layers_kernel, layers_order(*w_in.shape[1:], *w_out.shape[1:], seq, starts)),
        out_shape=(out(seq, dim), out(seq, dim), *[out(ROW, SIDE, dim // ROW, seq)] * SIDE, *[out(ROW, cat // ROW, seq)] * PAIR, out(line, dim),
                   *[out(line, wide // ROW)] * PAIR, out(seq, wide), out(seq, dim), out(PAIR, ROW, ROW, dim, dtype=F32),
                   out(PAIR, PAIR, PAIR, seq // PAIR, wide // ROW)),
        in_specs=[vmem, hbm, hbm] + [vmem] * TRIO,
        out_specs=[vmem] * PAIR + [hbm] * 13,
        scratch_shapes=[
            buffer(PAIR, dim, proj), buffer(PAIR, cat, dim), buffer(PAIR, seq, wide), buffer(seq, cat), buffer(PAIR, seq, dim),
            buffer(PAIR, seq, dim), buffer(PAIR, seq, dim),
            buffer(WIDE, SIDE * seq), buffer(SIDE * seq, WIDE), buffer(SIDE * seq, WIDE), buffer(seq, dim), buffer(seq, dim),
            buffer(SIDE * seq, seq, dtype=F32), buffer(SIDE * seq, seq, dtype=F32), buffer(SIDE * seq, seq), buffer(SIDE * seq, seq),
            buffer(seq, WIDE, dtype=F32), buffer(seq, WIDE, dtype=F32), buffer(WIDE, WIDE),
            buffer(dim, seq), buffer(dim, seq), buffer(dim, seq, dtype=F32), buffer(PAIR, seq, LANE, dtype=F32),
            buffer(PAIR, cat, seq), buffer(PAIR, SIDE, PAIR, dim // ROW, seq), buffer(dim, seq), buffer(PAIR, ROW, dim, dtype=F32),
            buffer(ROW, ROW, dim, dtype=F32), buffer(ROW, dim, dtype=F32), buffer(ROW, dim, dtype=F32),
            sem((SIDE,)), sem((13,)), sem((15,)), sem((107,)), sem((11,)), sem((40,)),
        ],
        compiler_params=pltpu.CompilerParams(collective_id=PAIR, has_side_effects=True, vmem_limit_bytes=67043328),
        name="run_layers",
    )(scale, w_in, w_out, x, dy, freq)


PARTS = (("i", "x", "z", "y", 0, STRIP), ("i", "x", "z", "y", STRIP, 384), ("i", "x", "y", "z", 0, STRIP), ("i", "x", "y", "z", STRIP, 384),
         ("o", "y", "z", "y", 0, 384), ("o", "z", "y", "z", 384, 384))


def reduce_order(rows, rows_b, starts):
    rate = 11650.0
    tasks = []
    sizes = {"y": WIDE * 896 / (PAIR * rate), "z": WIDE * 896 / (PAIR * rate), "x": WIDE * 768 / (PAIR * rate)}
    for axis in "yzx":
        size = sizes[axis]
        tasks.append((("swap", axis), (0, 0), starts[PAIR] if axis == "x" else starts[TRIO], [], [],
                      [((axis, by), size * n) for by, n in ((-1, 0.5), (1, 1), (-1, 1), (1, 1))], SHORT))
        tasks.append((("relay", axis), (0, 0), ZERO, [(("swap", axis), 0)], [], [((axis, -1), size / PAIR)], SHORT))
        for o, needs in ((1, [(("swap", axis), 1)]), (-1, [(("swap", axis), PAIR)]), (PAIR, [(("swap", axis), TRIO), (("relay", axis), 0)])):
            tasks.append((("near", axis, o), (0, PAIR), ZERO, needs, [], [("chip", 1.6)], QUICK))
    tasks.append((("fetch", 0), (5, 0), ZERO, [], [("make", 1, len(PARTS) - 1)], [], QUICK))
    for l in (1, 0):
        late = 1 - l
        for c, (kind, first, then, last, at, width) in enumerate(PARTS):
            needs, cost = [], 1.6 * width / STRIP
            if l == 0:
                needs = [(("near", last if kind == "i" else "x", o), 0) for o in AROUND]
            tasks.append((("make", l, c), (9 * late, c), starts[late], needs, [] if l else [("fetch", 0)], [], cost))
            full = SIDE * SIDE * (rows if kind == "i" else rows_b) * width / rate
            sends = [[((first, by), full / ROW) for by in BOTH], [((first, by), full / SIDE) for by in BOTH],
                     [((then, o), full / 16) for o in (1, -1, 1)], []]
            piece = full / 16
            sends += [[((then, o), piece) for o in (1, -1, 1)], [((last, by), SIDE * piece) for by in BOTH],
                      [((last, by), PAIR * piece) for by in BOTH], []]
            for s in range(ROW):
                task = ("sum", l, c, s)
                needs = [(("sum", l, c, s - 1), k) for k in range(len(sends[s - 1]))] if s else []
                tasks.append((task, (late, -s), ZERO, needs, [("make", l, c)] if s == 0 else [("sum", l, c, s - 1)], sends[s], SHORT))
    return plan(tasks)


def reduce_kernel(order, *refs):
    hy, hz, mx = refs[0:PAIR], refs[PAIR:SIDE], refs[SIDE:6]
    yx1, zy1, zz1, z0, y0, sc = refs[6:12]
    oa, ob = refs[12:14]
    n = len(PARTS)
    total, half, full, small, front = (refs[14 + k * n:14 + (k + 1) * n] for k in range(5))
    (hbuf, zbuf, mbuf, ybuf, scbuf, rz, ry, ssem, rsem, isem, osem) = refs[14 + 5 * n:]
    position = chip_position()
    x, y, zc, core = position
    place = {"x": x, "y": y, "z": zc}
    twin = device_at(x, y, zc, 1 - core)
    spots, peers = around(position)

    def spot(axis, o):
        return spots[axis, o % SIDE]

    def peer(axis, o):
        return peers[axis, o % SIDE]

    seq, wide = z0.shape
    own = wide // ROW
    loads, moving = {}, []

    def load(key, src, dst):
        copy = pltpu.make_async_copy(src, dst, isem.at[len(moving)])
        moving.append(key)
        copy.start()
        loads[key] = copy

    def fetch(l):
        if not l:
            load(("h", 0, "y"), hy[0], hbuf.at[0, 0])
        else:
            load(("z", 1, "z"), zz1, zbuf.at[1, 1])
        load(("h", l, "z"), hz[l], hbuf.at[l, 1])
        load(("m", l), mx[l], mbuf.at[l])
        if l:
            load(("y", 1), yx1, ybuf.at[1])
        load(("s", l), sc.at[l], scbuf.at[l])

    load(("z", 1, "y"), zy1, zbuf.at[1, 0])
    load(("h", 1, "y"), hy[1], hbuf.at[1, 0])
    done = set()

    def loaded(*keys):
        for key in keys:
            if key not in done:
                loads[key].wait()
                done.add(key)

    announce([peer(axis, o) for axis in "xyz" for o in AROUND] + [twin])
    fetch(1)
    links = Links(ssem, rsem)

    def columns(axis, o):
        return lanes(((0 if axis == "y" else SIDE) + spot(axis, o)) * own, own)

    def tokens(axis, o, index):
        return pl.ds(pl.multiple_of((PAIR * spot(axis, o) + index) * seq, seq), seq)

    def target(axis):
        return ybuf.at[0] if axis == "x" else zbuf.at[0, "yz".index(axis)]

    def leaving(axis):
        return dict(batch=("swap", axis), whole=target(axis).at[pl.ds(0, OTHERS * seq + seq // PAIR)])

    def half_at(axis, o, k):
        start = (PAIR * spot(axis, o) + core) * seq + k * (seq // PAIR)
        return target(axis).at[pl.ds(pl.multiple_of(start, seq // PAIR), seq // PAIR)]

    def relay_of(axis):
        return ry if axis == "x" else rz.at["yz".index(axis)]

    def swap(axis):
        def part(o, rows=slice(None)):
            return y0.at[rows] if axis == "x" else z0.at[rows, columns(axis, o)]

        mine = target(axis).at[tokens(axis, 0, core)]
        links.send(("relay", axis), part(PAIR, pl.ds(seq // PAIR, seq // PAIR)), relay_of(axis), peer(axis, -1), **leaving(axis))
        for by in BOTH:
            links.send(("swap", axis, by), part(by), mine, peer(axis, by), **leaving(axis))
        links.send(("swap", axis, PAIR), part(PAIR, pl.ds(0, seq // PAIR)), half_at(axis, 0, 0), peer(axis, PAIR), **leaving(axis))
        links.send(("near", axis), part(0), mine, twin, **leaving(axis))
        load(("own", axis), part(0), mine)

    def relay(axis):
        links.arrive(("relay", axis), relay_of(axis))
        links.send(("relayed", axis), relay_of(axis), half_at(axis, 1, 1), peer(axis, -1), **leaving(axis))

    def near(axis, o):
        landed = target(axis).at[tokens(axis, -o, core)]
        if o == PAIR:
            links.arrive(("swap", axis, PAIR), half_at(axis, PAIR, 0))
            links.arrive(("relayed", axis), half_at(axis, PAIR, 1))
        else:
            links.arrive(("swap", axis, o), landed)
        links.send(("near", axis), landed, landed, twin, **leaving(axis))

    def joined(axis):
        if axis not in done:
            done.add(axis)
            loaded(("own", axis))
            links.arrive(("near", axis), target(axis).at[pl.ds(0, SIDE * seq)])

    def joined_lanes(ref, l, i):
        return jnp.concatenate([ref[l, i, k].reshape(-1, ref.shape[-1]) for k in range(ROW)], axis=1)

    def make(l, c):
        kind, first, then, last, at, width = PARTS[c]
        if kind == "i":
            i = "yz".index(last)
            loaded(("h", l, last))
            if l:
                loaded(("z", l, last))
            else:
                joined(last)
            size = total[c].shape[TRIO]
            for lo in range(0, width, WIDE):
                hi = min(width, lo + WIDE)
                part = product(joined_lanes(hbuf, l, i), zbuf[l, i, :, at + lo:at + hi])
                for r in range(16):
                    total[c][l, r // SIDE, r % SIDE, :, lo:hi] = part[r * size:(r + 1) * size]
            return
        loaded(("m", l), ("s", l))
        if l:
            loaded(("y", l))
        else:
            joined("x")
        part = product(jnp.concatenate([mbuf[l, k] for k in range(ROW)], axis=1), ybuf[l, :, at:at + width])
        size = total[c].shape[TRIO]

        def put(r, value):
            total[c][(l, r // SIDE, r % SIDE) if first == "y" else (l, r % SIDE, r // SIDE)] = value

        for r in range(part.shape[0] // size):
            put(r, part[r * size:(r + 1) * size])
        gain = jnp.sum(jnp.sum(scbuf[l, :, :, at:at + width], axis=0), axis=0, keepdims=True)
        row = lax.broadcasted_iota(jnp.int32, (size, width), 0)
        put(15, jnp.where(row == 0, gain, ZERO))

    def area(l, c, o, whole):
        kind, first, then, last, at, width = PARTS[c]
        inner = (spot(then, whole) if isinstance(whole, int) else whole)
        outer = spot(last, o)
        if kind == "i":
            cols = lanes(((0 if last == "y" else SIDE) + outer) * own + at, width)
            return oa.at[l, inner, :, cols]
        cols = pl.ds(at, width)
        return ob.at[l, outer, inner, :, cols] if last == "y" else ob.at[l, inner, outer, :, cols]

    def add(l, c, s):
        kind, first, then, last, at, width = PARTS[c]
        t = total[c].at[l]
        sums = dict(batch=(l, c, 0), whole=t)
        lines = dict(batch=(l, c, 1), whole=t.at[pl.ds(0, PAIR)])
        singles = dict(batch=(l, c, PAIR), whole=t.at[pl.ds(0, PAIR), pl.ds(0, TRIO)])
        if s == 0:
            far = t.at[spot(first, PAIR)]
            for k, by in enumerate(BOTH):
                links.send((l, c, "half"), far.at[pl.ds(PAIR * k, PAIR)], half[c].at[l, k], peer(first, by), **sums)
        elif s == 1:
            links.arrive((l, c, "half"), half[c].at[l])
            for k, by in enumerate(BOTH):
                mine = t.at[spot(first, by)]
                add_into(mine.at[pl.ds(PAIR * k, PAIR)], half[c].at[l, k])
                links.send((l, c, "full"), mine, full[c].at[l, k], peer(first, by), **sums)
        elif s == PAIR:
            mine = t.at[spot(first, 0)]
            links.arrive((l, c, "full"), full[c].at[l])
            for k in range(PAIR):
                add_into(mine, full[c].at[l, k])
            for k, o in enumerate(AROUND):
                links.send((l, c, "small"), mine.at[spot(then, o)], small[c].at[l, k], peer(then, o), **singles)
        elif s == TRIO:
            links.arrive((l, c, "small"), small[c].at[l])
            mine = t.at[spot(first, 0), spot(then, 0)]
            front[c][l] = (mine[ALL] + small[c][l, 0]) + (small[c][l, 1] + small[c][l, PAIR])
        elif s == SIDE:
            src, dst = front[c].at[l], area(l, c, 0, 0)
            for o in AROUND:
                links.send((l, c, "a1"), src, dst, peer(then, o), **singles)
            copy = pltpu.make_async_copy(src, dst, osem.at[l, c])
            copy.start()
            loads["front", l, c] = copy
        elif s == 5:
            loaded(("front", l, c))
            links.arrive((l, c, "a1"), t.at[0, pl.ds(0, TRIO)])
            line = area(l, c, 0, slice(None))
            for by in BOTH:
                links.send((l, c, "a2"), line, line, peer(last, by), **lines)
        elif s == 6:
            links.arrive((l, c, "a2"), t.at[pl.ds(0, PAIR)])
            for k, by in enumerate(BOTH):
                part = area(l, c, -by, pl.ds(PAIR * k, PAIR))
                links.send((l, c, "a3"), part, part, peer(last, by), **sums)
        else:
            links.arrive((l, c, "a3"), area(l, c, PAIR, slice(None)))

    stages = {"swap": swap, "relay": relay, "near": near, "fetch": fetch, "make": make, "sum": add}
    for kind, *task in order:
        stages[kind](*task)
    links.drain()


def add_into(dst, src):
    @pl.loop(0, dst.shape[0])
    def _(i):
        if len(dst.shape) == SIDE:
            for j in range(dst.shape[1]):
                dst[i, j] += src[i, j]
        else:
            dst[i] += src[i]


def around(position):
    place, core = dict(zip("xyz", position)), position[TRIO]
    spots = {(axis, o): step(place[axis], o) for axis in "xyz" for o in range(SIDE)}
    peers = {}
    for axis in "xyz":
        for o in range(1, SIDE):
            moved = {**place, axis: spots[axis, o]}
            peers[axis, o] = device_at(moved["x"], moved["y"], moved["z"], core)
    return spots, peers


def reduce_gradients(operands, starts=(ZERO, ZERO, 20.0, 3.0)):
    hbm = pl.BlockSpec(memory_space=pltpu.HBM)
    h_rows, m_rows, y_cols, z_cols, z_own, y_own, scale_parts = operands
    part, part_b = h_rows[0].shape[PAIR] // SIDE, (m_rows[0].shape[1] + BAND) // 16
    (line, dim), wide = y_cols.shape, z_own.shape[1]
    out = lambda *shape: jax.ShapeDtypeStruct(shape, F32)
    sem = pltpu.SemaphoreType.DMA

    def buffers(*lead):
        return [pltpu.VMEM((PAIR, *lead, part if e[0] == "i" else part_b, e[5]), F32) for e in PARTS]

    return pl.pallas_call(
        functools.partial(reduce_kernel, reduce_order(part, part_b, starts)),
        out_shape=(out(PAIR, SIDE, part, wide), out(PAIR, SIDE, SIDE, part_b, dim)),
        in_specs=[hbm] * 12,
        out_specs=[hbm] * PAIR,
        scratch_shapes=[
            *buffers(SIDE, SIDE), *buffers(PAIR, PAIR), *buffers(PAIR, SIDE), *buffers(TRIO), *buffers(),
            pltpu.VMEM((PAIR, PAIR, *h_rows[0].shape), BF), pltpu.VMEM((PAIR, PAIR, line, wide // ROW), BF), pltpu.VMEM((PAIR, *m_rows[0].shape), BF),
            pltpu.VMEM((PAIR, line, dim), BF), pltpu.VMEM(scale_parts.shape, F32),
            pltpu.VMEM((PAIR, z_own.shape[0] // PAIR, wide // ROW), BF), pltpu.VMEM((y_own.shape[0] // PAIR, dim), BF),
            sem((39,)), sem((90,)), sem((14,)), sem((PAIR, len(PARTS))),
        ],
        compiler_params=pltpu.CompilerParams(collective_id=1, has_side_effects=True, vmem_limit_bytes=67043328),
        name="reduce_gradients",
    )(*h_rows, *m_rows, y_cols, *z_cols, z_own, y_own, scale_parts)


def finish_kernel(count, in_ref, out_ref, y_ref, gx_ref, in_grad, out_grad, y_out, gx_out, scale_out, in_buf, out_buf, y_buf, gx_buf, came, left):
    moves = [(out_ref.at[l, p], out_buf.at[l, pl.ds(SIDE * p, SIDE)]) for l in range(PAIR) for p in range(SIDE)]
    moves += [(y_ref, y_buf), (gx_ref, gx_buf)]
    size, width = in_buf.shape[PAIR:]
    moves += [(in_ref.at[l, p, :, pl.ds(0, width)], in_buf.at[l, p]) for l in range(PAIR) for p in range(SIDE)]
    loads = [pltpu.make_async_copy(src, dst, came.at[k]) for k, (src, dst) in enumerate(moves)]
    for copy in loads:
        copy.start()
    stores = []

    def store(src, dst):
        copy = pltpu.make_async_copy(src, dst, left.at[len(stores)])
        copy.start()
        stores.append(copy)

    for l in range(PAIR):
        for p in range(SIDE):
            loads[SIDE * l + p].wait()
        store(out_buf.at[l, pl.ds(0, 15)], out_grad.at[l])
    for k, (src, dst) in enumerate(((y_buf, y_out), (gx_buf, gx_out))):
        loads[ROW + k].wait()
        store(src, dst)
    me = lax.axis_index("fsdp")
    for l in range(PAIR):
        for f in range(ROW):
            @pl.when(me == f)
            def _():
                scale_out[l:l + 1] = out_buf[l, 15, 0:1, f * count:(f + 1) * count]
    for l in range(PAIR):
        for p in range(SIDE):
            loads[10 + SIDE * l + p].wait()
            store(in_buf.at[l, p], in_grad.at[l, pl.ds(p * size, size)])
    for copy in stores:
        copy.wait()


def finish(in_sums, out_sums, y, gx, rows, proj):
    hbm = pl.BlockSpec(memory_space=pltpu.HBM)
    out = lambda *shape, dtype=F32: jax.ShapeDtypeStruct(shape, dtype)
    size, (depth, dim) = in_sums.shape[PAIR], out_sums.shape[TRIO:]
    in_grad, out_grad, y_out, gx_out, scale = pl.pallas_call(
        functools.partial(finish_kernel, rows),
        out_shape=(out(PAIR, rows, proj), out(PAIR, 15, depth, dim), out(*y.shape, dtype=BF), out(*gx.shape, dtype=BF), out(PAIR, rows)),
        in_specs=[hbm] * SIDE,
        out_specs=[hbm] * SIDE + [pl.BlockSpec(memory_space=pltpu.VMEM)],
        scratch_shapes=[
            pltpu.VMEM((PAIR, SIDE, size, proj), F32), pltpu.VMEM((PAIR, 16, depth, dim), F32), pltpu.VMEM(y.shape, BF), pltpu.VMEM(gx.shape, BF),
            pltpu.SemaphoreType.DMA((18,)), pltpu.SemaphoreType.DMA((12,)),
        ],
        compiler_params=pltpu.CompilerParams(vmem_limit_bytes=67043328),
        name="finish",
    )(in_sums, out_sums, y, gx)
    return y_out[None], gx_out[None], scale, in_grad, out_grad.reshape(PAIR, 15 * depth, dim)


def solution(mesh):
    fsdp_size = mesh.shape["fsdp"]
    batch_spec = P(("dp", "fsdp"), None, None)
    scale_spec = P(None, "fsdp")
    weight_spec = P(None, "fsdp", None)

    def device_step(x_in, grad_y, norm_scale, w_in, w_out):
        n_layers = w_in.shape[0]
        seq_len, model_dim = x_in.shape[1:]
        proj_dim = w_in.shape[PAIR]
        ff_dim = w_out.shape[1] * fsdp_size - model_dim
        head_dim = (proj_dim - model_dim - PAIR * ff_dim) // PAIR
        rows, rows_out = norm_scale.shape[1], w_out.shape[1]
        half_dim = head_dim // PAIR
        freq = 10000.0 ** (-np.arange(half_dim, dtype=np.float32) * 2.0 / head_dim)
        freq = jnp.asarray(np.tile(freq.astype(np.float32), (ROW, LANE // half_dim)))
        hidden, grad_hidden, *rest = run_layers(x_in[0], grad_y[0], norm_scale, w_in, w_out, freq)
        in_sums, out_sums = reduce_gradients((rest[0:SIDE], rest[SIDE:6], rest[6], rest[OTHERS:9], rest[9], rest[10], rest[11]))
        return finish(in_sums, out_sums, hidden, grad_hidden, rows, proj_dim)

    return jax.shard_map(
        device_step,
        mesh=mesh,
        in_specs=(batch_spec, batch_spec, scale_spec, weight_spec, weight_spec),
        out_specs=(batch_spec, batch_spec, scale_spec, weight_spec, weight_spec),
        check_vma=False,
    )
```

```python
import functools
import jax
import jax.numpy as jnp
import numpy as np
from jax import lax
from jax.experimental import pallas as pl
from jax.experimental.pallas import tpu as pltpu
from jax.sharding import PartitionSpec as P

MESH_ID = pl.DeviceIdType.MESH
BOTH = (1, -1)
AROUND = (1, -1, 2)
PARTS = (True, False)
ALL, ZERO = ..., 0.0
OTHERS = 7
QUICK, SHORT = 0.2, 0.3
LANE, WIDE, STRIP, HEAD = 128, 256, 512, 64
ROW, BAND, SIDE, TRIO, PAIR = 8, 32, 4, 3, 2


class Links:
    def __init__(self, send_sems, recv_sems):
        self.send_sems, self.recv_sems = send_sems, recv_sems
        self.slots, self.batches, self.sent, self.count = {}, {}, {}, 0

    def _landing(self, key, lane):
        if key not in self.slots:
            self.slots[key] = self.count
            self.count += 1 if lane is None else PAIR
        return self.recv_sems.at[self.slots[key] + (0 if lane is None else lane)]

    def send(self, key, src, dst, device, landing=None, whole=None, batch=None, lane=None):
        leaving = self.batches.setdefault(batch or key, len(self.batches))
        copy = pltpu.make_async_remote_copy(
            src_ref=src, dst_ref=dst, send_sem=self.send_sems.at[leaving], recv_sem=self._landing(landing or key, lane),
            device_id=device, device_id_type=MESH_ID)
        copy.start()
        self.sent[batch or key] = (src if whole is None else whole, leaving)

    def arrive(self, key, landed, lane=None):
        pltpu.make_async_copy(landed, landed, self._landing(key, lane)).wait()

    def drain(self):
        for left, leaving in self.sent.values():
            pltpu.make_async_copy(left, left, self.send_sems.at[leaving]).wait()
        self.sent.clear()


def rem(a, n):
    return a % n if isinstance(a, int) else lax.rem(a, n)


def chip_position():
    f, d = lax.axis_index("fsdp"), lax.axis_index("dp")
    return f // PAIR, rem(d, SIDE), d // SIDE, rem(f, PAIR)


def device_at(x, y, z, core):
    return (z * SIDE + y, x * PAIR + core)


def step(coord, by):
    return rem(coord + SIDE + by, SIDE)


def announce(devices):
    barrier = pltpu.get_barrier_semaphore()
    for device in devices:
        pl.semaphore_signal(barrier, inc=1, device_id=device, device_id_type=MESH_ID)
    pl.semaphore_wait(barrier, len(devices))


def plan(tasks, latency=2.5):
    free, landed, order, now = {}, {}, [], ZERO
    left = list(tasks)
    while left:
        best = None
        for place, (name, rank, start, needs, after, _, _) in enumerate(left):
            if all(n[0] in landed for n in needs) and all(n in landed for n in after):
                ready = max([start, now] + [landed[task][i] for task, i in needs])
                best = min(best or (ready, rank, place), (ready, rank, place))
        now, _, place = best
        name, _, _, _, _, sends, cost = left.pop(place)
        order.append(name)
        now += cost
        landed[name] = []
        for link, time, *more in sends:
            free[link] = max(now, free.get(link, ZERO)) + time
            landed[name].append(free[link] + latency + sum(more))
    return order


def layers_order(rows_i, cols_i, rows_o, cols_o, seq, starts):
    rate = 23300.0
    tasks = []
    for m in range(SIDE):
        is_in = m % PAIR == 0
        edge = cols_i // LANE * SIDE // 9 // PAIR * WIDE
        size = {"y": rows_i // SIDE * edge, "x": rows_i * (cols_i - PAIR * edge)} if is_in else {"y": rows_o // SIDE * cols_o // PAIR}
        size["z"] = size["y"]
        colors = "yzx" if is_in else "yz"
        tasks.append((("lend", m), 5, 3.0 + SIDE * m, [], [], [("chip", (rows_i * cols_i if is_in else rows_o * cols_o) / 120000.0)], QUICK))
        for color in colors:
            cost = size[color] / rate
            both = [(("x", by), cost) for by in BOTH]
            spread = [((color, by), cost) for by in BOTH] if color != "x" else []
            tasks.append((("reach", m, color), m, starts[m], [], [], both, QUICK))
            for i, by in enumerate(BOTH):
                tasks.append((("relay", m, color, by), m, ZERO, [(("reach", m, color), i)], [], [(("x", by), cost / PAIR)] + spread, QUICK))
            halves = [(("relay", m, color, by), 0) for by in BOTH]
            tasks.append((("far", m, color), m, ZERO, halves, [], spread, QUICK))
            if color == "x":
                continue
            for off, source, first in ((-1, ("relay", m, color, 1), 1), (1, ("relay", m, color, -1), 1), (PAIR, ("far", m, color), 0)):
                for i, by in enumerate(BOTH):
                    tasks.append((("pass", m, color, off, by), m, ZERO, [(source, first + i)], [], [((color, by), cost / PAIR)], QUICK))
                halves = [(("pass", m, color, off, by), 0) for by in BOTH]
                tasks.append((("close", m, color, off), m, ZERO, halves, [], [], QUICK))
        for off in (-1, 1, PAIR):
            last = [("close", m, color, off) for color in "yz"]
            if is_in:
                last.append(("far", m, "x") if off == PAIR else ("relay", m, "x", -off))
            tasks.append((("hand", m, off), m, ZERO, [], last, [("chip", (rows_i * cols_i if is_in else rows_o * cols_o) / 120000.0)], QUICK))
    before = []

    def work(name, cost, mats=()):
        needs = [(("hand", m, off), 0) for m in mats for off in (-1, 1, PAIR)] + [(("lend", m), 0) for m in mats]
        tasks.append((name, 99, ZERO, needs, list(before), [], cost))
        before[:] = [name]

    for l in range(PAIR):
        work(("norm", l), 0.8)
        work(("project", l), 4.0, [PAIR * l])
        work(("attend", l), 4.2)
        work(("mlp", l), 2.2)
        work(("put", l), 1.6, [PAIR * l + 1])
    for l in (1, 0):
        work(("back_out", l), 2.9)
        work(("back_mlp", l), 2.0)
        work(("back_heads", l), 1.0)
        work(("back_quad", l), 6.0)
        work(("back_keys", l), QUICK)
        for i in range(PAIR):
            work(("back_in", l, i), 1.3 + 0.6 * i)
        work(("back_norm", l), 1.0)
    def send(name, rank, start, after, sends):
        tasks.append((name, rank, start, [], [after] if after else [], sends, 0.4))

    def follow(name, rank, needs, sends):
        tasks.append((name, rank, ZERO, needs, [], sends, QUICK))

    def both(axis, size):
        return [((axis, by), size / rate, margin) for by in BOTH]

    model, margin = rows_i * ROW, 0.5
    for l in (1, 0):
        for axis in "yz":
            name = ("send_h", l, axis)
            send(name, 20 - l, 58.0, ("norm", l), both(axis, seq * model))
            for i, by in enumerate(BOTH):
                for index in range(PAIR):
                    follow(("pass_h", l, axis, by, index), 10, [(name, i)], [((axis, by), seq * model / SIDE / rate, margin)])
        send(("send_m", l), 22 - l, ZERO, ("mlp", l), both("x", PAIR * seq * rows_o) + both("x", PAIR * seq * rows_o))
        if l == 0:
            send(("own_y",), 15, ZERO, ("back_norm", 1), [])
            send(("send_scale", l), 15, ZERO, ("back_norm", l), [])
            continue
        name = ("send_y", l)
        send(name, 12, 42.0, None, both("x", seq * model))
        for i, by in enumerate(BOTH):
            follow(("pass_y", l, by), 12, [(name, i)], [(("x", by), seq * model / PAIR / rate, margin)])
        follow(("far_y", l), 12, [(("pass_y", l, by), 0) for by in BOTH], [])
        for axis in "zy":
            name = ("send_z", l, axis)
            share = seq * (cols_i + LANE) / ROW
            send(name, 13, ZERO, ("back_mlp", l), both(axis, share / PAIR) + both(axis, share))
            if axis == "y":
                name = ("rest_z", l)
                send(name, 13, ZERO, ("back_keys", l), both(axis, share / ROW) + both(axis, share / SIDE))
            for i, by in enumerate(BOTH):
                follow(("pass_z", l, axis, by), 13, [(name, i)], [((axis, by), share / PAIR / rate, margin)])
                follow(("twin_z", l, axis, by), 14, [(name, PAIR + i)], [])
            follow(("far_z", l, axis), 14, [(("pass_z", l, axis, by), 0) for by in BOTH], [])
        send(("send_scale", l), 15, ZERO, ("back_norm", l), [])
    send(("own_z",), 15, ZERO, ("back_keys", 0), [])
    return plan(tasks)


def gather_stages(links, position, shard_i, shard_o, wi, wo, lsem):
    x, y, z, core = position
    twin = device_at(x, y, z, 1 - core)
    rows_i, cols_i = shard_i.shape[1:]
    rows_o, cols_o = shard_o.shape[1:]
    quarter_i, quarter_o = rows_i // SIDE, rows_o // SIDE
    third_i = cols_i // LANE * SIDE // 9 // PAIR * WIDE
    half_o = cols_o // PAIR
    cut_o = quarter_o // 16 * ROW + ROW if quarter_o % 16 else quarter_o // PAIR
    place = {"x": x, "y": y, "z": z}

    spots = {(axis, o): step(place[axis], o) for axis in "xyz" for o in range(SIDE)}

    def spot(axis, o):
        return spots[axis, o % SIDE]

    table = {}
    for axis in "xyz":
        for o in range(1, SIDE):
            moved = {**place, axis: spot(axis, o)}
            table[axis, o] = device_at(moved["x"], moved["y"], moved["z"], core)

    def peer(axis, o):
        return table[axis, o % SIDE]

    mats = []
    for l in range(PAIR):
        mats.append((shard_i.at[l], wi.at[l], rows_i, True))
        mats.append((shard_o.at[l], wo.at[l], rows_o, False))

    def region(is_in, color, q):
        if is_in:
            if color == "x":
                lo, hi = PAIR * third_i, cols_i
                rows = (0, rows_i)
            else:
                lo, hi = (0, third_i) if color == "y" else (third_i, PAIR * third_i)
                rows = (q * quarter_i, quarter_i)
            mid = lo + ((hi - lo) // LANE + 1) // PAIR * LANE
            return (rows, (lo, hi - lo)), (rows, (lo, mid - lo)), (rows, (mid, hi - mid))
        cols = (0, half_o) if color == "y" else (half_o, half_o)
        start = q * quarter_o
        return ((start, quarter_o), cols), ((start, cut_o), cols), ((start + cut_o, quarter_o - cut_o), cols)

    def at(m, xb, area):
        (r, nr), (c, nc) = area
        _, out, size, _ = mats[m]
        return out.at[pl.ds(pl.multiple_of((PAIR * xb + core) * size + r, ROW), nr), pl.ds(c, nc)]

    def block(m, xb, index):
        _, out, size, _ = mats[m]
        return out.at[pl.ds(pl.multiple_of((PAIR * xb + index) * size, BAND), size)]

    def group(m, color):
        _, out, _, is_in = mats[m]
        (_, nr), (c, nc) = region(is_in, color, 0)[0]
        return dict(batch=(m, color), whole=out.at[pl.ds(0, nr * (TRIO if color == "x" else 12)), pl.ds(c, nc)])

    def reach(m, color):
        src, _, _, is_in = mats[m]
        area = region(is_in, color, place[color])[0]
        for by in BOTH:
            links.send((m, "x1", color, by), src.at[pl.ds(pl.multiple_of(area[0][0], ROW), area[0][1]), pl.ds(*area[1])], at(m, x, area), peer("x", by), **group(m, color))

    def launch(m, color, off):
        is_in = mats[m][TRIO]
        moved = at(m, spot("x", off), region(is_in, color, place[color])[0])
        for by in BOTH:
            links.send((m, "p1", color, off, by), moved, moved, peer(color, by), **group(m, color))

    def relay(m, color, by):
        is_in = mats[m][TRIO]
        xb = spot("x", -by)
        areas = region(is_in, color, place[color])
        links.arrive((m, "x1", color, by), at(m, xb, areas[0]))
        part = at(m, xb, areas[1] if by == 1 else areas[PAIR])
        links.send((m, "x2", color), part, part, peer("x", by), **group(m, color))
        if color != "x":
            launch(m, color, -by)

    def far(m, color):
        is_in = mats[m][TRIO]
        links.arrive((m, "x2", color), at(m, spot("x", PAIR), region(is_in, color, place[color])[0]))
        if color != "x":
            launch(m, color, PAIR)

    def pass_on(m, color, off, by):
        is_in = mats[m][TRIO]
        xb = spot("x", off)
        areas = region(is_in, color, spot(color, -by))
        links.arrive((m, "p1", color, off, by), at(m, xb, areas[0]))
        part = at(m, xb, areas[1] if by == 1 else areas[PAIR])
        links.send((m, "p2", color, off), part, part, peer(color, by), **group(m, color))

    def close(m, color, off):
        is_in = mats[m][TRIO]
        links.arrive((m, "p2", color, off), at(m, spot("x", off), region(is_in, color, spot(color, PAIR))[0]))

    def four(m):
        _, out, size, _ = mats[m]
        return out.at[pl.ds(0, SIDE * size)]

    def give(m, src, dst):
        links.send((m, "chip"), src, dst, twin, batch=(m, "chip"), whole=four(m))

    def hand(m, off):
        whole = block(m, spot("x", off), core)
        give(m, whole, whole)

    owns = []

    def begin():
        for m, (src, _, _, _) in enumerate(mats):
            copy = pltpu.make_async_copy(src, block(m, x, core), lsem.at[m])
            copy.start()
            owns.append(copy)

    def lend(m):
        give(m, mats[m][0], block(m, x, core))

    def ready(m):
        owns[m].wait()
        links.arrive((m, "chip"), four(m))

    return begin, ready, peer, {"reach": reach, "relay": relay, "far": far, "pass": pass_on, "close": close, "hand": hand, "lend": lend}


BF, F32 = jnp.bfloat16, jnp.float32


def product(a, b, contract=((1,), (0,))):
    return lax.dot_general(a, b, (contract, ((), ())), preferred_element_type=F32)


def lanes(start, size):
    return pl.ds(start if isinstance(start, int) else pl.multiple_of(start, LANE), size)


def layers_kernel(order, sc_ref, wi_ref, wo_ref, x_ref, dy_ref, freq_ref,
                  y_ref, gx_ref, hy_a, hy_b, hz_a, hz_b, mx_a, mx_b, yx_b, zy_b, zz_b, z_a, dy_a, sc_out, relay_z,
                  wi, wo, z, om, h, hid, qr, kts, vsl, ksl, turned_q, turned_o, scores, dscores, pcat, dscat, cos_ref, sin_ref, turn_ref,
                  dot_heads, qt, dht, dkv, omt, ht, dyt, sc, gains, own_gain, gain_ref, load_sems, own_sems, send_sems, recv_sems,
                  share_send_sems, share_recv_sems):
    seq, dim = x_ref.shape
    ff = (wi.shape[PAIR] - dim - LANE) // PAIR
    position = chip_position()
    x, y, zc, core = position
    twin = device_at(x, y, zc, 1 - core)
    me = PAIR * x + core
    links, shared = Links(send_sems, recv_sems), Links(share_send_sems, share_recv_sems)
    stored = []
    spots, _ = around(position)
    h_out, m_out, y_out, z_out = {"y": (hy_a, hy_b), "z": (hz_a, hz_b)}, (mx_a, mx_b), {1: yx_b}, {(1, "y"): zy_b, (1, "z"): zz_b}
    middle = hid.at[1]
    begin, ready, peer, stages = gather_stages(links, position, wi_ref, wo_ref, wi, wo, load_sems)
    others = [(zc * SIDE + y, rem(me + k, ROW)) for k in range(1, ROW)]

    def spot(axis, o):
        return spots[axis, o % SIDE]

    def device(axis, o, index):
        moved = {"x": x, "y": y, "z": zc, axis: spot(axis, o)}
        return device_at(moved["x"], moved["y"], moved["z"], index)

    own_gain[ALL] = jnp.zeros(own_gain.shape, F32)
    count = sc_ref.shape[1]
    for f in range(ROW):
        @pl.when(me == f)
        def _():
            own_gain[0:PAIR, f * count:(f + 1) * count] = sc_ref[ALL].astype(F32)
    announce(others + [device(axis, o, index) for axis in "yz" for o in AROUND for index in range(PAIR)])
    begin()
    for k, far in enumerate(others):
        links.send(("sc",), own_gain, gains.at[me], far, batch=("sc",), whole=gains.at[pl.ds(0, OTHERS)])

    def keep(src, dst):
        copy = pltpu.make_async_copy(src, dst, own_sems.at[len(stored)])
        copy.start()
        stored.append(copy)

    def tokens(axis, o, index):
        return pl.ds(pl.multiple_of((PAIR * spot(axis, o) + index) * seq, seq), seq)

    def place(axis, o, index):
        return PAIR * spot(axis, o) + index

    def columns(axis, o):
        size = z.shape[PAIR] // ROW
        return lanes(((0 if axis == "y" else SIDE) + spot(axis, o)) * size, size)

    def several(batch, ref, n):
        whole = ref.at[pl.ds(0, n * seq if batch[0][0] in "yz" else n)]
        return dict(batch=batch, whole=whole)

    def send_h(l, axis):
        out = h_out[axis][l].at[place(axis, 0, core)]
        for by in BOTH:
            for index in range(PAIR):
                shared.send(("h", l, axis, by), ht.at[l, :, index], out, device(axis, by, index), lane=core, **several(("h", l, axis), h_out[axis][l], OTHERS))
        shared.send(("h", l, axis), ht.at[l, :, 1 - core], out, twin, **several(("h", l, axis), h_out[axis][l], OTHERS))
        keep(ht.at[l, :, core], out)

    def pass_h(l, axis, by, index):
        out = h_out[axis][l]
        shared.arrive(("h", l, axis, by), out.at[place(axis, -by, index)], index)
        part = out.at[place(axis, -by, index), pl.ds(1 - by, PAIR)]
        shared.send(("h", l, axis), part, part, device(axis, by, core), **several(("h", l, axis), out, OTHERS))

    def arrive_h(l):
        for axis in "yz":
            shared.arrive(("h", l, axis), h_out[axis][l].at[pl.ds(0, TRIO)])

    def row_block(l, o, index):
        size = omt.shape[1] // ROW
        return omt.at[l, pl.ds(pl.multiple_of((PAIR * spot("x", o) + index) * size, BAND), size)]

    def send_m(l):
        out, batch = m_out[l].at[place("x", 0, core)], several(("m", l), m_out[l], OTHERS)
        for o in AROUND:
            for index in range(PAIR):
                shared.send(("m", l), row_block(l, o, index), out, device("x", o, index), **batch)
        shared.send(("m", l), row_block(l, 0, 1 - core), out, twin, **batch)
        keep(row_block(l, 0, core), out)

    def arrive_m(l):
        shared.arrive(("m", l), m_out[l].at[pl.ds(0, OTHERS)])

    def token_half(axis, o, k):
        return pl.ds(pl.multiple_of((PAIR * spot(axis, o) + core) * seq + k * (seq // PAIR), seq // PAIR), seq // PAIR)

    def send_y(l):
        src, out = dy_ref, y_out[l].at[tokens("x", 0, core)]
        for by in BOTH:
            shared.send(("y", l, by), src, out, device("x", by, core), **several(("y", l), y_out[l], OTHERS))
        shared.send(("y", l), src, out, twin, **several(("y", l), y_out[l], OTHERS))
        keep(src, out)

    def pass_y(l, by):
        landed, part = y_out[l].at[tokens("x", -by, core)], y_out[l].at[token_half("x", -by, (1 - by) // PAIR)]
        shared.arrive(("y", l, by), landed)
        shared.send(("y2", l), part, part, device("x", by, core), **several(("y", l), y_out[l], OTHERS))
        shared.send(("y", l), landed, landed, twin, **several(("y", l), y_out[l], OTHERS))

    def far_y(l):
        landed = y_out[l].at[tokens("x", PAIR, core)]
        shared.arrive(("y2", l), landed)
        shared.send(("y", l), landed, landed, twin, **several(("y", l), y_out[l], OTHERS))

    def arrive_y(l):
        shared.arrive(("y", l), y_out[l].at[pl.ds(0, SIDE * seq)])

    def push_z(l, axis, o, ready):
        out = z_out[l, axis].at[tokens(axis, 0, core)]
        batch = several(("z", l, axis), z_out[l, axis], ROW)

        def start():
            if o != PAIR:
                shared.send(("z", l, axis, o), z.at[l, :, columns(axis, o)], out, device(axis, o, core), **batch)
                return
            for k, by in enumerate(BOTH):
                shared.send(("zr", l, axis, by), z.at[l, pl.ds(k * (seq // PAIR), seq // PAIR), columns(axis, PAIR)], relay_z.at[l, "yz".index(axis), k],
                            device(axis, by, core), **batch)

        if ready is None:
            start()
        else:
            pl.when(ready)(start)

    def own_part(l, axis):
        out, mine = z_out[l, axis].at[tokens(axis, 0, core)], z.at[l, :, columns(axis, 0)]
        shared.send(("z", l, axis), mine, out, twin, **several(("z", l, axis), z_out[l, axis], ROW))
        keep(mine, out)

    def send_z(l, axis):
        for o in (PAIR, 1, -1):
            push_z(l, axis, o, spot(axis, o) != 0 if axis == "y" else None)
        if axis == "z":
            own_part(l, axis)

    def rest_z(l):
        for o in (PAIR, 1, -1):
            push_z(l, "y", o, spot("y", o) == 0)
        own_part(l, "y")

    def pass_z(l, axis, by):
        k = (1 - by) // PAIR
        half = relay_z.at[l, "yz".index(axis), k]
        shared.arrive(("zr", l, axis, by), half)
        shared.send(("z2", l, axis), half, z_out[l, axis].at[token_half(axis, -by, k)], device(axis, by, core), **several(("z", l, axis), z_out[l, axis], ROW))

    def twin_z(l, axis, by):
        landed = z_out[l, axis].at[tokens(axis, -by, core)]
        shared.arrive(("z", l, axis, by), landed)
        shared.send(("z", l, axis), landed, landed, twin, **several(("z", l, axis), z_out[l, axis], ROW))

    def far_z(l, axis):
        landed = z_out[l, axis].at[tokens(axis, PAIR, core)]
        shared.arrive(("z2", l, axis), landed)
        shared.send(("z", l, axis), landed, landed, twin, **several(("z", l, axis), z_out[l, axis], ROW))

    def arrive_z(l, axis):
        shared.arrive(("z", l, axis), z_out[l, axis].at[pl.ds(0, SIDE * seq)])

    def send_scale(l):
        for far in others:
            shared.send(("scale", l), sc.at[l], sc_out.at[l, me], far, batch=("scale", l), whole=sc_out.at[l, pl.ds(0, OTHERS)])
        keep(sc.at[l], sc_out.at[l, me])

    def arrive_scale(l):
        shared.arrive(("scale", l), sc_out.at[l, pl.ds(0, OTHERS)])

    gains[me] = own_gain[ALL]
    z[:, :, wi.shape[PAIR]:] = jnp.zeros((PAIR, seq, z.shape[PAIR] - wi.shape[PAIR]), BF)
    entry = (x_ref, hid.at[0])
    angle = lax.broadcasted_iota(jnp.int32, (seq, LANE), 0).astype(F32) * freq_ref[0:1]
    for half in range(PAIR):
        cos_ref[:, LANE * half:LANE * (half + 1)] = jnp.cos(angle)
        sin_ref[:, LANE * half:LANE * (half + 1)] = jnp.sin(angle)
    lane = lax.broadcasted_iota(jnp.int32, turn_ref.shape, 1)
    down = lax.broadcasted_iota(jnp.int32, turn_ref.shape, 0) - lane
    low = rem(lane, HEAD) < BAND
    turn_ref[ALL] = jnp.where(low & (down == BAND), -1.0, jnp.where(jnp.logical_not(low) & (down == -BAND), 1.0, ZERO)).astype(BF)
    kts[ALL] = jnp.zeros(kts.shape, BF)
    pcat[ALL] = jnp.zeros(pcat.shape, BF)
    dscat[ALL] = jnp.zeros(dscat.shape, BF)

    def normalise(l, src):
        @pl.loop(0, seq // BAND, unroll=SIDE)
        def _(r):
            rows = pl.ds(pl.multiple_of(r * BAND, BAND), BAND)
            v = src[rows].astype(F32)
            v = v - jnp.mean(v, axis=-1, keepdims=True)
            var = jnp.mean(v * v, axis=-1, keepdims=True)
            h[l, rows] = (v * lax.rsqrt(var + 1e-6) * gain_ref[l:l + 1]).astype(BF)

    def project(l):
        strip = wi.shape[PAIR] // 5

        @pl.loop(0, 5)
        def _(i):
            at = lanes(i * strip, strip)
            z[l, :, at] = product(h[l], wi[l, :, at]).astype(BF)

    def heads(l):
        cos, sin = cos_ref[ALL], sin_ref[ALL]
        for g in range(dim // WIDE):
            q = z[l, :, g * WIDE:(g + 1) * WIDE]
            qr[l, :, g * WIDE:(g + 1) * WIDE] = ((q.astype(F32) * cos + product(q, turn_ref[ALL]) * sin) * 0.125).astype(BF)
        kv = z[l, :, dim:dim + LANE]
        turned = kv.astype(F32) * cos[:, :LANE] + product(kv, turn_ref[:LANE, :LANE]) * sin[:, :LANE]
        first = lax.broadcasted_iota(jnp.int32, turned.shape, 1) < HEAD
        key_lo = jnp.where(first, turned, ZERO)
        val_hi = jnp.where(first, ZERO, kv.astype(F32))
        return key_lo, pltpu.roll(key_lo, HEAD, 1), pltpu.roll(val_hi, HEAD, 1), val_hi

    def slot_rows(ref, lo, hi):
        zero = jnp.zeros((seq, LANE), BF)
        lo, hi = lo.astype(BF), hi.astype(BF)
        for i, (left, right) in enumerate(((lo, zero), (hi, zero), (zero, lo), (zero, hi))):
            ref[i * seq:(i + 1) * seq, :LANE] = left
            ref[i * seq:(i + 1) * seq, LANE:] = right

    def slot_cols(ref, lo):
        flat = lo.T[:HEAD].astype(BF)
        for i in range(SIDE):
            ref[HEAD * i:HEAD * (i + 1), i * seq:(i + 1) * seq] = flat

    def chances(i, half):
        at = slice(LANE * half, LANE * (half + 1))
        blocks = [pl.ds(pl.multiple_of(i * seq + LANE * k, LANE), LANE) for k in range(half + 1)]
        s = [scores[keys, at] for keys in blocks]
        lower = lax.broadcasted_iota(jnp.int32, s[-1].shape, 1) >= lax.broadcasted_iota(jnp.int32, s[-1].shape, 0)
        s[-1] = jnp.where(lower, s[-1], -1e30)
        top = functools.reduce(jnp.maximum, [jnp.max(v, axis=0, keepdims=True) for v in s])
        e = [jnp.exp(v - top) for v in s]
        scale = 1.0 / sum(jnp.sum(v, axis=0, keepdims=True) for v in e)
        return at, [(keys, v * scale) for keys, v in zip(blocks, e)]

    def attend(l):
        key_lo, key_hi, val_lo, _ = heads(l)
        slot_rows(ksl, key_lo, key_hi)
        slot_cols(kts, val_lo)
        flip(lambda at: qr[l, :, lanes(at, WIDE)], qt, dim)

        @pl.loop(0, dim // WIDE)
        def _(g):
            rows = pl.ds(pl.multiple_of(g * WIDE, WIDE), WIDE)
            scores[ALL] = product(ksl[ALL], qt[rows])

            @pl.loop(0, SIDE)
            def _(i):
                for half in range(PAIR):
                    at, blocks = chances(i, half)
                    for keys, p in blocks:
                        pcat[keys, at] = p.astype(BF)
            flat = product(kts[ALL], pcat[ALL]).astype(BF)
            omt[l, rows] = flat
            om[:, lanes(g * WIDE, WIDE)] = flat.T

    def mlp(l):
        @pl.loop(0, seq // BAND)
        def _(r):
            rows = pl.ds(pl.multiple_of(r * BAND, BAND), BAND)

            @pl.loop(0, ff // STRIP)
            def _(i):
                gate = z[l, rows, lanes(dim + LANE + i * STRIP, STRIP)].astype(F32)
                up = z[l, rows, lanes(dim + LANE + ff + i * STRIP, STRIP)].astype(F32)
                om[rows, lanes(dim + i * STRIP, STRIP)] = (gate * jax.nn.sigmoid(gate) * up).astype(BF)

    def put_out(l, dst):
        for n in range(dim // WIDE):
            cols = slice(n * WIDE, (n + 1) * WIDE)
            total = product(om[ALL], wo[l, :, cols])
            dst[:, cols] = (entry[l][:, cols].astype(F32) + total).astype(BF)

    def flip(src, dst, width, first=0):
        @pl.loop(first // WIDE, width // WIDE)
        def _(i):
            dst[pl.ds(pl.multiple_of(i * WIDE, WIDE), WIDE)] = src(i * WIDE).T

    upstream = (middle, dy_ref)

    def back_out(l):
        dy = upstream[l]
        flip(lambda at: dy[:, lanes(at, WIDE)], dyt, dim)

        @pl.loop(0, wo.shape[1] // dim)
        def _(n):
            rows = pl.ds(pl.multiple_of(n * dim, dim), dim)
            part = product(wo[l, rows], dyt[ALL]).astype(BF)
            om[:, lanes(n * dim, dim)] = part.T

            @pl.when(n == 0)
            def _():
                dot_heads[ALL] = part

    def back_mlp(l):
        @pl.loop(0, seq // BAND)
        def _(r):
            rows = pl.ds(pl.multiple_of(r * BAND, BAND), BAND)

            @pl.loop(0, ff // STRIP)
            def _(i):
                gate_at, up_at = lanes(dim + LANE + i * STRIP, STRIP), lanes(dim + LANE + ff + i * STRIP, STRIP)
                gate, up = z[l, rows, gate_at].astype(F32), z[l, rows, up_at].astype(F32)
                d = om[rows, lanes(dim + i * STRIP, STRIP)].astype(F32)
                sig = jax.nn.sigmoid(gate)
                du = d * up
                z[l, rows, gate_at] = (du * sig + du * gate * (sig * (1.0 - sig))).astype(BF)
                z[l, rows, up_at] = (d * (gate * sig)).astype(BF)

    def back_heads(l):
        key_lo, key_hi, val_lo, val_hi = heads(l)
        slot_rows(ksl, key_lo, key_hi)
        slot_rows(vsl, val_lo, val_hi)
        slot_cols(kts, key_lo)
        dkv[ALL] = jnp.zeros(dkv.shape, F32)
        flip(lambda at: qr[l, :, lanes(at, WIDE)], qt, dim)
        for at in range(0, dim, LANE):
            pair = slice(at, at + LANE)
            turned_q[:, pair] = pltpu.roll(qr[l, :, pair].astype(F32), HEAD, 1).astype(BF)
            turned_o[:, pair] = pltpu.roll(om[:, pair].astype(F32), HEAD, 1).astype(BF)

    def back_quad(l):
        @pl.loop(0, dim // WIDE)
        def _(g):
            quad(l, g)

    def quad(l, g):
        cols = pl.ds(pl.multiple_of(g * WIDE, WIDE), WIDE)
        scores[ALL] = product(ksl[ALL], qt[cols])
        dscores[ALL] = product(vsl[ALL], dot_heads[cols])

        @pl.loop(0, SIDE)
        def _(i):
            for half in range(PAIR):
                at, blocks = chances(i, half)
                given = [p * dscores[keys, at].astype(BF).astype(F32) for keys, p in blocks]
                total = sum(jnp.sum(v, axis=0, keepdims=True) for v in given)
                for (keys, p), v in zip(blocks, given):
                    pcat[keys, at] = p.astype(BF)
                    dscat[keys, at] = (v - p * total).astype(BF)
        dq = product(kts[ALL], dscat[ALL]).astype(BF).T
        back = dq.astype(F32) * cos_ref[ALL] - product(dq, turn_ref[ALL]) * sin_ref[ALL]
        z[l, :, cols] = (back * 0.125).astype(BF)
        def pieces(left, even, odd):
            for i in range(SIDE):
                pair = lanes(g * WIDE + i // PAIR * LANE, LANE)
                yield product(left[i * seq:(i + 1) * seq, :], odd(pair) if i % PAIR else even(pair))

        dkv[0] += sum(pieces(dscat, lambda at: qr[l, :, at], lambda at: turned_q[:, at]))
        dkv[1] += sum(pieces(pcat, lambda at: turned_o[:, at], lambda at: om[:, at]))

    def back_keys(l):
        dk = dkv[0].astype(BF)
        turned = dk.astype(F32) * cos_ref[:, :LANE] - product(dk, turn_ref[:LANE, :LANE]) * sin_ref[:, :LANE]
        first = lax.broadcasted_iota(jnp.int32, turned.shape, 1) < HEAD
        z[l, :, dim:dim + LANE] = jnp.where(first, turned, dkv[1]).astype(BF)

    def back_in(l, half):
        width = wi.shape[PAIR] // 5
        at = slice(PAIR * half * width, (PAIR + TRIO * half) * width)
        part = product(wi[l, :, at], z[l, :, at], ((1,), (1,)))
        dht[ALL] = dht[ALL] + part if half else part

    def back_norm(l):
        dy, dst = upstream[l], (gx_ref, middle)[l]
        for i in range(dim // WIDE):
            cols = slice(i * WIDE, (i + 1) * WIDE)
            h[l, :, cols] = dht[cols].T.astype(BF)
        sc[l] = jnp.zeros(sc.shape[1:], F32)

        @pl.loop(0, seq // BAND, unroll=SIDE)
        def _(r):
            rows = pl.ds(pl.multiple_of(r * BAND, BAND), BAND)
            v = entry[l][rows].astype(F32)
            v = v - jnp.mean(v, axis=-1, keepdims=True)
            scale = lax.rsqrt(jnp.mean(v * v, axis=-1, keepdims=True) + 1e-6)
            hat = v * scale
            d = h[l, rows].astype(F32)
            each = (d * hat).reshape(SIDE, ROW, dim)
            sc[l] += (each[0] + each[1]) + (each[PAIR] + each[TRIO])
            d = d * gain_ref[l:l + 1]
            d = scale * (d - jnp.mean(d, axis=-1, keepdims=True) - hat * jnp.mean(d * hat, axis=-1, keepdims=True))
            dst[rows] = (dy[rows].astype(F32) + d.astype(BF).astype(F32)).astype(BF)

    def do_norm(l):
        if l == 0:
            links.arrive(("sc",), gains.at[pl.ds(0, OTHERS)])
            gain_ref[ALL] = jnp.sum(gains[ALL], axis=0)
        normalise(l, entry[l])
        for i in range(dim // WIDE):
            flat = h[l, :, i * WIDE:(i + 1) * WIDE].T
            size = ht.shape[TRIO]
            for b in range(ROW):
                lo, hi = max(b * size, i * WIDE), min((b + 1) * size, (i + 1) * WIDE)
                if lo < hi:
                    ht[l, b // PAIR, b % PAIR, lo - b * size:hi - b * size] = flat[lo - i * WIDE:hi - i * WIDE]

    def do_project(l):
        ready(PAIR * l)
        project(l)

    def do_mlp(l):
        mlp(l)
        flip(lambda at: om[:, lanes(at, WIDE)], omt.at[l], om.shape[1], dim)

    def do_put(l):
        ready(PAIR * l + 1)
        put_out(l, hid.at[0] if l == 0 else y_ref)

    stages.update(
        norm=do_norm, project=do_project, attend=attend, mlp=do_mlp, put=do_put, back_out=back_out, back_mlp=back_mlp, back_heads=back_heads,
        back_quad=back_quad, back_keys=back_keys, back_in=back_in, back_norm=back_norm, send_h=send_h, pass_h=pass_h, send_m=send_m, send_y=send_y, pass_y=pass_y, far_y=far_y, send_z=send_z, rest_z=rest_z, pass_z=pass_z, twin_z=twin_z, far_z=far_z,
        send_scale=send_scale, own_z=lambda: keep(z.at[0], z_a), own_y=lambda: keep(middle, dy_a))
    for kind, *task in order:
        stages[kind](*task)
    for l in range(PAIR):
        arrive_h(l)
        arrive_m(l)
        arrive_scale(l)
    arrive_y(1)
    for l, axis in z_out:
        arrive_z(l, axis)
    for copy in stored:
        copy.wait()
    shared.drain()
    links.drain()


def run_layers(x, dy, scale, w_in, w_out, freq, starts=(ZERO, 10.0, 20.0, 30.0)):
    seq, dim = x.shape
    proj, cat = w_in.shape[PAIR], ROW * w_out.shape[1]
    wide = proj + LANE
    hbm, vmem = pl.BlockSpec(memory_space=pltpu.HBM), pl.BlockSpec(memory_space=pltpu.VMEM)
    out = lambda *shape, dtype=BF: jax.ShapeDtypeStruct(shape, dtype)
    buffer = lambda *shape, dtype=BF: pltpu.VMEM(shape, dtype)
    sem = pltpu.SemaphoreType.DMA
    line = ROW * seq
    return pl.pallas_call(
        functools.partial(layers_kernel, layers_order(*w_in.shape[1:], *w_out.shape[1:], seq, starts)),
        out_shape=(out(seq, dim), out(seq, dim), *[out(ROW, SIDE, dim // ROW, seq)] * SIDE, *[out(ROW, cat // ROW, seq)] * PAIR, out(line, dim),
                   *[out(line, wide // ROW)] * PAIR, out(seq, wide), out(seq, dim), out(PAIR, ROW, ROW, dim, dtype=F32),
                   out(PAIR, PAIR, PAIR, seq // PAIR, wide // ROW)),
        in_specs=[vmem, hbm, hbm] + [vmem] * TRIO,
        out_specs=[vmem] * PAIR + [hbm] * 13,
        scratch_shapes=[
            buffer(PAIR, dim, proj), buffer(PAIR, cat, dim), buffer(PAIR, seq, wide), buffer(seq, cat), buffer(PAIR, seq, dim),
            buffer(PAIR, seq, dim), buffer(PAIR, seq, dim),
            buffer(WIDE, SIDE * seq), buffer(SIDE * seq, WIDE), buffer(SIDE * seq, WIDE), buffer(seq, dim), buffer(seq, dim),
            buffer(SIDE * seq, seq, dtype=F32), buffer(SIDE * seq, seq, dtype=F32), buffer(SIDE * seq, seq), buffer(SIDE * seq, seq),
            buffer(seq, WIDE, dtype=F32), buffer(seq, WIDE, dtype=F32), buffer(WIDE, WIDE),
            buffer(dim, seq), buffer(dim, seq), buffer(dim, seq, dtype=F32), buffer(PAIR, seq, LANE, dtype=F32),
            buffer(PAIR, cat, seq), buffer(PAIR, SIDE, PAIR, dim // ROW, seq), buffer(dim, seq), buffer(PAIR, ROW, dim, dtype=F32),
            buffer(ROW, ROW, dim, dtype=F32), buffer(ROW, dim, dtype=F32), buffer(ROW, dim, dtype=F32),
            sem((SIDE,)), sem((13,)), sem((15,)), sem((107,)), sem((11,)), sem((40,)),
        ],
        compiler_params=pltpu.CompilerParams(collective_id=PAIR, has_side_effects=True, vmem_limit_bytes=67043328),
        name="run_layers",
    )(scale, w_in, w_out, x, dy, freq)


PARTS = (("i", "x", "z", "y", 0, STRIP), ("i", "x", "z", "y", STRIP, 384), ("i", "x", "y", "z", 0, STRIP), ("i", "x", "y", "z", STRIP, 384),
         ("o", "y", "z", "y", 0, 384), ("o", "z", "y", "z", 384, 384))


def reduce_order(rows, rows_b, starts):
    rate = 11650.0
    tasks = []
    sizes = {"y": WIDE * 896 / (PAIR * rate), "z": WIDE * 896 / (PAIR * rate), "x": WIDE * 768 / (PAIR * rate)}
    for axis in "yzx":
        size = sizes[axis]
        tasks.append((("swap", axis), (0, 0), starts[PAIR] if axis == "x" else starts[TRIO], [], [],
                      [((axis, by), size * n) for by, n in ((-1, 0.5), (1, 1), (-1, 1), (1, 1))], SHORT))
        tasks.append((("relay", axis), (0, 0), ZERO, [(("swap", axis), 0)], [], [((axis, -1), size / PAIR)], SHORT))
        for o, needs in ((1, [(("swap", axis), 1)]), (-1, [(("swap", axis), PAIR)]), (PAIR, [(("swap", axis), TRIO), (("relay", axis), 0)])):
            tasks.append((("near", axis, o), (0, PAIR), ZERO, needs, [], [("chip", 1.6)], QUICK))
    tasks.append((("fetch", 0), (5, 0), ZERO, [], [("make", 1, len(PARTS) - 1)], [], QUICK))
    for l in (1, 0):
        late = 1 - l
        for c, (kind, first, then, last, at, width) in enumerate(PARTS):
            needs, cost = [], 1.6 * width / STRIP
            if l == 0:
                needs = [(("near", last if kind == "i" else "x", o), 0) for o in AROUND]
            tasks.append((("make", l, c), (9 * late, c), starts[late], needs, [] if l else [("fetch", 0)], [], cost))
            full = SIDE * SIDE * (rows if kind == "i" else rows_b) * width / rate
            sends = [[((first, by), full / ROW) for by in BOTH], [((first, by), full / SIDE) for by in BOTH],
                     [((then, o), full / 16) for o in (1, -1, 1)], []]
            piece = full / 16
            sends += [[((then, o), piece) for o in (1, -1, 1)], [((last, by), SIDE * piece) for by in BOTH],
                      [((last, by), PAIR * piece) for by in BOTH], []]
            for s in range(ROW):
                task = ("sum", l, c, s)
                needs = [(("sum", l, c, s - 1), k) for k in range(len(sends[s - 1]))] if s else []
                tasks.append((task, (late, -s), ZERO, needs, [("make", l, c)] if s == 0 else [("sum", l, c, s - 1)], sends[s], SHORT))
    return plan(tasks)


def reduce_kernel(order, *refs):
    hy, hz, mx = refs[0:PAIR], refs[PAIR:SIDE], refs[SIDE:6]
    yx1, zy1, zz1, z0, y0, sc = refs[6:12]
    oa, ob = refs[12:14]
    n = len(PARTS)
    total, half, full, small, front = (refs[14 + k * n:14 + (k + 1) * n] for k in range(5))
    (hbuf, zbuf, mbuf, ybuf, scbuf, rz, ry, ssem, rsem, isem, osem) = refs[14 + 5 * n:]
    position = chip_position()
    x, y, zc, core = position
    place = {"x": x, "y": y, "z": zc}
    twin = device_at(x, y, zc, 1 - core)
    spots, peers = around(position)

    def spot(axis, o):
        return spots[axis, o % SIDE]

    def peer(axis, o):
        return peers[axis, o % SIDE]

    seq, wide = z0.shape
    own = wide // ROW
    loads, moving = {}, []

    def load(key, src, dst):
        copy = pltpu.make_async_copy(src, dst, isem.at[len(moving)])
        moving.append(key)
        copy.start()
        loads[key] = copy

    def fetch(l):
        if not l:
            load(("h", 0, "y"), hy[0], hbuf.at[0, 0])
        else:
            load(("z", 1, "z"), zz1, zbuf.at[1, 1])
        load(("h", l, "z"), hz[l], hbuf.at[l, 1])
        load(("m", l), mx[l], mbuf.at[l])
        if l:
            load(("y", 1), yx1, ybuf.at[1])
        load(("s", l), sc.at[l], scbuf.at[l])

    load(("z", 1, "y"), zy1, zbuf.at[1, 0])
    load(("h", 1, "y"), hy[1], hbuf.at[1, 0])
    done = set()

    def loaded(*keys):
        for key in keys:
            if key not in done:
                loads[key].wait()
                done.add(key)

    announce([peer(axis, o) for axis in "xyz" for o in AROUND] + [twin])
    fetch(1)
    links = Links(ssem, rsem)

    def columns(axis, o):
        return lanes(((0 if axis == "y" else SIDE) + spot(axis, o)) * own, own)

    def tokens(axis, o, index):
        return pl.ds(pl.multiple_of((PAIR * spot(axis, o) + index) * seq, seq), seq)

    def target(axis):
        return ybuf.at[0] if axis == "x" else zbuf.at[0, "yz".index(axis)]

    def leaving(axis):
        return dict(batch=("swap", axis), whole=target(axis).at[pl.ds(0, OTHERS * seq + seq // PAIR)])

    def half_at(axis, o, k):
        start = (PAIR * spot(axis, o) + core) * seq + k * (seq // PAIR)
        return target(axis).at[pl.ds(pl.multiple_of(start, seq // PAIR), seq // PAIR)]

    def relay_of(axis):
        return ry if axis == "x" else rz.at["yz".index(axis)]

    def swap(axis):
        def part(o, rows=slice(None)):
            return y0.at[rows] if axis == "x" else z0.at[rows, columns(axis, o)]

        mine = target(axis).at[tokens(axis, 0, core)]
        links.send(("relay", axis), part(PAIR, pl.ds(seq // PAIR, seq // PAIR)), relay_of(axis), peer(axis, -1), **leaving(axis))
        for by in BOTH:
            links.send(("swap", axis, by), part(by), mine, peer(axis, by), **leaving(axis))
        links.send(("swap", axis, PAIR), part(PAIR, pl.ds(0, seq // PAIR)), half_at(axis, 0, 0), peer(axis, PAIR), **leaving(axis))
        links.send(("near", axis), part(0), mine, twin, **leaving(axis))
        load(("own", axis), part(0), mine)

    def relay(axis):
        links.arrive(("relay", axis), relay_of(axis))
        links.send(("relayed", axis), relay_of(axis), half_at(axis, 1, 1), peer(axis, -1), **leaving(axis))

    def near(axis, o):
        landed = target(axis).at[tokens(axis, -o, core)]
        if o == PAIR:
            links.arrive(("swap", axis, PAIR), half_at(axis, PAIR, 0))
            links.arrive(("relayed", axis), half_at(axis, PAIR, 1))
        else:
            links.arrive(("swap", axis, o), landed)
        links.send(("near", axis), landed, landed, twin, **leaving(axis))

    def joined(axis):
        if axis not in done:
            done.add(axis)
            loaded(("own", axis))
            links.arrive(("near", axis), target(axis).at[pl.ds(0, SIDE * seq)])

    def joined_lanes(ref, l, i):
        return jnp.concatenate([ref[l, i, k].reshape(-1, ref.shape[-1]) for k in range(ROW)], axis=1)

    def make(l, c):
        kind, first, then, last, at, width = PARTS[c]
        if kind == "i":
            i = "yz".index(last)
            loaded(("h", l, last))
            if l:
                loaded(("z", l, last))
            else:
                joined(last)
            size = total[c].shape[TRIO]
            for lo in range(0, width, WIDE):
                hi = min(width, lo + WIDE)
                part = product(joined_lanes(hbuf, l, i), zbuf[l, i, :, at + lo:at + hi])
                for r in range(16):
                    total[c][l, r // SIDE, r % SIDE, :, lo:hi] = part[r * size:(r + 1) * size]
            return
        loaded(("m", l), ("s", l))
        if l:
            loaded(("y", l))
        else:
            joined("x")
        part = product(jnp.concatenate([mbuf[l, k] for k in range(ROW)], axis=1), ybuf[l, :, at:at + width])
        size = total[c].shape[TRIO]

        def put(r, value):
            total[c][(l, r // SIDE, r % SIDE) if first == "y" else (l, r % SIDE, r // SIDE)] = value

        for r in range(part.shape[0] // size):
            put(r, part[r * size:(r + 1) * size])
        gain = jnp.sum(jnp.sum(scbuf[l, :, :, at:at + width], axis=0), axis=0, keepdims=True)
        row = lax.broadcasted_iota(jnp.int32, (size, width), 0)
        put(15, jnp.where(row == 0, gain, ZERO))

    def area(l, c, o, whole):
        kind, first, then, last, at, width = PARTS[c]
        inner = (spot(then, whole) if isinstance(whole, int) else whole)
        outer = spot(last, o)
        if kind == "i":
            cols = lanes(((0 if last == "y" else SIDE) + outer) * own + at, width)
            return oa.at[l, inner, :, cols]
        cols = pl.ds(at, width)
        return ob.at[l, outer, inner, :, cols] if last == "y" else ob.at[l, inner, outer, :, cols]

    def add(l, c, s):
        kind, first, then, last, at, width = PARTS[c]
        t = total[c].at[l]
        sums = dict(batch=(l, c, 0), whole=t)
        lines = dict(batch=(l, c, 1), whole=t.at[pl.ds(0, PAIR)])
        singles = dict(batch=(l, c, PAIR), whole=t.at[pl.ds(0, PAIR), pl.ds(0, TRIO)])
        if s == 0:
            far = t.at[spot(first, PAIR)]
            for k, by in enumerate(BOTH):
                links.send((l, c, "half"), far.at[pl.ds(PAIR * k, PAIR)], half[c].at[l, k], peer(first, by), **sums)
        elif s == 1:
            links.arrive((l, c, "half"), half[c].at[l])
            for k, by in enumerate(BOTH):
                mine = t.at[spot(first, by)]
                add_into(mine.at[pl.ds(PAIR * k, PAIR)], half[c].at[l, k])
                links.send((l, c, "full"), mine, full[c].at[l, k], peer(first, by), **sums)
        elif s == PAIR:
            mine = t.at[spot(first, 0)]
            links.arrive((l, c, "full"), full[c].at[l])
            for k in range(PAIR):
                add_into(mine, full[c].at[l, k])
            for k, o in enumerate(AROUND):
                links.send((l, c, "small"), mine.at[spot(then, o)], small[c].at[l, k], peer(then, o), **singles)
        elif s == TRIO:
            links.arrive((l, c, "small"), small[c].at[l])
            mine = t.at[spot(first, 0), spot(then, 0)]
            front[c][l] = (mine[ALL] + small[c][l, 0]) + (small[c][l, 1] + small[c][l, PAIR])
        elif s == SIDE:
            src, dst = front[c].at[l], area(l, c, 0, 0)
            for o in AROUND:
                links.send((l, c, "a1"), src, dst, peer(then, o), **singles)
            copy = pltpu.make_async_copy(src, dst, osem.at[l, c])
            copy.start()
            loads["front", l, c] = copy
        elif s == 5:
            loaded(("front", l, c))
            links.arrive((l, c, "a1"), t.at[0, pl.ds(0, TRIO)])
            line = area(l, c, 0, slice(None))
            for by in BOTH:
                links.send((l, c, "a2"), line, line, peer(last, by), **lines)
        elif s == 6:
            links.arrive((l, c, "a2"), t.at[pl.ds(0, PAIR)])
            for k, by in enumerate(BOTH):
                part = area(l, c, -by, pl.ds(PAIR * k, PAIR))
                links.send((l, c, "a3"), part, part, peer(last, by), **sums)
        else:
            links.arrive((l, c, "a3"), area(l, c, PAIR, slice(None)))

    stages = {"swap": swap, "relay": relay, "near": near, "fetch": fetch, "make": make, "sum": add}
    for kind, *task in order:
        stages[kind](*task)
    links.drain()


def add_into(dst, src):
    @pl.loop(0, dst.shape[0])
    def _(i):
        if len(dst.shape) == SIDE:
            for j in range(dst.shape[1]):
                dst[i, j] += src[i, j]
        else:
            dst[i] += src[i]


def around(position):
    place, core = dict(zip("xyz", position)), position[TRIO]
    spots = {(axis, o): step(place[axis], o) for axis in "xyz" for o in range(SIDE)}
    peers = {}
    for axis in "xyz":
        for o in range(1, SIDE):
            moved = {**place, axis: spots[axis, o]}
            peers[axis, o] = device_at(moved["x"], moved["y"], moved["z"], core)
    return spots, peers


def reduce_gradients(operands, starts=(ZERO, ZERO, 20.0, 3.0)):
    hbm = pl.BlockSpec(memory_space=pltpu.HBM)
    h_rows, m_rows, y_cols, z_cols, z_own, y_own, scale_parts = operands
    part, part_b = h_rows[0].shape[PAIR] // SIDE, (m_rows[0].shape[1] + BAND) // 16
    (line, dim), wide = y_cols.shape, z_own.shape[1]
    out = lambda *shape: jax.ShapeDtypeStruct(shape, F32)
    sem = pltpu.SemaphoreType.DMA

    def buffers(*lead):
        return [pltpu.VMEM((PAIR, *lead, part if e[0] == "i" else part_b, e[5]), F32) for e in PARTS]

    return pl.pallas_call(
        functools.partial(reduce_kernel, reduce_order(part, part_b, starts)),
        out_shape=(out(PAIR, SIDE, part, wide), out(PAIR, SIDE, SIDE, part_b, dim)),
        in_specs=[hbm] * 12,
        out_specs=[hbm] * PAIR,
        scratch_shapes=[
            *buffers(SIDE, SIDE), *buffers(PAIR, PAIR), *buffers(PAIR, SIDE), *buffers(TRIO), *buffers(),
            pltpu.VMEM((PAIR, PAIR, *h_rows[0].shape), BF), pltpu.VMEM((PAIR, PAIR, line, wide // ROW), BF), pltpu.VMEM((PAIR, *m_rows[0].shape), BF),
            pltpu.VMEM((PAIR, line, dim), BF), pltpu.VMEM(scale_parts.shape, F32),
            pltpu.VMEM((PAIR, z_own.shape[0] // PAIR, wide // ROW), BF), pltpu.VMEM((y_own.shape[0] // PAIR, dim), BF),
            sem((39,)), sem((90,)), sem((14,)), sem((PAIR, len(PARTS))),
        ],
        compiler_params=pltpu.CompilerParams(collective_id=1, has_side_effects=True, vmem_limit_bytes=67043328),
        name="reduce_gradients",
    )(*h_rows, *m_rows, y_cols, *z_cols, z_own, y_own, scale_parts)


def finish_kernel(count, in_ref, out_ref, y_ref, gx_ref, in_grad, out_grad, y_out, gx_out, scale_out, in_buf, out_buf, y_buf, gx_buf, came, left):
    moves = [(out_ref.at[l, p], out_buf.at[l, pl.ds(SIDE * p, SIDE)]) for l in range(PAIR) for p in range(SIDE)]
    moves += [(y_ref, y_buf), (gx_ref, gx_buf)]
    size, width = in_buf.shape[PAIR:]
    moves += [(in_ref.at[l, p, :, pl.ds(0, width)], in_buf.at[l, p]) for l in range(PAIR) for p in range(SIDE)]
    loads = [pltpu.make_async_copy(src, dst, came.at[k]) for k, (src, dst) in enumerate(moves)]
    for copy in loads:
        copy.start()
    stores = []

    def store(src, dst):
        copy = pltpu.make_async_copy(src, dst, left.at[len(stores)])
        copy.start()
        stores.append(copy)

    for l in range(PAIR):
        for p in range(SIDE):
            loads[SIDE * l + p].wait()
        store(out_buf.at[l, pl.ds(0, 15)], out_grad.at[l])
    for k, (src, dst) in enumerate(((y_buf, y_out), (gx_buf, gx_out))):
        loads[ROW + k].wait()
        store(src, dst)
    me = lax.axis_index("fsdp")
    for l in range(PAIR):
        for f in range(ROW):
            @pl.when(me == f)
            def _():
                scale_out[l:l + 1] = out_buf[l, 15, 0:1, f * count:(f + 1) * count]
    for l in range(PAIR):
        for p in range(SIDE):
            loads[10 + SIDE * l + p].wait()
            store(in_buf.at[l, p], in_grad.at[l, pl.ds(p * size, size)])
    for copy in stores:
        copy.wait()


def finish(in_sums, out_sums, y, gx, rows, proj):
    hbm = pl.BlockSpec(memory_space=pltpu.HBM)
    out = lambda *shape, dtype=F32: jax.ShapeDtypeStruct(shape, dtype)
    size, (depth, dim) = in_sums.shape[PAIR], out_sums.shape[TRIO:]
    in_grad, out_grad, y_out, gx_out, scale = pl.pallas_call(
        functools.partial(finish_kernel, rows),
        out_shape=(out(PAIR, rows, proj), out(PAIR, 15, depth, dim), out(*y.shape, dtype=BF), out(*gx.shape, dtype=BF), out(PAIR, rows)),
        in_specs=[hbm] * SIDE,
        out_specs=[hbm] * SIDE + [pl.BlockSpec(memory_space=pltpu.VMEM)],
        scratch_shapes=[
            pltpu.VMEM((PAIR, SIDE, size, proj), F32), pltpu.VMEM((PAIR, 16, depth, dim), F32), pltpu.VMEM(y.shape, BF), pltpu.VMEM(gx.shape, BF),
            pltpu.SemaphoreType.DMA((18,)), pltpu.SemaphoreType.DMA((12,)),
        ],
        compiler_params=pltpu.CompilerParams(vmem_limit_bytes=67043328),
        name="finish",
    )(in_sums, out_sums, y, gx)
    return y_out[None], gx_out[None], scale, in_grad, out_grad.reshape(PAIR, 15 * depth, dim)


def solution(mesh):
    fsdp_size = mesh.shape["fsdp"]
    batch_spec = P(("dp", "fsdp"), None, None)
    scale_spec = P(None, "fsdp")
    weight_spec = P(None, "fsdp", None)

    def device_step(x_in, grad_y, norm_scale, w_in, w_out):
        n_layers = w_in.shape[0]
        seq_len, model_dim = x_in.shape[1:]
        proj_dim = w_in.shape[PAIR]
        ff_dim = w_out.shape[1] * fsdp_size - model_dim
        head_dim = (proj_dim - model_dim - PAIR * ff_dim) // PAIR
        rows, rows_out = norm_scale.shape[1], w_out.shape[1]
        half_dim = head_dim // PAIR
        freq = 10000.0 ** (-np.arange(half_dim, dtype=np.float32) * 2.0 / head_dim)
        freq = jnp.asarray(np.tile(freq.astype(np.float32), (ROW, LANE // half_dim)))
        hidden, grad_hidden, *rest = run_layers(x_in[0], grad_y[0], norm_scale, w_in, w_out, freq)
        in_sums, out_sums = reduce_gradients((rest[0:SIDE], rest[SIDE:6], rest[6], rest[OTHERS:9], rest[9], rest[10], rest[11]))
        return finish(in_sums, out_sums, hidden, grad_hidden, rows, proj_dim)

    return jax.shard_map(
        device_step,
        mesh=mesh,
        in_specs=(batch_spec, batch_spec, scale_spec, weight_spec, weight_spec),
        out_specs=(batch_spec, batch_spec, scale_spec, weight_spec, weight_spec),
        check_vma=False,
    )
```

```python
import functools
import jax
import jax.numpy as jnp
import numpy as np
from jax import lax
from jax.experimental import pallas as pl
from jax.experimental.pallas import tpu as pltpu
from jax.sharding import PartitionSpec as P

MESH_ID = pl.DeviceIdType.MESH
BOTH = (1, -1)
AROUND = (1, -1, 2)
PARTS = (True, False)
ALL, ZERO = ..., 0.0
OTHERS = 7
QUICK, SHORT = 0.2, 0.3
LANE, WIDE, STRIP, HEAD = 128, 256, 512, 64
ROW, BAND, SIDE, TRIO, PAIR = 8, 32, 4, 3, 2


class Links:
    def __init__(self, send_sems, recv_sems):
        self.send_sems, self.recv_sems = send_sems, recv_sems
        self.slots, self.batches, self.sent, self.count = {}, {}, {}, 0

    def _landing(self, key, lane):
        if key not in self.slots:
            self.slots[key] = self.count
            self.count += 1 if lane is None else PAIR
        return self.recv_sems.at[self.slots[key] + (0 if lane is None else lane)]

    def send(self, key, src, dst, device, landing=None, whole=None, batch=None, lane=None):
        leaving = self.batches.setdefault(batch or key, len(self.batches))
        copy = pltpu.make_async_remote_copy(
            src_ref=src, dst_ref=dst, send_sem=self.send_sems.at[leaving], recv_sem=self._landing(landing or key, lane),
            device_id=device, device_id_type=MESH_ID)
        copy.start()
        self.sent[batch or key] = (src if whole is None else whole, leaving)

    def arrive(self, key, landed, lane=None):
        pltpu.make_async_copy(landed, landed, self._landing(key, lane)).wait()

    def drain(self):
        for left, leaving in self.sent.values():
            pltpu.make_async_copy(left, left, self.send_sems.at[leaving]).wait()
        self.sent.clear()


def rem(a, n):
    return a % n if isinstance(a, int) else lax.rem(a, n)


def chip_position():
    f, d = lax.axis_index("fsdp"), lax.axis_index("dp")
    return f // PAIR, rem(d, SIDE), d // SIDE, rem(f, PAIR)


def device_at(x, y, z, core):
    return (z * SIDE + y, x * PAIR + core)


def step(coord, by):
    return rem(coord + SIDE + by, SIDE)


def announce(devices):
    barrier = pltpu.get_barrier_semaphore()
    for device in devices:
        pl.semaphore_signal(barrier, inc=1, device_id=device, device_id_type=MESH_ID)
    pl.semaphore_wait(barrier, len(devices))


def plan(tasks, latency=2.5):
    free, landed, order, now = {}, {}, [], ZERO
    left = list(tasks)
    while left:
        best = None
        for place, (name, rank, start, needs, after, _, _) in enumerate(left):
            if all(n[0] in landed for n in needs) and all(n in landed for n in after):
                ready = max([start, now] + [landed[task][i] for task, i in needs])
                best = min(best or (ready, rank, place), (ready, rank, place))
        now, _, place = best
        name, _, _, _, _, sends, cost = left.pop(place)
        order.append(name)
        now += cost
        landed[name] = []
        for link, time, *more in sends:
            free[link] = max(now, free.get(link, ZERO)) + time
            landed[name].append(free[link] + latency + sum(more))
    return order


def layers_order(rows_i, cols_i, rows_o, cols_o, seq, starts):
    rate = 23300.0
    tasks = []
    for m in range(SIDE):
        is_in = m % PAIR == 0
        edge = cols_i // LANE * SIDE // 9 // PAIR * WIDE
        size = {"y": rows_i // SIDE * edge, "x": rows_i * (cols_i - PAIR * edge)} if is_in else {"y": rows_o // SIDE * cols_o // PAIR}
        size["z"] = size["y"]
        colors = "yzx" if is_in else "yz"
        tasks.append((("lend", m), 5, 3.0 + SIDE * m, [], [], [("chip", (rows_i * cols_i if is_in else rows_o * cols_o) / 150000.0)], QUICK))
        for color in colors:
            cost = size[color] / rate
            both = [(("x", by), cost) for by in BOTH]
            spread = [((color, by), cost) for by in BOTH] if color != "x" else []
            tasks.append((("reach", m, color), m, starts[m], [], [], both, QUICK))
            for i, by in enumerate(BOTH):
                tasks.append((("relay", m, color, by), m, ZERO, [(("reach", m, color), i)], [], [(("x", by), cost / PAIR)] + spread, QUICK))
            halves = [(("relay", m, color, by), 0) for by in BOTH]
            tasks.append((("far", m, color), m, ZERO, halves, [], spread, QUICK))
            if color == "x":
                continue
            for off, source, first in ((-1, ("relay", m, color, 1), 1), (1, ("relay", m, color, -1), 1), (PAIR, ("far", m, color), 0)):
                for i, by in enumerate(BOTH):
                    tasks.append((("pass", m, color, off, by), m, ZERO, [(source, first + i)], [], [((color, by), cost / PAIR)], QUICK))
                halves = [(("pass", m, color, off, by), 0) for by in BOTH]
                tasks.append((("close", m, color, off), m, ZERO, halves, [], [], QUICK))
        for off in (-1, 1, PAIR):
            last = [("close", m, color, off) for color in "yz"]
            if is_in:
                last.append(("far", m, "x") if off == PAIR else ("relay", m, "x", -off))
            tasks.append((("hand", m, off), m, ZERO, [], last, [("chip", (rows_i * cols_i if is_in else rows_o * cols_o) / 150000.0)], QUICK))
    before = []

    def work(name, cost, mats=()):
        needs = [(("hand", m, off), 0) for m in mats for off in (-1, 1, PAIR)] + [(("lend", m), 0) for m in mats]
        tasks.append((name, 99, ZERO, needs, list(before), [], cost))
        before[:] = [name]

    for l in range(PAIR):
        work(("norm", l), 0.8)
        work(("project", l), 4.0, [PAIR * l])
        work(("attend", l), 4.2)
        work(("mlp", l), 2.2)
        work(("put", l), 1.6, [PAIR * l + 1])
    for l in (1, 0):
        work(("back_out", l), 2.9)
        work(("back_mlp", l), 2.0)
        work(("back_heads", l), 1.0)
        work(("back_quad", l), 6.0)
        work(("back_keys", l), QUICK)
        for i in range(PAIR):
            work(("back_in", l, i), 1.3 + 0.6 * i)
        work(("back_norm", l), 1.0)
    def send(name, rank, start, after, sends):
        tasks.append((name, rank, start, [], [after] if after else [], sends, 0.4))

    def follow(name, rank, needs, sends):
        tasks.append((name, rank, ZERO, needs, [], sends, QUICK))

    def both(axis, size):
        return [((axis, by), size / rate, margin) for by in BOTH]

    model, margin = rows_i * ROW, 2.0
    for l in (1, 0):
        for axis in "yz":
            name = ("send_h", l, axis)
            send(name, 20 - l, 58.0, ("norm", l), both(axis, seq * model))
            for i, by in enumerate(BOTH):
                for index in range(PAIR):
                    follow(("pass_h", l, axis, by, index), 10, [(name, i)], [((axis, by), seq * model / SIDE / rate, margin)])
        name = ("send_m", l)
        send(name, 22 - l, ZERO, ("mlp", l), both("x", seq * rows_o) + both("x", PAIR * seq * rows_o))
        for i, by in enumerate(BOTH):
            for index in range(PAIR):
                follow(("pass_m", l, by, index), 11, [(name, i)], [(("x", by), seq * rows_o / PAIR / rate, margin)])
        if l == 0:
            send(("own_y",), 15, ZERO, ("back_norm", 1), [])
            send(("send_scale", l), 15, ZERO, ("back_norm", l), [])
            continue
        name = ("send_y", l)
        send(name, 12, 42.0, None, both("x", seq * model))
        for i, by in enumerate(BOTH):
            follow(("pass_y", l, by), 12, [(name, i)], [(("x", by), seq * model / PAIR / rate, margin)])
        follow(("far_y", l), 12, [(("pass_y", l, by), 0) for by in BOTH], [])
        for axis in "zy":
            name = ("send_z", l, axis)
            share = seq * (cols_i + LANE) / ROW
            send(name, 13, ZERO, ("back_mlp", l), both(axis, share / PAIR) + both(axis, share))
            if axis == "y":
                name = ("rest_z", l)
                send(name, 13, ZERO, ("back_keys", l), both(axis, share / ROW) + both(axis, share / SIDE))
            for i, by in enumerate(BOTH):
                follow(("pass_z", l, axis, by), 13, [(name, i)], [((axis, by), share / PAIR / rate, margin)])
                follow(("twin_z", l, axis, by), 14, [(name, PAIR + i)], [])
            follow(("far_z", l, axis), 14, [(("pass_z", l, axis, by), 0) for by in BOTH], [])
        send(("send_scale", l), 15, ZERO, ("back_norm", l), [])
    send(("own_z",), 15, ZERO, ("back_keys", 0), [])
    return plan(tasks)


def gather_stages(links, position, shard_i, shard_o, wi, wo, lsem):
    x, y, z, core = position
    twin = device_at(x, y, z, 1 - core)
    rows_i, cols_i = shard_i.shape[1:]
    rows_o, cols_o = shard_o.shape[1:]
    quarter_i, quarter_o = rows_i // SIDE, rows_o // SIDE
    third_i = cols_i // LANE * SIDE // 9 // PAIR * WIDE
    half_o = cols_o // PAIR
    cut_o = quarter_o // 16 * ROW + ROW if quarter_o % 16 else quarter_o // PAIR
    place = {"x": x, "y": y, "z": z}

    spots = {(axis, o): step(place[axis], o) for axis in "xyz" for o in range(SIDE)}

    def spot(axis, o):
        return spots[axis, o % SIDE]

    table = {}
    for axis in "xyz":
        for o in range(1, SIDE):
            moved = {**place, axis: spot(axis, o)}
            table[axis, o] = device_at(moved["x"], moved["y"], moved["z"], core)

    def peer(axis, o):
        return table[axis, o % SIDE]

    mats = []
    for l in range(PAIR):
        mats.append((shard_i.at[l], wi.at[l], rows_i, True))
        mats.append((shard_o.at[l], wo.at[l], rows_o, False))

    def region(is_in, color, q):
        if is_in:
            if color == "x":
                lo, hi = PAIR * third_i, cols_i
                rows = (0, rows_i)
            else:
                lo, hi = (0, third_i) if color == "y" else (third_i, PAIR * third_i)
                rows = (q * quarter_i, quarter_i)
            mid = lo + ((hi - lo) // LANE + 1) // PAIR * LANE
            return (rows, (lo, hi - lo)), (rows, (lo, mid - lo)), (rows, (mid, hi - mid))
        cols = (0, half_o) if color == "y" else (half_o, half_o)
        start = q * quarter_o
        return ((start, quarter_o), cols), ((start, cut_o), cols), ((start + cut_o, quarter_o - cut_o), cols)

    def at(m, xb, area):
        (r, nr), (c, nc) = area
        _, out, size, _ = mats[m]
        return out.at[pl.ds(pl.multiple_of((PAIR * xb + core) * size + r, ROW), nr), pl.ds(c, nc)]

    def block(m, xb, index):
        _, out, size, _ = mats[m]
        return out.at[pl.ds(pl.multiple_of((PAIR * xb + index) * size, BAND), size)]

    def group(m, color):
        _, out, _, is_in = mats[m]
        (_, nr), (c, nc) = region(is_in, color, 0)[0]
        return dict(batch=(m, color), whole=out.at[pl.ds(0, nr * (TRIO if color == "x" else 12)), pl.ds(c, nc)])

    def reach(m, color):
        src, _, _, is_in = mats[m]
        area = region(is_in, color, place[color])[0]
        for by in BOTH:
            links.send((m, "x1", color, by), src.at[pl.ds(pl.multiple_of(area[0][0], ROW), area[0][1]), pl.ds(*area[1])], at(m, x, area), peer("x", by), **group(m, color))

    def launch(m, color, off):
        is_in = mats[m][TRIO]
        moved = at(m, spot("x", off), region(is_in, color, place[color])[0])
        for by in BOTH:
            links.send((m, "p1", color, off, by), moved, moved, peer(color, by), **group(m, color))

    def relay(m, color, by):
        is_in = mats[m][TRIO]
        xb = spot("x", -by)
        areas = region(is_in, color, place[color])
        links.arrive((m, "x1", color, by), at(m, xb, areas[0]))
        part = at(m, xb, areas[1] if by == 1 else areas[PAIR])
        links.send((m, "x2", color), part, part, peer("x", by), **group(m, color))
        if color != "x":
            launch(m, color, -by)

    def far(m, color):
        is_in = mats[m][TRIO]
        links.arrive((m, "x2", color), at(m, spot("x", PAIR), region(is_in, color, place[color])[0]))
        if color != "x":
            launch(m, color, PAIR)

    def pass_on(m, color, off, by):
        is_in = mats[m][TRIO]
        xb = spot("x", off)
        areas = region(is_in, color, spot(color, -by))
        links.arrive((m, "p1", color, off, by), at(m, xb, areas[0]))
        part = at(m, xb, areas[1] if by == 1 else areas[PAIR])
        links.send((m, "p2", color, off), part, part, peer(color, by), **group(m, color))

    def close(m, color, off):
        is_in = mats[m][TRIO]
        links.arrive((m, "p2", color, off), at(m, spot("x", off), region(is_in, color, spot(color, PAIR))[0]))

    def four(m):
        _, out, size, _ = mats[m]
        return out.at[pl.ds(0, SIDE * size)]

    def give(m, src, dst):
        links.send((m, "chip"), src, dst, twin, batch=(m, "chip"), whole=four(m))

    def hand(m, off):
        whole = block(m, spot("x", off), core)
        give(m, whole, whole)

    owns = []

    def begin():
        for m, (src, _, _, _) in enumerate(mats):
            copy = pltpu.make_async_copy(src, block(m, x, core), lsem.at[m])
            copy.start()
            owns.append(copy)

    def lend(m):
        give(m, mats[m][0], block(m, x, core))

    def ready(m):
        owns[m].wait()
        links.arrive((m, "chip"), four(m))

    return begin, ready, peer, {"reach": reach, "relay": relay, "far": far, "pass": pass_on, "close": close, "hand": hand, "lend": lend}


BF, F32 = jnp.bfloat16, jnp.float32


def product(a, b, contract=((1,), (0,))):
    return lax.dot_general(a, b, (contract, ((), ())), preferred_element_type=F32)


def lanes(start, size):
    return pl.ds(start if isinstance(start, int) else pl.multiple_of(start, LANE), size)


def layers_kernel(order, sc_ref, wi_ref, wo_ref, x_ref, dy_ref, freq_ref,
                  y_ref, gx_ref, hy_a, hy_b, hz_a, hz_b, mx_a, mx_b, yx_b, zy_b, zz_b, z_a, dy_a, sc_out, relay_m, relay_z,
                  wi, wo, z, om, h, hid, qr, kts, vsl, ksl, turned_q, turned_o, scores, dscores, pcat, dscat, cos_ref, sin_ref, turn_ref,
                  dot_heads, qt, dht, dkv, omt, ht, dyt, sc, gains, own_gain, gain_ref, load_sems, own_sems, send_sems, recv_sems,
                  share_send_sems, share_recv_sems):
    seq, dim = x_ref.shape
    ff = (wi.shape[PAIR] - dim - LANE) // PAIR
    position = chip_position()
    x, y, zc, core = position
    twin = device_at(x, y, zc, 1 - core)
    me = PAIR * x + core
    links, shared = Links(send_sems, recv_sems), Links(share_send_sems, share_recv_sems)
    stored = []
    spots, _ = around(position)
    h_out, m_out, y_out, z_out = {"y": (hy_a, hy_b), "z": (hz_a, hz_b)}, (mx_a, mx_b), {1: yx_b}, {(1, "y"): zy_b, (1, "z"): zz_b}
    middle = hid.at[1]
    begin, ready, peer, stages = gather_stages(links, position, wi_ref, wo_ref, wi, wo, load_sems)
    others = [(zc * SIDE + y, rem(me + k, ROW)) for k in range(1, ROW)]

    def spot(axis, o):
        return spots[axis, o % SIDE]

    def device(axis, o, index):
        moved = {"x": x, "y": y, "z": zc, axis: spot(axis, o)}
        return device_at(moved["x"], moved["y"], moved["z"], index)

    own_gain[ALL] = jnp.zeros(own_gain.shape, F32)
    count = sc_ref.shape[1]
    for f in range(ROW):
        @pl.when(me == f)
        def _():
            own_gain[0:PAIR, f * count:(f + 1) * count] = sc_ref[ALL].astype(F32)
    announce(others + [device(axis, o, index) for axis in "yz" for o in AROUND for index in range(PAIR)])
    begin()
    for k, far in enumerate(others):
        links.send(("sc",), own_gain, gains.at[me], far, batch=("sc",), whole=gains.at[pl.ds(0, OTHERS)])

    def keep(src, dst):
        copy = pltpu.make_async_copy(src, dst, own_sems.at[len(stored)])
        copy.start()
        stored.append(copy)

    def tokens(axis, o, index):
        return pl.ds(pl.multiple_of((PAIR * spot(axis, o) + index) * seq, seq), seq)

    def place(axis, o, index):
        return PAIR * spot(axis, o) + index

    def columns(axis, o):
        size = z.shape[PAIR] // ROW
        return lanes(((0 if axis == "y" else SIDE) + spot(axis, o)) * size, size)

    def several(batch, ref, n):
        whole = ref.at[pl.ds(0, n * seq if batch[0][0] in "yz" else n)]
        return dict(batch=batch, whole=whole)

    def send_h(l, axis):
        out = h_out[axis][l].at[place(axis, 0, core)]
        for by in BOTH:
            for index in range(PAIR):
                shared.send(("h", l, axis, by), ht.at[l, :, index], out, device(axis, by, index), lane=core, **several(("h", l, axis), h_out[axis][l], OTHERS))
        shared.send(("h", l, axis), ht.at[l, :, 1 - core], out, twin, **several(("h", l, axis), h_out[axis][l], OTHERS))
        keep(ht.at[l, :, core], out)

    def pass_h(l, axis, by, index):
        out = h_out[axis][l]
        shared.arrive(("h", l, axis, by), out.at[place(axis, -by, index)], index)
        part = out.at[place(axis, -by, index), pl.ds(1 - by, PAIR)]
        shared.send(("h", l, axis), part, part, device(axis, by, core), **several(("h", l, axis), out, OTHERS))

    def arrive_h(l):
        for axis in "yz":
            shared.arrive(("h", l, axis), h_out[axis][l].at[pl.ds(0, TRIO)])

    def row_block(l, o, index, part=None):
        size = omt.shape[1] // ROW
        start = (PAIR * spot("x", o) + index) * size
        if part is not None:
            size = size // PAIR
            start = start + part * size
        return omt.at[l, pl.ds(pl.multiple_of(start, 16), size)]

    def row_half(k):
        size = m_out[0].shape[1] // PAIR
        return pl.ds(k * size, size)

    def send_m(l):
        out = m_out[l].at[place("x", 0, core)]
        for k, by in enumerate(BOTH):
            for index in range(PAIR):
                shared.send(("mr", l, by), row_block(l, PAIR, index, k), relay_m.at[l, k, core], device("x", by, index), lane=core, **several(("m", l), m_out[l], OTHERS))
        for by in BOTH:
            for index in range(PAIR):
                shared.send(("m", l), row_block(l, by, index), out, device("x", by, index), **several(("m", l), m_out[l], OTHERS))
        shared.send(("m", l), row_block(l, 0, 1 - core), out, twin, **several(("m", l), m_out[l], OTHERS))
        keep(row_block(l, 0, core), out)

    def pass_m(l, by, index):
        k = (1 - by) // PAIR
        shared.arrive(("mr", l, by), relay_m.at[l, k, index], index)
        shared.send(("m", l), relay_m.at[l, k, index], m_out[l].at[place("x", -by, index), row_half(k)], device("x", by, core),
                    **several(("m2", l), m_out[l], PAIR))

    def arrive_m(l):
        shared.arrive(("m", l), m_out[l].at[pl.ds(0, OTHERS)])

    def token_half(axis, o, k):
        return pl.ds(pl.multiple_of((PAIR * spot(axis, o) + core) * seq + k * (seq // PAIR), seq // PAIR), seq // PAIR)

    def send_y(l):
        src, out = dy_ref, y_out[l].at[tokens("x", 0, core)]
        for by in BOTH:
            shared.send(("y", l, by), src, out, device("x", by, core), **several(("y", l), y_out[l], OTHERS))
        shared.send(("y", l), src, out, twin, **several(("y", l), y_out[l], OTHERS))
        keep(src, out)

    def pass_y(l, by):
        landed, part = y_out[l].at[tokens("x", -by, core)], y_out[l].at[token_half("x", -by, (1 - by) // PAIR)]
        shared.arrive(("y", l, by), landed)
        shared.send(("y2", l), part, part, device("x", by, core), **several(("y", l), y_out[l], OTHERS))
        shared.send(("y", l), landed, landed, twin, **several(("y", l), y_out[l], OTHERS))

    def far_y(l):
        landed = y_out[l].at[tokens("x", PAIR, core)]
        shared.arrive(("y2", l), landed)
        shared.send(("y", l), landed, landed, twin, **several(("y", l), y_out[l], OTHERS))

    def arrive_y(l):
        shared.arrive(("y", l), y_out[l].at[pl.ds(0, SIDE * seq)])

    def push_z(l, axis, o, ready):
        out = z_out[l, axis].at[tokens(axis, 0, core)]
        batch = several(("z", l, axis), z_out[l, axis], ROW)

        def start():
            if o != PAIR:
                shared.send(("z", l, axis, o), z.at[l, :, columns(axis, o)], out, device(axis, o, core), **batch)
                return
            for k, by in enumerate(BOTH):
                shared.send(("zr", l, axis, by), z.at[l, pl.ds(k * (seq // PAIR), seq // PAIR), columns(axis, PAIR)], relay_z.at[l, "yz".index(axis), k],
                            device(axis, by, core), **batch)

        if ready is None:
            start()
        else:
            pl.when(ready)(start)

    def own_part(l, axis):
        out, mine = z_out[l, axis].at[tokens(axis, 0, core)], z.at[l, :, columns(axis, 0)]
        shared.send(("z", l, axis), mine, out, twin, **several(("z", l, axis), z_out[l, axis], ROW))
        keep(mine, out)

    def send_z(l, axis):
        for o in (PAIR, 1, -1):
            push_z(l, axis, o, spot(axis, o) != 0 if axis == "y" else None)
        if axis == "z":
            own_part(l, axis)

    def rest_z(l):
        for o in (PAIR, 1, -1):
            push_z(l, "y", o, spot("y", o) == 0)
        own_part(l, "y")

    def pass_z(l, axis, by):
        k = (1 - by) // PAIR
        half = relay_z.at[l, "yz".index(axis), k]
        shared.arrive(("zr", l, axis, by), half)
        shared.send(("z2", l, axis), half, z_out[l, axis].at[token_half(axis, -by, k)], device(axis, by, core), **several(("z", l, axis), z_out[l, axis], ROW))

    def twin_z(l, axis, by):
        landed = z_out[l, axis].at[tokens(axis, -by, core)]
        shared.arrive(("z", l, axis, by), landed)
        shared.send(("z", l, axis), landed, landed, twin, **several(("z", l, axis), z_out[l, axis], ROW))

    def far_z(l, axis):
        landed = z_out[l, axis].at[tokens(axis, PAIR, core)]
        shared.arrive(("z2", l, axis), landed)
        shared.send(("z", l, axis), landed, landed, twin, **several(("z", l, axis), z_out[l, axis], ROW))

    def arrive_z(l, axis):
        shared.arrive(("z", l, axis), z_out[l, axis].at[pl.ds(0, SIDE * seq)])

    def send_scale(l):
        for far in others:
            shared.send(("scale", l), sc.at[l], sc_out.at[l, me], far, batch=("scale", l), whole=sc_out.at[l, pl.ds(0, OTHERS)])
        keep(sc.at[l], sc_out.at[l, me])

    def arrive_scale(l):
        shared.arrive(("scale", l), sc_out.at[l, pl.ds(0, OTHERS)])

    gains[me] = own_gain[ALL]
    z[:, :, wi.shape[PAIR]:] = jnp.zeros((PAIR, seq, z.shape[PAIR] - wi.shape[PAIR]), BF)
    entry = (x_ref, hid.at[0])
    angle = lax.broadcasted_iota(jnp.int32, (seq, LANE), 0).astype(F32) * freq_ref[0:1]
    for half in range(PAIR):
        cos_ref[:, LANE * half:LANE * (half + 1)] = jnp.cos(angle)
        sin_ref[:, LANE * half:LANE * (half + 1)] = jnp.sin(angle)
    lane = lax.broadcasted_iota(jnp.int32, turn_ref.shape, 1)
    down = lax.broadcasted_iota(jnp.int32, turn_ref.shape, 0) - lane
    low = rem(lane, HEAD) < BAND
    turn_ref[ALL] = jnp.where(low & (down == BAND), -1.0, jnp.where(jnp.logical_not(low) & (down == -BAND), 1.0, ZERO)).astype(BF)
    kts[ALL] = jnp.zeros(kts.shape, BF)
    pcat[ALL] = jnp.zeros(pcat.shape, BF)
    dscat[ALL] = jnp.zeros(dscat.shape, BF)

    def normalise(l, src):
        @pl.loop(0, seq // BAND, unroll=SIDE)
        def _(r):
            rows = pl.ds(pl.multiple_of(r * BAND, BAND), BAND)
            v = src[rows].astype(F32)
            v = v - jnp.mean(v, axis=-1, keepdims=True)
            var = jnp.mean(v * v, axis=-1, keepdims=True)
            h[l, rows] = (v * lax.rsqrt(var + 1e-6) * gain_ref[l:l + 1]).astype(BF)

    def project(l):
        strip = wi.shape[PAIR] // 5

        @pl.loop(0, 5)
        def _(i):
            at = lanes(i * strip, strip)
            z[l, :, at] = product(h[l], wi[l, :, at]).astype(BF)

    def heads(l):
        cos, sin = cos_ref[ALL], sin_ref[ALL]
        for g in range(dim // WIDE):
            q = z[l, :, g * WIDE:(g + 1) * WIDE]
            qr[l, :, g * WIDE:(g + 1) * WIDE] = ((q.astype(F32) * cos + product(q, turn_ref[ALL]) * sin) * 0.125).astype(BF)
        kv = z[l, :, dim:dim + LANE]
        turned = kv.astype(F32) * cos[:, :LANE] + product(kv, turn_ref[:LANE, :LANE]) * sin[:, :LANE]
        first = lax.broadcasted_iota(jnp.int32, turned.shape, 1) < HEAD
        key_lo = jnp.where(first, turned, ZERO)
        val_hi = jnp.where(first, ZERO, kv.astype(F32))
        return key_lo, pltpu.roll(key_lo, HEAD, 1), pltpu.roll(val_hi, HEAD, 1), val_hi

    def slot_rows(ref, lo, hi):
        zero = jnp.zeros((seq, LANE), BF)
        lo, hi = lo.astype(BF), hi.astype(BF)
        for i, (left, right) in enumerate(((lo, zero), (hi, zero), (zero, lo), (zero, hi))):
            ref[i * seq:(i + 1) * seq, :LANE] = left
            ref[i * seq:(i + 1) * seq, LANE:] = right

    def slot_cols(ref, lo):
        flat = lo.T[:HEAD].astype(BF)
        for i in range(SIDE):
            ref[HEAD * i:HEAD * (i + 1), i * seq:(i + 1) * seq] = flat

    def chances(i, half):
        at = slice(LANE * half, LANE * (half + 1))
        blocks = [pl.ds(pl.multiple_of(i * seq + LANE * k, LANE), LANE) for k in range(half + 1)]
        s = [scores[keys, at] for keys in blocks]
        lower = lax.broadcasted_iota(jnp.int32, s[-1].shape, 1) >= lax.broadcasted_iota(jnp.int32, s[-1].shape, 0)
        s[-1] = jnp.where(lower, s[-1], -1e30)
        top = functools.reduce(jnp.maximum, [jnp.max(v, axis=0, keepdims=True) for v in s])
        e = [jnp.exp(v - top) for v in s]
        scale = 1.0 / sum(jnp.sum(v, axis=0, keepdims=True) for v in e)
        return at, [(keys, v * scale) for keys, v in zip(blocks, e)]

    def attend(l):
        key_lo, key_hi, val_lo, _ = heads(l)
        slot_rows(ksl, key_lo, key_hi)
        slot_cols(kts, val_lo)
        flip(lambda at: qr[l, :, lanes(at, WIDE)], qt, dim)

        @pl.loop(0, dim // WIDE)
        def _(g):
            rows = pl.ds(pl.multiple_of(g * WIDE, WIDE), WIDE)
            scores[ALL] = product(ksl[ALL], qt[rows])

            @pl.loop(0, SIDE)
            def _(i):
                for half in range(PAIR):
                    at, blocks = chances(i, half)
                    for keys, p in blocks:
                        pcat[keys, at] = p.astype(BF)
            flat = product(kts[ALL], pcat[ALL]).astype(BF)
            omt[l, rows] = flat
            om[:, lanes(g * WIDE, WIDE)] = flat.T

    def mlp(l):
        @pl.loop(0, seq // BAND)
        def _(r):
            rows = pl.ds(pl.multiple_of(r * BAND, BAND), BAND)

            @pl.loop(0, ff // STRIP)
            def _(i):
                gate = z[l, rows, lanes(dim + LANE + i * STRIP, STRIP)].astype(F32)
                up = z[l, rows, lanes(dim + LANE + ff + i * STRIP, STRIP)].astype(F32)
                om[rows, lanes(dim + i * STRIP, STRIP)] = (gate * jax.nn.sigmoid(gate) * up).astype(BF)

    def put_out(l, dst):
        for n in range(dim // WIDE):
            cols = slice(n * WIDE, (n + 1) * WIDE)
            total = product(om[ALL], wo[l, :, cols])
            dst[:, cols] = (entry[l][:, cols].astype(F32) + total).astype(BF)

    def flip(src, dst, width, first=0):
        @pl.loop(first // WIDE, width // WIDE)
        def _(i):
            dst[pl.ds(pl.multiple_of(i * WIDE, WIDE), WIDE)] = src(i * WIDE).T

    upstream = (middle, dy_ref)

    def back_out(l):
        dy = upstream[l]
        flip(lambda at: dy[:, lanes(at, WIDE)], dyt, dim)

        @pl.loop(0, wo.shape[1] // dim)
        def _(n):
            rows = pl.ds(pl.multiple_of(n * dim, dim), dim)
            part = product(wo[l, rows], dyt[ALL]).astype(BF)
            om[:, lanes(n * dim, dim)] = part.T

            @pl.when(n == 0)
            def _():
                dot_heads[ALL] = part

    def back_mlp(l):
        @pl.loop(0, seq // BAND)
        def _(r):
            rows = pl.ds(pl.multiple_of(r * BAND, BAND), BAND)

            @pl.loop(0, ff // STRIP)
            def _(i):
                gate_at, up_at = lanes(dim + LANE + i * STRIP, STRIP), lanes(dim + LANE + ff + i * STRIP, STRIP)
                gate, up = z[l, rows, gate_at].astype(F32), z[l, rows, up_at].astype(F32)
                d = om[rows, lanes(dim + i * STRIP, STRIP)].astype(F32)
                sig = jax.nn.sigmoid(gate)
                du = d * up
                z[l, rows, gate_at] = (du * sig + du * gate * (sig * (1.0 - sig))).astype(BF)
                z[l, rows, up_at] = (d * (gate * sig)).astype(BF)

    def back_heads(l):
        key_lo, key_hi, val_lo, val_hi = heads(l)
        slot_rows(ksl, key_lo, key_hi)
        slot_rows(vsl, val_lo, val_hi)
        slot_cols(kts, key_lo)
        dkv[ALL] = jnp.zeros(dkv.shape, F32)
        flip(lambda at: qr[l, :, lanes(at, WIDE)], qt, dim)
        for at in range(0, dim, LANE):
            pair = slice(at, at + LANE)
            turned_q[:, pair] = pltpu.roll(qr[l, :, pair].astype(F32), HEAD, 1).astype(BF)
            turned_o[:, pair] = pltpu.roll(om[:, pair].astype(F32), HEAD, 1).astype(BF)

    def back_quad(l):
        @pl.loop(0, dim // WIDE)
        def _(g):
            quad(l, g)

    def quad(l, g):
        cols = pl.ds(pl.multiple_of(g * WIDE, WIDE), WIDE)
        scores[ALL] = product(ksl[ALL], qt[cols])
        dscores[ALL] = product(vsl[ALL], dot_heads[cols])

        @pl.loop(0, SIDE)
        def _(i):
            for half in range(PAIR):
                at, blocks = chances(i, half)
                given = [p * dscores[keys, at].astype(BF).astype(F32) for keys, p in blocks]
                total = sum(jnp.sum(v, axis=0, keepdims=True) for v in given)
                for (keys, p), v in zip(blocks, given):
                    pcat[keys, at] = p.astype(BF)
                    dscat[keys, at] = (v - p * total).astype(BF)
        dq = product(kts[ALL], dscat[ALL]).astype(BF).T
        back = dq.astype(F32) * cos_ref[ALL] - product(dq, turn_ref[ALL]) * sin_ref[ALL]
        z[l, :, cols] = (back * 0.125).astype(BF)
        def pieces(left, even, odd):
            for i in range(SIDE):
                pair = lanes(g * WIDE + i // PAIR * LANE, LANE)
                yield product(left[i * seq:(i + 1) * seq, :], odd(pair) if i % PAIR else even(pair))

        dkv[0] += sum(pieces(dscat, lambda at: qr[l, :, at], lambda at: turned_q[:, at]))
        dkv[1] += sum(pieces(pcat, lambda at: turned_o[:, at], lambda at: om[:, at]))

    def back_keys(l):
        dk = dkv[0].astype(BF)
        turned = dk.astype(F32) * cos_ref[:, :LANE] - product(dk, turn_ref[:LANE, :LANE]) * sin_ref[:, :LANE]
        first = lax.broadcasted_iota(jnp.int32, turned.shape, 1) < HEAD
        z[l, :, dim:dim + LANE] = jnp.where(first, turned, dkv[1]).astype(BF)

    def back_in(l, half):
        width = wi.shape[PAIR] // 5
        at = slice(PAIR * half * width, (PAIR + TRIO * half) * width)
        part = product(wi[l, :, at], z[l, :, at], ((1,), (1,)))
        dht[ALL] = dht[ALL] + part if half else part

    def back_norm(l):
        dy, dst = upstream[l], (gx_ref, middle)[l]
        for i in range(dim // WIDE):
            cols = slice(i * WIDE, (i + 1) * WIDE)
            h[l, :, cols] = dht[cols].T.astype(BF)
        sc[l] = jnp.zeros(sc.shape[1:], F32)

        @pl.loop(0, seq // BAND, unroll=SIDE)
        def _(r):
            rows = pl.ds(pl.multiple_of(r * BAND, BAND), BAND)
            v = entry[l][rows].astype(F32)
            v = v - jnp.mean(v, axis=-1, keepdims=True)
            scale = lax.rsqrt(jnp.mean(v * v, axis=-1, keepdims=True) + 1e-6)
            hat = v * scale
            d = h[l, rows].astype(F32)
            each = (d * hat).reshape(SIDE, ROW, dim)
            sc[l] += (each[0] + each[1]) + (each[PAIR] + each[TRIO])
            d = d * gain_ref[l:l + 1]
            d = scale * (d - jnp.mean(d, axis=-1, keepdims=True) - hat * jnp.mean(d * hat, axis=-1, keepdims=True))
            dst[rows] = (dy[rows].astype(F32) + d.astype(BF).astype(F32)).astype(BF)

    def do_norm(l):
        if l == 0:
            links.arrive(("sc",), gains.at[pl.ds(0, OTHERS)])
            gain_ref[ALL] = jnp.sum(gains[ALL], axis=0)
        normalise(l, entry[l])
        for i in range(dim // WIDE):
            flat = h[l, :, i * WIDE:(i + 1) * WIDE].T
            size = ht.shape[TRIO]
            for b in range(ROW):
                lo, hi = max(b * size, i * WIDE), min((b + 1) * size, (i + 1) * WIDE)
                if lo < hi:
                    ht[l, b // PAIR, b % PAIR, lo - b * size:hi - b * size] = flat[lo - i * WIDE:hi - i * WIDE]

    def do_project(l):
        ready(PAIR * l)
        project(l)

    def do_mlp(l):
        mlp(l)
        flip(lambda at: om[:, lanes(at, WIDE)], omt.at[l], om.shape[1], dim)

    def do_put(l):
        ready(PAIR * l + 1)
        put_out(l, hid.at[0] if l == 0 else y_ref)

    stages.update(
        norm=do_norm, project=do_project, attend=attend, mlp=do_mlp, put=do_put, back_out=back_out, back_mlp=back_mlp, back_heads=back_heads,
        back_quad=back_quad, back_keys=back_keys, back_in=back_in, back_norm=back_norm, send_h=send_h, pass_h=pass_h, send_m=send_m,
        pass_m=pass_m, send_y=send_y, pass_y=pass_y, far_y=far_y, send_z=send_z, rest_z=rest_z, pass_z=pass_z, twin_z=twin_z, far_z=far_z,
        send_scale=send_scale, own_z=lambda: keep(z.at[0], z_a), own_y=lambda: keep(middle, dy_a))
    for kind, *task in order:
        stages[kind](*task)
    for l in range(PAIR):
        arrive_h(l)
        arrive_m(l)
        arrive_scale(l)
    arrive_y(1)
    for l, axis in z_out:
        arrive_z(l, axis)
    for copy in stored:
        copy.wait()
    shared.drain()
    links.drain()


def run_layers(x, dy, scale, w_in, w_out, freq, starts=(ZERO, 10.0, 20.0, 30.0)):
    seq, dim = x.shape
    proj, cat = w_in.shape[PAIR], ROW * w_out.shape[1]
    wide = proj + LANE
    hbm, vmem = pl.BlockSpec(memory_space=pltpu.HBM), pl.BlockSpec(memory_space=pltpu.VMEM)
    out = lambda *shape, dtype=BF: jax.ShapeDtypeStruct(shape, dtype)
    buffer = lambda *shape, dtype=BF: pltpu.VMEM(shape, dtype)
    sem = pltpu.SemaphoreType.DMA
    line = ROW * seq
    return pl.pallas_call(
        functools.partial(layers_kernel, layers_order(*w_in.shape[1:], *w_out.shape[1:], seq, starts)),
        out_shape=(out(seq, dim), out(seq, dim), *[out(ROW, SIDE, dim // ROW, seq)] * SIDE, *[out(ROW, cat // ROW, seq)] * PAIR, out(line, dim),
                   *[out(line, wide // ROW)] * PAIR, out(seq, wide), out(seq, dim), out(PAIR, ROW, ROW, dim, dtype=F32),
                   out(PAIR, PAIR, PAIR, cat // 16, seq), out(PAIR, PAIR, PAIR, seq // PAIR, wide // ROW)),
        in_specs=[vmem, hbm, hbm] + [vmem] * TRIO,
        out_specs=[vmem] * PAIR + [hbm] * 14,
        scratch_shapes=[
            buffer(PAIR, dim, proj), buffer(PAIR, cat, dim), buffer(PAIR, seq, wide), buffer(seq, cat), buffer(PAIR, seq, dim),
            buffer(PAIR, seq, dim), buffer(PAIR, seq, dim),
            buffer(WIDE, SIDE * seq), buffer(SIDE * seq, WIDE), buffer(SIDE * seq, WIDE), buffer(seq, dim), buffer(seq, dim),
            buffer(SIDE * seq, seq, dtype=F32), buffer(SIDE * seq, seq, dtype=F32), buffer(SIDE * seq, seq), buffer(SIDE * seq, seq),
            buffer(seq, WIDE, dtype=F32), buffer(seq, WIDE, dtype=F32), buffer(WIDE, WIDE),
            buffer(dim, seq), buffer(dim, seq), buffer(dim, seq, dtype=F32), buffer(PAIR, seq, LANE, dtype=F32),
            buffer(PAIR, cat, seq), buffer(PAIR, SIDE, PAIR, dim // ROW, seq), buffer(dim, seq), buffer(PAIR, ROW, dim, dtype=F32),
            buffer(ROW, ROW, dim, dtype=F32), buffer(ROW, dim, dtype=F32), buffer(ROW, dim, dtype=F32),
            sem((SIDE,)), sem((13,)), sem((15,)), sem((107,)), sem((13,)), sem((HEAD,)),
        ],
        compiler_params=pltpu.CompilerParams(collective_id=PAIR, has_side_effects=True, vmem_limit_bytes=67043328),
        name="run_layers",
    )(scale, w_in, w_out, x, dy, freq)


PARTS = (("i", "x", "z", "y", 0, STRIP), ("i", "x", "z", "y", STRIP, 384), ("i", "x", "y", "z", 0, STRIP), ("i", "x", "y", "z", STRIP, 384),
         ("o", "y", "z", "y", 0, 384), ("o", "z", "y", "z", 384, 384))


def reduce_order(rows, rows_b, starts):
    rate = 11650.0
    tasks = []
    sizes = {"y": WIDE * 896 / (PAIR * rate), "z": WIDE * 896 / (PAIR * rate), "x": WIDE * 768 / (PAIR * rate)}
    for axis in "yzx":
        size = sizes[axis]
        tasks.append((("swap", axis), (0, 0), starts[PAIR] if axis == "x" else starts[TRIO], [], [],
                      [((axis, by), size * n) for by, n in ((-1, 0.5), (1, 1), (-1, 1), (1, 1))], SHORT))
        tasks.append((("relay", axis), (0, 0), ZERO, [(("swap", axis), 0)], [], [((axis, -1), size / PAIR)], SHORT))
        for o, needs in ((1, [(("swap", axis), 1)]), (-1, [(("swap", axis), PAIR)]), (PAIR, [(("swap", axis), TRIO), (("relay", axis), 0)])):
            tasks.append((("near", axis, o), (0, PAIR), ZERO, needs, [], [("chip", 1.6)], QUICK))
    tasks.append((("fetch", 0), (5, 0), ZERO, [], [("make", 1, len(PARTS) - 1)], [], QUICK))
    for l in (1, 0):
        late = 1 - l
        for c, (kind, first, then, last, at, width) in enumerate(PARTS):
            needs, cost = [], 1.6 * width / STRIP
            if l == 0:
                needs = [(("near", last if kind == "i" else "x", o), 0) for o in AROUND]
            tasks.append((("make", l, c), (9 * late, c), starts[late], needs, [] if l else [("fetch", 0)], [], cost))
            full = SIDE * SIDE * (rows if kind == "i" else rows_b) * width / rate
            sends = [[((first, by), full / ROW) for by in BOTH], [((first, by), full / SIDE) for by in BOTH],
                     [((then, o), full / 16) for o in (1, -1, 1)], []]
            piece = full / 16
            sends += [[((then, o), piece) for o in (1, -1, 1)], [((last, by), SIDE * piece) for by in BOTH],
                      [((last, by), PAIR * piece) for by in BOTH], []]
            for s in range(ROW):
                task = ("sum", l, c, s)
                needs = [(("sum", l, c, s - 1), k) for k in range(len(sends[s - 1]))] if s else []
                tasks.append((task, (late, -s), ZERO, needs, [("make", l, c)] if s == 0 else [("sum", l, c, s - 1)], sends[s], SHORT))
    return plan(tasks)


def reduce_kernel(order, *refs):
    hy, hz, mx = refs[0:PAIR], refs[PAIR:SIDE], refs[SIDE:6]
    yx1, zy1, zz1, z0, y0, sc = refs[6:12]
    oa, ob = refs[12:14]
    n = len(PARTS)
    total, half, full, small, front = (refs[14 + k * n:14 + (k + 1) * n] for k in range(5))
    (hbuf, zbuf, mbuf, ybuf, scbuf, rz, ry, ssem, rsem, isem, osem) = refs[14 + 5 * n:]
    position = chip_position()
    x, y, zc, core = position
    place = {"x": x, "y": y, "z": zc}
    twin = device_at(x, y, zc, 1 - core)
    spots, peers = around(position)

    def spot(axis, o):
        return spots[axis, o % SIDE]

    def peer(axis, o):
        return peers[axis, o % SIDE]

    seq, wide = z0.shape
    own = wide // ROW
    loads, moving = {}, []

    def load(key, src, dst):
        copy = pltpu.make_async_copy(src, dst, isem.at[len(moving)])
        moving.append(key)
        copy.start()
        loads[key] = copy

    def fetch(l):
        if not l:
            load(("h", 0, "y"), hy[0], hbuf.at[0, 0])
        else:
            load(("z", 1, "z"), zz1, zbuf.at[1, 1])
        load(("h", l, "z"), hz[l], hbuf.at[l, 1])
        load(("m", l), mx[l], mbuf.at[l])
        if l:
            load(("y", 1), yx1, ybuf.at[1])
        load(("s", l), sc.at[l], scbuf.at[l])

    load(("z", 1, "y"), zy1, zbuf.at[1, 0])
    load(("h", 1, "y"), hy[1], hbuf.at[1, 0])
    done = set()

    def loaded(*keys):
        for key in keys:
            if key not in done:
                loads[key].wait()
                done.add(key)

    announce([peer(axis, o) for axis in "xyz" for o in AROUND] + [twin])
    fetch(1)
    links = Links(ssem, rsem)

    def columns(axis, o):
        return lanes(((0 if axis == "y" else SIDE) + spot(axis, o)) * own, own)

    def tokens(axis, o, index):
        return pl.ds(pl.multiple_of((PAIR * spot(axis, o) + index) * seq, seq), seq)

    def target(axis):
        return ybuf.at[0] if axis == "x" else zbuf.at[0, "yz".index(axis)]

    def leaving(axis):
        return dict(batch=("swap", axis), whole=target(axis).at[pl.ds(0, OTHERS * seq + seq // PAIR)])

    def half_at(axis, o, k):
        start = (PAIR * spot(axis, o) + core) * seq + k * (seq // PAIR)
        return target(axis).at[pl.ds(pl.multiple_of(start, seq // PAIR), seq // PAIR)]

    def relay_of(axis):
        return ry if axis == "x" else rz.at["yz".index(axis)]

    def swap(axis):
        def part(o, rows=slice(None)):
            return y0.at[rows] if axis == "x" else z0.at[rows, columns(axis, o)]

        mine = target(axis).at[tokens(axis, 0, core)]
        links.send(("relay", axis), part(PAIR, pl.ds(seq // PAIR, seq // PAIR)), relay_of(axis), peer(axis, -1), **leaving(axis))
        for by in BOTH:
            links.send(("swap", axis, by), part(by), mine, peer(axis, by), **leaving(axis))
        links.send(("swap", axis, PAIR), part(PAIR, pl.ds(0, seq // PAIR)), half_at(axis, 0, 0), peer(axis, PAIR), **leaving(axis))
        links.send(("near", axis), part(0), mine, twin, **leaving(axis))
        load(("own", axis), part(0), mine)

    def relay(axis):
        links.arrive(("relay", axis), relay_of(axis))
        links.send(("relayed", axis), relay_of(axis), half_at(axis, 1, 1), peer(axis, -1), **leaving(axis))

    def near(axis, o):
        landed = target(axis).at[tokens(axis, -o, core)]
        if o == PAIR:
            links.arrive(("swap", axis, PAIR), half_at(axis, PAIR, 0))
            links.arrive(("relayed", axis), half_at(axis, PAIR, 1))
        else:
            links.arrive(("swap", axis, o), landed)
        links.send(("near", axis), landed, landed, twin, **leaving(axis))

    def joined(axis):
        if axis not in done:
            done.add(axis)
            loaded(("own", axis))
            links.arrive(("near", axis), target(axis).at[pl.ds(0, SIDE * seq)])

    def joined_lanes(ref, l, i):
        return jnp.concatenate([ref[l, i, k].reshape(-1, ref.shape[-1]) for k in range(ROW)], axis=1)

    def make(l, c):
        kind, first, then, last, at, width = PARTS[c]
        if kind == "i":
            i = "yz".index(last)
            loaded(("h", l, last))
            if l:
                loaded(("z", l, last))
            else:
                joined(last)
            size = total[c].shape[TRIO]
            for lo in range(0, width, WIDE):
                hi = min(width, lo + WIDE)
                part = product(joined_lanes(hbuf, l, i), zbuf[l, i, :, at + lo:at + hi])
                for r in range(16):
                    total[c][l, r // SIDE, r % SIDE, :, lo:hi] = part[r * size:(r + 1) * size]
            return
        loaded(("m", l), ("s", l))
        if l:
            loaded(("y", l))
        else:
            joined("x")
        part = product(jnp.concatenate([mbuf[l, k] for k in range(ROW)], axis=1), ybuf[l, :, at:at + width])
        size = total[c].shape[TRIO]

        def put(r, value):
            total[c][(l, r // SIDE, r % SIDE) if first == "y" else (l, r % SIDE, r // SIDE)] = value

        for r in range(part.shape[0] // size):
            put(r, part[r * size:(r + 1) * size])
        gain = jnp.sum(jnp.sum(scbuf[l, :, :, at:at + width], axis=0), axis=0, keepdims=True)
        row = lax.broadcasted_iota(jnp.int32, (size, width), 0)
        put(15, jnp.where(row == 0, gain, ZERO))

    def area(l, c, o, whole):
        kind, first, then, last, at, width = PARTS[c]
        inner = (spot(then, whole) if isinstance(whole, int) else whole)
        outer = spot(last, o)
        if kind == "i":
            cols = lanes(((0 if last == "y" else SIDE) + outer) * own + at, width)
            return oa.at[l, inner, :, cols]
        cols = pl.ds(at, width)
        return ob.at[l, outer, inner, :, cols] if last == "y" else ob.at[l, inner, outer, :, cols]

    def add(l, c, s):
        kind, first, then, last, at, width = PARTS[c]
        t = total[c].at[l]
        sums = dict(batch=(l, c, 0), whole=t)
        lines = dict(batch=(l, c, 1), whole=t.at[pl.ds(0, PAIR)])
        singles = dict(batch=(l, c, PAIR), whole=t.at[pl.ds(0, PAIR), pl.ds(0, TRIO)])
        if s == 0:
            far = t.at[spot(first, PAIR)]
            for k, by in enumerate(BOTH):
                links.send((l, c, "half"), far.at[pl.ds(PAIR * k, PAIR)], half[c].at[l, k], peer(first, by), **sums)
        elif s == 1:
            links.arrive((l, c, "half"), half[c].at[l])
            for k, by in enumerate(BOTH):
                mine = t.at[spot(first, by)]
                add_into(mine.at[pl.ds(PAIR * k, PAIR)], half[c].at[l, k])
                links.send((l, c, "full"), mine, full[c].at[l, k], peer(first, by), **sums)
        elif s == PAIR:
            mine = t.at[spot(first, 0)]
            links.arrive((l, c, "full"), full[c].at[l])
            for k in range(PAIR):
                add_into(mine, full[c].at[l, k])
            for k, o in enumerate(AROUND):
                links.send((l, c, "small"), mine.at[spot(then, o)], small[c].at[l, k], peer(then, o), **singles)
        elif s == TRIO:
            links.arrive((l, c, "small"), small[c].at[l])
            mine = t.at[spot(first, 0), spot(then, 0)]
            front[c][l] = (mine[ALL] + small[c][l, 0]) + (small[c][l, 1] + small[c][l, PAIR])
        elif s == SIDE:
            src, dst = front[c].at[l], area(l, c, 0, 0)
            for o in AROUND:
                links.send((l, c, "a1"), src, dst, peer(then, o), **singles)
            copy = pltpu.make_async_copy(src, dst, osem.at[l, c])
            copy.start()
            loads["front", l, c] = copy
        elif s == 5:
            loaded(("front", l, c))
            links.arrive((l, c, "a1"), t.at[0, pl.ds(0, TRIO)])
            line = area(l, c, 0, slice(None))
            for by in BOTH:
                links.send((l, c, "a2"), line, line, peer(last, by), **lines)
        elif s == 6:
            links.arrive((l, c, "a2"), t.at[pl.ds(0, PAIR)])
            for k, by in enumerate(BOTH):
                part = area(l, c, -by, pl.ds(PAIR * k, PAIR))
                links.send((l, c, "a3"), part, part, peer(last, by), **sums)
        else:
            links.arrive((l, c, "a3"), area(l, c, PAIR, slice(None)))

    stages = {"swap": swap, "relay": relay, "near": near, "fetch": fetch, "make": make, "sum": add}
    for kind, *task in order:
        stages[kind](*task)
    links.drain()


def add_into(dst, src):
    @pl.loop(0, dst.shape[0])
    def _(i):
        if len(dst.shape) == SIDE:
            for j in range(dst.shape[1]):
                dst[i, j] += src[i, j]
        else:
            dst[i] += src[i]


def around(position):
    place, core = dict(zip("xyz", position)), position[TRIO]
    spots = {(axis, o): step(place[axis], o) for axis in "xyz" for o in range(SIDE)}
    peers = {}
    for axis in "xyz":
        for o in range(1, SIDE):
            moved = {**place, axis: spots[axis, o]}
            peers[axis, o] = device_at(moved["x"], moved["y"], moved["z"], core)
    return spots, peers


def reduce_gradients(operands, starts=(ZERO, ZERO, 20.0, 3.0)):
    hbm = pl.BlockSpec(memory_space=pltpu.HBM)
    h_rows, m_rows, y_cols, z_cols, z_own, y_own, scale_parts = operands
    part, part_b = h_rows[0].shape[PAIR] // SIDE, (m_rows[0].shape[1] + BAND) // 16
    (line, dim), wide = y_cols.shape, z_own.shape[1]
    out = lambda *shape: jax.ShapeDtypeStruct(shape, F32)
    sem = pltpu.SemaphoreType.DMA

    def buffers(*lead):
        return [pltpu.VMEM((PAIR, *lead, part if e[0] == "i" else part_b, e[5]), F32) for e in PARTS]

    return pl.pallas_call(
        functools.partial(reduce_kernel, reduce_order(part, part_b, starts)),
        out_shape=(out(PAIR, SIDE, part, wide), out(PAIR, SIDE, SIDE, part_b, dim)),
        in_specs=[hbm] * 12,
        out_specs=[hbm] * PAIR,
        scratch_shapes=[
            *buffers(SIDE, SIDE), *buffers(PAIR, PAIR), *buffers(PAIR, SIDE), *buffers(TRIO), *buffers(),
            pltpu.VMEM((PAIR, PAIR, *h_rows[0].shape), BF), pltpu.VMEM((PAIR, PAIR, line, wide // ROW), BF), pltpu.VMEM((PAIR, *m_rows[0].shape), BF),
            pltpu.VMEM((PAIR, line, dim), BF), pltpu.VMEM(scale_parts.shape, F32),
            pltpu.VMEM((PAIR, z_own.shape[0] // PAIR, wide // ROW), BF), pltpu.VMEM((y_own.shape[0] // PAIR, dim), BF),
            sem((39,)), sem((90,)), sem((14,)), sem((PAIR, len(PARTS))),
        ],
        compiler_params=pltpu.CompilerParams(collective_id=1, has_side_effects=True, vmem_limit_bytes=67043328),
        name="reduce_gradients",
    )(*h_rows, *m_rows, y_cols, *z_cols, z_own, y_own, scale_parts)


def finish_kernel(count, in_ref, out_ref, y_ref, gx_ref, in_grad, out_grad, y_out, gx_out, scale_out, in_buf, out_buf, y_buf, gx_buf, came, left):
    moves = [(out_ref.at[l, p], out_buf.at[l, pl.ds(SIDE * p, SIDE)]) for l in range(PAIR) for p in range(SIDE)]
    moves += [(y_ref, y_buf), (gx_ref, gx_buf)]
    size, width = in_buf.shape[PAIR:]
    moves += [(in_ref.at[l, p, :, pl.ds(0, width)], in_buf.at[l, p]) for l in range(PAIR) for p in range(SIDE)]
    loads = [pltpu.make_async_copy(src, dst, came.at[k]) for k, (src, dst) in enumerate(moves)]
    for copy in loads:
        copy.start()
    stores = []

    def store(src, dst):
        copy = pltpu.make_async_copy(src, dst, left.at[len(stores)])
        copy.start()
        stores.append(copy)

    for l in range(PAIR):
        for p in range(SIDE):
            loads[SIDE * l + p].wait()
        store(out_buf.at[l, pl.ds(0, 15)], out_grad.at[l])
    for k, (src, dst) in enumerate(((y_buf, y_out), (gx_buf, gx_out))):
        loads[ROW + k].wait()
        store(src, dst)
    me = lax.axis_index("fsdp")
    for l in range(PAIR):
        for f in range(ROW):
            @pl.when(me == f)
            def _():
                scale_out[l:l + 1] = out_buf[l, 15, 0:1, f * count:(f + 1) * count]
    for l in range(PAIR):
        for p in range(SIDE):
            loads[10 + SIDE * l + p].wait()
            store(in_buf.at[l, p], in_grad.at[l, pl.ds(p * size, size)])
    for copy in stores:
        copy.wait()


def finish(in_sums, out_sums, y, gx, rows, proj):
    hbm = pl.BlockSpec(memory_space=pltpu.HBM)
    out = lambda *shape, dtype=F32: jax.ShapeDtypeStruct(shape, dtype)
    size, (depth, dim) = in_sums.shape[PAIR], out_sums.shape[TRIO:]
    in_grad, out_grad, y_out, gx_out, scale = pl.pallas_call(
        functools.partial(finish_kernel, rows),
        out_shape=(out(PAIR, rows, proj), out(PAIR, 15, depth, dim), out(*y.shape, dtype=BF), out(*gx.shape, dtype=BF), out(PAIR, rows)),
        in_specs=[hbm] * SIDE,
        out_specs=[hbm] * SIDE + [pl.BlockSpec(memory_space=pltpu.VMEM)],
        scratch_shapes=[
            pltpu.VMEM((PAIR, SIDE, size, proj), F32), pltpu.VMEM((PAIR, 16, depth, dim), F32), pltpu.VMEM(y.shape, BF), pltpu.VMEM(gx.shape, BF),
            pltpu.SemaphoreType.DMA((18,)), pltpu.SemaphoreType.DMA((12,)),
        ],
        compiler_params=pltpu.CompilerParams(vmem_limit_bytes=67043328),
        name="finish",
    )(in_sums, out_sums, y, gx)
    return y_out[None], gx_out[None], scale, in_grad, out_grad.reshape(PAIR, 15 * depth, dim)


def solution(mesh):
    fsdp_size = mesh.shape["fsdp"]
    batch_spec = P(("dp", "fsdp"), None, None)
    scale_spec = P(None, "fsdp")
    weight_spec = P(None, "fsdp", None)

    def device_step(x_in, grad_y, norm_scale, w_in, w_out):
        n_layers = w_in.shape[0]
        seq_len, model_dim = x_in.shape[1:]
        proj_dim = w_in.shape[PAIR]
        ff_dim = w_out.shape[1] * fsdp_size - model_dim
        head_dim = (proj_dim - model_dim - PAIR * ff_dim) // PAIR
        rows, rows_out = norm_scale.shape[1], w_out.shape[1]
        half_dim = head_dim // PAIR
        freq = 10000.0 ** (-np.arange(half_dim, dtype=np.float32) * 2.0 / head_dim)
        freq = jnp.asarray(np.tile(freq.astype(np.float32), (ROW, LANE // half_dim)))
        hidden, grad_hidden, *rest = run_layers(x_in[0], grad_y[0], norm_scale, w_in, w_out, freq)
        in_sums, out_sums = reduce_gradients((rest[0:SIDE], rest[SIDE:6], rest[6], rest[OTHERS:9], rest[9], rest[10], rest[11]))
        return finish(in_sums, out_sums, hidden, grad_hidden, rows, proj_dim)

    return jax.shard_map(
        device_step,
        mesh=mesh,
        in_specs=(batch_spec, batch_spec, scale_spec, weight_spec, weight_spec),
        out_specs=(batch_spec, batch_spec, scale_spec, weight_spec, weight_spec),
        check_vma=False,
    )
```

```python
import functools
import jax
import jax.numpy as jnp
import numpy as np
from jax import lax
from jax.experimental import pallas as pl
from jax.experimental.pallas import tpu as pltpu
from jax.sharding import PartitionSpec as P

MESH_ID = pl.DeviceIdType.MESH
BOTH = (1, -1)
AROUND = (1, -1, 2)
PARTS = (True, False)
ALL, ZERO = ..., 0.0
OTHERS = 7
QUICK, SHORT = 0.2, 0.3
LANE, WIDE, STRIP, HEAD = 128, 256, 512, 64
ROW, BAND, SIDE, TRIO, PAIR = 8, 32, 4, 3, 2


class Links:
    def __init__(self, send_sems, recv_sems):
        self.send_sems, self.recv_sems = send_sems, recv_sems
        self.slots, self.batches, self.sent, self.count = {}, {}, {}, 0

    def _landing(self, key, lane):
        if key not in self.slots:
            self.slots[key] = self.count
            self.count += 1 if lane is None else PAIR
        return self.recv_sems.at[self.slots[key] + (0 if lane is None else lane)]

    def send(self, key, src, dst, device, landing=None, whole=None, batch=None, lane=None):
        leaving = self.batches.setdefault(batch or key, len(self.batches))
        copy = pltpu.make_async_remote_copy(
            src_ref=src, dst_ref=dst, send_sem=self.send_sems.at[leaving], recv_sem=self._landing(landing or key, lane),
            device_id=device, device_id_type=MESH_ID)
        copy.start()
        self.sent[batch or key] = (src if whole is None else whole, leaving)

    def arrive(self, key, landed, lane=None):
        pltpu.make_async_copy(landed, landed, self._landing(key, lane)).wait()

    def drain(self):
        for left, leaving in self.sent.values():
            pltpu.make_async_copy(left, left, self.send_sems.at[leaving]).wait()
        self.sent.clear()


def rem(a, n):
    return a % n if isinstance(a, int) else lax.rem(a, n)


def chip_position():
    f, d = lax.axis_index("fsdp"), lax.axis_index("dp")
    return f // PAIR, rem(d, SIDE), d // SIDE, rem(f, PAIR)


def device_at(x, y, z, core):
    return (z * SIDE + y, x * PAIR + core)


def step(coord, by):
    return rem(coord + SIDE + by, SIDE)


def announce(devices):
    barrier = pltpu.get_barrier_semaphore()
    for device in devices:
        pl.semaphore_signal(barrier, inc=1, device_id=device, device_id_type=MESH_ID)
    pl.semaphore_wait(barrier, len(devices))


def plan(tasks, latency=2.5):
    free, landed, order, now = {}, {}, [], ZERO
    left = list(tasks)
    while left:
        best = None
        for place, (name, rank, start, needs, after, _, _) in enumerate(left):
            if all(n[0] in landed for n in needs) and all(n in landed for n in after):
                ready = max([start, now] + [landed[task][i] for task, i in needs])
                best = min(best or (ready, rank, place), (ready, rank, place))
        now, _, place = best
        name, _, _, _, _, sends, cost = left.pop(place)
        order.append(name)
        now += cost
        landed[name] = []
        for link, time, *more in sends:
            free[link] = max(now, free.get(link, ZERO)) + time
            landed[name].append(free[link] + latency + sum(more))
    return order


def layers_order(rows_i, cols_i, rows_o, cols_o, seq, starts):
    rate = 23300.0
    tasks = []
    for m in range(SIDE):
        is_in = m % PAIR == 0
        edge = cols_i // LANE * SIDE // 9 // PAIR * WIDE
        size = {"y": rows_i // SIDE * edge, "x": rows_i * (cols_i - PAIR * edge)} if is_in else {"y": rows_o // SIDE * cols_o // PAIR}
        size["z"] = size["y"]
        colors = "yzx" if is_in else "yz"
        tasks.append((("lend", m), 5, 3.0 + SIDE * m, [], [], [("chip", (rows_i * cols_i if is_in else rows_o * cols_o) / 150000.0)], QUICK))
        for color in colors:
            cost = size[color] / rate
            both = [(("x", by), cost) for by in BOTH]
            spread = [((color, by), cost) for by in BOTH] if color != "x" else []
            tasks.append((("reach", m, color), m, starts[m], [], [], both, QUICK))
            for i, by in enumerate(BOTH):
                tasks.append((("relay", m, color, by), m, ZERO, [(("reach", m, color), i)], [], [(("x", by), cost / PAIR)] + spread, QUICK))
            halves = [(("relay", m, color, by), 0) for by in BOTH]
            tasks.append((("far", m, color), m, ZERO, halves, [], spread, QUICK))
            if color == "x":
                continue
            for off, source, first in ((-1, ("relay", m, color, 1), 1), (1, ("relay", m, color, -1), 1), (PAIR, ("far", m, color), 0)):
                for i, by in enumerate(BOTH):
                    tasks.append((("pass", m, color, off, by), m, ZERO, [(source, first + i)], [], [((color, by), cost / PAIR)], QUICK))
                halves = [(("pass", m, color, off, by), 0) for by in BOTH]
                tasks.append((("close", m, color, off), m, ZERO, halves, [], [], QUICK))
        for off in (-1, 1, PAIR):
            last = [("close", m, color, off) for color in "yz"]
            if is_in:
                last.append(("far", m, "x") if off == PAIR else ("relay", m, "x", -off))
            tasks.append((("hand", m, off), m, ZERO, [], last, [("chip", (rows_i * cols_i if is_in else rows_o * cols_o) / 150000.0)], QUICK))
    before = []

    def work(name, cost, mats=()):
        needs = [(("hand", m, off), 0) for m in mats for off in (-1, 1, PAIR)] + [(("lend", m), 0) for m in mats]
        tasks.append((name, 99, ZERO, needs, list(before), [], cost))
        before[:] = [name]

    for l in range(PAIR):
        work(("norm", l), 0.8)
        work(("project", l), 4.0, [PAIR * l])
        work(("attend", l), 4.2)
        work(("mlp", l), 2.2)
        work(("put", l), 1.6, [PAIR * l + 1])
    for l in (1, 0):
        work(("back_out", l), 2.9)
        work(("back_mlp", l), 2.0)
        work(("back_heads", l), 1.0)
        work(("back_quad", l), 6.0)
        work(("back_keys", l), QUICK)
        for i in range(PAIR):
            work(("back_in", l, i), 1.3 + 0.6 * i)
        work(("back_norm", l), 1.0)
    def send(name, rank, start, after, sends):
        tasks.append((name, rank, start, [], [after] if after else [], sends, 0.4))

    def follow(name, rank, needs, sends):
        tasks.append((name, rank, ZERO, needs, [], sends, QUICK))

    def both(axis, size):
        return [((axis, by), size / rate, margin) for by in BOTH]

    model, margin = rows_i * ROW, 2.0
    for l in (1, 0):
        for axis in "yz":
            name = ("send_h", l, axis)
            send(name, 20 - l, 58.0, ("norm", l), both(axis, seq * model))
            for i, by in enumerate(BOTH):
                for index in range(PAIR):
                    follow(("pass_h", l, axis, by, index), 10, [(name, i)], [((axis, by), seq * model / SIDE / rate, margin)])
        name = ("send_m", l)
        send(name, 22 - l, ZERO, ("mlp", l), both("x", seq * rows_o) + both("x", PAIR * seq * rows_o))
        for i, by in enumerate(BOTH):
            for index in range(PAIR):
                follow(("pass_m", l, by, index), 11, [(name, i)], [(("x", by), seq * rows_o / PAIR / rate, margin)])
        if l == 0:
            send(("own_y",), 15, ZERO, ("back_norm", 1), [])
            send(("send_scale", l), 15, ZERO, ("back_norm", l), [])
            continue
        name = ("send_y", l)
        send(name, 12, 42.0, None, both("x", seq * model))
        for i, by in enumerate(BOTH):
            follow(("pass_y", l, by), 12, [(name, i)], [(("x", by), seq * model / PAIR / rate, margin)])
        follow(("far_y", l), 12, [(("pass_y", l, by), 0) for by in BOTH], [])
        for axis in "zy":
            name = ("send_z", l, axis)
            share = seq * (cols_i + LANE) / ROW
            send(name, 13, ZERO, ("back_mlp", l), both(axis, share / PAIR) + both(axis, share))
            if axis == "y":
                name = ("rest_z", l)
                send(name, 13, ZERO, ("back_keys", l), both(axis, share / ROW) + both(axis, share / SIDE))
            for i, by in enumerate(BOTH):
                follow(("pass_z", l, axis, by), 13, [(name, i)], [((axis, by), share / PAIR / rate, margin)])
                follow(("twin_z", l, axis, by), 14, [(name, PAIR + i)], [])
            follow(("far_z", l, axis), 14, [(("pass_z", l, axis, by), 0) for by in BOTH], [])
        send(("send_scale", l), 15, ZERO, ("back_norm", l), [])
    send(("own_z",), 15, ZERO, ("back_keys", 0), [])
    return plan(tasks)


def gather_stages(links, position, shard_i, shard_o, wi, wo, lsem):
    x, y, z, core = position
    twin = device_at(x, y, z, 1 - core)
    rows_i, cols_i = shard_i.shape[1:]
    rows_o, cols_o = shard_o.shape[1:]
    quarter_i, quarter_o = rows_i // SIDE, rows_o // SIDE
    third_i = cols_i // LANE * SIDE // 9 // PAIR * WIDE
    half_o = cols_o // PAIR
    cut_o = quarter_o // 16 * ROW + ROW if quarter_o % 16 else quarter_o // PAIR
    place = {"x": x, "y": y, "z": z}

    spots = {(axis, o): step(place[axis], o) for axis in "xyz" for o in range(SIDE)}

    def spot(axis, o):
        return spots[axis, o % SIDE]

    table = {}
    for axis in "xyz":
        for o in range(1, SIDE):
            moved = {**place, axis: spot(axis, o)}
            table[axis, o] = device_at(moved["x"], moved["y"], moved["z"], core)

    def peer(axis, o):
        return table[axis, o % SIDE]

    mats = []
    for l in range(PAIR):
        mats.append((shard_i.at[l], wi.at[l], rows_i, True))
        mats.append((shard_o.at[l], wo.at[l], rows_o, False))

    def region(is_in, color, q):
        if is_in:
            if color == "x":
                lo, hi = PAIR * third_i, cols_i
                rows = (0, rows_i)
            else:
                lo, hi = (0, third_i) if color == "y" else (third_i, PAIR * third_i)
                rows = (q * quarter_i, quarter_i)
            mid = lo + ((hi - lo) // LANE + 1) // PAIR * LANE
            return (rows, (lo, hi - lo)), (rows, (lo, mid - lo)), (rows, (mid, hi - mid))
        cols = (0, half_o) if color == "y" else (half_o, half_o)
        start = q * quarter_o
        return ((start, quarter_o), cols), ((start, cut_o), cols), ((start + cut_o, quarter_o - cut_o), cols)

    def at(m, xb, area):
        (r, nr), (c, nc) = area
        _, out, size, _ = mats[m]
        return out.at[pl.ds(pl.multiple_of((PAIR * xb + core) * size + r, ROW), nr), pl.ds(c, nc)]

    def block(m, xb, index):
        _, out, size, _ = mats[m]
        return out.at[pl.ds(pl.multiple_of((PAIR * xb + index) * size, BAND), size)]

    def group(m, color):
        _, out, _, is_in = mats[m]
        (_, nr), (c, nc) = region(is_in, color, 0)[0]
        return dict(batch=(m, color), whole=out.at[pl.ds(0, nr * (TRIO if color == "x" else 12)), pl.ds(c, nc)])

    def reach(m, color):
        src, _, _, is_in = mats[m]
        area = region(is_in, color, place[color])[0]
        for by in BOTH:
            links.send((m, "x1", color, by), src.at[pl.ds(pl.multiple_of(area[0][0], ROW), area[0][1]), pl.ds(*area[1])], at(m, x, area), peer("x", by), **group(m, color))

    def launch(m, color, off):
        is_in = mats[m][TRIO]
        moved = at(m, spot("x", off), region(is_in, color, place[color])[0])
        for by in BOTH:
            links.send((m, "p1", color, off, by), moved, moved, peer(color, by), **group(m, color))

    def relay(m, color, by):
        is_in = mats[m][TRIO]
        xb = spot("x", -by)
        areas = region(is_in, color, place[color])
        links.arrive((m, "x1", color, by), at(m, xb, areas[0]))
        part = at(m, xb, areas[1] if by == 1 else areas[PAIR])
        links.send((m, "x2", color), part, part, peer("x", by), **group(m, color))
        if color != "x":
            launch(m, color, -by)

    def far(m, color):
        is_in = mats[m][TRIO]
        links.arrive((m, "x2", color), at(m, spot("x", PAIR), region(is_in, color, place[color])[0]))
        if color != "x":
            launch(m, color, PAIR)

    def pass_on(m, color, off, by):
        is_in = mats[m][TRIO]
        xb = spot("x", off)
        areas = region(is_in, color, spot(color, -by))
        links.arrive((m, "p1", color, off, by), at(m, xb, areas[0]))
        part = at(m, xb, areas[1] if by == 1 else areas[PAIR])
        links.send((m, "p2", color, off), part, part, peer(color, by), **group(m, color))

    def close(m, color, off):
        is_in = mats[m][TRIO]
        links.arrive((m, "p2", color, off), at(m, spot("x", off), region(is_in, color, spot(color, PAIR))[0]))

    def four(m):
        _, out, size, _ = mats[m]
        return out.at[pl.ds(0, SIDE * size)]

    def give(m, src, dst):
        links.send((m, "chip"), src, dst, twin, batch=(m, "chip"), whole=four(m))

    def hand(m, off):
        whole = block(m, spot("x", off), core)
        give(m, whole, whole)

    owns = []

    def begin():
        for m, (src, _, _, _) in enumerate(mats):
            copy = pltpu.make_async_copy(src, block(m, x, core), lsem.at[m])
            copy.start()
            owns.append(copy)

    def lend(m):
        give(m, mats[m][0], block(m, x, core))

    def ready(m):
        owns[m].wait()
        links.arrive((m, "chip"), four(m))

    return begin, ready, peer, {"reach": reach, "relay": relay, "far": far, "pass": pass_on, "close": close, "hand": hand, "lend": lend}


BF, F32 = jnp.bfloat16, jnp.float32


def product(a, b, contract=((1,), (0,))):
    return lax.dot_general(a, b, (contract, ((), ())), preferred_element_type=F32)


def lanes(start, size):
    return pl.ds(start if isinstance(start, int) else pl.multiple_of(start, LANE), size)


def layers_kernel(order, sc_ref, wi_ref, wo_ref, x_ref, dy_ref, freq_ref,
                  y_ref, gx_ref, hy_a, hy_b, hz_a, hz_b, mx_a, mx_b, yx_b, zy_b, zz_b, z_a, dy_a, sc_out, relay_m, relay_z,
                  wi, wo, z, om, h, hid, qr, kts, vsl, ksl, turned_q, turned_o, scores, dscores, pcat, dscat, cos_ref, sin_ref, turn_ref,
                  dot_heads, qt, dht, dkv, omt, ht, dyt, sc, gains, own_gain, gain_ref, load_sems, own_sems, send_sems, recv_sems,
                  share_send_sems, share_recv_sems):
    seq, dim = x_ref.shape
    ff = (wi.shape[PAIR] - dim - LANE) // PAIR
    position = chip_position()
    x, y, zc, core = position
    twin = device_at(x, y, zc, 1 - core)
    me = PAIR * x + core
    links, shared = Links(send_sems, recv_sems), Links(share_send_sems, share_recv_sems)
    stored = []
    spots, _ = around(position)
    h_out, m_out, y_out, z_out = {"y": (hy_a, hy_b), "z": (hz_a, hz_b)}, (mx_a, mx_b), {1: yx_b}, {(1, "y"): zy_b, (1, "z"): zz_b}
    middle = hid.at[1]
    begin, ready, peer, stages = gather_stages(links, position, wi_ref, wo_ref, wi, wo, load_sems)
    others = [(zc * SIDE + y, rem(me + k, ROW)) for k in range(1, ROW)]

    def spot(axis, o):
        return spots[axis, o % SIDE]

    def device(axis, o, index):
        moved = {"x": x, "y": y, "z": zc, axis: spot(axis, o)}
        return device_at(moved["x"], moved["y"], moved["z"], index)

    own_gain[ALL] = jnp.zeros(own_gain.shape, F32)
    count = sc_ref.shape[1]
    for f in range(ROW):
        @pl.when(me == f)
        def _():
            own_gain[0:PAIR, f * count:(f + 1) * count] = sc_ref[ALL].astype(F32)
    announce(others + [device(axis, o, index) for axis in "yz" for o in AROUND for index in range(PAIR)])
    begin()
    for k, far in enumerate(others):
        links.send(("sc",), own_gain, gains.at[me], far, batch=("sc",), whole=gains.at[pl.ds(0, OTHERS)])

    def keep(src, dst):
        copy = pltpu.make_async_copy(src, dst, own_sems.at[len(stored)])
        copy.start()
        stored.append(copy)

    def tokens(axis, o, index):
        return pl.ds(pl.multiple_of((PAIR * spot(axis, o) + index) * seq, seq), seq)

    def place(axis, o, index):
        return PAIR * spot(axis, o) + index

    def columns(axis, o):
        size = z.shape[PAIR] // ROW
        return lanes(((0 if axis == "y" else SIDE) + spot(axis, o)) * size, size)

    def several(batch, ref, n):
        whole = ref.at[pl.ds(0, n * seq if batch[0][0] in "yz" else n)]
        return dict(batch=batch, whole=whole)

    def send_h(l, axis):
        out = h_out[axis][l].at[place(axis, 0, core)]
        for by in BOTH:
            for index in range(PAIR):
                shared.send(("h", l, axis, by), ht.at[l, :, index], out, device(axis, by, index), lane=core, **several(("h", l, axis), h_out[axis][l], OTHERS))
        shared.send(("h", l, axis), ht.at[l, :, 1 - core], out, twin, **several(("h", l, axis), h_out[axis][l], OTHERS))
        keep(ht.at[l, :, core], out)

    def pass_h(l, axis, by, index):
        out = h_out[axis][l]
        shared.arrive(("h", l, axis, by), out.at[place(axis, -by, index)], index)
        part = out.at[place(axis, -by, index), pl.ds(1 - by, PAIR)]
        shared.send(("h", l, axis), part, part, device(axis, by, core), **several(("h", l, axis), out, OTHERS))

    def arrive_h(l):
        for axis in "yz":
            shared.arrive(("h", l, axis), h_out[axis][l].at[pl.ds(0, TRIO)])

    def row_block(l, o, index, part=None):
        size = omt.shape[1] // ROW
        start = (PAIR * spot("x", o) + index) * size
        if part is not None:
            size = size // PAIR
            start = start + part * size
        return omt.at[l, pl.ds(pl.multiple_of(start, 16), size)]

    def row_half(k):
        size = m_out[0].shape[1] // PAIR
        return pl.ds(k * size, size)

    def send_m(l):
        out = m_out[l].at[place("x", 0, core)]
        for k, by in enumerate(BOTH):
            for index in range(PAIR):
                shared.send(("mr", l, by), row_block(l, PAIR, index, k), relay_m.at[l, k, core], device("x", by, index), lane=core, **several(("m", l), m_out[l], OTHERS))
        for by in BOTH:
            for index in range(PAIR):
                shared.send(("m", l), row_block(l, by, index), out, device("x", by, index), **several(("m", l), m_out[l], OTHERS))
        shared.send(("m", l), row_block(l, 0, 1 - core), out, twin, **several(("m", l), m_out[l], OTHERS))
        keep(row_block(l, 0, core), out)

    def pass_m(l, by, index):
        k = (1 - by) // PAIR
        shared.arrive(("mr", l, by), relay_m.at[l, k, index], index)
        shared.send(("m", l), relay_m.at[l, k, index], m_out[l].at[place("x", -by, index), row_half(k)], device("x", by, core),
                    **several(("m2", l), m_out[l], PAIR))

    def arrive_m(l):
        shared.arrive(("m", l), m_out[l].at[pl.ds(0, OTHERS)])

    def token_half(axis, o, k):
        return pl.ds(pl.multiple_of((PAIR * spot(axis, o) + core) * seq + k * (seq // PAIR), seq // PAIR), seq // PAIR)

    def send_y(l):
        src, out = dy_ref, y_out[l].at[tokens("x", 0, core)]
        for by in BOTH:
            shared.send(("y", l, by), src, out, device("x", by, core), **several(("y", l), y_out[l], OTHERS))
        shared.send(("y", l), src, out, twin, **several(("y", l), y_out[l], OTHERS))
        keep(src, out)

    def pass_y(l, by):
        landed, part = y_out[l].at[tokens("x", -by, core)], y_out[l].at[token_half("x", -by, (1 - by) // PAIR)]
        shared.arrive(("y", l, by), landed)
        shared.send(("y2", l), part, part, device("x", by, core), **several(("y", l), y_out[l], OTHERS))
        shared.send(("y", l), landed, landed, twin, **several(("y", l), y_out[l], OTHERS))

    def far_y(l):
        landed = y_out[l].at[tokens("x", PAIR, core)]
        shared.arrive(("y2", l), landed)
        shared.send(("y", l), landed, landed, twin, **several(("y", l), y_out[l], OTHERS))

    def arrive_y(l):
        shared.arrive(("y", l), y_out[l].at[pl.ds(0, SIDE * seq)])

    def push_z(l, axis, o, ready):
        out = z_out[l, axis].at[tokens(axis, 0, core)]
        batch = several(("z", l, axis), z_out[l, axis], ROW)

        def start():
            if o != PAIR:
                shared.send(("z", l, axis, o), z.at[l, :, columns(axis, o)], out, device(axis, o, core), **batch)
                return
            for k, by in enumerate(BOTH):
                shared.send(("zr", l, axis, by), z.at[l, pl.ds(k * (seq // PAIR), seq // PAIR), columns(axis, PAIR)], relay_z.at[l, "yz".index(axis), k],
                            device(axis, by, core), **batch)

        if ready is None:
            start()
        else:
            pl.when(ready)(start)

    def own_part(l, axis):
        out, mine = z_out[l, axis].at[tokens(axis, 0, core)], z.at[l, :, columns(axis, 0)]
        shared.send(("z", l, axis), mine, out, twin, **several(("z", l, axis), z_out[l, axis], ROW))
        keep(mine, out)

    def send_z(l, axis):
        for o in (PAIR, 1, -1):
            push_z(l, axis, o, spot(axis, o) != 0 if axis == "y" else None)
        if axis == "z":
            own_part(l, axis)

    def rest_z(l):
        for o in (PAIR, 1, -1):
            push_z(l, "y", o, spot("y", o) == 0)
        own_part(l, "y")

    def pass_z(l, axis, by):
        k = (1 - by) // PAIR
        half = relay_z.at[l, "yz".index(axis), k]
        shared.arrive(("zr", l, axis, by), half)
        shared.send(("z2", l, axis), half, z_out[l, axis].at[token_half(axis, -by, k)], device(axis, by, core), **several(("z", l, axis), z_out[l, axis], ROW))

    def twin_z(l, axis, by):
        landed = z_out[l, axis].at[tokens(axis, -by, core)]
        shared.arrive(("z", l, axis, by), landed)
        shared.send(("z", l, axis), landed, landed, twin, **several(("z", l, axis), z_out[l, axis], ROW))

    def far_z(l, axis):
        landed = z_out[l, axis].at[tokens(axis, PAIR, core)]
        shared.arrive(("z2", l, axis), landed)
        shared.send(("z", l, axis), landed, landed, twin, **several(("z", l, axis), z_out[l, axis], ROW))

    def arrive_z(l, axis):
        shared.arrive(("z", l, axis), z_out[l, axis].at[pl.ds(0, SIDE * seq)])

    def send_scale(l):
        for far in others:
            shared.send(("scale", l), sc.at[l], sc_out.at[l, me], far, batch=("scale", l), whole=sc_out.at[l, pl.ds(0, OTHERS)])
        keep(sc.at[l], sc_out.at[l, me])

    def arrive_scale(l):
        shared.arrive(("scale", l), sc_out.at[l, pl.ds(0, OTHERS)])

    gains[me] = own_gain[ALL]
    z[:, :, wi.shape[PAIR]:] = jnp.zeros((PAIR, seq, z.shape[PAIR] - wi.shape[PAIR]), BF)
    entry = (x_ref, hid.at[0])
    angle = lax.broadcasted_iota(jnp.int32, (seq, LANE), 0).astype(F32) * freq_ref[0:1]
    for half in range(PAIR):
        cos_ref[:, LANE * half:LANE * (half + 1)] = jnp.cos(angle)
        sin_ref[:, LANE * half:LANE * (half + 1)] = jnp.sin(angle)
    lane = lax.broadcasted_iota(jnp.int32, turn_ref.shape, 1)
    down = lax.broadcasted_iota(jnp.int32, turn_ref.shape, 0) - lane
    low = rem(lane, HEAD) < BAND
    turn_ref[ALL] = jnp.where(low & (down == BAND), -1.0, jnp.where(jnp.logical_not(low) & (down == -BAND), 1.0, ZERO)).astype(BF)
    kts[ALL] = jnp.zeros(kts.shape, BF)
    pcat[ALL] = jnp.zeros(pcat.shape, BF)
    dscat[ALL] = jnp.zeros(dscat.shape, BF)

    def normalise(l, src):
        @pl.loop(0, seq // BAND, unroll=SIDE)
        def _(r):
            rows = pl.ds(pl.multiple_of(r * BAND, BAND), BAND)
            v = src[rows].astype(F32)
            v = v - jnp.mean(v, axis=-1, keepdims=True)
            var = jnp.mean(v * v, axis=-1, keepdims=True)
            h[l, rows] = (v * lax.rsqrt(var + 1e-6) * gain_ref[l:l + 1]).astype(BF)

    def project(l):
        strip = wi.shape[PAIR] // 5

        @pl.loop(0, 5)
        def _(i):
            at = lanes(i * strip, strip)
            z[l, :, at] = product(h[l], wi[l, :, at]).astype(BF)

    def heads(l):
        cos, sin = cos_ref[ALL], sin_ref[ALL]
        for g in range(dim // WIDE):
            q = z[l, :, g * WIDE:(g + 1) * WIDE]
            qr[l, :, g * WIDE:(g + 1) * WIDE] = ((q.astype(F32) * cos + product(q, turn_ref[ALL]) * sin) * 0.125).astype(BF)
        kv = z[l, :, dim:dim + LANE]
        turned = kv.astype(F32) * cos[:, :LANE] + product(kv, turn_ref[:LANE, :LANE]) * sin[:, :LANE]
        first = lax.broadcasted_iota(jnp.int32, turned.shape, 1) < HEAD
        key_lo = jnp.where(first, turned, ZERO)
        val_hi = jnp.where(first, ZERO, kv.astype(F32))
        return key_lo, pltpu.roll(key_lo, HEAD, 1), pltpu.roll(val_hi, HEAD, 1), val_hi

    def slot_rows(ref, lo, hi):
        zero = jnp.zeros((seq, LANE), BF)
        lo, hi = lo.astype(BF), hi.astype(BF)
        for i, (left, right) in enumerate(((lo, zero), (hi, zero), (zero, lo), (zero, hi))):
            ref[i * seq:(i + 1) * seq, :LANE] = left
            ref[i * seq:(i + 1) * seq, LANE:] = right

    def slot_cols(ref, lo):
        flat = lo.T[:HEAD].astype(BF)
        for i in range(SIDE):
            ref[HEAD * i:HEAD * (i + 1), i * seq:(i + 1) * seq] = flat

    def chances(i, half):
        at = slice(LANE * half, LANE * (half + 1))
        blocks = [pl.ds(pl.multiple_of(i * seq + LANE * k, LANE), LANE) for k in range(half + 1)]
        s = [scores[keys, at] for keys in blocks]
        lower = lax.broadcasted_iota(jnp.int32, s[-1].shape, 1) >= lax.broadcasted_iota(jnp.int32, s[-1].shape, 0)
        s[-1] = jnp.where(lower, s[-1], -1e30)
        top = functools.reduce(jnp.maximum, [jnp.max(v, axis=0, keepdims=True) for v in s])
        e = [jnp.exp(v - top) for v in s]
        scale = 1.0 / sum(jnp.sum(v, axis=0, keepdims=True) for v in e)
        return at, [(keys, v * scale) for keys, v in zip(blocks, e)]

    def attend(l):
        key_lo, key_hi, val_lo, _ = heads(l)
        slot_rows(ksl, key_lo, key_hi)
        slot_cols(kts, val_lo)
        flip(lambda at: qr[l, :, lanes(at, WIDE)], qt, dim)

        @pl.loop(0, dim // WIDE)
        def _(g):
            rows = pl.ds(pl.multiple_of(g * WIDE, WIDE), WIDE)
            scores[ALL] = product(ksl[ALL], qt[rows])

            @pl.loop(0, SIDE)
            def _(i):
                for half in range(PAIR):
                    at, blocks = chances(i, half)
                    for keys, p in blocks:
                        pcat[keys, at] = p.astype(BF)
            flat = product(kts[ALL], pcat[ALL]).astype(BF)
            omt[l, rows] = flat
            om[:, lanes(g * WIDE, WIDE)] = flat.T

    def mlp(l):
        @pl.loop(0, seq // BAND)
        def _(r):
            rows = pl.ds(pl.multiple_of(r * BAND, BAND), BAND)

            @pl.loop(0, ff // STRIP)
            def _(i):
                gate = z[l, rows, lanes(dim + LANE + i * STRIP, STRIP)].astype(F32)
                up = z[l, rows, lanes(dim + LANE + ff + i * STRIP, STRIP)].astype(F32)
                om[rows, lanes(dim + i * STRIP, STRIP)] = (gate * jax.nn.sigmoid(gate) * up).astype(BF)

    def put_out(l, dst):
        for n in range(dim // WIDE):
            cols = slice(n * WIDE, (n + 1) * WIDE)
            total = product(om[ALL], wo[l, :, cols])
            dst[:, cols] = (entry[l][:, cols].astype(F32) + total).astype(BF)

    def flip(src, dst, width, first=0):
        @pl.loop(first // WIDE, width // WIDE)
        def _(i):
            dst[pl.ds(pl.multiple_of(i * WIDE, WIDE), WIDE)] = src(i * WIDE).T

    upstream = (middle, dy_ref)

    def back_out(l):
        dy = upstream[l]
        flip(lambda at: dy[:, lanes(at, WIDE)], dyt, dim)

        @pl.loop(0, wo.shape[1] // dim)
        def _(n):
            rows = pl.ds(pl.multiple_of(n * dim, dim), dim)
            part = product(wo[l, rows], dyt[ALL]).astype(BF)
            om[:, lanes(n * dim, dim)] = part.T

            @pl.when(n == 0)
            def _():
                dot_heads[ALL] = part

    def back_mlp(l):
        @pl.loop(0, seq // BAND)
        def _(r):
            rows = pl.ds(pl.multiple_of(r * BAND, BAND), BAND)

            @pl.loop(0, ff // STRIP)
            def _(i):
                gate_at, up_at = lanes(dim + LANE + i * STRIP, STRIP), lanes(dim + LANE + ff + i * STRIP, STRIP)
                gate, up = z[l, rows, gate_at].astype(F32), z[l, rows, up_at].astype(F32)
                d = om[rows, lanes(dim + i * STRIP, STRIP)].astype(F32)
                sig = jax.nn.sigmoid(gate)
                du = d * up
                z[l, rows, gate_at] = (du * sig + du * gate * (sig * (1.0 - sig))).astype(BF)
                z[l, rows, up_at] = (d * (gate * sig)).astype(BF)

    def back_heads(l):
        key_lo, key_hi, val_lo, val_hi = heads(l)
        slot_rows(ksl, key_lo, key_hi)
        slot_rows(vsl, val_lo, val_hi)
        slot_cols(kts, key_lo)
        dkv[ALL] = jnp.zeros(dkv.shape, F32)
        flip(lambda at: qr[l, :, lanes(at, WIDE)], qt, dim)
        for at in range(0, dim, LANE):
            pair = slice(at, at + LANE)
            turned_q[:, pair] = pltpu.roll(qr[l, :, pair].astype(F32), HEAD, 1).astype(BF)
            turned_o[:, pair] = pltpu.roll(om[:, pair].astype(F32), HEAD, 1).astype(BF)

    def back_quad(l):
        @pl.loop(0, dim // WIDE)
        def _(g):
            quad(l, g)

    def quad(l, g):
        cols = pl.ds(pl.multiple_of(g * WIDE, WIDE), WIDE)
        scores[ALL] = product(ksl[ALL], qt[cols])
        dscores[ALL] = product(vsl[ALL], dot_heads[cols])

        @pl.loop(0, SIDE)
        def _(i):
            for half in range(PAIR):
                at, blocks = chances(i, half)
                given = [p * dscores[keys, at].astype(BF).astype(F32) for keys, p in blocks]
                total = sum(jnp.sum(v, axis=0, keepdims=True) for v in given)
                for (keys, p), v in zip(blocks, given):
                    pcat[keys, at] = p.astype(BF)
                    dscat[keys, at] = (v - p * total).astype(BF)
        dq = product(kts[ALL], dscat[ALL]).astype(BF).T
        back = dq.astype(F32) * cos_ref[ALL] - product(dq, turn_ref[ALL]) * sin_ref[ALL]
        z[l, :, cols] = (back * 0.125).astype(BF)
        def pieces(left, even, odd):
            for i in range(SIDE):
                pair = lanes(g * WIDE + i // PAIR * LANE, LANE)
                yield product(left[i * seq:(i + 1) * seq, :], odd(pair) if i % PAIR else even(pair))

        dkv[0] += sum(pieces(dscat, lambda at: qr[l, :, at], lambda at: turned_q[:, at]))
        dkv[1] += sum(pieces(pcat, lambda at: turned_o[:, at], lambda at: om[:, at]))

    def back_keys(l):
        dk = dkv[0].astype(BF)
        turned = dk.astype(F32) * cos_ref[:, :LANE] - product(dk, turn_ref[:LANE, :LANE]) * sin_ref[:, :LANE]
        first = lax.broadcasted_iota(jnp.int32, turned.shape, 1) < HEAD
        z[l, :, dim:dim + LANE] = jnp.where(first, turned, dkv[1]).astype(BF)

    def back_in(l, half):
        width = wi.shape[PAIR] // 5
        at = slice(PAIR * half * width, (PAIR + TRIO * half) * width)
        part = product(wi[l, :, at], z[l, :, at], ((1,), (1,)))
        dht[ALL] = dht[ALL] + part if half else part

    def back_norm(l):
        dy, dst = upstream[l], (gx_ref, middle)[l]
        for i in range(dim // WIDE):
            cols = slice(i * WIDE, (i + 1) * WIDE)
            h[l, :, cols] = dht[cols].T.astype(BF)
        sc[l] = jnp.zeros(sc.shape[1:], F32)

        @pl.loop(0, seq // BAND, unroll=SIDE)
        def _(r):
            rows = pl.ds(pl.multiple_of(r * BAND, BAND), BAND)
            v = entry[l][rows].astype(F32)
            v = v - jnp.mean(v, axis=-1, keepdims=True)
            scale = lax.rsqrt(jnp.mean(v * v, axis=-1, keepdims=True) + 1e-6)
            hat = v * scale
            d = h[l, rows].astype(F32)
            each = (d * hat).reshape(SIDE, ROW, dim)
            sc[l] += (each[0] + each[1]) + (each[PAIR] + each[TRIO])
            d = d * gain_ref[l:l + 1]
            d = scale * (d - jnp.mean(d, axis=-1, keepdims=True) - hat * jnp.mean(d * hat, axis=-1, keepdims=True))
            dst[rows] = (dy[rows].astype(F32) + d.astype(BF).astype(F32)).astype(BF)

    def do_norm(l):
        if l == 0:
            links.arrive(("sc",), gains.at[pl.ds(0, OTHERS)])
            gain_ref[ALL] = jnp.sum(gains[ALL], axis=0)
        normalise(l, entry[l])
        for i in range(dim // WIDE):
            flat = h[l, :, i * WIDE:(i + 1) * WIDE].T
            size = ht.shape[TRIO]
            for b in range(ROW):
                lo, hi = max(b * size, i * WIDE), min((b + 1) * size, (i + 1) * WIDE)
                if lo < hi:
                    ht[l, b // PAIR, b % PAIR, lo - b * size:hi - b * size] = flat[lo - i * WIDE:hi - i * WIDE]

    def do_project(l):
        ready(PAIR * l)
        project(l)

    def do_mlp(l):
        mlp(l)
        flip(lambda at: om[:, lanes(at, WIDE)], omt.at[l], om.shape[1], dim)

    def do_put(l):
        ready(PAIR * l + 1)
        put_out(l, hid.at[0] if l == 0 else y_ref)

    stages.update(
        norm=do_norm, project=do_project, attend=attend, mlp=do_mlp, put=do_put, back_out=back_out, back_mlp=back_mlp, back_heads=back_heads,
        back_quad=back_quad, back_keys=back_keys, back_in=back_in, back_norm=back_norm, send_h=send_h, pass_h=pass_h, send_m=send_m,
        pass_m=pass_m, send_y=send_y, pass_y=pass_y, far_y=far_y, send_z=send_z, rest_z=rest_z, pass_z=pass_z, twin_z=twin_z, far_z=far_z,
        send_scale=send_scale, own_z=lambda: keep(z.at[0], z_a), own_y=lambda: keep(middle, dy_a))
    for kind, *task in order:
        stages[kind](*task)
    for l in range(PAIR):
        arrive_h(l)
        arrive_m(l)
        arrive_scale(l)
    arrive_y(1)
    for l, axis in z_out:
        arrive_z(l, axis)
    for copy in stored:
        copy.wait()
    shared.drain()
    links.drain()


def run_layers(x, dy, scale, w_in, w_out, freq, starts=(ZERO, 10.0, 20.0, 30.0)):
    seq, dim = x.shape
    proj, cat = w_in.shape[PAIR], ROW * w_out.shape[1]
    wide = proj + LANE
    hbm, vmem = pl.BlockSpec(memory_space=pltpu.HBM), pl.BlockSpec(memory_space=pltpu.VMEM)
    out = lambda *shape, dtype=BF: jax.ShapeDtypeStruct(shape, dtype)
    buffer = lambda *shape, dtype=BF: pltpu.VMEM(shape, dtype)
    sem = pltpu.SemaphoreType.DMA
    line = ROW * seq
    return pl.pallas_call(
        functools.partial(layers_kernel, layers_order(*w_in.shape[1:], *w_out.shape[1:], seq, starts)),
        out_shape=(out(seq, dim), out(seq, dim), *[out(ROW, SIDE, dim // ROW, seq)] * SIDE, *[out(ROW, cat // ROW, seq)] * PAIR, out(line, dim),
                   *[out(line, wide // ROW)] * PAIR, out(seq, wide), out(seq, dim), out(PAIR, ROW, ROW, dim, dtype=F32),
                   out(PAIR, PAIR, PAIR, cat // 16, seq), out(PAIR, PAIR, PAIR, seq // PAIR, wide // ROW)),
        in_specs=[vmem, hbm, hbm] + [vmem] * TRIO,
        out_specs=[vmem] * PAIR + [hbm] * 14,
        scratch_shapes=[
            buffer(PAIR, dim, proj), buffer(PAIR, cat, dim), buffer(PAIR, seq, wide), buffer(seq, cat), buffer(PAIR, seq, dim),
            buffer(PAIR, seq, dim), buffer(PAIR, seq, dim),
            buffer(WIDE, SIDE * seq), buffer(SIDE * seq, WIDE), buffer(SIDE * seq, WIDE), buffer(seq, dim), buffer(seq, dim),
            buffer(SIDE * seq, seq, dtype=F32), buffer(SIDE * seq, seq, dtype=F32), buffer(SIDE * seq, seq), buffer(SIDE * seq, seq),
            buffer(seq, WIDE, dtype=F32), buffer(seq, WIDE, dtype=F32), buffer(WIDE, WIDE),
            buffer(dim, seq), buffer(dim, seq), buffer(dim, seq, dtype=F32), buffer(PAIR, seq, LANE, dtype=F32),
            buffer(PAIR, cat, seq), buffer(PAIR, SIDE, PAIR, dim // ROW, seq), buffer(dim, seq), buffer(PAIR, ROW, dim, dtype=F32),
            buffer(ROW, ROW, dim, dtype=F32), buffer(ROW, dim, dtype=F32), buffer(ROW, dim, dtype=F32),
            sem((SIDE,)), sem((13,)), sem((15,)), sem((107,)), sem((13,)), sem((HEAD,)),
        ],
        compiler_params=pltpu.CompilerParams(collective_id=PAIR, has_side_effects=True, vmem_limit_bytes=67043328),
        name="run_layers",
    )(scale, w_in, w_out, x, dy, freq)


PARTS = (("i", "x", "z", "y", 0, STRIP), ("i", "x", "z", "y", STRIP, 384), ("i", "x", "y", "z", 0, STRIP), ("i", "x", "y", "z", STRIP, 384),
         ("o", "y", "z", "y", 0, 384), ("o", "z", "y", "z", 384, 384))


def reduce_order(rows, rows_b, starts):
    rate = 11650.0
    tasks = []
    sizes = {"y": WIDE * 896 / (PAIR * rate), "z": WIDE * 896 / (PAIR * rate), "x": WIDE * 768 / (PAIR * rate)}
    for axis in "yzx":
        size = sizes[axis]
        tasks.append((("swap", axis), (0, 0), starts[PAIR] if axis == "x" else starts[TRIO], [], [],
                      [((axis, by), size * n) for by, n in ((-1, 0.5), (1, 1), (-1, 1), (1, 1))], SHORT))
        tasks.append((("relay", axis), (0, 0), ZERO, [(("swap", axis), 0)], [], [((axis, -1), size / PAIR)], SHORT))
        for o, needs in ((1, [(("swap", axis), 1)]), (-1, [(("swap", axis), PAIR)]), (PAIR, [(("swap", axis), TRIO), (("relay", axis), 0)])):
            tasks.append((("near", axis, o), (0, PAIR), ZERO, needs, [], [("chip", 1.6)], QUICK))
    tasks.append((("fetch", 0), (5, 0), ZERO, [], [("make", 1, len(PARTS) - 1)], [], QUICK))
    for l in (1, 0):
        late = 1 - l
        for c, (kind, first, then, last, at, width) in enumerate(PARTS):
            needs, cost = [], 1.6 * width / STRIP
            if l == 0:
                needs = [(("near", last if kind == "i" else "x", o), 0) for o in AROUND]
            tasks.append((("make", l, c), (9 * late, c), starts[late], needs, [] if l else [("fetch", 0)], [], cost))
            full = SIDE * SIDE * (rows if kind == "i" else rows_b) * width / rate
            sends = [[((first, by), full / ROW) for by in BOTH], [((first, by), full / SIDE) for by in BOTH],
                     [((then, o), full / 16) for o in (1, -1, 1)], []]
            piece = full / 16
            sends += [[((then, o), piece) for o in (1, -1, 1)], [((last, by), SIDE * piece) for by in BOTH],
                      [((last, by), PAIR * piece) for by in BOTH], []]
            for s in range(ROW):
                task = ("sum", l, c, s)
                needs = [(("sum", l, c, s - 1), k) for k in range(len(sends[s - 1]))] if s else []
                tasks.append((task, (late, -s), ZERO, needs, [("make", l, c)] if s == 0 else [("sum", l, c, s - 1)], sends[s], SHORT))
    return plan(tasks)


def reduce_kernel(order, *refs):
    hy, hz, mx = refs[0:PAIR], refs[PAIR:SIDE], refs[SIDE:6]
    yx1, zy1, zz1, z0, y0, sc = refs[6:12]
    oa, ob = refs[12:14]
    n = len(PARTS)
    total, half, full, small, front = (refs[14 + k * n:14 + (k + 1) * n] for k in range(5))
    (hbuf, zbuf, mbuf, ybuf, scbuf, rz, ry, ssem, rsem, isem, osem) = refs[14 + 5 * n:]
    position = chip_position()
    x, y, zc, core = position
    place = {"x": x, "y": y, "z": zc}
    twin = device_at(x, y, zc, 1 - core)
    spots, peers = around(position)

    def spot(axis, o):
        return spots[axis, o % SIDE]

    def peer(axis, o):
        return peers[axis, o % SIDE]

    seq, wide = z0.shape
    own = wide // ROW
    loads, moving = {}, []

    def load(key, src, dst):
        copy = pltpu.make_async_copy(src, dst, isem.at[len(moving)])
        moving.append(key)
        copy.start()
        loads[key] = copy

    def fetch(l):
        if not l:
            load(("h", 0, "y"), hy[0], hbuf.at[0, 0])
        else:
            load(("z", 1, "z"), zz1, zbuf.at[1, 1])
        load(("h", l, "z"), hz[l], hbuf.at[l, 1])
        load(("m", l), mx[l], mbuf.at[l])
        if l:
            load(("y", 1), yx1, ybuf.at[1])
        load(("s", l), sc.at[l], scbuf.at[l])

    load(("z", 1, "y"), zy1, zbuf.at[1, 0])
    load(("h", 1, "y"), hy[1], hbuf.at[1, 0])
    done = set()

    def loaded(*keys):
        for key in keys:
            if key not in done:
                loads[key].wait()
                done.add(key)

    announce([peer(axis, o) for axis in "xyz" for o in AROUND] + [twin])
    fetch(1)
    links = Links(ssem, rsem)

    def columns(axis, o):
        return lanes(((0 if axis == "y" else SIDE) + spot(axis, o)) * own, own)

    def tokens(axis, o, index):
        return pl.ds(pl.multiple_of((PAIR * spot(axis, o) + index) * seq, seq), seq)

    def target(axis):
        return ybuf.at[0] if axis == "x" else zbuf.at[0, "yz".index(axis)]

    def leaving(axis):
        return dict(batch=("swap", axis), whole=target(axis).at[pl.ds(0, OTHERS * seq + seq // PAIR)])

    def half_at(axis, o, k):
        start = (PAIR * spot(axis, o) + core) * seq + k * (seq // PAIR)
        return target(axis).at[pl.ds(pl.multiple_of(start, seq // PAIR), seq // PAIR)]

    def relay_of(axis):
        return ry if axis == "x" else rz.at["yz".index(axis)]

    def swap(axis):
        def part(o, rows=slice(None)):
            return y0.at[rows] if axis == "x" else z0.at[rows, columns(axis, o)]

        mine = target(axis).at[tokens(axis, 0, core)]
        links.send(("relay", axis), part(PAIR, pl.ds(seq // PAIR, seq // PAIR)), relay_of(axis), peer(axis, -1), **leaving(axis))
        for by in BOTH:
            links.send(("swap", axis, by), part(by), mine, peer(axis, by), **leaving(axis))
        links.send(("swap", axis, PAIR), part(PAIR, pl.ds(0, seq // PAIR)), half_at(axis, 0, 0), peer(axis, PAIR), **leaving(axis))
        links.send(("near", axis), part(0), mine, twin, **leaving(axis))
        load(("own", axis), part(0), mine)

    def relay(axis):
        links.arrive(("relay", axis), relay_of(axis))
        links.send(("relayed", axis), relay_of(axis), half_at(axis, 1, 1), peer(axis, -1), **leaving(axis))

    def near(axis, o):
        landed = target(axis).at[tokens(axis, -o, core)]
        if o == PAIR:
            links.arrive(("swap", axis, PAIR), half_at(axis, PAIR, 0))
            links.arrive(("relayed", axis), half_at(axis, PAIR, 1))
        else:
            links.arrive(("swap", axis, o), landed)
        links.send(("near", axis), landed, landed, twin, **leaving(axis))

    def joined(axis):
        if axis not in done:
            done.add(axis)
            loaded(("own", axis))
            links.arrive(("near", axis), target(axis).at[pl.ds(0, SIDE * seq)])

    def joined_lanes(ref, l, i):
        return jnp.concatenate([ref[l, i, k].reshape(-1, ref.shape[-1]) for k in range(ROW)], axis=1)

    def make(l, c):
        kind, first, then, last, at, width = PARTS[c]
        if kind == "i":
            i = "yz".index(last)
            loaded(("h", l, last))
            if l:
                loaded(("z", l, last))
            else:
                joined(last)
            size = total[c].shape[TRIO]
            for lo in range(0, width, WIDE):
                hi = min(width, lo + WIDE)
                part = product(joined_lanes(hbuf, l, i), zbuf[l, i, :, at + lo:at + hi])
                for r in range(16):
                    total[c][l, r // SIDE, r % SIDE, :, lo:hi] = part[r * size:(r + 1) * size]
            return
        loaded(("m", l), ("s", l))
        if l:
            loaded(("y", l))
        else:
            joined("x")
        part = product(jnp.concatenate([mbuf[l, k] for k in range(ROW)], axis=1), ybuf[l, :, at:at + width])
        size = total[c].shape[TRIO]

        def put(r, value):
            total[c][(l, r // SIDE, r % SIDE) if first == "y" else (l, r % SIDE, r // SIDE)] = value

        for r in range(part.shape[0] // size):
            put(r, part[r * size:(r + 1) * size])
        gain = jnp.sum(jnp.sum(scbuf[l, :, :, at:at + width], axis=0), axis=0, keepdims=True)
        row = lax.broadcasted_iota(jnp.int32, (size, width), 0)
        put(15, jnp.where(row == 0, gain, ZERO))

    def area(l, c, o, whole):
        kind, first, then, last, at, width = PARTS[c]
        inner = (spot(then, whole) if isinstance(whole, int) else whole)
        outer = spot(last, o)
        if kind == "i":
            cols = lanes(((0 if last == "y" else SIDE) + outer) * own + at, width)
            return oa.at[l, inner, :, cols]
        cols = pl.ds(at, width)
        return ob.at[l, outer, inner, :, cols] if last == "y" else ob.at[l, inner, outer, :, cols]

    def add(l, c, s):
        kind, first, then, last, at, width = PARTS[c]
        t = total[c].at[l]
        sums = dict(batch=(l, c, 0), whole=t)
        lines = dict(batch=(l, c, 1), whole=t.at[pl.ds(0, PAIR)])
        singles = dict(batch=(l, c, PAIR), whole=t.at[pl.ds(0, PAIR), pl.ds(0, TRIO)])
        if s == 0:
            far = t.at[spot(first, PAIR)]
            for k, by in enumerate(BOTH):
                links.send((l, c, "half"), far.at[pl.ds(PAIR * k, PAIR)], half[c].at[l, k], peer(first, by), **sums)
        elif s == 1:
            links.arrive((l, c, "half"), half[c].at[l])
            for k, by in enumerate(BOTH):
                mine = t.at[spot(first, by)]
                add_into(mine.at[pl.ds(PAIR * k, PAIR)], half[c].at[l, k])
                links.send((l, c, "full"), mine, full[c].at[l, k], peer(first, by), **sums)
        elif s == PAIR:
            mine = t.at[spot(first, 0)]
            links.arrive((l, c, "full"), full[c].at[l])
            for k in range(PAIR):
                add_into(mine, full[c].at[l, k])
            for k, o in enumerate(AROUND):
                links.send((l, c, "small"), mine.at[spot(then, o)], small[c].at[l, k], peer(then, o), **singles)
        elif s == TRIO:
            links.arrive((l, c, "small"), small[c].at[l])
            mine = t.at[spot(first, 0), spot(then, 0)]
            front[c][l] = (mine[ALL] + small[c][l, 0]) + (small[c][l, 1] + small[c][l, PAIR])
        elif s == SIDE:
            src, dst = front[c].at[l], area(l, c, 0, 0)
            for o in AROUND:
                links.send((l, c, "a1"), src, dst, peer(then, o), **singles)
            copy = pltpu.make_async_copy(src, dst, osem.at[l, c])
            copy.start()
            loads["front", l, c] = copy
        elif s == 5:
            loaded(("front", l, c))
            links.arrive((l, c, "a1"), t.at[0, pl.ds(0, TRIO)])
            line = area(l, c, 0, slice(None))
            for by in BOTH:
                links.send((l, c, "a2"), line, line, peer(last, by), **lines)
        elif s == 6:
            links.arrive((l, c, "a2"), t.at[pl.ds(0, PAIR)])
            for k, by in enumerate(BOTH):
                part = area(l, c, -by, pl.ds(PAIR * k, PAIR))
                links.send((l, c, "a3"), part, part, peer(last, by), **sums)
        else:
            links.arrive((l, c, "a3"), area(l, c, PAIR, slice(None)))

    stages = {"swap": swap, "relay": relay, "near": near, "fetch": fetch, "make": make, "sum": add}
    for kind, *task in order:
        stages[kind](*task)
    links.drain()


def add_into(dst, src):
    @pl.loop(0, dst.shape[0])
    def _(i):
        if len(dst.shape) == SIDE:
            for j in range(dst.shape[1]):
                dst[i, j] += src[i, j]
        else:
            dst[i] += src[i]


def around(position):
    place, core = dict(zip("xyz", position)), position[TRIO]
    spots = {(axis, o): step(place[axis], o) for axis in "xyz" for o in range(SIDE)}
    peers = {}
    for axis in "xyz":
        for o in range(1, SIDE):
            moved = {**place, axis: spots[axis, o]}
            peers[axis, o] = device_at(moved["x"], moved["y"], moved["z"], core)
    return spots, peers


def reduce_gradients(operands, starts=(ZERO, ZERO, 26.0, 1.0)):
    hbm = pl.BlockSpec(memory_space=pltpu.HBM)
    h_rows, m_rows, y_cols, z_cols, z_own, y_own, scale_parts = operands
    part, part_b = h_rows[0].shape[PAIR] // SIDE, (m_rows[0].shape[1] + BAND) // 16
    (line, dim), wide = y_cols.shape, z_own.shape[1]
    out = lambda *shape: jax.ShapeDtypeStruct(shape, F32)
    sem = pltpu.SemaphoreType.DMA

    def buffers(*lead):
        return [pltpu.VMEM((PAIR, *lead, part if e[0] == "i" else part_b, e[5]), F32) for e in PARTS]

    return pl.pallas_call(
        functools.partial(reduce_kernel, reduce_order(part, part_b, starts)),
        out_shape=(out(PAIR, SIDE, part, wide), out(PAIR, SIDE, SIDE, part_b, dim)),
        in_specs=[hbm] * 12,
        out_specs=[hbm] * PAIR,
        scratch_shapes=[
            *buffers(SIDE, SIDE), *buffers(PAIR, PAIR), *buffers(PAIR, SIDE), *buffers(TRIO), *buffers(),
            pltpu.VMEM((PAIR, PAIR, *h_rows[0].shape), BF), pltpu.VMEM((PAIR, PAIR, line, wide // ROW), BF), pltpu.VMEM((PAIR, *m_rows[0].shape), BF),
            pltpu.VMEM((PAIR, line, dim), BF), pltpu.VMEM(scale_parts.shape, F32),
            pltpu.VMEM((PAIR, z_own.shape[0] // PAIR, wide // ROW), BF), pltpu.VMEM((y_own.shape[0] // PAIR, dim), BF),
            sem((39,)), sem((90,)), sem((14,)), sem((PAIR, len(PARTS))),
        ],
        compiler_params=pltpu.CompilerParams(collective_id=1, has_side_effects=True, vmem_limit_bytes=67043328),
        name="reduce_gradients",
    )(*h_rows, *m_rows, y_cols, *z_cols, z_own, y_own, scale_parts)


def finish_kernel(count, in_ref, out_ref, y_ref, gx_ref, in_grad, out_grad, y_out, gx_out, scale_out, in_buf, out_buf, y_buf, gx_buf, came, left):
    moves = [(out_ref.at[l, p], out_buf.at[l, pl.ds(SIDE * p, SIDE)]) for l in range(PAIR) for p in range(SIDE)]
    moves += [(y_ref, y_buf), (gx_ref, gx_buf)]
    size, width = in_buf.shape[PAIR:]
    moves += [(in_ref.at[l, p, :, pl.ds(0, width)], in_buf.at[l, p]) for l in range(PAIR) for p in range(SIDE)]
    loads = [pltpu.make_async_copy(src, dst, came.at[k]) for k, (src, dst) in enumerate(moves)]
    for copy in loads:
        copy.start()
    stores = []

    def store(src, dst):
        copy = pltpu.make_async_copy(src, dst, left.at[len(stores)])
        copy.start()
        stores.append(copy)

    for l in range(PAIR):
        for p in range(SIDE):
            loads[SIDE * l + p].wait()
        store(out_buf.at[l, pl.ds(0, 15)], out_grad.at[l])
    for k, (src, dst) in enumerate(((y_buf, y_out), (gx_buf, gx_out))):
        loads[ROW + k].wait()
        store(src, dst)
    me = lax.axis_index("fsdp")
    for l in range(PAIR):
        for f in range(ROW):
            @pl.when(me == f)
            def _():
                scale_out[l:l + 1] = out_buf[l, 15, 0:1, f * count:(f + 1) * count]
    for l in range(PAIR):
        for p in range(SIDE):
            loads[10 + SIDE * l + p].wait()
            store(in_buf.at[l, p], in_grad.at[l, pl.ds(p * size, size)])
    for copy in stores:
        copy.wait()


def finish(in_sums, out_sums, y, gx, rows, proj):
    hbm = pl.BlockSpec(memory_space=pltpu.HBM)
    out = lambda *shape, dtype=F32: jax.ShapeDtypeStruct(shape, dtype)
    size, (depth, dim) = in_sums.shape[PAIR], out_sums.shape[TRIO:]
    in_grad, out_grad, y_out, gx_out, scale = pl.pallas_call(
        functools.partial(finish_kernel, rows),
        out_shape=(out(PAIR, rows, proj), out(PAIR, 15, depth, dim), out(*y.shape, dtype=BF), out(*gx.shape, dtype=BF), out(PAIR, rows)),
        in_specs=[hbm] * SIDE,
        out_specs=[hbm] * SIDE + [pl.BlockSpec(memory_space=pltpu.VMEM)],
        scratch_shapes=[
            pltpu.VMEM((PAIR, SIDE, size, proj), F32), pltpu.VMEM((PAIR, 16, depth, dim), F32), pltpu.VMEM(y.shape, BF), pltpu.VMEM(gx.shape, BF),
            pltpu.SemaphoreType.DMA((18,)), pltpu.SemaphoreType.DMA((12,)),
        ],
        compiler_params=pltpu.CompilerParams(vmem_limit_bytes=67043328),
        name="finish",
    )(in_sums, out_sums, y, gx)
    return y_out[None], gx_out[None], scale, in_grad, out_grad.reshape(PAIR, 15 * depth, dim)


def solution(mesh):
    fsdp_size = mesh.shape["fsdp"]
    batch_spec = P(("dp", "fsdp"), None, None)
    scale_spec = P(None, "fsdp")
    weight_spec = P(None, "fsdp", None)

    def device_step(x_in, grad_y, norm_scale, w_in, w_out):
        n_layers = w_in.shape[0]
        seq_len, model_dim = x_in.shape[1:]
        proj_dim = w_in.shape[PAIR]
        ff_dim = w_out.shape[1] * fsdp_size - model_dim
        head_dim = (proj_dim - model_dim - PAIR * ff_dim) // PAIR
        rows, rows_out = norm_scale.shape[1], w_out.shape[1]
        half_dim = head_dim // PAIR
        freq = 10000.0 ** (-np.arange(half_dim, dtype=np.float32) * 2.0 / head_dim)
        freq = jnp.asarray(np.tile(freq.astype(np.float32), (ROW, LANE // half_dim)))
        hidden, grad_hidden, *rest = run_layers(x_in[0], grad_y[0], norm_scale, w_in, w_out, freq)
        in_sums, out_sums = reduce_gradients((rest[0:SIDE], rest[SIDE:6], rest[6], rest[OTHERS:9], rest[9], rest[10], rest[11]))
        return finish(in_sums, out_sums, hidden, grad_hidden, rows, proj_dim)

    return jax.shard_map(
        device_step,
        mesh=mesh,
        in_specs=(batch_spec, batch_spec, scale_spec, weight_spec, weight_spec),
        out_specs=(batch_spec, batch_spec, scale_spec, weight_spec, weight_spec),
        check_vma=False,
    )
```
